128 devices in a mesh: dp: 2 (over core), fsdp: 64 (over z, y, x).
Axes of the slice: x: 4, y: 4, z: 4, core: 2. Of those that a mesh axis runs over, the one named last changes fastest.
Arguments:
- dec_in: bfloat16 [256, 512, 768], P(('dp', 'fsdp'))
- enc_out: bfloat16 [256, 768, 768], P(('dp', 'fsdp'))
- src_lens: int32 [256], P(('dp', 'fsdp'))
- tgt_lens: int32 [256], P(('dp', 'fsdp'))
- y_cot: bfloat16 [256, 512, 768], P(('dp', 'fsdp'))
- attn_w: bfloat16 [6144, 768], P('fsdp')
- ffn_w: bfloat16 [6144, 768], P('fsdp')
- vec_params: bfloat16 [14592], P('fsdp')
Outputs:
- output 1: bfloat16 [256, 512, 768], P(('dp', 'fsdp'))
- output 2: bfloat16 [256, 512, 768], P(('dp', 'fsdp'))
- output 3: bfloat16 [256, 768, 768], P(('dp', 'fsdp'))
- output 4: float32 [6144, 768], P('fsdp')
- output 5: float32 [6144, 768], P('fsdp')
- output 6: float32 [14592], P('fsdp')
All inputs are finite; a program needn't handle non-finite values.
Results may differ from the reference program's by a relative error of at most 0.016307.
Values are sent between devices in bfloat16 or wider.
A program may use at most 1 GiB of HBM per device.

```python
import jax
import jax.numpy as jnp
from jax import lax

BATCH_ALL = 256
TGT_LEN = 512
SRC_LEN = 768
D_MODEL = 768
NUM_HEADS = 12
FFN_DIM = 3072
HEAD_DIM = D_MODEL // NUM_HEADS
VEC_LEN = 15 * D_MODEL + FFN_DIM


def setup_inputs(seed: int = 0) -> dict:
    key_list = jax.random.split(jax.random.key(seed), 10)
    token_shift = 0.5 * jax.random.normal(key_list[0], (BATCH_ALL, TGT_LEN, 1), jnp.float32)
    column_mean = 0.3 * jax.random.normal(key_list[1], (1, 1, D_MODEL), jnp.float32)
    x_val = jax.random.normal(key_list[2], (BATCH_ALL, TGT_LEN, D_MODEL), jnp.float32) + token_shift + column_mean
    enc_val = jax.random.normal(key_list[3], (BATCH_ALL, SRC_LEN, D_MODEL), jnp.float32)
    src_draw = jax.random.randint(key_list[4], (BATCH_ALL,), SRC_LEN // 4, SRC_LEN + 1)
    tgt_draw = jax.random.randint(key_list[5], (BATCH_ALL,), TGT_LEN // 4, TGT_LEN + 1)
    first_row = jnp.arange(BATCH_ALL) == 0
    src_lens = jnp.where(first_row, SRC_LEN, src_draw).astype(jnp.int32)
    tgt_lens = jnp.where(first_row, TGT_LEN, tgt_draw).astype(jnp.int32)
    dy_val = jax.random.normal(key_list[6], (BATCH_ALL, TGT_LEN, D_MODEL), jnp.float32)
    attn_val = jax.random.normal(key_list[7], (8 * D_MODEL, D_MODEL), jnp.float32) * D_MODEL ** -0.5
    row_ids = jnp.arange(2 * FFN_DIM)[:, None]
    ffn_scale = jnp.where(row_ids < FFN_DIM, D_MODEL ** -0.5, FFN_DIM ** -0.5)
    ffn_val = jax.random.normal(key_list[8], (2 * FFN_DIM, D_MODEL), jnp.float32) * ffn_scale
    slot_ids = jnp.arange(VEC_LEN) // D_MODEL
    is_gain = ((slot_ids == 9) | (slot_ids == 11) | (slot_ids == 13)).astype(jnp.float32)
    vec_val = 0.3 * jax.random.normal(key_list[9], (VEC_LEN,), jnp.float32) + is_gain
    return {'dec_in': x_val.astype(jnp.bfloat16), 'enc_out': enc_val.astype(jnp.bfloat16), 'src_lens': src_lens, 'tgt_lens': tgt_lens, 'y_cot': dy_val.astype(jnp.bfloat16), 'attn_w': attn_val.astype(jnp.bfloat16), 'ffn_w': ffn_val.astype(jnp.bfloat16), 'vec_params': vec_val.astype(jnp.bfloat16)}


def layer_norm(resid_in, vec_f, slot_idx):
    ln_gain = vec_f[slot_idx * D_MODEL:(slot_idx + 1) * D_MODEL]
    ln_shift = vec_f[(slot_idx + 1) * D_MODEL:(slot_idx + 2) * D_MODEL]
    row_mean = jnp.mean(resid_in, axis=-1, keepdims=True)
    centred = resid_in - row_mean
    row_var = jnp.mean(centred * centred, axis=-1, keepdims=True)
    return centred * lax.rsqrt(row_var + 1e-5) * ln_gain + ln_shift


def attend(q_rows, k_rows, v_rows, key_mask):
    q_heads = q_rows.astype(jnp.float32).reshape(q_rows.shape[0], NUM_HEADS, HEAD_DIM)
    k_heads = k_rows.astype(jnp.float32).reshape(k_rows.shape[0], NUM_HEADS, HEAD_DIM)
    v_heads = v_rows.astype(jnp.float32).reshape(v_rows.shape[0], NUM_HEADS, HEAD_DIM)
    scores = jnp.einsum('qhd,khd->hqk', q_heads, k_heads)
    scores = jnp.where(key_mask[None], scores, -1e30)
    attn_prob = jax.nn.softmax(scores, axis=-1).astype(jnp.bfloat16).astype(jnp.float32)
    attn_out = jnp.einsum('hqk,khd->qhd', attn_prob, v_heads)
    return attn_out.reshape(q_rows.shape[0], D_MODEL).astype(jnp.bfloat16)


def layer_one(x_row, enc_row, src_n, tgt_n, attn_f, ffn_f, vec_f):
    def linear(h_rows, slot_idx):
        w_mat = attn_f[slot_idx * D_MODEL:(slot_idx + 1) * D_MODEL]
        b_vec = vec_f[slot_idx * D_MODEL:(slot_idx + 1) * D_MODEL]
        return jnp.dot(h_rows, w_mat, preferred_element_type=jnp.float32) + b_vec

    x_f = x_row.astype(jnp.float32)
    enc_f = enc_row.astype(jnp.float32)
    tgt_pos = jnp.arange(TGT_LEN)
    self_mask = (tgt_pos[None, :] <= tgt_pos[:, None]) & (tgt_pos[None, :] < tgt_n)
    cross_mask = jnp.broadcast_to(jnp.arange(SRC_LEN)[None, :] < src_n, (TGT_LEN, SRC_LEN))
    q_self = (linear(x_f, 0) * 0.125).astype(jnp.bfloat16)
    k_self = linear(x_f, 1).astype(jnp.bfloat16)
    v_self = linear(x_f, 2).astype(jnp.bfloat16)
    o_self = attend(q_self, k_self, v_self, self_mask).astype(jnp.float32)
    h_one = layer_norm(x_f + linear(o_self, 3), vec_f, 9).astype(jnp.bfloat16).astype(jnp.float32)
    q_cross = (linear(h_one, 4) * 0.125).astype(jnp.bfloat16)
    k_cross = linear(enc_f, 5).astype(jnp.bfloat16)
    v_cross = linear(enc_f, 6).astype(jnp.bfloat16)
    o_cross = attend(q_cross, k_cross, v_cross, cross_mask).astype(jnp.float32)
    h_two = layer_norm(h_one + linear(o_cross, 7), vec_f, 11).astype(jnp.bfloat16).astype(jnp.float32)
    up_proj = jnp.dot(h_two, ffn_f[:FFN_DIM].T, preferred_element_type=jnp.float32) + vec_f[15 * D_MODEL:]
    gelu_out = jax.nn.gelu(up_proj, approximate=False).astype(jnp.bfloat16).astype(jnp.float32)
    down_proj = jnp.dot(gelu_out, ffn_f[FFN_DIM:], preferred_element_type=jnp.float32) + vec_f[8 * D_MODEL:9 * D_MODEL]
    return layer_norm(h_two + down_proj, vec_f, 13).astype(jnp.bfloat16)


def reference(dec_in, enc_out, src_lens, tgt_lens, y_cot, attn_w, ffn_w, vec_params):
    attn_f = attn_w.astype(jnp.float32)
    ffn_f = ffn_w.astype(jnp.float32)
    vec_f = vec_params.astype(jnp.float32)

    def one_sample(grad_sums, sample):
        x_row, enc_row, src_n, tgt_n, cot_row = sample

        def forward(x_arg, enc_arg, attn_arg, ffn_arg, vec_arg):
            return layer_one(x_arg, enc_arg, src_n, tgt_n, attn_arg, ffn_arg, vec_arg)

        y_row, pull_back = jax.vjp(forward, x_row, enc_row, attn_f, ffn_f, vec_f)
        dx_row, denc_row, g_attn, g_ffn, g_vec = pull_back(cot_row)
        new_sums = (grad_sums[0] + g_attn, grad_sums[1] + g_ffn, grad_sums[2] + g_vec)
        return new_sums, (y_row, dx_row, denc_row)

    zero_sums = (jnp.zeros_like(attn_f), jnp.zeros_like(ffn_f), jnp.zeros_like(vec_f))
    grad_sums, outs_stack = lax.scan(one_sample, zero_sums, (dec_in, enc_out, src_lens, tgt_lens, y_cot))
    grad_scale = 1.0 / (BATCH_ALL * TGT_LEN)
    return outs_stack[0], outs_stack[1], outs_stack[2], grad_sums[0] * grad_scale, grad_sums[1] * grad_scale, grad_sums[2] * grad_scale
```

```python
import jax
import jax.numpy as jnp
from jax import lax
from jax.sharding import PartitionSpec as P

HEAD_DIM = 64
LN_EPS = 1e-5
MASK_FILL = -1e30


def norm_fwd(resid_in, ln_gain, ln_shift):
    row_mean = jnp.mean(resid_in, axis=-1, keepdims=True)
    centred = resid_in - row_mean
    inv_std = lax.rsqrt(jnp.mean(centred * centred, axis=-1, keepdims=True) + LN_EPS)
    normed = centred * inv_std
    return (normed * ln_gain + ln_shift).astype(jnp.bfloat16), normed, inv_std


def norm_bwd(d_out, normed, inv_std, ln_gain):
    d_norm = d_out * ln_gain
    d_resid = inv_std * (d_norm - jnp.mean(d_norm, axis=-1, keepdims=True) - normed * jnp.mean(d_norm * normed, axis=-1, keepdims=True))
    return d_resid, jnp.sum(d_out * normed, axis=(0, 1)), jnp.sum(d_out, axis=(0, 1))


def attn_fwd(q_heads, k_heads, v_heads, key_mask):
    scores = jnp.einsum('bthe,bshe->bhts', q_heads, k_heads, preferred_element_type=jnp.float32)
    scores = jnp.where(key_mask[:, None], scores, MASK_FILL)
    attn_prob = jax.nn.softmax(scores, axis=-1)
    attn_out = jnp.einsum('bhts,bshe->bthe', attn_prob.astype(jnp.bfloat16), v_heads, preferred_element_type=jnp.float32)
    return attn_out.astype(jnp.bfloat16), attn_prob


def attn_bwd(d_out, q_heads, k_heads, v_heads, attn_prob):
    d_prob = jnp.einsum('bthe,bshe->bhts', d_out, v_heads, preferred_element_type=jnp.float32)
    d_value = jnp.einsum('bhts,bthe->bshe', attn_prob.astype(jnp.bfloat16), d_out, preferred_element_type=jnp.float32)
    d_score = (attn_prob * (d_prob - jnp.sum(attn_prob * d_prob, axis=-1, keepdims=True))).astype(jnp.bfloat16)
    d_query = jnp.einsum('bhts,bshe->bthe', d_score, k_heads, preferred_element_type=jnp.float32)
    d_key = jnp.einsum('bhts,bthe->bshe', d_score, q_heads, preferred_element_type=jnp.float32)
    return d_query, d_key, d_value


def gelu_grad(up_proj):
    norm_cdf = 0.5 * (1.0 + lax.erf(up_proj * 0.7071067811865476))
    norm_pdf = 0.3989422804014327 * jnp.exp(-0.5 * up_proj * up_proj)
    return norm_cdf + up_proj * norm_pdf


def unpack_params(attn_full, ffn_full, vec_full):
    d_model = attn_full.shape[1]
    ffn_dim = ffn_full.shape[0] // 2
    vec_f = vec_full.astype(jnp.float32)
    return dict(attn_mats=attn_full.reshape(8, d_model, d_model), w_up=ffn_full[:ffn_dim], w_down=ffn_full[ffn_dim:], biases=vec_f[:15 * d_model].reshape(15, d_model), up_bias=vec_f[15 * d_model:])


def layer_forward(dec_in, enc_out, src_lens, tgt_lens, weights):
    n_batch, n_tgt, d_model = dec_in.shape
    n_src = enc_out.shape[1]
    n_heads = d_model // HEAD_DIM
    attn_mats = weights['attn_mats']
    biases = weights['biases']
    tgt_pos = jnp.arange(n_tgt)
    self_mask = (tgt_pos[None, None, :] <= tgt_pos[None, :, None]) & (tgt_pos[None, None, :] < tgt_lens[:, None, None])
    cross_mask = jnp.arange(n_src)[None, None, :] < src_lens[:, None, None]
    q_scale = jnp.array([0.125, 1.0, 1.0], jnp.float32)[:, None]
    qkv_self = jnp.einsum('btd,nde->btne', dec_in, attn_mats[0:3], preferred_element_type=jnp.float32) + biases[0:3]
    qkv_self = (qkv_self * q_scale).astype(jnp.bfloat16).reshape(n_batch, n_tgt, 3, n_heads, HEAD_DIM)
    o_self, p_self = attn_fwd(qkv_self[:, :, 0], qkv_self[:, :, 1], qkv_self[:, :, 2], self_mask)
    o_self = o_self.reshape(n_batch, n_tgt, d_model)
    resid_one = dec_in.astype(jnp.float32) + jnp.einsum('btd,de->bte', o_self, attn_mats[3], preferred_element_type=jnp.float32) + biases[3]
    h_one, normed_one, inv_one = norm_fwd(resid_one, biases[9], biases[10])
    q_cross = ((jnp.einsum('btd,de->bte', h_one, attn_mats[4], preferred_element_type=jnp.float32) + biases[4]) * 0.125).astype(jnp.bfloat16).reshape(n_batch, n_tgt, n_heads, HEAD_DIM)
    kv_cross = (jnp.einsum('bsd,nde->bsne', enc_out, attn_mats[5:7], preferred_element_type=jnp.float32) + biases[5:7]).astype(jnp.bfloat16).reshape(n_batch, n_src, 2, n_heads, HEAD_DIM)
    o_cross, p_cross = attn_fwd(q_cross, kv_cross[:, :, 0], kv_cross[:, :, 1], cross_mask)
    o_cross = o_cross.reshape(n_batch, n_tgt, d_model)
    resid_two = h_one.astype(jnp.float32) + jnp.einsum('btd,de->bte', o_cross, attn_mats[7], preferred_element_type=jnp.float32) + biases[7]
    h_two, normed_two, inv_two = norm_fwd(resid_two, biases[11], biases[12])
    up_proj = jnp.einsum('btd,fd->btf', h_two, weights['w_up'], preferred_element_type=jnp.float32) + weights['up_bias']
    gelu_out = jax.nn.gelu(up_proj, approximate=False).astype(jnp.bfloat16)
    resid_three = h_two.astype(jnp.float32) + jnp.einsum('btf,fd->btd', gelu_out, weights['w_down'], preferred_element_type=jnp.float32) + biases[8]
    y_out, normed_three, inv_three = norm_fwd(resid_three, biases[13], biases[14])
    saved_acts = dict(qkv_self=qkv_self, p_self=p_self, o_self=o_self, normed_one=normed_one, inv_one=inv_one, h_one=h_one, q_cross=q_cross, kv_cross=kv_cross, p_cross=p_cross, o_cross=o_cross, normed_two=normed_two, inv_two=inv_two, h_two=h_two, up_proj=up_proj, gelu_out=gelu_out, normed_three=normed_three, inv_three=inv_three)
    return y_out, saved_acts


def layer_backward(y_cot, dec_in, enc_out, saved_acts, weights):
    n_batch, n_tgt, d_model = dec_in.shape
    n_src = enc_out.shape[1]
    n_heads = d_model // HEAD_DIM
    attn_mats = weights['attn_mats']
    biases = weights['biases']
    d_res3, g_gain3, g_shift3 = norm_bwd(y_cot.astype(jnp.float32), saved_acts['normed_three'], saved_acts['inv_three'], biases[13])
    d_res3_b = d_res3.astype(jnp.bfloat16)
    g_down = jnp.einsum('btf,btd->fd', saved_acts['gelu_out'], d_res3_b, preferred_element_type=jnp.float32)
    d_gelu = jnp.einsum('btd,fd->btf', d_res3_b, weights['w_down'], preferred_element_type=jnp.float32)
    d_up = d_gelu * gelu_grad(saved_acts['up_proj'])
    d_up_b = d_up.astype(jnp.bfloat16)
    g_up = jnp.einsum('btf,btd->fd', d_up_b, saved_acts['h_two'], preferred_element_type=jnp.float32)
    d_h2 = d_res3 + jnp.einsum('btf,fd->btd', d_up_b, weights['w_up'], preferred_element_type=jnp.float32)
    d_res2, g_gain2, g_shift2 = norm_bwd(d_h2, saved_acts['normed_two'], saved_acts['inv_two'], biases[11])
    d_res2_b = d_res2.astype(jnp.bfloat16)
    g_out_cross = jnp.einsum('btd,bte->de', saved_acts['o_cross'], d_res2_b, preferred_element_type=jnp.float32)
    d_o_cross = jnp.einsum('bte,de->btd', d_res2_b, attn_mats[7], preferred_element_type=jnp.float32).astype(jnp.bfloat16).reshape(n_batch, n_tgt, n_heads, HEAD_DIM)
    kv_cross = saved_acts['kv_cross']
    dq_cross, dk_cross, dv_cross = attn_bwd(d_o_cross, saved_acts['q_cross'], kv_cross[:, :, 0], kv_cross[:, :, 1], saved_acts['p_cross'])
    dq_cross = dq_cross.reshape(n_batch, n_tgt, d_model) * 0.125
    dq_cross_b = dq_cross.astype(jnp.bfloat16)
    g_q_cross = jnp.einsum('btd,bte->de', saved_acts['h_one'], dq_cross_b, preferred_element_type=jnp.float32)
    d_kv = jnp.stack([dk_cross, dv_cross], axis=2).reshape(n_batch, n_src, 2, d_model)
    d_kv_b = d_kv.astype(jnp.bfloat16)
    g_kv_cross = jnp.einsum('bsd,bsne->nde', enc_out, d_kv_b, preferred_element_type=jnp.float32)
    enc_grad = jnp.einsum('bsne,nde->bsd', d_kv_b, attn_mats[5:7], preferred_element_type=jnp.float32).astype(jnp.bfloat16)
    d_h1 = d_res2 + jnp.einsum('bte,de->btd', dq_cross_b, attn_mats[4], preferred_element_type=jnp.float32)
    d_res1, g_gain1, g_shift1 = norm_bwd(d_h1, saved_acts['normed_one'], saved_acts['inv_one'], biases[9])
    d_res1_b = d_res1.astype(jnp.bfloat16)
    g_out_self = jnp.einsum('btd,bte->de', saved_acts['o_self'], d_res1_b, preferred_element_type=jnp.float32)
    d_o_self = jnp.einsum('bte,de->btd', d_res1_b, attn_mats[3], preferred_element_type=jnp.float32).astype(jnp.bfloat16).reshape(n_batch, n_tgt, n_heads, HEAD_DIM)
    qkv_self = saved_acts['qkv_self']
    dq_self, dk_self, dv_self = attn_bwd(d_o_self, qkv_self[:, :, 0], qkv_self[:, :, 1], qkv_self[:, :, 2], saved_acts['p_self'])
    d_qkv = jnp.stack([dq_self * 0.125, dk_self, dv_self], axis=2).reshape(n_batch, n_tgt, 3, d_model)
    d_qkv_b = d_qkv.astype(jnp.bfloat16)
    g_qkv = jnp.einsum('btd,btne->nde', dec_in, d_qkv_b, preferred_element_type=jnp.float32)
    dec_grad = (d_res1 + jnp.einsum('btne,nde->btd', d_qkv_b, attn_mats[0:3], preferred_element_type=jnp.float32)).astype(jnp.bfloat16)
    g_attn = jnp.concatenate([g_qkv, g_out_self[None], g_q_cross[None], g_kv_cross, g_out_cross[None]], axis=0).reshape(8 * d_model, d_model)
    g_ffn = jnp.concatenate([g_up, g_down], axis=0)
    g_vec = jnp.concatenate([jnp.sum(d_qkv, axis=(0, 1)).reshape(-1), jnp.sum(d_res1, axis=(0, 1)), jnp.sum(dq_cross, axis=(0, 1)), jnp.sum(d_kv, axis=(0, 1)).reshape(-1), jnp.sum(d_res2, axis=(0, 1)), jnp.sum(d_res3, axis=(0, 1)), g_gain1, g_shift1, g_gain2, g_shift2, g_gain3, g_shift3, jnp.sum(d_up, axis=(0, 1))])
    return dec_grad, enc_grad, g_attn, g_ffn, g_vec


def solution(mesh):
    n_fsdp = mesh.shape['fsdp']
    n_dp = mesh.shape['dp']
    batch_axes = ('dp', 'fsdp')
    all_axes = ('fsdp', 'dp')
    act_spec = P(batch_axes, None, None)
    len_spec = P(batch_axes)
    row_spec = P('fsdp', None)
    vec_spec = P('fsdp')

    def gather_rows(w_rows):
        half = w_rows.shape[0] // n_dp
        mine = lax.dynamic_slice_in_dim(w_rows, lax.axis_index('dp') * half, half, 0)
        return lax.all_gather(mine, all_axes, axis=0, tiled=True)

    def gather_vec(vec_rows):
        n_own = vec_rows.shape[0]
        mine = jnp.where(lax.axis_index('dp') == 0, vec_rows, jnp.zeros_like(vec_rows))
        full = lax.dynamic_update_slice_in_dim(jnp.zeros((n_own * n_fsdp,), vec_rows.dtype), mine, lax.axis_index('fsdp') * n_own, 0)
        return lax.psum(full, all_axes)

    def scatter_rows(full_grad):
        return lax.all_gather(lax.psum_scatter(full_grad, all_axes, scatter_dimension=0, tiled=True), 'dp', axis=0, tiled=True)

    def scatter_vec(full_grad):
        n_own = full_grad.shape[0] // n_fsdp
        return lax.dynamic_slice_in_dim(lax.psum(full_grad, all_axes), lax.axis_index('fsdp') * n_own, n_own, 0)

    def device_step(dec_in, enc_out, src_lens, tgt_lens, y_cot, attn_w, ffn_w, vec_params):
        weights = unpack_params(gather_rows(attn_w), gather_rows(ffn_w), gather_vec(vec_params))
        y_out, saved_acts = layer_forward(dec_in, enc_out, src_lens, tgt_lens, weights)
        dec_grad, enc_grad, g_attn, g_ffn, g_vec = layer_backward(y_cot, dec_in, enc_out, saved_acts, weights)
        grad_scale = 1.0 / (dec_in.shape[0] * dec_in.shape[1] * n_fsdp * n_dp)
        return y_out, dec_grad, enc_grad, scatter_rows(g_attn * grad_scale), scatter_rows(g_ffn * grad_scale), scatter_vec(g_vec * grad_scale)

    return jax.shard_map(device_step, mesh=mesh, in_specs=(act_spec, act_spec, len_spec, len_spec, act_spec, row_spec, row_spec, vec_spec), out_specs=(act_spec, act_spec, act_spec, row_spec, row_spec, vec_spec), check_vma=False)
```

```python
import functools
import jax
import jax.numpy as jnp
from jax import lax
from jax.experimental import pallas as pl
from jax.experimental.pallas import tpu as pltpu
from jax.sharding import PartitionSpec as P

HEAD_DIM = 64
LN_EPS = 1e-5
MASK_FILL = -1e30
VMEM_BYTES = 60 * 1024 * 1024
F32 = jnp.float32
BF16 = jnp.bfloat16
GROUP = 256
PAIR = 128


def dot(lhs, rhs, contract=((1,), (0,))):
    return lax.dot_general(lhs, rhs, (contract, ((), ())), preferred_element_type=F32)


def dot_nt(lhs, rhs):
    return dot(lhs, rhs, ((1,), (1,)))


def dot_tn(lhs, rhs):
    return dot(lhs, rhs, ((0,), (0,)))


def norm_rows(resid, gain, shift):
    mean = jnp.mean(resid, axis=-1, keepdims=True)
    centred = resid - mean
    inv_std = lax.rsqrt(jnp.mean(centred * centred, axis=-1, keepdims=True) + LN_EPS)
    normed = centred * inv_std
    return (normed * gain + shift).astype(BF16), normed, inv_std


def norm_rows_bwd(d_out, normed, inv_std, gain):
    d_norm = d_out * gain
    return inv_std * (d_norm - jnp.mean(d_norm, axis=-1, keepdims=True) - normed * jnp.mean(d_norm * normed, axis=-1, keepdims=True))


def col_sum(values):
    return jnp.sum(values, axis=0, keepdims=True)


def head_masks(pair_q, pair_k, head, n_valid):
    lane_q = lax.broadcasted_iota(jnp.int32, pair_q.shape, 1)
    lane_k = lax.broadcasted_iota(jnp.int32, pair_k.shape, 1)
    row_k = lax.broadcasted_iota(jnp.int32, pair_k.shape, 0)
    spare = HEAD_DIM * (1 - head)
    own_q = (lane_q >= HEAD_DIM * head) & (lane_q < HEAD_DIM * (head + 1))
    own_k = (lane_k >= HEAD_DIM * head) & (lane_k < HEAD_DIM * (head + 1))
    q_f = jnp.where(own_q, pair_q.astype(F32), jnp.where(lane_q == spare, 1.0, 0.0)).astype(BF16)
    k_f = jnp.where(own_k, pair_k.astype(F32), jnp.where((lane_k == spare) & (row_k >= n_valid), MASK_FILL, 0.0)).astype(BF16)
    return q_f, k_f


def half_only(pair, head):
    lane = lax.broadcasted_iota(jnp.int32, pair.shape, 1)
    own = (lane >= HEAD_DIM * head) & (lane < HEAD_DIM * (head + 1))
    return jnp.where(own, pair.astype(F32), 0.0).astype(pair.dtype)


def join_halves(first, second):
    lane = lax.broadcasted_iota(jnp.int32, first.shape, 1)
    return jnp.where(lane < HEAD_DIM, first, second)


def scores_t(q_f, k_f, causal):
    s_t = dot_nt(k_f, q_f)
    if causal:
        key_i = lax.broadcasted_iota(jnp.int32, s_t.shape, 0)
        qry_i = lax.broadcasted_iota(jnp.int32, s_t.shape, 1)
        s_t = jnp.where(key_i <= qry_i, s_t, MASK_FILL)
    return s_t


def attend_group(q_g, k_g, v_g, n_valid, causal, lse_ref):
    o_parts = []
    for pair in range(GROUP // PAIR):
        cols = slice(pair * PAIR, (pair + 1) * PAIR)
        q2, k2, v2 = q_g[:, cols], k_g[:, cols], v_g[:, cols]
        v2_t = v2.T
        for head in range(2):
            q_f, k_f = head_masks(q2, k2, head, n_valid)
            s_t = scores_t(q_f, k_f, causal)
            top = jnp.max(s_t, axis=0, keepdims=True)
            e_t = jnp.exp(s_t - top)
            total = jnp.sum(e_t, axis=0, keepdims=True)
            p_t = (e_t * (1.0 / total)).astype(BF16)
            lse_ref[0, 0, pl.ds(2 * pair + head, 1), :] = top + jnp.log(total)
            o_parts.append(dot(v2_t[HEAD_DIM * head:HEAD_DIM * (head + 1)], p_t))
    return jnp.concatenate(o_parts, axis=0).T.astype(BF16)


def attend_group_bwd(d_o, q_g, k_g, v_g, n_valid, causal, lse_ref):
    dq_t, dk, dv = [], [], []
    for pair in range(GROUP // PAIR):
        cols = slice(pair * PAIR, (pair + 1) * PAIR)
        q2, k2, v2, do2 = q_g[:, cols], k_g[:, cols], v_g[:, cols], d_o[:, cols]
        k2_t = k2.T
        dk_h, dv_h = [], []
        for head in range(2):
            q_f, k_f = head_masks(q2, k2, head, n_valid)
            s_t = scores_t(q_f, k_f, causal)
            p_t = jnp.exp(s_t - lse_ref[0, 0, pl.ds(2 * pair + head, 1), :])
            dp_t = dot_nt(half_only(v2, head), do2)
            weighted = p_t * dp_t
            ds_t = (weighted - p_t * jnp.sum(weighted, axis=0, keepdims=True)).astype(BF16)
            dv_h.append(dot(p_t.astype(BF16), do2))
            dk_h.append(dot(ds_t, q2))
            dq_t.append(dot(k2_t[HEAD_DIM * head:HEAD_DIM * (head + 1)], ds_t))
        dk.append(join_halves(*dk_h))
        dv.append(join_halves(*dv_h))
    return jnp.concatenate(dq_t, axis=0).T * 0.125, jnp.concatenate(dk, axis=1), jnp.concatenate(dv, axis=1)


def attn_fwd_kernel(causal, slots, lens_ref, x_ref, kv_ref, wq_ref, wk_ref, wv_ref, wo_ref, bias_ref, rows_ref,
                    q_ref, k_ref, v_ref, o_ref, lse_ref, h_ref, normed_ref, inv_ref, acc_ref):
    q_row, k_row, v_row, o_row, gain_row = slots
    sample, group = pl.program_id(0), pl.program_id(1)
    x_b, kv_b = x_ref[...], kv_ref[...]
    q_g = ((dot(x_b, wq_ref[...]) + bias_ref[q_row:q_row + 1, :]) * 0.125).astype(BF16)
    k_g = (dot(kv_b, wk_ref[...]) + bias_ref[k_row:k_row + 1, :]).astype(BF16)
    v_g = (dot(kv_b, wv_ref[...]) + bias_ref[v_row:v_row + 1, :]).astype(BF16)
    q_ref[...], k_ref[...], v_ref[...] = q_g, k_g, v_g
    o_g = attend_group(q_g, k_g, v_g, lens_ref[sample], causal, lse_ref)
    o_ref[...] = o_g
    part = dot(o_g, wo_ref[...])

    @pl.when(group == 0)
    def _():
        acc_ref[...] = x_ref[...].astype(F32) + part

    @pl.when(group > 0)
    def _():
        acc_ref[...] += part

    @pl.when(group == pl.num_programs(1) - 1)
    def _():
        resid = acc_ref[...] + rows_ref[o_row:o_row + 1, :]
        h_out, normed, inv_std = norm_rows(resid, rows_ref[gain_row:gain_row + 1, :], rows_ref[gain_row + 1:gain_row + 2, :])
        h_ref[...], normed_ref[...], inv_ref[...] = h_out, normed, inv_std


def attn_forward(x, kv, lens, attn_full, bias_rows, mats, slots, causal):
    d_model = x.shape[-1]
    n_batch = lens.shape[0]
    n_q, n_k = x.shape[0] // n_batch, kv.shape[0] // n_batch
    n_groups = d_model // GROUP
    col = lambda mat: pl.BlockSpec((d_model, GROUP), lambda b, g: (mat, g))
    row = lambda mat: pl.BlockSpec((GROUP, d_model), lambda b, g: (mat * n_groups + g, 0))
    q_blk = pl.BlockSpec((n_q, GROUP), lambda b, g: (b, g))
    k_blk = pl.BlockSpec((n_k, GROUP), lambda b, g: (b, g))
    tok = lambda n: pl.BlockSpec((n, d_model), lambda b, g: (b, 0))
    n_heads_g = GROUP // HEAD_DIM
    out_shape = (
        jax.ShapeDtypeStruct(x.shape, BF16), jax.ShapeDtypeStruct(kv.shape, BF16), jax.ShapeDtypeStruct(kv.shape, BF16),
        jax.ShapeDtypeStruct(x.shape, BF16), jax.ShapeDtypeStruct((n_batch, n_groups, n_heads_g, n_q), F32),
        jax.ShapeDtypeStruct(x.shape, BF16), jax.ShapeDtypeStruct(x.shape, F32), jax.ShapeDtypeStruct((x.shape[0], 1), F32))
    return pl.pallas_call(
        functools.partial(attn_fwd_kernel, causal, slots),
        grid=(n_batch, n_groups),
        in_specs=[pl.BlockSpec(memory_space=pltpu.SMEM), tok(n_q), tok(n_k), col(mats[0]), col(mats[1]), col(mats[2]), row(mats[3]),
                  pl.BlockSpec((bias_rows.shape[0], GROUP), lambda b, g: (0, g)), pl.BlockSpec(bias_rows.shape, lambda b, g: (0, 0))],
        out_specs=[q_blk, k_blk, k_blk, q_blk, pl.BlockSpec((1, 1, n_heads_g, n_q), lambda b, g: (b, g, 0, 0)),
                   tok(n_q), tok(n_q), pl.BlockSpec((n_q, 1), lambda b, g: (b, 0))],
        out_shape=out_shape,
        scratch_shapes=[pltpu.VMEM((n_q, d_model), F32)],
        compiler_params=pltpu.CompilerParams(vmem_limit_bytes=VMEM_BYTES, dimension_semantics=('arbitrary', 'arbitrary')),
        cost_estimate=pl.CostEstimate(flops=2 * d_model * d_model * (2 * x.shape[0] + 2 * kv.shape[0]) + 16 * x.shape[0] * n_k * d_model, bytes_accessed=20 * x.shape[0] * d_model, transcendentals=0),
        name='attn_fwd',
    )(lens, x, kv, attn_full, attn_full, attn_full, attn_full, bias_rows, bias_rows)


def attn_bwd_kernel(causal, gain_row, lens_ref, dres_ref, wq_ref, wk_ref, wv_ref, wo_ref, q_ref, k_ref, v_ref, lse_ref,
                    rows_ref, normed_ref, inv_ref, dq_ref, dk_ref, dv_ref, dx_ref, dkv_ref, sums_ref, tail_ref, acc_ref, acc_kv_ref):
    sample, group = pl.program_id(0), pl.program_id(1)
    d_o = dot_nt(dres_ref[...].astype(BF16), wo_ref[...]).astype(BF16)
    dq, dk, dv = attend_group_bwd(d_o, q_ref[...], k_ref[...], v_ref[...], lens_ref[sample], causal, lse_ref)
    sums_ref[0, 0:1, :] = col_sum(dq)
    sums_ref[0, 1:2, :] = col_sum(dk)
    sums_ref[0, 2:3, :] = col_sum(dv)
    dq_b, dk_b, dv_b = dq.astype(BF16), dk.astype(BF16), dv.astype(BF16)
    dq_ref[...], dk_ref[...], dv_ref[...] = dq_b, dk_b, dv_b
    part_q = dot_nt(dq_b, wq_ref[...])
    part_kv = dot_nt(dk_b, wk_ref[...]) + dot_nt(dv_b, wv_ref[...])
    last = pl.num_programs(1) - 1
    if causal:
        @pl.when(group == 0)
        def _():
            acc_ref[...] = dres_ref[...] + part_q + part_kv

        @pl.when(group > 0)
        def _():
            acc_ref[...] += part_q + part_kv

        @pl.when(group == last)
        def _():
            dx_ref[...] = acc_ref[...].astype(BF16)
            tail_ref[...] = jnp.zeros_like(tail_ref)
    else:
        @pl.when(group == 0)
        def _():
            acc_ref[...] = dres_ref[...] + part_q
            acc_kv_ref[...] = part_kv

        @pl.when(group > 0)
        def _():
            acc_ref[...] += part_q
            acc_kv_ref[...] += part_kv

        @pl.when(group == last)
        def _():
            d_h = acc_ref[...]
            normed = normed_ref[...]
            d_resid = norm_rows_bwd(d_h, normed, inv_ref[...], rows_ref[gain_row:gain_row + 1, :])
            dx_ref[...] = d_resid
            dkv_ref[...] = acc_kv_ref[...].astype(BF16)
            tail_ref[0, 0:1, :] = col_sum(d_resid)
            tail_ref[0, 1:2, :] = col_sum(d_h * normed)
            tail_ref[0, 2:3, :] = col_sum(d_h)


def attn_backward(dres, q, k, v, lse, lens, attn_full, bias_rows, mats, causal, gain_row=0, normed=None, inv_std=None):
    d_model = q.shape[-1]
    n_batch = lens.shape[0]
    n_q, n_k = q.shape[0] // n_batch, k.shape[0] // n_batch
    n_groups = d_model // GROUP
    col = lambda mat: pl.BlockSpec((d_model, GROUP), lambda b, g: (mat, g))
    row = lambda mat: pl.BlockSpec((GROUP, d_model), lambda b, g: (mat * n_groups + g, 0))
    q_blk = pl.BlockSpec((n_q, GROUP), lambda b, g: (b, g))
    k_blk = pl.BlockSpec((n_k, GROUP), lambda b, g: (b, g))
    tok = lambda n: pl.BlockSpec((n, d_model), lambda b, g: (b, 0))
    n_heads_g = GROUP // HEAD_DIM
    whole_rows = pl.BlockSpec(bias_rows.shape, lambda b, g: (0, 0))
    kernel = functools.partial(attn_bwd_kernel, causal, gain_row)
    in_specs = [pl.BlockSpec(memory_space=pltpu.SMEM), tok(n_q), col(mats[0]), col(mats[1]), col(mats[2]), row(mats[3]), q_blk, k_blk, k_blk,
                pl.BlockSpec((1, 1, n_heads_g, n_q), lambda b, g: (b, g, 0, 0)), whole_rows]
    args = [lens, dres, attn_full, attn_full, attn_full, attn_full, q, k, v, lse, bias_rows]
    sums_blk = pl.BlockSpec((1, 8, GROUP), lambda b, g: (b, 0, g))
    tail_blk = pl.BlockSpec((1, 8, d_model), lambda b, g: (b, 0, 0))
    tail_shape = jax.ShapeDtypeStruct((n_batch, 8, d_model), F32)
    out_shape = [jax.ShapeDtypeStruct(q.shape, BF16), jax.ShapeDtypeStruct(k.shape, BF16), jax.ShapeDtypeStruct(k.shape, BF16),
                 jax.ShapeDtypeStruct(q.shape, BF16 if causal else F32)]
    out_specs = [q_blk, k_blk, k_blk, tok(n_q)]
    scratch = [pltpu.VMEM((n_q, d_model), F32)]
    if causal:
        def body(*refs):
            ins, rest = refs[:11], refs[11:]
            dq, dk, dv, dx, sums, tail, acc = rest
            kernel(*ins, None, None, dq, dk, dv, dx, None, sums, tail, acc, None)
    else:
        in_specs += [tok(n_q), pl.BlockSpec((n_q, 1), lambda b, g: (b, 0))]
        args += [normed, inv_std]
        out_shape.append(jax.ShapeDtypeStruct(k.shape, BF16))
        out_specs.append(tok(n_k))
        scratch.append(pltpu.VMEM((n_k, d_model), F32))
        body = kernel
    out_shape += [tail_shape, tail_shape]
    out_specs += [sums_blk, tail_blk]
    return pl.pallas_call(
        body, grid=(n_batch, n_groups), in_specs=in_specs, out_specs=out_specs, out_shape=out_shape, scratch_shapes=scratch,
        compiler_params=pltpu.CompilerParams(vmem_limit_bytes=VMEM_BYTES, dimension_semantics=('arbitrary', 'arbitrary')),
        cost_estimate=pl.CostEstimate(flops=2 * d_model * d_model * (2 * q.shape[0] + 2 * k.shape[0]) + 40 * q.shape[0] * n_k * d_model, bytes_accessed=20 * q.shape[0] * d_model, transcendentals=0),
        name='attn_bwd',
    )(*args)


def ffn_kernel(h_ref, dy_ref, up_ref, down_ref, rows_ref, bias_ref, normed_ref, inv_ref,
               y_ref, gelu_ref, dup_ref, dres3_ref, dres2_ref, tail_ref, upsum_ref):
    step = pl.program_id(0)
    h_b = h_ref[...]
    up = dot_nt(h_b, up_ref[...]) + bias_ref[...]
    cdf = 0.5 * (1.0 + lax.erf(up * 0.7071067811865476))
    gelu = (up * cdf).astype(BF16)
    slope = cdf + up * (0.3989422804014327 * jnp.exp(-0.5 * up * up))
    gelu_ref[...] = gelu
    resid = h_b.astype(F32) + dot(gelu, down_ref[...]) + rows_ref[8:9, :]
    y_b, normed3, inv3 = norm_rows(resid, rows_ref[13:14, :], rows_ref[14:15, :])
    y_ref[...] = y_b
    dy = dy_ref[...].astype(F32)
    d_res3 = norm_rows_bwd(dy, normed3, inv3, rows_ref[13:14, :])
    d_res3_b = d_res3.astype(BF16)
    dres3_ref[...] = d_res3_b
    d_up = dot_nt(d_res3_b, down_ref[...]) * slope
    d_up_b = d_up.astype(BF16)
    dup_ref[...] = d_up_b
    d_h2 = d_res3 + dot(d_up_b, up_ref[...])
    normed2 = normed_ref[...]
    d_res2 = norm_rows_bwd(d_h2, normed2, inv_ref[...], rows_ref[11:12, :])
    dres2_ref[...] = d_res2
    tail = jnp.concatenate([col_sum(d_res2), col_sum(d_res3), col_sum(d_h2 * normed2), col_sum(d_h2), col_sum(dy * normed3), col_sum(dy),
                            jnp.zeros((2, dy.shape[1]), F32)], axis=0)
    up_sum = col_sum(d_up)

    @pl.when(step == 0)
    def _():
        tail_ref[...] = tail
        upsum_ref[...] = up_sum

    @pl.when(step > 0)
    def _():
        tail_ref[...] += tail
        upsum_ref[...] += up_sum


def ffn_both(h2, dy, ffn_full, bias_rows, up_bias, normed2, inv2, block=256):
    n_tok, d_model = h2.shape
    ffn_dim = ffn_full.shape[0] // 2
    tok = pl.BlockSpec((block, d_model), lambda i: (i, 0))
    wide = pl.BlockSpec((block, ffn_dim), lambda i: (i, 0))
    once = lambda shape, idx: pl.BlockSpec(shape, lambda i: idx, pipeline_mode=pl.Buffered(1))
    return pl.pallas_call(
        ffn_kernel, grid=(n_tok // block,),
        in_specs=[tok, tok, once((ffn_dim, d_model), (0, 0)), once((ffn_dim, d_model), (1, 0)), once(bias_rows.shape, (0, 0)), once((1, ffn_dim), (0, 0)),
                  tok, pl.BlockSpec((block, 1), lambda i: (i, 0))],
        out_specs=[tok, wide, wide, tok, tok, pl.BlockSpec((8, d_model), lambda i: (0, 0)), pl.BlockSpec((1, ffn_dim), lambda i: (0, 0))],
        out_shape=[jax.ShapeDtypeStruct(h2.shape, BF16), jax.ShapeDtypeStruct((n_tok, ffn_dim), BF16), jax.ShapeDtypeStruct((n_tok, ffn_dim), BF16),
                   jax.ShapeDtypeStruct(h2.shape, BF16), jax.ShapeDtypeStruct(h2.shape, F32),
                   jax.ShapeDtypeStruct((8, d_model), F32), jax.ShapeDtypeStruct((1, ffn_dim), F32)],
        compiler_params=pltpu.CompilerParams(vmem_limit_bytes=VMEM_BYTES, dimension_semantics=('arbitrary',)),
        cost_estimate=pl.CostEstimate(flops=8 * n_tok * d_model * ffn_dim, bytes_accessed=30 * n_tok * d_model, transcendentals=0),
        name='ffn_both',
    )(h2, dy, ffn_full, ffn_full, bias_rows, up_bias, normed2, inv2)


def layer_acts(dec_in, enc_out, src_lens, tgt_lens, y_cot, attn_full, ffn_full, vec_full):
    n_batch, n_tgt, d_model = dec_in.shape
    x = dec_in.reshape(-1, d_model)
    enc = enc_out.reshape(-1, d_model)
    dy = y_cot.reshape(-1, d_model)
    vec_f = vec_full.astype(F32)
    bias_rows = jnp.pad(vec_f[:15 * d_model].reshape(15, d_model), ((0, 1), (0, 0)))
    up_bias = vec_f[15 * d_model:].reshape(1, -1)
    q1, k1, v1, o1, lse1, h1, normed1, inv1 = attn_forward(x, x, tgt_lens, attn_full, bias_rows, (0, 1, 2, 3), (0, 1, 2, 3, 9), True)
    q2, k2, v2, o2, lse2, h2, normed2, inv2 = attn_forward(h1, enc, src_lens, attn_full, bias_rows, (4, 5, 6, 7), (4, 5, 6, 7, 11), False)
    y, gelu, d_up, d_res3, d_res2, ffn_tail, up_sum = ffn_both(h2, dy, ffn_full, bias_rows, up_bias, normed2, inv2)
    dq2, dk2, dv2, d_res1, d_enc, sums2, tail2 = attn_backward(d_res2, q2, k2, v2, lse2, src_lens, attn_full, bias_rows, (4, 5, 6, 7), False, 9, normed1, inv1)
    dq1, dk1, dv1, d_x, sums1, _ = attn_backward(d_res1, q1, k1, v1, lse1, tgt_lens, attn_full, bias_rows, (0, 1, 2, 3), True)
    s1, s2, t2 = jnp.sum(sums1, axis=0), jnp.sum(sums2, axis=0), jnp.sum(tail2, axis=0)
    g_vec = jnp.concatenate([s1[0:3].reshape(-1), t2[0], s2[0:3].reshape(-1), ffn_tail[0], ffn_tail[1], t2[1], t2[2], ffn_tail[2], ffn_tail[3], ffn_tail[4], ffn_tail[5], up_sum[0]])
    pairs = ((x, dq1), (x, dk1), (x, dv1), (o1, d_res1.astype(BF16)), (h1, dq2), (enc, dk2), (enc, dv2), (o2, d_res2.astype(BF16)))
    ffn_pairs = ((d_up, h2), (gelu, d_res3))
    return y.reshape(dec_in.shape), d_x.reshape(dec_in.shape), d_enc.reshape(enc_out.shape), pairs, ffn_pairs, g_vec


def solution(mesh):
    n_fsdp = mesh.shape['fsdp']
    n_dp = mesh.shape['dp']
    batch_axes = ('dp', 'fsdp')
    all_axes = ('fsdp', 'dp')
    act_spec = P(batch_axes, None, None)
    len_spec = P(batch_axes)
    row_spec = P('fsdp', None)
    vec_spec = P('fsdp')

    def gather_rows(w_rows):
        half = w_rows.shape[0] // n_dp
        mine = lax.dynamic_slice_in_dim(w_rows, lax.axis_index('dp') * half, half, 0)
        return lax.all_gather(mine, all_axes, axis=0, tiled=True)

    def gather_vec(vec_rows):
        n_own = vec_rows.shape[0]
        mine = jnp.where(lax.axis_index('dp') == 0, vec_rows, jnp.zeros_like(vec_rows))
        full = lax.dynamic_update_slice_in_dim(jnp.zeros((n_own * n_fsdp,), vec_rows.dtype), mine, lax.axis_index('fsdp') * n_own, 0)
        return lax.psum(full, all_axes)

    def scatter_rows(full_grad):
        return lax.all_gather(lax.psum_scatter(full_grad, all_axes, scatter_dimension=0, tiled=True), 'dp', axis=0, tiled=True)

    def scatter_vec(full_grad):
        n_own = full_grad.shape[0] // n_fsdp
        return lax.dynamic_slice_in_dim(lax.psum(full_grad, all_axes), lax.axis_index('fsdp') * n_own, n_own, 0)

    def device_step(dec_in, enc_out, src_lens, tgt_lens, y_cot, attn_w, ffn_w, vec_params):
        y_out, dec_grad, enc_grad, pairs, ffn_pairs, g_vec = layer_acts(dec_in, enc_out, src_lens, tgt_lens, y_cot, gather_rows(attn_w), gather_rows(ffn_w), gather_vec(vec_params))
        grad_scale = 1.0 / (dec_in.shape[0] * dec_in.shape[1] * n_fsdp * n_dp)
        g_ffn = jnp.concatenate([dot_tn(lhs, rhs) for lhs, rhs in ffn_pairs], axis=0) * grad_scale
        g_attn = jnp.concatenate([dot_tn(lhs, rhs) for lhs, rhs in pairs], axis=0) * grad_scale
        return y_out, dec_grad, enc_grad, scatter_rows(g_attn), scatter_rows(g_ffn), scatter_vec(g_vec * grad_scale)

    return jax.shard_map(device_step, mesh=mesh, in_specs=(act_spec, act_spec, len_spec, len_spec, act_spec, row_spec, row_spec, vec_spec), out_specs=(act_spec, act_spec, act_spec, row_spec, row_spec, vec_spec), check_vma=False)
```

```python
import functools
import jax
import jax.numpy as jnp
from jax import lax
from jax.experimental import pallas as pl
from jax.experimental.pallas import tpu as pltpu
from jax.sharding import PartitionSpec as P

HEAD_DIM = 64
LN_EPS = 1e-5
MASK_FILL = -1e30
VMEM_BYTES = 60 * 1024 * 1024
F32 = jnp.float32
BF16 = jnp.bfloat16
GROUP = 256
PAIR = 128


def dot(lhs, rhs, contract=((1,), (0,))):
    return lax.dot_general(lhs, rhs, (contract, ((), ())), preferred_element_type=F32)


def dot_nt(lhs, rhs):
    return dot(lhs, rhs, ((1,), (1,)))


def dot_tn(lhs, rhs):
    return dot(lhs, rhs, ((0,), (0,)))


def norm_rows(resid, gain, shift):
    mean = jnp.mean(resid, axis=-1, keepdims=True)
    centred = resid - mean
    inv_std = lax.rsqrt(jnp.mean(centred * centred, axis=-1, keepdims=True) + LN_EPS)
    normed = centred * inv_std
    return (normed * gain + shift).astype(BF16), normed, inv_std


def norm_rows_bwd(d_out, normed, inv_std, gain):
    d_norm = d_out * gain
    return inv_std * (d_norm - jnp.mean(d_norm, axis=-1, keepdims=True) - normed * jnp.mean(d_norm * normed, axis=-1, keepdims=True))


def col_sum(values):
    return jnp.sum(values, axis=0, keepdims=True)


def head_masks(pair_q, pair_k, head, n_valid):
    lane_q = lax.broadcasted_iota(jnp.int32, pair_q.shape, 1)
    lane_k = lax.broadcasted_iota(jnp.int32, pair_k.shape, 1)
    row_k = lax.broadcasted_iota(jnp.int32, pair_k.shape, 0)
    spare = HEAD_DIM * (1 - head)
    own_q = (lane_q >= HEAD_DIM * head) & (lane_q < HEAD_DIM * (head + 1))
    own_k = (lane_k >= HEAD_DIM * head) & (lane_k < HEAD_DIM * (head + 1))
    q_f = jnp.where(own_q, pair_q.astype(F32), jnp.where(lane_q == spare, 1.0, 0.0)).astype(BF16)
    k_f = jnp.where(own_k, pair_k.astype(F32), jnp.where((lane_k == spare) & (row_k >= n_valid), MASK_FILL, 0.0)).astype(BF16)
    return q_f, k_f


def half_only(pair, head):
    lane = lax.broadcasted_iota(jnp.int32, pair.shape, 1)
    own = (lane >= HEAD_DIM * head) & (lane < HEAD_DIM * (head + 1))
    return jnp.where(own, pair.astype(F32), 0.0).astype(pair.dtype)


def join_halves(first, second):
    lane = lax.broadcasted_iota(jnp.int32, first.shape, 1)
    return jnp.where(lane < HEAD_DIM, first, second)


def scores_t(q_f, k_f, causal):
    s_t = dot_nt(k_f, q_f)
    if causal:
        key_i = lax.broadcasted_iota(jnp.int32, s_t.shape, 0)
        qry_i = lax.broadcasted_iota(jnp.int32, s_t.shape, 1)
        s_t = jnp.where(key_i <= qry_i, s_t, MASK_FILL)
    return s_t


def attend_group(q_g, k_g, v_g, n_valid, causal, lse_ref):
    o_parts = []
    for pair in range(GROUP // PAIR):
        cols = slice(pair * PAIR, (pair + 1) * PAIR)
        q2, k2, v2 = q_g[:, cols], k_g[:, cols], v_g[:, cols]
        v2_t = v2.T
        for head in range(2):
            q_f, k_f = head_masks(q2, k2, head, n_valid)
            s_t = scores_t(q_f, k_f, causal)
            top = jnp.max(s_t, axis=0, keepdims=True)
            e_t = jnp.exp(s_t - top)
            total = jnp.sum(e_t, axis=0, keepdims=True)
            p_t = (e_t * (1.0 / total)).astype(BF16)
            lse_ref[0, 0, pl.ds(2 * pair + head, 1), :] = top + jnp.log(total)
            o_parts.append(dot(v2_t[HEAD_DIM * head:HEAD_DIM * (head + 1)], p_t))
    return jnp.concatenate(o_parts, axis=0).T.astype(BF16)


def attend_group_bwd(d_o, q_g, k_g, v_g, n_valid, causal, lse_ref):
    dq_t, dk, dv = [], [], []
    for pair in range(GROUP // PAIR):
        cols = slice(pair * PAIR, (pair + 1) * PAIR)
        q2, k2, v2, do2 = q_g[:, cols], k_g[:, cols], v_g[:, cols], d_o[:, cols]
        k2_t = k2.T
        dk_h, dv_h = [], []
        for head in range(2):
            q_f, k_f = head_masks(q2, k2, head, n_valid)
            s_t = scores_t(q_f, k_f, causal)
            p_t = jnp.exp(s_t - lse_ref[0, 0, pl.ds(2 * pair + head, 1), :])
            dp_t = dot_nt(half_only(v2, head), do2)
            weighted = p_t * dp_t
            ds_t = (weighted - p_t * jnp.sum(weighted, axis=0, keepdims=True)).astype(BF16)
            dv_h.append(dot(p_t.astype(BF16), do2))
            dk_h.append(dot(ds_t, q2))
            dq_t.append(dot(k2_t[HEAD_DIM * head:HEAD_DIM * (head + 1)], ds_t))
        dk.append(join_halves(*dk_h))
        dv.append(join_halves(*dv_h))
    return jnp.concatenate(dq_t, axis=0).T * 0.125, jnp.concatenate(dk, axis=1), jnp.concatenate(dv, axis=1)


def attn_fwd_kernel(causal, slots, lens_ref, x_ref, kv_ref, wq_ref, wk_ref, wv_ref, wo_ref, bias_ref, rows_ref,
                    q_ref, k_ref, v_ref, o_ref, lse_ref, h_ref, normed_ref, inv_ref, acc_ref):
    q_row, k_row, v_row, o_row, gain_row = slots
    sample, group = pl.program_id(0), pl.program_id(1)
    x_b, kv_b = x_ref[...], kv_ref[...]
    q_g = ((dot(x_b, wq_ref[...]) + bias_ref[q_row:q_row + 1, :]) * 0.125).astype(BF16)
    k_g = (dot(kv_b, wk_ref[...]) + bias_ref[k_row:k_row + 1, :]).astype(BF16)
    v_g = (dot(kv_b, wv_ref[...]) + bias_ref[v_row:v_row + 1, :]).astype(BF16)
    q_ref[...], k_ref[...], v_ref[...] = q_g, k_g, v_g
    o_g = attend_group(q_g, k_g, v_g, lens_ref[sample], causal, lse_ref)
    o_ref[...] = o_g
    part = dot(o_g, wo_ref[...])

    @pl.when(group == 0)
    def _():
        acc_ref[...] = x_ref[...].astype(F32) + part

    @pl.when(group > 0)
    def _():
        acc_ref[...] += part

    @pl.when(group == pl.num_programs(1) - 1)
    def _():
        resid = acc_ref[...] + rows_ref[o_row:o_row + 1, :]
        h_out, normed, inv_std = norm_rows(resid, rows_ref[gain_row:gain_row + 1, :], rows_ref[gain_row + 1:gain_row + 2, :])
        h_ref[...], normed_ref[...], inv_ref[...] = h_out, normed, inv_std


def attn_forward(x, kv, lens, attn_full, bias_rows, mats, slots, causal):
    d_model = x.shape[-1]
    n_batch = lens.shape[0]
    n_q, n_k = x.shape[0] // n_batch, kv.shape[0] // n_batch
    n_groups = d_model // GROUP
    col = lambda mat: pl.BlockSpec((d_model, GROUP), lambda b, g: (mat, g))
    row = lambda mat: pl.BlockSpec((GROUP, d_model), lambda b, g: (mat * n_groups + g, 0))
    q_blk = pl.BlockSpec((n_q, GROUP), lambda b, g: (b, g))
    k_blk = pl.BlockSpec((n_k, GROUP), lambda b, g: (b, g))
    tok = lambda n: pl.BlockSpec((n, d_model), lambda b, g: (b, 0))
    n_heads_g = GROUP // HEAD_DIM
    out_shape = (
        jax.ShapeDtypeStruct(x.shape, BF16), jax.ShapeDtypeStruct(kv.shape, BF16), jax.ShapeDtypeStruct(kv.shape, BF16),
        jax.ShapeDtypeStruct(x.shape, BF16), jax.ShapeDtypeStruct((n_batch, n_groups, n_heads_g, n_q), F32),
        jax.ShapeDtypeStruct(x.shape, BF16), jax.ShapeDtypeStruct(x.shape, F32), jax.ShapeDtypeStruct((x.shape[0], 1), F32))
    return pl.pallas_call(
        functools.partial(attn_fwd_kernel, causal, slots),
        grid=(n_batch, n_groups),
        in_specs=[pl.BlockSpec(memory_space=pltpu.SMEM), tok(n_q), tok(n_k), col(mats[0]), col(mats[1]), col(mats[2]), row(mats[3]),
                  pl.BlockSpec((bias_rows.shape[0], GROUP), lambda b, g: (0, g)), pl.BlockSpec(bias_rows.shape, lambda b, g: (0, 0))],
        out_specs=[q_blk, k_blk, k_blk, q_blk, pl.BlockSpec((1, 1, n_heads_g, n_q), lambda b, g: (b, g, 0, 0)),
                   tok(n_q), tok(n_q), pl.BlockSpec((n_q, 1), lambda b, g: (b, 0))],
        out_shape=out_shape,
        scratch_shapes=[pltpu.VMEM((n_q, d_model), F32)],
        compiler_params=pltpu.CompilerParams(vmem_limit_bytes=VMEM_BYTES, dimension_semantics=('arbitrary', 'arbitrary')),
        cost_estimate=pl.CostEstimate(flops=2 * d_model * d_model * (2 * x.shape[0] + 2 * kv.shape[0]) + 16 * x.shape[0] * n_k * d_model, bytes_accessed=20 * x.shape[0] * d_model, transcendentals=0),
        name='attn_fwd',
    )(lens, x, kv, attn_full, attn_full, attn_full, attn_full, bias_rows, bias_rows)


def attn_bwd_kernel(causal, gain_row, lens_ref, dres_ref, wq_ref, wk_ref, wv_ref, wo_ref, q_ref, k_ref, v_ref, lse_ref,
                    rows_ref, normed_ref, inv_ref, dq_ref, dk_ref, dv_ref, dx_ref, dkv_ref, sums_ref, tail_ref, acc_ref, acc_kv_ref):
    sample, group = pl.program_id(0), pl.program_id(1)
    d_o = dot_nt(dres_ref[...].astype(BF16), wo_ref[...]).astype(BF16)
    dq, dk, dv = attend_group_bwd(d_o, q_ref[...], k_ref[...], v_ref[...], lens_ref[sample], causal, lse_ref)
    sums_ref[0, 0:1, :] = col_sum(dq)
    sums_ref[0, 1:2, :] = col_sum(dk)
    sums_ref[0, 2:3, :] = col_sum(dv)
    dq_b, dk_b, dv_b = dq.astype(BF16), dk.astype(BF16), dv.astype(BF16)
    dq_ref[...], dk_ref[...], dv_ref[...] = dq_b, dk_b, dv_b
    part_q = dot_nt(dq_b, wq_ref[...])
    part_kv = dot_nt(dk_b, wk_ref[...]) + dot_nt(dv_b, wv_ref[...])
    last = pl.num_programs(1) - 1
    if causal:
        @pl.when(group == 0)
        def _():
            acc_ref[...] = dres_ref[...] + part_q + part_kv

        @pl.when(group > 0)
        def _():
            acc_ref[...] += part_q + part_kv

        @pl.when(group == last)
        def _():
            dx_ref[...] = acc_ref[...].astype(BF16)
            tail_ref[...] = jnp.zeros_like(tail_ref)
    else:
        @pl.when(group == 0)
        def _():
            acc_ref[...] = dres_ref[...] + part_q
            acc_kv_ref[...] = part_kv

        @pl.when(group > 0)
        def _():
            acc_ref[...] += part_q
            acc_kv_ref[...] += part_kv

        @pl.when(group == last)
        def _():
            d_h = acc_ref[...]
            normed = normed_ref[...]
            d_resid = norm_rows_bwd(d_h, normed, inv_ref[...], rows_ref[gain_row:gain_row + 1, :])
            dx_ref[...] = d_resid
            dkv_ref[...] = acc_kv_ref[...].astype(BF16)
            tail_ref[0, 0:1, :] = col_sum(d_resid)
            tail_ref[0, 1:2, :] = col_sum(d_h * normed)
            tail_ref[0, 2:3, :] = col_sum(d_h)


def attn_backward(dres, q, k, v, lse, lens, attn_full, bias_rows, mats, causal, gain_row=0, normed=None, inv_std=None):
    d_model = q.shape[-1]
    n_batch = lens.shape[0]
    n_q, n_k = q.shape[0] // n_batch, k.shape[0] // n_batch
    n_groups = d_model // GROUP
    col = lambda mat: pl.BlockSpec((d_model, GROUP), lambda b, g: (mat, g))
    row = lambda mat: pl.BlockSpec((GROUP, d_model), lambda b, g: (mat * n_groups + g, 0))
    q_blk = pl.BlockSpec((n_q, GROUP), lambda b, g: (b, g))
    k_blk = pl.BlockSpec((n_k, GROUP), lambda b, g: (b, g))
    tok = lambda n: pl.BlockSpec((n, d_model), lambda b, g: (b, 0))
    n_heads_g = GROUP // HEAD_DIM
    whole_rows = pl.BlockSpec(bias_rows.shape, lambda b, g: (0, 0))
    kernel = functools.partial(attn_bwd_kernel, causal, gain_row)
    in_specs = [pl.BlockSpec(memory_space=pltpu.SMEM), tok(n_q), col(mats[0]), col(mats[1]), col(mats[2]), row(mats[3]), q_blk, k_blk, k_blk,
                pl.BlockSpec((1, 1, n_heads_g, n_q), lambda b, g: (b, g, 0, 0)), whole_rows]
    args = [lens, dres, attn_full, attn_full, attn_full, attn_full, q, k, v, lse, bias_rows]
    sums_blk = pl.BlockSpec((1, 8, GROUP), lambda b, g: (b, 0, g))
    tail_blk = pl.BlockSpec((1, 8, d_model), lambda b, g: (b, 0, 0))
    tail_shape = jax.ShapeDtypeStruct((n_batch, 8, d_model), F32)
    out_shape = [jax.ShapeDtypeStruct(q.shape, BF16), jax.ShapeDtypeStruct(k.shape, BF16), jax.ShapeDtypeStruct(k.shape, BF16),
                 jax.ShapeDtypeStruct(q.shape, BF16 if causal else F32)]
    out_specs = [q_blk, k_blk, k_blk, tok(n_q)]
    scratch = [pltpu.VMEM((n_q, d_model), F32)]
    if causal:
        def body(*refs):
            ins, rest = refs[:11], refs[11:]
            dq, dk, dv, dx, sums, tail, acc = rest
            kernel(*ins, None, None, dq, dk, dv, dx, None, sums, tail, acc, None)
    else:
        in_specs += [tok(n_q), pl.BlockSpec((n_q, 1), lambda b, g: (b, 0))]
        args += [normed, inv_std]
        out_shape.append(jax.ShapeDtypeStruct(k.shape, BF16))
        out_specs.append(tok(n_k))
        scratch.append(pltpu.VMEM((n_k, d_model), F32))
        body = kernel
    out_shape += [tail_shape, tail_shape]
    out_specs += [sums_blk, tail_blk]
    return pl.pallas_call(
        body, grid=(n_batch, n_groups), in_specs=in_specs, out_specs=out_specs, out_shape=out_shape, scratch_shapes=scratch,
        compiler_params=pltpu.CompilerParams(vmem_limit_bytes=VMEM_BYTES, dimension_semantics=('arbitrary', 'arbitrary')),
        cost_estimate=pl.CostEstimate(flops=2 * d_model * d_model * (2 * q.shape[0] + 2 * k.shape[0]) + 40 * q.shape[0] * n_k * d_model, bytes_accessed=20 * q.shape[0] * d_model, transcendentals=0),
        name='attn_bwd',
    )(*args)


def ffn_kernel(h_ref, dy_ref, up_ref, down_ref, rows_ref, bias_ref, normed_ref, inv_ref,
               y_ref, gelu_ref, dup_ref, dres3_ref, dres2_ref, tail_ref, upsum_ref):
    step = pl.program_id(0)
    h_b = h_ref[...]
    up = dot_nt(h_b, up_ref[...]) + bias_ref[...]
    cdf = 0.5 * (1.0 + lax.erf(up * 0.7071067811865476))
    gelu = (up * cdf).astype(BF16)
    slope = cdf + up * (0.3989422804014327 * jnp.exp(-0.5 * up * up))
    gelu_ref[...] = gelu
    resid = h_b.astype(F32) + dot(gelu, down_ref[...]) + rows_ref[8:9, :]
    y_b, normed3, inv3 = norm_rows(resid, rows_ref[13:14, :], rows_ref[14:15, :])
    y_ref[...] = y_b
    dy = dy_ref[...].astype(F32)
    d_res3 = norm_rows_bwd(dy, normed3, inv3, rows_ref[13:14, :])
    d_res3_b = d_res3.astype(BF16)
    dres3_ref[...] = d_res3_b
    d_up = dot_nt(d_res3_b, down_ref[...]) * slope
    d_up_b = d_up.astype(BF16)
    dup_ref[...] = d_up_b
    d_h2 = d_res3 + dot(d_up_b, up_ref[...])
    normed2 = normed_ref[...]
    d_res2 = norm_rows_bwd(d_h2, normed2, inv_ref[...], rows_ref[11:12, :])
    dres2_ref[...] = d_res2
    tail = jnp.concatenate([col_sum(d_res2), col_sum(d_res3), col_sum(d_h2 * normed2), col_sum(d_h2), col_sum(dy * normed3), col_sum(dy),
                            jnp.zeros((2, dy.shape[1]), F32)], axis=0)
    up_sum = col_sum(d_up)

    @pl.when(step == 0)
    def _():
        tail_ref[...] = tail
        upsum_ref[...] = up_sum

    @pl.when(step > 0)
    def _():
        tail_ref[...] += tail
        upsum_ref[...] += up_sum


def ffn_both(h2, dy, ffn_full, bias_rows, up_bias, normed2, inv2, block=256):
    n_tok, d_model = h2.shape
    ffn_dim = ffn_full.shape[0] // 2
    tok = pl.BlockSpec((block, d_model), lambda i: (i, 0))
    wide = pl.BlockSpec((block, ffn_dim), lambda i: (i, 0))
    once = lambda shape, idx: pl.BlockSpec(shape, lambda i: idx, pipeline_mode=pl.Buffered(1))
    return pl.pallas_call(
        ffn_kernel, grid=(n_tok // block,),
        in_specs=[tok, tok, once((ffn_dim, d_model), (0, 0)), once((ffn_dim, d_model), (1, 0)), once(bias_rows.shape, (0, 0)), once((1, ffn_dim), (0, 0)),
                  tok, pl.BlockSpec((block, 1), lambda i: (i, 0))],
        out_specs=[tok, wide, wide, tok, tok, pl.BlockSpec((8, d_model), lambda i: (0, 0)), pl.BlockSpec((1, ffn_dim), lambda i: (0, 0))],
        out_shape=[jax.ShapeDtypeStruct(h2.shape, BF16), jax.ShapeDtypeStruct((n_tok, ffn_dim), BF16), jax.ShapeDtypeStruct((n_tok, ffn_dim), BF16),
                   jax.ShapeDtypeStruct(h2.shape, BF16), jax.ShapeDtypeStruct(h2.shape, F32),
                   jax.ShapeDtypeStruct((8, d_model), F32), jax.ShapeDtypeStruct((1, ffn_dim), F32)],
        compiler_params=pltpu.CompilerParams(vmem_limit_bytes=VMEM_BYTES, dimension_semantics=('arbitrary',)),
        cost_estimate=pl.CostEstimate(flops=8 * n_tok * d_model * ffn_dim, bytes_accessed=30 * n_tok * d_model, transcendentals=0),
        name='ffn_both',
    )(h2, dy, ffn_full, ffn_full, bias_rows, up_bias, normed2, inv2)


def layer_acts(dec_in, enc_out, src_lens, tgt_lens, y_cot, attn_full, ffn_full, vec_full):
    n_batch, n_tgt, d_model = dec_in.shape
    x = dec_in.reshape(-1, d_model)
    enc = enc_out.reshape(-1, d_model)
    dy = y_cot.reshape(-1, d_model)
    vec_f = vec_full.astype(F32)
    bias_rows = jnp.pad(vec_f[:15 * d_model].reshape(15, d_model), ((0, 1), (0, 0)))
    up_bias = vec_f[15 * d_model:].reshape(1, -1)
    q1, k1, v1, o1, lse1, h1, normed1, inv1 = attn_forward(x, x, tgt_lens, attn_full, bias_rows, (0, 1, 2, 3), (0, 1, 2, 3, 9), True)
    q2, k2, v2, o2, lse2, h2, normed2, inv2 = attn_forward(h1, enc, src_lens, attn_full, bias_rows, (4, 5, 6, 7), (4, 5, 6, 7, 11), False)
    y, gelu, d_up, d_res3, d_res2, ffn_tail, up_sum = ffn_both(h2, dy, ffn_full, bias_rows, up_bias, normed2, inv2)
    dq2, dk2, dv2, d_res1, d_enc, sums2, tail2 = attn_backward(d_res2, q2, k2, v2, lse2, src_lens, attn_full, bias_rows, (4, 5, 6, 7), False, 9, normed1, inv1)
    dq1, dk1, dv1, d_x, sums1, _ = attn_backward(d_res1, q1, k1, v1, lse1, tgt_lens, attn_full, bias_rows, (0, 1, 2, 3), True)
    s1, s2, t2 = jnp.sum(sums1, axis=0), jnp.sum(sums2, axis=0), jnp.sum(tail2, axis=0)
    g_vec = jnp.concatenate([s1[0:3].reshape(-1), t2[0], s2[0:3].reshape(-1), ffn_tail[0], ffn_tail[1], t2[1], t2[2], ffn_tail[2], ffn_tail[3], ffn_tail[4], ffn_tail[5], up_sum[0]])
    pairs = ((x, dq1), (x, dk1), (x, dv1), (o1, d_res1.astype(BF16)), (h1, dq2), (enc, dk2), (enc, dv2), (o2, d_res2.astype(BF16)))
    ffn_pairs = ((d_up, h2), (gelu, d_res3))
    return y.reshape(dec_in.shape), d_x.reshape(dec_in.shape), d_enc.reshape(enc_out.shape), pairs, ffn_pairs, g_vec
SIDE = 4
LANES = 128
COLOURS = 3
DIM_ORDER = ((2, 1, 0), (1, 0, 2), (0, 2, 1))
MESH_ID = pl.DeviceIdType.MESH


def torus_place():
    chip = lax.axis_index('fsdp')
    return (chip // (SIDE * SIDE), (chip // SIDE) % SIDE, chip % SIDE)


def chip_at(place, dim, shift):
    moved = [lax.rem(p + shift + SIDE, SIDE) if d == dim else p for d, p in enumerate(place)]
    return (moved[0] * SIDE + moved[1]) * SIDE + moved[2]


def meet_neighbours(place):
    barrier = pltpu.get_barrier_semaphore()
    core = lax.axis_index('dp')
    for dim in range(3):
        for shift in (1, -1):
            pl.semaphore_signal(barrier, inc=1, device_id=(core, chip_at(place, dim, shift)), device_id_type=MESH_ID)
    pl.semaphore_signal(barrier, inc=1, device_id=(1 - core, lax.axis_index('fsdp')), device_id_type=MESH_ID)
    pl.semaphore_wait(barrier, 7)


class Counter:
    def __init__(self):
        self.used = 0

    def take(self):
        self.used += 1
        return self.used - 1


def rs_kernel(scale, rows, vec_rows, gffn_ref, gattn_ref, gvec_ref, offn_ref, oattn_ref, ovec_ref,
              acc0, acc1, g10, g11, d10, d11, g20, g21, d20, d21, g30, g31, d30, d31, stage, send_sem, recv_sem, load_sem):
    core = lax.axis_index('dp')
    chip = lax.axis_index('fsdp')
    place = torus_place()
    acc = (acc0, acc1)
    got = ((g10, g20, g30), (g11, g21, g31))
    far = ((d10, d20, d30), (d11, d21, d31))
    height = (rows, rows + vec_rows)
    counter = Counter()
    started = []

    def remote(src, dst, device):
        i = counter.take()
        return pltpu.make_async_remote_copy(src_ref=src, dst_ref=dst, send_sem=send_sem.at[i], recv_sem=recv_sem.at[i], device_id=device, device_id_type=MESH_ID)

    def start(copy):
        copy.start()
        started.append(copy)

    sibling = (1 - core, chip)

    def columns(of_core, colour):
        return pl.ds(pl.multiple_of((of_core * COLOURS + colour) * LANES, LANES), LANES)

    def slot(colour, d):
        dim = DIM_ORDER[colour][0]
        where = [slice(None)] * 3
        where[dim] = lax.rem(place[dim] + d, SIDE)
        return tuple(where)

    pieces = [(q, d, colour) for q in range(2) for d in (2, 1, 3, 0) for colour in range(COLOURS)]
    sources = (gffn_ref, gattn_ref)

    def swap_copies(q, d, colour):
        where = slot(colour, d)
        cols = columns(1 - core, colour)
        copies = [remote(sources[q].at[where + (slice(None), cols)], acc[q].at[(colour,) + where + (pl.ds(0, rows), slice(None))], sibling)]
        if q == 1:
            copies.append(remote(gvec_ref.at[where + (slice(None), cols)], acc[q].at[(colour,) + where + (pl.ds(rows, vec_rows), slice(None))], sibling))
        return copies

    swaps = [swap_copies(*piece) for piece in pieces]

    def load_copies(i):
        q, d, colour = pieces[i]
        where = slot(colour, d)
        cols = columns(core, colour)
        buf = i % 3
        copies = [pltpu.make_async_copy(sources[q].at[where + (slice(None), cols)], stage.at[buf, :, :, pl.ds(0, rows), :], load_sem.at[buf, 0])]
        if q == 1:
            copies.append(pltpu.make_async_copy(gvec_ref.at[where + (slice(None), cols)], stage.at[buf, :, :, pl.ds(rows, vec_rows), :], load_sem.at[buf, 1]))
        return copies

    def ring_copies(q, colour, phase):
        order = DIM_ORDER[colour]
        dim = order[phase]
        rest = sorted(order[phase + 1:])
        n_low = rows // 2

        def block(d, half=None):
            where = [None, None, None]
            for done in order[:phase]:
                where[done] = place[done]
            where[dim] = lax.rem(place[dim] + d, SIDE)
            for i, r in enumerate(rest):
                where[r] = slice(None) if half is None or i > 0 else pl.ds(2 * half, 2)
            tail = (slice(None), slice(None))
            if phase == 2 and half is not None:
                tail = (pl.ds(0, n_low) if half == 0 else pl.ds(n_low, height[q] - n_low), slice(None))
            return acc[q].at[(colour,) + tuple(where) + tail]

        def half_of(ref, direction, half):
            if phase == 2:
                return ref.at[colour, direction, pl.ds(0, n_low) if half == 0 else pl.ds(n_low, height[q] - n_low), :]
            return ref.at[colour, direction, pl.ds(2 * half, 2)]

        def far_of(direction, half):
            if phase == 2:
                return far[q][phase].at[colour, direction, pl.ds(0, n_low if half == 0 else height[q] - n_low), :]
            return far[q][phase].at[colour, direction]

        out = []
        for direction, shift in enumerate((1, -1)):
            device = (core, chip_at(place, dim, shift))
            near = shift % SIDE
            out.append(dict(
                far=remote(block(2, direction), far_of(direction, direction), device),
                own=remote(block(near, 1 - direction), half_of(got[q][phase], direction, 1 - direction), device),
                fed=remote(block(near, direction), half_of(got[q][phase], direction, direction), device),
                fed_view=block(near, direction), far_view=far_of(direction, direction)))
        return out, block(0), [got[q][phase].at[colour, direction] for direction in range(2)]

    rings = {(q, colour, phase): ring_copies(q, colour, phase) for q in range(2) for colour in range(COLOURS) for phase in range(3)}

    def add_into(dst, sources, n_lead):
        def body(i, _):
            idx = {0: (), 1: (i,), 2: (i // SIDE, i % SIDE)}[n_lead]
            total = dst[idx]
            for src in sources:
                total = total + src[idx]
            dst[idx] = total
            return 0

        count = 1
        for n in dst.shape[:n_lead]:
            count *= n
        if n_lead == 0:
            total = dst[...]
            for src in sources:
                total = total + src[...]
            dst[...] = total
        else:
            lax.fori_loop(0, count, body, 0)

    def absorb(i):
        q, d, colour = pieces[i]
        for copy in load_copies(i):
            copy.wait()
        for copy in swaps[i]:
            copy.wait_recv()
        n = height[q]
        add_into(acc[q].at[(colour,) + slot(colour, d)], [stage.at[i % 3, :, :, pl.ds(0, n), :]], 2)
        if i + 3 < len(pieces):
            for copy in load_copies(i + 3):
                copy.start()
        first = rings[(q, colour, 0)][0]
        if d == 2:
            start(first[0]['far'])
            start(first[1]['far'])
        elif d == 1:
            start(first[0]['own'])
        elif d == 3:
            start(first[1]['own'])

    def send_first(q, colour, phase):
        dirs = rings[(q, colour, phase)][0]
        for direction in dirs:
            start(direction['far'])
        for direction in dirs:
            start(direction['own'])

    def relay(q, colour, phase):
        dirs = rings[(q, colour, phase)][0]
        for direction in dirs:
            direction['far'].wait_recv()
            add_into(direction['fed_view'], [direction['far_view']], 2 - phase)
        for direction in dirs:
            start(direction['fed'])

    def settle(q, colour, phase):
        dirs, mine, arrived = rings[(q, colour, phase)]
        for direction in dirs:
            direction['own'].wait_recv()
            direction['fed'].wait_recv()
        add_into(mine, arrived, 2 - phase)
        if phase < 2:
            send_first(q, colour, phase + 1)

    outs = (offn_ref, oattn_ref)
    local, finals = [], []

    def finish(q, colour):
        done = acc[q].at[colour, place[0], place[1], place[2]]
        done[...] = done[...] * scale
        cols = columns(core, colour)
        parts = [(done.at[pl.ds(0, rows), :], outs[q].at[:, cols])]
        if q == 1:
            parts.append((done.at[pl.ds(rows, vec_rows), :], ovec_ref.at[:, cols]))
        for src, dst in parts:
            i = counter.take()
            keep = pltpu.make_async_copy(src, dst, load_sem.at[3 + len(local) // 2, len(local) % 2])
            keep.start()
            local.append(keep)
            give = pltpu.make_async_remote_copy(src_ref=src, dst_ref=dst, send_sem=send_sem.at[i], recv_sem=recv_sem.at[i], device_id=sibling, device_id_type=MESH_ID)
            start(give)
            finals.append(give)

    colours = range(COLOURS)
    meet_neighbours(place)
    for i in range(3):
        for copy in load_copies(i):
            copy.start()
    for group in swaps:
        for copy in group:
            start(copy)
    per_chunk = len(pieces) // 2
    for i in range(9):
        absorb(i)
    for colour in colours:
        relay(0, colour, 0)
    for i in range(9, per_chunk + 9):
        absorb(i)
    for colour in colours:
        settle(0, colour, 0)
    for colour in colours:
        relay(1, colour, 0)
    for i in range(per_chunk + 9, 2 * per_chunk):
        absorb(i)
    for colour in colours:
        relay(0, colour, 1)
    for colour in colours:
        settle(1, colour, 0)
    for colour in colours:
        settle(0, colour, 1)
    for colour in colours:
        relay(1, colour, 1)
    for colour in colours:
        relay(0, colour, 2)
    for colour in colours:
        settle(1, colour, 1)
    for colour in colours:
        settle(0, colour, 2)
        finish(0, colour)
    for colour in colours:
        relay(1, colour, 2)
    for colour in colours:
        settle(1, colour, 2)
        finish(1, colour)
    for copy in finals:
        copy.wait_recv()
    for copy in started:
        copy.wait_send()
    for copy in local:
        copy.wait()


def scatter_grads(g_ffn, g_attn, g_vec, scale):
    n_chips = SIDE ** 3
    width = 2 * COLOURS * LANES
    rows, vec_rows = g_ffn.shape[0] // n_chips, g_vec.shape[0] // n_chips
    as_torus = lambda g: g.reshape(SIDE, SIDE, SIDE, g.shape[0] // n_chips, width)
    heights = (rows, rows + vec_rows)
    n_low = rows // 2
    buf = lambda shape: [pltpu.VMEM((COLOURS,) + shape(h) + (LANES,), F32) for h in heights]
    n_copies = 2 * COLOURS * 3 * 2 * 3 + 2 * COLOURS * 4 + COLOURS * 4 + 9
    scratch = (buf(lambda h: (SIDE, SIDE, SIDE, h)) + buf(lambda h: (2, SIDE, SIDE, h)) + buf(lambda h: (2, 2, SIDE, h))
               + buf(lambda h: (2, SIDE, h)) + buf(lambda h: (2, 2, h)) + buf(lambda h: (2, h)) + buf(lambda h: (2, max(n_low, h - n_low)))
               + [pltpu.VMEM((3, SIDE, SIDE, heights[1], LANES), F32), pltpu.SemaphoreType.DMA((n_copies,)), pltpu.SemaphoreType.DMA((n_copies,)), pltpu.SemaphoreType.DMA((8, 2))])
    anywhere = pl.BlockSpec(memory_space=pl.ANY)
    sent = 4 * width * n_chips * (2 * rows + vec_rows)
    return pl.pallas_call(
        functools.partial(rs_kernel, scale, rows, vec_rows),
        in_specs=[anywhere] * 3, out_specs=[anywhere] * 3,
        out_shape=[jax.ShapeDtypeStruct((rows, width), F32), jax.ShapeDtypeStruct((rows, width), F32), jax.ShapeDtypeStruct((vec_rows, width), F32)],
        scratch_shapes=scratch,
        compiler_params=pltpu.CompilerParams(collective_id=1, has_side_effects=True, vmem_limit_bytes=62 * 1024 * 1024),
        cost_estimate=pl.CostEstimate(flops=10 ** 9, bytes_accessed=2 * sent, transcendentals=0),
        name='scatter_grads',
    )(as_torus(g_ffn), as_torus(g_attn), as_torus(g_vec))


def solution(mesh):
    n_fsdp = mesh.shape['fsdp']
    n_dp = mesh.shape['dp']
    batch_axes = ('dp', 'fsdp')
    all_axes = ('fsdp', 'dp')
    act_spec = P(batch_axes, None, None)
    len_spec = P(batch_axes)
    row_spec = P('fsdp', None)
    vec_spec = P('fsdp')

    def gather_rows(w_rows):
        half = w_rows.shape[0] // n_dp
        mine = lax.dynamic_slice_in_dim(w_rows, lax.axis_index('dp') * half, half, 0)
        return lax.all_gather(mine, all_axes, axis=0, tiled=True)

    def gather_vec(vec_rows):
        n_own = vec_rows.shape[0]
        mine = jnp.where(lax.axis_index('dp') == 0, vec_rows, jnp.zeros_like(vec_rows))
        full = lax.dynamic_update_slice_in_dim(jnp.zeros((n_own * n_fsdp,), vec_rows.dtype), mine, lax.axis_index('fsdp') * n_own, 0)
        return lax.psum(full, all_axes)

    def device_step(dec_in, enc_out, src_lens, tgt_lens, y_cot, attn_w, ffn_w, vec_params):
        y_out, dec_grad, enc_grad, pairs, ffn_pairs, g_vec = layer_acts(dec_in, enc_out, src_lens, tgt_lens, y_cot, gather_rows(attn_w), gather_rows(ffn_w), gather_vec(vec_params))
        grad_scale = 1.0 / (dec_in.shape[0] * dec_in.shape[1] * n_fsdp * n_dp)
        g_ffn = jnp.concatenate([dot_tn(lhs, rhs) for lhs, rhs in ffn_pairs], axis=0)
        g_attn = jnp.concatenate([dot_tn(lhs, rhs) for lhs, rhs in pairs], axis=0)
        n_vec = vec_params.shape[0]
        vec_rows = jnp.pad(g_vec.reshape(n_fsdp, 1, n_vec), ((0, 0), (0, 7), (0, dec_in.shape[2] - n_vec))).reshape(n_fsdp * 8, -1)
        ffn_out, attn_out, vec_out = scatter_grads(g_ffn, g_attn, vec_rows, grad_scale)
        return y_out, dec_grad, enc_grad, attn_out, ffn_out, vec_out[0, :n_vec]

    return jax.shard_map(device_step, mesh=mesh, in_specs=(act_spec, act_spec, len_spec, len_spec, act_spec, row_spec, row_spec, vec_spec), out_specs=(act_spec, act_spec, act_spec, row_spec, row_spec, vec_spec), check_vma=False)
```

```python
import functools
import jax
import jax.numpy as jnp
from jax import lax
from jax.experimental import pallas as pl
from jax.experimental.pallas import tpu as pltpu
from jax.sharding import PartitionSpec as P

HEAD_DIM = 64
LN_EPS = 1e-5
MASK_FILL = -1e30
VMEM_BYTES = 60 * 1024 * 1024
F32 = jnp.float32
BF16 = jnp.bfloat16
GROUP = 256
PAIR = 128


def dot(lhs, rhs, contract=((1,), (0,))):
    return lax.dot_general(lhs, rhs, (contract, ((), ())), preferred_element_type=F32)


def dot_nt(lhs, rhs):
    return dot(lhs, rhs, ((1,), (1,)))


def dot_tn(lhs, rhs):
    return dot(lhs, rhs, ((0,), (0,)))


def norm_rows(resid, gain, shift):
    mean = jnp.mean(resid, axis=-1, keepdims=True)
    centred = resid - mean
    inv_std = lax.rsqrt(jnp.mean(centred * centred, axis=-1, keepdims=True) + LN_EPS)
    normed = centred * inv_std
    return (normed * gain + shift).astype(BF16), normed, inv_std


def norm_rows_bwd(d_out, normed, inv_std, gain):
    d_norm = d_out * gain
    return inv_std * (d_norm - jnp.mean(d_norm, axis=-1, keepdims=True) - normed * jnp.mean(d_norm * normed, axis=-1, keepdims=True))


def col_sum(values):
    return jnp.sum(values, axis=0, keepdims=True)


def head_masks(pair_q, pair_k, head, n_valid):
    lane_q = lax.broadcasted_iota(jnp.int32, pair_q.shape, 1)
    lane_k = lax.broadcasted_iota(jnp.int32, pair_k.shape, 1)
    row_k = lax.broadcasted_iota(jnp.int32, pair_k.shape, 0)
    spare = HEAD_DIM * (1 - head)
    own_q = (lane_q >= HEAD_DIM * head) & (lane_q < HEAD_DIM * (head + 1))
    own_k = (lane_k >= HEAD_DIM * head) & (lane_k < HEAD_DIM * (head + 1))
    q_f = jnp.where(own_q, pair_q.astype(F32), jnp.where(lane_q == spare, 1.0, 0.0)).astype(BF16)
    k_f = jnp.where(own_k, pair_k.astype(F32), jnp.where((lane_k == spare) & (row_k >= n_valid), MASK_FILL, 0.0)).astype(BF16)
    return q_f, k_f


def half_only(pair, head):
    lane = lax.broadcasted_iota(jnp.int32, pair.shape, 1)
    own = (lane >= HEAD_DIM * head) & (lane < HEAD_DIM * (head + 1))
    return jnp.where(own, pair.astype(F32), 0.0).astype(pair.dtype)


def join_halves(first, second):
    lane = lax.broadcasted_iota(jnp.int32, first.shape, 1)
    return jnp.where(lane < HEAD_DIM, first, second)


def scores_t(q_f, k_f, causal):
    s_t = dot_nt(k_f, q_f)
    if causal:
        key_i = lax.broadcasted_iota(jnp.int32, s_t.shape, 0)
        qry_i = lax.broadcasted_iota(jnp.int32, s_t.shape, 1)
        s_t = jnp.where(key_i <= qry_i, s_t, MASK_FILL)
    return s_t


def attend_group(q_g, k_g, v_g, n_valid, causal, lse_ref):
    o_parts = []
    for pair in range(GROUP // PAIR):
        cols = slice(pair * PAIR, (pair + 1) * PAIR)
        q2, k2, v2 = q_g[:, cols], k_g[:, cols], v_g[:, cols]
        v2_t = v2.T
        for head in range(2):
            q_f, k_f = head_masks(q2, k2, head, n_valid)
            s_t = scores_t(q_f, k_f, causal)
            top = jnp.max(s_t, axis=0, keepdims=True)
            e_t = jnp.exp(s_t - top)
            total = jnp.sum(e_t, axis=0, keepdims=True)
            p_t = (e_t * (1.0 / total)).astype(BF16)
            lse_ref[0, 0, pl.ds(2 * pair + head, 1), :] = top + jnp.log(total)
            o_parts.append(dot(v2_t[HEAD_DIM * head:HEAD_DIM * (head + 1)], p_t))
    return jnp.concatenate(o_parts, axis=0).T.astype(BF16)


def attend_group_bwd(d_o, q_g, k_g, v_g, n_valid, causal, lse_ref):
    dq_t, dk, dv = [], [], []
    for pair in range(GROUP // PAIR):
        cols = slice(pair * PAIR, (pair + 1) * PAIR)
        q2, k2, v2, do2 = q_g[:, cols], k_g[:, cols], v_g[:, cols], d_o[:, cols]
        k2_t = k2.T
        dk_h, dv_h = [], []
        for head in range(2):
            q_f, k_f = head_masks(q2, k2, head, n_valid)
            s_t = scores_t(q_f, k_f, causal)
            p_t = jnp.exp(s_t - lse_ref[0, 0, pl.ds(2 * pair + head, 1), :])
            dp_t = dot_nt(half_only(v2, head), do2)
            weighted = p_t * dp_t
            ds_t = (weighted - p_t * jnp.sum(weighted, axis=0, keepdims=True)).astype(BF16)
            dv_h.append(dot(p_t.astype(BF16), do2))
            dk_h.append(dot(ds_t, q2))
            dq_t.append(dot(k2_t[HEAD_DIM * head:HEAD_DIM * (head + 1)], ds_t))
        dk.append(join_halves(*dk_h))
        dv.append(join_halves(*dv_h))
    return jnp.concatenate(dq_t, axis=0).T * 0.125, jnp.concatenate(dk, axis=1), jnp.concatenate(dv, axis=1)


def attn_fwd_kernel(causal, slots, lens_ref, x_ref, kv_ref, wq_ref, wk_ref, wv_ref, wo_ref, bias_ref, rows_ref,
                    q_ref, k_ref, v_ref, o_ref, lse_ref, h_ref, normed_ref, inv_ref, acc_ref):
    q_row, k_row, v_row, o_row, gain_row = slots
    sample, group = pl.program_id(0), pl.program_id(1)
    x_b, kv_b = x_ref[...], kv_ref[...]
    q_g = ((dot(x_b, wq_ref[...]) + bias_ref[q_row:q_row + 1, :]) * 0.125).astype(BF16)
    k_g = (dot(kv_b, wk_ref[...]) + bias_ref[k_row:k_row + 1, :]).astype(BF16)
    v_g = (dot(kv_b, wv_ref[...]) + bias_ref[v_row:v_row + 1, :]).astype(BF16)
    q_ref[...], k_ref[...], v_ref[...] = q_g, k_g, v_g
    o_g = attend_group(q_g, k_g, v_g, lens_ref[sample], causal, lse_ref)
    o_ref[...] = o_g
    part = dot(o_g, wo_ref[...])

    @pl.when(group == 0)
    def _():
        acc_ref[...] = x_ref[...].astype(F32) + part

    @pl.when(group > 0)
    def _():
        acc_ref[...] += part

    @pl.when(group == pl.num_programs(1) - 1)
    def _():
        resid = acc_ref[...] + rows_ref[o_row:o_row + 1, :]
        h_out, normed, inv_std = norm_rows(resid, rows_ref[gain_row:gain_row + 1, :], rows_ref[gain_row + 1:gain_row + 2, :])
        h_ref[...], normed_ref[...], inv_ref[...] = h_out, normed, inv_std


def attn_forward(x, kv, lens, attn_full, bias_rows, mats, slots, causal):
    d_model = x.shape[-1]
    n_batch = lens.shape[0]
    n_q, n_k = x.shape[0] // n_batch, kv.shape[0] // n_batch
    n_groups = d_model // GROUP
    col = lambda mat: pl.BlockSpec((d_model, GROUP), lambda b, g: (mat, g))
    row = lambda mat: pl.BlockSpec((GROUP, d_model), lambda b, g: (mat * n_groups + g, 0))
    q_blk = pl.BlockSpec((n_q, GROUP), lambda b, g: (b, g))
    k_blk = pl.BlockSpec((n_k, GROUP), lambda b, g: (b, g))
    tok = lambda n: pl.BlockSpec((n, d_model), lambda b, g: (b, 0))
    n_heads_g = GROUP // HEAD_DIM
    out_shape = (
        jax.ShapeDtypeStruct(x.shape, BF16), jax.ShapeDtypeStruct(kv.shape, BF16), jax.ShapeDtypeStruct(kv.shape, BF16),
        jax.ShapeDtypeStruct(x.shape, BF16), jax.ShapeDtypeStruct((n_batch, n_groups, n_heads_g, n_q), F32),
        jax.ShapeDtypeStruct(x.shape, BF16), jax.ShapeDtypeStruct(x.shape, F32), jax.ShapeDtypeStruct((x.shape[0], 1), F32))
    return pl.pallas_call(
        functools.partial(attn_fwd_kernel, causal, slots),
        grid=(n_batch, n_groups),
        in_specs=[pl.BlockSpec(memory_space=pltpu.SMEM), tok(n_q), tok(n_k), col(mats[0]), col(mats[1]), col(mats[2]), row(mats[3]),
                  pl.BlockSpec((bias_rows.shape[0], GROUP), lambda b, g: (0, g)), pl.BlockSpec(bias_rows.shape, lambda b, g: (0, 0))],
        out_specs=[q_blk, k_blk, k_blk, q_blk, pl.BlockSpec((1, 1, n_heads_g, n_q), lambda b, g: (b, g, 0, 0)),
                   tok(n_q), tok(n_q), pl.BlockSpec((n_q, 1), lambda b, g: (b, 0))],
        out_shape=out_shape,
        scratch_shapes=[pltpu.VMEM((n_q, d_model), F32)],
        compiler_params=pltpu.CompilerParams(vmem_limit_bytes=VMEM_BYTES, dimension_semantics=('arbitrary', 'arbitrary')),
        cost_estimate=pl.CostEstimate(flops=2 * d_model * d_model * (2 * x.shape[0] + 2 * kv.shape[0]) + 16 * x.shape[0] * n_k * d_model, bytes_accessed=20 * x.shape[0] * d_model, transcendentals=0),
        name='attn_fwd',
    )(lens, x, kv, attn_full, attn_full, attn_full, attn_full, bias_rows, bias_rows)


def attn_bwd_kernel(causal, gain_row, lens_ref, dres_ref, wq_ref, wk_ref, wv_ref, wo_ref, q_ref, k_ref, v_ref, lse_ref,
                    rows_ref, normed_ref, inv_ref, dq_ref, dk_ref, dv_ref, dx_ref, dkv_ref, sums_ref, tail_ref, acc_ref, acc_kv_ref):
    sample, group = pl.program_id(0), pl.program_id(1)
    d_o = dot_nt(dres_ref[...].astype(BF16), wo_ref[...]).astype(BF16)
    dq, dk, dv = attend_group_bwd(d_o, q_ref[...], k_ref[...], v_ref[...], lens_ref[sample], causal, lse_ref)
    sums_ref[0, 0:1, :] = col_sum(dq)
    sums_ref[0, 1:2, :] = col_sum(dk)
    sums_ref[0, 2:3, :] = col_sum(dv)
    dq_b, dk_b, dv_b = dq.astype(BF16), dk.astype(BF16), dv.astype(BF16)
    dq_ref[...], dk_ref[...], dv_ref[...] = dq_b, dk_b, dv_b
    part_q = dot_nt(dq_b, wq_ref[...])
    part_kv = dot_nt(dk_b, wk_ref[...]) + dot_nt(dv_b, wv_ref[...])
    last = pl.num_programs(1) - 1
    if causal:
        @pl.when(group == 0)
        def _():
            acc_ref[...] = dres_ref[...] + part_q + part_kv

        @pl.when(group > 0)
        def _():
            acc_ref[...] += part_q + part_kv

        @pl.when(group == last)
        def _():
            dx_ref[...] = acc_ref[...].astype(BF16)
            tail_ref[...] = jnp.zeros_like(tail_ref)
    else:
        @pl.when(group == 0)
        def _():
            acc_ref[...] = dres_ref[...] + part_q
            acc_kv_ref[...] = part_kv

        @pl.when(group > 0)
        def _():
            acc_ref[...] += part_q
            acc_kv_ref[...] += part_kv

        @pl.when(group == last)
        def _():
            d_h = acc_ref[...]
            normed = normed_ref[...]
            d_resid = norm_rows_bwd(d_h, normed, inv_ref[...], rows_ref[gain_row:gain_row + 1, :])
            dx_ref[...] = d_resid
            dkv_ref[...] = acc_kv_ref[...].astype(BF16)
            tail_ref[0, 0:1, :] = col_sum(d_resid)
            tail_ref[0, 1:2, :] = col_sum(d_h * normed)
            tail_ref[0, 2:3, :] = col_sum(d_h)


def attn_backward(dres, q, k, v, lse, lens, attn_full, bias_rows, mats, causal, gain_row=0, normed=None, inv_std=None):
    d_model = q.shape[-1]
    n_batch = lens.shape[0]
    n_q, n_k = q.shape[0] // n_batch, k.shape[0] // n_batch
    n_groups = d_model // GROUP
    col = lambda mat: pl.BlockSpec((d_model, GROUP), lambda b, g: (mat, g))
    row = lambda mat: pl.BlockSpec((GROUP, d_model), lambda b, g: (mat * n_groups + g, 0))
    q_blk = pl.BlockSpec((n_q, GROUP), lambda b, g: (b, g))
    k_blk = pl.BlockSpec((n_k, GROUP), lambda b, g: (b, g))
    tok = lambda n: pl.BlockSpec((n, d_model), lambda b, g: (b, 0))
    n_heads_g = GROUP // HEAD_DIM
    whole_rows = pl.BlockSpec(bias_rows.shape, lambda b, g: (0, 0))
    kernel = functools.partial(attn_bwd_kernel, causal, gain_row)
    in_specs = [pl.BlockSpec(memory_space=pltpu.SMEM), tok(n_q), col(mats[0]), col(mats[1]), col(mats[2]), row(mats[3]), q_blk, k_blk, k_blk,
                pl.BlockSpec((1, 1, n_heads_g, n_q), lambda b, g: (b, g, 0, 0)), whole_rows]
    args = [lens, dres, attn_full, attn_full, attn_full, attn_full, q, k, v, lse, bias_rows]
    sums_blk = pl.BlockSpec((1, 8, GROUP), lambda b, g: (b, 0, g))
    tail_blk = pl.BlockSpec((1, 8, d_model), lambda b, g: (b, 0, 0))
    tail_shape = jax.ShapeDtypeStruct((n_batch, 8, d_model), F32)
    out_shape = [jax.ShapeDtypeStruct(q.shape, BF16), jax.ShapeDtypeStruct(k.shape, BF16), jax.ShapeDtypeStruct(k.shape, BF16),
                 jax.ShapeDtypeStruct(q.shape, BF16 if causal else F32)]
    out_specs = [q_blk, k_blk, k_blk, tok(n_q)]
    scratch = [pltpu.VMEM((n_q, d_model), F32)]
    if causal:
        def body(*refs):
            ins, rest = refs[:11], refs[11:]
            dq, dk, dv, dx, sums, tail, acc = rest
            kernel(*ins, None, None, dq, dk, dv, dx, None, sums, tail, acc, None)
    else:
        in_specs += [tok(n_q), pl.BlockSpec((n_q, 1), lambda b, g: (b, 0))]
        args += [normed, inv_std]
        out_shape.append(jax.ShapeDtypeStruct(k.shape, BF16))
        out_specs.append(tok(n_k))
        scratch.append(pltpu.VMEM((n_k, d_model), F32))
        body = kernel
    out_shape += [tail_shape, tail_shape]
    out_specs += [sums_blk, tail_blk]
    return pl.pallas_call(
        body, grid=(n_batch, n_groups), in_specs=in_specs, out_specs=out_specs, out_shape=out_shape, scratch_shapes=scratch,
        compiler_params=pltpu.CompilerParams(vmem_limit_bytes=VMEM_BYTES, dimension_semantics=('arbitrary', 'arbitrary')),
        cost_estimate=pl.CostEstimate(flops=2 * d_model * d_model * (2 * q.shape[0] + 2 * k.shape[0]) + 40 * q.shape[0] * n_k * d_model, bytes_accessed=20 * q.shape[0] * d_model, transcendentals=0),
        name='attn_bwd',
    )(*args)


def ffn_kernel(h_ref, dy_ref, up_ref, down_ref, rows_ref, bias_ref, normed_ref, inv_ref,
               y_ref, gelu_ref, dup_ref, dres3_ref, dres2_ref, tail_ref, upsum_ref):
    step = pl.program_id(0)
    h_b = h_ref[...]
    up = dot_nt(h_b, up_ref[...]) + bias_ref[...]
    cdf = 0.5 * (1.0 + lax.erf(up * 0.7071067811865476))
    gelu = (up * cdf).astype(BF16)
    slope = cdf + up * (0.3989422804014327 * jnp.exp(-0.5 * up * up))
    gelu_ref[...] = gelu
    resid = h_b.astype(F32) + dot(gelu, down_ref[...]) + rows_ref[8:9, :]
    y_b, normed3, inv3 = norm_rows(resid, rows_ref[13:14, :], rows_ref[14:15, :])
    y_ref[...] = y_b
    dy = dy_ref[...].astype(F32)
    d_res3 = norm_rows_bwd(dy, normed3, inv3, rows_ref[13:14, :])
    d_res3_b = d_res3.astype(BF16)
    dres3_ref[...] = d_res3_b
    d_up = dot_nt(d_res3_b, down_ref[...]) * slope
    d_up_b = d_up.astype(BF16)
    dup_ref[...] = d_up_b
    d_h2 = d_res3 + dot(d_up_b, up_ref[...])
    normed2 = normed_ref[...]
    d_res2 = norm_rows_bwd(d_h2, normed2, inv_ref[...], rows_ref[11:12, :])
    dres2_ref[...] = d_res2
    tail = jnp.concatenate([col_sum(d_res2), col_sum(d_res3), col_sum(d_h2 * normed2), col_sum(d_h2), col_sum(dy * normed3), col_sum(dy),
                            jnp.zeros((2, dy.shape[1]), F32)], axis=0)
    up_sum = col_sum(d_up)

    @pl.when(step == 0)
    def _():
        tail_ref[...] = tail
        upsum_ref[...] = up_sum

    @pl.when(step > 0)
    def _():
        tail_ref[...] += tail
        upsum_ref[...] += up_sum


def ffn_both(h2, dy, ffn_full, bias_rows, up_bias, normed2, inv2, block=256):
    n_tok, d_model = h2.shape
    ffn_dim = ffn_full.shape[0] // 2
    tok = pl.BlockSpec((block, d_model), lambda i: (i, 0))
    wide = pl.BlockSpec((block, ffn_dim), lambda i: (i, 0))
    once = lambda shape, idx: pl.BlockSpec(shape, lambda i: idx, pipeline_mode=pl.Buffered(1))
    return pl.pallas_call(
        ffn_kernel, grid=(n_tok // block,),
        in_specs=[tok, tok, once((ffn_dim, d_model), (0, 0)), once((ffn_dim, d_model), (1, 0)), once(bias_rows.shape, (0, 0)), once((1, ffn_dim), (0, 0)),
                  tok, pl.BlockSpec((block, 1), lambda i: (i, 0))],
        out_specs=[tok, wide, wide, tok, tok, pl.BlockSpec((8, d_model), lambda i: (0, 0)), pl.BlockSpec((1, ffn_dim), lambda i: (0, 0))],
        out_shape=[jax.ShapeDtypeStruct(h2.shape, BF16), jax.ShapeDtypeStruct((n_tok, ffn_dim), BF16), jax.ShapeDtypeStruct((n_tok, ffn_dim), BF16),
                   jax.ShapeDtypeStruct(h2.shape, BF16), jax.ShapeDtypeStruct(h2.shape, F32),
                   jax.ShapeDtypeStruct((8, d_model), F32), jax.ShapeDtypeStruct((1, ffn_dim), F32)],
        compiler_params=pltpu.CompilerParams(vmem_limit_bytes=VMEM_BYTES, dimension_semantics=('arbitrary',)),
        cost_estimate=pl.CostEstimate(flops=8 * n_tok * d_model * ffn_dim, bytes_accessed=30 * n_tok * d_model, transcendentals=0),
        name='ffn_both',
    )(h2, dy, ffn_full, ffn_full, bias_rows, up_bias, normed2, inv2)


def layer_acts(dec_in, enc_out, src_lens, tgt_lens, y_cot, attn_full, ffn_full, vec_full):
    n_batch, n_tgt, d_model = dec_in.shape
    x = dec_in.reshape(-1, d_model)
    enc = enc_out.reshape(-1, d_model)
    dy = y_cot.reshape(-1, d_model)
    vec_f = vec_full.astype(F32)
    bias_rows = jnp.pad(vec_f[:15 * d_model].reshape(15, d_model), ((0, 1), (0, 0)))
    up_bias = vec_f[15 * d_model:].reshape(1, -1)
    q1, k1, v1, o1, lse1, h1, normed1, inv1 = attn_forward(x, x, tgt_lens, attn_full, bias_rows, (0, 1, 2, 3), (0, 1, 2, 3, 9), True)
    q2, k2, v2, o2, lse2, h2, normed2, inv2 = attn_forward(h1, enc, src_lens, attn_full, bias_rows, (4, 5, 6, 7), (4, 5, 6, 7, 11), False)
    y, gelu, d_up, d_res3, d_res2, ffn_tail, up_sum = ffn_both(h2, dy, ffn_full, bias_rows, up_bias, normed2, inv2)
    dq2, dk2, dv2, d_res1, d_enc, sums2, tail2 = attn_backward(d_res2, q2, k2, v2, lse2, src_lens, attn_full, bias_rows, (4, 5, 6, 7), False, 9, normed1, inv1)
    dq1, dk1, dv1, d_x, sums1, _ = attn_backward(d_res1, q1, k1, v1, lse1, tgt_lens, attn_full, bias_rows, (0, 1, 2, 3), True)
    s1, s2, t2 = jnp.sum(sums1, axis=0), jnp.sum(sums2, axis=0), jnp.sum(tail2, axis=0)
    g_vec = jnp.concatenate([s1[0:3].reshape(-1), t2[0], s2[0:3].reshape(-1), ffn_tail[0], ffn_tail[1], t2[1], t2[2], ffn_tail[2], ffn_tail[3], ffn_tail[4], ffn_tail[5], up_sum[0]])
    pairs = ((x, dq1), (x, dk1), (x, dv1), (o1, d_res1.astype(BF16)), (h1, dq2), (enc, dk2), (enc, dv2), (o2, d_res2.astype(BF16)))
    ffn_pairs = ((d_up, h2), (gelu, d_res3))
    return y.reshape(dec_in.shape), d_x.reshape(dec_in.shape), d_enc.reshape(enc_out.shape), pairs, ffn_pairs, g_vec
SIDE = 4
LANES = 128
COLOURS = 3
DIM_ORDER = ((2, 1, 0), (1, 0, 2), (0, 2, 1))
MESH_ID = pl.DeviceIdType.MESH


def torus_place():
    chip = lax.axis_index('fsdp')
    return (chip // (SIDE * SIDE), (chip // SIDE) % SIDE, chip % SIDE)


def chip_at(place, dim, shift):
    moved = [lax.rem(p + shift + SIDE, SIDE) if d == dim else p for d, p in enumerate(place)]
    return (moved[0] * SIDE + moved[1]) * SIDE + moved[2]


def meet_neighbours(place):
    barrier = pltpu.get_barrier_semaphore()
    core = lax.axis_index('dp')
    for dim in range(3):
        for shift in (1, -1):
            pl.semaphore_signal(barrier, inc=1, device_id=(core, chip_at(place, dim, shift)), device_id_type=MESH_ID)
    pl.semaphore_signal(barrier, inc=1, device_id=(1 - core, lax.axis_index('fsdp')), device_id_type=MESH_ID)
    pl.semaphore_wait(barrier, 7)


class Counter:
    def __init__(self):
        self.used = 0

    def take(self):
        self.used += 1
        return self.used - 1


def rs_kernel(scale, rows, vec_rows, gffn_ref, gattn_ref, gvec_ref, offn_ref, oattn_ref, ovec_ref,
              acc0, acc1, g10, g11, d10, d11, g20, g21, d20, d21, g30, g31, d30, d31, stage, send_sem, recv_sem, load_sem):
    core = lax.axis_index('dp')
    chip = lax.axis_index('fsdp')
    place = torus_place()
    acc = (acc0, acc1)
    got = ((g10, g20, g30), (g11, g21, g31))
    far = ((d10, d20, d30), (d11, d21, d31))
    height = (rows, rows + vec_rows)
    counter = Counter()
    started = []

    def remote(src, dst, device):
        i = counter.take()
        return pltpu.make_async_remote_copy(src_ref=src, dst_ref=dst, send_sem=send_sem.at[i], recv_sem=recv_sem.at[i], device_id=device, device_id_type=MESH_ID)

    def start(copy):
        copy.start()
        started.append(copy)

    sibling = (1 - core, chip)

    def columns(of_core, colour):
        return pl.ds(pl.multiple_of((of_core * COLOURS + colour) * LANES, LANES), LANES)

    def slot(colour, d):
        dim = DIM_ORDER[colour][0]
        where = [slice(None)] * 3
        where[dim] = lax.rem(place[dim] + d, SIDE)
        return tuple(where)

    pieces = [(q, d, colour) for q in range(2) for d in (2, 1, 3, 0) for colour in range(COLOURS)]
    sources = (gffn_ref, gattn_ref)

    def swap_copies(q, d, colour):
        where = slot(colour, d)
        cols = columns(1 - core, colour)
        copies = [remote(sources[q].at[where + (slice(None), cols)], acc[q].at[(colour,) + where + (pl.ds(0, rows), slice(None))], sibling)]
        if q == 1:
            copies.append(remote(gvec_ref.at[where + (slice(None), cols)], acc[q].at[(colour,) + where + (pl.ds(rows, vec_rows), slice(None))], sibling))
        return copies

    swaps = [swap_copies(*piece) for piece in pieces]

    def load_copies(i):
        q, d, colour = pieces[i]
        where = slot(colour, d)
        cols = columns(core, colour)
        buf = i % 3
        copies = [pltpu.make_async_copy(sources[q].at[where + (slice(None), cols)], stage.at[buf, :, :, pl.ds(0, rows), :], load_sem.at[buf, 0])]
        if q == 1:
            copies.append(pltpu.make_async_copy(gvec_ref.at[where + (slice(None), cols)], stage.at[buf, :, :, pl.ds(rows, vec_rows), :], load_sem.at[buf, 1]))
        return copies

    def ring_copies(q, colour, phase):
        order = DIM_ORDER[colour]
        dim = order[phase]
        rest = sorted(order[phase + 1:])
        n_low = rows // 2

        def block(d, half=None):
            where = [None, None, None]
            for done in order[:phase]:
                where[done] = place[done]
            where[dim] = lax.rem(place[dim] + d, SIDE)
            for i, r in enumerate(rest):
                where[r] = slice(None) if half is None or i > 0 else pl.ds(2 * half, 2)
            tail = (slice(None), slice(None))
            if phase == 2 and half is not None:
                tail = (pl.ds(0, n_low) if half == 0 else pl.ds(n_low, height[q] - n_low), slice(None))
            return acc[q].at[(colour,) + tuple(where) + tail]

        def half_of(ref, direction, half):
            if phase == 2:
                return ref.at[colour, direction, pl.ds(0, n_low) if half == 0 else pl.ds(n_low, height[q] - n_low), :]
            return ref.at[colour, direction, pl.ds(2 * half, 2)]

        def far_of(direction, half):
            if phase == 2:
                return far[q][phase].at[colour, direction, pl.ds(0, n_low if half == 0 else height[q] - n_low), :]
            return far[q][phase].at[colour, direction]

        out = []
        for direction, shift in enumerate((1, -1)):
            device = (core, chip_at(place, dim, shift))
            near = shift % SIDE
            out.append(dict(
                far=remote(block(2, direction), far_of(direction, direction), device),
                own=remote(block(near, 1 - direction), half_of(got[q][phase], direction, 1 - direction), device),
                fed=remote(block(near, direction), half_of(got[q][phase], direction, direction), device),
                fed_view=block(near, direction), far_view=far_of(direction, direction)))
        return out, block(0), [got[q][phase].at[colour, direction] for direction in range(2)]

    rings = {(q, colour, phase): ring_copies(q, colour, phase) for q in range(2) for colour in range(COLOURS) for phase in range(3)}

    def add_into(dst, sources, n_lead):
        def body(i, _):
            idx = {0: (), 1: (i,), 2: (i // SIDE, i % SIDE)}[n_lead]
            total = dst[idx]
            for src in sources:
                total = total + src[idx]
            dst[idx] = total
            return 0

        count = 1
        for n in dst.shape[:n_lead]:
            count *= n
        if n_lead == 0:
            total = dst[...]
            for src in sources:
                total = total + src[...]
            dst[...] = total
        else:
            lax.fori_loop(0, count, body, 0)

    def absorb(i):
        q, d, colour = pieces[i]
        for copy in load_copies(i):
            copy.wait()
        for copy in swaps[i]:
            copy.wait_recv()
        n = height[q]
        add_into(acc[q].at[(colour,) + slot(colour, d)], [stage.at[i % 3, :, :, pl.ds(0, n), :]], 2)
        if i + 3 < len(pieces):
            for copy in load_copies(i + 3):
                copy.start()
        first = rings[(q, colour, 0)][0]
        if d == 2:
            start(first[0]['far'])
            start(first[1]['far'])
        elif d == 1:
            start(first[0]['own'])
        elif d == 3:
            start(first[1]['own'])

    def send_first(q, colour, phase):
        dirs = rings[(q, colour, phase)][0]
        for direction in dirs:
            start(direction['far'])
        for direction in dirs:
            start(direction['own'])

    def relay(q, colour, phase):
        dirs = rings[(q, colour, phase)][0]
        for direction in dirs:
            direction['far'].wait_recv()
            add_into(direction['fed_view'], [direction['far_view']], 2 - phase)
        for direction in dirs:
            start(direction['fed'])

    def settle(q, colour, phase):
        dirs, mine, arrived = rings[(q, colour, phase)]
        for direction in dirs:
            direction['own'].wait_recv()
            direction['fed'].wait_recv()
        add_into(mine, arrived, 2 - phase)
        if phase < 2:
            send_first(q, colour, phase + 1)

    outs = (offn_ref, oattn_ref)
    local, finals = [], []

    def finish(q, colour):
        done = acc[q].at[colour, place[0], place[1], place[2]]
        done[...] = done[...] * scale
        cols = columns(core, colour)
        parts = [(done.at[pl.ds(0, rows), :], outs[q].at[:, cols])]
        if q == 1:
            parts.append((done.at[pl.ds(rows, vec_rows), :], ovec_ref.at[:, cols]))
        for src, dst in parts:
            i = counter.take()
            keep = pltpu.make_async_copy(src, dst, load_sem.at[3 + len(local) // 2, len(local) % 2])
            keep.start()
            local.append(keep)
            give = pltpu.make_async_remote_copy(src_ref=src, dst_ref=dst, send_sem=send_sem.at[i], recv_sem=recv_sem.at[i], device_id=sibling, device_id_type=MESH_ID)
            start(give)
            finals.append(give)

    colours = range(COLOURS)
    meet_neighbours(place)
    for i in range(3):
        for copy in load_copies(i):
            copy.start()
    for group in swaps:
        for copy in group:
            start(copy)
    per_chunk = len(pieces) // 2
    for i in range(9):
        absorb(i)
    for colour in colours:
        relay(0, colour, 0)
    for i in range(9, per_chunk + 9):
        absorb(i)
    for colour in colours:
        settle(0, colour, 0)
    for colour in colours:
        relay(1, colour, 0)
    for i in range(per_chunk + 9, 2 * per_chunk):
        absorb(i)
    for colour in colours:
        relay(0, colour, 1)
    for colour in colours:
        settle(1, colour, 0)
    for colour in colours:
        settle(0, colour, 1)
    for colour in colours:
        relay(1, colour, 1)
    for colour in colours:
        relay(0, colour, 2)
    for colour in colours:
        settle(1, colour, 1)
    for colour in colours:
        settle(0, colour, 2)
        finish(0, colour)
    for colour in colours:
        relay(1, colour, 2)
    for colour in colours:
        settle(1, colour, 2)
        finish(1, colour)
    for copy in finals:
        copy.wait_recv()
    for copy in started:
        copy.wait_send()
    for copy in local:
        copy.wait()


def scatter_grads(g_ffn, g_attn, g_vec, scale):
    n_chips = SIDE ** 3
    width = 2 * COLOURS * LANES
    rows, vec_rows = g_ffn.shape[0] // n_chips, g_vec.shape[0] // n_chips
    as_torus = lambda g: g.reshape(SIDE, SIDE, SIDE, g.shape[0] // n_chips, width)
    heights = (rows, rows + vec_rows)
    n_low = rows // 2
    buf = lambda shape: [pltpu.VMEM((COLOURS,) + shape(h) + (LANES,), F32) for h in heights]
    n_copies = 2 * COLOURS * 3 * 2 * 3 + 2 * COLOURS * 4 + COLOURS * 4 + 9
    scratch = (buf(lambda h: (SIDE, SIDE, SIDE, h)) + buf(lambda h: (2, SIDE, SIDE, h)) + buf(lambda h: (2, 2, SIDE, h))
               + buf(lambda h: (2, SIDE, h)) + buf(lambda h: (2, 2, h)) + buf(lambda h: (2, h)) + buf(lambda h: (2, max(n_low, h - n_low)))
               + [pltpu.VMEM((3, SIDE, SIDE, heights[1], LANES), F32), pltpu.SemaphoreType.DMA((n_copies,)), pltpu.SemaphoreType.DMA((n_copies,)), pltpu.SemaphoreType.DMA((8, 2))])
    anywhere = pl.BlockSpec(memory_space=pl.ANY)
    sent = 4 * width * n_chips * (2 * rows + vec_rows)
    return pl.pallas_call(
        functools.partial(rs_kernel, scale, rows, vec_rows),
        in_specs=[anywhere] * 3, out_specs=[anywhere] * 3,
        out_shape=[jax.ShapeDtypeStruct((rows, width), F32), jax.ShapeDtypeStruct((rows, width), F32), jax.ShapeDtypeStruct((vec_rows, width), F32)],
        scratch_shapes=scratch,
        compiler_params=pltpu.CompilerParams(collective_id=1, has_side_effects=True, vmem_limit_bytes=62 * 1024 * 1024),
        cost_estimate=pl.CostEstimate(flops=10 ** 9, bytes_accessed=2 * sent, transcendentals=0),
        name='scatter_grads',
    )(as_torus(g_ffn), as_torus(g_attn), as_torus(g_vec))


def ag_kernel(attn_ref, ffn_ref, vec_ref, oattn_ref, offn_ref, vec_out, attn_v, ffn_v, send_sem, recv_sem, load_sem):
    core = lax.axis_index('dp')
    chip = lax.axis_index('fsdp')
    place = torus_place()
    sibling = (1 - core, chip)
    owns = (attn_ref, ffn_ref, vec_ref)
    bufs = (attn_v, ffn_v, vec_out)
    outs = (oattn_ref, offn_ref)
    rows, width = attn_ref.shape
    band = rows // (2 * COLOURS)
    vec_high = vec_ref.shape[0]
    counter, loads = Counter(), Counter()
    started, stores = [], []
    streams = [(w, colour) for w in range(2) for colour in range(COLOURS)] + [(2, 1)]

    def remote(src, dst, device):
        i = counter.take()
        return pltpu.make_async_remote_copy(src_ref=src, dst_ref=dst, send_sem=send_sem.at[i], recv_sem=recv_sem.at[i], device_id=device, device_id_type=MESH_ID)

    def start(copy):
        copy.start()
        started.append(copy)

    def band_rows(colour):
        return pl.ds(pl.multiple_of((core * COLOURS + colour) * band, band), band)

    def tail_of(w, colour, half=None):
        if w == 2:
            return (slice(None) if half is None else pl.ds(half * (vec_high // 2), vec_high // 2), slice(None))
        return (band_rows(colour), slice(None) if half is None else pl.ds(half * (width // 2), width // 2))

    def ring_copies(w, colour, phase):
        order = DIM_ORDER[colour]
        dim = order[phase]
        have = sorted(order[:phase])

        def index(shift, half=None):
            where = [place[0], place[1], place[2]]
            where[dim] = lax.rem(place[dim] + shift + SIDE, SIDE)
            for i, h in enumerate(have):
                where[h] = slice(None) if half is None or i > 0 else pl.ds(2 * half, 2)
            return tuple(where) + tail_of(w, colour, half if phase == 0 else None)

        out = []
        for direction, shift in enumerate((1, -1)):
            device = (core, chip_at(place, dim, shift))
            mine = owns[w].at[tail_of(w, colour)] if phase == 0 else bufs[w].at[index(0)]
            out.append(dict(
                near=remote(mine, bufs[w].at[index(0)], device),
                far=remote(bufs[w].at[index(-shift, direction)], bufs[w].at[index(-shift, direction)], device),
                near_at=index(-shift), far_at=index(2, direction)))
        return out

    rings = {(w, colour, phase): ring_copies(w, colour, phase) for w, colour in streams for phase in range(3)}

    def plane_at(colour):
        last = DIM_ORDER[colour][2]
        return tuple(place[d] if d == last else slice(None) for d in range(3)) + (band_rows(colour), slice(None))

    def publish(w, at):
        i = counter.take()
        keep = pltpu.make_async_copy(bufs[w].at[at], outs[w].at[at], load_sem.at[loads.take()])
        keep.start()
        stores.append(keep)
        give = pltpu.make_async_remote_copy(src_ref=bufs[w].at[at], dst_ref=outs[w].at[at], send_sem=send_sem.at[i], recv_sem=recv_sem.at[i], device_id=sibling, device_id_type=MESH_ID)
        start(give)
        finals.append(give)

    finals = []

    def send_near(w, phase):
        for sw, colour in streams:
            if sw == w:
                for direction in rings[(w, colour, phase)]:
                    start(direction['near'])

    def pass_on(w, phase):
        for sw, colour in streams:
            if sw == w:
                for direction in rings[(w, colour, phase)]:
                    direction['near'].wait_recv()
                    start(direction['far'])
        if phase == 2 and w < 2:
            for sw, colour in streams:
                if sw == w:
                    for direction in rings[(w, colour, phase)]:
                        publish(w, direction['near_at'])

    def complete(w, phase):
        for sw, colour in streams:
            if sw == w:
                for direction in rings[(w, colour, phase)]:
                    direction['far'].wait_recv()
                if phase == 2 and w < 2:
                    for direction in rings[(w, colour, phase)]:
                        publish(w, direction['far_at'])
        if phase < 2:
            send_near(w, phase + 1)
        if phase == 1 and w < 2:
            for colour in range(COLOURS):
                publish(w, plane_at(colour))

    for w, colour in streams:
        bufs[w][(place[0], place[1], place[2]) + tail_of(w, colour)] = owns[w][tail_of(w, colour)]
    meet_neighbours(place)
    for w in (0, 2, 1):
        send_near(w, 0)
    for phase in range(3):
        for w in (0, 2, 1):
            pass_on(w, phase)
        for w in (0, 2, 1):
            complete(w, phase)
    for copy in finals:
        copy.wait_recv()
    for copy in started:
        copy.wait_send()
    for copy in stores:
        copy.wait()


def gather_params(attn_w, ffn_w, vec_rows):
    rows, width = attn_w.shape
    full = (SIDE, SIDE, SIDE, rows, width)
    n_copies = 3 * 4 * 7 + 2 * COLOURS * 5
    vmem = pl.BlockSpec(memory_space=pltpu.VMEM)
    anywhere = pl.BlockSpec(memory_space=pl.ANY)
    attn_full, ffn_full, vec_full = pl.pallas_call(
        ag_kernel,
        in_specs=[vmem] * 3, out_specs=[anywhere, anywhere, vmem],
        out_shape=[jax.ShapeDtypeStruct(full, BF16), jax.ShapeDtypeStruct(full, BF16), jax.ShapeDtypeStruct((SIDE, SIDE, SIDE) + vec_rows.shape, F32)],
        scratch_shapes=[pltpu.VMEM(full, BF16), pltpu.VMEM(full, BF16), pltpu.SemaphoreType.DMA((n_copies,)), pltpu.SemaphoreType.DMA((n_copies,)),
                        pltpu.SemaphoreType.DMA((2 * COLOURS * 5,))],
        compiler_params=pltpu.CompilerParams(collective_id=2, has_side_effects=True, vmem_limit_bytes=VMEM_BYTES),
        cost_estimate=pl.CostEstimate(flops=10 ** 9, bytes_accessed=4 * rows * width * SIDE ** 3, transcendentals=0),
        name='gather_params',
    )(attn_w, ffn_w, vec_rows)
    return attn_full.reshape(-1, width), ffn_full.reshape(-1, width), vec_full


def square_grads(pairs, d_model):
    blocks = [dot_tn(lhs[:, i:i + d_model], rhs) for lhs, rhs in pairs for i in range(0, lhs.shape[1], d_model)]
    return jnp.concatenate(blocks, axis=0)


def solution(mesh):
    n_fsdp = mesh.shape['fsdp']
    n_dp = mesh.shape['dp']
    batch_axes = ('dp', 'fsdp')
    act_spec = P(batch_axes, None, None)
    len_spec = P(batch_axes)
    row_spec = P('fsdp', None)
    vec_spec = P('fsdp')

    def device_step(dec_in, enc_out, src_lens, tgt_lens, y_cot, attn_w, ffn_w, vec_params):
        d_model, n_vec = dec_in.shape[2], vec_params.shape[0]
        vec_rows = jnp.pad(vec_params.astype(F32), (0, 16 * LANES - n_vec)).reshape(16, LANES)
        attn_full, ffn_full, vec_tiles = gather_params(attn_w, ffn_w, vec_rows)
        vec_full = vec_tiles.reshape(n_fsdp, 16, LANES)[:, :2].reshape(n_fsdp, 2 * LANES)[:, :n_vec].reshape(-1)
        y_out, dec_grad, enc_grad, pairs, ffn_pairs, g_vec = layer_acts(dec_in, enc_out, src_lens, tgt_lens, y_cot, attn_full, ffn_full, vec_full)
        grad_scale = 1.0 / (dec_in.shape[0] * dec_in.shape[1] * n_fsdp * n_dp)
        g_rows = jnp.pad(g_vec.reshape(n_fsdp, 1, n_vec), ((0, 0), (0, 7), (0, d_model - n_vec))).reshape(n_fsdp * 8, -1)
        ffn_out, attn_out, vec_out = scatter_grads(square_grads(ffn_pairs, d_model), square_grads(pairs, d_model), g_rows, grad_scale)
        return y_out, dec_grad, enc_grad, attn_out, ffn_out, vec_out[0, :n_vec]

    return jax.shard_map(device_step, mesh=mesh, in_specs=(act_spec, act_spec, len_spec, len_spec, act_spec, row_spec, row_spec, vec_spec), out_specs=(act_spec, act_spec, act_spec, row_spec, row_spec, vec_spec), check_vma=False)
```

```python
import functools
import jax
import jax.numpy as jnp
from jax import lax
from jax.experimental import pallas as pl
from jax.experimental.pallas import tpu as pltpu
from jax.sharding import PartitionSpec as P

HEAD_DIM = 64
LN_EPS = 1e-5
MASK_FILL = -1e30
VMEM_BYTES = 60 * 1024 * 1024
F32 = jnp.float32
BF16 = jnp.bfloat16
GROUP = 256
PAIR = 128


def dot(lhs, rhs, contract=((1,), (0,))):
    return lax.dot_general(lhs, rhs, (contract, ((), ())), preferred_element_type=F32)


def dot_nt(lhs, rhs):
    return dot(lhs, rhs, ((1,), (1,)))


def dot_tn(lhs, rhs):
    return dot(lhs, rhs, ((0,), (0,)))


def norm_rows(resid, gain, shift):
    mean = jnp.mean(resid, axis=-1, keepdims=True)
    centred = resid - mean
    inv_std = lax.rsqrt(jnp.mean(centred * centred, axis=-1, keepdims=True) + LN_EPS)
    normed = centred * inv_std
    return (normed * gain + shift).astype(BF16), normed, inv_std


def norm_rows_bwd(d_out, normed, inv_std, gain):
    d_norm = d_out * gain
    return inv_std * (d_norm - jnp.mean(d_norm, axis=-1, keepdims=True) - normed * jnp.mean(d_norm * normed, axis=-1, keepdims=True))


def col_sum(values):
    return jnp.sum(values, axis=0, keepdims=True)


def lane_row(head, dtype=BF16):
    lane = lax.broadcasted_iota(jnp.int32, (1, PAIR), 1)
    return jnp.where((lane >= HEAD_DIM * head) & (lane < HEAD_DIM * (head + 1)), 1.0, 0.0).astype(dtype)


def spare_lane(head):
    lane = lax.broadcasted_iota(jnp.int32, (1, PAIR), 1)
    return jnp.where(lane == HEAD_DIM * (1 - head), 1.0, 0.0)


def mask_fill(n_rows, n_valid):
    row = lax.broadcasted_iota(jnp.int32, (n_rows, PAIR), 0)
    return jnp.where(row >= n_valid, MASK_FILL, 0.0)


def head_masks(pair_q, pair_k, head, fill):
    q_f = pair_q * lane_row(head) + spare_lane(head).astype(BF16)
    k_f = pair_k * lane_row(head) + (fill * spare_lane(head)).astype(BF16)
    return q_f, k_f


def half_only(pair, head):
    return pair * lane_row(head)


def join_halves(first, second):
    lane = lax.broadcasted_iota(jnp.int32, first.shape, 1)
    return jnp.where(lane < HEAD_DIM, first, second)


def score_blocks(n_heads, n_q, n_k, causal, step):
    if not causal:
        return [(head, 0, n_q, n_k) for head in range(n_heads)]
    return [(head, first, step, first + step) for head in range(n_heads) for first in range(0, n_q, step)]


def scores_t(q_f, k_f, causal, first):
    s_t = dot_nt(k_f, q_f)
    if causal:
        key_i = lax.broadcasted_iota(jnp.int32, s_t.shape, 0)
        qry_i = lax.broadcasted_iota(jnp.int32, s_t.shape, 1) + first
        s_t = jnp.where(key_i <= qry_i, s_t, MASK_FILL)
    return s_t


def pair_of(group, head):
    return group[:, head // 2 * PAIR:(head // 2 + 1) * PAIR]


def masked_pairs(q_g, k_g, n_valid):
    fill = mask_fill(k_g.shape[0], n_valid)
    cache = {}

    def get(head):
        if head not in cache:
            cache[head] = head_masks(pair_of(q_g, head), pair_of(k_g, head), head % 2, fill)
        return cache[head]

    return get


def stack_heads(parts, n_heads):
    return jnp.concatenate([jnp.concatenate(parts[head], axis=1) for head in range(n_heads)], axis=0)


def run_ahead(blocks, produce, transform, consume, delay):
    ahead = produce(blocks[0])
    waiting = []
    for i, block in enumerate(blocks):
        now = ahead
        if i + 1 < len(blocks):
            ahead = produce(blocks[i + 1])
        waiting.append((block, transform(block, now)))
        if len(waiting) > delay:
            consume(*waiting.pop(0))
    for item in waiting:
        consume(*item)


def attend_group(q_g, k_g, v_g, n_valid, causal, lse_ref):
    n_heads = GROUP // HEAD_DIM
    o_parts = [[] for _ in range(n_heads)]
    v_t = v_g.T
    masked = masked_pairs(q_g, k_g, n_valid)

    def produce(block):
        head, first, n_q, n_k = block
        q_f, k_f = masked(head)
        return scores_t(q_f[first:first + n_q], k_f[:n_k], causal, first)

    def transform(block, s_t):
        head, first, n_q, n_k = block
        top = jnp.max(s_t, axis=0, keepdims=True)
        e_t = jnp.exp(s_t - top)
        total = jnp.sum(e_t, axis=0, keepdims=True)
        lse_ref[0, 0, head:head + 1, first:first + n_q] = top + jnp.log(total)
        return (e_t * (1.0 / total)).astype(BF16)

    def consume(block, p_t):
        head, first, n_q, n_k = block
        o_parts[head].append(dot(v_t[HEAD_DIM * head:HEAD_DIM * (head + 1), :n_k], p_t))

    run_ahead(score_blocks(n_heads, q_g.shape[0], k_g.shape[0], causal, 128), produce, transform, consume, 2)
    return stack_heads(o_parts, n_heads).T.astype(BF16)


def attend_group_bwd(d_o, q_g, k_g, v_g, n_valid, causal, lse_ref):
    n_heads = GROUP // HEAD_DIM
    k_t = k_g.T
    dq_t, dk_h, dv_h = [[] for _ in range(n_heads)], [None] * n_heads, [None] * n_heads
    masked = masked_pairs(q_g, k_g, n_valid)
    v_half = {}

    def produce(block):
        head, first, n_q, n_k = block
        q_f, k_f = masked(head)
        if head not in v_half:
            v_half[head] = half_only(pair_of(v_g, head), head % 2)
        rows = slice(first, first + n_q)
        return scores_t(q_f[rows], k_f[:n_k], causal, first), dot_nt(v_half[head][:n_k], pair_of(d_o, head)[rows])

    def transform(block, products):
        head, first, n_q, n_k = block
        s_t, dp_t = products
        p_t = jnp.exp(s_t - lse_ref[0, 0, head:head + 1, first:first + n_q])
        weighted = p_t * dp_t
        return p_t.astype(BF16), (weighted - p_t * jnp.sum(weighted, axis=0, keepdims=True)).astype(BF16)

    def grow(old, new):
        if old is None:
            return new
        n_old = old.shape[0]
        return old + new if n_old == new.shape[0] else jnp.concatenate([old + new[:n_old], new[n_old:]], axis=0)

    def consume(block, operands):
        head, first, n_q, n_k = block
        p_b, ds_t = operands
        rows = slice(first, first + n_q)
        dv_h[head] = grow(dv_h[head], dot(p_b, pair_of(d_o, head)[rows]))
        dk_h[head] = grow(dk_h[head], dot(ds_t, pair_of(q_g, head)[rows]))
        dq_t[head].append(dot(k_t[HEAD_DIM * head:HEAD_DIM * (head + 1), :n_k], ds_t))

    run_ahead(score_blocks(n_heads, q_g.shape[0], k_g.shape[0], causal, 256), produce, transform, consume, 0)
    join = lambda parts: jnp.concatenate([join_halves(parts[h], parts[h + 1]) for h in range(0, n_heads, 2)], axis=1)
    return stack_heads(dq_t, n_heads).T * 0.125, join(dk_h), join(dv_h)


def attn_fwd_kernel(causal, slots, lens_ref, x_ref, kv_ref, wq_ref, wk_ref, wv_ref, w_all, bias_ref, rows_ref,
                    q_ref, k_ref, v_ref, o_ref, lse_ref, h_ref, normed_ref, inv_ref, o_all, wo_v, load_sem):
    q_row, k_row, v_row, o_row, gain_row, o_mat = slots
    sample, group = pl.program_id(0), pl.program_id(1)
    d_model = wo_v.shape[0]
    fetch = pltpu.make_async_copy(w_all.at[pl.ds(o_mat * d_model, d_model), :], wo_v, load_sem)

    @pl.when((sample == 0) & (group == 0))
    def _():
        fetch.start()

    x_b, kv_b = x_ref[...], kv_ref[...]
    q_g = ((dot(x_b, wq_ref[...]) + bias_ref[q_row:q_row + 1, :]) * 0.125).astype(BF16)
    k_g = (dot(kv_b, wk_ref[...]) + bias_ref[k_row:k_row + 1, :]).astype(BF16)
    v_g = (dot(kv_b, wv_ref[...]) + bias_ref[v_row:v_row + 1, :]).astype(BF16)
    q_ref[...], k_ref[...], v_ref[...] = q_g, k_g, v_g
    o_g = attend_group(q_g, k_g, v_g, lens_ref[sample], causal, lse_ref)
    o_ref[...] = o_g
    o_all[:, pl.ds(pl.multiple_of(group * GROUP, GROUP), GROUP)] = o_g

    @pl.when((sample == 0) & (group == pl.num_programs(1) - 1))
    def _():
        fetch.wait()

    @pl.when(group == pl.num_programs(1) - 1)
    def _():
        resid = x_ref[...].astype(F32) + dot(o_all[...], wo_v[...]) + rows_ref[o_row:o_row + 1, :]
        h_out, normed, inv_std = norm_rows(resid, rows_ref[gain_row:gain_row + 1, :], rows_ref[gain_row + 1:gain_row + 2, :])
        h_ref[...], normed_ref[...], inv_ref[...] = h_out, normed, inv_std


def attn_forward(x, kv, lens, attn_full, bias_rows, mats, slots, causal):
    d_model = x.shape[-1]
    n_batch = lens.shape[0]
    n_q, n_k = x.shape[0] // n_batch, kv.shape[0] // n_batch
    n_groups = d_model // GROUP
    col = lambda mat: pl.BlockSpec((d_model, GROUP), lambda b, g: (mat, g))
    q_blk = pl.BlockSpec((n_q, GROUP), lambda b, g: (b, g))
    k_blk = pl.BlockSpec((n_k, GROUP), lambda b, g: (b, g))
    tok = lambda n: pl.BlockSpec((n, d_model), lambda b, g: (b, 0))
    n_heads_g = GROUP // HEAD_DIM
    out_shape = (
        jax.ShapeDtypeStruct(x.shape, BF16), jax.ShapeDtypeStruct(kv.shape, BF16), jax.ShapeDtypeStruct(kv.shape, BF16),
        jax.ShapeDtypeStruct(x.shape, BF16), jax.ShapeDtypeStruct((n_batch, n_groups, n_heads_g, n_q), F32),
        jax.ShapeDtypeStruct(x.shape, BF16), jax.ShapeDtypeStruct(x.shape, F32), jax.ShapeDtypeStruct((x.shape[0], 1), F32))
    return pl.pallas_call(
        functools.partial(attn_fwd_kernel, causal, slots + (mats[3],)),
        grid=(n_batch, n_groups),
        in_specs=[pl.BlockSpec(memory_space=pltpu.SMEM), tok(n_q), tok(n_k), col(mats[0]), col(mats[1]), col(mats[2]), pl.BlockSpec(memory_space=pl.ANY),
                  pl.BlockSpec((bias_rows.shape[0], GROUP), lambda b, g: (0, g)), pl.BlockSpec(bias_rows.shape, lambda b, g: (0, 0))],
        out_specs=[q_blk, k_blk, k_blk, q_blk, pl.BlockSpec((1, 1, n_heads_g, n_q), lambda b, g: (b, g, 0, 0)),
                   tok(n_q), tok(n_q), pl.BlockSpec((n_q, 1), lambda b, g: (b, 0))],
        out_shape=out_shape,
        scratch_shapes=[pltpu.VMEM((n_q, d_model), BF16), pltpu.VMEM((d_model, d_model), BF16), pltpu.SemaphoreType.DMA],
        compiler_params=pltpu.CompilerParams(vmem_limit_bytes=VMEM_BYTES, dimension_semantics=('arbitrary', 'arbitrary')),
        cost_estimate=pl.CostEstimate(flops=2 * d_model * d_model * (2 * x.shape[0] + 2 * kv.shape[0]) + 16 * x.shape[0] * n_k * d_model, bytes_accessed=20 * x.shape[0] * d_model, transcendentals=0),
        name='attn_fwd',
    )(lens, x, kv, attn_full, attn_full, attn_full, attn_full, bias_rows, bias_rows)


def attn_bwd_kernel(causal, gain_row, mats, lens_ref, dres_ref, wo_ref, w_all, q_ref, k_ref, v_ref, lse_ref,
                    rows_ref, normed_ref, inv_ref, dq_ref, dk_ref, dv_ref, dx_ref, dkv_ref, sums_ref, tail_ref, d_all, dk_all, dv_all, w_v, load_sem):
    sample, group = pl.program_id(0), pl.program_id(1)
    d_model = w_v.shape[1]
    fetches = [pltpu.make_async_copy(w_all.at[pl.ds(mat * d_model, d_model), :], w_v.at[i], load_sem.at[i]) for i, mat in enumerate(mats[:3])]

    @pl.when((sample == 0) & (group == 0))
    def _():
        for fetch in fetches:
            fetch.start()

    d_o = dot_nt(dres_ref[...].astype(BF16), wo_ref[...]).astype(BF16)
    dq, dk, dv = attend_group_bwd(d_o, q_ref[...], k_ref[...], v_ref[...], lens_ref[sample], causal, lse_ref)
    sums_ref[0, 0:1, :] = col_sum(dq)
    sums_ref[0, 1:2, :] = col_sum(dk)
    sums_ref[0, 2:3, :] = col_sum(dv)
    cols = pl.ds(pl.multiple_of(group * GROUP, GROUP), GROUP)
    for full, out, value in ((d_all, dq_ref, dq), (dk_all, dk_ref, dk), (dv_all, dv_ref, dv)):
        rounded = value.astype(BF16)
        out[...] = rounded
        full[:, cols] = rounded

    @pl.when((sample == 0) & (group == pl.num_programs(1) - 1))
    def _():
        for fetch in fetches:
            fetch.wait()

    @pl.when(group == pl.num_programs(1) - 1)
    def _():
        d_kv = dot_nt(dk_all[...], w_v[1]) + dot_nt(dv_all[...], w_v[2])
        d_h = dres_ref[...] + dot_nt(d_all[...], w_v[0])
        if causal:
            dx_ref[...] = (d_h + d_kv).astype(BF16)
            tail_ref[...] = jnp.zeros_like(tail_ref)
        else:
            dkv_ref[...] = d_kv.astype(BF16)
            normed = normed_ref[...]
            d_resid = norm_rows_bwd(d_h, normed, inv_ref[...], rows_ref[gain_row:gain_row + 1, :])
            dx_ref[...] = d_resid
            tail_ref[0, 0:1, :] = col_sum(d_resid)
            tail_ref[0, 1:2, :] = col_sum(d_h * normed)
            tail_ref[0, 2:3, :] = col_sum(d_h)


def attn_backward(dres, q, k, v, lse, lens, attn_full, bias_rows, mats, causal, gain_row=0, normed=None, inv_std=None):
    d_model = q.shape[-1]
    n_batch = lens.shape[0]
    n_q, n_k = q.shape[0] // n_batch, k.shape[0] // n_batch
    n_groups = d_model // GROUP
    row = lambda mat: pl.BlockSpec((GROUP, d_model), lambda b, g: (mat * n_groups + g, 0))
    q_blk = pl.BlockSpec((n_q, GROUP), lambda b, g: (b, g))
    k_blk = pl.BlockSpec((n_k, GROUP), lambda b, g: (b, g))
    tok = lambda n: pl.BlockSpec((n, d_model), lambda b, g: (b, 0))
    n_heads_g = GROUP // HEAD_DIM
    whole_rows = pl.BlockSpec(bias_rows.shape, lambda b, g: (0, 0))
    kernel = functools.partial(attn_bwd_kernel, causal, gain_row, mats)
    in_specs = [pl.BlockSpec(memory_space=pltpu.SMEM), tok(n_q), row(mats[3]), pl.BlockSpec(memory_space=pl.ANY), q_blk, k_blk, k_blk,
                pl.BlockSpec((1, 1, n_heads_g, n_q), lambda b, g: (b, g, 0, 0)), whole_rows]
    args = [lens, dres, attn_full, attn_full, q, k, v, lse, bias_rows]
    sums_blk = pl.BlockSpec((1, 8, GROUP), lambda b, g: (b, 0, g))
    tail_blk = pl.BlockSpec((1, 8, d_model), lambda b, g: (b, 0, 0))
    tail_shape = jax.ShapeDtypeStruct((n_batch, 8, d_model), F32)
    out_shape = [jax.ShapeDtypeStruct(q.shape, BF16), jax.ShapeDtypeStruct(k.shape, BF16), jax.ShapeDtypeStruct(k.shape, BF16),
                 jax.ShapeDtypeStruct(q.shape, BF16 if causal else F32)]
    out_specs = [q_blk, k_blk, k_blk, tok(n_q)]
    scratch = [pltpu.VMEM((n_q, d_model), BF16), pltpu.VMEM((n_k, d_model), BF16), pltpu.VMEM((n_k, d_model), BF16),
               pltpu.VMEM((3, d_model, d_model), BF16), pltpu.SemaphoreType.DMA((3,))]
    n_in = len(args)
    if causal:
        def body(*refs):
            ins, (dq, dk, dv, dx, sums, tail), rest = refs[:n_in], refs[n_in:n_in + 6], refs[n_in + 6:]
            kernel(*ins, None, None, dq, dk, dv, dx, None, sums, tail, *rest)
    else:
        in_specs += [tok(n_q), pl.BlockSpec((n_q, 1), lambda b, g: (b, 0))]
        args += [normed, inv_std]
        out_shape.append(jax.ShapeDtypeStruct(k.shape, BF16))
        out_specs.append(tok(n_k))
        body = kernel
    out_shape += [tail_shape, tail_shape]
    out_specs += [sums_blk, tail_blk]
    return pl.pallas_call(
        body, grid=(n_batch, n_groups), in_specs=in_specs, out_specs=out_specs, out_shape=out_shape, scratch_shapes=scratch,
        compiler_params=pltpu.CompilerParams(vmem_limit_bytes=VMEM_BYTES, dimension_semantics=('arbitrary', 'arbitrary')),
        cost_estimate=pl.CostEstimate(flops=2 * d_model * d_model * (2 * q.shape[0] + 2 * k.shape[0]) + 40 * q.shape[0] * n_k * d_model, bytes_accessed=20 * q.shape[0] * d_model, transcendentals=0),
        name='attn_bwd',
    )(*args)


def ffn_kernel(n_blocks, h_ref, dy_ref, up_ref, down_ref, rows_ref, bias_ref, normed_ref, inv_ref,
               y_ref, grad_ref, dres2_ref, tail_ref, upsum_ref, gelu_all, dup_all, dres3_all, h_all):
    step = pl.program_id(0)
    block, d_model = h_ref.shape
    n_square = gelu_all.shape[1] // d_model

    @pl.when(step < n_blocks)
    def _():
        rows = pl.ds(pl.multiple_of(step * block, block), block)
        h_b = h_ref[...]
        h_all[rows, :] = h_b
        up = dot_nt(h_b, up_ref[...]) + bias_ref[...]
        cdf = 0.5 * (1.0 + lax.erf(up * 0.7071067811865476))
        gelu = (up * cdf).astype(BF16)
        slope = cdf + up * (0.3989422804014327 * jnp.exp(-0.5 * up * up))
        gelu_all[rows, :] = gelu
        resid = h_b.astype(F32) + dot(gelu, down_ref[...]) + rows_ref[8:9, :]
        y_b, normed3, inv3 = norm_rows(resid, rows_ref[13:14, :], rows_ref[14:15, :])
        y_ref[...] = y_b
        dy = dy_ref[...].astype(F32)
        d_res3 = norm_rows_bwd(dy, normed3, inv3, rows_ref[13:14, :])
        d_res3_b = d_res3.astype(BF16)
        dres3_all[rows, :] = d_res3_b
        d_up = dot_nt(d_res3_b, down_ref[...]) * slope
        d_up_b = d_up.astype(BF16)
        dup_all[rows, :] = d_up_b
        d_h2 = d_res3 + dot(d_up_b, up_ref[...])
        normed2 = normed_ref[...]
        d_res2 = norm_rows_bwd(d_h2, normed2, inv_ref[...], rows_ref[11:12, :])
        dres2_ref[...] = d_res2
        tail = jnp.concatenate([col_sum(d_res2), col_sum(d_res3), col_sum(d_h2 * normed2), col_sum(d_h2), col_sum(dy * normed3), col_sum(dy),
                                jnp.zeros((2, dy.shape[1]), F32)], axis=0)
        up_sum = col_sum(d_up)

        @pl.when(step == 0)
        def _():
            tail_ref[...] = tail
            upsum_ref[...] = up_sum

        @pl.when(step > 0)
        def _():
            tail_ref[...] += tail
            upsum_ref[...] += up_sum

    square = step - n_blocks
    cols = pl.ds(pl.multiple_of(lax.rem(square + 2 * n_square, n_square) * d_model, d_model), d_model)

    @pl.when((square >= 0) & (square < n_square))
    def _():
        grad_ref[...] = dot_tn(dup_all[:, cols], h_all[...])

    @pl.when(square >= n_square)
    def _():
        grad_ref[...] = dot_tn(gelu_all[:, cols], dres3_all[...])


def ffn_both(h2, dy, ffn_full, bias_rows, up_bias, normed2, inv2, block=256):
    n_tok, d_model = h2.shape
    ffn_dim = ffn_full.shape[0] // 2
    n_blocks = n_tok // block
    n_steps = n_blocks + ffn_full.shape[0] // d_model
    at = lambda i: jnp.minimum(i, n_blocks - 1)
    tok = pl.BlockSpec((block, d_model), lambda i: (at(i), 0))
    once = lambda shape, idx: pl.BlockSpec(shape, lambda i: idx, pipeline_mode=pl.Buffered(1))
    return pl.pallas_call(
        functools.partial(ffn_kernel, n_blocks), grid=(n_steps,),
        in_specs=[tok, tok, once((ffn_dim, d_model), (0, 0)), once((ffn_dim, d_model), (1, 0)), once(bias_rows.shape, (0, 0)), once((1, ffn_dim), (0, 0)),
                  tok, pl.BlockSpec((block, 1), lambda i: (at(i), 0))],
        out_specs=[tok, pl.BlockSpec((d_model, d_model), lambda i: (jnp.maximum(i - n_blocks, 0), 0)), tok, pl.BlockSpec((8, d_model), lambda i: (0, 0)), pl.BlockSpec((1, ffn_dim), lambda i: (0, 0))],
        out_shape=[jax.ShapeDtypeStruct(h2.shape, BF16), jax.ShapeDtypeStruct(ffn_full.shape, F32), jax.ShapeDtypeStruct(h2.shape, F32),
                   jax.ShapeDtypeStruct((8, d_model), F32), jax.ShapeDtypeStruct((1, ffn_dim), F32)],
        scratch_shapes=[pltpu.VMEM((n_tok, ffn_dim), BF16), pltpu.VMEM((n_tok, ffn_dim), BF16), pltpu.VMEM((n_tok, d_model), BF16), pltpu.VMEM((n_tok, d_model), BF16)],
        compiler_params=pltpu.CompilerParams(vmem_limit_bytes=VMEM_BYTES, dimension_semantics=('arbitrary',)),
        cost_estimate=pl.CostEstimate(flops=12 * n_tok * d_model * ffn_dim, bytes_accessed=30 * n_tok * d_model, transcendentals=0),
        name='ffn_both',
    )(h2, dy, ffn_full, ffn_full, bias_rows, up_bias, normed2, inv2)


def layer_acts(dec_in, enc_out, src_lens, tgt_lens, y_cot, attn_full, ffn_full, vec_full):
    n_batch, n_tgt, d_model = dec_in.shape
    x = dec_in.reshape(-1, d_model)
    enc = enc_out.reshape(-1, d_model)
    dy = y_cot.reshape(-1, d_model)
    vec_f = vec_full.astype(F32)
    bias_rows = jnp.pad(vec_f[:15 * d_model].reshape(15, d_model), ((0, 1), (0, 0)))
    up_bias = vec_f[15 * d_model:].reshape(1, -1)
    q1, k1, v1, o1, lse1, h1, normed1, inv1 = attn_forward(x, x, tgt_lens, attn_full, bias_rows, (0, 1, 2, 3), (0, 1, 2, 3, 9), True)
    q2, k2, v2, o2, lse2, h2, normed2, inv2 = attn_forward(h1, enc, src_lens, attn_full, bias_rows, (4, 5, 6, 7), (4, 5, 6, 7, 11), False)
    y, g_ffn, d_res2, ffn_tail, up_sum = ffn_both(h2, dy, ffn_full, bias_rows, up_bias, normed2, inv2)
    dq2, dk2, dv2, d_res1, d_enc, sums2, tail2 = attn_backward(d_res2, q2, k2, v2, lse2, src_lens, attn_full, bias_rows, (4, 5, 6, 7), False, 9, normed1, inv1)
    dq1, dk1, dv1, d_x, sums1, _ = attn_backward(d_res1, q1, k1, v1, lse1, tgt_lens, attn_full, bias_rows, (0, 1, 2, 3), True)
    s1, s2, t2 = jnp.sum(sums1, axis=0), jnp.sum(sums2, axis=0), jnp.sum(tail2, axis=0)
    g_vec = jnp.concatenate([s1[0:3].reshape(-1), t2[0], s2[0:3].reshape(-1), ffn_tail[0], ffn_tail[1], t2[1], t2[2], ffn_tail[2], ffn_tail[3], ffn_tail[4], ffn_tail[5], up_sum[0]])
    pairs = ((x, dq1), (x, dk1), (x, dv1), (o1, d_res1.astype(BF16)), (h1, dq2), (enc, dk2), (enc, dv2), (o2, d_res2.astype(BF16)))
    return y.reshape(dec_in.shape), d_x.reshape(dec_in.shape), d_enc.reshape(enc_out.shape), pairs, g_ffn, g_vec
SIDE = 4
LANES = 128
COLOURS = 3
DIM_ORDER = ((2, 1, 0), (1, 0, 2), (0, 2, 1))
MESH_ID = pl.DeviceIdType.MESH


def torus_place():
    chip = lax.axis_index('fsdp')
    return (chip // (SIDE * SIDE), (chip // SIDE) % SIDE, chip % SIDE)


def chip_at(place, dim, shift):
    moved = [lax.rem(p + shift + SIDE, SIDE) if d == dim else p for d, p in enumerate(place)]
    return (moved[0] * SIDE + moved[1]) * SIDE + moved[2]


def meet_neighbours(place):
    barrier = pltpu.get_barrier_semaphore()
    core = lax.axis_index('dp')
    for dim in range(3):
        for shift in (1, -1):
            pl.semaphore_signal(barrier, inc=1, device_id=(core, chip_at(place, dim, shift)), device_id_type=MESH_ID)
    pl.semaphore_signal(barrier, inc=1, device_id=(1 - core, lax.axis_index('fsdp')), device_id_type=MESH_ID)
    pl.semaphore_wait(barrier, 7)


class Counter:
    def __init__(self):
        self.used = 0

    def take(self):
        self.used += 1
        return self.used - 1


def rs_kernel(scale, rows, vec_rows, gffn_ref, gattn_ref, gvec_ref, offn_ref, oattn_ref, ovec_ref,
              acc0, acc1, g10, g11, d10, d11, g20, g21, d20, d21, g30, g31, d30, d31, stage, send_sem, recv_sem, load_sem):
    core = lax.axis_index('dp')
    chip = lax.axis_index('fsdp')
    place = torus_place()
    acc = (acc0, acc1)
    got = ((g10, g20, g30), (g11, g21, g31))
    far = ((d10, d20, d30), (d11, d21, d31))
    height = (rows, rows + vec_rows)
    counter = Counter()
    started = []

    def remote(src, dst, device):
        i = counter.take()
        return pltpu.make_async_remote_copy(src_ref=src, dst_ref=dst, send_sem=send_sem.at[i], recv_sem=recv_sem.at[i], device_id=device, device_id_type=MESH_ID)

    def start(copy):
        copy.start()
        started.append(copy)

    sibling = (1 - core, chip)

    def columns(of_core, colour):
        return pl.ds(pl.multiple_of((of_core * COLOURS + colour) * LANES, LANES), LANES)

    def slot(colour, d):
        dim = DIM_ORDER[colour][0]
        where = [slice(None)] * 3
        where[dim] = lax.rem(place[dim] + d, SIDE)
        return tuple(where)

    pieces = [(q, d, colour) for q in range(2) for d in (2, 1, 3, 0) for colour in range(COLOURS)]
    sources = (gffn_ref, gattn_ref)

    def swap_copies(q, d, colour):
        where = slot(colour, d)
        cols = columns(1 - core, colour)
        copies = [remote(sources[q].at[where + (slice(None), cols)], acc[q].at[(colour,) + where + (pl.ds(0, rows), slice(None))], sibling)]
        if q == 1:
            copies.append(remote(gvec_ref.at[where + (slice(None), cols)], acc[q].at[(colour,) + where + (pl.ds(rows, vec_rows), slice(None))], sibling))
        return copies

    swaps = [swap_copies(*piece) for piece in pieces]

    def load_copies(i):
        q, d, colour = pieces[i]
        where = slot(colour, d)
        cols = columns(core, colour)
        buf = i % 3
        copies = [pltpu.make_async_copy(sources[q].at[where + (slice(None), cols)], stage.at[buf, :, :, pl.ds(0, rows), :], load_sem.at[buf, 0])]
        if q == 1:
            copies.append(pltpu.make_async_copy(gvec_ref.at[where + (slice(None), cols)], stage.at[buf, :, :, pl.ds(rows, vec_rows), :], load_sem.at[buf, 1]))
        return copies

    def ring_copies(q, colour, phase):
        order = DIM_ORDER[colour]
        dim = order[phase]
        rest = sorted(order[phase + 1:])
        n_low = rows // 2

        def block(d, half=None):
            where = [None, None, None]
            for done in order[:phase]:
                where[done] = place[done]
            where[dim] = lax.rem(place[dim] + d, SIDE)
            for i, r in enumerate(rest):
                where[r] = slice(None) if half is None or i > 0 else pl.ds(2 * half, 2)
            tail = (slice(None), slice(None))
            if phase == 2 and half is not None:
                tail = (pl.ds(0, n_low) if half == 0 else pl.ds(n_low, height[q] - n_low), slice(None))
            return acc[q].at[(colour,) + tuple(where) + tail]

        def half_of(ref, direction, half):
            if phase == 2:
                return ref.at[colour, direction, pl.ds(0, n_low) if half == 0 else pl.ds(n_low, height[q] - n_low), :]
            return ref.at[colour, direction, pl.ds(2 * half, 2)]

        def far_of(direction, half):
            if phase == 2:
                return far[q][phase].at[colour, direction, pl.ds(0, n_low if half == 0 else height[q] - n_low), :]
            return far[q][phase].at[colour, direction]

        out = []
        for direction, shift in enumerate((1, -1)):
            device = (core, chip_at(place, dim, shift))
            near = shift % SIDE
            out.append(dict(
                far=remote(block(2, direction), far_of(direction, direction), device),
                own=remote(block(near, 1 - direction), half_of(got[q][phase], direction, 1 - direction), device),
                fed=remote(block(near, direction), half_of(got[q][phase], direction, direction), device),
                fed_view=block(near, direction), far_view=far_of(direction, direction)))
        return out, block(0), [got[q][phase].at[colour, direction] for direction in range(2)]

    rings = {(q, colour, phase): ring_copies(q, colour, phase) for q in range(2) for colour in range(COLOURS) for phase in range(3)}

    def add_into(dst, sources, n_lead):
        def body(i, _):
            idx = {0: (), 1: (i,), 2: (i // SIDE, i % SIDE)}[n_lead]
            total = dst[idx]
            for src in sources:
                total = total + src[idx]
            dst[idx] = total
            return 0

        count = 1
        for n in dst.shape[:n_lead]:
            count *= n
        if n_lead == 0:
            total = dst[...]
            for src in sources:
                total = total + src[...]
            dst[...] = total
        else:
            lax.fori_loop(0, count, body, 0)

    def absorb(i):
        q, d, colour = pieces[i]
        for copy in load_copies(i):
            copy.wait()
        for copy in swaps[i]:
            copy.wait_recv()
        n = height[q]
        add_into(acc[q].at[(colour,) + slot(colour, d)], [stage.at[i % 3, :, :, pl.ds(0, n), :]], 2)
        if i + 3 < len(pieces):
            for copy in load_copies(i + 3):
                copy.start()
        first = rings[(q, colour, 0)][0]
        if d == 2:
            start(first[0]['far'])
            start(first[1]['far'])
        elif d == 1:
            start(first[0]['own'])
        elif d == 3:
            start(first[1]['own'])

    def send_first(q, colour, phase):
        dirs = rings[(q, colour, phase)][0]
        for direction in dirs:
            start(direction['far'])
        for direction in dirs:
            start(direction['own'])

    def relay(q, colour, phase):
        dirs = rings[(q, colour, phase)][0]
        for direction in dirs:
            direction['far'].wait_recv()
            add_into(direction['fed_view'], [direction['far_view']], 2 - phase)
        for direction in dirs:
            start(direction['fed'])

    def settle(q, colour, phase):
        dirs, mine, arrived = rings[(q, colour, phase)]
        for direction in dirs:
            direction['own'].wait_recv()
            direction['fed'].wait_recv()
        add_into(mine, arrived, 2 - phase)
        if phase < 2:
            send_first(q, colour, phase + 1)

    outs = (offn_ref, oattn_ref)
    local, finals = [], []

    def finish(q, colour):
        done = acc[q].at[colour, place[0], place[1], place[2]]
        done[...] = done[...] * scale
        cols = columns(core, colour)
        parts = [(done.at[pl.ds(0, rows), :], outs[q].at[:, cols])]
        if q == 1:
            parts.append((done.at[pl.ds(rows, vec_rows), :], ovec_ref.at[:, cols]))
        for src, dst in parts:
            i = counter.take()
            keep = pltpu.make_async_copy(src, dst, load_sem.at[3 + len(local) // 2, len(local) % 2])
            keep.start()
            local.append(keep)
            give = pltpu.make_async_remote_copy(src_ref=src, dst_ref=dst, send_sem=send_sem.at[i], recv_sem=recv_sem.at[i], device_id=sibling, device_id_type=MESH_ID)
            start(give)
            finals.append(give)

    colours = range(COLOURS)
    meet_neighbours(place)
    for i in range(3):
        for copy in load_copies(i):
            copy.start()
    for group in swaps:
        for copy in group:
            start(copy)
    per_chunk = len(pieces) // 2
    for i in range(9):
        absorb(i)
    for colour in colours:
        relay(0, colour, 0)
    for i in range(9, per_chunk + 9):
        absorb(i)
    for colour in colours:
        settle(0, colour, 0)
    for colour in colours:
        relay(1, colour, 0)
    for i in range(per_chunk + 9, 2 * per_chunk):
        absorb(i)
    for colour in colours:
        relay(0, colour, 1)
    for colour in colours:
        settle(1, colour, 0)
    for colour in colours:
        settle(0, colour, 1)
    for colour in colours:
        relay(1, colour, 1)
    for colour in colours:
        relay(0, colour, 2)
    for colour in colours:
        settle(1, colour, 1)
    for colour in colours:
        settle(0, colour, 2)
        finish(0, colour)
    for colour in colours:
        relay(1, colour, 2)
    for colour in colours:
        settle(1, colour, 2)
        finish(1, colour)
    for copy in finals:
        copy.wait_recv()
    for copy in started:
        copy.wait_send()
    for copy in local:
        copy.wait()


def scatter_grads(g_ffn, g_attn, g_vec, scale):
    n_chips = SIDE ** 3
    width = 2 * COLOURS * LANES
    rows, vec_rows = g_ffn.shape[0] // n_chips, g_vec.shape[0] // n_chips
    as_torus = lambda g: g.reshape(SIDE, SIDE, SIDE, g.shape[0] // n_chips, width)
    heights = (rows, rows + vec_rows)
    n_low = rows // 2
    buf = lambda shape: [pltpu.VMEM((COLOURS,) + shape(h) + (LANES,), F32) for h in heights]
    n_copies = 2 * COLOURS * 3 * 2 * 3 + 2 * COLOURS * 4 + COLOURS * 4 + 9
    scratch = (buf(lambda h: (SIDE, SIDE, SIDE, h)) + buf(lambda h: (2, SIDE, SIDE, h)) + buf(lambda h: (2, 2, SIDE, h))
               + buf(lambda h: (2, SIDE, h)) + buf(lambda h: (2, 2, h)) + buf(lambda h: (2, h)) + buf(lambda h: (2, max(n_low, h - n_low)))
               + [pltpu.VMEM((3, SIDE, SIDE, heights[1], LANES), F32), pltpu.SemaphoreType.DMA((n_copies,)), pltpu.SemaphoreType.DMA((n_copies,)), pltpu.SemaphoreType.DMA((8, 2))])
    anywhere = pl.BlockSpec(memory_space=pl.ANY)
    sent = 4 * width * n_chips * (2 * rows + vec_rows)
    return pl.pallas_call(
        functools.partial(rs_kernel, scale, rows, vec_rows),
        in_specs=[anywhere] * 3, out_specs=[anywhere] * 3,
        out_shape=[jax.ShapeDtypeStruct((rows, width), F32), jax.ShapeDtypeStruct((rows, width), F32), jax.ShapeDtypeStruct((vec_rows, width), F32)],
        scratch_shapes=scratch,
        compiler_params=pltpu.CompilerParams(collective_id=1, has_side_effects=True, vmem_limit_bytes=62 * 1024 * 1024),
        cost_estimate=pl.CostEstimate(flops=10 ** 9, bytes_accessed=2 * sent, transcendentals=0),
        name='scatter_grads',
    )(as_torus(g_ffn), as_torus(g_attn), as_torus(g_vec))


def ag_kernel(attn_ref, ffn_ref, vec_ref, oattn_ref, offn_ref, vec_out, attn_v, ffn_v, send_sem, recv_sem, load_sem):
    core = lax.axis_index('dp')
    chip = lax.axis_index('fsdp')
    place = torus_place()
    sibling = (1 - core, chip)
    owns = (attn_ref, ffn_ref, vec_ref)
    bufs = (attn_v, ffn_v, vec_out)
    outs = (oattn_ref, offn_ref)
    rows, width = attn_ref.shape
    band = rows // (2 * COLOURS)
    vec_high = vec_ref.shape[0]
    counter, loads = Counter(), Counter()
    started, stores = [], []
    streams = [(w, colour) for w in range(2) for colour in range(COLOURS)] + [(2, 1)]

    def remote(src, dst, device):
        i = counter.take()
        return pltpu.make_async_remote_copy(src_ref=src, dst_ref=dst, send_sem=send_sem.at[i], recv_sem=recv_sem.at[i], device_id=device, device_id_type=MESH_ID)

    def start(copy):
        copy.start()
        started.append(copy)

    def band_rows(colour):
        return pl.ds(pl.multiple_of((core * COLOURS + colour) * band, band), band)

    def tail_of(w, colour, half=None):
        if w == 2:
            return (slice(None) if half is None else pl.ds(half * (vec_high // 2), vec_high // 2), slice(None))
        return (band_rows(colour), slice(None) if half is None else pl.ds(half * (width // 2), width // 2))

    def ring_copies(w, colour, phase):
        order = DIM_ORDER[colour]
        dim = order[phase]
        have = sorted(order[:phase])

        def index(shift, half=None):
            where = [place[0], place[1], place[2]]
            where[dim] = lax.rem(place[dim] + shift + SIDE, SIDE)
            for i, h in enumerate(have):
                where[h] = slice(None) if half is None or i > 0 else pl.ds(2 * half, 2)
            return tuple(where) + tail_of(w, colour, half if phase == 0 else None)

        out = []
        for direction, shift in enumerate((1, -1)):
            device = (core, chip_at(place, dim, shift))
            mine = owns[w].at[tail_of(w, colour)] if phase == 0 else bufs[w].at[index(0)]
            out.append(dict(
                near=remote(mine, bufs[w].at[index(0)], device),
                far=remote(bufs[w].at[index(-shift, direction)], bufs[w].at[index(-shift, direction)], device),
                near_at=index(-shift), far_at=index(2, direction)))
        return out

    rings = {(w, colour, phase): ring_copies(w, colour, phase) for w, colour in streams for phase in range(3)}

    def plane_at(colour):
        last = DIM_ORDER[colour][2]
        return tuple(place[d] if d == last else slice(None) for d in range(3)) + (band_rows(colour), slice(None))

    def publish(w, at):
        i = counter.take()
        keep = pltpu.make_async_copy(bufs[w].at[at], outs[w].at[at], load_sem.at[loads.take()])
        keep.start()
        stores.append(keep)
        give = pltpu.make_async_remote_copy(src_ref=bufs[w].at[at], dst_ref=outs[w].at[at], send_sem=send_sem.at[i], recv_sem=recv_sem.at[i], device_id=sibling, device_id_type=MESH_ID)
        start(give)
        finals.append(give)

    finals = []

    def send_near(w, phase):
        for sw, colour in streams:
            if sw == w:
                for direction in rings[(w, colour, phase)]:
                    start(direction['near'])

    def pass_on(w, phase):
        for sw, colour in streams:
            if sw == w:
                for direction in rings[(w, colour, phase)]:
                    direction['near'].wait_recv()
                    start(direction['far'])
        if phase == 2 and w < 2:
            for sw, colour in streams:
                if sw == w:
                    for direction in rings[(w, colour, phase)]:
                        publish(w, direction['near_at'])

    def complete(w, phase):
        for sw, colour in streams:
            if sw == w:
                for direction in rings[(w, colour, phase)]:
                    direction['far'].wait_recv()
                if phase == 2 and w < 2:
                    for direction in rings[(w, colour, phase)]:
                        publish(w, direction['far_at'])
        if phase < 2:
            send_near(w, phase + 1)
        if phase == 1 and w < 2:
            for colour in range(COLOURS):
                publish(w, plane_at(colour))

    for w, colour in streams:
        bufs[w][(place[0], place[1], place[2]) + tail_of(w, colour)] = owns[w][tail_of(w, colour)]
    meet_neighbours(place)
    for w in (0, 2, 1):
        send_near(w, 0)
    for phase in range(3):
        for w in (0, 2, 1):
            pass_on(w, phase)
        for w in (0, 2, 1):
            complete(w, phase)
    for copy in finals:
        copy.wait_recv()
    for copy in started:
        copy.wait_send()
    for copy in stores:
        copy.wait()


def gather_params(attn_w, ffn_w, vec_rows):
    rows, width = attn_w.shape
    full = (SIDE, SIDE, SIDE, rows, width)
    n_copies = 3 * 4 * 7 + 2 * COLOURS * 5
    vmem = pl.BlockSpec(memory_space=pltpu.VMEM)
    anywhere = pl.BlockSpec(memory_space=pl.ANY)
    attn_full, ffn_full, vec_full = pl.pallas_call(
        ag_kernel,
        in_specs=[vmem] * 3, out_specs=[anywhere, anywhere, vmem],
        out_shape=[jax.ShapeDtypeStruct(full, BF16), jax.ShapeDtypeStruct(full, BF16), jax.ShapeDtypeStruct((SIDE, SIDE, SIDE) + vec_rows.shape, F32)],
        scratch_shapes=[pltpu.VMEM(full, BF16), pltpu.VMEM(full, BF16), pltpu.SemaphoreType.DMA((n_copies,)), pltpu.SemaphoreType.DMA((n_copies,)),
                        pltpu.SemaphoreType.DMA((2 * COLOURS * 5,))],
        compiler_params=pltpu.CompilerParams(collective_id=2, has_side_effects=True, vmem_limit_bytes=VMEM_BYTES),
        cost_estimate=pl.CostEstimate(flops=10 ** 9, bytes_accessed=4 * rows * width * SIDE ** 3, transcendentals=0),
        name='gather_params',
    )(attn_w, ffn_w, vec_rows)
    return attn_full.reshape(-1, width), ffn_full.reshape(-1, width), vec_full


def square_grads(pairs, d_model):
    blocks = [dot_tn(lhs[:, i:i + d_model], rhs) for lhs, rhs in pairs for i in range(0, lhs.shape[1], d_model)]
    return jnp.concatenate(blocks, axis=0)


def solution(mesh):
    n_fsdp = mesh.shape['fsdp']
    n_dp = mesh.shape['dp']
    batch_axes = ('dp', 'fsdp')
    act_spec = P(batch_axes, None, None)
    len_spec = P(batch_axes)
    row_spec = P('fsdp', None)
    vec_spec = P('fsdp')

    def device_step(dec_in, enc_out, src_lens, tgt_lens, y_cot, attn_w, ffn_w, vec_params):
        d_model, n_vec = dec_in.shape[2], vec_params.shape[0]
        vec_rows = jnp.pad(vec_params.astype(F32), (0, 16 * LANES - n_vec)).reshape(16, LANES)
        attn_full, ffn_full, vec_tiles = gather_params(attn_w, ffn_w, vec_rows)
        vec_full = vec_tiles.reshape(n_fsdp, 16, LANES)[:, :2].reshape(n_fsdp, 2 * LANES)[:, :n_vec].reshape(-1)
        y_out, dec_grad, enc_grad, pairs, g_ffn, g_vec = layer_acts(dec_in, enc_out, src_lens, tgt_lens, y_cot, attn_full, ffn_full, vec_full)
        grad_scale = 1.0 / (dec_in.shape[0] * dec_in.shape[1] * n_fsdp * n_dp)
        g_rows = jnp.pad(g_vec.reshape(n_fsdp, 1, n_vec), ((0, 0), (0, 7), (0, d_model - n_vec))).reshape(n_fsdp * 8, -1)
        ffn_out, attn_out, vec_out = scatter_grads(g_ffn, square_grads(pairs, d_model), g_rows, grad_scale)
        return y_out, dec_grad, enc_grad, attn_out, ffn_out, vec_out[0, :n_vec]

    return jax.shard_map(device_step, mesh=mesh, in_specs=(act_spec, act_spec, len_spec, len_spec, act_spec, row_spec, row_spec, vec_spec), out_specs=(act_spec, act_spec, act_spec, row_spec, row_spec, vec_spec), check_vma=False)
```

```python
import functools
import jax
import jax.numpy as jnp
from jax import lax
from jax.experimental import pallas as pl
from jax.experimental.pallas import tpu as pltpu
from jax.sharding import PartitionSpec as P

ZERO, ONE, TWO, THREE = range(4)
ALL = ...
HEAD_DIM = 64
LN_EPS = 1e-5
MASK_FILL = -1e30
VMEM_BYTES = 60 * 1024 * 1024
F32 = jnp.float32
BF16 = jnp.bfloat16
GROUP = 256
PAIR = 128


SIDE = 4
LANES = 128
COLOURS = THREE
DIM_ORDER = ((TWO, ONE, ZERO), (ONE, ZERO, TWO), (ZERO, TWO, ONE))
MESH_ID = pl.DeviceIdType.MESH


def torus_place():
    chip = lax.axis_index('fsdp')
    return (chip // (SIDE * SIDE), lax.rem(chip // SIDE, SIDE), lax.rem(chip, SIDE))


def chip_at(place, dim, shift):
    moved = [lax.rem(p + shift + SIDE, SIDE) if d == dim else p for d, p in enumerate(place)]
    return (moved[ZERO] * SIDE + moved[ONE]) * SIDE + moved[TWO]


def meet_neighbours(place):
    barrier = pltpu.get_barrier_semaphore()
    core = lax.axis_index('dp')
    for dim in range(THREE):
        for shift in (ONE, -ONE):
            pl.semaphore_signal(barrier, inc=ONE, device_id=(core, chip_at(place, dim, shift)), device_id_type=MESH_ID)
    pl.semaphore_signal(barrier, inc=ONE, device_id=(ONE - core, lax.axis_index('fsdp')), device_id_type=MESH_ID)
    pl.semaphore_wait(barrier, 7)


class Scatter:
    def __init__(self, scale, sources, outs, scratch, resident=False):
        self.scale, self.outs, self.resident = scale, outs, resident
        self.sources = [(ref, pl.ds(first, n)) for ref, first, n in sources]
        (self.acc, g1, d1, g2, d2, g3, d3, self.send_sem, self.recv_sem, self.load_sem, *stage) = scratch
        self.stage = None if resident else stage[ZERO]
        self.got, self.far = (g1, g2, g3), (d1, d2, d3)
        self.heights = [n for _, _, n in sources]
        self.offsets = [sum(self.heights[:i]) for i in range(len(sources))]
        self.height = sum(self.heights)
        self.n_low = self.heights[ZERO] // TWO
        self.core, self.chip, self.place = lax.axis_index('dp'), lax.axis_index('fsdp'), torus_place()
        self.pieces = [(d, colour) for d in (TWO, ONE, THREE, ZERO) for colour in range(COLOURS)]

    @staticmethod
    def scratch_shapes(heights, resident=False):
        h = sum(heights)
        n_low = heights[ZERO] // TWO
        buf = lambda *shape: pltpu.VMEM((COLOURS,) + shape + (LANES,), F32)
        n = Scatter.n_copies(len(heights))
        return [buf(SIDE, SIDE, SIDE, h), buf(TWO, SIDE, SIDE, h), buf(TWO, TWO, SIDE, h), buf(TWO, SIDE, h), buf(TWO, TWO, h), buf(TWO, h), buf(TWO, max(n_low, h - n_low)),
                pltpu.SemaphoreType.DMA((n,)), pltpu.SemaphoreType.DMA((n,)), pltpu.SemaphoreType.DMA((THREE + COLOURS, len(heights)))] + (
                    [] if resident else [pltpu.VMEM((THREE, SIDE, SIDE, h, LANES), F32)])

    @staticmethod
    def n_copies(n_parts):
        return 12 * n_parts + COLOURS * 18 + COLOURS * n_parts

    def remote(self, i, src, dst, device):
        return pltpu.make_async_remote_copy(src_ref=src, dst_ref=dst, send_sem=self.send_sem.at[i], recv_sem=self.recv_sem.at[i], device_id=device, device_id_type=MESH_ID)

    def columns(self, of_core, colour):
        return pl.ds(pl.multiple_of((of_core * COLOURS + colour) * LANES, LANES), LANES)

    def slot(self, d, colour):
        dim = DIM_ORDER[colour][ZERO]
        where = [slice(None)] * THREE
        where[dim] = lax.rem(self.place[dim] + d, SIDE)
        return tuple(where)

    def rows_of(self, part):
        return pl.ds(self.offsets[part], self.heights[part])

    def swaps(self, piece):
        d, colour = self.pieces[piece]
        where, cols = self.slot(d, colour), self.columns(ONE - self.core, colour)
        n = len(self.sources)
        return [self.remote(piece * n + i, src.at[where + (rows, cols)], self.acc.at[(colour,) + where + (self.rows_of(i), slice(None))], (ONE - self.core, self.chip))
                for i, (src, rows) in enumerate(self.sources)]

    def loads(self, piece):
        d, colour = self.pieces[piece]
        where, cols = self.slot(d, colour), self.columns(self.core, colour)
        if self.resident:
            return []
        return [pltpu.make_async_copy(src.at[where + (rows, cols)], self.stage.at[piece % THREE, :, :, self.rows_of(i), :], self.load_sem.at[piece % THREE, i])
                for i, (src, rows) in enumerate(self.sources)]

    def split_rows(self, half):
        return pl.ds(ZERO, self.n_low) if half == ZERO else pl.ds(self.n_low, self.height - self.n_low)

    def block(self, colour, phase, d, half=None):
        order = DIM_ORDER[colour]
        where = [None, None, None]
        for done in order[:phase]:
            where[done] = self.place[done]
        where[order[phase]] = lax.rem(self.place[order[phase]] + d, SIDE)
        for i, rest in enumerate(sorted(order[phase + ONE:])):
            where[rest] = slice(None) if half is None or i > ZERO else pl.ds(TWO * half, TWO)
        rows = self.split_rows(half) if phase == TWO and half is not None else slice(None)
        return self.acc.at[(colour,) + tuple(where) + (rows, slice(None))]

    def got_half(self, colour, phase, direction, half):
        where = self.split_rows(half) if phase == TWO else pl.ds(TWO * half, TWO)
        return self.got[phase].at[colour, direction, where]

    def far_part(self, colour, phase, direction):
        if phase == TWO:
            return self.far[phase].at[colour, direction, pl.ds(ZERO, self.n_low if direction == ZERO else self.height - self.n_low), :]
        return self.far[phase].at[colour, direction]

    def ring(self, colour, phase, direction):
        shift = ONE - TWO * direction
        device = (self.core, chip_at(self.place, DIM_ORDER[colour][phase], shift))
        i = 12 * len(self.sources) + ((colour * THREE + phase) * TWO + direction) * THREE
        near = shift % SIDE
        return (self.remote(i, self.block(colour, phase, TWO, direction), self.far_part(colour, phase, direction), device),
                self.remote(i + ONE, self.block(colour, phase, near, ONE - direction), self.got_half(colour, phase, direction, ONE - direction), device),
                self.remote(i + TWO, self.block(colour, phase, near, direction), self.got_half(colour, phase, direction, direction), device))

    def gives(self, colour):
        n = len(self.sources)
        base = 12 * n + COLOURS * 18 + colour * n
        done = self.acc.at[colour, self.place[ZERO], self.place[ONE], self.place[TWO]]
        cols = self.columns(self.core, colour)
        pairs = [(done.at[self.rows_of(i), :], out.at[:, cols]) for i, out in enumerate(self.outs)]
        return [(self.remote(base + i, src, dst, (ONE - self.core, self.chip)), pltpu.make_async_copy(src, dst, self.load_sem.at[THREE + colour, i])) for i, (src, dst) in enumerate(pairs)]

    def add_into(self, dst, sources, n_lead):
        def body(i, _):
            idx = (i,) if n_lead == ONE else (i // SIDE, lax.rem(i, SIDE))
            total = dst[idx]
            for src in sources:
                total = total + src[idx]
            dst[idx] = total
            return ZERO

        if n_lead == ZERO:
            total = dst[ALL]
            for src in sources:
                total = total + src[ALL]
            dst[ALL] = total
        else:
            count = dst.shape[ZERO] * (dst.shape[ONE] if n_lead == TWO else ONE)
            lax.fori_loop(ZERO, count, body, ZERO)


    def begin(self):
        for piece in range(THREE):
            for copy in self.loads(piece):
                copy.start()
        for piece in range(len(self.pieces)):
            for copy in self.swaps(piece):
                copy.start()

    def absorb(self, turn):
        for piece in range(turn * COLOURS, (turn + ONE) * COLOURS):
            d, colour = self.pieces[piece]
            for copy in self.loads(piece):
                copy.wait()
            for copy in self.swaps(piece):
                copy.wait_recv()
            where = self.slot(d, colour)
            if self.resident:
                for i, (src, rows) in enumerate(self.sources):
                    self.add_into(self.acc.at[(colour,) + where + (self.rows_of(i), slice(None))], [src.at[where + (rows, self.columns(self.core, colour))]], TWO)
            else:
                self.add_into(self.acc.at[(colour,) + where], [self.stage.at[piece % THREE]], TWO)
            if piece + THREE < len(self.pieces):
                for copy in self.loads(piece + THREE):
                    copy.start()
            if turn == ZERO:
                for direction in range(TWO):
                    self.ring(colour, ZERO, direction)[ZERO].start()
            elif turn < THREE:
                self.ring(colour, ZERO, turn - ONE)[ONE].start()

    def relay(self, phase):
        for colour in range(COLOURS):
            for direction in range(TWO):
                far, _, fed = self.ring(colour, phase, direction)
                far.wait_recv()
                self.add_into(self.block(colour, phase, (ONE - TWO * direction) % SIDE, direction), [self.far_part(colour, phase, direction)], TWO - phase)
            for direction in range(TWO):
                self.ring(colour, phase, direction)[TWO].start()

    def settle(self, phase):
        for colour in range(COLOURS):
            for direction in range(TWO):
                _, own, fed = self.ring(colour, phase, direction)
                own.wait_recv()
                fed.wait_recv()
            self.add_into(self.block(colour, phase, ZERO), [self.got[phase].at[colour, direction] for direction in range(TWO)], TWO - phase)
            if phase < TWO:
                for kind in range(TWO):
                    for direction in range(TWO):
                        self.ring(colour, phase + ONE, direction)[kind].start()
            else:
                done = self.acc.at[colour, self.place[ZERO], self.place[ONE], self.place[TWO]]
                done[ALL] = done[ALL] * self.scale
                for give, keep in self.gives(colour):
                    keep.start()
                    give.start()

    def end(self):
        for colour in range(COLOURS):
            for give, keep in self.gives(colour):
                give.wait_recv()
                give.wait_send()
                keep.wait()
        for piece in range(len(self.pieces)):
            for copy in self.swaps(piece):
                copy.wait_send()
        for colour in range(COLOURS):
            for phase in range(THREE):
                for direction in range(TWO):
                    for copy in self.ring(colour, phase, direction):
                        copy.wait_send()


def rs_kernel(scale, *refs):
    scatter = Scatter(scale, [(ref, ZERO, ref.shape[THREE]) for ref in refs[:TWO]], refs[TWO:4], refs[4:], resident=True)
    meet_neighbours(scatter.place)
    scatter.begin()
    for turn in range(THREE):
        scatter.absorb(turn)
    scatter.relay(ZERO)
    scatter.absorb(THREE)
    scatter.settle(ZERO)
    for phase in (ONE, TWO):
        scatter.relay(phase)
        scatter.settle(phase)
    scatter.end()


def as_torus(rows):
    return rows.reshape(SIDE, SIDE, SIDE, rows.shape[ZERO] // SIDE ** THREE, rows.shape[ONE])


def scatter_grads(g_attn, g_vec, scale):
    sources = [as_torus(g_attn), as_torus(g_vec)]
    heights = [src.shape[THREE] for src in sources]
    width = g_attn.shape[ONE]
    anywhere = pl.BlockSpec(memory_space=pl.ANY)
    return pl.pallas_call(
        functools.partial(rs_kernel, scale),
        in_specs=[pl.BlockSpec(memory_space=pltpu.VMEM)] * TWO, out_specs=[anywhere] * TWO,
        out_shape=[jax.ShapeDtypeStruct((h, width), F32) for h in heights],
        scratch_shapes=Scatter.scratch_shapes(heights, resident=True),
        compiler_params=pltpu.CompilerParams(collective_id=ONE, has_side_effects=True, vmem_limit_bytes=32 * 1024 * 1024),
        cost_estimate=pl.CostEstimate(flops=10 ** 9, bytes_accessed=8 * width * g_attn.shape[ZERO], transcendentals=ZERO),
        name='scatter_grads',
    )(*sources)


class Gather:
    def __init__(self, send_sem, recv_sem, base=ZERO):
        self.send_sem, self.recv_sem = send_sem, recv_sem
        self.used = base
        self.core, self.chip, self.place = lax.axis_index('dp'), lax.axis_index('fsdp'), torus_place()
        self.sibling = (ONE - self.core, self.chip)
        self.started = []

    def remote(self, src, dst, device):
        i = self.used
        self.used += ONE
        return pltpu.make_async_remote_copy(src_ref=src, dst_ref=dst, send_sem=self.send_sem.at[i], recv_sem=self.recv_sem.at[i], device_id=device, device_id_type=MESH_ID)

    def start(self, copy):
        copy.start()
        self.started.append(copy)

    def ring(self, colour, phase, view, own=None):
        order = DIM_ORDER[colour]
        dim = order[phase]
        have = sorted(order[:phase])

        def index(shift, half=None):
            where = [self.place[ZERO], self.place[ONE], self.place[TWO]]
            where[dim] = lax.rem(self.place[dim] + shift + SIDE, SIDE)
            for i, h in enumerate(have):
                where[h] = slice(None) if half is None or i > ZERO else pl.ds(TWO * half, TWO)
            return tuple(where)

        out = []
        for direction, shift in enumerate((ONE, -ONE)):
            device = (self.core, chip_at(self.place, dim, shift))
            half = direction if phase == ZERO else None
            near_dst = view(index(ZERO), None)
            out.append(dict(
                near=self.remote(near_dst if own is None else own, near_dst, device),
                far=self.remote(view(index(-shift, direction), half), view(index(-shift, direction), half), device),
                near_at=index(-shift), far_at=index(TWO, direction)))
        return out


def ag_kernel(attn_ref, ffn_ref, vec_ref, oattn_ref, planes_ref, vec_out, attn_v, send_sem, recv_sem, load_sem):
    net = Gather(send_sem, recv_sem)
    core, place = net.core, net.place
    rows, width = attn_ref.shape
    band = rows // (TWO * COLOURS)
    vec_high = vec_ref.shape[ZERO]
    stores, finals = [], []

    def band_rows(colour):
        return pl.ds(pl.multiple_of((core * COLOURS + colour) * band, band), band)

    def columns(half):
        return slice(None) if half is None else pl.ds(half * (width // TWO), width // TWO)

    def attn_view(colour):
        return lambda where, half: attn_v.at[where + (band_rows(colour), columns(half))]

    def ffn_view(colour):
        last = DIM_ORDER[colour][TWO]
        return lambda where, half: planes_ref.at[(colour,) + tuple(w for d, w in enumerate(where) if d != last) + (slice(None), columns(half))]

    def vec_view(where, half):
        return vec_out.at[where + (slice(None) if half is None else pl.ds(half * (vec_high // TWO), vec_high // TWO), slice(None))]

    colours = range(COLOURS)
    attn_own = [attn_ref.at[band_rows(colour), :] for colour in colours]
    ffn_own = [ffn_ref.at[band_rows(colour), :] for colour in colours]
    rings = {('attn', phase): [net.ring(colour, phase, attn_view(colour), attn_own[colour] if phase == ZERO else None) for colour in colours] for phase in range(THREE)}
    rings |= {('ffn', phase): [net.ring(colour, phase, ffn_view(colour), ffn_own[colour] if phase == ZERO else None) for colour in colours] for phase in range(TWO)}
    rings |= {('vec', phase): [net.ring(ONE, phase, vec_view, vec_ref if phase == ZERO else None)] for phase in range(THREE)}

    def publish(at):
        keep = pltpu.make_async_copy(attn_v.at[at], oattn_ref.at[at], load_sem.at[len(stores)])
        keep.start()
        stores.append(keep)
        give = net.remote(attn_v.at[at], oattn_ref.at[at], net.sibling)
        net.start(give)
        finals.append(give)

    def send_near(name, phase):
        for ring in rings.get((name, phase), ()):
            for way in ring:
                net.start(way['near'])

    def pass_on(name, phase):
        for ring in rings.get((name, phase), ()):
            for way in ring:
                way['near'].wait_recv()
                net.start(way['far'])
        if phase == TWO and name == 'attn':
            for colour in colours:
                for way in rings[(name, phase)][colour]:
                    publish(way['near_at'] + (band_rows(colour), slice(None)))

    def complete(name, phase):
        for colour, ring in enumerate(rings.get((name, phase), ())):
            for way in ring:
                way['far'].wait_recv()
            if phase < TWO and (name, phase + ONE) in rings:
                for way in rings[(name, phase + ONE)][colour]:
                    net.start(way['near'])
            if phase == TWO and name == 'attn':
                for way in ring:
                    publish(way['far_at'] + (band_rows(colour), slice(None)))
        if phase == ONE and name == 'attn':
            for colour in colours:
                last = DIM_ORDER[colour][TWO]
                publish(tuple(place[d] if d == last else slice(None) for d in range(THREE)) + (band_rows(colour), slice(None)))

    for colour in colours:
        attn_v[(place[ZERO], place[ONE], place[TWO]) + (band_rows(colour), slice(None))] = attn_ref[band_rows(colour), :]
        kept = [place[d] for d in range(THREE) if d != DIM_ORDER[colour][TWO]]
        planes_ref[(colour, kept[ZERO], kept[ONE])] = ffn_ref[band_rows(colour), :]
    vec_out[place[ZERO], place[ONE], place[TWO]] = vec_ref[ALL]
    meet_neighbours(place)
    names = ('attn', 'vec', 'ffn')
    for name in names:
        send_near(name, ZERO)
    for phase in range(THREE):
        for name in names:
            pass_on(name, phase)
        for name in names:
            complete(name, phase)
    for copy in finals:
        copy.wait_recv()
    for copy in net.started:
        copy.wait_send()
    for copy in stores:
        copy.wait()


def gather_params(attn_w, ffn_w, vec_rows):
    rows, width = attn_w.shape
    full = (SIDE, SIDE, SIDE, rows, width)
    n_copies = COLOURS * 4 * (THREE + TWO) + 4 * THREE + COLOURS * 5
    vmem = pl.BlockSpec(memory_space=pltpu.VMEM)
    return pl.pallas_call(
        ag_kernel,
        in_specs=[vmem] * THREE, out_specs=[pl.BlockSpec(memory_space=pl.ANY), vmem, vmem],
        out_shape=[jax.ShapeDtypeStruct(full, BF16), jax.ShapeDtypeStruct((COLOURS, SIDE, SIDE, rows // (TWO * COLOURS), width), BF16),
                   jax.ShapeDtypeStruct((SIDE, SIDE, SIDE) + vec_rows.shape, F32)],
        scratch_shapes=[pltpu.VMEM(full, BF16), pltpu.SemaphoreType.DMA((n_copies,)), pltpu.SemaphoreType.DMA((n_copies,)), pltpu.SemaphoreType.DMA((COLOURS * 5,))],
        compiler_params=pltpu.CompilerParams(collective_id=TWO, has_side_effects=True, vmem_limit_bytes=VMEM_BYTES),
        cost_estimate=pl.CostEstimate(flops=10 ** 9, bytes_accessed=4 * rows * width * SIDE ** THREE, transcendentals=ZERO),
        name='gather_params',
    )(attn_w, ffn_w, vec_rows)


class LastPhase:
    def __init__(self, planes, out, near, far, send_sem, recv_sem, load_sem):
        self.planes, self.out, self.near, self.far = planes, out, near, far
        self.send_sem, self.recv_sem, self.load_sem = send_sem, recv_sem, load_sem
        self.core, self.chip, self.place = lax.axis_index('dp'), lax.axis_index('fsdp'), torus_place()
        self.band = planes.shape[THREE]

    @staticmethod
    def scratch_shapes(planes):
        colours, side, _, band, width = planes.shape
        sems = [pltpu.SemaphoreType.DMA((9 * COLOURS,)), pltpu.SemaphoreType.DMA((9 * COLOURS,)), pltpu.SemaphoreType.DMA((5 * COLOURS,))]
        return [pltpu.VMEM((colours, TWO, side, side, band, width), BF16), pltpu.VMEM((colours, TWO, side // TWO, side, band, width), BF16)] + sems

    def remote(self, i, src, dst, device):
        return pltpu.make_async_remote_copy(src_ref=src, dst_ref=dst, send_sem=self.send_sem.at[i], recv_sem=self.recv_sem.at[i], device_id=device, device_id_type=MESH_ID)

    def ring(self, colour, direction):
        device = (self.core, chip_at(self.place, DIM_ORDER[colour][TWO], ONE - TWO * direction))
        i = 9 * colour + TWO * direction
        got = self.near.at[colour, direction]
        return (self.remote(i, self.planes.at[colour], got, device),
                self.remote(i + ONE, got.at[pl.ds(TWO * direction, TWO)], self.far.at[colour, direction], device))

    def shares(self, colour):
        last = DIM_ORDER[colour][TWO]
        rows = pl.ds(pl.multiple_of((self.core * COLOURS + colour) * self.band, self.band), self.band)
        views = [(self.planes.at[colour], ZERO, None)]
        views += [(self.near.at[colour, direction], TWO * direction - ONE, None) for direction in range(TWO)]
        views += [(self.far.at[colour, direction], TWO, direction) for direction in range(TWO)]
        out = []
        for n, (src, shift, half) in enumerate(views):
            where = [slice(None)] * THREE
            where[last] = lax.rem(self.place[last] + shift + SIDE, SIDE)
            if half is not None:
                where[min(d for d in range(THREE) if d != last)] = pl.ds(TWO * half, TWO)
            dst = self.out.at[tuple(where) + (rows, slice(None))]
            out.append((self.remote(9 * colour + 4 + n, src, dst, (ONE - self.core, self.chip)), pltpu.make_async_copy(src, dst, self.load_sem.at[5 * colour + n])))
        return out

    def share(self, colour, which):
        for n in which:
            give, keep = self.shares(colour)[n]
            give.start()
            keep.start()

    def begin(self):
        for colour in range(COLOURS):
            for direction in range(TWO):
                self.ring(colour, direction)[ZERO].start()
        for colour in range(COLOURS):
            self.share(colour, (ZERO,))

    def pass_on(self):
        for colour in range(COLOURS):
            for direction in range(TWO):
                near, far = self.ring(colour, direction)
                near.wait_recv()
                far.start()
            self.share(colour, (ONE, TWO))

    def complete(self):
        for colour in range(COLOURS):
            for direction in range(TWO):
                self.ring(colour, direction)[ONE].wait_recv()
            self.share(colour, (THREE, 4))

    def end(self):
        for colour in range(COLOURS):
            for give, keep in self.shares(colour):
                give.wait_recv()
                give.wait_send()
                keep.wait()
            for direction in range(TWO):
                for copy in self.ring(colour, direction):
                    copy.wait_send()


def dot(lhs, rhs, contract=((ONE,), (ZERO,))):
    return lax.dot_general(lhs, rhs, (contract, ((), ())), preferred_element_type=F32)


def dot_nt(lhs, rhs):
    return dot(lhs, rhs, ((ONE,), (ONE,)))


def dot_tn(lhs, rhs):
    return dot(lhs, rhs, ((ZERO,), (ZERO,)))


def norm_rows(resid, gain, shift):
    mean = jnp.mean(resid, axis=-ONE, keepdims=True)
    centred = resid - mean
    inv_std = lax.rsqrt(jnp.mean(centred * centred, axis=-ONE, keepdims=True) + LN_EPS)
    normed = centred * inv_std
    return (normed * gain + shift).astype(BF16), normed, inv_std


def norm_rows_bwd(d_out, normed, inv_std, gain):
    d_norm = d_out * gain
    return inv_std * (d_norm - jnp.mean(d_norm, axis=-ONE, keepdims=True) - normed * jnp.mean(d_norm * normed, axis=-ONE, keepdims=True))


def col_sum(values):
    return jnp.sum(values, axis=ZERO, keepdims=True)


def lane_row(head, dtype=BF16):
    lane = lax.broadcasted_iota(jnp.int32, (ONE, PAIR), ONE)
    return jnp.where((lane >= HEAD_DIM * head) & (lane < HEAD_DIM * (head + ONE)), 1.0, 0.0).astype(dtype)


def spare_lane(head):
    lane = lax.broadcasted_iota(jnp.int32, (ONE, PAIR), ONE)
    return jnp.where(lane == HEAD_DIM * (ONE - head), 1.0, 0.0)


def mask_fill(n_rows, n_valid):
    row = lax.broadcasted_iota(jnp.int32, (n_rows, PAIR), ZERO)
    return jnp.where(row >= n_valid, MASK_FILL, 0.0)


def head_masks(pair_q, pair_k, head, fill):
    q_f = pair_q * lane_row(head) + spare_lane(head).astype(BF16)
    k_f = pair_k * lane_row(head) + (fill * spare_lane(head)).astype(BF16)
    return q_f, k_f


def half_only(pair, head):
    return pair * lane_row(head)


def join_halves(first, second):
    lane = lax.broadcasted_iota(jnp.int32, first.shape, ONE)
    return jnp.where(lane < HEAD_DIM, first, second)


def score_blocks(n_heads, n_q, n_k, causal, step):
    if not causal:
        return [(head, ZERO, n_q, n_k) for head in range(n_heads)]
    return [(head, first, step, first + step) for head in range(n_heads) for first in range(ZERO, n_q, step)]


def scores_t(q_f, k_f, causal, first):
    s_t = dot_nt(k_f, q_f)
    if causal:
        key_i = lax.broadcasted_iota(jnp.int32, s_t.shape, ZERO)
        qry_i = lax.broadcasted_iota(jnp.int32, s_t.shape, ONE) + first
        s_t = jnp.where(key_i <= qry_i, s_t, MASK_FILL)
    return s_t


def pair_of(group, head):
    return group[:, head // TWO * PAIR:(head // TWO + ONE) * PAIR]


def masked_pairs(q_g, k_g, n_valid):
    fill = mask_fill(k_g.shape[ZERO], n_valid)
    cache = {}

    def get(head):
        if head not in cache:
            cache[head] = head_masks(pair_of(q_g, head), pair_of(k_g, head), head % TWO, fill)
        return cache[head]

    return get


def stack_heads(parts, n_heads):
    return jnp.concatenate([jnp.concatenate(parts[head], axis=ONE) for head in range(n_heads)], axis=ZERO)


def run_ahead(blocks, produce, transform, consume, delay):
    ahead = produce(blocks[ZERO])
    waiting = []
    for i, block in enumerate(blocks):
        now = ahead
        if i + ONE < len(blocks):
            ahead = produce(blocks[i + ONE])
        waiting.append((block, transform(block, now)))
        if len(waiting) > delay:
            consume(*waiting.pop(ZERO))
    for item in waiting:
        consume(*item)


def attend_group(q_g, k_g, v_g, n_valid, causal, lse_ref):
    n_heads = GROUP // HEAD_DIM
    o_parts = [[] for _ in range(n_heads)]
    v_t = v_g.T
    masked = masked_pairs(q_g, k_g, n_valid)

    def produce(block):
        head, first, n_q, n_k = block
        q_f, k_f = masked(head)
        return scores_t(q_f[first:first + n_q], k_f[:n_k], causal, first)

    def transform(block, s_t):
        head, first, n_q, n_k = block
        top = jnp.max(s_t, axis=ZERO, keepdims=True)
        e_t = jnp.exp(s_t - top)
        total = jnp.sum(e_t, axis=ZERO, keepdims=True)
        lse_ref[ZERO, ZERO, head:head + ONE, first:first + n_q] = top + jnp.log(total)
        return (e_t * (1.0 / total)).astype(BF16)

    def consume(block, p_t):
        head, first, n_q, n_k = block
        o_parts[head].append(dot(v_t[HEAD_DIM * head:HEAD_DIM * (head + ONE), :n_k], p_t))

    run_ahead(score_blocks(n_heads, q_g.shape[ZERO], k_g.shape[ZERO], causal, 128), produce, transform, consume, TWO)
    return stack_heads(o_parts, n_heads).T.astype(BF16)


def attend_group_bwd(d_o, q_g, k_g, v_g, n_valid, causal, lse_ref, between=None):
    n_heads = GROUP // HEAD_DIM
    k_t = k_g.T
    dq_t, dk_h, dv_h = [[] for _ in range(n_heads)], [None] * n_heads, [None] * n_heads
    masked = masked_pairs(q_g, k_g, n_valid)
    v_half = {}

    def produce(block):
        head, first, n_q, n_k = block
        q_f, k_f = masked(head)
        if head not in v_half:
            v_half[head] = half_only(pair_of(v_g, head), head % TWO)
        rows = slice(first, first + n_q)
        return scores_t(q_f[rows], k_f[:n_k], causal, first), dot_nt(v_half[head][:n_k], pair_of(d_o, head)[rows])

    def transform(block, products):
        head, first, n_q, n_k = block
        s_t, dp_t = products
        p_t = jnp.exp(s_t - lse_ref[ZERO, ZERO, head:head + ONE, first:first + n_q])
        weighted = p_t * dp_t
        return p_t.astype(BF16), (weighted - p_t * jnp.sum(weighted, axis=ZERO, keepdims=True)).astype(BF16)

    def grow(old, new):
        if old is None:
            return new
        n_old = old.shape[ZERO]
        return old + new if n_old == new.shape[ZERO] else jnp.concatenate([old + new[:n_old], new[n_old:]], axis=ZERO)

    def consume(block, operands):
        head, first, n_q, n_k = block
        p_b, ds_t = operands
        rows = slice(first, first + n_q)
        dv_h[head] = grow(dv_h[head], dot(p_b, pair_of(d_o, head)[rows]))
        dk_h[head] = grow(dk_h[head], dot(ds_t, pair_of(q_g, head)[rows]))
        dq_t[head].append(dot(k_t[HEAD_DIM * head:HEAD_DIM * (head + ONE), :n_k], ds_t))

    blocks = score_blocks(n_heads, q_g.shape[ZERO], k_g.shape[ZERO], causal, 256)
    if between is None:
        run_ahead(blocks, produce, transform, consume, ZERO)
    else:
        n_first = len(blocks) // TWO
        run_ahead(blocks[:n_first], produce, transform, consume, ZERO)
        between()
        run_ahead(blocks[n_first:], produce, transform, consume, ZERO)
    join = lambda parts: jnp.concatenate([join_halves(parts[h], parts[h + ONE]) for h in range(ZERO, n_heads, TWO)], axis=ONE)
    return stack_heads(dq_t, n_heads).T * 0.125, join(dk_h), join(dv_h)


def attn_fwd_kernel(causal, slots, guest, lens_ref, x_ref, kv_ref, wq_ref, wk_ref, wv_ref, w_all, bias_ref, rows_ref,
                    q_ref, k_ref, v_ref, o_ref, lse_ref, h_ref, normed_ref, inv_ref, o_all, wo_v, load_sem):
    q_row, k_row, v_row, o_row, gain_row, o_mat = slots
    sample, group = pl.program_id(ZERO), pl.program_id(ONE)
    d_model = wo_v.shape[ZERO]
    fetch = pltpu.make_async_copy(w_all.at[pl.ds(o_mat * d_model, d_model), :], wo_v, load_sem)

    @pl.when((sample == ZERO) & (group == ZERO))
    def _():
        fetch.start()

    turn = sample * pl.num_programs(ONE) + group
    if guest is not None:
        for where, steps in ((ZERO, (lambda: meet_neighbours(guest.place), guest.begin)), (THREE, (guest.pass_on,)), (5, (guest.complete,))):
            @pl.when(turn == where)
            def _():
                for step in steps:
                    step()

    x_b, kv_b = x_ref[ALL], kv_ref[ALL]
    q_g = ((dot(x_b, wq_ref[ALL]) + bias_ref[q_row:q_row + ONE, :]) * 0.125).astype(BF16)
    k_g = (dot(kv_b, wk_ref[ALL]) + bias_ref[k_row:k_row + ONE, :]).astype(BF16)
    v_g = (dot(kv_b, wv_ref[ALL]) + bias_ref[v_row:v_row + ONE, :]).astype(BF16)
    q_ref[ALL], k_ref[ALL], v_ref[ALL] = q_g, k_g, v_g
    o_g = attend_group(q_g, k_g, v_g, lens_ref[sample], causal, lse_ref)
    o_ref[ALL] = o_g
    o_all[:, pl.ds(pl.multiple_of(group * GROUP, GROUP), GROUP)] = o_g

    @pl.when((sample == ZERO) & (group == pl.num_programs(ONE) - ONE))
    def _():
        fetch.wait()

    @pl.when(group == pl.num_programs(ONE) - ONE)
    def _():
        resid = x_ref[ALL].astype(F32) + dot(o_all[ALL], wo_v[ALL]) + rows_ref[o_row:o_row + ONE, :]
        h_out, normed, inv_std = norm_rows(resid, rows_ref[gain_row:gain_row + ONE, :], rows_ref[gain_row + ONE:gain_row + TWO, :])
        h_ref[ALL], normed_ref[ALL], inv_ref[ALL] = h_out, normed, inv_std

    if guest is not None:
        @pl.when(turn == pl.num_programs(ZERO) * pl.num_programs(ONE) - ONE)
        def _():
            guest.end()


def attn_forward(x, kv, lens, attn_full, bias_rows, mats, slots, causal, planes=None, full_rows=None):
    d_model = x.shape[-ONE]
    n_batch = lens.shape[ZERO]
    n_q, n_k = x.shape[ZERO] // n_batch, kv.shape[ZERO] // n_batch
    n_groups = d_model // GROUP
    col = lambda mat: pl.BlockSpec((d_model, GROUP), lambda b, g: (mat, g))
    q_blk = pl.BlockSpec((n_q, GROUP), lambda b, g: (b, g))
    k_blk = pl.BlockSpec((n_k, GROUP), lambda b, g: (b, g))
    tok = lambda n: pl.BlockSpec((n, d_model), lambda b, g: (b, ZERO))
    n_heads_g = GROUP // HEAD_DIM
    out_shape = (
        jax.ShapeDtypeStruct(x.shape, BF16), jax.ShapeDtypeStruct(kv.shape, BF16), jax.ShapeDtypeStruct(kv.shape, BF16),
        jax.ShapeDtypeStruct(x.shape, BF16), jax.ShapeDtypeStruct((n_batch, n_groups, n_heads_g, n_q), F32),
        jax.ShapeDtypeStruct(x.shape, BF16), jax.ShapeDtypeStruct(x.shape, F32), jax.ShapeDtypeStruct((x.shape[ZERO], ONE), F32))
    kernel = functools.partial(attn_fwd_kernel, causal, slots + (mats[THREE],))
    in_specs = [pl.BlockSpec(memory_space=pltpu.SMEM), tok(n_q), tok(n_k), col(mats[ZERO]), col(mats[ONE]), col(mats[TWO]), pl.BlockSpec(memory_space=pl.ANY),
                pl.BlockSpec((bias_rows.shape[ZERO], GROUP), lambda b, g: (ZERO, g)), pl.BlockSpec(bias_rows.shape, lambda b, g: (ZERO, ZERO))]
    out_specs = [q_blk, k_blk, k_blk, q_blk, pl.BlockSpec((ONE, ONE, n_heads_g, n_q), lambda b, g: (b, g, ZERO, ZERO)),
                 tok(n_q), tok(n_q), pl.BlockSpec((n_q, ONE), lambda b, g: (b, ZERO))]
    scratch = [pltpu.VMEM((n_q, d_model), BF16), pltpu.VMEM((d_model, d_model), BF16), pltpu.SemaphoreType.DMA]
    args = [lens, x, kv, attn_full, attn_full, attn_full, attn_full, bias_rows, bias_rows]
    params = dict(vmem_limit_bytes=VMEM_BYTES, dimension_semantics=('arbitrary', 'arbitrary'))
    if planes is None:
        body = functools.partial(kernel, None)
    else:
        n_in, n_out, n_own = len(args), len(out_specs), len(scratch)

        def body(*refs):
            ins, held, outs, whole, rest = refs[:n_in], refs[n_in], refs[n_in + ONE:n_in + ONE + n_out], refs[n_in + ONE + n_out], refs[n_in + TWO + n_out:]
            kernel(LastPhase(held, whole, *rest[n_own:]), *ins, *outs, *rest[:n_own])

        in_specs.append(pl.BlockSpec(memory_space=pltpu.VMEM))
        args.append(planes)
        out_specs.append(pl.BlockSpec(memory_space=pl.ANY))
        out_shape += (jax.ShapeDtypeStruct((SIDE, SIDE, SIDE, full_rows // SIDE ** THREE, d_model), BF16),)
        scratch += LastPhase.scratch_shapes(planes)
        params |= dict(collective_id=5, has_side_effects=True)
    return pl.pallas_call(
        body, grid=(n_batch, n_groups), in_specs=in_specs, out_specs=out_specs, out_shape=out_shape, scratch_shapes=scratch,
        compiler_params=pltpu.CompilerParams(**params),
        cost_estimate=pl.CostEstimate(flops=TWO * d_model * d_model * (TWO * x.shape[ZERO] + TWO * kv.shape[ZERO]) + 16 * x.shape[ZERO] * n_k * d_model, bytes_accessed=20 * x.shape[ZERO] * d_model, transcendentals=ZERO),
        name='attn_fwd',
    )(*args)


def attn_bwd_kernel(causal, gain_row, mats, guest, lens_ref, dres_ref, wo_ref, w_all, q_ref, k_ref, v_ref, lse_ref,
                    rows_ref, normed_ref, inv_ref, dq_ref, dk_ref, dv_ref, dx_ref, dkv_ref, sums_ref, tail_ref, d_all, dk_all, dv_all, w_v, load_sem):
    sample, group = pl.program_id(ZERO), pl.program_id(ONE)
    d_model = w_v.shape[ONE]
    fetches = [pltpu.make_async_copy(w_all.at[pl.ds(mat * d_model, d_model), :], w_v.at[i], load_sem.at[i]) for i, mat in enumerate(mats[:THREE])]

    @pl.when((sample == ZERO) & (group == ZERO))
    def _():
        for fetch in fetches:
            fetch.start()

    turn = sample * pl.num_programs(ONE) + group
    if guest is not None:
        guest(ZERO, TWO * turn)
    d_o = dot_nt(dres_ref[ALL].astype(BF16), wo_ref[ALL]).astype(BF16)
    between = None if guest is None else functools.partial(guest, ONE, TWO * turn + ONE)
    dq, dk, dv = attend_group_bwd(d_o, q_ref[ALL], k_ref[ALL], v_ref[ALL], lens_ref[sample], causal, lse_ref, between)
    sums_ref[ZERO, ZERO:ONE, :] = col_sum(dq)
    sums_ref[ZERO, ONE:TWO, :] = col_sum(dk)
    sums_ref[ZERO, TWO:THREE, :] = col_sum(dv)
    cols = pl.ds(pl.multiple_of(group * GROUP, GROUP), GROUP)
    for full, out, value in ((d_all, dq_ref, dq), (dk_all, dk_ref, dk), (dv_all, dv_ref, dv)):
        rounded = value.astype(BF16)
        out[ALL] = rounded
        full[:, cols] = rounded

    @pl.when((sample == ZERO) & (group == pl.num_programs(ONE) - ONE))
    def _():
        for fetch in fetches:
            fetch.wait()

    @pl.when(group == pl.num_programs(ONE) - ONE)
    def _():
        d_kv = dot_nt(dk_all[ALL], w_v[ONE]) + dot_nt(dv_all[ALL], w_v[TWO])
        d_h = dres_ref[ALL] + dot_nt(d_all[ALL], w_v[ZERO])
        if causal:
            dx_ref[ALL] = (d_h + d_kv).astype(BF16)
            tail_ref[ALL] = jnp.zeros_like(tail_ref)
        else:
            dkv_ref[ALL] = d_kv.astype(BF16)
            normed = normed_ref[ALL]
            d_resid = norm_rows_bwd(d_h, normed, inv_ref[ALL], rows_ref[gain_row:gain_row + ONE, :])
            dx_ref[ALL] = d_resid
            tail_ref[ZERO, ZERO:ONE, :] = col_sum(d_resid)
            tail_ref[ZERO, ONE:TWO, :] = col_sum(d_h * normed)
            tail_ref[ZERO, TWO:THREE, :] = col_sum(d_h)

    if guest is not None:
        guest(TWO, TWO * turn + TWO)


def scatter_guest(scatter, plans, parity, position):
    absorb, relay, settle = (lambda *turns: [functools.partial(scatter.absorb, turn) for turn in turns]), (lambda phase: functools.partial(scatter.relay, phase)), (lambda phase: functools.partial(scatter.settle, phase))
    plan = {ZERO: [functools.partial(meet_neighbours, scatter.place), scatter.begin]} | plans(absorb, relay, settle)
    plan[12] = plan.get(12, []) + [scatter.end]
    for where, steps in plan.items():
        if where % TWO == parity % TWO and (where == 12) == (parity == TWO):
            @pl.when(position == where)
            def _():
                for step in steps:
                    step()


def attn_backward(dres, q, k, v, lse, lens, attn_full, bias_rows, mats, causal, g_rows, part, plans, scale, gain_row=ZERO, normed=None, inv_std=None):
    d_model = q.shape[-ONE]
    n_batch = lens.shape[ZERO]
    n_q, n_k = q.shape[ZERO] // n_batch, k.shape[ZERO] // n_batch
    n_groups = d_model // GROUP
    row = lambda mat: pl.BlockSpec((GROUP, d_model), lambda b, g: (mat * n_groups + g, ZERO))
    q_blk = pl.BlockSpec((n_q, GROUP), lambda b, g: (b, g))
    k_blk = pl.BlockSpec((n_k, GROUP), lambda b, g: (b, g))
    tok = lambda n: pl.BlockSpec((n, d_model), lambda b, g: (b, ZERO))
    n_heads_g = GROUP // HEAD_DIM
    whole_rows = pl.BlockSpec(bias_rows.shape, lambda b, g: (ZERO, ZERO))
    kernel = functools.partial(attn_bwd_kernel, causal, gain_row, mats)
    params = dict(vmem_limit_bytes=VMEM_BYTES, dimension_semantics=('arbitrary', 'arbitrary'))
    in_specs = [pl.BlockSpec(memory_space=pltpu.SMEM), tok(n_q), row(mats[THREE]), pl.BlockSpec(memory_space=pl.ANY), q_blk, k_blk, k_blk,
                pl.BlockSpec((ONE, ONE, n_heads_g, n_q), lambda b, g: (b, g, ZERO, ZERO)), whole_rows]
    args = [lens, dres, attn_full, attn_full, q, k, v, lse, bias_rows]
    sums_blk = pl.BlockSpec((ONE, 8, GROUP), lambda b, g: (b, ZERO, g))
    tail_blk = pl.BlockSpec((ONE, 8, d_model), lambda b, g: (b, ZERO, ZERO))
    tail_shape = jax.ShapeDtypeStruct((n_batch, 8, d_model), F32)
    out_shape = [jax.ShapeDtypeStruct(q.shape, BF16), jax.ShapeDtypeStruct(k.shape, BF16), jax.ShapeDtypeStruct(k.shape, BF16),
                 jax.ShapeDtypeStruct(q.shape, BF16 if causal else F32)]
    out_specs = [q_blk, k_blk, k_blk, tok(n_q)]
    own = [pltpu.VMEM((n_q, d_model), BF16), pltpu.VMEM((n_k, d_model), BF16), pltpu.VMEM((n_k, d_model), BF16),
           pltpu.VMEM((THREE, d_model, d_model), BF16), pltpu.SemaphoreType.DMA((THREE,))]
    if not causal:
        in_specs += [tok(n_q), pl.BlockSpec((n_q, ONE), lambda b, g: (b, ZERO))]
        args += [normed, inv_std]
        out_shape.append(jax.ShapeDtypeStruct(k.shape, BF16))
        out_specs.append(tok(n_k))
    out_shape += [tail_shape, tail_shape]
    out_specs += [sums_blk, tail_blk]
    n_in, n_out, n_own = len(args), len(out_shape), len(own)
    first_row, n_rows = part

    def body(*refs):
        ins, source, outs, total, rest = refs[:n_in], refs[n_in], refs[n_in + ONE:n_in + ONE + n_out], refs[n_in + ONE + n_out], refs[n_in + TWO + n_out:]
        scatter = Scatter(scale, [(source, first_row, n_rows)], [total], rest[n_own:])
        if causal:
            ins, outs = ins + (None, None), outs[:4] + (None,) + outs[4:]
        kernel(functools.partial(scatter_guest, scatter, plans), *ins, *outs, *rest[:n_own])

    anywhere = pl.BlockSpec(memory_space=pl.ANY)
    in_specs.append(anywhere)
    args.append(as_torus(g_rows))
    out_specs.append(anywhere)
    out_shape.append(jax.ShapeDtypeStruct((n_rows, d_model), F32))
    scratch = own + Scatter.scratch_shapes([n_rows])
    params = dict(collective_id=THREE + causal, has_side_effects=True, vmem_limit_bytes=63 * 1024 * 1024, dimension_semantics=('arbitrary', 'arbitrary'))
    return pl.pallas_call(
        body, grid=(n_batch, n_groups), in_specs=in_specs, out_specs=out_specs, out_shape=out_shape, scratch_shapes=scratch,
        compiler_params=pltpu.CompilerParams(**params),
        cost_estimate=pl.CostEstimate(flops=TWO * d_model * d_model * (TWO * q.shape[ZERO] + TWO * k.shape[ZERO]) + 40 * q.shape[ZERO] * n_k * d_model, bytes_accessed=20 * q.shape[ZERO] * d_model, transcendentals=ZERO),
        name='attn_bwd',
    )(*args)


def ffn_kernel(n_blocks, h_ref, dy_ref, up_ref, down_ref, rows_ref, bias_ref, normed_ref, inv_ref,
               y_ref, grad_ref, dres2_ref, tail_ref, upsum_ref, gelu_all, dup_all, dres3_all, h_all):
    step = pl.program_id(ZERO)
    block, d_model = h_ref.shape
    n_square = gelu_all.shape[ONE] // d_model

    @pl.when(step < n_blocks)
    def _():
        rows = pl.ds(pl.multiple_of(step * block, block), block)
        h_b = h_ref[ALL]
        h_all[rows, :] = h_b
        up = dot_nt(h_b, up_ref[ALL]) + bias_ref[ALL]
        cdf = 0.5 * (1.0 + lax.erf(up * 0.7071067811865476))
        gelu = (up * cdf).astype(BF16)
        slope = cdf + up * (0.3989422804014327 * jnp.exp(-0.5 * up * up))
        gelu_all[rows, :] = gelu
        resid = h_b.astype(F32) + dot(gelu, down_ref[ALL]) + rows_ref[8:9, :]
        y_b, normed3, inv3 = norm_rows(resid, rows_ref[13:14, :], rows_ref[14:15, :])
        y_ref[ALL] = y_b
        dy = dy_ref[ALL].astype(F32)
        d_res3 = norm_rows_bwd(dy, normed3, inv3, rows_ref[13:14, :])
        d_res3_b = d_res3.astype(BF16)
        dres3_all[rows, :] = d_res3_b
        d_up = dot_nt(d_res3_b, down_ref[ALL]) * slope
        d_up_b = d_up.astype(BF16)
        dup_all[rows, :] = d_up_b
        d_h2 = d_res3 + dot(d_up_b, up_ref[ALL])
        normed2 = normed_ref[ALL]
        d_res2 = norm_rows_bwd(d_h2, normed2, inv_ref[ALL], rows_ref[11:12, :])
        dres2_ref[ALL] = d_res2
        tail = jnp.concatenate([col_sum(d_res2), col_sum(d_res3), col_sum(d_h2 * normed2), col_sum(d_h2), col_sum(dy * normed3), col_sum(dy),
                                jnp.zeros((TWO, dy.shape[ONE]), F32)], axis=ZERO)
        up_sum = col_sum(d_up)

        @pl.when(step == ZERO)
        def _():
            tail_ref[ALL] = tail
            upsum_ref[ALL] = up_sum

        @pl.when(step > ZERO)
        def _():
            tail_ref[ALL] += tail
            upsum_ref[ALL] += up_sum

    square = step - n_blocks
    cols = pl.ds(pl.multiple_of(lax.rem(square + TWO * n_square, n_square) * d_model, d_model), d_model)

    @pl.when((square >= ZERO) & (square < n_square))
    def _():
        grad_ref[ALL] = dot_tn(dup_all[:, cols], h_all[ALL])

    @pl.when(square >= n_square)
    def _():
        grad_ref[ALL] = dot_tn(gelu_all[:, cols], dres3_all[ALL])


def ffn_both(h2, dy, ffn_full, bias_rows, up_bias, normed2, inv2, block=256):
    n_tok, d_model = h2.shape
    ffn_dim = ffn_full.shape[ZERO] // TWO
    n_blocks = n_tok // block
    n_steps = n_blocks + ffn_full.shape[ZERO] // d_model
    at = lambda i: jnp.minimum(i, n_blocks - ONE)
    tok = pl.BlockSpec((block, d_model), lambda i: (at(i), ZERO))
    once = lambda shape, idx: pl.BlockSpec(shape, lambda i: idx, pipeline_mode=pl.Buffered(ONE))
    return pl.pallas_call(
        functools.partial(ffn_kernel, n_blocks), grid=(n_steps,),
        in_specs=[tok, tok, once((ffn_dim, d_model), (ZERO, ZERO)), once((ffn_dim, d_model), (ONE, ZERO)), once(bias_rows.shape, (ZERO, ZERO)), once((ONE, ffn_dim), (ZERO, ZERO)),
                  tok, pl.BlockSpec((block, ONE), lambda i: (at(i), ZERO))],
        out_specs=[tok, pl.BlockSpec((d_model, d_model), lambda i: (jnp.maximum(i - n_blocks, ZERO), ZERO)), tok, pl.BlockSpec((8, d_model), lambda i: (ZERO, ZERO)), pl.BlockSpec((ONE, ffn_dim), lambda i: (ZERO, ZERO))],
        out_shape=[jax.ShapeDtypeStruct(h2.shape, BF16), jax.ShapeDtypeStruct(ffn_full.shape, F32), jax.ShapeDtypeStruct(h2.shape, F32),
                   jax.ShapeDtypeStruct((8, d_model), F32), jax.ShapeDtypeStruct((ONE, ffn_dim), F32)],
        scratch_shapes=[pltpu.VMEM((n_tok, ffn_dim), BF16), pltpu.VMEM((n_tok, ffn_dim), BF16), pltpu.VMEM((n_tok, d_model), BF16), pltpu.VMEM((n_tok, d_model), BF16)],
        compiler_params=pltpu.CompilerParams(vmem_limit_bytes=VMEM_BYTES, dimension_semantics=('arbitrary',)),
        cost_estimate=pl.CostEstimate(flops=12 * n_tok * d_model * ffn_dim, bytes_accessed=30 * n_tok * d_model, transcendentals=ZERO),
        name='ffn_both',
    )(h2, dy, ffn_full, ffn_full, bias_rows, up_bias, normed2, inv2)


def CROSS_PLAN(absorb, relay, settle):
    return {ONE: absorb(ZERO), TWO: absorb(ONE), THREE: absorb(TWO, THREE), 4: [relay(ZERO)], 7: [settle(ZERO)], 8: [relay(ONE)], 10: [settle(ONE)], 11: [relay(TWO)], 12: [settle(TWO)]}


def SELF_PLAN(absorb, relay, settle):
    return {ONE: absorb(ZERO, ONE), TWO: absorb(TWO, THREE), 4: [relay(ZERO)], 7: [settle(ZERO)], 9: [relay(ONE)], 11: [settle(ONE)], 12: [relay(TWO), settle(TWO)]}


def solution(mesh):
    n_fsdp = mesh.shape['fsdp']
    n_dp = mesh.shape['dp']
    batch_axes = ('dp', 'fsdp')
    act_spec = P(batch_axes, None, None)
    len_spec = P(batch_axes)
    row_spec = P('fsdp', None)
    vec_spec = P('fsdp')

    def device_step(dec_in, enc_out, src_lens, tgt_lens, y_cot, attn_w, ffn_w, vec_params):
        d_model, n_vec = dec_in.shape[TWO], vec_params.shape[ZERO]
        scale = 1.0 / (dec_in.shape[ZERO] * dec_in.shape[ONE] * n_fsdp * n_dp)
        x, enc, dy = (a.reshape(-ONE, d_model) for a in (dec_in, enc_out, y_cot))
        vec_rows = jnp.pad(vec_params.astype(F32), (ZERO, 16 * LANES - n_vec)).reshape(16, LANES)
        attn_tiles, planes, vec_tiles = gather_params(attn_w, ffn_w, vec_rows)
        attn_full = attn_tiles.reshape(-ONE, d_model)
        vec_f = vec_tiles.reshape(n_fsdp, 16, LANES)[:, :TWO].reshape(n_fsdp, TWO * LANES)[:, :n_vec].reshape(-ONE)
        bias_rows = jnp.pad(vec_f[:15 * d_model].reshape(15, d_model), ((ZERO, ONE), (ZERO, ZERO)))
        up_bias = vec_f[15 * d_model:].reshape(ONE, -ONE)
        n_early = TWO * ffn_w.shape[ZERO] // THREE
        q1, k1, v1, o1, lse1, h1, normed1, inv1, ffn_tiles = attn_forward(x, x, tgt_lens, attn_full, bias_rows, (ZERO, ONE, TWO, THREE), (ZERO, ONE, TWO, THREE, 9), True, planes, ffn_w.shape[ZERO] * n_fsdp)
        ffn_full = ffn_tiles.reshape(-ONE, d_model)
        q2, k2, v2, o2, lse2, h2, normed2, inv2 = attn_forward(h1, enc, src_lens, attn_full, bias_rows, (4, 5, 6, 7), (4, 5, 6, 7, 11), False)
        y, g_ffn, d_res2, ffn_tail, up_sum = ffn_both(h2, dy, ffn_full, bias_rows, up_bias, normed2, inv2)
        dq2, dk2, dv2, d_res1, d_enc, sums2, tail2, ffn_early = attn_backward(d_res2, q2, k2, v2, lse2, src_lens, attn_full, bias_rows, (4, 5, 6, 7), False, g_ffn, (ZERO, n_early), CROSS_PLAN, scale, 9, normed1, inv1)
        dq1, dk1, dv1, d_x, sums1, _, ffn_late = attn_backward(d_res1, q1, k1, v1, lse1, tgt_lens, attn_full, bias_rows, (ZERO, ONE, TWO, THREE), True, g_ffn, (n_early, ffn_w.shape[ZERO] - n_early), SELF_PLAN, scale)
        s1, s2, t2 = jnp.sum(sums1, axis=ZERO), jnp.sum(sums2, axis=ZERO), jnp.sum(tail2, axis=ZERO)
        g_vec = jnp.concatenate([s1[ZERO:THREE].reshape(-ONE), t2[ZERO], s2[ZERO:THREE].reshape(-ONE), ffn_tail[ZERO], ffn_tail[ONE], t2[ONE], t2[TWO], ffn_tail[TWO], ffn_tail[THREE], ffn_tail[4], ffn_tail[5], up_sum[ZERO]])
        g_rows = jnp.pad(g_vec.reshape(n_fsdp, ONE, n_vec), ((ZERO, ZERO), (ZERO, 7), (ZERO, d_model - n_vec))).reshape(n_fsdp * 8, -ONE)
        pairs = ((x, dq1), (x, dk1), (x, dv1), (o1, d_res1.astype(BF16)), (h1, dq2), (enc, dk2), (enc, dv2), (o2, d_res2.astype(BF16)))
        g_attn = jnp.concatenate([dot_tn(lhs, rhs) for lhs, rhs in pairs], axis=ZERO)
        attn_out, vec_out = scatter_grads(g_attn, g_rows, scale)
        return y.reshape(dec_in.shape), d_x.reshape(dec_in.shape), d_enc.reshape(enc_out.shape), attn_out, jnp.concatenate([ffn_early, ffn_late], axis=ZERO), vec_out[ZERO, :n_vec]

    return jax.shard_map(device_step, mesh=mesh, in_specs=(act_spec, act_spec, len_spec, len_spec, act_spec, row_spec, row_spec, vec_spec), out_specs=(act_spec, act_spec, act_spec, row_spec, row_spec, vec_spec), check_vma=False)
```

```python
import functools
import jax
import jax.numpy as jnp
from jax import lax
from jax.experimental import pallas as pl
from jax.experimental.pallas import tpu as pltpu
from jax.sharding import PartitionSpec as P

ZERO, ONE, TWO, THREE = range(4)
ALL = ...
HEAD_DIM = 64
LN_EPS = 1e-5
MASK_FILL = -1e30
VMEM_BYTES = 60 * 1024 * 1024
F32 = jnp.float32
BF16 = jnp.bfloat16
GROUP = 256
PAIR = 128


SIDE = 4
LANES = 128
COLOURS = THREE
DIM_ORDER = ((TWO, ONE, ZERO), (ONE, ZERO, TWO), (ZERO, TWO, ONE))
MESH_ID = pl.DeviceIdType.MESH


def torus_place():
    chip = lax.axis_index('fsdp')
    return (chip // (SIDE * SIDE), lax.rem(chip // SIDE, SIDE), lax.rem(chip, SIDE))


def chip_at(place, dim, shift):
    moved = [lax.rem(p + shift + SIDE, SIDE) if d == dim else p for d, p in enumerate(place)]
    return (moved[ZERO] * SIDE + moved[ONE]) * SIDE + moved[TWO]


RINGS, PLANES = 'rings', 'planes'


def meet_neighbours(place, reach=PLANES):
    barrier = pltpu.get_barrier_semaphore()
    core, chip = lax.axis_index('dp'), lax.axis_index('fsdp')
    signal = lambda device: pl.semaphore_signal(barrier, inc=ONE, device_id=device, device_id_type=MESH_ID)
    signal((ONE - core, chip))
    if reach == RINGS:
        for dim in range(THREE):
            for shift in (ONE, -ONE):
                signal((core, chip_at(place, dim, shift)))
        pl.semaphore_wait(barrier, 7)
        return

    def other(step, _):
        steps = (step // (SIDE * SIDE), lax.rem(step // SIDE, SIDE), lax.rem(step, SIDE))
        moved = [lax.rem(p + s, SIDE) for p, s in zip(place, steps)]

        @pl.when(steps[ZERO] * steps[ONE] * steps[TWO] == ZERO)
        def _():
            signal((core, (moved[ZERO] * SIDE + moved[ONE]) * SIDE + moved[TWO]))

        return ZERO

    lax.fori_loop(ONE, SIDE ** THREE, other, ZERO)
    pl.semaphore_wait(barrier, SIDE ** THREE - (SIDE - ONE) ** THREE)


class Scatter:
    def __init__(self, scale, sources, outs, scratch, resident=False):
        self.scale, self.outs, self.resident = scale, outs, resident
        self.sources = [(ref, pl.ds(first, n)) for ref, first, n in sources]
        (self.acc, self.got, self.far, self.plane, self.send_sem, self.recv_sem, self.load_sem, *stage) = scratch
        self.stage = None if resident else stage[ZERO]
        self.heights = [n for _, _, n in sources]
        self.offsets = [sum(self.heights[:i]) for i in range(len(sources))]
        self.core, self.chip, self.place = lax.axis_index('dp'), lax.axis_index('fsdp'), torus_place()
        self.sibling = (ONE - self.core, self.chip)

    @staticmethod
    def scratch_shapes(heights, resident=False):
        h = sum(heights)
        buf = lambda *shape: pltpu.VMEM((COLOURS,) + shape + (h, LANES), F32)
        n = Scatter.base(len(heights), THREE)
        sems = [pltpu.SemaphoreType.DMA((n,)), pltpu.SemaphoreType.DMA((n,)), pltpu.SemaphoreType.DMA((THREE + COLOURS, len(heights)))]
        stage = [] if resident else [pltpu.VMEM((THREE, SIDE, SIDE, h, LANES), F32)]
        return [buf(SIDE, SIDE, SIDE), buf(TWO, SIDE, SIDE), buf(TWO, TWO, SIDE), buf(SIDE * SIDE)] + sems + stage

    @staticmethod
    def base(n_parts, section):
        sizes = (COLOURS * SIDE * n_parts, COLOURS * 10, COLOURS * SIDE * SIDE, COLOURS * n_parts)
        return sum(sizes[:section]) if section < THREE else sum(sizes)

    def remote(self, section, i, src, dst, device):
        n = Scatter.base(len(self.sources), section) + i if section < THREE else Scatter.base(len(self.sources), TWO) + COLOURS * SIDE * SIDE + i
        return pltpu.make_async_remote_copy(src_ref=src, dst_ref=dst, send_sem=self.send_sem.at[n], recv_sem=self.recv_sem.at[n], device_id=device, device_id_type=MESH_ID)

    def columns(self, of_core, colour):
        return pl.ds(pl.multiple_of((of_core * COLOURS + colour) * LANES, LANES), LANES)

    def rows_of(self, part):
        return pl.ds(self.offsets[part], self.heights[part])

    def group(self, colour, d):
        dim = DIM_ORDER[colour][ZERO]
        where = [slice(None)] * THREE
        where[dim] = lax.rem(self.place[dim] + d, SIDE)
        return tuple(where)

    def swap(self, i, colour, part, where):
        src, rows = self.sources[part]
        return self.remote(ZERO, i, src.at[where + (rows, self.columns(ONE - self.core, colour))], self.acc.at[(colour,) + where + (self.rows_of(part), slice(None))], self.sibling)

    def swaps(self, turn, parts=None):
        out = []
        for colour in range(COLOURS):
            for part in range(len(self.sources)) if parts is None else parts:
                where = (turn, slice(None), slice(None)) if self.resident else self.group(colour, TURNS[turn])
                out.append(self.swap((turn * COLOURS + colour) * len(self.sources) + part, colour, part, where))
        return out

    def load(self, turn, colour):
        where, cols, buf = self.group(colour, TURNS[turn]), self.columns(self.core, colour), (turn * COLOURS + colour) % THREE
        return [pltpu.make_async_copy(src.at[where + (rows, cols)], self.stage.at[buf, :, :, self.rows_of(i), :], self.load_sem.at[buf, i]) for i, (src, rows) in enumerate(self.sources)]

    def ring(self, colour, direction):
        shift = ONE - TWO * direction
        dim = DIM_ORDER[colour][ZERO]
        device = (self.core, chip_at(self.place, dim, shift))
        i = (colour * TWO + direction) * 5
        near = lax.rem(self.place[dim] + shift + SIDE, SIDE)
        across = lax.rem(self.place[dim] + TWO, SIDE)

        def at(target, half_at):
            where = [slice(None)] * THREE
            where[dim] = target
            where[ZERO if dim != ZERO else ONE] = half_at
            return self.acc.at[(colour,) + tuple(where)]

        def half_copies(base, target, half, ref, first):
            if dim == ZERO:
                return [(None, self.remote(ONE, base, at(target, pl.ds(TWO * half, TWO)), ref.at[pl.ds(first, TWO)], device))]
            return [(TWO * half + k, self.remote(ONE, base + k, at(target, pl.ds(TWO * half + k, ONE)), ref.at[pl.ds(first + k, ONE)], device)) for k in range(TWO)]

        got = self.got.at[colour, direction]
        far = half_copies(i, across, direction, self.far.at[colour, direction], ZERO)
        own = half_copies(i + TWO, near, ONE - direction, got, TWO * (ONE - direction))
        fed = self.remote(ONE, i + 4, at(near, pl.ds(TWO * direction, TWO)), got.at[pl.ds(TWO * direction, TWO)], device)
        return far, own, fed, at(near, pl.ds(TWO * direction, TWO))

    def mine(self, colour):
        return self.acc.at[(colour,) + self.group(colour, ZERO)]

    def plane_copy(self, colour, step):
        dims = sorted(DIM_ORDER[colour][ONE:])
        moved = list(self.place)
        for d, s in zip(dims, (step // SIDE, lax.rem(step, SIDE))):
            moved[d] = lax.rem(self.place[d] + s, SIDE)
        device = (self.core, (moved[ZERO] * SIDE + moved[ONE]) * SIDE + moved[TWO])
        return self.remote(TWO, colour * SIDE * SIDE + step, self.acc.at[colour, moved[ZERO], moved[ONE], moved[TWO]], self.plane.at[colour, step], device)

    def each_step(self, body):
        def run(step, _):
            body(step)
            return ZERO

        lax.fori_loop(ONE, SIDE * SIDE, run, ZERO)

    def gives(self, colour):
        n = len(self.sources)
        done = self.acc.at[colour, self.place[ZERO], self.place[ONE], self.place[TWO]]
        cols = self.columns(self.core, colour)
        pairs = [(done.at[self.rows_of(i), :], out.at[:, cols]) for i, out in enumerate(self.outs)]
        return [(self.remote(THREE, colour * n + i, src, dst, self.sibling), pltpu.make_async_copy(src, dst, self.load_sem.at[THREE + colour, i])) for i, (src, dst) in enumerate(pairs)]

    def add_into(self, dst, sources):
        def body(i, _):
            idx = (i // SIDE, lax.rem(i, SIDE))
            total = dst[idx]
            for src in sources:
                total = total + src[idx]
            dst[idx] = total
            return ZERO

        lax.fori_loop(ZERO, dst.shape[ZERO] * SIDE, body, ZERO)


    def begin(self):
        for colour in range(COLOURS):
            for copy in self.load(ZERO, colour):
                copy.start()
        for turn in range(SIDE):
            for copy in self.swaps(turn):
                copy.start()

    def absorb(self, turn):
        swaps = self.swaps(turn)
        n = len(self.sources)
        for colour in range(COLOURS):
            for copy in self.load(turn, colour):
                copy.wait()
            for copy in swaps[colour * n:(colour + ONE) * n]:
                copy.wait_recv()
            self.add_into(self.acc.at[(colour,) + self.group(colour, TURNS[turn])], [self.stage.at[(turn * COLOURS + colour) % THREE]])
            if turn + ONE < SIDE:
                for copy in self.load(turn + ONE, colour):
                    copy.start()
            for direction in range(TWO):
                far, own, _, _ = self.ring(colour, direction)
                if turn == ZERO or turn == ONE + direction:
                    for _, copy in far if turn == ZERO else own:
                        copy.start()

    def absorb_plane(self, z):
        for colour, copy in enumerate(self.swaps(z, (ZERO,))):
            copy.wait_recv()
            self.add_into(self.acc.at[colour, z, :, :, self.rows_of(ZERO), :], [self.sources[ZERO][ZERO].at[z, :, :, :, self.columns(self.core, colour)]])
            for direction in range(TWO):
                far, own, _, _ = self.ring(colour, direction)
                if DIM_ORDER[colour][ZERO] != ZERO:
                    for at_z, copy in far + own:
                        if at_z == z:
                            copy.start()
                else:
                    away = lax.rem(z - self.place[ZERO] + SIDE, SIDE)
                    for steps, copies in ((TWO, far), ((ONE - TWO * direction) % SIDE, own)):
                        @pl.when(away == steps)
                        def _():
                            for _, copy in copies:
                                copy.start()

    def relay(self):
        for colour in range(COLOURS):
            rings = [self.ring(colour, direction) for direction in range(TWO)]
            for direction, (far, _, _, fed_view) in enumerate(rings):
                for _, copy in far:
                    copy.wait_recv()
                self.add_into(fed_view, [self.far.at[colour, direction]])
            for _, _, fed, _ in rings:
                fed.start()

    def settle(self):
        for colour in range(COLOURS):
            for direction in range(TWO):
                _, own, fed, _ = self.ring(colour, direction)
                for _, copy in own:
                    copy.wait_recv()
                fed.wait_recv()
            self.add_into(self.mine(colour), [self.got.at[colour, direction] for direction in range(TWO)])
            self.each_step(lambda step: self.plane_copy(colour, step).start())

    def finish(self):
        for colour in range(COLOURS):
            self.each_step(lambda step: self.plane_copy(colour, step).wait_recv())
            done = self.acc.at[colour, self.place[ZERO], self.place[ONE], self.place[TWO]]
            done[ALL] = lax.fori_loop(ONE, SIDE * SIDE, lambda step, total: total + self.plane[colour, step], done[ALL]) * self.scale
        for colour in range(COLOURS):
            for give, keep in self.gives(colour):
                keep.start()
                give.start()

    def end(self):
        for colour in range(COLOURS):
            for give, keep in self.gives(colour):
                give.wait_recv()
                give.wait_send()
                keep.wait()
            self.each_step(lambda step: self.plane_copy(colour, step).wait_send())
            for direction in range(TWO):
                far, own, fed, _ = self.ring(colour, direction)
                for _, copy in far + own + [(None, fed)]:
                    copy.wait_send()
        for turn in range(SIDE):
            for copy in self.swaps(turn):
                copy.wait_send()


TURNS = (TWO, ONE, THREE, ZERO)


def last_kernel(scale, table, n_mats, *refs):
    n_lhs = ONE + max(lhs for lhs, _ in table)
    lhs_refs, rhs_refs, vec_ref, outs = refs[:n_lhs], refs[n_lhs:n_lhs + n_mats], refs[n_lhs + n_mats], refs[n_lhs + n_mats + ONE:n_lhs + n_mats + THREE]
    sums, lhs_v, rhs_v, load_sem = refs[n_lhs + n_mats + THREE:n_lhs + n_mats + 7]
    rows = sums.shape[THREE]
    scatter = Scatter(scale, [(sums, ZERO, rows), (vec_ref, ZERO, vec_ref.shape[THREE])], outs, refs[n_lhs + n_mats + 7:], resident=True)
    d_model = sums.shape[4]

    def fetch(mat):
        lhs, rhs = lhs_refs[table[mat][ZERO]], rhs_refs[table[mat][ONE]]
        n = lhs.shape[ZERO]
        return [pltpu.make_async_copy(src, dst.at[mat % TWO, pl.ds(ZERO, n), :], load_sem.at[mat % TWO, i]) for i, (src, dst) in enumerate(((lhs, lhs_v), (rhs, rhs_v)))], n

    def make(mat):
        copies, n = fetch(mat)
        for copy in copies:
            copy.wait()
        total = dot_tn(lhs_v[mat % TWO, :n, :], rhs_v[mat % TWO, :n, :])
        z, y = mat // TWO, TWO * (mat % TWO)
        for y_add in range(TWO):
            for x in range(SIDE):
                first = (y_add * SIDE + x) * rows
                sums[z, y + y_add, x] = total[first:first + rows]
        if mat + TWO < n_mats:
            for copy in fetch(mat + TWO)[ZERO]:
                copy.start()

    for mat in range(TWO):
        for copy in fetch(mat)[ZERO]:
            copy.start()
    meet_neighbours(scatter.place)
    vec_swaps = [copy for z in range(SIDE) for copy in scatter.swaps(z, (ONE,))]
    for copy in vec_swaps:
        copy.start()
    for z in range(SIDE):
        for mat in (TWO * z, TWO * z + ONE):
            make(mat)
        if z == ZERO:
            for copy in vec_swaps:
                copy.wait_recv()
            for colour in range(COLOURS):
                for plane in range(SIDE):
                    scatter.add_into(scatter.acc.at[colour, plane, :, :, scatter.rows_of(ONE), :], [vec_ref.at[plane, :, :, :, scatter.columns(scatter.core, colour)]])
        else:
            scatter.absorb_plane(z - ONE)
        for copy in scatter.swaps(z, (ZERO,)):
            copy.start()
    scatter.absorb_plane(SIDE - ONE)
    scatter.relay()
    scatter.settle()
    scatter.finish()
    scatter.end()


def as_torus(rows):
    return rows.reshape(SIDE, SIDE, SIDE, rows.shape[ZERO] // SIDE ** THREE, rows.shape[ONE])


def scatter_products(pairs, g_vec, scale):
    lhs_list = []
    for lhs, _ in pairs:
        if not any(lhs is known for known in lhs_list):
            lhs_list.append(lhs)
    table = tuple((next(i for i, known in enumerate(lhs_list) if known is lhs), i) for i, (lhs, _) in enumerate(pairs))
    d_model = pairs[ZERO][ZERO].shape[ONE]
    n_chips = SIDE ** THREE
    rows = len(pairs) * d_model // n_chips
    vec = as_torus(g_vec)
    heights = [rows, vec.shape[THREE]]
    deepest = max(lhs.shape[ZERO] for lhs in lhs_list)
    anywhere = pl.BlockSpec(memory_space=pl.ANY)
    return pl.pallas_call(
        functools.partial(last_kernel, scale, table, len(pairs)),
        in_specs=[anywhere] * (len(lhs_list) + len(pairs)) + [pl.BlockSpec(memory_space=pltpu.VMEM)], out_specs=[anywhere] * TWO,
        out_shape=[jax.ShapeDtypeStruct((h, d_model), F32) for h in heights],
        scratch_shapes=[pltpu.VMEM((SIDE, SIDE, SIDE, rows, d_model), F32), pltpu.VMEM((TWO, deepest, d_model), BF16), pltpu.VMEM((TWO, deepest, d_model), BF16),
                        pltpu.SemaphoreType.DMA((TWO, TWO))] + Scatter.scratch_shapes(heights, resident=True),
        compiler_params=pltpu.CompilerParams(collective_id=ONE, has_side_effects=True, vmem_limit_bytes=VMEM_BYTES),
        cost_estimate=pl.CostEstimate(flops=TWO * len(pairs) * d_model * d_model * deepest, bytes_accessed=8 * d_model * d_model * len(pairs), transcendentals=ZERO),
        name='scatter_products',
    )(*lhs_list, *[rhs for _, rhs in pairs], vec)


def ag_kernel(attn_ref, ffn_ref, vec_ref, oattn_ref, planes_ref, vec_out, attn_v, send_sem, recv_sem, load_sem):
    core, chip, place = lax.axis_index('dp'), lax.axis_index('fsdp'), torus_place()
    sibling = (ONE - core, chip)
    rows, width = attn_ref.shape
    band = rows // (TWO * COLOURS)
    vec_high = vec_ref.shape[ZERO]
    n_plane = SIDE * SIDE
    colours = range(COLOURS)

    def remote(i, src, dst, device):
        return pltpu.make_async_remote_copy(src_ref=src, dst_ref=dst, send_sem=send_sem.at[i], recv_sem=recv_sem.at[i], device_id=device, device_id_type=MESH_ID)

    def band_rows(colour):
        return pl.ds(pl.multiple_of((core * COLOURS + colour) * band, band), band)

    def plane_dims(colour):
        return sorted(DIM_ORDER[colour][:TWO])

    streams = [(kind, colour) for kind in ('attn', 'ffn') for colour in colours] + [('vec', ONE)]

    def here(kind, colour):
        if kind == 'attn':
            return attn_ref.at[band_rows(colour), :], attn_v.at[place[ZERO], place[ONE], place[TWO], band_rows(colour), :]
        if kind == 'ffn':
            a, b = plane_dims(colour)
            return ffn_ref.at[band_rows(colour), :], planes_ref.at[colour, place[a], place[b]]
        return vec_ref, vec_out.at[place[ZERO], place[ONE], place[TWO]]

    def plane_copy(n, step):
        kind, colour = streams[n]
        moved = list(place)
        for d, s in zip(plane_dims(colour), (step // SIDE, lax.rem(step, SIDE))):
            moved[d] = lax.rem(place[d] + s, SIDE)
        src, dst = here(kind, colour)
        return remote(n * n_plane + step, src, dst, (core, (moved[ZERO] * SIDE + moved[ONE]) * SIDE + moved[TWO]))

    def each_step(body):
        def run(step, _):
            body(step)
            return ZERO

        lax.fori_loop(ONE, n_plane, run, ZERO)

    def plane_at(colour, shift, half=None):
        last = DIM_ORDER[colour][TWO]
        where = [slice(None)] * THREE
        where[last] = lax.rem(place[last] + shift + SIDE, SIDE)
        if half is not None:
            where[min(plane_dims(colour))] = pl.ds(TWO * half, TWO)
        return tuple(where)

    def whole(kind, colour, at):
        return attn_v.at[at + (band_rows(colour), slice(None))] if kind == 'attn' else vec_out.at[at]

    rounds = [(kind, colour) for kind, colour in streams if kind != 'ffn']
    ring_base = len(streams) * n_plane

    def ring(n, direction):
        kind, colour = rounds[n]
        shift = ONE - TWO * direction
        device = (core, chip_at(place, DIM_ORDER[colour][TWO], shift))
        i = ring_base + (n * TWO + direction) * TWO
        near, far = whole(kind, colour, plane_at(colour, ZERO)), whole(kind, colour, plane_at(colour, -shift, direction))
        return remote(i, near, near, device), remote(i + ONE, far, far, device)

    share_base = ring_base + 4 * len(rounds)

    def share(colour, which):
        at = (plane_at(colour, ZERO), plane_at(colour, -ONE), plane_at(colour, ONE), plane_at(colour, TWO, ZERO), plane_at(colour, TWO, ONE))[which] + (band_rows(colour), slice(None))
        i = colour * 5 + which
        return remote(share_base + i, attn_v.at[at], oattn_ref.at[at], sibling), pltpu.make_async_copy(attn_v.at[at], oattn_ref.at[at], load_sem.at[i])

    def publish(colour, pieces):
        for which in pieces:
            for copy in share(colour, which):
                copy.start()

    for kind, colour in streams:
        src, dst = here(kind, colour)
        dst[ALL] = src[ALL]
    meet_neighbours(place, PLANES)
    order = [ZERO, ONE, TWO, 6, THREE, 4, 5]
    for n in order:
        each_step(lambda step: plane_copy(n, step).start())
    for n, (kind, colour) in enumerate(rounds):
        which = streams.index((kind, colour))
        each_step(lambda step: plane_copy(which, step).wait_recv())
        for direction in range(TWO):
            ring(n, direction)[ZERO].start()
    for colour in colours:
        publish(colour, (ZERO,))
    for n in range(THREE, 6):
        each_step(lambda step: plane_copy(n, step).wait_recv())
    for n, (kind, colour) in enumerate(rounds):
        for direction in range(TWO):
            near, far = ring(n, direction)
            near.wait_recv()
            far.start()
        if kind == 'attn':
            publish(colour, (ONE, TWO))
    for n, (kind, colour) in enumerate(rounds):
        for direction in range(TWO):
            ring(n, direction)[ONE].wait_recv()
        if kind == 'attn':
            publish(colour, (THREE, 4))
    for colour in colours:
        for which in range(5):
            give, keep = share(colour, which)
            give.wait_recv()
            give.wait_send()
            keep.wait()
    for n in range(len(rounds)):
        for direction in range(TWO):
            for copy in ring(n, direction):
                copy.wait_send()
    for n in order:
        each_step(lambda step: plane_copy(n, step).wait_send())


def gather_params(attn_w, ffn_w, vec_rows):
    rows, width = attn_w.shape
    full = (SIDE, SIDE, SIDE, rows, width)
    n_copies = 7 * SIDE * SIDE + 4 * 4 + COLOURS * 5
    vmem = pl.BlockSpec(memory_space=pltpu.VMEM)
    return pl.pallas_call(
        ag_kernel,
        in_specs=[vmem] * THREE, out_specs=[pl.BlockSpec(memory_space=pl.ANY), vmem, vmem],
        out_shape=[jax.ShapeDtypeStruct(full, BF16), jax.ShapeDtypeStruct((COLOURS, SIDE, SIDE, rows // (TWO * COLOURS), width), BF16),
                   jax.ShapeDtypeStruct((SIDE, SIDE, SIDE) + vec_rows.shape, F32)],
        scratch_shapes=[pltpu.VMEM(full, BF16), pltpu.SemaphoreType.DMA((n_copies,)), pltpu.SemaphoreType.DMA((n_copies,)), pltpu.SemaphoreType.DMA((COLOURS * 5,))],
        compiler_params=pltpu.CompilerParams(collective_id=TWO, has_side_effects=True, vmem_limit_bytes=VMEM_BYTES),
        cost_estimate=pl.CostEstimate(flops=10 ** 9, bytes_accessed=4 * rows * width * SIDE ** THREE, transcendentals=ZERO),
        name='gather_params',
    )(attn_w, ffn_w, vec_rows)


class LastPhase:
    def __init__(self, planes, out, near, far, send_sem, recv_sem, load_sem):
        self.planes, self.out, self.near, self.far = planes, out, near, far
        self.send_sem, self.recv_sem, self.load_sem = send_sem, recv_sem, load_sem
        self.core, self.chip, self.place = lax.axis_index('dp'), lax.axis_index('fsdp'), torus_place()
        self.band = planes.shape[THREE]

    @staticmethod
    def scratch_shapes(planes):
        colours, side, _, band, width = planes.shape
        sems = [pltpu.SemaphoreType.DMA((9 * COLOURS,)), pltpu.SemaphoreType.DMA((9 * COLOURS,)), pltpu.SemaphoreType.DMA((5 * COLOURS,))]
        return [pltpu.VMEM((colours, TWO, side, side, band, width), BF16), pltpu.VMEM((colours, TWO, side // TWO, side, band, width), BF16)] + sems

    def remote(self, i, src, dst, device):
        return pltpu.make_async_remote_copy(src_ref=src, dst_ref=dst, send_sem=self.send_sem.at[i], recv_sem=self.recv_sem.at[i], device_id=device, device_id_type=MESH_ID)

    def ring(self, colour, direction):
        device = (self.core, chip_at(self.place, DIM_ORDER[colour][TWO], ONE - TWO * direction))
        i = 9 * colour + TWO * direction
        got = self.near.at[colour, direction]
        return (self.remote(i, self.planes.at[colour], got, device),
                self.remote(i + ONE, got.at[pl.ds(TWO * direction, TWO)], self.far.at[colour, direction], device))

    def shares(self, colour):
        last = DIM_ORDER[colour][TWO]
        rows = pl.ds(pl.multiple_of((self.core * COLOURS + colour) * self.band, self.band), self.band)
        views = [(self.planes.at[colour], ZERO, None)]
        views += [(self.near.at[colour, direction], TWO * direction - ONE, None) for direction in range(TWO)]
        views += [(self.far.at[colour, direction], TWO, direction) for direction in range(TWO)]
        out = []
        for n, (src, shift, half) in enumerate(views):
            where = [slice(None)] * THREE
            where[last] = lax.rem(self.place[last] + shift + SIDE, SIDE)
            if half is not None:
                where[min(d for d in range(THREE) if d != last)] = pl.ds(TWO * half, TWO)
            dst = self.out.at[tuple(where) + (rows, slice(None))]
            out.append((self.remote(9 * colour + 4 + n, src, dst, (ONE - self.core, self.chip)), pltpu.make_async_copy(src, dst, self.load_sem.at[5 * colour + n])))
        return out

    def share(self, colour, which):
        for n in which:
            give, keep = self.shares(colour)[n]
            give.start()
            keep.start()

    def begin(self):
        for colour in range(COLOURS):
            for direction in range(TWO):
                self.ring(colour, direction)[ZERO].start()
        for colour in range(COLOURS):
            self.share(colour, (ZERO,))

    def pass_on(self):
        for colour in range(COLOURS):
            for direction in range(TWO):
                near, far = self.ring(colour, direction)
                near.wait_recv()
                far.start()
            self.share(colour, (ONE, TWO))

    def complete(self):
        for colour in range(COLOURS):
            for direction in range(TWO):
                self.ring(colour, direction)[ONE].wait_recv()
            self.share(colour, (THREE, 4))

    def end(self):
        for colour in range(COLOURS):
            for give, keep in self.shares(colour):
                give.wait_recv()
                give.wait_send()
                keep.wait()
            for direction in range(TWO):
                for copy in self.ring(colour, direction):
                    copy.wait_send()


def dot(lhs, rhs, contract=((ONE,), (ZERO,))):
    return lax.dot_general(lhs, rhs, (contract, ((), ())), preferred_element_type=F32)


def dot_nt(lhs, rhs):
    return dot(lhs, rhs, ((ONE,), (ONE,)))


def dot_tn(lhs, rhs):
    return dot(lhs, rhs, ((ZERO,), (ZERO,)))


def norm_rows(resid, gain, shift):
    mean = jnp.mean(resid, axis=-ONE, keepdims=True)
    centred = resid - mean
    inv_std = lax.rsqrt(jnp.mean(centred * centred, axis=-ONE, keepdims=True) + LN_EPS)
    normed = centred * inv_std
    return (normed * gain + shift).astype(BF16), normed, inv_std


def norm_rows_bwd(d_out, normed, inv_std, gain):
    d_norm = d_out * gain
    return inv_std * (d_norm - jnp.mean(d_norm, axis=-ONE, keepdims=True) - normed * jnp.mean(d_norm * normed, axis=-ONE, keepdims=True))


def col_sum(values):
    return jnp.sum(values, axis=ZERO, keepdims=True)


def lane_row(head, dtype=BF16):
    lane = lax.broadcasted_iota(jnp.int32, (ONE, PAIR), ONE)
    return jnp.where((lane >= HEAD_DIM * head) & (lane < HEAD_DIM * (head + ONE)), 1.0, 0.0).astype(dtype)


def spare_lane(head):
    lane = lax.broadcasted_iota(jnp.int32, (ONE, PAIR), ONE)
    return jnp.where(lane == HEAD_DIM * (ONE - head), 1.0, 0.0)


def mask_fill(n_rows, n_valid):
    row = lax.broadcasted_iota(jnp.int32, (n_rows, PAIR), ZERO)
    return jnp.where(row >= n_valid, MASK_FILL, 0.0)


def head_masks(pair_q, pair_k, head, fill):
    q_f = pair_q * lane_row(head) + spare_lane(head).astype(BF16)
    k_f = pair_k * lane_row(head) + (fill * spare_lane(head)).astype(BF16)
    return q_f, k_f


def half_only(pair, head):
    return pair * lane_row(head)


def join_halves(first, second):
    lane = lax.broadcasted_iota(jnp.int32, first.shape, ONE)
    return jnp.where(lane < HEAD_DIM, first, second)


def score_blocks(n_heads, n_q, n_k, causal, step):
    if not causal:
        return [(head, ZERO, n_q, n_k) for head in range(n_heads)]
    return [(head, first, step, first + step) for head in range(n_heads) for first in range(ZERO, n_q, step)]


def scores_t(q_f, k_f, causal, first):
    s_t = dot_nt(k_f, q_f)
    if causal:
        key_i = lax.broadcasted_iota(jnp.int32, s_t.shape, ZERO)
        qry_i = lax.broadcasted_iota(jnp.int32, s_t.shape, ONE) + first
        s_t = jnp.where(key_i <= qry_i, s_t, MASK_FILL)
    return s_t


def pair_of(group, head):
    return group[:, head // TWO * PAIR:(head // TWO + ONE) * PAIR]


def masked_pairs(q_g, k_g, n_valid):
    fill = mask_fill(k_g.shape[ZERO], n_valid)
    cache = {}

    def get(head):
        if head not in cache:
            cache[head] = head_masks(pair_of(q_g, head), pair_of(k_g, head), head % TWO, fill)
        return cache[head]

    return get


def stack_heads(parts, n_heads):
    return jnp.concatenate([jnp.concatenate(parts[head], axis=ONE) for head in range(n_heads)], axis=ZERO)


def run_ahead(blocks, produce, transform, consume, delay):
    ahead = produce(blocks[ZERO])
    waiting = []
    for i, block in enumerate(blocks):
        now = ahead
        if i + ONE < len(blocks):
            ahead = produce(blocks[i + ONE])
        waiting.append((block, transform(block, now)))
        if len(waiting) > delay:
            consume(*waiting.pop(ZERO))
    for item in waiting:
        consume(*item)


def attend_group(q_g, k_g, v_g, n_valid, causal, lse_ref):
    n_heads = GROUP // HEAD_DIM
    o_parts = [[] for _ in range(n_heads)]
    v_t = v_g.T
    masked = masked_pairs(q_g, k_g, n_valid)

    def produce(block):
        head, first, n_q, n_k = block
        q_f, k_f = masked(head)
        return scores_t(q_f[first:first + n_q], k_f[:n_k], causal, first)

    def transform(block, s_t):
        head, first, n_q, n_k = block
        top = jnp.max(s_t, axis=ZERO, keepdims=True)
        e_t = jnp.exp(s_t - top)
        total = jnp.sum(e_t, axis=ZERO, keepdims=True)
        lse_ref[ZERO, ZERO, head:head + ONE, first:first + n_q] = top + jnp.log(total)
        return (e_t * (1.0 / total)).astype(BF16)

    def consume(block, p_t):
        head, first, n_q, n_k = block
        o_parts[head].append(dot(v_t[HEAD_DIM * head:HEAD_DIM * (head + ONE), :n_k], p_t))

    run_ahead(score_blocks(n_heads, q_g.shape[ZERO], k_g.shape[ZERO], causal, 128), produce, transform, consume, TWO)
    return stack_heads(o_parts, n_heads).T.astype(BF16)


def attend_group_bwd(d_o, q_g, k_g, v_g, n_valid, causal, lse_ref, between=None):
    n_heads = GROUP // HEAD_DIM
    k_t = k_g.T
    dq_t, dk_h, dv_h = [[] for _ in range(n_heads)], [None] * n_heads, [None] * n_heads
    masked = masked_pairs(q_g, k_g, n_valid)
    v_half = {}

    def produce(block):
        head, first, n_q, n_k = block
        q_f, k_f = masked(head)
        if head not in v_half:
            v_half[head] = half_only(pair_of(v_g, head), head % TWO)
        rows = slice(first, first + n_q)
        return scores_t(q_f[rows], k_f[:n_k], causal, first), dot_nt(v_half[head][:n_k], pair_of(d_o, head)[rows])

    def transform(block, products):
        head, first, n_q, n_k = block
        s_t, dp_t = products
        p_t = jnp.exp(s_t - lse_ref[ZERO, ZERO, head:head + ONE, first:first + n_q])
        weighted = p_t * dp_t
        return p_t.astype(BF16), (weighted - p_t * jnp.sum(weighted, axis=ZERO, keepdims=True)).astype(BF16)

    def grow(old, new):
        if old is None:
            return new
        n_old = old.shape[ZERO]
        return old + new if n_old == new.shape[ZERO] else jnp.concatenate([old + new[:n_old], new[n_old:]], axis=ZERO)

    def consume(block, operands):
        head, first, n_q, n_k = block
        p_b, ds_t = operands
        rows = slice(first, first + n_q)
        dv_h[head] = grow(dv_h[head], dot(p_b, pair_of(d_o, head)[rows]))
        dk_h[head] = grow(dk_h[head], dot(ds_t, pair_of(q_g, head)[rows]))
        dq_t[head].append(dot(k_t[HEAD_DIM * head:HEAD_DIM * (head + ONE), :n_k], ds_t))

    blocks = score_blocks(n_heads, q_g.shape[ZERO], k_g.shape[ZERO], causal, 256)
    if between is None:
        run_ahead(blocks, produce, transform, consume, ZERO)
    else:
        n_first = len(blocks) // TWO
        run_ahead(blocks[:n_first], produce, transform, consume, ZERO)
        between()
        run_ahead(blocks[n_first:], produce, transform, consume, ZERO)
    join = lambda parts: jnp.concatenate([join_halves(parts[h], parts[h + ONE]) for h in range(ZERO, n_heads, TWO)], axis=ONE)
    return stack_heads(dq_t, n_heads).T * 0.125, join(dk_h), join(dv_h)


def attn_fwd_kernel(causal, slots, guest, lens_ref, x_ref, kv_ref, wq_ref, wk_ref, wv_ref, w_all, bias_ref, rows_ref,
                    q_ref, k_ref, v_ref, o_ref, lse_ref, h_ref, normed_ref, inv_ref, o_all, wo_v, load_sem):
    q_row, k_row, v_row, o_row, gain_row, o_mat = slots
    sample, group = pl.program_id(ZERO), pl.program_id(ONE)
    d_model = wo_v.shape[ZERO]
    fetch = pltpu.make_async_copy(w_all.at[pl.ds(o_mat * d_model, d_model), :], wo_v, load_sem)

    @pl.when((sample == ZERO) & (group == ZERO))
    def _():
        fetch.start()

    turn = sample * pl.num_programs(ONE) + group
    if guest is not None:
        for where, steps in ((ZERO, (lambda: meet_neighbours(guest.place, RINGS), guest.begin)), (THREE, (guest.pass_on,)), (5, (guest.complete,))):
            @pl.when(turn == where)
            def _():
                for step in steps:
                    step()

    x_b, kv_b = x_ref[ALL], kv_ref[ALL]
    q_g = ((dot(x_b, wq_ref[ALL]) + bias_ref[q_row:q_row + ONE, :]) * 0.125).astype(BF16)
    k_g = (dot(kv_b, wk_ref[ALL]) + bias_ref[k_row:k_row + ONE, :]).astype(BF16)
    v_g = (dot(kv_b, wv_ref[ALL]) + bias_ref[v_row:v_row + ONE, :]).astype(BF16)
    q_ref[ALL], k_ref[ALL], v_ref[ALL] = q_g, k_g, v_g
    o_g = attend_group(q_g, k_g, v_g, lens_ref[sample], causal, lse_ref)
    o_ref[ALL] = o_g
    o_all[:, pl.ds(pl.multiple_of(group * GROUP, GROUP), GROUP)] = o_g

    @pl.when((sample == ZERO) & (group == pl.num_programs(ONE) - ONE))
    def _():
        fetch.wait()

    @pl.when(group == pl.num_programs(ONE) - ONE)
    def _():
        resid = x_ref[ALL].astype(F32) + dot(o_all[ALL], wo_v[ALL]) + rows_ref[o_row:o_row + ONE, :]
        h_out, normed, inv_std = norm_rows(resid, rows_ref[gain_row:gain_row + ONE, :], rows_ref[gain_row + ONE:gain_row + TWO, :])
        h_ref[ALL], normed_ref[ALL], inv_ref[ALL] = h_out, normed, inv_std

    if guest is not None:
        @pl.when(turn == pl.num_programs(ZERO) * pl.num_programs(ONE) - ONE)
        def _():
            guest.end()


def attn_forward(x, kv, lens, attn_full, bias_rows, mats, slots, causal, planes=None, full_rows=None):
    d_model = x.shape[-ONE]
    n_batch = lens.shape[ZERO]
    n_q, n_k = x.shape[ZERO] // n_batch, kv.shape[ZERO] // n_batch
    n_groups = d_model // GROUP
    col = lambda mat: pl.BlockSpec((d_model, GROUP), lambda b, g: (mat, g))
    q_blk = pl.BlockSpec((n_q, GROUP), lambda b, g: (b, g))
    k_blk = pl.BlockSpec((n_k, GROUP), lambda b, g: (b, g))
    tok = lambda n: pl.BlockSpec((n, d_model), lambda b, g: (b, ZERO))
    n_heads_g = GROUP // HEAD_DIM
    out_shape = (
        jax.ShapeDtypeStruct(x.shape, BF16), jax.ShapeDtypeStruct(kv.shape, BF16), jax.ShapeDtypeStruct(kv.shape, BF16),
        jax.ShapeDtypeStruct(x.shape, BF16), jax.ShapeDtypeStruct((n_batch, n_groups, n_heads_g, n_q), F32),
        jax.ShapeDtypeStruct(x.shape, BF16), jax.ShapeDtypeStruct(x.shape, F32), jax.ShapeDtypeStruct((x.shape[ZERO], ONE), F32))
    kernel = functools.partial(attn_fwd_kernel, causal, slots + (mats[THREE],))
    in_specs = [pl.BlockSpec(memory_space=pltpu.SMEM), tok(n_q), tok(n_k), col(mats[ZERO]), col(mats[ONE]), col(mats[TWO]), pl.BlockSpec(memory_space=pl.ANY),
                pl.BlockSpec((bias_rows.shape[ZERO], GROUP), lambda b, g: (ZERO, g)), pl.BlockSpec(bias_rows.shape, lambda b, g: (ZERO, ZERO))]
    out_specs = [q_blk, k_blk, k_blk, q_blk, pl.BlockSpec((ONE, ONE, n_heads_g, n_q), lambda b, g: (b, g, ZERO, ZERO)),
                 tok(n_q), tok(n_q), pl.BlockSpec((n_q, ONE), lambda b, g: (b, ZERO))]
    scratch = [pltpu.VMEM((n_q, d_model), BF16), pltpu.VMEM((d_model, d_model), BF16), pltpu.SemaphoreType.DMA]
    args = [lens, x, kv, attn_full, attn_full, attn_full, attn_full, bias_rows, bias_rows]
    params = dict(vmem_limit_bytes=VMEM_BYTES, dimension_semantics=('arbitrary', 'arbitrary'))
    if planes is None:
        body = functools.partial(kernel, None)
    else:
        n_in, n_out, n_own = len(args), len(out_specs), len(scratch)

        def body(*refs):
            ins, held, outs, whole, rest = refs[:n_in], refs[n_in], refs[n_in + ONE:n_in + ONE + n_out], refs[n_in + ONE + n_out], refs[n_in + TWO + n_out:]
            kernel(LastPhase(held, whole, *rest[n_own:]), *ins, *outs, *rest[:n_own])

        in_specs.append(pl.BlockSpec(memory_space=pltpu.VMEM))
        args.append(planes)
        out_specs.append(pl.BlockSpec(memory_space=pl.ANY))
        out_shape += (jax.ShapeDtypeStruct((SIDE, SIDE, SIDE, full_rows // SIDE ** THREE, d_model), BF16),)
        scratch += LastPhase.scratch_shapes(planes)
        params |= dict(collective_id=5, has_side_effects=True)
    return pl.pallas_call(
        body, grid=(n_batch, n_groups), in_specs=in_specs, out_specs=out_specs, out_shape=out_shape, scratch_shapes=scratch,
        compiler_params=pltpu.CompilerParams(**params),
        cost_estimate=pl.CostEstimate(flops=TWO * d_model * d_model * (TWO * x.shape[ZERO] + TWO * kv.shape[ZERO]) + 16 * x.shape[ZERO] * n_k * d_model, bytes_accessed=20 * x.shape[ZERO] * d_model, transcendentals=ZERO),
        name='attn_fwd',
    )(*args)


def attn_bwd_kernel(causal, gain_row, mats, guest, lens_ref, dres_ref, wo_ref, w_all, q_ref, k_ref, v_ref, lse_ref,
                    rows_ref, normed_ref, inv_ref, dq_ref, dk_ref, dv_ref, dx_ref, dkv_ref, sums_ref, tail_ref, d_all, dk_all, dv_all, w_v, load_sem):
    sample, group = pl.program_id(ZERO), pl.program_id(ONE)
    d_model = w_v.shape[ONE]
    fetches = [pltpu.make_async_copy(w_all.at[pl.ds(mat * d_model, d_model), :], w_v.at[i], load_sem.at[i]) for i, mat in enumerate(mats[:THREE])]

    @pl.when((sample == ZERO) & (group == ZERO))
    def _():
        for fetch in fetches:
            fetch.start()

    turn = sample * pl.num_programs(ONE) + group
    if guest is not None:
        guest(ZERO, TWO * turn)
    d_o = dot_nt(dres_ref[ALL].astype(BF16), wo_ref[ALL]).astype(BF16)
    between = None if guest is None else functools.partial(guest, ONE, TWO * turn + ONE)
    dq, dk, dv = attend_group_bwd(d_o, q_ref[ALL], k_ref[ALL], v_ref[ALL], lens_ref[sample], causal, lse_ref, between)
    sums_ref[ZERO, ZERO:ONE, :] = col_sum(dq)
    sums_ref[ZERO, ONE:TWO, :] = col_sum(dk)
    sums_ref[ZERO, TWO:THREE, :] = col_sum(dv)
    cols = pl.ds(pl.multiple_of(group * GROUP, GROUP), GROUP)
    for full, out, value in ((d_all, dq_ref, dq), (dk_all, dk_ref, dk), (dv_all, dv_ref, dv)):
        rounded = value.astype(BF16)
        out[ALL] = rounded
        full[:, cols] = rounded

    @pl.when((sample == ZERO) & (group == pl.num_programs(ONE) - ONE))
    def _():
        for fetch in fetches:
            fetch.wait()

    @pl.when(group == pl.num_programs(ONE) - ONE)
    def _():
        d_kv = dot_nt(dk_all[ALL], w_v[ONE]) + dot_nt(dv_all[ALL], w_v[TWO])
        d_h = dres_ref[ALL] + dot_nt(d_all[ALL], w_v[ZERO])
        if causal:
            dx_ref[ALL] = (d_h + d_kv).astype(BF16)
            tail_ref[ALL] = jnp.zeros_like(tail_ref)
        else:
            dkv_ref[ALL] = d_kv.astype(BF16)
            normed = normed_ref[ALL]
            d_resid = norm_rows_bwd(d_h, normed, inv_ref[ALL], rows_ref[gain_row:gain_row + ONE, :])
            dx_ref[ALL] = d_resid
            tail_ref[ZERO, ZERO:ONE, :] = col_sum(d_resid)
            tail_ref[ZERO, ONE:TWO, :] = col_sum(d_h * normed)
            tail_ref[ZERO, TWO:THREE, :] = col_sum(d_h)

    if guest is not None:
        guest(TWO, TWO * turn + TWO)


def scatter_guest(scatter, plans, parity, position):
    steps = dict(relay=scatter.relay, settle=scatter.settle, finish=scatter.finish, end=scatter.end)
    steps |= {turn: functools.partial(scatter.absorb, turn) for turn in range(SIDE)}
    plan = {ZERO: [functools.partial(meet_neighbours, scatter.place), scatter.begin]} | {where: [steps[name] for name in names] for where, names in plans.items()}
    for where, steps in plan.items():
        if where % TWO == parity % TWO and (where == 12) == (parity == TWO):
            @pl.when(position == where)
            def _():
                for step in steps:
                    step()


def attn_backward(dres, q, k, v, lse, lens, attn_full, bias_rows, mats, causal, g_rows, part, plans, scale, gain_row=ZERO, normed=None, inv_std=None):
    d_model = q.shape[-ONE]
    n_batch = lens.shape[ZERO]
    n_q, n_k = q.shape[ZERO] // n_batch, k.shape[ZERO] // n_batch
    n_groups = d_model // GROUP
    row = lambda mat: pl.BlockSpec((GROUP, d_model), lambda b, g: (mat * n_groups + g, ZERO))
    q_blk = pl.BlockSpec((n_q, GROUP), lambda b, g: (b, g))
    k_blk = pl.BlockSpec((n_k, GROUP), lambda b, g: (b, g))
    tok = lambda n: pl.BlockSpec((n, d_model), lambda b, g: (b, ZERO))
    n_heads_g = GROUP // HEAD_DIM
    whole_rows = pl.BlockSpec(bias_rows.shape, lambda b, g: (ZERO, ZERO))
    kernel = functools.partial(attn_bwd_kernel, causal, gain_row, mats)
    params = dict(vmem_limit_bytes=VMEM_BYTES, dimension_semantics=('arbitrary', 'arbitrary'))
    in_specs = [pl.BlockSpec(memory_space=pltpu.SMEM), tok(n_q), row(mats[THREE]), pl.BlockSpec(memory_space=pl.ANY), q_blk, k_blk, k_blk,
                pl.BlockSpec((ONE, ONE, n_heads_g, n_q), lambda b, g: (b, g, ZERO, ZERO)), whole_rows]
    args = [lens, dres, attn_full, attn_full, q, k, v, lse, bias_rows]
    sums_blk = pl.BlockSpec((ONE, 8, GROUP), lambda b, g: (b, ZERO, g))
    tail_blk = pl.BlockSpec((ONE, 8, d_model), lambda b, g: (b, ZERO, ZERO))
    tail_shape = jax.ShapeDtypeStruct((n_batch, 8, d_model), F32)
    out_shape = [jax.ShapeDtypeStruct(q.shape, BF16), jax.ShapeDtypeStruct(k.shape, BF16), jax.ShapeDtypeStruct(k.shape, BF16),
                 jax.ShapeDtypeStruct(q.shape, BF16 if causal else F32)]
    out_specs = [q_blk, k_blk, k_blk, tok(n_q)]
    own = [pltpu.VMEM((n_q, d_model), BF16), pltpu.VMEM((n_k, d_model), BF16), pltpu.VMEM((n_k, d_model), BF16),
           pltpu.VMEM((THREE, d_model, d_model), BF16), pltpu.SemaphoreType.DMA((THREE,))]
    if not causal:
        in_specs += [tok(n_q), pl.BlockSpec((n_q, ONE), lambda b, g: (b, ZERO))]
        args += [normed, inv_std]
        out_shape.append(jax.ShapeDtypeStruct(k.shape, BF16))
        out_specs.append(tok(n_k))
    out_shape += [tail_shape, tail_shape]
    out_specs += [sums_blk, tail_blk]
    n_in, n_out, n_own = len(args), len(out_shape), len(own)
    first_row, n_rows = part

    def body(*refs):
        ins, source, outs, total, rest = refs[:n_in], refs[n_in], refs[n_in + ONE:n_in + ONE + n_out], refs[n_in + ONE + n_out], refs[n_in + TWO + n_out:]
        scatter = Scatter(scale, [(source, first_row, n_rows)], [total], rest[n_own:])
        if causal:
            ins, outs = ins + (None, None), outs[:4] + (None,) + outs[4:]
        kernel(functools.partial(scatter_guest, scatter, plans), *ins, *outs, *rest[:n_own])

    anywhere = pl.BlockSpec(memory_space=pl.ANY)
    in_specs.append(anywhere)
    args.append(as_torus(g_rows))
    out_specs.append(anywhere)
    out_shape.append(jax.ShapeDtypeStruct((n_rows, d_model), F32))
    scratch = own + Scatter.scratch_shapes([n_rows])
    params = dict(collective_id=THREE + causal, has_side_effects=True, vmem_limit_bytes=63 * 1024 * 1024, dimension_semantics=('arbitrary', 'arbitrary'))
    return pl.pallas_call(
        body, grid=(n_batch, n_groups), in_specs=in_specs, out_specs=out_specs, out_shape=out_shape, scratch_shapes=scratch,
        compiler_params=pltpu.CompilerParams(**params),
        cost_estimate=pl.CostEstimate(flops=TWO * d_model * d_model * (TWO * q.shape[ZERO] + TWO * k.shape[ZERO]) + 40 * q.shape[ZERO] * n_k * d_model, bytes_accessed=20 * q.shape[ZERO] * d_model, transcendentals=ZERO),
        name='attn_bwd',
    )(*args)


def ffn_kernel(n_blocks, h_ref, dy_ref, up_ref, down_ref, rows_ref, bias_ref, normed_ref, inv_ref,
               y_ref, grad_ref, dres2_ref, tail_ref, upsum_ref, gelu_all, dup_all, dres3_all, h_all):
    step = pl.program_id(ZERO)
    block, d_model = h_ref.shape
    n_square = gelu_all.shape[ONE] // d_model

    @pl.when(step < n_blocks)
    def _():
        rows = pl.ds(pl.multiple_of(step * block, block), block)
        h_b = h_ref[ALL]
        h_all[rows, :] = h_b
        up = dot_nt(h_b, up_ref[ALL]) + bias_ref[ALL]
        cdf = 0.5 * (1.0 + lax.erf(up * 0.7071067811865476))
        gelu = (up * cdf).astype(BF16)
        slope = cdf + up * (0.3989422804014327 * jnp.exp(-0.5 * up * up))
        gelu_all[rows, :] = gelu
        resid = h_b.astype(F32) + dot(gelu, down_ref[ALL]) + rows_ref[8:9, :]
        y_b, normed3, inv3 = norm_rows(resid, rows_ref[13:14, :], rows_ref[14:15, :])
        y_ref[ALL] = y_b
        dy = dy_ref[ALL].astype(F32)
        d_res3 = norm_rows_bwd(dy, normed3, inv3, rows_ref[13:14, :])
        d_res3_b = d_res3.astype(BF16)
        dres3_all[rows, :] = d_res3_b
        d_up = dot_nt(d_res3_b, down_ref[ALL]) * slope
        d_up_b = d_up.astype(BF16)
        dup_all[rows, :] = d_up_b
        d_h2 = d_res3 + dot(d_up_b, up_ref[ALL])
        normed2 = normed_ref[ALL]
        d_res2 = norm_rows_bwd(d_h2, normed2, inv_ref[ALL], rows_ref[11:12, :])
        dres2_ref[ALL] = d_res2
        tail = jnp.concatenate([col_sum(d_res2), col_sum(d_res3), col_sum(d_h2 * normed2), col_sum(d_h2), col_sum(dy * normed3), col_sum(dy),
                                jnp.zeros((TWO, dy.shape[ONE]), F32)], axis=ZERO)
        up_sum = col_sum(d_up)

        @pl.when(step == ZERO)
        def _():
            tail_ref[ALL] = tail
            upsum_ref[ALL] = up_sum

        @pl.when(step > ZERO)
        def _():
            tail_ref[ALL] += tail
            upsum_ref[ALL] += up_sum

    square = step - n_blocks
    cols = pl.ds(pl.multiple_of(lax.rem(square + TWO * n_square, n_square) * d_model, d_model), d_model)

    @pl.when((square >= ZERO) & (square < n_square))
    def _():
        grad_ref[ALL] = dot_tn(dup_all[:, cols], h_all[ALL])

    @pl.when(square >= n_square)
    def _():
        grad_ref[ALL] = dot_tn(gelu_all[:, cols], dres3_all[ALL])


def ffn_both(h2, dy, ffn_full, bias_rows, up_bias, normed2, inv2, block=256):
    n_tok, d_model = h2.shape
    ffn_dim = ffn_full.shape[ZERO] // TWO
    n_blocks = n_tok // block
    n_steps = n_blocks + ffn_full.shape[ZERO] // d_model
    at = lambda i: jnp.minimum(i, n_blocks - ONE)
    tok = pl.BlockSpec((block, d_model), lambda i: (at(i), ZERO))
    once = lambda shape, idx: pl.BlockSpec(shape, lambda i: idx, pipeline_mode=pl.Buffered(ONE))
    return pl.pallas_call(
        functools.partial(ffn_kernel, n_blocks), grid=(n_steps,),
        in_specs=[tok, tok, once((ffn_dim, d_model), (ZERO, ZERO)), once((ffn_dim, d_model), (ONE, ZERO)), once(bias_rows.shape, (ZERO, ZERO)), once((ONE, ffn_dim), (ZERO, ZERO)),
                  tok, pl.BlockSpec((block, ONE), lambda i: (at(i), ZERO))],
        out_specs=[tok, pl.BlockSpec((d_model, d_model), lambda i: (jnp.maximum(i - n_blocks, ZERO), ZERO)), tok, pl.BlockSpec((8, d_model), lambda i: (ZERO, ZERO)), pl.BlockSpec((ONE, ffn_dim), lambda i: (ZERO, ZERO))],
        out_shape=[jax.ShapeDtypeStruct(h2.shape, BF16), jax.ShapeDtypeStruct(ffn_full.shape, F32), jax.ShapeDtypeStruct(h2.shape, F32),
                   jax.ShapeDtypeStruct((8, d_model), F32), jax.ShapeDtypeStruct((ONE, ffn_dim), F32)],
        scratch_shapes=[pltpu.VMEM((n_tok, ffn_dim), BF16), pltpu.VMEM((n_tok, ffn_dim), BF16), pltpu.VMEM((n_tok, d_model), BF16), pltpu.VMEM((n_tok, d_model), BF16)],
        compiler_params=pltpu.CompilerParams(vmem_limit_bytes=VMEM_BYTES, dimension_semantics=('arbitrary',)),
        cost_estimate=pl.CostEstimate(flops=12 * n_tok * d_model * ffn_dim, bytes_accessed=30 * n_tok * d_model, transcendentals=ZERO),
        name='ffn_both',
    )(h2, dy, ffn_full, ffn_full, bias_rows, up_bias, normed2, inv2)


CROSS_PLAN = {ONE: (ZERO,), TWO: (ONE,), THREE: (TWO, THREE), 5: ('relay',), 8: ('settle',), 12: ('finish', 'end')}
SELF_PLAN = {ONE: (ZERO, ONE), TWO: (TWO, THREE), 4: ('relay',), 7: ('settle',), 11: ('finish',), 12: ('end',)}


def solution(mesh):
    n_fsdp = mesh.shape['fsdp']
    n_dp = mesh.shape['dp']
    batch_axes = ('dp', 'fsdp')
    act_spec = P(batch_axes, None, None)
    len_spec = P(batch_axes)
    row_spec = P('fsdp', None)
    vec_spec = P('fsdp')

    def device_step(dec_in, enc_out, src_lens, tgt_lens, y_cot, attn_w, ffn_w, vec_params):
        d_model, n_vec = dec_in.shape[TWO], vec_params.shape[ZERO]
        scale = 1.0 / (dec_in.shape[ZERO] * dec_in.shape[ONE] * n_fsdp * n_dp)
        x, enc, dy = (a.reshape(-ONE, d_model) for a in (dec_in, enc_out, y_cot))
        vec_rows = jnp.pad(vec_params.astype(F32), (ZERO, 16 * LANES - n_vec)).reshape(16, LANES)
        attn_tiles, planes, vec_tiles = gather_params(attn_w, ffn_w, vec_rows)
        attn_full = attn_tiles.reshape(-ONE, d_model)
        vec_f = vec_tiles.reshape(n_fsdp, 16, LANES)[:, :TWO].reshape(n_fsdp, TWO * LANES)[:, :n_vec].reshape(-ONE)
        bias_rows = jnp.pad(vec_f[:15 * d_model].reshape(15, d_model), ((ZERO, ONE), (ZERO, ZERO)))
        up_bias = vec_f[15 * d_model:].reshape(ONE, -ONE)
        n_early = 5 * ffn_w.shape[ZERO] // 6
        q1, k1, v1, o1, lse1, h1, normed1, inv1, ffn_tiles = attn_forward(x, x, tgt_lens, attn_full, bias_rows, (ZERO, ONE, TWO, THREE), (ZERO, ONE, TWO, THREE, 9), True, planes, ffn_w.shape[ZERO] * n_fsdp)
        ffn_full = ffn_tiles.reshape(-ONE, d_model)
        q2, k2, v2, o2, lse2, h2, normed2, inv2 = attn_forward(h1, enc, src_lens, attn_full, bias_rows, (4, 5, 6, 7), (4, 5, 6, 7, 11), False)
        y, g_ffn, d_res2, ffn_tail, up_sum = ffn_both(h2, dy, ffn_full, bias_rows, up_bias, normed2, inv2)
        dq2, dk2, dv2, d_res1, d_enc, sums2, tail2, ffn_early = attn_backward(d_res2, q2, k2, v2, lse2, src_lens, attn_full, bias_rows, (4, 5, 6, 7), False, g_ffn, (ZERO, n_early), CROSS_PLAN, scale, 9, normed1, inv1)
        dq1, dk1, dv1, d_x, sums1, _, ffn_late = attn_backward(d_res1, q1, k1, v1, lse1, tgt_lens, attn_full, bias_rows, (ZERO, ONE, TWO, THREE), True, g_ffn, (n_early, ffn_w.shape[ZERO] - n_early), SELF_PLAN, scale)
        s1, s2, t2 = jnp.sum(sums1, axis=ZERO), jnp.sum(sums2, axis=ZERO), jnp.sum(tail2, axis=ZERO)
        g_vec = jnp.concatenate([s1[ZERO:THREE].reshape(-ONE), t2[ZERO], s2[ZERO:THREE].reshape(-ONE), ffn_tail[ZERO], ffn_tail[ONE], t2[ONE], t2[TWO], ffn_tail[TWO], ffn_tail[THREE], ffn_tail[4], ffn_tail[5], up_sum[ZERO]])
        g_rows = jnp.pad(g_vec.reshape(n_fsdp, ONE, n_vec), ((ZERO, ZERO), (ZERO, 7), (ZERO, d_model - n_vec))).reshape(n_fsdp * 8, -ONE)
        pairs = ((x, dq1), (x, dk1), (x, dv1), (o1, d_res1.astype(BF16)), (h1, dq2), (enc, dk2), (enc, dv2), (o2, d_res2.astype(BF16)))
        attn_out, vec_out = scatter_products(pairs, g_rows, scale)
        return y.reshape(dec_in.shape), d_x.reshape(dec_in.shape), d_enc.reshape(enc_out.shape), attn_out, jnp.concatenate([ffn_early, ffn_late], axis=ZERO), vec_out[ZERO, :n_vec]

    return jax.shard_map(device_step, mesh=mesh, in_specs=(act_spec, act_spec, len_spec, len_spec, act_spec, row_spec, row_spec, vec_spec), out_specs=(act_spec, act_spec, act_spec, row_spec, row_spec, vec_spec), check_vma=False)
```

```python
import functools
import jax
import jax.numpy as jnp
from jax import lax
from jax.experimental import pallas as pl
from jax.experimental.pallas import tpu as pltpu
from jax.sharding import PartitionSpec as P

ZERO, ONE, TWO, THREE = range(4)
ALL = ...
HEAD_DIM = 64
LN_EPS = 1e-5
MASK_FILL = -1e30
VMEM_BYTES = 60 * 1024 * 1024
F32 = jnp.float32
BF16 = jnp.bfloat16
GROUP = 256
PAIR = 128


SIDE = 4
LANES = 128
COLOURS = THREE
STAGES = TWO
DIM_ORDER = ((TWO, ONE, ZERO), (ONE, ZERO, TWO), (ZERO, TWO, ONE))
MESH_ID = pl.DeviceIdType.MESH


def torus_place():
    chip = lax.axis_index('fsdp')
    return (chip // (SIDE * SIDE), lax.rem(chip // SIDE, SIDE), lax.rem(chip, SIDE))


def chip_at(place, dim, shift):
    moved = [lax.rem(p + shift + SIDE, SIDE) if d == dim else p for d, p in enumerate(place)]
    return (moved[ZERO] * SIDE + moved[ONE]) * SIDE + moved[TWO]


def meet_neighbours(place):
    barrier = pltpu.get_barrier_semaphore()
    core = lax.axis_index('dp')
    for dim in range(THREE):
        for shift in (ONE, -ONE):
            pl.semaphore_signal(barrier, inc=ONE, device_id=(core, chip_at(place, dim, shift)), device_id_type=MESH_ID)
    pl.semaphore_signal(barrier, inc=ONE, device_id=(ONE - core, lax.axis_index('fsdp')), device_id_type=MESH_ID)
    pl.semaphore_wait(barrier, 7)


class Scatter:
    def __init__(self, scale, sources, outs, scratch, resident=False):
        self.scale, self.outs, self.resident = scale, outs, resident
        self.sources = [(ref, pl.ds(first, n)) for ref, first, n in sources]
        (self.acc, g1, d1, g2, d2, g3, d3, self.send_sem, self.recv_sem, self.load_sem, *stage) = scratch
        self.stage = None if resident else stage[ZERO]
        self.got, self.far = (g1, g2, g3), (d1, d2, d3)
        self.heights = [n for _, _, n in sources]
        self.offsets = [sum(self.heights[:i]) for i in range(len(sources))]
        self.height = sum(self.heights)
        self.n_low = self.heights[ZERO] // TWO
        self.core, self.chip, self.place = lax.axis_index('dp'), lax.axis_index('fsdp'), torus_place()
        self.pieces = [(d, colour) for d in (TWO, ONE, THREE, ZERO) for colour in range(COLOURS)]

    @staticmethod
    def scratch_shapes(heights, resident=False):
        h = sum(heights)
        n_low = heights[ZERO] // TWO
        buf = lambda *shape: pltpu.VMEM((COLOURS,) + shape + (LANES,), F32)
        n = Scatter.n_copies(len(heights))
        return [buf(SIDE, SIDE, SIDE, h), buf(TWO, SIDE, SIDE, h), buf(TWO, TWO, SIDE, h), buf(TWO, SIDE, h), buf(TWO, TWO, h), buf(TWO, h), buf(TWO, max(n_low, h - n_low)),
                pltpu.SemaphoreType.DMA((n,)), pltpu.SemaphoreType.DMA((n,)), pltpu.SemaphoreType.DMA((THREE + COLOURS, len(heights)))] + (
                    [] if resident else [pltpu.VMEM((STAGES, SIDE, SIDE, h, LANES), F32)])

    @staticmethod
    def n_copies(n_parts):
        return 12 * n_parts + COLOURS * 18 + COLOURS * n_parts

    def remote(self, i, src, dst, device):
        return pltpu.make_async_remote_copy(src_ref=src, dst_ref=dst, send_sem=self.send_sem.at[i], recv_sem=self.recv_sem.at[i], device_id=device, device_id_type=MESH_ID)

    def columns(self, of_core, colour):
        return pl.ds(pl.multiple_of((of_core * COLOURS + colour) * LANES, LANES), LANES)

    def slot(self, d, colour):
        dim = DIM_ORDER[colour][ZERO]
        where = [slice(None)] * THREE
        where[dim] = lax.rem(self.place[dim] + d, SIDE)
        return tuple(where)

    def rows_of(self, part):
        return pl.ds(self.offsets[part], self.heights[part])

    def swaps(self, piece):
        d, colour = self.pieces[piece]
        where, cols = self.slot(d, colour), self.columns(ONE - self.core, colour)
        n = len(self.sources)
        return [self.remote(piece * n + i, src.at[where + (rows, cols)], self.acc.at[(colour,) + where + (self.rows_of(i), slice(None))], (ONE - self.core, self.chip))
                for i, (src, rows) in enumerate(self.sources)]

    def loads(self, piece):
        d, colour = self.pieces[piece]
        where, cols = self.slot(d, colour), self.columns(self.core, colour)
        if self.resident:
            return []
        return [pltpu.make_async_copy(src.at[where + (rows, cols)], self.stage.at[piece % STAGES, :, :, self.rows_of(i), :], self.load_sem.at[piece % STAGES, i])
                for i, (src, rows) in enumerate(self.sources)]

    def split_rows(self, half):
        return pl.ds(ZERO, self.n_low) if half == ZERO else pl.ds(self.n_low, self.height - self.n_low)

    def block(self, colour, phase, d, half=None):
        order = DIM_ORDER[colour]
        where = [None, None, None]
        for done in order[:phase]:
            where[done] = self.place[done]
        where[order[phase]] = lax.rem(self.place[order[phase]] + d, SIDE)
        for i, rest in enumerate(sorted(order[phase + ONE:])):
            where[rest] = slice(None) if half is None or i > ZERO else pl.ds(TWO * half, TWO)
        rows = self.split_rows(half) if phase == TWO and half is not None else slice(None)
        return self.acc.at[(colour,) + tuple(where) + (rows, slice(None))]

    def got_half(self, colour, phase, direction, half):
        where = self.split_rows(half) if phase == TWO else pl.ds(TWO * half, TWO)
        return self.got[phase].at[colour, direction, where]

    def far_part(self, colour, phase, direction):
        if phase == TWO:
            return self.far[phase].at[colour, direction, pl.ds(ZERO, self.n_low if direction == ZERO else self.height - self.n_low), :]
        return self.far[phase].at[colour, direction]

    def ring(self, colour, phase, direction):
        shift = ONE - TWO * direction
        device = (self.core, chip_at(self.place, DIM_ORDER[colour][phase], shift))
        i = 12 * len(self.sources) + ((colour * THREE + phase) * TWO + direction) * THREE
        near = shift % SIDE
        return (self.remote(i, self.block(colour, phase, TWO, direction), self.far_part(colour, phase, direction), device),
                self.remote(i + ONE, self.block(colour, phase, near, ONE - direction), self.got_half(colour, phase, direction, ONE - direction), device),
                self.remote(i + TWO, self.block(colour, phase, near, direction), self.got_half(colour, phase, direction, direction), device))

    def gives(self, colour):
        n = len(self.sources)
        base = 12 * n + COLOURS * 18 + colour * n
        done = self.acc.at[colour, self.place[ZERO], self.place[ONE], self.place[TWO]]
        cols = self.columns(self.core, colour)
        pairs = [(done.at[self.rows_of(i), :], out.at[:, cols]) for i, out in enumerate(self.outs)]
        return [(self.remote(base + i, src, dst, (ONE - self.core, self.chip)), pltpu.make_async_copy(src, dst, self.load_sem.at[THREE + colour, i])) for i, (src, dst) in enumerate(pairs)]

    def add_into(self, dst, sources, n_lead):
        def body(i, _):
            idx = (i,) if n_lead == ONE else (i // SIDE, lax.rem(i, SIDE))
            total = dst[idx]
            for src in sources:
                total = total + src[idx]
            dst[idx] = total
            return ZERO

        if n_lead == ZERO:
            total = dst[ALL]
            for src in sources:
                total = total + src[ALL]
            dst[ALL] = total
        else:
            count = dst.shape[ZERO] * (dst.shape[ONE] if n_lead == TWO else ONE)
            lax.fori_loop(ZERO, count, body, ZERO)


    def begin(self):
        for piece in range(STAGES):
            for copy in self.loads(piece):
                copy.start()
        for piece in range(len(self.pieces)):
            for copy in self.swaps(piece):
                copy.start()

    def absorb(self, turn):
        for piece in range(turn * COLOURS, (turn + ONE) * COLOURS):
            d, colour = self.pieces[piece]
            for copy in self.loads(piece):
                copy.wait()
            for copy in self.swaps(piece):
                copy.wait_recv()
            where = self.slot(d, colour)
            if self.resident:
                for i, (src, rows) in enumerate(self.sources):
                    self.add_into(self.acc.at[(colour,) + where + (self.rows_of(i), slice(None))], [src.at[where + (rows, self.columns(self.core, colour))]], TWO)
            else:
                self.add_into(self.acc.at[(colour,) + where], [self.stage.at[piece % STAGES]], TWO)
            if piece + STAGES < len(self.pieces):
                for copy in self.loads(piece + STAGES):
                    copy.start()
            if turn == ZERO:
                for direction in range(TWO):
                    self.ring(colour, ZERO, direction)[ZERO].start()
            elif turn < THREE:
                self.ring(colour, ZERO, turn - ONE)[ONE].start()

    def relay(self, phase):
        for colour in range(COLOURS):
            for direction in range(TWO):
                far, _, fed = self.ring(colour, phase, direction)
                far.wait_recv()
                self.add_into(self.block(colour, phase, (ONE - TWO * direction) % SIDE, direction), [self.far_part(colour, phase, direction)], TWO - phase)
            for direction in range(TWO):
                self.ring(colour, phase, direction)[TWO].start()

    def settle(self, phase):
        for colour in range(COLOURS):
            for direction in range(TWO):
                _, own, fed = self.ring(colour, phase, direction)
                own.wait_recv()
                fed.wait_recv()
            self.add_into(self.block(colour, phase, ZERO), [self.got[phase].at[colour, direction] for direction in range(TWO)], TWO - phase)
            if phase < TWO:
                for kind in range(TWO):
                    for direction in range(TWO):
                        self.ring(colour, phase + ONE, direction)[kind].start()
            else:
                done = self.acc.at[colour, self.place[ZERO], self.place[ONE], self.place[TWO]]
                done[ALL] = done[ALL] * self.scale
                for give, keep in self.gives(colour):
                    keep.start()
                    give.start()

    def end(self):
        for colour in range(COLOURS):
            for give, keep in self.gives(colour):
                give.wait_recv()
                give.wait_send()
                keep.wait()
        for piece in range(len(self.pieces)):
            for copy in self.swaps(piece):
                copy.wait_send()
        for colour in range(COLOURS):
            for phase in range(THREE):
                for direction in range(TWO):
                    for copy in self.ring(colour, phase, direction):
                        copy.wait_send()


def rs_kernel(scale, *refs):
    scatter = Scatter(scale, [(ref, ZERO, ref.shape[THREE]) for ref in refs[:TWO]], refs[TWO:4], refs[4:])
    meet_neighbours(scatter.place)
    scatter.begin()
    for turn in range(THREE):
        scatter.absorb(turn)
    scatter.relay(ZERO)
    scatter.absorb(THREE)
    scatter.settle(ZERO)
    for phase in (ONE, TWO):
        scatter.relay(phase)
        scatter.settle(phase)
    scatter.end()


def as_torus(rows):
    return rows.reshape(SIDE, SIDE, SIDE, rows.shape[ZERO] // SIDE ** THREE, rows.shape[ONE])


def scatter_grads(g_attn, g_vec, scale):
    sources = [as_torus(g_attn), as_torus(g_vec)]
    heights = [src.shape[THREE] for src in sources]
    width = g_attn.shape[ONE]
    anywhere = pl.BlockSpec(memory_space=pl.ANY)
    return pl.pallas_call(
        functools.partial(rs_kernel, scale),
        in_specs=[anywhere] * TWO, out_specs=[anywhere] * TWO,
        out_shape=[jax.ShapeDtypeStruct((h, width), F32) for h in heights],
        scratch_shapes=Scatter.scratch_shapes(heights),
        compiler_params=pltpu.CompilerParams(collective_id=ONE, has_side_effects=True, vmem_limit_bytes=VMEM_BYTES),
        cost_estimate=pl.CostEstimate(flops=10 ** 9, bytes_accessed=8 * width * g_attn.shape[ZERO], transcendentals=ZERO),
        name='scatter_grads',
    )(*sources)


class Gather:
    def __init__(self, send_sem, recv_sem, base=ZERO):
        self.send_sem, self.recv_sem = send_sem, recv_sem
        self.used = base
        self.core, self.chip, self.place = lax.axis_index('dp'), lax.axis_index('fsdp'), torus_place()
        self.sibling = (ONE - self.core, self.chip)
        self.started = []

    def remote(self, src, dst, device):
        i = self.used
        self.used += ONE
        return pltpu.make_async_remote_copy(src_ref=src, dst_ref=dst, send_sem=self.send_sem.at[i], recv_sem=self.recv_sem.at[i], device_id=device, device_id_type=MESH_ID)

    def start(self, copy):
        copy.start()
        self.started.append(copy)

    def ring(self, colour, phase, view, own=None):
        order = DIM_ORDER[colour]
        dim = order[phase]
        have = sorted(order[:phase])

        def index(shift, half=None):
            where = [self.place[ZERO], self.place[ONE], self.place[TWO]]
            where[dim] = lax.rem(self.place[dim] + shift + SIDE, SIDE)
            for i, h in enumerate(have):
                where[h] = slice(None) if half is None or i > ZERO else pl.ds(TWO * half, TWO)
            return tuple(where)

        out = []
        for direction, shift in enumerate((ONE, -ONE)):
            device = (self.core, chip_at(self.place, dim, shift))
            half = direction if phase == ZERO else None
            near_dst = view(index(ZERO), None)
            out.append(dict(
                near=self.remote(near_dst if own is None else own, near_dst, device),
                far=self.remote(view(index(-shift, direction), half), view(index(-shift, direction), half), device),
                near_at=index(-shift), far_at=index(TWO, direction)))
        return out


def ag_kernel(attn_ref, ffn_ref, vec_ref, oattn_ref, planes_ref, vec_out, attn_v, send_sem, recv_sem, load_sem):
    net = Gather(send_sem, recv_sem)
    core, place = net.core, net.place
    rows, width = attn_ref.shape
    band = rows // (TWO * COLOURS)
    vec_high = vec_ref.shape[ZERO]
    stores, finals = [], []

    def band_rows(colour):
        return pl.ds(pl.multiple_of((core * COLOURS + colour) * band, band), band)

    def columns(half):
        return slice(None) if half is None else pl.ds(half * (width // TWO), width // TWO)

    def attn_view(colour):
        return lambda where, half: attn_v.at[where + (band_rows(colour), columns(half))]

    def ffn_view(colour):
        last = DIM_ORDER[colour][TWO]
        return lambda where, half: planes_ref.at[(colour,) + tuple(w for d, w in enumerate(where) if d != last) + (slice(None), columns(half))]

    def vec_view(where, half):
        return vec_out.at[where + (slice(None) if half is None else pl.ds(half * (vec_high // TWO), vec_high // TWO), slice(None))]

    colours = range(COLOURS)
    attn_own = [attn_ref.at[band_rows(colour), :] for colour in colours]
    ffn_own = [ffn_ref.at[band_rows(colour), :] for colour in colours]
    rings = {('attn', phase): [net.ring(colour, phase, attn_view(colour), attn_own[colour] if phase == ZERO else None) for colour in colours] for phase in range(THREE)}
    rings |= {('ffn', phase): [net.ring(colour, phase, ffn_view(colour), ffn_own[colour] if phase == ZERO else None) for colour in colours] for phase in range(TWO)}
    rings |= {('vec', phase): [net.ring(ONE, phase, vec_view, vec_ref if phase == ZERO else None)] for phase in range(THREE)}

    def publish(at):
        keep = pltpu.make_async_copy(attn_v.at[at], oattn_ref.at[at], load_sem.at[len(stores)])
        keep.start()
        stores.append(keep)
        give = net.remote(attn_v.at[at], oattn_ref.at[at], net.sibling)
        net.start(give)
        finals.append(give)

    def send_near(name, phase):
        for ring in rings.get((name, phase), ()):
            for way in ring:
                net.start(way['near'])

    def pass_on(name, phase):
        for ring in rings.get((name, phase), ()):
            for way in ring:
                way['near'].wait_recv()
                net.start(way['far'])
        if phase == TWO and name == 'attn':
            for colour in colours:
                for way in rings[(name, phase)][colour]:
                    publish(way['near_at'] + (band_rows(colour), slice(None)))

    def complete(name, phase):
        for colour, ring in enumerate(rings.get((name, phase), ())):
            for way in ring:
                way['far'].wait_recv()
            if phase < TWO and (name, phase + ONE) in rings:
                for way in rings[(name, phase + ONE)][colour]:
                    net.start(way['near'])
            if phase == TWO and name == 'attn':
                for way in ring:
                    publish(way['far_at'] + (band_rows(colour), slice(None)))
        if phase == ONE and name == 'attn':
            for colour in colours:
                last = DIM_ORDER[colour][TWO]
                publish(tuple(place[d] if d == last else slice(None) for d in range(THREE)) + (band_rows(colour), slice(None)))

    for colour in colours:
        attn_v[(place[ZERO], place[ONE], place[TWO]) + (band_rows(colour), slice(None))] = attn_ref[band_rows(colour), :]
        kept = [place[d] for d in range(THREE) if d != DIM_ORDER[colour][TWO]]
        planes_ref[(colour, kept[ZERO], kept[ONE])] = ffn_ref[band_rows(colour), :]
    vec_out[place[ZERO], place[ONE], place[TWO]] = vec_ref[ALL]
    meet_neighbours(place)
    names = ('attn', 'vec', 'ffn')
    for name in names:
        send_near(name, ZERO)
    for phase in range(THREE):
        for name in names:
            pass_on(name, phase)
        for name in names:
            complete(name, phase)
    for copy in finals:
        copy.wait_recv()
    for copy in net.started:
        copy.wait_send()
    for copy in stores:
        copy.wait()


def gather_params(attn_w, ffn_w, vec_rows):
    rows, width = attn_w.shape
    full = (SIDE, SIDE, SIDE, rows, width)
    n_copies = COLOURS * 4 * (THREE + TWO) + 4 * THREE + COLOURS * 5
    vmem = pl.BlockSpec(memory_space=pltpu.VMEM)
    return pl.pallas_call(
        ag_kernel,
        in_specs=[vmem] * THREE, out_specs=[pl.BlockSpec(memory_space=pl.ANY), vmem, vmem],
        out_shape=[jax.ShapeDtypeStruct(full, BF16), jax.ShapeDtypeStruct((COLOURS, SIDE, SIDE, rows // (TWO * COLOURS), width), BF16),
                   jax.ShapeDtypeStruct((SIDE, SIDE, SIDE) + vec_rows.shape, F32)],
        scratch_shapes=[pltpu.VMEM(full, BF16), pltpu.SemaphoreType.DMA((n_copies,)), pltpu.SemaphoreType.DMA((n_copies,)), pltpu.SemaphoreType.DMA((COLOURS * 5,))],
        compiler_params=pltpu.CompilerParams(collective_id=TWO, has_side_effects=True, vmem_limit_bytes=VMEM_BYTES),
        cost_estimate=pl.CostEstimate(flops=10 ** 9, bytes_accessed=4 * rows * width * SIDE ** THREE, transcendentals=ZERO),
        name='gather_params',
    )(attn_w, ffn_w, vec_rows)


class LastPhase:
    def __init__(self, planes, out, near, far, send_sem, recv_sem, load_sem):
        self.planes, self.out, self.near, self.far = planes, out, near, far
        self.send_sem, self.recv_sem, self.load_sem = send_sem, recv_sem, load_sem
        self.core, self.chip, self.place = lax.axis_index('dp'), lax.axis_index('fsdp'), torus_place()
        self.band = planes.shape[THREE]

    @staticmethod
    def scratch_shapes(planes):
        colours, side, _, band, width = planes.shape
        sems = [pltpu.SemaphoreType.DMA((9 * COLOURS,)), pltpu.SemaphoreType.DMA((9 * COLOURS,)), pltpu.SemaphoreType.DMA((5 * COLOURS,))]
        return [pltpu.VMEM((colours, TWO, side, side, band, width), BF16), pltpu.VMEM((colours, TWO, side // TWO, side, band, width), BF16)] + sems

    def remote(self, i, src, dst, device):
        return pltpu.make_async_remote_copy(src_ref=src, dst_ref=dst, send_sem=self.send_sem.at[i], recv_sem=self.recv_sem.at[i], device_id=device, device_id_type=MESH_ID)

    def ring(self, colour, direction):
        device = (self.core, chip_at(self.place, DIM_ORDER[colour][TWO], ONE - TWO * direction))
        i = 9 * colour + TWO * direction
        got = self.near.at[colour, direction]
        return (self.remote(i, self.planes.at[colour], got, device),
                self.remote(i + ONE, got.at[pl.ds(TWO * direction, TWO)], self.far.at[colour, direction], device))

    def shares(self, colour):
        last = DIM_ORDER[colour][TWO]
        rows = pl.ds(pl.multiple_of((self.core * COLOURS + colour) * self.band, self.band), self.band)
        views = [(self.planes.at[colour], ZERO, None)]
        views += [(self.near.at[colour, direction], TWO * direction - ONE, None) for direction in range(TWO)]
        views += [(self.far.at[colour, direction], TWO, direction) for direction in range(TWO)]
        out = []
        for n, (src, shift, half) in enumerate(views):
            where = [slice(None)] * THREE
            where[last] = lax.rem(self.place[last] + shift + SIDE, SIDE)
            if half is not None:
                where[min(d for d in range(THREE) if d != last)] = pl.ds(TWO * half, TWO)
            dst = self.out.at[tuple(where) + (rows, slice(None))]
            out.append((self.remote(9 * colour + 4 + n, src, dst, (ONE - self.core, self.chip)), pltpu.make_async_copy(src, dst, self.load_sem.at[5 * colour + n])))
        return out

    def share(self, colour, which):
        for n in which:
            give, keep = self.shares(colour)[n]
            give.start()
            keep.start()

    def begin(self):
        for colour in range(COLOURS):
            for direction in range(TWO):
                self.ring(colour, direction)[ZERO].start()
        for colour in range(COLOURS):
            self.share(colour, (ZERO,))

    def pass_on(self):
        for colour in range(COLOURS):
            for direction in range(TWO):
                near, far = self.ring(colour, direction)
                near.wait_recv()
                far.start()
            self.share(colour, (ONE, TWO))

    def complete(self):
        for colour in range(COLOURS):
            for direction in range(TWO):
                self.ring(colour, direction)[ONE].wait_recv()
            self.share(colour, (THREE, 4))

    def end(self):
        for colour in range(COLOURS):
            for give, keep in self.shares(colour):
                give.wait_recv()
                give.wait_send()
                keep.wait()
            for direction in range(TWO):
                for copy in self.ring(colour, direction):
                    copy.wait_send()


def dot(lhs, rhs, contract=((ONE,), (ZERO,))):
    return lax.dot_general(lhs, rhs, (contract, ((), ())), preferred_element_type=F32)


def dot_nt(lhs, rhs):
    return dot(lhs, rhs, ((ONE,), (ONE,)))


def dot_tn(lhs, rhs):
    return dot(lhs, rhs, ((ZERO,), (ZERO,)))


def norm_rows(resid, gain, shift):
    mean = jnp.mean(resid, axis=-ONE, keepdims=True)
    centred = resid - mean
    inv_std = lax.rsqrt(jnp.mean(centred * centred, axis=-ONE, keepdims=True) + LN_EPS)
    normed = centred * inv_std
    return (normed * gain + shift).astype(BF16), normed, inv_std


def norm_rows_bwd(d_out, normed, inv_std, gain):
    d_norm = d_out * gain
    return inv_std * (d_norm - jnp.mean(d_norm, axis=-ONE, keepdims=True) - normed * jnp.mean(d_norm * normed, axis=-ONE, keepdims=True))


def col_sum(values):
    return jnp.sum(values, axis=ZERO, keepdims=True)


def lane_row(head, dtype=BF16):
    lane = lax.broadcasted_iota(jnp.int32, (ONE, PAIR), ONE)
    return jnp.where((lane >= HEAD_DIM * head) & (lane < HEAD_DIM * (head + ONE)), 1.0, 0.0).astype(dtype)


def spare_lane(head):
    lane = lax.broadcasted_iota(jnp.int32, (ONE, PAIR), ONE)
    return jnp.where(lane == HEAD_DIM * (ONE - head), 1.0, 0.0)


def mask_fill(n_rows, n_valid):
    row = lax.broadcasted_iota(jnp.int32, (n_rows, PAIR), ZERO)
    return jnp.where(row >= n_valid, MASK_FILL, 0.0)


def head_masks(pair_q, pair_k, head, fill):
    q_f = pair_q * lane_row(head) + spare_lane(head).astype(BF16)
    k_f = pair_k * lane_row(head) + (fill * spare_lane(head)).astype(BF16)
    return q_f, k_f


def half_only(pair, head):
    return pair * lane_row(head)


def join_halves(first, second):
    lane = lax.broadcasted_iota(jnp.int32, first.shape, ONE)
    return jnp.where(lane < HEAD_DIM, first, second)


def score_blocks(n_heads, n_q, n_k, causal, step):
    if not causal:
        return [(head, ZERO, n_q, n_k) for head in range(n_heads)]
    return [(head, first, step, first + step) for head in range(n_heads) for first in range(ZERO, n_q, step)]


def scores_t(q_f, k_f, causal, first):
    s_t = dot_nt(k_f, q_f)
    if causal:
        key_i = lax.broadcasted_iota(jnp.int32, s_t.shape, ZERO)
        qry_i = lax.broadcasted_iota(jnp.int32, s_t.shape, ONE) + first
        s_t = jnp.where(key_i <= qry_i, s_t, MASK_FILL)
    return s_t


def pair_of(group, head):
    return group[:, head // TWO * PAIR:(head // TWO + ONE) * PAIR]


def masked_pairs(q_g, k_g, n_valid):
    fill = mask_fill(k_g.shape[ZERO], n_valid)
    cache = {}

    def get(head):
        if head not in cache:
            cache[head] = head_masks(pair_of(q_g, head), pair_of(k_g, head), head % TWO, fill)
        return cache[head]

    return get


def stack_heads(parts, n_heads):
    return jnp.concatenate([jnp.concatenate(parts[head], axis=ONE) for head in range(n_heads)], axis=ZERO)


def run_ahead(blocks, produce, transform, consume, delay):
    ahead = produce(blocks[ZERO])
    waiting = []
    for i, block in enumerate(blocks):
        now = ahead
        if i + ONE < len(blocks):
            ahead = produce(blocks[i + ONE])
        waiting.append((block, transform(block, now)))
        if len(waiting) > delay:
            consume(*waiting.pop(ZERO))
    for item in waiting:
        consume(*item)


def attend_group(q_g, k_g, v_g, n_valid, causal, lse_ref):
    n_heads = GROUP // HEAD_DIM
    o_parts = [[] for _ in range(n_heads)]
    v_t = v_g.T
    masked = masked_pairs(q_g, k_g, n_valid)

    def produce(block):
        head, first, n_q, n_k = block
        q_f, k_f = masked(head)
        return scores_t(q_f[first:first + n_q], k_f[:n_k], causal, first)

    def transform(block, s_t):
        head, first, n_q, n_k = block
        top = jnp.max(s_t, axis=ZERO, keepdims=True)
        e_t = jnp.exp(s_t - top)
        total = jnp.sum(e_t, axis=ZERO, keepdims=True)
        lse_ref[ZERO, ZERO, head:head + ONE, first:first + n_q] = top + jnp.log(total)
        return (e_t * (1.0 / total)).astype(BF16)

    def consume(block, p_t):
        head, first, n_q, n_k = block
        o_parts[head].append(dot(v_t[HEAD_DIM * head:HEAD_DIM * (head + ONE), :n_k], p_t))

    run_ahead(score_blocks(n_heads, q_g.shape[ZERO], k_g.shape[ZERO], causal, 128), produce, transform, consume, TWO)
    return stack_heads(o_parts, n_heads).T.astype(BF16)


def attend_group_bwd(d_o, q_g, k_g, v_g, n_valid, causal, lse_ref, between=None):
    n_heads = GROUP // HEAD_DIM
    k_t = k_g.T
    dq_t, dk_h, dv_h = [[] for _ in range(n_heads)], [None] * n_heads, [None] * n_heads
    masked = masked_pairs(q_g, k_g, n_valid)
    v_half = {}

    def produce(block):
        head, first, n_q, n_k = block
        q_f, k_f = masked(head)
        if head not in v_half:
            v_half[head] = half_only(pair_of(v_g, head), head % TWO)
        rows = slice(first, first + n_q)
        return scores_t(q_f[rows], k_f[:n_k], causal, first), dot_nt(v_half[head][:n_k], pair_of(d_o, head)[rows])

    def transform(block, products):
        head, first, n_q, n_k = block
        s_t, dp_t = products
        p_t = jnp.exp(s_t - lse_ref[ZERO, ZERO, head:head + ONE, first:first + n_q])
        weighted = p_t * dp_t
        return p_t.astype(BF16), (weighted - p_t * jnp.sum(weighted, axis=ZERO, keepdims=True)).astype(BF16)

    def grow(old, new):
        if old is None:
            return new
        n_old = old.shape[ZERO]
        return old + new if n_old == new.shape[ZERO] else jnp.concatenate([old + new[:n_old], new[n_old:]], axis=ZERO)

    def consume(block, operands):
        head, first, n_q, n_k = block
        p_b, ds_t = operands
        rows = slice(first, first + n_q)
        dv_h[head] = grow(dv_h[head], dot(p_b, pair_of(d_o, head)[rows]))
        dk_h[head] = grow(dk_h[head], dot(ds_t, pair_of(q_g, head)[rows]))
        dq_t[head].append(dot(k_t[HEAD_DIM * head:HEAD_DIM * (head + ONE), :n_k], ds_t))

    blocks = score_blocks(n_heads, q_g.shape[ZERO], k_g.shape[ZERO], causal, 256)
    if between is None:
        run_ahead(blocks, produce, transform, consume, ZERO)
    else:
        n_first = len(blocks) // TWO
        run_ahead(blocks[:n_first], produce, transform, consume, ZERO)
        between()
        run_ahead(blocks[n_first:], produce, transform, consume, ZERO)
    join = lambda parts: jnp.concatenate([join_halves(parts[h], parts[h + ONE]) for h in range(ZERO, n_heads, TWO)], axis=ONE)
    return stack_heads(dq_t, n_heads).T * 0.125, join(dk_h), join(dv_h)


def attn_fwd_kernel(causal, slots, guest, lens_ref, x_ref, kv_ref, wq_ref, wk_ref, wv_ref, w_all, bias_ref, rows_ref,
                    q_ref, k_ref, v_ref, o_ref, lse_ref, h_ref, normed_ref, inv_ref, o_all, wo_v, load_sem):
    q_row, k_row, v_row, o_row, gain_row, o_mat = slots
    sample, group = pl.program_id(ZERO), pl.program_id(ONE)
    d_model = wo_v.shape[ZERO]
    fetch = pltpu.make_async_copy(w_all.at[pl.ds(o_mat * d_model, d_model), :], wo_v, load_sem)

    @pl.when((sample == ZERO) & (group == ZERO))
    def _():
        fetch.start()

    turn = sample * pl.num_programs(ONE) + group
    if guest is not None:
        for where, steps in ((ZERO, (lambda: meet_neighbours(guest.place), guest.begin)), (THREE, (guest.pass_on,)), (5, (guest.complete,))):
            @pl.when(turn == where)
            def _():
                for step in steps:
                    step()

    x_b, kv_b = x_ref[ALL], kv_ref[ALL]
    q_g = ((dot(x_b, wq_ref[ALL]) + bias_ref[q_row:q_row + ONE, :]) * 0.125).astype(BF16)
    k_g = (dot(kv_b, wk_ref[ALL]) + bias_ref[k_row:k_row + ONE, :]).astype(BF16)
    v_g = (dot(kv_b, wv_ref[ALL]) + bias_ref[v_row:v_row + ONE, :]).astype(BF16)
    q_ref[ALL], k_ref[ALL], v_ref[ALL] = q_g, k_g, v_g
    o_g = attend_group(q_g, k_g, v_g, lens_ref[sample], causal, lse_ref)
    o_ref[ALL] = o_g
    o_all[:, pl.ds(pl.multiple_of(group * GROUP, GROUP), GROUP)] = o_g

    @pl.when((sample == ZERO) & (group == pl.num_programs(ONE) - ONE))
    def _():
        fetch.wait()

    @pl.when(group == pl.num_programs(ONE) - ONE)
    def _():
        resid = x_ref[ALL].astype(F32) + dot(o_all[ALL], wo_v[ALL]) + rows_ref[o_row:o_row + ONE, :]
        h_out, normed, inv_std = norm_rows(resid, rows_ref[gain_row:gain_row + ONE, :], rows_ref[gain_row + ONE:gain_row + TWO, :])
        h_ref[ALL], normed_ref[ALL], inv_ref[ALL] = h_out, normed, inv_std

    if guest is not None:
        @pl.when(turn == pl.num_programs(ZERO) * pl.num_programs(ONE) - ONE)
        def _():
            guest.end()


def attn_forward(x, kv, lens, attn_full, bias_rows, mats, slots, causal, planes=None, full_rows=None):
    d_model = x.shape[-ONE]
    n_batch = lens.shape[ZERO]
    n_q, n_k = x.shape[ZERO] // n_batch, kv.shape[ZERO] // n_batch
    n_groups = d_model // GROUP
    col = lambda mat: pl.BlockSpec((d_model, GROUP), lambda b, g: (mat, g))
    q_blk = pl.BlockSpec((n_q, GROUP), lambda b, g: (b, g))
    k_blk = pl.BlockSpec((n_k, GROUP), lambda b, g: (b, g))
    tok = lambda n: pl.BlockSpec((n, d_model), lambda b, g: (b, ZERO))
    n_heads_g = GROUP // HEAD_DIM
    out_shape = (
        jax.ShapeDtypeStruct(x.shape, BF16), jax.ShapeDtypeStruct(kv.shape, BF16), jax.ShapeDtypeStruct(kv.shape, BF16),
        jax.ShapeDtypeStruct(x.shape, BF16), jax.ShapeDtypeStruct((n_batch, n_groups, n_heads_g, n_q), F32),
        jax.ShapeDtypeStruct(x.shape, BF16), jax.ShapeDtypeStruct(x.shape, F32), jax.ShapeDtypeStruct((x.shape[ZERO], ONE), F32))
    kernel = functools.partial(attn_fwd_kernel, causal, slots + (mats[THREE],))
    in_specs = [pl.BlockSpec(memory_space=pltpu.SMEM), tok(n_q), tok(n_k), col(mats[ZERO]), col(mats[ONE]), col(mats[TWO]), pl.BlockSpec(memory_space=pl.ANY),
                pl.BlockSpec((bias_rows.shape[ZERO], GROUP), lambda b, g: (ZERO, g)), pl.BlockSpec(bias_rows.shape, lambda b, g: (ZERO, ZERO))]
    out_specs = [q_blk, k_blk, k_blk, q_blk, pl.BlockSpec((ONE, ONE, n_heads_g, n_q), lambda b, g: (b, g, ZERO, ZERO)),
                 tok(n_q), tok(n_q), pl.BlockSpec((n_q, ONE), lambda b, g: (b, ZERO))]
    scratch = [pltpu.VMEM((n_q, d_model), BF16), pltpu.VMEM((d_model, d_model), BF16), pltpu.SemaphoreType.DMA]
    args = [lens, x, kv, attn_full, attn_full, attn_full, attn_full, bias_rows, bias_rows]
    params = dict(vmem_limit_bytes=VMEM_BYTES, dimension_semantics=('arbitrary', 'arbitrary'))
    if planes is None:
        body = functools.partial(kernel, None)
    else:
        n_in, n_out, n_own = len(args), len(out_specs), len(scratch)

        def body(*refs):
            ins, held, outs, whole, rest = refs[:n_in], refs[n_in], refs[n_in + ONE:n_in + ONE + n_out], refs[n_in + ONE + n_out], refs[n_in + TWO + n_out:]
            kernel(LastPhase(held, whole, *rest[n_own:]), *ins, *outs, *rest[:n_own])

        in_specs.append(pl.BlockSpec(memory_space=pltpu.VMEM))
        args.append(planes)
        out_specs.append(pl.BlockSpec(memory_space=pl.ANY))
        out_shape += (jax.ShapeDtypeStruct((SIDE, SIDE, SIDE, full_rows // SIDE ** THREE, d_model), BF16),)
        scratch += LastPhase.scratch_shapes(planes)
        params |= dict(collective_id=5, has_side_effects=True)
    return pl.pallas_call(
        body, grid=(n_batch, n_groups), in_specs=in_specs, out_specs=out_specs, out_shape=out_shape, scratch_shapes=scratch,
        compiler_params=pltpu.CompilerParams(**params),
        cost_estimate=pl.CostEstimate(flops=TWO * d_model * d_model * (TWO * x.shape[ZERO] + TWO * kv.shape[ZERO]) + 16 * x.shape[ZERO] * n_k * d_model, bytes_accessed=20 * x.shape[ZERO] * d_model, transcendentals=ZERO),
        name='attn_fwd',
    )(*args)


def attn_bwd_kernel(causal, gain_row, mats, lhs_of, guest, lens_ref, dres_ref, wo_ref, w_all, q_ref, k_ref, v_ref, lse_ref,
                    rows_ref, normed_ref, inv_ref, lhs_refs, dx_ref, dkv_ref, sums_ref, tail_ref, grads_ref,
                    d_all, dk_all, dv_all, dres_all, w_v, lhs_vs, grad_v, load_sem):
    sample, group = pl.program_id(ZERO), pl.program_id(ONE)
    d_model = w_v.shape[ONE]
    n_q, n_k = q_ref.shape[ZERO], k_ref.shape[ZERO]
    last = pl.num_programs(ONE) - ONE
    fetches = [pltpu.make_async_copy(w_all.at[pl.ds(mat * d_model, d_model), :], w_v.at[i], load_sem.at[i]) for i, mat in enumerate(mats[:THREE])]
    lhs_fetch = lambda i: pltpu.make_async_copy(lhs_refs[i], lhs_vs[i % TWO].at[pl.ds(ZERO, lhs_refs[i].shape[ZERO]), :], load_sem.at[THREE + i])

    @pl.when((sample == ZERO) & (group == ZERO))
    def _():
        for fetch in fetches + [lhs_fetch(ZERO), lhs_fetch(ONE)]:
            fetch.start()

    turn = sample * pl.num_programs(ONE) + group
    guest(ZERO, TWO * turn)
    q_rows = pl.ds(pl.multiple_of(sample * n_q, n_q), n_q)
    k_rows = pl.ds(pl.multiple_of(sample * n_k, n_k), n_k)
    d_o = dot_nt(dres_ref[ALL].astype(BF16), wo_ref[ALL]).astype(BF16)
    dq, dk, dv = attend_group_bwd(d_o, q_ref[ALL], k_ref[ALL], v_ref[ALL], lens_ref[sample], causal, lse_ref, None if causal else functools.partial(guest, ONE, TWO * turn + ONE))
    cols = pl.ds(pl.multiple_of(group * GROUP, GROUP), GROUP)
    for i, (full, rows, value) in enumerate(((d_all, q_rows, dq), (dk_all, k_rows, dk), (dv_all, k_rows, dv))):
        sums_ref[ZERO, i:i + ONE, :] = col_sum(value)
        full[rows, cols] = value.astype(BF16)

    @pl.when(group == ZERO)
    def _():
        dres_all[q_rows, :] = dres_ref[ALL].astype(BF16)

    @pl.when((sample == ZERO) & (group == last))
    def _():
        for fetch in fetches:
            fetch.wait()

    @pl.when(group == last)
    def _():
        d_kv = dot_nt(dk_all[k_rows, :], w_v[ONE]) + dot_nt(dv_all[k_rows, :], w_v[TWO])
        d_h = dres_ref[ALL] + dot_nt(d_all[q_rows, :], w_v[ZERO])
        if causal:
            dx_ref[ALL] = (d_h + d_kv).astype(BF16)
            tail_ref[ALL] = jnp.zeros_like(tail_ref)
        else:
            dkv_ref[ALL] = d_kv.astype(BF16)
            normed = normed_ref[ALL]
            d_resid = norm_rows_bwd(d_h, normed, inv_ref[ALL], rows_ref[gain_row:gain_row + ONE, :])
            dx_ref[ALL] = d_resid
            tail_ref[ZERO, ZERO:ONE, :] = col_sum(d_resid)
            tail_ref[ZERO, ONE:TWO, :] = col_sum(d_h * normed)
            tail_ref[ZERO, TWO:THREE, :] = col_sum(d_h)

    @pl.when(turn == pl.num_programs(ZERO) * pl.num_programs(ONE) - ONE)
    def _():
        guest(TWO, 12)
        stores = []
        for i, (rhs, which) in enumerate(zip((d_all, dk_all, dv_all, dres_all), lhs_of)):
            if which not in lhs_of[:i]:
                lhs_fetch(which).wait()
            if i >= TWO:
                stores[i - TWO].wait()
            grad_v[i % TWO] = dot_tn(lhs_vs[which % TWO][pl.ds(ZERO, rhs.shape[ZERO]), :], rhs[ALL])
            store = pltpu.make_async_copy(grad_v.at[i % TWO], grads_ref.at[pl.ds(mats[i] * d_model, d_model), :], load_sem.at[6 + i])
            store.start()
            stores.append(store)
            if i == ZERO and len(lhs_refs) > TWO:
                lhs_fetch(TWO).start()
            guest(TWO, 13 + i)
        for store in stores[TWO:]:
            store.wait()


def scatter_guest(scatter, plan, parity, position):
    steps = dict(end=scatter.end) | {('relay', p): functools.partial(scatter.relay, p) for p in range(THREE)}
    steps |= {('settle', p): functools.partial(scatter.settle, p) for p in range(THREE)} | {turn: functools.partial(scatter.absorb, turn) for turn in range(SIDE)}
    if parity == TWO:
        for name in plan.get(position, ()):
            steps[name]()
        return
    if parity == ZERO:
        @pl.when(position == ZERO)
        def _():
            meet_neighbours(scatter.place)
            scatter.begin()
    for where, names in plan.items():
        if where < 12 and where % TWO == parity:
            @pl.when(position == where)
            def _():
                for name in names:
                    steps[name]()


def no_guest(parity, position):
    pass


def attn_backward(dres, q, k, v, lse, lens, attn_full, bias_rows, mats, causal, lhs_list, lhs_of, g_rows=None, scale=None, gain_row=ZERO, normed=None, inv_std=None, grads=None):
    d_model = q.shape[-ONE]
    n_batch = lens.shape[ZERO]
    n_q, n_k = q.shape[ZERO] // n_batch, k.shape[ZERO] // n_batch
    n_groups = d_model // GROUP
    row = lambda mat: pl.BlockSpec((GROUP, d_model), lambda b, g: (mat * n_groups + g, ZERO))
    q_blk = pl.BlockSpec((n_q, GROUP), lambda b, g: (b, g))
    k_blk = pl.BlockSpec((n_k, GROUP), lambda b, g: (b, g))
    tok = lambda n: pl.BlockSpec((n, d_model), lambda b, g: (b, ZERO))
    n_heads_g = GROUP // HEAD_DIM
    anywhere = pl.BlockSpec(memory_space=pl.ANY)
    in_specs = [pl.BlockSpec(memory_space=pltpu.SMEM), tok(n_q), row(mats[THREE]), anywhere, q_blk, k_blk, k_blk,
                pl.BlockSpec((ONE, ONE, n_heads_g, n_q), lambda b, g: (b, g, ZERO, ZERO)), pl.BlockSpec(bias_rows.shape, lambda b, g: (ZERO, ZERO))]
    args = [lens, dres, attn_full, attn_full, q, k, v, lse, bias_rows]
    tail_shape = jax.ShapeDtypeStruct((n_batch, 8, d_model), F32)
    out_shape = [jax.ShapeDtypeStruct(q.shape, BF16 if causal else F32)]
    out_specs = [tok(n_q)]
    if not causal:
        late = dict(pipeline_mode=pl.Buffered(ONE))
        in_specs += [pl.BlockSpec((n_q, d_model), lambda b, g: (b, ZERO), **late), pl.BlockSpec((n_q, ONE), lambda b, g: (b, ZERO), **late)]
        args += [normed, inv_std]
        out_shape.append(jax.ShapeDtypeStruct(k.shape, BF16))
        out_specs.append(tok(n_k))
    n_lhs_at = len(args)
    args += list(lhs_list)
    in_specs += [anywhere] * len(lhs_list)
    out_shape += [tail_shape, tail_shape, jax.ShapeDtypeStruct(attn_full.shape, F32)]
    out_specs += [pl.BlockSpec((ONE, 8, GROUP), lambda b, g: (b, ZERO, g)), pl.BlockSpec((ONE, 8, d_model), lambda b, g: (b, ZERO, ZERO)), anywhere]
    both = lambda n: pltpu.VMEM((n_batch * n, d_model), BF16)
    own = [both(n_q), both(n_k), both(n_k), both(n_q), pltpu.VMEM((THREE, d_model, d_model), BF16), pltpu.VMEM(lhs_list[ZERO].shape, BF16), pltpu.VMEM(lhs_list[ONE].shape, BF16),
           pltpu.VMEM((TWO, d_model, d_model), F32), pltpu.SemaphoreType.DMA((10,))]
    kernel = functools.partial(attn_bwd_kernel, causal, gain_row, mats, lhs_of)
    params = dict(vmem_limit_bytes=VMEM_BYTES, dimension_semantics=('arbitrary', 'arbitrary'))
    aliases = {}
    if causal:
        args.append(grads)
        in_specs.append(anywhere)
        aliases = {len(args) - ONE: len(out_shape) - ONE}
    else:
        args.append(as_torus(g_rows))
        in_specs.append(anywhere)
        n_rows = args[-ONE].shape[THREE]
        out_shape.append(jax.ShapeDtypeStruct((n_rows, d_model), F32))
        out_specs.append(anywhere)
        params |= dict(collective_id=THREE, has_side_effects=True, vmem_limit_bytes=67043328)
    scratch = own + ([] if causal else Scatter.scratch_shapes([n_rows]))
    n_in, n_out, n_own = len(args), len(out_shape), len(own)

    def body(*refs):
        ins, outs, rest = refs[:n_in], refs[n_in:n_in + n_out], refs[n_in + n_out:]
        lhs_refs, (d_all, dk_all, dv_all, dres_all, w_v, lhs_a, lhs_b, grad_v, load_sem) = ins[n_lhs_at:-ONE], rest[:n_own]
        held = (d_all, dk_all, dv_all, dres_all, w_v, (lhs_a, lhs_b), grad_v, load_sem)
        if causal:
            dx, sums, tail, grads_ref = outs
            kernel(no_guest, *ins[:n_lhs_at], None, None, lhs_refs, dx, None, sums, tail, grads_ref, *held)
        else:
            dx, dkv, sums, tail, grads_ref, total = outs
            scatter = Scatter(scale, [(ins[-ONE], ZERO, n_rows)], [total], rest[n_own:])
            kernel(functools.partial(scatter_guest, scatter, CROSS_PLAN), *ins[:n_lhs_at], lhs_refs, dx, dkv, sums, tail, grads_ref, *held)

    return pl.pallas_call(
        body, grid=(n_batch, n_groups), in_specs=in_specs, out_specs=out_specs, out_shape=out_shape, scratch_shapes=scratch, input_output_aliases=aliases,
        compiler_params=pltpu.CompilerParams(**params),
        cost_estimate=pl.CostEstimate(flops=TWO * d_model * d_model * (TWO * q.shape[ZERO] + TWO * k.shape[ZERO]) + 40 * q.shape[ZERO] * n_k * d_model, bytes_accessed=20 * q.shape[ZERO] * d_model, transcendentals=ZERO),
        name='attn_bwd',
    )(*args)


def ffn_kernel(n_blocks, h_ref, dy_ref, up_ref, down_ref, rows_ref, bias_ref, normed_ref, inv_ref,
               y_ref, grad_ref, dres2_ref, tail_ref, upsum_ref, gelu_all, dup_all, dres3_all, h_all):
    step = pl.program_id(ZERO)
    block, d_model = h_ref.shape
    n_square = gelu_all.shape[ONE] // d_model

    @pl.when(step < n_blocks)
    def _():
        rows = pl.ds(pl.multiple_of(step * block, block), block)
        h_b = h_ref[ALL]
        h_all[rows, :] = h_b
        up = dot_nt(h_b, up_ref[ALL]) + bias_ref[ALL]
        cdf = 0.5 * (1.0 + lax.erf(up * 0.7071067811865476))
        gelu = (up * cdf).astype(BF16)
        slope = cdf + up * (0.3989422804014327 * jnp.exp(-0.5 * up * up))
        gelu_all[rows, :] = gelu
        resid = h_b.astype(F32) + dot(gelu, down_ref[ALL]) + rows_ref[8:9, :]
        y_b, normed3, inv3 = norm_rows(resid, rows_ref[13:14, :], rows_ref[14:15, :])
        y_ref[ALL] = y_b
        dy = dy_ref[ALL].astype(F32)
        d_res3 = norm_rows_bwd(dy, normed3, inv3, rows_ref[13:14, :])
        d_res3_b = d_res3.astype(BF16)
        dres3_all[rows, :] = d_res3_b
        d_up = dot_nt(d_res3_b, down_ref[ALL]) * slope
        d_up_b = d_up.astype(BF16)
        dup_all[rows, :] = d_up_b
        d_h2 = d_res3 + dot(d_up_b, up_ref[ALL])
        normed2 = normed_ref[ALL]
        d_res2 = norm_rows_bwd(d_h2, normed2, inv_ref[ALL], rows_ref[11:12, :])
        dres2_ref[ALL] = d_res2
        tail = jnp.concatenate([col_sum(d_res2), col_sum(d_res3), col_sum(d_h2 * normed2), col_sum(d_h2), col_sum(dy * normed3), col_sum(dy),
                                jnp.zeros((TWO, dy.shape[ONE]), F32)], axis=ZERO)
        up_sum = col_sum(d_up)

        @pl.when(step == ZERO)
        def _():
            tail_ref[ALL] = tail
            upsum_ref[ALL] = up_sum

        @pl.when(step > ZERO)
        def _():
            tail_ref[ALL] += tail
            upsum_ref[ALL] += up_sum

    square = step - n_blocks
    cols = pl.ds(pl.multiple_of(lax.rem(square + TWO * n_square, n_square) * d_model, d_model), d_model)

    @pl.when((square >= ZERO) & (square < n_square))
    def _():
        grad_ref[ALL] = dot_tn(dup_all[:, cols], h_all[ALL])

    @pl.when(square >= n_square)
    def _():
        grad_ref[ALL] = dot_tn(gelu_all[:, cols], dres3_all[ALL])


def ffn_both(h2, dy, ffn_full, bias_rows, up_bias, normed2, inv2, block=256):
    n_tok, d_model = h2.shape
    ffn_dim = ffn_full.shape[ZERO] // TWO
    n_blocks = n_tok // block
    n_steps = n_blocks + ffn_full.shape[ZERO] // d_model
    at = lambda i: jnp.minimum(i, n_blocks - ONE)
    tok = pl.BlockSpec((block, d_model), lambda i: (at(i), ZERO))
    once = lambda shape, idx: pl.BlockSpec(shape, lambda i: idx, pipeline_mode=pl.Buffered(ONE))
    return pl.pallas_call(
        functools.partial(ffn_kernel, n_blocks), grid=(n_steps,),
        in_specs=[tok, tok, once((ffn_dim, d_model), (ZERO, ZERO)), once((ffn_dim, d_model), (ONE, ZERO)), once(bias_rows.shape, (ZERO, ZERO)), once((ONE, ffn_dim), (ZERO, ZERO)),
                  tok, pl.BlockSpec((block, ONE), lambda i: (at(i), ZERO))],
        out_specs=[tok, pl.BlockSpec((d_model, d_model), lambda i: (jnp.maximum(i - n_blocks, ZERO), ZERO)), tok, pl.BlockSpec((8, d_model), lambda i: (ZERO, ZERO)), pl.BlockSpec((ONE, ffn_dim), lambda i: (ZERO, ZERO))],
        out_shape=[jax.ShapeDtypeStruct(h2.shape, BF16), jax.ShapeDtypeStruct(ffn_full.shape, F32), jax.ShapeDtypeStruct(h2.shape, F32),
                   jax.ShapeDtypeStruct((8, d_model), F32), jax.ShapeDtypeStruct((ONE, ffn_dim), F32)],
        scratch_shapes=[pltpu.VMEM((n_tok, ffn_dim), BF16), pltpu.VMEM((n_tok, ffn_dim), BF16), pltpu.VMEM((n_tok, d_model), BF16), pltpu.VMEM((n_tok, d_model), BF16)],
        compiler_params=pltpu.CompilerParams(vmem_limit_bytes=VMEM_BYTES, dimension_semantics=('arbitrary',)),
        cost_estimate=pl.CostEstimate(flops=12 * n_tok * d_model * ffn_dim, bytes_accessed=30 * n_tok * d_model, transcendentals=ZERO),
        name='ffn_both',
    )(h2, dy, ffn_full, ffn_full, bias_rows, up_bias, normed2, inv2)


CROSS_PLAN = {ONE: (ZERO,), TWO: (ONE,), THREE: (TWO,), 4: (THREE,), 5: (('relay', ZERO),), 9: (('settle', ZERO),), 11: (('relay', ONE),), 12: (('settle', ONE),), 13: (('relay', TWO),), 15: (('settle', TWO),), 16: ('end',)}


def solution(mesh):
    n_fsdp = mesh.shape['fsdp']
    n_dp = mesh.shape['dp']
    batch_axes = ('dp', 'fsdp')
    act_spec = P(batch_axes, None, None)
    len_spec = P(batch_axes)
    row_spec = P('fsdp', None)
    vec_spec = P('fsdp')

    def device_step(dec_in, enc_out, src_lens, tgt_lens, y_cot, attn_w, ffn_w, vec_params):
        d_model, n_vec = dec_in.shape[TWO], vec_params.shape[ZERO]
        scale = 1.0 / (dec_in.shape[ZERO] * dec_in.shape[ONE] * n_fsdp * n_dp)
        x, enc, dy = (a.reshape(-ONE, d_model) for a in (dec_in, enc_out, y_cot))
        vec_rows = jnp.pad(vec_params.astype(F32), (ZERO, 16 * LANES - n_vec)).reshape(16, LANES)
        attn_tiles, planes, vec_tiles = gather_params(attn_w, ffn_w, vec_rows)
        attn_full = attn_tiles.reshape(-ONE, d_model)
        vec_f = vec_tiles.reshape(n_fsdp, 16, LANES)[:, :TWO].reshape(n_fsdp, TWO * LANES)[:, :n_vec].reshape(-ONE)
        bias_rows = jnp.pad(vec_f[:15 * d_model].reshape(15, d_model), ((ZERO, ONE), (ZERO, ZERO)))
        up_bias = vec_f[15 * d_model:].reshape(ONE, -ONE)
        q1, k1, v1, o1, lse1, h1, normed1, inv1 = attn_forward(x, x, tgt_lens, attn_full, bias_rows, (ZERO, ONE, TWO, THREE), (ZERO, ONE, TWO, THREE, 9), True)
        q2, k2, v2, o2, lse2, h2, normed2, inv2, ffn_tiles = attn_forward(h1, enc, src_lens, attn_full, bias_rows, (4, 5, 6, 7), (4, 5, 6, 7, 11), False, planes, ffn_w.shape[ZERO] * n_fsdp)
        ffn_full = ffn_tiles.reshape(-ONE, d_model)
        y, g_ffn, d_res2, ffn_tail, up_sum = ffn_both(h2, dy, ffn_full, bias_rows, up_bias, normed2, inv2)
        d_res1, d_enc, sums2, tail2, grads, ffn_out = attn_backward(d_res2, q2, k2, v2, lse2, src_lens, attn_full, bias_rows, (4, 5, 6, 7), False, (h1, enc, o2), (ZERO, ONE, ONE, TWO), g_ffn, scale, 9, normed1, inv1)
        d_x, sums1, _, grads = attn_backward(d_res1, q1, k1, v1, lse1, tgt_lens, attn_full, bias_rows, (ZERO, ONE, TWO, THREE), True, (x, o1), (ZERO, ZERO, ZERO, ONE), grads=grads)
        s1, s2, t2 = jnp.sum(sums1, axis=ZERO), jnp.sum(sums2, axis=ZERO), jnp.sum(tail2, axis=ZERO)
        g_vec = jnp.concatenate([s1[ZERO:THREE].reshape(-ONE), t2[ZERO], s2[ZERO:THREE].reshape(-ONE), ffn_tail[ZERO], ffn_tail[ONE], t2[ONE], t2[TWO], ffn_tail[TWO], ffn_tail[THREE], ffn_tail[4], ffn_tail[5], up_sum[ZERO]])
        g_rows = jnp.pad(g_vec.reshape(n_fsdp, ONE, n_vec), ((ZERO, ZERO), (ZERO, 7), (ZERO, d_model - n_vec))).reshape(n_fsdp * 8, -ONE)
        attn_out, vec_out = scatter_grads(grads, g_rows, scale)
        return y.reshape(dec_in.shape), d_x.reshape(dec_in.shape), d_enc.reshape(enc_out.shape), attn_out, ffn_out, vec_out[ZERO, :n_vec]

    return jax.shard_map(device_step, mesh=mesh, in_specs=(act_spec, act_spec, len_spec, len_spec, act_spec, row_spec, row_spec, vec_spec), out_specs=(act_spec, act_spec, act_spec, row_spec, row_spec, vec_spec), check_vma=False)
```

```python
import functools
import jax
import jax.numpy as jnp
from jax import lax
from jax.experimental import pallas as pl
from jax.experimental.pallas import tpu as pltpu
from jax.sharding import PartitionSpec as P

ZERO, ONE, TWO, THREE = range(4)
ALL = ...
HEAD_DIM = 64
LN_EPS = 1e-5
MASK_FILL = -1e30
VMEM_BYTES = 60 * 1024 * 1024
F32 = jnp.float32
BF16 = jnp.bfloat16
GROUP = 256
PAIR = 128


SIDE = 4
LANES = 128
COLOURS = THREE
STAGES = TWO
DIM_ORDER = ((TWO, ONE, ZERO), (ONE, ZERO, TWO), (ZERO, TWO, ONE))
MESH_ID = pl.DeviceIdType.MESH


def torus_place():
    chip = lax.axis_index('fsdp')
    return (chip // (SIDE * SIDE), lax.rem(chip // SIDE, SIDE), lax.rem(chip, SIDE))


def chip_at(place, dim, shift):
    moved = [lax.rem(p + shift + SIDE, SIDE) if d == dim else p for d, p in enumerate(place)]
    return (moved[ZERO] * SIDE + moved[ONE]) * SIDE + moved[TWO]


def meet_neighbours(place):
    barrier = pltpu.get_barrier_semaphore()
    core = lax.axis_index('dp')
    for dim in range(THREE):
        for shift in (ONE, -ONE):
            pl.semaphore_signal(barrier, inc=ONE, device_id=(core, chip_at(place, dim, shift)), device_id_type=MESH_ID)
    pl.semaphore_signal(barrier, inc=ONE, device_id=(ONE - core, lax.axis_index('fsdp')), device_id_type=MESH_ID)
    pl.semaphore_wait(barrier, 7)


class Scatter:
    def __init__(self, scale, sources, outs, scratch, resident=False):
        self.scale, self.outs, self.resident = scale, outs, resident
        self.sources = [(ref, pl.ds(first, n)) for ref, first, n in sources]
        (self.acc, g1, d1, g2, d2, g3, d3, self.send_sem, self.recv_sem, self.load_sem, *stage) = scratch
        self.stage = None if resident else stage[ZERO]
        self.got, self.far = (g1, g2, g3), (d1, d2, d3)
        self.heights = [n for _, _, n in sources]
        self.offsets = [sum(self.heights[:i]) for i in range(len(sources))]
        self.height = sum(self.heights)
        self.n_low = self.heights[ZERO] // TWO
        self.core, self.chip, self.place = lax.axis_index('dp'), lax.axis_index('fsdp'), torus_place()
        self.pieces = [(d, colour) for d in (TWO, ONE, THREE, ZERO) for colour in range(COLOURS)]

    @staticmethod
    def scratch_shapes(heights, resident=False):
        h = sum(heights)
        n_low = heights[ZERO] // TWO
        buf = lambda *shape: pltpu.VMEM((COLOURS,) + shape + (LANES,), F32)
        n = Scatter.n_copies(len(heights))
        return [buf(SIDE, SIDE, SIDE, h), buf(TWO, SIDE, SIDE, h), buf(TWO, TWO, SIDE, h), buf(TWO, SIDE, h), buf(TWO, TWO, h), buf(TWO, h), buf(TWO, max(n_low, h - n_low)),
                pltpu.SemaphoreType.DMA((n,)), pltpu.SemaphoreType.DMA((n,)), pltpu.SemaphoreType.DMA((THREE + COLOURS, len(heights)))] + (
                    [] if resident else [pltpu.VMEM((STAGES, SIDE, SIDE, h, LANES), F32)])

    @staticmethod
    def n_copies(n_parts):
        return 12 * n_parts + COLOURS * 18 + COLOURS * n_parts

    def remote(self, i, src, dst, device):
        return pltpu.make_async_remote_copy(src_ref=src, dst_ref=dst, send_sem=self.send_sem.at[i], recv_sem=self.recv_sem.at[i], device_id=device, device_id_type=MESH_ID)

    def columns(self, of_core, colour):
        return pl.ds(pl.multiple_of((of_core * COLOURS + colour) * LANES, LANES), LANES)

    def slot(self, d, colour):
        dim = DIM_ORDER[colour][ZERO]
        where = [slice(None)] * THREE
        where[dim] = lax.rem(self.place[dim] + d, SIDE)
        return tuple(where)

    def rows_of(self, part):
        return pl.ds(self.offsets[part], self.heights[part])

    def swaps(self, piece):
        d, colour = self.pieces[piece]
        where, cols = self.slot(d, colour), self.columns(ONE - self.core, colour)
        n = len(self.sources)
        return [self.remote(piece * n + i, src.at[where + (rows, cols)], self.acc.at[(colour,) + where + (self.rows_of(i), slice(None))], (ONE - self.core, self.chip))
                for i, (src, rows) in enumerate(self.sources)]

    def loads(self, piece):
        d, colour = self.pieces[piece]
        where, cols = self.slot(d, colour), self.columns(self.core, colour)
        if self.resident:
            return []
        return [pltpu.make_async_copy(src.at[where + (rows, cols)], self.stage.at[piece % STAGES, :, :, self.rows_of(i), :], self.load_sem.at[piece % STAGES, i])
                for i, (src, rows) in enumerate(self.sources)]

    def split_rows(self, half):
        return pl.ds(ZERO, self.n_low) if half == ZERO else pl.ds(self.n_low, self.height - self.n_low)

    def block(self, colour, phase, d, half=None):
        order = DIM_ORDER[colour]
        where = [None, None, None]
        for done in order[:phase]:
            where[done] = self.place[done]
        where[order[phase]] = lax.rem(self.place[order[phase]] + d, SIDE)
        for i, rest in enumerate(sorted(order[phase + ONE:])):
            where[rest] = slice(None) if half is None or i > ZERO else pl.ds(TWO * half, TWO)
        rows = self.split_rows(half) if phase == TWO and half is not None else slice(None)
        return self.acc.at[(colour,) + tuple(where) + (rows, slice(None))]

    def got_half(self, colour, phase, direction, half):
        where = self.split_rows(half) if phase == TWO else pl.ds(TWO * half, TWO)
        return self.got[phase].at[colour, direction, where]

    def far_part(self, colour, phase, direction):
        if phase == TWO:
            return self.far[phase].at[colour, direction, pl.ds(ZERO, self.n_low if direction == ZERO else self.height - self.n_low), :]
        return self.far[phase].at[colour, direction]

    def ring(self, colour, phase, direction):
        shift = ONE - TWO * direction
        device = (self.core, chip_at(self.place, DIM_ORDER[colour][phase], shift))
        i = 12 * len(self.sources) + ((colour * THREE + phase) * TWO + direction) * THREE
        near = shift % SIDE
        return (self.remote(i, self.block(colour, phase, TWO, direction), self.far_part(colour, phase, direction), device),
                self.remote(i + ONE, self.block(colour, phase, near, ONE - direction), self.got_half(colour, phase, direction, ONE - direction), device),
                self.remote(i + TWO, self.block(colour, phase, near, direction), self.got_half(colour, phase, direction, direction), device))

    def gives(self, colour):
        n = len(self.sources)
        base = 12 * n + COLOURS * 18 + colour * n
        done = self.acc.at[colour, self.place[ZERO], self.place[ONE], self.place[TWO]]
        cols = self.columns(self.core, colour)
        pairs = [(done.at[self.rows_of(i), :], out.at[:, cols]) for i, out in enumerate(self.outs)]
        return [(self.remote(base + i, src, dst, (ONE - self.core, self.chip)), pltpu.make_async_copy(src, dst, self.load_sem.at[THREE + colour, i])) for i, (src, dst) in enumerate(pairs)]

    def add_into(self, dst, sources, n_lead):
        def body(i, _):
            total = dst[i]
            for src in sources:
                total = total + src[i]
            dst[i] = total
            return ZERO

        if n_lead == TWO:
            lax.fori_loop(ZERO, dst.shape[ZERO], body, ZERO)
        else:
            total = dst[ALL]
            for src in sources:
                total = total + src[ALL]
            dst[ALL] = total


    def begin(self):
        for piece in range(STAGES):
            for copy in self.loads(piece):
                copy.start()
        for piece in range(len(self.pieces)):
            for copy in self.swaps(piece):
                copy.start()

    def absorb(self, turn):
        for piece in range(turn * COLOURS, (turn + ONE) * COLOURS):
            d, colour = self.pieces[piece]
            for copy in self.loads(piece):
                copy.wait()
            for copy in self.swaps(piece):
                copy.wait_recv()
            where = self.slot(d, colour)
            if self.resident:
                for i, (src, rows) in enumerate(self.sources):
                    self.add_into(self.acc.at[(colour,) + where + (self.rows_of(i), slice(None))], [src.at[where + (rows, self.columns(self.core, colour))]], TWO)
            else:
                self.add_into(self.acc.at[(colour,) + where], [self.stage.at[piece % STAGES]], TWO)
            if piece + STAGES < len(self.pieces):
                for copy in self.loads(piece + STAGES):
                    copy.start()
            if turn == ZERO:
                for direction in range(TWO):
                    self.ring(colour, ZERO, direction)[ZERO].start()
            elif turn < THREE:
                self.ring(colour, ZERO, turn - ONE)[ONE].start()

    def relay(self, phase):
        for colour in range(COLOURS):
            for direction in range(TWO):
                far, _, fed = self.ring(colour, phase, direction)
                far.wait_recv()
                self.add_into(self.block(colour, phase, (ONE - TWO * direction) % SIDE, direction), [self.far_part(colour, phase, direction)], TWO - phase)
            for direction in range(TWO):
                self.ring(colour, phase, direction)[TWO].start()

    def settle(self, phase):
        for colour in range(COLOURS):
            for direction in range(TWO):
                _, own, fed = self.ring(colour, phase, direction)
                own.wait_recv()
                fed.wait_recv()
            self.add_into(self.block(colour, phase, ZERO), [self.got[phase].at[colour, direction] for direction in range(TWO)], TWO - phase)
            if phase < TWO:
                for kind in range(TWO):
                    for direction in range(TWO):
                        self.ring(colour, phase + ONE, direction)[kind].start()
            else:
                done = self.acc.at[colour, self.place[ZERO], self.place[ONE], self.place[TWO]]
                done[ALL] = done[ALL] * self.scale
                for give, keep in self.gives(colour):
                    keep.start()
                    give.start()

    def end(self):
        for colour in range(COLOURS):
            for give, keep in self.gives(colour):
                give.wait_recv()
                give.wait_send()
                keep.wait()
        for piece in range(len(self.pieces)):
            for copy in self.swaps(piece):
                copy.wait_send()
        for colour in range(COLOURS):
            for phase in range(THREE):
                for direction in range(TWO):
                    for copy in self.ring(colour, phase, direction):
                        copy.wait_send()


def rs_kernel(scale, *refs):
    scatter = Scatter(scale, [(ref, ZERO, ref.shape[THREE]) for ref in refs[:TWO]], refs[TWO:4], refs[4:])
    meet_neighbours(scatter.place)
    scatter.begin()
    for turn in range(THREE):
        scatter.absorb(turn)
    scatter.relay(ZERO)
    scatter.absorb(THREE)
    scatter.settle(ZERO)
    for phase in (ONE, TWO):
        scatter.relay(phase)
        scatter.settle(phase)
    scatter.end()


def as_torus(rows):
    return rows.reshape(SIDE, SIDE, SIDE, rows.shape[ZERO] // SIDE ** THREE, rows.shape[ONE])


def scatter_grads(g_attn, g_vec, scale):
    sources = [as_torus(g_attn), as_torus(g_vec)]
    heights = [src.shape[THREE] for src in sources]
    width = g_attn.shape[ONE]
    anywhere = pl.BlockSpec(memory_space=pl.ANY)
    return pl.pallas_call(
        functools.partial(rs_kernel, scale),
        in_specs=[anywhere] * TWO, out_specs=[anywhere] * TWO,
        out_shape=[jax.ShapeDtypeStruct((h, width), F32) for h in heights],
        scratch_shapes=Scatter.scratch_shapes(heights),
        compiler_params=pltpu.CompilerParams(collective_id=ONE, has_side_effects=True, vmem_limit_bytes=VMEM_BYTES),
        cost_estimate=pl.CostEstimate(flops=10 ** 9, bytes_accessed=8 * width * g_attn.shape[ZERO], transcendentals=ZERO),
        name='scatter_grads',
    )(*sources)


class Gather:
    def __init__(self, send_sem, recv_sem, base=ZERO):
        self.send_sem, self.recv_sem = send_sem, recv_sem
        self.used = base
        self.core, self.chip, self.place = lax.axis_index('dp'), lax.axis_index('fsdp'), torus_place()
        self.sibling = (ONE - self.core, self.chip)
        self.started = []

    def remote(self, src, dst, device):
        i = self.used
        self.used += ONE
        return pltpu.make_async_remote_copy(src_ref=src, dst_ref=dst, send_sem=self.send_sem.at[i], recv_sem=self.recv_sem.at[i], device_id=device, device_id_type=MESH_ID)

    def start(self, copy):
        copy.start()
        self.started.append(copy)

    def ring(self, colour, phase, view, own=None):
        order = DIM_ORDER[colour]
        dim = order[phase]
        have = sorted(order[:phase])

        def index(shift, half=None):
            where = [self.place[ZERO], self.place[ONE], self.place[TWO]]
            where[dim] = lax.rem(self.place[dim] + shift + SIDE, SIDE)
            for i, h in enumerate(have):
                where[h] = slice(None) if half is None or i > ZERO else pl.ds(TWO * half, TWO)
            return tuple(where)

        out = []
        for direction, shift in enumerate((ONE, -ONE)):
            device = (self.core, chip_at(self.place, dim, shift))
            half = direction if phase == ZERO else None
            near_dst = view(index(ZERO), None)
            out.append(dict(
                near=self.remote(near_dst if own is None else own, near_dst, device),
                far=self.remote(view(index(-shift, direction), half), view(index(-shift, direction), half), device),
                near_at=index(-shift), far_at=index(TWO, direction)))
        return out


def ag_kernel(attn_ref, ffn_ref, vec_ref, oattn_ref, planes_ref, vec_out, attn_v, send_sem, recv_sem, load_sem):
    net = Gather(send_sem, recv_sem)
    core, place = net.core, net.place
    rows, width = attn_ref.shape
    band = rows // (TWO * COLOURS)
    vec_high = vec_ref.shape[ZERO]
    stores, finals = [], []

    def band_rows(colour):
        return pl.ds(pl.multiple_of((core * COLOURS + colour) * band, band), band)

    def columns(half):
        return slice(None) if half is None else pl.ds(half * (width // TWO), width // TWO)

    def attn_view(colour):
        return lambda where, half: attn_v.at[where + (band_rows(colour), columns(half))]

    def ffn_view(colour):
        last = DIM_ORDER[colour][TWO]
        return lambda where, half: planes_ref.at[(colour,) + tuple(w for d, w in enumerate(where) if d != last) + (slice(None), columns(half))]

    def vec_view(where, half):
        return vec_out.at[where + (slice(None) if half is None else pl.ds(half * (vec_high // TWO), vec_high // TWO), slice(None))]

    colours = range(COLOURS)
    attn_own = [attn_ref.at[band_rows(colour), :] for colour in colours]
    ffn_own = [ffn_ref.at[band_rows(colour), :] for colour in colours]
    rings = {('attn', phase): [net.ring(colour, phase, attn_view(colour), attn_own[colour] if phase == ZERO else None) for colour in colours] for phase in range(THREE)}
    rings |= {('ffn', phase): [net.ring(colour, phase, ffn_view(colour), ffn_own[colour] if phase == ZERO else None) for colour in colours] for phase in range(TWO)}
    rings |= {('vec', phase): [net.ring(ONE, phase, vec_view, vec_ref if phase == ZERO else None)] for phase in range(THREE)}

    def publish(at):
        keep = pltpu.make_async_copy(attn_v.at[at], oattn_ref.at[at], load_sem.at[len(stores)])
        keep.start()
        stores.append(keep)
        give = net.remote(attn_v.at[at], oattn_ref.at[at], net.sibling)
        net.start(give)
        finals.append(give)

    def send_near(name, phase):
        for ring in rings.get((name, phase), ()):
            for way in ring:
                net.start(way['near'])

    def pass_on(name, phase):
        for ring in rings.get((name, phase), ()):
            for way in ring:
                way['near'].wait_recv()
                net.start(way['far'])
        if phase == TWO and name == 'attn':
            for colour in colours:
                for way in rings[(name, phase)][colour]:
                    publish(way['near_at'] + (band_rows(colour), slice(None)))

    def complete(name, phase):
        for colour, ring in enumerate(rings.get((name, phase), ())):
            for way in ring:
                way['far'].wait_recv()
            if phase < TWO and (name, phase + ONE) in rings:
                for way in rings[(name, phase + ONE)][colour]:
                    net.start(way['near'])
            if phase == TWO and name == 'attn':
                for way in ring:
                    publish(way['far_at'] + (band_rows(colour), slice(None)))
        if phase == ONE and name == 'attn':
            for colour in colours:
                last = DIM_ORDER[colour][TWO]
                publish(tuple(place[d] if d == last else slice(None) for d in range(THREE)) + (band_rows(colour), slice(None)))

    for colour in colours:
        attn_v[(place[ZERO], place[ONE], place[TWO]) + (band_rows(colour), slice(None))] = attn_ref[band_rows(colour), :]
        kept = [place[d] for d in range(THREE) if d != DIM_ORDER[colour][TWO]]
        planes_ref[(colour, kept[ZERO], kept[ONE])] = ffn_ref[band_rows(colour), :]
    vec_out[place[ZERO], place[ONE], place[TWO]] = vec_ref[ALL]
    meet_neighbours(place)
    names = ('attn', 'vec', 'ffn')
    for name in names:
        send_near(name, ZERO)
    for phase in range(THREE):
        for name in names:
            pass_on(name, phase)
        for name in names:
            complete(name, phase)
    for copy in finals:
        copy.wait_recv()
    for copy in net.started:
        copy.wait_send()
    for copy in stores:
        copy.wait()


def gather_params(attn_w, ffn_w, vec_rows):
    rows, width = attn_w.shape
    full = (SIDE, SIDE, SIDE, rows, width)
    n_copies = COLOURS * 4 * (THREE + TWO) + 4 * THREE + COLOURS * 5
    vmem = pl.BlockSpec(memory_space=pltpu.VMEM)
    return pl.pallas_call(
        ag_kernel,
        in_specs=[vmem] * THREE, out_specs=[pl.BlockSpec(memory_space=pl.ANY), vmem, vmem],
        out_shape=[jax.ShapeDtypeStruct(full, BF16), jax.ShapeDtypeStruct((COLOURS, SIDE, SIDE, rows // (TWO * COLOURS), width), BF16),
                   jax.ShapeDtypeStruct((SIDE, SIDE, SIDE) + vec_rows.shape, F32)],
        scratch_shapes=[pltpu.VMEM(full, BF16), pltpu.SemaphoreType.DMA((n_copies,)), pltpu.SemaphoreType.DMA((n_copies,)), pltpu.SemaphoreType.DMA((COLOURS * 5,))],
        compiler_params=pltpu.CompilerParams(collective_id=TWO, has_side_effects=True, vmem_limit_bytes=VMEM_BYTES),
        cost_estimate=pl.CostEstimate(flops=10 ** 9, bytes_accessed=4 * rows * width * SIDE ** THREE, transcendentals=ZERO),
        name='gather_params',
    )(attn_w, ffn_w, vec_rows)


class LastPhase:
    def __init__(self, planes, out, near, far, send_sem, recv_sem, load_sem):
        self.planes, self.out, self.near, self.far = planes, out, near, far
        self.send_sem, self.recv_sem, self.load_sem = send_sem, recv_sem, load_sem
        self.core, self.chip, self.place = lax.axis_index('dp'), lax.axis_index('fsdp'), torus_place()
        self.band = planes.shape[THREE]

    @staticmethod
    def scratch_shapes(planes):
        colours, side, _, band, width = planes.shape
        sems = [pltpu.SemaphoreType.DMA((9 * COLOURS,)), pltpu.SemaphoreType.DMA((9 * COLOURS,)), pltpu.SemaphoreType.DMA((5 * COLOURS,))]
        return [pltpu.VMEM((colours, TWO, side, side, band, width), BF16), pltpu.VMEM((colours, TWO, side // TWO, side, band, width), BF16)] + sems

    def remote(self, i, src, dst, device):
        return pltpu.make_async_remote_copy(src_ref=src, dst_ref=dst, send_sem=self.send_sem.at[i], recv_sem=self.recv_sem.at[i], device_id=device, device_id_type=MESH_ID)

    def ring(self, colour, direction):
        device = (self.core, chip_at(self.place, DIM_ORDER[colour][TWO], ONE - TWO * direction))
        i = 9 * colour + TWO * direction
        got = self.near.at[colour, direction]
        return (self.remote(i, self.planes.at[colour], got, device),
                self.remote(i + ONE, got.at[pl.ds(TWO * direction, TWO)], self.far.at[colour, direction], device))

    def shares(self, colour):
        last = DIM_ORDER[colour][TWO]
        rows = pl.ds(pl.multiple_of((self.core * COLOURS + colour) * self.band, self.band), self.band)
        views = [(self.planes.at[colour], ZERO, None)]
        views += [(self.near.at[colour, direction], TWO * direction - ONE, None) for direction in range(TWO)]
        views += [(self.far.at[colour, direction], TWO, direction) for direction in range(TWO)]
        out = []
        for n, (src, shift, half) in enumerate(views):
            where = [slice(None)] * THREE
            where[last] = lax.rem(self.place[last] + shift + SIDE, SIDE)
            if half is not None:
                where[min(d for d in range(THREE) if d != last)] = pl.ds(TWO * half, TWO)
            dst = self.out.at[tuple(where) + (rows, slice(None))]
            out.append((self.remote(9 * colour + 4 + n, src, dst, (ONE - self.core, self.chip)), pltpu.make_async_copy(src, dst, self.load_sem.at[5 * colour + n])))
        return out

    def share(self, colour, which):
        for n in which:
            give, keep = self.shares(colour)[n]
            give.start()
            keep.start()

    def begin(self):
        for colour in range(COLOURS):
            for direction in range(TWO):
                self.ring(colour, direction)[ZERO].start()
        for colour in range(COLOURS):
            self.share(colour, (ZERO,))

    def pass_on(self):
        for colour in range(COLOURS):
            for direction in range(TWO):
                near, far = self.ring(colour, direction)
                near.wait_recv()
                far.start()
            self.share(colour, (ONE, TWO))

    def complete(self):
        for colour in range(COLOURS):
            for direction in range(TWO):
                self.ring(colour, direction)[ONE].wait_recv()
            self.share(colour, (THREE, 4))

    def end(self):
        for colour in range(COLOURS):
            for give, keep in self.shares(colour):
                give.wait_recv()
                give.wait_send()
                keep.wait()
            for direction in range(TWO):
                for copy in self.ring(colour, direction):
                    copy.wait_send()


def dot(lhs, rhs, contract=((ONE,), (ZERO,))):
    return lax.dot_general(lhs, rhs, (contract, ((), ())), preferred_element_type=F32)


def dot_nt(lhs, rhs):
    return dot(lhs, rhs, ((ONE,), (ONE,)))


def dot_tn(lhs, rhs):
    return dot(lhs, rhs, ((ZERO,), (ZERO,)))


def norm_rows(resid, gain, shift):
    mean = jnp.mean(resid, axis=-ONE, keepdims=True)
    centred = resid - mean
    inv_std = lax.rsqrt(jnp.mean(centred * centred, axis=-ONE, keepdims=True) + LN_EPS)
    normed = centred * inv_std
    return (normed * gain + shift).astype(BF16), normed, inv_std


def norm_rows_bwd(d_out, normed, inv_std, gain):
    d_norm = d_out * gain
    return inv_std * (d_norm - jnp.mean(d_norm, axis=-ONE, keepdims=True) - normed * jnp.mean(d_norm * normed, axis=-ONE, keepdims=True))


def col_sum(values):
    return jnp.sum(values, axis=ZERO, keepdims=True)


def lane_row(head, dtype=BF16):
    lane = lax.broadcasted_iota(jnp.int32, (ONE, PAIR), ONE)
    return jnp.where((lane >= HEAD_DIM * head) & (lane < HEAD_DIM * (head + ONE)), 1.0, 0.0).astype(dtype)


def spare_lane(head):
    lane = lax.broadcasted_iota(jnp.int32, (ONE, PAIR), ONE)
    return jnp.where(lane == HEAD_DIM * (ONE - head), 1.0, 0.0)


def mask_fill(n_rows, n_valid):
    row = lax.broadcasted_iota(jnp.int32, (n_rows, PAIR), ZERO)
    return jnp.where(row >= n_valid, MASK_FILL, 0.0)


def head_masks(pair_q, pair_k, head, fill):
    q_f = pair_q * lane_row(head) + spare_lane(head).astype(BF16)
    k_f = pair_k * lane_row(head) + (fill * spare_lane(head)).astype(BF16)
    return q_f, k_f


def half_only(pair, head):
    return pair * lane_row(head)


def join_halves(first, second):
    lane = lax.broadcasted_iota(jnp.int32, first.shape, ONE)
    return jnp.where(lane < HEAD_DIM, first, second)


def score_blocks(n_heads, n_q, n_k, causal, step):
    if not causal:
        return [(head, ZERO, n_q, n_k) for head in range(n_heads)]
    return [(head, first, step, first + step) for head in range(n_heads) for first in range(ZERO, n_q, step)]


def scores_t(q_f, k_f, causal, first):
    s_t = dot_nt(k_f, q_f)
    if causal:
        key_i = lax.broadcasted_iota(jnp.int32, s_t.shape, ZERO)
        qry_i = lax.broadcasted_iota(jnp.int32, s_t.shape, ONE) + first
        s_t = jnp.where(key_i <= qry_i, s_t, MASK_FILL)
    return s_t


def pair_of(group, head):
    return group[:, head // TWO * PAIR:(head // TWO + ONE) * PAIR]


def masked_pairs(q_g, k_g, n_valid):
    fill = mask_fill(k_g.shape[ZERO], n_valid)
    cache = {}

    def get(head):
        if head not in cache:
            cache[head] = head_masks(pair_of(q_g, head), pair_of(k_g, head), head % TWO, fill)
        return cache[head]

    return get


def stack_heads(parts, n_heads):
    return jnp.concatenate([jnp.concatenate(parts[head], axis=ONE) for head in range(n_heads)], axis=ZERO)


def run_ahead(blocks, produce, transform, consume, delay):
    ahead = produce(blocks[ZERO])
    waiting = []
    for i, block in enumerate(blocks):
        now = ahead
        if i + ONE < len(blocks):
            ahead = produce(blocks[i + ONE])
        waiting.append((block, transform(block, now)))
        if len(waiting) > delay:
            consume(*waiting.pop(ZERO))
    for item in waiting:
        consume(*item)


def attend_group(q_g, k_g, v_g, n_valid, causal, lse_ref):
    n_heads = GROUP // HEAD_DIM
    o_parts = [[] for _ in range(n_heads)]
    v_t = v_g.T
    masked = masked_pairs(q_g, k_g, n_valid)

    def produce(block):
        head, first, n_q, n_k = block
        q_f, k_f = masked(head)
        return scores_t(q_f[first:first + n_q], k_f[:n_k], causal, first)

    def transform(block, s_t):
        head, first, n_q, n_k = block
        top = jnp.max(s_t, axis=ZERO, keepdims=True)
        e_t = jnp.exp(s_t - top)
        total = jnp.sum(e_t, axis=ZERO, keepdims=True)
        lse_ref[ZERO, ZERO, head:head + ONE, first:first + n_q] = top + jnp.log(total)
        return (e_t * (1.0 / total)).astype(BF16)

    def consume(block, p_t):
        head, first, n_q, n_k = block
        o_parts[head].append(dot(v_t[HEAD_DIM * head:HEAD_DIM * (head + ONE), :n_k], p_t))

    run_ahead(score_blocks(n_heads, q_g.shape[ZERO], k_g.shape[ZERO], causal, 128), produce, transform, consume, TWO)
    return stack_heads(o_parts, n_heads).T.astype(BF16)


def attend_group_bwd(d_o, q_g, k_g, v_g, n_valid, causal, lse_ref, between=None):
    n_heads = GROUP // HEAD_DIM
    k_t = k_g.T
    dq_t, dk_h, dv_h = [[] for _ in range(n_heads)], [None] * n_heads, [None] * n_heads
    masked = masked_pairs(q_g, k_g, n_valid)
    v_half = {}

    def produce(block):
        head, first, n_q, n_k = block
        q_f, k_f = masked(head)
        if head not in v_half:
            v_half[head] = half_only(pair_of(v_g, head), head % TWO)
        rows = slice(first, first + n_q)
        return scores_t(q_f[rows], k_f[:n_k], causal, first), dot_nt(v_half[head][:n_k], pair_of(d_o, head)[rows])

    def transform(block, products):
        head, first, n_q, n_k = block
        s_t, dp_t = products
        p_t = jnp.exp(s_t - lse_ref[ZERO, ZERO, head:head + ONE, first:first + n_q])
        weighted = p_t * dp_t
        return p_t.astype(BF16), (weighted - p_t * jnp.sum(weighted, axis=ZERO, keepdims=True)).astype(BF16)

    def grow(old, new):
        if old is None:
            return new
        n_old = old.shape[ZERO]
        return old + new if n_old == new.shape[ZERO] else jnp.concatenate([old + new[:n_old], new[n_old:]], axis=ZERO)

    def consume(block, operands):
        head, first, n_q, n_k = block
        p_b, ds_t = operands
        rows = slice(first, first + n_q)
        dv_h[head] = grow(dv_h[head], dot(p_b, pair_of(d_o, head)[rows]))
        dk_h[head] = grow(dk_h[head], dot(ds_t, pair_of(q_g, head)[rows]))
        dq_t[head].append(dot(k_t[HEAD_DIM * head:HEAD_DIM * (head + ONE), :n_k], ds_t))

    blocks = score_blocks(n_heads, q_g.shape[ZERO], k_g.shape[ZERO], causal, 256)
    if between is None:
        run_ahead(blocks, produce, transform, consume, ZERO)
    else:
        n_first = len(blocks) // TWO
        run_ahead(blocks[:n_first], produce, transform, consume, ZERO)
        between()
        run_ahead(blocks[n_first:], produce, transform, consume, ZERO)
    join = lambda parts: jnp.concatenate([join_halves(parts[h], parts[h + ONE]) for h in range(ZERO, n_heads, TWO)], axis=ONE)
    return stack_heads(dq_t, n_heads).T * 0.125, join(dk_h), join(dv_h)


def attn_fwd_kernel(causal, slots, guest, lens_ref, x_ref, kv_ref, wq_ref, wk_ref, wv_ref, w_all, bias_ref, rows_ref,
                    q_ref, k_ref, v_ref, o_ref, lse_ref, h_ref, normed_ref, inv_ref, o_all, wo_v, load_sem):
    q_row, k_row, v_row, o_row, gain_row, o_mat = slots
    sample, group = pl.program_id(ZERO), pl.program_id(ONE)
    d_model = wo_v.shape[ZERO]
    fetch = pltpu.make_async_copy(w_all.at[pl.ds(o_mat * d_model, d_model), :], wo_v, load_sem)

    @pl.when((sample == ZERO) & (group == ZERO))
    def _():
        fetch.start()

    turn = sample * pl.num_programs(ONE) + group
    if guest is not None:
        for where, steps in ((ZERO, (lambda: meet_neighbours(guest.place), guest.begin)), (THREE, (guest.pass_on,)), (5, (guest.complete,))):
            @pl.when(turn == where)
            def _():
                for step in steps:
                    step()

    x_b, kv_b = x_ref[ALL], kv_ref[ALL]
    q_g = ((dot(x_b, wq_ref[ALL]) + bias_ref[q_row:q_row + ONE, :]) * 0.125).astype(BF16)
    k_g = (dot(kv_b, wk_ref[ALL]) + bias_ref[k_row:k_row + ONE, :]).astype(BF16)
    v_g = (dot(kv_b, wv_ref[ALL]) + bias_ref[v_row:v_row + ONE, :]).astype(BF16)
    q_ref[ALL], k_ref[ALL], v_ref[ALL] = q_g, k_g, v_g
    o_g = attend_group(q_g, k_g, v_g, lens_ref[sample], causal, lse_ref)
    o_ref[ALL] = o_g
    o_all[:, pl.ds(pl.multiple_of(group * GROUP, GROUP), GROUP)] = o_g

    @pl.when((sample == ZERO) & (group == pl.num_programs(ONE) - ONE))
    def _():
        fetch.wait()

    @pl.when(group == pl.num_programs(ONE) - ONE)
    def _():
        resid = x_ref[ALL].astype(F32) + dot(o_all[ALL], wo_v[ALL]) + rows_ref[o_row:o_row + ONE, :]
        h_out, normed, inv_std = norm_rows(resid, rows_ref[gain_row:gain_row + ONE, :], rows_ref[gain_row + ONE:gain_row + TWO, :])
        h_ref[ALL], normed_ref[ALL], inv_ref[ALL] = h_out, normed, inv_std

    if guest is not None:
        @pl.when(turn == pl.num_programs(ZERO) * pl.num_programs(ONE) - ONE)
        def _():
            guest.end()


def attn_forward(x, kv, lens, attn_full, bias_rows, mats, slots, causal, planes=None, full_rows=None):
    d_model = x.shape[-ONE]
    n_batch = lens.shape[ZERO]
    n_q, n_k = x.shape[ZERO] // n_batch, kv.shape[ZERO] // n_batch
    n_groups = d_model // GROUP
    col = lambda mat: pl.BlockSpec((d_model, GROUP), lambda b, g: (mat, g))
    q_blk = pl.BlockSpec((n_q, GROUP), lambda b, g: (b, g))
    k_blk = pl.BlockSpec((n_k, GROUP), lambda b, g: (b, g))
    tok = lambda n: pl.BlockSpec((n, d_model), lambda b, g: (b, ZERO))
    n_heads_g = GROUP // HEAD_DIM
    out_shape = (
        jax.ShapeDtypeStruct(x.shape, BF16), jax.ShapeDtypeStruct(kv.shape, BF16), jax.ShapeDtypeStruct(kv.shape, BF16),
        jax.ShapeDtypeStruct(x.shape, BF16), jax.ShapeDtypeStruct((n_batch, n_groups, n_heads_g, n_q), F32),
        jax.ShapeDtypeStruct(x.shape, BF16), jax.ShapeDtypeStruct(x.shape, F32), jax.ShapeDtypeStruct((x.shape[ZERO], ONE), F32))
    kernel = functools.partial(attn_fwd_kernel, causal, slots + (mats[THREE],))
    in_specs = [pl.BlockSpec(memory_space=pltpu.SMEM), tok(n_q), tok(n_k), col(mats[ZERO]), col(mats[ONE]), col(mats[TWO]), pl.BlockSpec(memory_space=pl.ANY),
                pl.BlockSpec((bias_rows.shape[ZERO], GROUP), lambda b, g: (ZERO, g)), pl.BlockSpec(bias_rows.shape, lambda b, g: (ZERO, ZERO))]
    out_specs = [q_blk, k_blk, k_blk, q_blk, pl.BlockSpec((ONE, ONE, n_heads_g, n_q), lambda b, g: (b, g, ZERO, ZERO)),
                 tok(n_q), tok(n_q), pl.BlockSpec((n_q, ONE), lambda b, g: (b, ZERO))]
    scratch = [pltpu.VMEM((n_q, d_model), BF16), pltpu.VMEM((d_model, d_model), BF16), pltpu.SemaphoreType.DMA]
    args = [lens, x, kv, attn_full, attn_full, attn_full, attn_full, bias_rows, bias_rows]
    params = dict(vmem_limit_bytes=VMEM_BYTES, dimension_semantics=('arbitrary', 'arbitrary'))
    if planes is None:
        body = functools.partial(kernel, None)
    else:
        n_in, n_out, n_own = len(args), len(out_specs), len(scratch)

        def body(*refs):
            ins, held, outs, whole, rest = refs[:n_in], refs[n_in], refs[n_in + ONE:n_in + ONE + n_out], refs[n_in + ONE + n_out], refs[n_in + TWO + n_out:]
            kernel(LastPhase(held, whole, *rest[n_own:]), *ins, *outs, *rest[:n_own])

        in_specs.append(pl.BlockSpec(memory_space=pltpu.VMEM))
        args.append(planes)
        out_specs.append(pl.BlockSpec(memory_space=pl.ANY))
        out_shape += (jax.ShapeDtypeStruct((SIDE, SIDE, SIDE, full_rows // SIDE ** THREE, d_model), BF16),)
        scratch += LastPhase.scratch_shapes(planes)
        params |= dict(collective_id=5, has_side_effects=True)
    return pl.pallas_call(
        body, grid=(n_batch, n_groups), in_specs=in_specs, out_specs=out_specs, out_shape=out_shape, scratch_shapes=scratch,
        compiler_params=pltpu.CompilerParams(**params),
        cost_estimate=pl.CostEstimate(flops=TWO * d_model * d_model * (TWO * x.shape[ZERO] + TWO * kv.shape[ZERO]) + 16 * x.shape[ZERO] * n_k * d_model, bytes_accessed=20 * x.shape[ZERO] * d_model, transcendentals=ZERO),
        name='attn_fwd',
    )(*args)


def attn_bwd_kernel(causal, gain_row, mats, lhs_of, guest, lens_ref, dres_ref, wo_ref, w_all, q_ref, k_ref, v_ref, lse_ref,
                    rows_ref, normed_ref, inv_ref, lhs_refs, dx_ref, dkv_ref, sums_ref, tail_ref, grads_ref,
                    d_all, dk_all, dv_all, dres_all, w_v, lhs_vs, grad_v, load_sem):
    sample, group = pl.program_id(ZERO), pl.program_id(ONE)
    d_model = w_v.shape[ONE]
    n_q, n_k = q_ref.shape[ZERO], k_ref.shape[ZERO]
    last = pl.num_programs(ONE) - ONE
    fetches = [pltpu.make_async_copy(w_all.at[pl.ds(mat * d_model, d_model), :], w_v.at[i], load_sem.at[i]) for i, mat in enumerate(mats[:THREE])]
    lhs_fetch = lambda i: pltpu.make_async_copy(lhs_refs[i], lhs_vs[i % TWO].at[pl.ds(ZERO, lhs_refs[i].shape[ZERO]), :], load_sem.at[THREE + i])

    @pl.when((sample == ZERO) & (group == ZERO))
    def _():
        for fetch in fetches + [lhs_fetch(ZERO), lhs_fetch(ONE)]:
            fetch.start()

    turn = sample * pl.num_programs(ONE) + group
    guest(ZERO, TWO * turn)
    q_rows = pl.ds(pl.multiple_of(sample * n_q, n_q), n_q)
    k_rows = pl.ds(pl.multiple_of(sample * n_k, n_k), n_k)
    d_o = dot_nt(dres_ref[ALL].astype(BF16), wo_ref[ALL]).astype(BF16)
    dq, dk, dv = attend_group_bwd(d_o, q_ref[ALL], k_ref[ALL], v_ref[ALL], lens_ref[sample], causal, lse_ref, None if causal else functools.partial(guest, ONE, TWO * turn + ONE))
    cols = pl.ds(pl.multiple_of(group * GROUP, GROUP), GROUP)
    for i, (full, rows, value) in enumerate(((d_all, q_rows, dq), (dk_all, k_rows, dk), (dv_all, k_rows, dv))):
        sums_ref[ZERO, i:i + ONE, :] = col_sum(value)
        full[rows, cols] = value.astype(BF16)

    @pl.when(group == ZERO)
    def _():
        dres_all[q_rows, :] = dres_ref[ALL].astype(BF16)

    @pl.when((sample == ZERO) & (group == last))
    def _():
        for fetch in fetches:
            fetch.wait()

    @pl.when(group == last)
    def _():
        d_kv = dot_nt(dk_all[k_rows, :], w_v[ONE]) + dot_nt(dv_all[k_rows, :], w_v[TWO])
        d_h = dres_ref[ALL] + dot_nt(d_all[q_rows, :], w_v[ZERO])
        if causal:
            dx_ref[ALL] = (d_h + d_kv).astype(BF16)
            tail_ref[ALL] = jnp.zeros_like(tail_ref)
        else:
            dkv_ref[ALL] = d_kv.astype(BF16)
            normed = normed_ref[ALL]
            d_resid = norm_rows_bwd(d_h, normed, inv_ref[ALL], rows_ref[gain_row:gain_row + ONE, :])
            dx_ref[ALL] = d_resid
            tail_ref[ZERO, ZERO:ONE, :] = col_sum(d_resid)
            tail_ref[ZERO, ONE:TWO, :] = col_sum(d_h * normed)
            tail_ref[ZERO, TWO:THREE, :] = col_sum(d_h)

    @pl.when(turn == pl.num_programs(ZERO) * pl.num_programs(ONE) - ONE)
    def _():
        guest(TWO, 12)
        stores = []
        for i, (rhs, which) in enumerate(zip((d_all, dk_all, dv_all, dres_all), lhs_of)):
            if which not in lhs_of[:i]:
                lhs_fetch(which).wait()
            if i >= TWO:
                stores[i - TWO].wait()
            grad_v[i % TWO] = dot_tn(lhs_vs[which % TWO][pl.ds(ZERO, rhs.shape[ZERO]), :], rhs[ALL])
            store = pltpu.make_async_copy(grad_v.at[i % TWO], grads_ref.at[pl.ds(mats[i] * d_model, d_model), :], load_sem.at[6 + i])
            store.start()
            stores.append(store)
            if i == ZERO and len(lhs_refs) > TWO:
                lhs_fetch(TWO).start()
            guest(TWO, 13 + i)
        for store in stores[TWO:]:
            store.wait()


def scatter_guest(scatter, plan, parity, position):
    steps = dict(end=scatter.end) | {('relay', p): functools.partial(scatter.relay, p) for p in range(THREE)}
    steps |= {('settle', p): functools.partial(scatter.settle, p) for p in range(THREE)} | {turn: functools.partial(scatter.absorb, turn) for turn in range(SIDE)}
    if parity == TWO:
        for name in plan.get(position, ()):
            steps[name]()
        return
    if parity == ZERO:
        @pl.when(position == ZERO)
        def _():
            meet_neighbours(scatter.place)
            scatter.begin()
    for where, names in plan.items():
        if where < 12 and where % TWO == parity:
            @pl.when(position == where)
            def _():
                for name in names:
                    steps[name]()


def no_guest(parity, position):
    pass


def attn_backward(dres, q, k, v, lse, lens, attn_full, bias_rows, mats, causal, lhs_list, lhs_of, g_rows=None, scale=None, gain_row=ZERO, normed=None, inv_std=None, grads=None):
    d_model = q.shape[-ONE]
    n_batch = lens.shape[ZERO]
    n_q, n_k = q.shape[ZERO] // n_batch, k.shape[ZERO] // n_batch
    n_groups = d_model // GROUP
    row = lambda mat: pl.BlockSpec((GROUP, d_model), lambda b, g: (mat * n_groups + g, ZERO))
    q_blk = pl.BlockSpec((n_q, GROUP), lambda b, g: (b, g))
    k_blk = pl.BlockSpec((n_k, GROUP), lambda b, g: (b, g))
    tok = lambda n: pl.BlockSpec((n, d_model), lambda b, g: (b, ZERO))
    n_heads_g = GROUP // HEAD_DIM
    anywhere = pl.BlockSpec(memory_space=pl.ANY)
    in_specs = [pl.BlockSpec(memory_space=pltpu.SMEM), tok(n_q), row(mats[THREE]), anywhere, q_blk, k_blk, k_blk,
                pl.BlockSpec((ONE, ONE, n_heads_g, n_q), lambda b, g: (b, g, ZERO, ZERO)), pl.BlockSpec(bias_rows.shape, lambda b, g: (ZERO, ZERO))]
    args = [lens, dres, attn_full, attn_full, q, k, v, lse, bias_rows]
    tail_shape = jax.ShapeDtypeStruct((n_batch, 8, d_model), F32)
    out_shape = [jax.ShapeDtypeStruct(q.shape, BF16 if causal else F32)]
    out_specs = [tok(n_q)]
    if not causal:
        late = dict(pipeline_mode=pl.Buffered(ONE))
        in_specs += [pl.BlockSpec((n_q, d_model), lambda b, g: (b, ZERO), **late), pl.BlockSpec((n_q, ONE), lambda b, g: (b, ZERO), **late)]
        args += [normed, inv_std]
        out_shape.append(jax.ShapeDtypeStruct(k.shape, BF16))
        out_specs.append(tok(n_k))
    n_lhs_at = len(args)
    args += list(lhs_list)
    in_specs += [anywhere] * len(lhs_list)
    out_shape += [tail_shape, tail_shape, jax.ShapeDtypeStruct(attn_full.shape, F32)]
    out_specs += [pl.BlockSpec((ONE, 8, GROUP), lambda b, g: (b, ZERO, g)), pl.BlockSpec((ONE, 8, d_model), lambda b, g: (b, ZERO, ZERO)), anywhere]
    both = lambda n: pltpu.VMEM((n_batch * n, d_model), BF16)
    own = [both(n_q), both(n_k), both(n_k), both(n_q), pltpu.VMEM((THREE, d_model, d_model), BF16), pltpu.VMEM(lhs_list[ZERO].shape, BF16), pltpu.VMEM(lhs_list[ONE].shape, BF16),
           pltpu.VMEM((TWO, d_model, d_model), F32), pltpu.SemaphoreType.DMA((10,))]
    kernel = functools.partial(attn_bwd_kernel, causal, gain_row, mats, lhs_of)
    params = dict(vmem_limit_bytes=VMEM_BYTES, dimension_semantics=('arbitrary', 'arbitrary'))
    aliases = {}
    if causal:
        args.append(grads)
        in_specs.append(anywhere)
        aliases = {len(args) - ONE: len(out_shape) - ONE}
    else:
        args.append(as_torus(g_rows))
        in_specs.append(anywhere)
        n_rows = args[-ONE].shape[THREE]
        out_shape.append(jax.ShapeDtypeStruct((n_rows, d_model), F32))
        out_specs.append(anywhere)
        params |= dict(collective_id=THREE, has_side_effects=True, vmem_limit_bytes=67043328)
    scratch = own + ([] if causal else Scatter.scratch_shapes([n_rows]))
    n_in, n_out, n_own = len(args), len(out_shape), len(own)

    def body(*refs):
        ins, outs, rest = refs[:n_in], refs[n_in:n_in + n_out], refs[n_in + n_out:]
        lhs_refs, (d_all, dk_all, dv_all, dres_all, w_v, lhs_a, lhs_b, grad_v, load_sem) = ins[n_lhs_at:-ONE], rest[:n_own]
        held = (d_all, dk_all, dv_all, dres_all, w_v, (lhs_a, lhs_b), grad_v, load_sem)
        if causal:
            dx, sums, tail, grads_ref = outs
            kernel(no_guest, *ins[:n_lhs_at], None, None, lhs_refs, dx, None, sums, tail, grads_ref, *held)
        else:
            dx, dkv, sums, tail, grads_ref, total = outs
            scatter = Scatter(scale, [(ins[-ONE], ZERO, n_rows)], [total], rest[n_own:])
            kernel(functools.partial(scatter_guest, scatter, CROSS_PLAN), *ins[:n_lhs_at], lhs_refs, dx, dkv, sums, tail, grads_ref, *held)

    return pl.pallas_call(
        body, grid=(n_batch, n_groups), in_specs=in_specs, out_specs=out_specs, out_shape=out_shape, scratch_shapes=scratch, input_output_aliases=aliases,
        compiler_params=pltpu.CompilerParams(**params),
        cost_estimate=pl.CostEstimate(flops=TWO * d_model * d_model * (TWO * q.shape[ZERO] + TWO * k.shape[ZERO]) + 40 * q.shape[ZERO] * n_k * d_model, bytes_accessed=20 * q.shape[ZERO] * d_model, transcendentals=ZERO),
        name='attn_bwd',
    )(*args)


def ffn_kernel(n_blocks, h_ref, dy_ref, up_ref, down_ref, rows_ref, bias_ref, normed_ref, inv_ref,
               y_ref, grad_ref, dres2_ref, tail_ref, upsum_ref, gelu_all, dup_all, dres3_all, h_all):
    step = pl.program_id(ZERO)
    block, d_model = h_ref.shape
    n_square = gelu_all.shape[ONE] // d_model

    @pl.when(step < n_blocks)
    def _():
        rows = pl.ds(pl.multiple_of(step * block, block), block)
        h_b = h_ref[ALL]
        h_all[rows, :] = h_b
        up = dot_nt(h_b, up_ref[ALL]) + bias_ref[ALL]
        cdf = 0.5 * (1.0 + lax.erf(up * 0.7071067811865476))
        gelu = (up * cdf).astype(BF16)
        slope = cdf + up * (0.3989422804014327 * jnp.exp(-0.5 * up * up))
        gelu_all[rows, :] = gelu
        resid = h_b.astype(F32) + dot(gelu, down_ref[ALL]) + rows_ref[8:9, :]
        y_b, normed3, inv3 = norm_rows(resid, rows_ref[13:14, :], rows_ref[14:15, :])
        y_ref[ALL] = y_b
        dy = dy_ref[ALL].astype(F32)
        d_res3 = norm_rows_bwd(dy, normed3, inv3, rows_ref[13:14, :])
        d_res3_b = d_res3.astype(BF16)
        dres3_all[rows, :] = d_res3_b
        d_up = dot_nt(d_res3_b, down_ref[ALL]) * slope
        d_up_b = d_up.astype(BF16)
        dup_all[rows, :] = d_up_b
        d_h2 = d_res3 + dot(d_up_b, up_ref[ALL])
        normed2 = normed_ref[ALL]
        d_res2 = norm_rows_bwd(d_h2, normed2, inv_ref[ALL], rows_ref[11:12, :])
        dres2_ref[ALL] = d_res2
        tail = jnp.concatenate([col_sum(d_res2), col_sum(d_res3), col_sum(d_h2 * normed2), col_sum(d_h2), col_sum(dy * normed3), col_sum(dy),
                                jnp.zeros((TWO, dy.shape[ONE]), F32)], axis=ZERO)
        up_sum = col_sum(d_up)

        @pl.when(step == ZERO)
        def _():
            tail_ref[ALL] = tail
            upsum_ref[ALL] = up_sum

        @pl.when(step > ZERO)
        def _():
            tail_ref[ALL] += tail
            upsum_ref[ALL] += up_sum

    square = step - n_blocks
    cols = pl.ds(pl.multiple_of(lax.rem(square + TWO * n_square, n_square) * d_model, d_model), d_model)

    @pl.when((square >= ZERO) & (square < n_square))
    def _():
        grad_ref[ALL] = dot_tn(dup_all[:, cols], h_all[ALL])

    @pl.when(square >= n_square)
    def _():
        grad_ref[ALL] = dot_tn(gelu_all[:, cols], dres3_all[ALL])


def ffn_both(h2, dy, ffn_full, bias_rows, up_bias, normed2, inv2, block=256):
    n_tok, d_model = h2.shape
    ffn_dim = ffn_full.shape[ZERO] // TWO
    n_blocks = n_tok // block
    n_steps = n_blocks + ffn_full.shape[ZERO] // d_model
    at = lambda i: jnp.minimum(i, n_blocks - ONE)
    tok = pl.BlockSpec((block, d_model), lambda i: (at(i), ZERO))
    once = lambda shape, idx: pl.BlockSpec(shape, lambda i: idx, pipeline_mode=pl.Buffered(ONE))
    return pl.pallas_call(
        functools.partial(ffn_kernel, n_blocks), grid=(n_steps,),
        in_specs=[tok, tok, once((ffn_dim, d_model), (ZERO, ZERO)), once((ffn_dim, d_model), (ONE, ZERO)), once(bias_rows.shape, (ZERO, ZERO)), once((ONE, ffn_dim), (ZERO, ZERO)),
                  tok, pl.BlockSpec((block, ONE), lambda i: (at(i), ZERO))],
        out_specs=[tok, pl.BlockSpec((d_model, d_model), lambda i: (jnp.maximum(i - n_blocks, ZERO), ZERO)), tok, pl.BlockSpec((8, d_model), lambda i: (ZERO, ZERO)), pl.BlockSpec((ONE, ffn_dim), lambda i: (ZERO, ZERO))],
        out_shape=[jax.ShapeDtypeStruct(h2.shape, BF16), jax.ShapeDtypeStruct(ffn_full.shape, F32), jax.ShapeDtypeStruct(h2.shape, F32),
                   jax.ShapeDtypeStruct((8, d_model), F32), jax.ShapeDtypeStruct((ONE, ffn_dim), F32)],
        scratch_shapes=[pltpu.VMEM((n_tok, ffn_dim), BF16), pltpu.VMEM((n_tok, ffn_dim), BF16), pltpu.VMEM((n_tok, d_model), BF16), pltpu.VMEM((n_tok, d_model), BF16)],
        compiler_params=pltpu.CompilerParams(vmem_limit_bytes=VMEM_BYTES, dimension_semantics=('arbitrary',)),
        cost_estimate=pl.CostEstimate(flops=12 * n_tok * d_model * ffn_dim, bytes_accessed=30 * n_tok * d_model, transcendentals=ZERO),
        name='ffn_both',
    )(h2, dy, ffn_full, ffn_full, bias_rows, up_bias, normed2, inv2)


CROSS_PLAN = {ONE: (ZERO,), TWO: (ONE,), THREE: (TWO,), 4: (THREE,), 5: (('relay', ZERO),), 9: (('settle', ZERO),), 11: (('relay', ONE),), 12: (('settle', ONE),), 13: (('relay', TWO),), 15: (('settle', TWO),), 16: ('end',)}


def solution(mesh):
    n_fsdp = mesh.shape['fsdp']
    n_dp = mesh.shape['dp']
    batch_axes = ('dp', 'fsdp')
    act_spec = P(batch_axes, None, None)
    len_spec = P(batch_axes)
    row_spec = P('fsdp', None)
    vec_spec = P('fsdp')

    def device_step(dec_in, enc_out, src_lens, tgt_lens, y_cot, attn_w, ffn_w, vec_params):
        d_model, n_vec = dec_in.shape[TWO], vec_params.shape[ZERO]
        scale = 1.0 / (dec_in.shape[ZERO] * dec_in.shape[ONE] * n_fsdp * n_dp)
        x, enc, dy = (a.reshape(-ONE, d_model) for a in (dec_in, enc_out, y_cot))
        vec_rows = jnp.pad(vec_params.astype(F32), (ZERO, 16 * LANES - n_vec)).reshape(16, LANES)
        attn_tiles, planes, vec_tiles = gather_params(attn_w, ffn_w, vec_rows)
        attn_full = attn_tiles.reshape(-ONE, d_model)
        vec_f = vec_tiles.reshape(n_fsdp, 16, LANES)[:, :TWO].reshape(n_fsdp, TWO * LANES)[:, :n_vec].reshape(-ONE)
        bias_rows = jnp.pad(vec_f[:15 * d_model].reshape(15, d_model), ((ZERO, ONE), (ZERO, ZERO)))
        up_bias = vec_f[15 * d_model:].reshape(ONE, -ONE)
        q1, k1, v1, o1, lse1, h1, normed1, inv1 = attn_forward(x, x, tgt_lens, attn_full, bias_rows, (ZERO, ONE, TWO, THREE), (ZERO, ONE, TWO, THREE, 9), True)
        q2, k2, v2, o2, lse2, h2, normed2, inv2, ffn_tiles = attn_forward(h1, enc, src_lens, attn_full, bias_rows, (4, 5, 6, 7), (4, 5, 6, 7, 11), False, planes, ffn_w.shape[ZERO] * n_fsdp)
        ffn_full = ffn_tiles.reshape(-ONE, d_model)
        y, g_ffn, d_res2, ffn_tail, up_sum = ffn_both(h2, dy, ffn_full, bias_rows, up_bias, normed2, inv2)
        d_res1, d_enc, sums2, tail2, grads, ffn_out = attn_backward(d_res2, q2, k2, v2, lse2, src_lens, attn_full, bias_rows, (4, 5, 6, 7), False, (h1, enc, o2), (ZERO, ONE, ONE, TWO), g_ffn, scale, 9, normed1, inv1)
        d_x, sums1, _, grads = attn_backward(d_res1, q1, k1, v1, lse1, tgt_lens, attn_full, bias_rows, (ZERO, ONE, TWO, THREE), True, (x, o1), (ZERO, ZERO, ZERO, ONE), grads=grads)
        s1, s2, t2 = jnp.sum(sums1, axis=ZERO), jnp.sum(sums2, axis=ZERO), jnp.sum(tail2, axis=ZERO)
        g_vec = jnp.concatenate([s1[ZERO:THREE].reshape(-ONE), t2[ZERO], s2[ZERO:THREE].reshape(-ONE), ffn_tail[ZERO], ffn_tail[ONE], t2[ONE], t2[TWO], ffn_tail[TWO], ffn_tail[THREE], ffn_tail[4], ffn_tail[5], up_sum[ZERO]])
        g_rows = jnp.pad(g_vec.reshape(n_fsdp, ONE, n_vec), ((ZERO, ZERO), (ZERO, 7), (ZERO, d_model - n_vec))).reshape(n_fsdp * 8, -ONE)
        attn_out, vec_out = scatter_grads(grads, g_rows, scale)
        return y.reshape(dec_in.shape), d_x.reshape(dec_in.shape), d_enc.reshape(enc_out.shape), attn_out, ffn_out, vec_out[ZERO, :n_vec]

    return jax.shard_map(device_step, mesh=mesh, in_specs=(act_spec, act_spec, len_spec, len_spec, act_spec, row_spec, row_spec, vec_spec), out_specs=(act_spec, act_spec, act_spec, row_spec, row_spec, vec_spec), check_vma=False)
```

```python
import functools
import jax
import jax.numpy as jnp
from jax import lax
from jax.experimental import pallas as pl
from jax.experimental.pallas import tpu as pltpu
from jax.sharding import PartitionSpec as P

ZERO, ONE, TWO, THREE = range(4)
ALL = ...
HEAD_DIM = 64
LN_EPS = 1e-5
MASK_FILL = -1e30
VMEM_BYTES = 60 * 1024 * 1024
F32 = jnp.float32
BF16 = jnp.bfloat16
GROUP = 256
PAIR = 128


SIDE = 4
LANES = 128
COLOURS = THREE
STAGES = TWO
DIM_ORDER = ((TWO, ONE, ZERO), (ONE, ZERO, TWO), (ZERO, TWO, ONE))
MESH_ID = pl.DeviceIdType.MESH


def torus_place():
    chip = lax.axis_index('fsdp')
    return (chip // (SIDE * SIDE), lax.rem(chip // SIDE, SIDE), lax.rem(chip, SIDE))


def chip_at(place, dim, shift):
    moved = [lax.rem(p + shift + SIDE, SIDE) if d == dim else p for d, p in enumerate(place)]
    return (moved[ZERO] * SIDE + moved[ONE]) * SIDE + moved[TWO]


def meet_neighbours(place):
    barrier = pltpu.get_barrier_semaphore()
    core = lax.axis_index('dp')
    for dim in range(THREE):
        for shift in (ONE, -ONE):
            pl.semaphore_signal(barrier, inc=ONE, device_id=(core, chip_at(place, dim, shift)), device_id_type=MESH_ID)
    pl.semaphore_signal(barrier, inc=ONE, device_id=(ONE - core, lax.axis_index('fsdp')), device_id_type=MESH_ID)
    pl.semaphore_wait(barrier, 7)


class Scatter:
    def __init__(self, scale, sources, outs, scratch, resident=False):
        self.scale, self.outs, self.resident = scale, outs, resident
        self.sources = [(ref, pl.ds(first, n)) for ref, first, n in sources]
        (self.acc, g1, d1, g2, d2, g3, d3, self.send_sem, self.recv_sem, self.load_sem, *stage) = scratch
        self.stage = None if resident else stage[ZERO]
        self.got, self.far = (g1, g2, g3), (d1, d2, d3)
        self.heights = [n for _, _, n in sources]
        self.offsets = [sum(self.heights[:i]) for i in range(len(sources))]
        self.height = sum(self.heights)
        self.n_low = self.heights[ZERO] // TWO
        self.core, self.chip, self.place = lax.axis_index('dp'), lax.axis_index('fsdp'), torus_place()
        self.pieces = [(d, colour) for d in (TWO, ONE, THREE, ZERO) for colour in range(COLOURS)]

    @staticmethod
    def scratch_shapes(heights, resident=False):
        h = sum(heights)
        n_low = heights[ZERO] // TWO
        buf = lambda *shape: pltpu.VMEM((COLOURS,) + shape + (LANES,), F32)
        n = Scatter.n_copies(len(heights))
        return [buf(SIDE, SIDE, SIDE, h), buf(TWO, SIDE, SIDE, h), buf(TWO, TWO, SIDE, h), buf(TWO, SIDE, h), buf(TWO, TWO, h), buf(TWO, h), buf(TWO, max(n_low, h - n_low)),
                pltpu.SemaphoreType.DMA((n,)), pltpu.SemaphoreType.DMA((n,)), pltpu.SemaphoreType.DMA((THREE + COLOURS, len(heights)))] + (
                    [] if resident else [pltpu.VMEM((STAGES, SIDE, SIDE, h, LANES), F32)])

    @staticmethod
    def n_copies(n_parts):
        return 12 * n_parts + COLOURS * 18 + COLOURS * n_parts

    def remote(self, i, src, dst, device):
        return pltpu.make_async_remote_copy(src_ref=src, dst_ref=dst, send_sem=self.send_sem.at[i], recv_sem=self.recv_sem.at[i], device_id=device, device_id_type=MESH_ID)

    def columns(self, of_core, colour):
        return pl.ds(pl.multiple_of((of_core * COLOURS + colour) * LANES, LANES), LANES)

    def slot(self, d, colour):
        dim = DIM_ORDER[colour][ZERO]
        where = [slice(None)] * THREE
        where[dim] = lax.rem(self.place[dim] + d, SIDE)
        return tuple(where)

    def rows_of(self, part):
        return pl.ds(self.offsets[part], self.heights[part])

    def swaps(self, piece):
        d, colour = self.pieces[piece]
        where, cols = self.slot(d, colour), self.columns(ONE - self.core, colour)
        n = len(self.sources)
        return [self.remote(piece * n + i, src.at[where + (rows, cols)], self.acc.at[(colour,) + where + (self.rows_of(i), slice(None))], (ONE - self.core, self.chip))
                for i, (src, rows) in enumerate(self.sources)]

    def loads(self, piece):
        d, colour = self.pieces[piece]
        where, cols = self.slot(d, colour), self.columns(self.core, colour)
        if self.resident:
            return []
        return [pltpu.make_async_copy(src.at[where + (rows, cols)], self.stage.at[piece % STAGES, :, :, self.rows_of(i), :], self.load_sem.at[piece % STAGES, i])
                for i, (src, rows) in enumerate(self.sources)]

    def split_rows(self, half):
        return pl.ds(ZERO, self.n_low) if half == ZERO else pl.ds(self.n_low, self.height - self.n_low)

    def block(self, colour, phase, d, half=None):
        order = DIM_ORDER[colour]
        where = [None, None, None]
        for done in order[:phase]:
            where[done] = self.place[done]
        where[order[phase]] = lax.rem(self.place[order[phase]] + d, SIDE)
        for i, rest in enumerate(sorted(order[phase + ONE:])):
            where[rest] = slice(None) if half is None or i > ZERO else pl.ds(TWO * half, TWO)
        rows = self.split_rows(half) if phase == TWO and half is not None else slice(None)
        return self.acc.at[(colour,) + tuple(where) + (rows, slice(None))]

    def got_half(self, colour, phase, direction, half):
        where = self.split_rows(half) if phase == TWO else pl.ds(TWO * half, TWO)
        return self.got[phase].at[colour, direction, where]

    def far_part(self, colour, phase, direction):
        if phase == TWO:
            return self.far[phase].at[colour, direction, pl.ds(ZERO, self.n_low if direction == ZERO else self.height - self.n_low), :]
        return self.far[phase].at[colour, direction]

    def ring(self, colour, phase, direction):
        shift = ONE - TWO * direction
        device = (self.core, chip_at(self.place, DIM_ORDER[colour][phase], shift))
        i = 12 * len(self.sources) + ((colour * THREE + phase) * TWO + direction) * THREE
        near = shift % SIDE
        return (self.remote(i, self.block(colour, phase, TWO, direction), self.far_part(colour, phase, direction), device),
                self.remote(i + ONE, self.block(colour, phase, near, ONE - direction), self.got_half(colour, phase, direction, ONE - direction), device),
                self.remote(i + TWO, self.block(colour, phase, near, direction), self.got_half(colour, phase, direction, direction), device))

    def gives(self, colour):
        n = len(self.sources)
        base = 12 * n + COLOURS * 18 + colour * n
        done = self.acc.at[colour, self.place[ZERO], self.place[ONE], self.place[TWO]]
        cols = self.columns(self.core, colour)
        pairs = [(done.at[self.rows_of(i), :], out.at[:, cols]) for i, out in enumerate(self.outs)]
        return [(self.remote(base + i, src, dst, (ONE - self.core, self.chip)), pltpu.make_async_copy(src, dst, self.load_sem.at[THREE + colour, i])) for i, (src, dst) in enumerate(pairs)]

    def add_into(self, dst, sources, n_lead):
        def body(i, _):
            total = dst[i]
            for src in sources:
                total = total + src[i]
            dst[i] = total
            return ZERO

        if n_lead == TWO:
            lax.fori_loop(ZERO, dst.shape[ZERO], body, ZERO)
        else:
            total = dst[ALL]
            for src in sources:
                total = total + src[ALL]
            dst[ALL] = total


    def begin(self):
        for piece in range(STAGES):
            for copy in self.loads(piece):
                copy.start()
        for piece in range(len(self.pieces)):
            for copy in self.swaps(piece):
                copy.start()

    def absorb(self, turn):
        for piece in range(turn * COLOURS, (turn + ONE) * COLOURS):
            d, colour = self.pieces[piece]
            for copy in self.loads(piece):
                copy.wait()
            for copy in self.swaps(piece):
                copy.wait_recv()
            where = self.slot(d, colour)
            if self.resident:
                for i, (src, rows) in enumerate(self.sources):
                    self.add_into(self.acc.at[(colour,) + where + (self.rows_of(i), slice(None))], [src.at[where + (rows, self.columns(self.core, colour))]], TWO)
            else:
                self.add_into(self.acc.at[(colour,) + where], [self.stage.at[piece % STAGES]], TWO)
            if piece + STAGES < len(self.pieces):
                for copy in self.loads(piece + STAGES):
                    copy.start()
            if turn == ZERO:
                for direction in range(TWO):
                    self.ring(colour, ZERO, direction)[ZERO].start()
            elif turn < THREE:
                self.ring(colour, ZERO, turn - ONE)[ONE].start()

    def relay(self, phase):
        for colour in range(COLOURS):
            for direction in range(TWO):
                far, _, fed = self.ring(colour, phase, direction)
                far.wait_recv()
                self.add_into(self.block(colour, phase, (ONE - TWO * direction) % SIDE, direction), [self.far_part(colour, phase, direction)], TWO - phase)
            for direction in range(TWO):
                self.ring(colour, phase, direction)[TWO].start()

    def settle(self, phase):
        for colour in range(COLOURS):
            for direction in range(TWO):
                _, own, fed = self.ring(colour, phase, direction)
                own.wait_recv()
                fed.wait_recv()
            self.add_into(self.block(colour, phase, ZERO), [self.got[phase].at[colour, direction] for direction in range(TWO)], TWO - phase)
            if phase < TWO:
                for kind in range(TWO):
                    for direction in range(TWO):
                        self.ring(colour, phase + ONE, direction)[kind].start()
            else:
                done = self.acc.at[colour, self.place[ZERO], self.place[ONE], self.place[TWO]]
                done[ALL] = done[ALL] * self.scale
                for give, keep in self.gives(colour):
                    keep.start()
                    give.start()

    def end(self):
        for colour in range(COLOURS):
            for give, keep in self.gives(colour):
                give.wait_recv()
                give.wait_send()
                keep.wait()
        for piece in range(len(self.pieces)):
            for copy in self.swaps(piece):
                copy.wait_send()
        for colour in range(COLOURS):
            for phase in range(THREE):
                for direction in range(TWO):
                    for copy in self.ring(colour, phase, direction):
                        copy.wait_send()


def rs_kernel(scale, *refs):
    scatter = Scatter(scale, [(ref, ZERO, ref.shape[THREE]) for ref in refs[:TWO]], refs[TWO:4], refs[4:])
    meet_neighbours(scatter.place)
    scatter.begin()
    for turn in range(THREE):
        scatter.absorb(turn)
    scatter.relay(ZERO)
    scatter.absorb(THREE)
    scatter.settle(ZERO)
    for phase in (ONE, TWO):
        scatter.relay(phase)
        scatter.settle(phase)
    scatter.end()


def as_torus(rows):
    return rows.reshape(SIDE, SIDE, SIDE, rows.shape[ZERO] // SIDE ** THREE, rows.shape[ONE])


def scatter_grads(g_attn, g_vec, scale):
    sources = [as_torus(g_attn), as_torus(g_vec)]
    heights = [src.shape[THREE] for src in sources]
    width = g_attn.shape[ONE]
    anywhere = pl.BlockSpec(memory_space=pl.ANY)
    return pl.pallas_call(
        functools.partial(rs_kernel, scale),
        in_specs=[anywhere] * TWO, out_specs=[anywhere] * TWO,
        out_shape=[jax.ShapeDtypeStruct((h, width), F32) for h in heights],
        scratch_shapes=Scatter.scratch_shapes(heights),
        compiler_params=pltpu.CompilerParams(collective_id=ONE, has_side_effects=True, vmem_limit_bytes=VMEM_BYTES),
        cost_estimate=pl.CostEstimate(flops=10 ** 9, bytes_accessed=8 * width * g_attn.shape[ZERO], transcendentals=ZERO),
        name='scatter_grads',
    )(*sources)


class Gather:
    def __init__(self, send_sem, recv_sem, base=ZERO):
        self.send_sem, self.recv_sem = send_sem, recv_sem
        self.used = base
        self.core, self.chip, self.place = lax.axis_index('dp'), lax.axis_index('fsdp'), torus_place()
        self.sibling = (ONE - self.core, self.chip)
        self.started = []

    def remote(self, src, dst, device):
        i = self.used
        self.used += ONE
        return pltpu.make_async_remote_copy(src_ref=src, dst_ref=dst, send_sem=self.send_sem.at[i], recv_sem=self.recv_sem.at[i], device_id=device, device_id_type=MESH_ID)

    def start(self, copy):
        copy.start()
        self.started.append(copy)

    def ring(self, colour, phase, view, own=None, split=False):
        order = DIM_ORDER[colour]
        dim = order[phase]
        have = sorted(order[:phase])

        def index(shift, half=None):
            where = [self.place[ZERO], self.place[ONE], self.place[TWO]]
            where[dim] = lax.rem(self.place[dim] + shift + SIDE, SIDE)
            for i, h in enumerate(have):
                where[h] = slice(None) if half is None or i > ZERO else pl.ds(TWO * half, TWO)
            return tuple(where)

        out = []
        for direction, shift in enumerate((ONE, -ONE)):
            device = (self.core, chip_at(self.place, dim, shift))
            half = direction if phase == ZERO else None
            near_dst = view(index(ZERO), None)
            if split:
                near = [self.remote(view(index(ZERO, h), None), view(index(ZERO, h), None), device) for h in (direction, ONE - direction)]
            else:
                near = [self.remote(near_dst if own is None else own, near_dst, device)]
            out.append(dict(
                near=near,
                far=self.remote(view(index(-shift, direction), half), view(index(-shift, direction), half), device),
                near_at=index(-shift), far_at=index(TWO, direction)))
        return out


def ag_kernel(attn_ref, ffn_ref, vec_ref, oattn_ref, planes_ref, vec_out, attn_v, send_sem, recv_sem, load_sem):
    net = Gather(send_sem, recv_sem)
    core, place = net.core, net.place
    rows, width = attn_ref.shape
    band = rows // (TWO * COLOURS)
    vec_high = vec_ref.shape[ZERO]
    stores, finals = [], []

    def band_rows(colour):
        return pl.ds(pl.multiple_of((core * COLOURS + colour) * band, band), band)

    def columns(half):
        return slice(None) if half is None else pl.ds(half * (width // TWO), width // TWO)

    def attn_view(colour):
        return lambda where, half: attn_v.at[where + (band_rows(colour), columns(half))]

    def ffn_view(colour):
        last = DIM_ORDER[colour][TWO]
        return lambda where, half: planes_ref.at[(colour,) + tuple(w for d, w in enumerate(where) if d != last) + (slice(None), columns(half))]

    def vec_view(where, half):
        return vec_out.at[where + (slice(None) if half is None else pl.ds(half * (vec_high // TWO), vec_high // TWO), slice(None))]

    colours = range(COLOURS)
    attn_own = [attn_ref.at[band_rows(colour), :] for colour in colours]
    ffn_own = [ffn_ref.at[band_rows(colour), :] for colour in colours]
    rings = {('attn', phase): [net.ring(colour, phase, attn_view(colour), attn_own[colour] if phase == ZERO else None, phase > ZERO) for colour in colours] for phase in range(THREE)}
    rings |= {('ffn', phase): [net.ring(colour, phase, ffn_view(colour), ffn_own[colour] if phase == ZERO else None, phase > ZERO) for colour in colours] for phase in range(TWO)}
    rings |= {('vec', phase): [net.ring(ONE, phase, vec_view, vec_ref if phase == ZERO else None)] for phase in range(THREE)}

    def publish(at):
        keep = pltpu.make_async_copy(attn_v.at[at], oattn_ref.at[at], load_sem.at[len(stores)])
        keep.start()
        stores.append(keep)
        give = net.remote(attn_v.at[at], oattn_ref.at[at], net.sibling)
        net.start(give)
        finals.append(give)

    def send_near(name, phase):
        for ring in rings.get((name, phase), ()):
            for way in ring:
                for copy in way['near']:
                    net.start(copy)

    def pass_on(name, phase):
        for ring in rings.get((name, phase), ()):
            for way in ring:
                way['near'][ZERO].wait_recv()
                net.start(way['far'])
        if phase == TWO and name == 'attn':
            for colour in colours:
                for way in rings[(name, phase)][colour]:
                    way['near'][ONE].wait_recv()
                    publish(way['near_at'] + (band_rows(colour), slice(None)))

    def complete(name, phase):
        for colour, ring in enumerate(rings.get((name, phase), ())):
            for way in ring:
                way['far'].wait_recv()
                if phase == ONE and name != 'vec':
                    way['near'][ONE].wait_recv()
            if phase < TWO and (name, phase + ONE) in rings:
                for way in rings[(name, phase + ONE)][colour]:
                    for copy in way['near']:
                        net.start(copy)
            if phase == TWO and name == 'attn':
                for way in ring:
                    publish(way['far_at'] + (band_rows(colour), slice(None)))
        if phase == ONE and name == 'attn':
            for colour in colours:
                last = DIM_ORDER[colour][TWO]
                publish(tuple(place[d] if d == last else slice(None) for d in range(THREE)) + (band_rows(colour), slice(None)))

    for colour in colours:
        attn_v[(place[ZERO], place[ONE], place[TWO]) + (band_rows(colour), slice(None))] = attn_ref[band_rows(colour), :]
        kept = [place[d] for d in range(THREE) if d != DIM_ORDER[colour][TWO]]
        planes_ref[(colour, kept[ZERO], kept[ONE])] = ffn_ref[band_rows(colour), :]
    vec_out[place[ZERO], place[ONE], place[TWO]] = vec_ref[ALL]
    meet_neighbours(place)
    names = ('attn', 'vec', 'ffn')
    for name in names:
        send_near(name, ZERO)
    for phase in range(THREE):
        for name in names:
            pass_on(name, phase)
        for name in names:
            complete(name, phase)
    for copy in finals:
        copy.wait_recv()
    for copy in net.started:
        copy.wait_send()
    for copy in stores:
        copy.wait()


def gather_params(attn_w, ffn_w, vec_rows):
    rows, width = attn_w.shape
    full = (SIDE, SIDE, SIDE, rows, width)
    n_copies = COLOURS * (4 * TWO + 6 * THREE) + 4 * THREE + COLOURS * 5
    vmem = pl.BlockSpec(memory_space=pltpu.VMEM)
    return pl.pallas_call(
        ag_kernel,
        in_specs=[vmem] * THREE, out_specs=[pl.BlockSpec(memory_space=pl.ANY), vmem, vmem],
        out_shape=[jax.ShapeDtypeStruct(full, BF16), jax.ShapeDtypeStruct((COLOURS, SIDE, SIDE, rows // (TWO * COLOURS), width), BF16),
                   jax.ShapeDtypeStruct((SIDE, SIDE, SIDE) + vec_rows.shape, F32)],
        scratch_shapes=[pltpu.VMEM(full, BF16), pltpu.SemaphoreType.DMA((n_copies,)), pltpu.SemaphoreType.DMA((n_copies,)), pltpu.SemaphoreType.DMA((COLOURS * 5,))],
        compiler_params=pltpu.CompilerParams(collective_id=TWO, has_side_effects=True, vmem_limit_bytes=VMEM_BYTES),
        cost_estimate=pl.CostEstimate(flops=10 ** 9, bytes_accessed=4 * rows * width * SIDE ** THREE, transcendentals=ZERO),
        name='gather_params',
    )(attn_w, ffn_w, vec_rows)


class LastPhase:
    def __init__(self, planes, out, near, far, send_sem, recv_sem, load_sem):
        self.planes, self.out, self.near, self.far = planes, out, near, far
        self.send_sem, self.recv_sem, self.load_sem = send_sem, recv_sem, load_sem
        self.core, self.chip, self.place = lax.axis_index('dp'), lax.axis_index('fsdp'), torus_place()
        self.band = planes.shape[THREE]

    @staticmethod
    def scratch_shapes(planes):
        colours, side, _, band, width = planes.shape
        sems = [pltpu.SemaphoreType.DMA((11 * COLOURS,)), pltpu.SemaphoreType.DMA((11 * COLOURS,)), pltpu.SemaphoreType.DMA((5 * COLOURS,))]
        return [pltpu.VMEM((colours, TWO, side, side, band, width), BF16), pltpu.VMEM((colours, TWO, side // TWO, side, band, width), BF16)] + sems

    def remote(self, i, src, dst, device):
        return pltpu.make_async_remote_copy(src_ref=src, dst_ref=dst, send_sem=self.send_sem.at[i], recv_sem=self.recv_sem.at[i], device_id=device, device_id_type=MESH_ID)

    def ring(self, colour, direction):
        device = (self.core, chip_at(self.place, DIM_ORDER[colour][TWO], ONE - TWO * direction))
        i = 11 * colour + THREE * direction
        got = self.near.at[colour, direction]
        near = [self.remote(i + n, self.planes.at[colour, pl.ds(TWO * half, TWO)], got.at[pl.ds(TWO * half, TWO)], device) for n, half in enumerate((direction, ONE - direction))]
        return near + [self.remote(i + TWO, got.at[pl.ds(TWO * direction, TWO)], self.far.at[colour, direction], device)]

    def shares(self, colour):
        last = DIM_ORDER[colour][TWO]
        rows = pl.ds(pl.multiple_of((self.core * COLOURS + colour) * self.band, self.band), self.band)
        views = [(self.planes.at[colour], ZERO, None)]
        views += [(self.near.at[colour, direction], TWO * direction - ONE, None) for direction in range(TWO)]
        views += [(self.far.at[colour, direction], TWO, direction) for direction in range(TWO)]
        out = []
        for n, (src, shift, half) in enumerate(views):
            where = [slice(None)] * THREE
            where[last] = lax.rem(self.place[last] + shift + SIDE, SIDE)
            if half is not None:
                where[min(d for d in range(THREE) if d != last)] = pl.ds(TWO * half, TWO)
            dst = self.out.at[tuple(where) + (rows, slice(None))]
            out.append((self.remote(11 * colour + 6 + n, src, dst, (ONE - self.core, self.chip)), pltpu.make_async_copy(src, dst, self.load_sem.at[5 * colour + n])))
        return out

    def share(self, colour, which):
        for n in which:
            give, keep = self.shares(colour)[n]
            give.start()
            keep.start()

    def begin(self):
        for colour in range(COLOURS):
            for direction in range(TWO):
                for copy in self.ring(colour, direction)[:TWO]:
                    copy.start()
        for colour in range(COLOURS):
            self.share(colour, (ZERO,))

    def pass_on(self):
        for colour in range(COLOURS):
            for direction in range(TWO):
                first, _, far = self.ring(colour, direction)
                first.wait_recv()
                far.start()
        for colour in range(COLOURS):
            for direction in range(TWO):
                self.ring(colour, direction)[ONE].wait_recv()
            self.share(colour, (ONE, TWO))

    def complete(self):
        for colour in range(COLOURS):
            for direction in range(TWO):
                self.ring(colour, direction)[TWO].wait_recv()
            self.share(colour, (THREE, 4))

    def end(self):
        for colour in range(COLOURS):
            for give, keep in self.shares(colour):
                give.wait_recv()
                give.wait_send()
                keep.wait()
            for direction in range(TWO):
                for copy in self.ring(colour, direction):
                    copy.wait_send()


def dot(lhs, rhs, contract=((ONE,), (ZERO,))):
    return lax.dot_general(lhs, rhs, (contract, ((), ())), preferred_element_type=F32)


def dot_nt(lhs, rhs):
    return dot(lhs, rhs, ((ONE,), (ONE,)))


def dot_tn(lhs, rhs):
    return dot(lhs, rhs, ((ZERO,), (ZERO,)))


def norm_rows(resid, gain, shift):
    mean = jnp.mean(resid, axis=-ONE, keepdims=True)
    centred = resid - mean
    inv_std = lax.rsqrt(jnp.mean(centred * centred, axis=-ONE, keepdims=True) + LN_EPS)
    normed = centred * inv_std
    return (normed * gain + shift).astype(BF16), normed, inv_std


def norm_rows_bwd(d_out, normed, inv_std, gain):
    d_norm = d_out * gain
    return inv_std * (d_norm - jnp.mean(d_norm, axis=-ONE, keepdims=True) - normed * jnp.mean(d_norm * normed, axis=-ONE, keepdims=True))


def col_sum(values):
    return jnp.sum(values, axis=ZERO, keepdims=True)


def lane_row(head, dtype=BF16):
    lane = lax.broadcasted_iota(jnp.int32, (ONE, PAIR), ONE)
    return jnp.where((lane >= HEAD_DIM * head) & (lane < HEAD_DIM * (head + ONE)), 1.0, 0.0).astype(dtype)


def spare_lane(head):
    lane = lax.broadcasted_iota(jnp.int32, (ONE, PAIR), ONE)
    return jnp.where(lane == HEAD_DIM * (ONE - head), 1.0, 0.0)


def mask_fill(n_rows, n_valid):
    row = lax.broadcasted_iota(jnp.int32, (n_rows, PAIR), ZERO)
    return jnp.where(row >= n_valid, MASK_FILL, 0.0)


def head_masks(pair_q, pair_k, head, fill):
    q_f = pair_q * lane_row(head) + spare_lane(head).astype(BF16)
    k_f = pair_k * lane_row(head) + (fill * spare_lane(head)).astype(BF16)
    return q_f, k_f


def half_only(pair, head):
    return pair * lane_row(head)


def join_halves(first, second):
    lane = lax.broadcasted_iota(jnp.int32, first.shape, ONE)
    return jnp.where(lane < HEAD_DIM, first, second)


def score_blocks(n_heads, n_q, n_k, causal, step):
    if not causal:
        return [(head, ZERO, n_q, n_k) for head in range(n_heads)]
    return [(head, first, step, first + step) for head in range(n_heads) for first in range(ZERO, n_q, step)]


def scores_t(q_f, k_f, causal, first):
    s_t = dot_nt(k_f, q_f)
    if causal:
        key_i = lax.broadcasted_iota(jnp.int32, s_t.shape, ZERO)
        qry_i = lax.broadcasted_iota(jnp.int32, s_t.shape, ONE) + first
        s_t = jnp.where(key_i <= qry_i, s_t, MASK_FILL)
    return s_t


def pair_of(group, head):
    return group[:, head // TWO * PAIR:(head // TWO + ONE) * PAIR]


def masked_pairs(q_g, k_g, n_valid):
    fill = mask_fill(k_g.shape[ZERO], n_valid)
    cache = {}

    def get(head):
        if head not in cache:
            cache[head] = head_masks(pair_of(q_g, head), pair_of(k_g, head), head % TWO, fill)
        return cache[head]

    return get


def stack_heads(parts, n_heads):
    return jnp.concatenate([jnp.concatenate(parts[head], axis=ONE) for head in range(n_heads)], axis=ZERO)


def run_ahead(blocks, produce, transform, consume, delay):
    ahead = produce(blocks[ZERO])
    waiting = []
    for i, block in enumerate(blocks):
        now = ahead
        if i + ONE < len(blocks):
            ahead = produce(blocks[i + ONE])
        waiting.append((block, transform(block, now)))
        if len(waiting) > delay:
            consume(*waiting.pop(ZERO))
    for item in waiting:
        consume(*item)


def attend_group(q_g, k_g, v_g, n_valid, causal, lse_ref):
    n_heads = GROUP // HEAD_DIM
    o_parts = [[] for _ in range(n_heads)]
    v_t = v_g.T
    masked = masked_pairs(q_g, k_g, n_valid)

    def produce(block):
        head, first, n_q, n_k = block
        q_f, k_f = masked(head)
        return scores_t(q_f[first:first + n_q], k_f[:n_k], causal, first)

    def transform(block, s_t):
        head, first, n_q, n_k = block
        top = jnp.max(s_t, axis=ZERO, keepdims=True)
        e_t = jnp.exp(s_t - top)
        total = jnp.sum(e_t, axis=ZERO, keepdims=True)
        lse_ref[ZERO, ZERO, head:head + ONE, first:first + n_q] = top + jnp.log(total)
        return (e_t * (1.0 / total)).astype(BF16)

    def consume(block, p_t):
        head, first, n_q, n_k = block
        o_parts[head].append(dot(v_t[HEAD_DIM * head:HEAD_DIM * (head + ONE), :n_k], p_t))

    run_ahead(score_blocks(n_heads, q_g.shape[ZERO], k_g.shape[ZERO], causal, 128), produce, transform, consume, TWO)
    return stack_heads(o_parts, n_heads).T.astype(BF16)


def attend_group_bwd(d_o, q_g, k_g, v_g, n_valid, causal, lse_ref, between=None):
    n_heads = GROUP // HEAD_DIM
    k_t = k_g.T
    dq_t, dk_h, dv_h = [[] for _ in range(n_heads)], [None] * n_heads, [None] * n_heads
    masked = masked_pairs(q_g, k_g, n_valid)
    v_half = {}

    def produce(block):
        head, first, n_q, n_k = block
        q_f, k_f = masked(head)
        if head not in v_half:
            v_half[head] = half_only(pair_of(v_g, head), head % TWO)
        rows = slice(first, first + n_q)
        return scores_t(q_f[rows], k_f[:n_k], causal, first), dot_nt(v_half[head][:n_k], pair_of(d_o, head)[rows])

    def transform(block, products):
        head, first, n_q, n_k = block
        s_t, dp_t = products
        p_t = jnp.exp(s_t - lse_ref[ZERO, ZERO, head:head + ONE, first:first + n_q])
        weighted = p_t * dp_t
        return p_t.astype(BF16), (weighted - p_t * jnp.sum(weighted, axis=ZERO, keepdims=True)).astype(BF16)

    def grow(old, new):
        if old is None:
            return new
        n_old = old.shape[ZERO]
        return old + new if n_old == new.shape[ZERO] else jnp.concatenate([old + new[:n_old], new[n_old:]], axis=ZERO)

    def consume(block, operands):
        head, first, n_q, n_k = block
        p_b, ds_t = operands
        rows = slice(first, first + n_q)
        dv_h[head] = grow(dv_h[head], dot(p_b, pair_of(d_o, head)[rows]))
        dk_h[head] = grow(dk_h[head], dot(ds_t, pair_of(q_g, head)[rows]))
        dq_t[head].append(dot(k_t[HEAD_DIM * head:HEAD_DIM * (head + ONE), :n_k], ds_t))

    blocks = score_blocks(n_heads, q_g.shape[ZERO], k_g.shape[ZERO], causal, 256)
    if between is None:
        run_ahead(blocks, produce, transform, consume, ZERO)
    else:
        n_first = len(blocks) // TWO
        run_ahead(blocks[:n_first], produce, transform, consume, ZERO)
        between()
        run_ahead(blocks[n_first:], produce, transform, consume, ZERO)
    join = lambda parts: jnp.concatenate([join_halves(parts[h], parts[h + ONE]) for h in range(ZERO, n_heads, TWO)], axis=ONE)
    return stack_heads(dq_t, n_heads).T * 0.125, join(dk_h), join(dv_h)


def attn_fwd_kernel(causal, slots, guest, lens_ref, x_ref, kv_ref, wq_ref, wk_ref, wv_ref, w_all, bias_ref, rows_ref,
                    q_ref, k_ref, v_ref, o_ref, lse_ref, h_ref, normed_ref, inv_ref, o_all, wo_v, load_sem):
    q_row, k_row, v_row, o_row, gain_row, o_mat = slots
    sample, group = pl.program_id(ZERO), pl.program_id(ONE)
    d_model = wo_v.shape[ZERO]
    fetch = pltpu.make_async_copy(w_all.at[pl.ds(o_mat * d_model, d_model), :], wo_v, load_sem)

    @pl.when((sample == ZERO) & (group == ZERO))
    def _():
        fetch.start()

    turn = sample * pl.num_programs(ONE) + group
    if guest is not None:
        for where, steps in ((ZERO, (lambda: meet_neighbours(guest.place), guest.begin)), (THREE, (guest.pass_on,)), (5, (guest.complete,))):
            @pl.when(turn == where)
            def _():
                for step in steps:
                    step()

    x_b, kv_b = x_ref[ALL], kv_ref[ALL]
    q_g = ((dot(x_b, wq_ref[ALL]) + bias_ref[q_row:q_row + ONE, :]) * 0.125).astype(BF16)
    k_g = (dot(kv_b, wk_ref[ALL]) + bias_ref[k_row:k_row + ONE, :]).astype(BF16)
    v_g = (dot(kv_b, wv_ref[ALL]) + bias_ref[v_row:v_row + ONE, :]).astype(BF16)
    q_ref[ALL], k_ref[ALL], v_ref[ALL] = q_g, k_g, v_g
    o_g = attend_group(q_g, k_g, v_g, lens_ref[sample], causal, lse_ref)
    o_ref[ALL] = o_g
    o_all[:, pl.ds(pl.multiple_of(group * GROUP, GROUP), GROUP)] = o_g

    @pl.when((sample == ZERO) & (group == pl.num_programs(ONE) - ONE))
    def _():
        fetch.wait()

    @pl.when(group == pl.num_programs(ONE) - ONE)
    def _():
        resid = x_ref[ALL].astype(F32) + dot(o_all[ALL], wo_v[ALL]) + rows_ref[o_row:o_row + ONE, :]
        h_out, normed, inv_std = norm_rows(resid, rows_ref[gain_row:gain_row + ONE, :], rows_ref[gain_row + ONE:gain_row + TWO, :])
        h_ref[ALL], normed_ref[ALL], inv_ref[ALL] = h_out, normed, inv_std

    if guest is not None:
        @pl.when(turn == pl.num_programs(ZERO) * pl.num_programs(ONE) - ONE)
        def _():
            guest.end()


def attn_forward(x, kv, lens, attn_full, bias_rows, mats, slots, causal, planes=None, full_rows=None):
    d_model = x.shape[-ONE]
    n_batch = lens.shape[ZERO]
    n_q, n_k = x.shape[ZERO] // n_batch, kv.shape[ZERO] // n_batch
    n_groups = d_model // GROUP
    col = lambda mat: pl.BlockSpec((d_model, GROUP), lambda b, g: (mat, g))
    q_blk = pl.BlockSpec((n_q, GROUP), lambda b, g: (b, g))
    k_blk = pl.BlockSpec((n_k, GROUP), lambda b, g: (b, g))
    tok = lambda n: pl.BlockSpec((n, d_model), lambda b, g: (b, ZERO))
    n_heads_g = GROUP // HEAD_DIM
    out_shape = (
        jax.ShapeDtypeStruct(x.shape, BF16), jax.ShapeDtypeStruct(kv.shape, BF16), jax.ShapeDtypeStruct(kv.shape, BF16),
        jax.ShapeDtypeStruct(x.shape, BF16), jax.ShapeDtypeStruct((n_batch, n_groups, n_heads_g, n_q), F32),
        jax.ShapeDtypeStruct(x.shape, BF16), jax.ShapeDtypeStruct(x.shape, F32), jax.ShapeDtypeStruct((x.shape[ZERO], ONE), F32))
    kernel = functools.partial(attn_fwd_kernel, causal, slots + (mats[THREE],))
    in_specs = [pl.BlockSpec(memory_space=pltpu.SMEM), tok(n_q), tok(n_k), col(mats[ZERO]), col(mats[ONE]), col(mats[TWO]), pl.BlockSpec(memory_space=pl.ANY),
                pl.BlockSpec((bias_rows.shape[ZERO], GROUP), lambda b, g: (ZERO, g)), pl.BlockSpec(bias_rows.shape, lambda b, g: (ZERO, ZERO))]
    out_specs = [q_blk, k_blk, k_blk, q_blk, pl.BlockSpec((ONE, ONE, n_heads_g, n_q), lambda b, g: (b, g, ZERO, ZERO)),
                 tok(n_q), tok(n_q), pl.BlockSpec((n_q, ONE), lambda b, g: (b, ZERO))]
    scratch = [pltpu.VMEM((n_q, d_model), BF16), pltpu.VMEM((d_model, d_model), BF16), pltpu.SemaphoreType.DMA]
    args = [lens, x, kv, attn_full, attn_full, attn_full, attn_full, bias_rows, bias_rows]
    params = dict(vmem_limit_bytes=VMEM_BYTES, dimension_semantics=('arbitrary', 'arbitrary'))
    if planes is None:
        body = functools.partial(kernel, None)
    else:
        n_in, n_out, n_own = len(args), len(out_specs), len(scratch)

        def body(*refs):
            ins, held, outs, whole, rest = refs[:n_in], refs[n_in], refs[n_in + ONE:n_in + ONE + n_out], refs[n_in + ONE + n_out], refs[n_in + TWO + n_out:]
            kernel(LastPhase(held, whole, *rest[n_own:]), *ins, *outs, *rest[:n_own])

        in_specs.append(pl.BlockSpec(memory_space=pltpu.VMEM))
        args.append(planes)
        out_specs.append(pl.BlockSpec(memory_space=pl.ANY))
        out_shape += (jax.ShapeDtypeStruct((SIDE, SIDE, SIDE, full_rows // SIDE ** THREE, d_model), BF16),)
        scratch += LastPhase.scratch_shapes(planes)
        params |= dict(collective_id=5, has_side_effects=True)
    return pl.pallas_call(
        body, grid=(n_batch, n_groups), in_specs=in_specs, out_specs=out_specs, out_shape=out_shape, scratch_shapes=scratch,
        compiler_params=pltpu.CompilerParams(**params),
        cost_estimate=pl.CostEstimate(flops=TWO * d_model * d_model * (TWO * x.shape[ZERO] + TWO * kv.shape[ZERO]) + 16 * x.shape[ZERO] * n_k * d_model, bytes_accessed=20 * x.shape[ZERO] * d_model, transcendentals=ZERO),
        name='attn_fwd',
    )(*args)


def attn_bwd_kernel(causal, gain_row, mats, lhs_of, guest, lens_ref, dres_ref, wo_ref, w_all, q_ref, k_ref, v_ref, lse_ref,
                    rows_ref, normed_ref, inv_ref, lhs_refs, dx_ref, dkv_ref, sums_ref, tail_ref, grads_ref,
                    d_all, dk_all, dv_all, dres_all, w_v, lhs_vs, grad_v, load_sem):
    sample, group = pl.program_id(ZERO), pl.program_id(ONE)
    d_model = w_v.shape[ONE]
    n_q, n_k = q_ref.shape[ZERO], k_ref.shape[ZERO]
    last = pl.num_programs(ONE) - ONE
    fetches = [pltpu.make_async_copy(w_all.at[pl.ds(mat * d_model, d_model), :], w_v.at[i], load_sem.at[i]) for i, mat in enumerate(mats[:THREE])]
    lhs_fetch = lambda i: pltpu.make_async_copy(lhs_refs[i], lhs_vs[i % TWO].at[pl.ds(ZERO, lhs_refs[i].shape[ZERO]), :], load_sem.at[THREE + i])

    @pl.when((sample == ZERO) & (group == ZERO))
    def _():
        for fetch in fetches + [lhs_fetch(ZERO), lhs_fetch(ONE)]:
            fetch.start()

    turn = sample * pl.num_programs(ONE) + group
    guest(ZERO, TWO * turn)
    q_rows = pl.ds(pl.multiple_of(sample * n_q, n_q), n_q)
    k_rows = pl.ds(pl.multiple_of(sample * n_k, n_k), n_k)
    d_o = dot_nt(dres_ref[ALL].astype(BF16), wo_ref[ALL]).astype(BF16)
    dq, dk, dv = attend_group_bwd(d_o, q_ref[ALL], k_ref[ALL], v_ref[ALL], lens_ref[sample], causal, lse_ref, None if causal else functools.partial(guest, ONE, TWO * turn + ONE))
    cols = pl.ds(pl.multiple_of(group * GROUP, GROUP), GROUP)
    for i, (full, rows, value) in enumerate(((d_all, q_rows, dq), (dk_all, k_rows, dk), (dv_all, k_rows, dv))):
        sums_ref[ZERO, i:i + ONE, :] = col_sum(value)
        full[rows, cols] = value.astype(BF16)

    @pl.when(group == ZERO)
    def _():
        dres_all[q_rows, :] = dres_ref[ALL].astype(BF16)

    @pl.when((sample == ZERO) & (group == last))
    def _():
        for fetch in fetches:
            fetch.wait()

    guest(THREE, turn)

    @pl.when(group == last)
    def _():
        d_kv = dot_nt(dk_all[k_rows, :], w_v[ONE]) + dot_nt(dv_all[k_rows, :], w_v[TWO])
        d_h = dres_ref[ALL] + dot_nt(d_all[q_rows, :], w_v[ZERO])
        if causal:
            dx_ref[ALL] = (d_h + d_kv).astype(BF16)
            tail_ref[ALL] = jnp.zeros_like(tail_ref)
        else:
            dkv_ref[ALL] = d_kv.astype(BF16)
            normed = normed_ref[ALL]
            d_resid = norm_rows_bwd(d_h, normed, inv_ref[ALL], rows_ref[gain_row:gain_row + ONE, :])
            dx_ref[ALL] = d_resid
            tail_ref[ZERO, ZERO:ONE, :] = col_sum(d_resid)
            tail_ref[ZERO, ONE:TWO, :] = col_sum(d_h * normed)
            tail_ref[ZERO, TWO:THREE, :] = col_sum(d_h)

    @pl.when(turn == pl.num_programs(ZERO) * pl.num_programs(ONE) - ONE)
    def _():
        guest(TWO, 12)
        stores = []
        for i, (rhs, which) in enumerate(zip((d_all, dk_all, dv_all, dres_all), lhs_of)):
            if which not in lhs_of[:i]:
                lhs_fetch(which).wait()
            if i >= TWO:
                stores[i - TWO].wait()
            grad_v[i % TWO] = dot_tn(lhs_vs[which % TWO][pl.ds(ZERO, rhs.shape[ZERO]), :], rhs[ALL])
            store = pltpu.make_async_copy(grad_v.at[i % TWO], grads_ref.at[pl.ds(mats[i] * d_model, d_model), :], load_sem.at[6 + i])
            store.start()
            stores.append(store)
            if i == ZERO and len(lhs_refs) > TWO:
                lhs_fetch(TWO).start()
            guest(TWO, 13 + i)
        for store in stores[TWO:]:
            store.wait()


def scatter_guest(scatter, plan, parity, position):
    steps = dict(end=scatter.end) | {('relay', p): functools.partial(scatter.relay, p) for p in range(THREE)}
    steps |= {('settle', p): functools.partial(scatter.settle, p) for p in range(THREE)} | {turn: functools.partial(scatter.absorb, turn) for turn in range(SIDE)}
    if parity == TWO:
        for name in plan.get(position, ()):
            steps[name]()
        return
    if parity == THREE:
        @pl.when(position == 5)
        def _():
            for name in plan['late']:
                steps[name]()
        return
    if parity == ZERO:
        @pl.when(position == ZERO)
        def _():
            meet_neighbours(scatter.place)
            scatter.begin()
    for where, names in plan.items():
        if where != 'late' and where < 12 and where % TWO == parity:
            @pl.when(position == where)
            def _():
                for name in names:
                    steps[name]()


def no_guest(parity, position):
    pass


def attn_backward(dres, q, k, v, lse, lens, attn_full, bias_rows, mats, causal, lhs_list, lhs_of, g_rows=None, scale=None, gain_row=ZERO, normed=None, inv_std=None, grads=None):
    d_model = q.shape[-ONE]
    n_batch = lens.shape[ZERO]
    n_q, n_k = q.shape[ZERO] // n_batch, k.shape[ZERO] // n_batch
    n_groups = d_model // GROUP
    row = lambda mat: pl.BlockSpec((GROUP, d_model), lambda b, g: (mat * n_groups + g, ZERO))
    q_blk = pl.BlockSpec((n_q, GROUP), lambda b, g: (b, g))
    k_blk = pl.BlockSpec((n_k, GROUP), lambda b, g: (b, g))
    tok = lambda n: pl.BlockSpec((n, d_model), lambda b, g: (b, ZERO))
    n_heads_g = GROUP // HEAD_DIM
    anywhere = pl.BlockSpec(memory_space=pl.ANY)
    in_specs = [pl.BlockSpec(memory_space=pltpu.SMEM), tok(n_q), row(mats[THREE]), anywhere, q_blk, k_blk, k_blk,
                pl.BlockSpec((ONE, ONE, n_heads_g, n_q), lambda b, g: (b, g, ZERO, ZERO)), pl.BlockSpec(bias_rows.shape, lambda b, g: (ZERO, ZERO))]
    args = [lens, dres, attn_full, attn_full, q, k, v, lse, bias_rows]
    tail_shape = jax.ShapeDtypeStruct((n_batch, 8, d_model), F32)
    out_shape = [jax.ShapeDtypeStruct(q.shape, BF16 if causal else F32)]
    out_specs = [tok(n_q)]
    if not causal:
        late = dict(pipeline_mode=pl.Buffered(ONE))
        in_specs += [pl.BlockSpec((n_q, d_model), lambda b, g: (b, ZERO), **late), pl.BlockSpec((n_q, ONE), lambda b, g: (b, ZERO), **late)]
        args += [normed, inv_std]
        out_shape.append(jax.ShapeDtypeStruct(k.shape, BF16))
        out_specs.append(tok(n_k))
    n_lhs_at = len(args)
    args += list(lhs_list)
    in_specs += [anywhere] * len(lhs_list)
    out_shape += [tail_shape, tail_shape, jax.ShapeDtypeStruct(attn_full.shape, F32)]
    out_specs += [pl.BlockSpec((ONE, 8, GROUP), lambda b, g: (b, ZERO, g)), pl.BlockSpec((ONE, 8, d_model), lambda b, g: (b, ZERO, ZERO)), anywhere]
    both = lambda n: pltpu.VMEM((n_batch * n, d_model), BF16)
    own = [both(n_q), both(n_k), both(n_k), both(n_q), pltpu.VMEM((THREE, d_model, d_model), BF16), pltpu.VMEM(lhs_list[ZERO].shape, BF16), pltpu.VMEM(lhs_list[ONE].shape, BF16),
           pltpu.VMEM((TWO, d_model, d_model), F32), pltpu.SemaphoreType.DMA((10,))]
    kernel = functools.partial(attn_bwd_kernel, causal, gain_row, mats, lhs_of)
    params = dict(vmem_limit_bytes=VMEM_BYTES, dimension_semantics=('arbitrary', 'arbitrary'))
    aliases = {}
    if causal:
        args.append(grads)
        in_specs.append(anywhere)
        aliases = {len(args) - ONE: len(out_shape) - ONE}
    else:
        args.append(as_torus(g_rows))
        in_specs.append(anywhere)
        n_rows = args[-ONE].shape[THREE]
        out_shape.append(jax.ShapeDtypeStruct((n_rows, d_model), F32))
        out_specs.append(anywhere)
        params |= dict(collective_id=THREE, has_side_effects=True, vmem_limit_bytes=67043328)
    scratch = own + ([] if causal else Scatter.scratch_shapes([n_rows]))
    n_in, n_out, n_own = len(args), len(out_shape), len(own)

    def body(*refs):
        ins, outs, rest = refs[:n_in], refs[n_in:n_in + n_out], refs[n_in + n_out:]
        lhs_refs, (d_all, dk_all, dv_all, dres_all, w_v, lhs_a, lhs_b, grad_v, load_sem) = ins[n_lhs_at:-ONE], rest[:n_own]
        held = (d_all, dk_all, dv_all, dres_all, w_v, (lhs_a, lhs_b), grad_v, load_sem)
        if causal:
            dx, sums, tail, grads_ref = outs
            kernel(no_guest, *ins[:n_lhs_at], None, None, lhs_refs, dx, None, sums, tail, grads_ref, *held)
        else:
            dx, dkv, sums, tail, grads_ref, total = outs
            scatter = Scatter(scale, [(ins[-ONE], ZERO, n_rows)], [total], rest[n_own:])
            kernel(functools.partial(scatter_guest, scatter, CROSS_PLAN), *ins[:n_lhs_at], lhs_refs, dx, dkv, sums, tail, grads_ref, *held)

    return pl.pallas_call(
        body, grid=(n_batch, n_groups), in_specs=in_specs, out_specs=out_specs, out_shape=out_shape, scratch_shapes=scratch, input_output_aliases=aliases,
        compiler_params=pltpu.CompilerParams(**params),
        cost_estimate=pl.CostEstimate(flops=TWO * d_model * d_model * (TWO * q.shape[ZERO] + TWO * k.shape[ZERO]) + 40 * q.shape[ZERO] * n_k * d_model, bytes_accessed=20 * q.shape[ZERO] * d_model, transcendentals=ZERO),
        name='attn_bwd',
    )(*args)


def ffn_kernel(n_blocks, h_ref, dy_ref, up_ref, down_ref, rows_ref, bias_ref, normed_ref, inv_ref,
               y_ref, grad_ref, dres2_ref, tail_ref, upsum_ref, gelu_all, dup_all, dres3_all, h_all):
    step = pl.program_id(ZERO)
    block, d_model = h_ref.shape
    n_square = gelu_all.shape[ONE] // d_model

    @pl.when(step < n_blocks)
    def _():
        rows = pl.ds(pl.multiple_of(step * block, block), block)
        h_b = h_ref[ALL]
        h_all[rows, :] = h_b
        up = dot_nt(h_b, up_ref[ALL]) + bias_ref[ALL]
        cdf = 0.5 * (1.0 + lax.erf(up * 0.7071067811865476))
        gelu = (up * cdf).astype(BF16)
        slope = cdf + up * (0.3989422804014327 * jnp.exp(-0.5 * up * up))
        gelu_all[rows, :] = gelu
        resid = h_b.astype(F32) + dot(gelu, down_ref[ALL]) + rows_ref[8:9, :]
        y_b, normed3, inv3 = norm_rows(resid, rows_ref[13:14, :], rows_ref[14:15, :])
        y_ref[ALL] = y_b
        dy = dy_ref[ALL].astype(F32)
        d_res3 = norm_rows_bwd(dy, normed3, inv3, rows_ref[13:14, :])
        d_res3_b = d_res3.astype(BF16)
        dres3_all[rows, :] = d_res3_b
        d_up = dot_nt(d_res3_b, down_ref[ALL]) * slope
        d_up_b = d_up.astype(BF16)
        dup_all[rows, :] = d_up_b
        d_h2 = d_res3 + dot(d_up_b, up_ref[ALL])
        normed2 = normed_ref[ALL]
        d_res2 = norm_rows_bwd(d_h2, normed2, inv_ref[ALL], rows_ref[11:12, :])
        dres2_ref[ALL] = d_res2
        tail = jnp.concatenate([col_sum(d_res2), col_sum(d_res3), col_sum(d_h2 * normed2), col_sum(d_h2), col_sum(dy * normed3), col_sum(dy),
                                jnp.zeros((TWO, dy.shape[ONE]), F32)], axis=ZERO)
        up_sum = col_sum(d_up)

        @pl.when(step == ZERO)
        def _():
            tail_ref[ALL] = tail
            upsum_ref[ALL] = up_sum

        @pl.when(step > ZERO)
        def _():
            tail_ref[ALL] += tail
            upsum_ref[ALL] += up_sum

    square = step - n_blocks
    cols = pl.ds(pl.multiple_of(lax.rem(square + TWO * n_square, n_square) * d_model, d_model), d_model)

    @pl.when((square >= ZERO) & (square < n_square))
    def _():
        grad_ref[ALL] = dot_tn(dup_all[:, cols], h_all[ALL])

    @pl.when(square >= n_square)
    def _():
        grad_ref[ALL] = dot_tn(gelu_all[:, cols], dres3_all[ALL])


def ffn_both(h2, dy, ffn_full, bias_rows, up_bias, normed2, inv2, block=256):
    n_tok, d_model = h2.shape
    ffn_dim = ffn_full.shape[ZERO] // TWO
    n_blocks = n_tok // block
    n_steps = n_blocks + ffn_full.shape[ZERO] // d_model
    at = lambda i: jnp.minimum(i, n_blocks - ONE)
    tok = pl.BlockSpec((block, d_model), lambda i: (at(i), ZERO))
    once = lambda shape, idx: pl.BlockSpec(shape, lambda i: idx, pipeline_mode=pl.Buffered(ONE))
    return pl.pallas_call(
        functools.partial(ffn_kernel, n_blocks), grid=(n_steps,),
        in_specs=[tok, tok, once((ffn_dim, d_model), (ZERO, ZERO)), once((ffn_dim, d_model), (ONE, ZERO)), once(bias_rows.shape, (ZERO, ZERO)), once((ONE, ffn_dim), (ZERO, ZERO)),
                  tok, pl.BlockSpec((block, ONE), lambda i: (at(i), ZERO))],
        out_specs=[tok, pl.BlockSpec((d_model, d_model), lambda i: (jnp.maximum(i - n_blocks, ZERO), ZERO)), tok, pl.BlockSpec((8, d_model), lambda i: (ZERO, ZERO)), pl.BlockSpec((ONE, ffn_dim), lambda i: (ZERO, ZERO))],
        out_shape=[jax.ShapeDtypeStruct(h2.shape, BF16), jax.ShapeDtypeStruct(ffn_full.shape, F32), jax.ShapeDtypeStruct(h2.shape, F32),
                   jax.ShapeDtypeStruct((8, d_model), F32), jax.ShapeDtypeStruct((ONE, ffn_dim), F32)],
        scratch_shapes=[pltpu.VMEM((n_tok, ffn_dim), BF16), pltpu.VMEM((n_tok, ffn_dim), BF16), pltpu.VMEM((n_tok, d_model), BF16), pltpu.VMEM((n_tok, d_model), BF16)],
        compiler_params=pltpu.CompilerParams(vmem_limit_bytes=VMEM_BYTES, dimension_semantics=('arbitrary',)),
        cost_estimate=pl.CostEstimate(flops=12 * n_tok * d_model * ffn_dim, bytes_accessed=30 * n_tok * d_model, transcendentals=ZERO),
        name='ffn_both',
    )(h2, dy, ffn_full, ffn_full, bias_rows, up_bias, normed2, inv2)


CROSS_PLAN = {ONE: (ZERO,), TWO: (ONE,), THREE: (TWO,), 4: (THREE,), 5: (('relay', ZERO),), 9: (('settle', ZERO),), 10: (('relay', ONE),), 'late': (('settle', ONE),), 12: (('relay', TWO),), 14: (('settle', TWO),), 16: ('end',)}


def solution(mesh):
    n_fsdp = mesh.shape['fsdp']
    n_dp = mesh.shape['dp']
    batch_axes = ('dp', 'fsdp')
    act_spec = P(batch_axes, None, None)
    len_spec = P(batch_axes)
    row_spec = P('fsdp', None)
    vec_spec = P('fsdp')

    def device_step(dec_in, enc_out, src_lens, tgt_lens, y_cot, attn_w, ffn_w, vec_params):
        d_model, n_vec = dec_in.shape[TWO], vec_params.shape[ZERO]
        scale = 1.0 / (dec_in.shape[ZERO] * dec_in.shape[ONE] * n_fsdp * n_dp)
        x, enc, dy = (a.reshape(-ONE, d_model) for a in (dec_in, enc_out, y_cot))
        vec_rows = jnp.pad(vec_params.astype(F32), (ZERO, 16 * LANES - n_vec)).reshape(16, LANES)
        attn_tiles, planes, vec_tiles = gather_params(attn_w, ffn_w, vec_rows)
        attn_full = attn_tiles.reshape(-ONE, d_model)
        vec_f = vec_tiles.reshape(n_fsdp, 16, LANES)[:, :TWO].reshape(n_fsdp, TWO * LANES)[:, :n_vec].reshape(-ONE)
        bias_rows = jnp.pad(vec_f[:15 * d_model].reshape(15, d_model), ((ZERO, ONE), (ZERO, ZERO)))
        up_bias = vec_f[15 * d_model:].reshape(ONE, -ONE)
        q1, k1, v1, o1, lse1, h1, normed1, inv1 = attn_forward(x, x, tgt_lens, attn_full, bias_rows, (ZERO, ONE, TWO, THREE), (ZERO, ONE, TWO, THREE, 9), True)
        q2, k2, v2, o2, lse2, h2, normed2, inv2, ffn_tiles = attn_forward(h1, enc, src_lens, attn_full, bias_rows, (4, 5, 6, 7), (4, 5, 6, 7, 11), False, planes, ffn_w.shape[ZERO] * n_fsdp)
        ffn_full = ffn_tiles.reshape(-ONE, d_model)
        y, g_ffn, d_res2, ffn_tail, up_sum = ffn_both(h2, dy, ffn_full, bias_rows, up_bias, normed2, inv2)
        d_res1, d_enc, sums2, tail2, grads, ffn_out = attn_backward(d_res2, q2, k2, v2, lse2, src_lens, attn_full, bias_rows, (4, 5, 6, 7), False, (h1, enc, o2), (ZERO, ONE, ONE, TWO), g_ffn, scale, 9, normed1, inv1)
        d_x, sums1, _, grads = attn_backward(d_res1, q1, k1, v1, lse1, tgt_lens, attn_full, bias_rows, (ZERO, ONE, TWO, THREE), True, (x, o1), (ZERO, ZERO, ZERO, ONE), grads=grads)
        s1, s2, t2 = jnp.sum(sums1, axis=ZERO), jnp.sum(sums2, axis=ZERO), jnp.sum(tail2, axis=ZERO)
        g_vec = jnp.concatenate([s1[ZERO:THREE].reshape(-ONE), t2[ZERO], s2[ZERO:THREE].reshape(-ONE), ffn_tail[ZERO], ffn_tail[ONE], t2[ONE], t2[TWO], ffn_tail[TWO], ffn_tail[THREE], ffn_tail[4], ffn_tail[5], up_sum[ZERO]])
        g_rows = jnp.pad(g_vec.reshape(n_fsdp, ONE, n_vec), ((ZERO, ZERO), (ZERO, 7), (ZERO, d_model - n_vec))).reshape(n_fsdp * 8, -ONE)
        attn_out, vec_out = scatter_grads(grads, g_rows, scale)
        return y.reshape(dec_in.shape), d_x.reshape(dec_in.shape), d_enc.reshape(enc_out.shape), attn_out, ffn_out, vec_out[ZERO, :n_vec]

    return jax.shard_map(device_step, mesh=mesh, in_specs=(act_spec, act_spec, len_spec, len_spec, act_spec, row_spec, row_spec, vec_spec), out_specs=(act_spec, act_spec, act_spec, row_spec, row_spec, vec_spec), check_vma=False)
```

```python
import functools
import jax
import jax.numpy as jnp
from jax import lax
from jax.experimental import pallas as pl
from jax.experimental.pallas import tpu as pltpu
from jax.sharding import PartitionSpec as P

ZERO, ONE, TWO, THREE = range(4)
ALL = ...
HEAD_DIM = 64
LN_EPS = 1e-5
MASK_FILL = -1e30
VMEM_BYTES = 60 * 1024 * 1024
F32 = jnp.float32
BF16 = jnp.bfloat16
GROUP = 256
PAIR = 128


SIDE = 4
LANES = 128
COLOURS = THREE
STAGES = TWO
DIM_ORDER = ((TWO, ONE, ZERO), (ONE, ZERO, TWO), (ZERO, TWO, ONE))
MESH_ID = pl.DeviceIdType.MESH


def torus_place():
    chip = lax.axis_index('fsdp')
    return (chip // (SIDE * SIDE), lax.rem(chip // SIDE, SIDE), lax.rem(chip, SIDE))


def chip_at(place, dim, shift):
    moved = [lax.rem(p + shift + SIDE, SIDE) if d == dim else p for d, p in enumerate(place)]
    return (moved[ZERO] * SIDE + moved[ONE]) * SIDE + moved[TWO]


def meet_neighbours(place):
    barrier = pltpu.get_barrier_semaphore()
    core = lax.axis_index('dp')
    for dim in range(THREE):
        for shift in (ONE, -ONE):
            pl.semaphore_signal(barrier, inc=ONE, device_id=(core, chip_at(place, dim, shift)), device_id_type=MESH_ID)
    pl.semaphore_signal(barrier, inc=ONE, device_id=(ONE - core, lax.axis_index('fsdp')), device_id_type=MESH_ID)
    pl.semaphore_wait(barrier, 7)


class Scatter:
    def __init__(self, scale, sources, outs, scratch, resident=False):
        self.scale, self.outs, self.resident = scale, outs, resident
        self.sources = [(ref, pl.ds(first, n)) for ref, first, n in sources]
        (self.acc, g1, d1, g2, d2, g3, d3, self.send_sem, self.recv_sem, self.load_sem, *stage) = scratch
        self.stage = None if resident else stage[ZERO]
        self.got, self.far = (g1, g2, g3), (d1, d2, d3)
        self.heights = [n for _, _, n in sources]
        self.offsets = [sum(self.heights[:i]) for i in range(len(sources))]
        self.height = sum(self.heights)
        self.n_low = self.heights[ZERO] // TWO
        self.core, self.chip, self.place = lax.axis_index('dp'), lax.axis_index('fsdp'), torus_place()
        self.pieces = [(d, colour) for d in (TWO, ONE, THREE, ZERO) for colour in range(COLOURS)]

    @staticmethod
    def scratch_shapes(heights, resident=False):
        h = sum(heights)
        n_low = heights[ZERO] // TWO
        buf = lambda *shape: pltpu.VMEM((COLOURS,) + shape + (LANES,), F32)
        n = Scatter.n_copies(len(heights))
        return [buf(SIDE, SIDE, SIDE, h), buf(TWO, SIDE, SIDE, h), buf(TWO, TWO, SIDE, h), buf(TWO, SIDE, h), buf(TWO, TWO, h), buf(TWO, h), buf(TWO, max(n_low, h - n_low)),
                pltpu.SemaphoreType.DMA((n,)), pltpu.SemaphoreType.DMA((n,)), pltpu.SemaphoreType.DMA((THREE + COLOURS, len(heights)))] + (
                    [] if resident else [pltpu.VMEM((STAGES, SIDE, SIDE, h, LANES), F32)])

    @staticmethod
    def n_copies(n_parts):
        return 12 * n_parts + COLOURS * 18 + COLOURS * n_parts

    def remote(self, i, src, dst, device):
        return pltpu.make_async_remote_copy(src_ref=src, dst_ref=dst, send_sem=self.send_sem.at[i], recv_sem=self.recv_sem.at[i], device_id=device, device_id_type=MESH_ID)

    def columns(self, of_core, colour):
        return pl.ds(pl.multiple_of((of_core * COLOURS + colour) * LANES, LANES), LANES)

    def slot(self, d, colour):
        dim = DIM_ORDER[colour][ZERO]
        where = [slice(None)] * THREE
        where[dim] = lax.rem(self.place[dim] + d, SIDE)
        return tuple(where)

    def rows_of(self, part):
        return pl.ds(self.offsets[part], self.heights[part])

    def swaps(self, piece):
        d, colour = self.pieces[piece]
        where, cols = self.slot(d, colour), self.columns(ONE - self.core, colour)
        n = len(self.sources)
        return [self.remote(piece * n + i, src.at[where + (rows, cols)], self.acc.at[(colour,) + where + (self.rows_of(i), slice(None))], (ONE - self.core, self.chip))
                for i, (src, rows) in enumerate(self.sources)]

    def loads(self, piece):
        d, colour = self.pieces[piece]
        where, cols = self.slot(d, colour), self.columns(self.core, colour)
        if self.resident:
            return []
        return [pltpu.make_async_copy(src.at[where + (rows, cols)], self.stage.at[piece % STAGES, :, :, self.rows_of(i), :], self.load_sem.at[piece % STAGES, i])
                for i, (src, rows) in enumerate(self.sources)]

    def split_rows(self, half):
        return pl.ds(ZERO, self.n_low) if half == ZERO else pl.ds(self.n_low, self.height - self.n_low)

    def block(self, colour, phase, d, half=None):
        order = DIM_ORDER[colour]
        where = [None, None, None]
        for done in order[:phase]:
            where[done] = self.place[done]
        where[order[phase]] = lax.rem(self.place[order[phase]] + d, SIDE)
        for i, rest in enumerate(sorted(order[phase + ONE:])):
            where[rest] = slice(None) if half is None or i > ZERO else pl.ds(TWO * half, TWO)
        rows = self.split_rows(half) if phase == TWO and half is not None else slice(None)
        return self.acc.at[(colour,) + tuple(where) + (rows, slice(None))]

    def got_half(self, colour, phase, direction, half):
        where = self.split_rows(half) if phase == TWO else pl.ds(TWO * half, TWO)
        return self.got[phase].at[colour, direction, where]

    def far_part(self, colour, phase, direction):
        if phase == TWO:
            return self.far[phase].at[colour, direction, pl.ds(ZERO, self.n_low if direction == ZERO else self.height - self.n_low), :]
        return self.far[phase].at[colour, direction]

    def ring(self, colour, phase, direction):
        shift = ONE - TWO * direction
        device = (self.core, chip_at(self.place, DIM_ORDER[colour][phase], shift))
        i = 12 * len(self.sources) + ((colour * THREE + phase) * TWO + direction) * THREE
        near = shift % SIDE
        return (self.remote(i, self.block(colour, phase, TWO, direction), self.far_part(colour, phase, direction), device),
                self.remote(i + ONE, self.block(colour, phase, near, ONE - direction), self.got_half(colour, phase, direction, ONE - direction), device),
                self.remote(i + TWO, self.block(colour, phase, near, direction), self.got_half(colour, phase, direction, direction), device))

    def gives(self, colour):
        n = len(self.sources)
        base = 12 * n + COLOURS * 18 + colour * n
        done = self.acc.at[colour, self.place[ZERO], self.place[ONE], self.place[TWO]]
        cols = self.columns(self.core, colour)
        pairs = [(done.at[self.rows_of(i), :], out.at[:, cols]) for i, out in enumerate(self.outs)]
        return [(self.remote(base + i, src, dst, (ONE - self.core, self.chip)), pltpu.make_async_copy(src, dst, self.load_sem.at[THREE + colour, i])) for i, (src, dst) in enumerate(pairs)]

    def add_into(self, dst, sources, n_lead):
        def body(i, _):
            total = dst[i]
            for src in sources:
                total = total + src[i]
            dst[i] = total
            return ZERO

        if n_lead == TWO:
            lax.fori_loop(ZERO, dst.shape[ZERO], body, ZERO)
        else:
            total = dst[ALL]
            for src in sources:
                total = total + src[ALL]
            dst[ALL] = total


    def begin(self):
        for piece in range(STAGES):
            for copy in self.loads(piece):
                copy.start()
        for piece in range(len(self.pieces)):
            for copy in self.swaps(piece):
                copy.start()

    def absorb(self, turn):
        for piece in range(turn * COLOURS, (turn + ONE) * COLOURS):
            d, colour = self.pieces[piece]
            for copy in self.loads(piece):
                copy.wait()
            for copy in self.swaps(piece):
                copy.wait_recv()
            where = self.slot(d, colour)
            if self.resident:
                for i, (src, rows) in enumerate(self.sources):
                    self.add_into(self.acc.at[(colour,) + where + (self.rows_of(i), slice(None))], [src.at[where + (rows, self.columns(self.core, colour))]], TWO)
            else:
                self.add_into(self.acc.at[(colour,) + where], [self.stage.at[piece % STAGES]], TWO)
            if piece + STAGES < len(self.pieces):
                for copy in self.loads(piece + STAGES):
                    copy.start()
            if turn == ZERO:
                for direction in range(TWO):
                    self.ring(colour, ZERO, direction)[ZERO].start()
            elif turn < THREE:
                self.ring(colour, ZERO, turn - ONE)[ONE].start()

    def relay(self, phase):
        for colour in range(COLOURS):
            for direction in range(TWO):
                far, _, fed = self.ring(colour, phase, direction)
                far.wait_recv()
                self.add_into(self.block(colour, phase, (ONE - TWO * direction) % SIDE, direction), [self.far_part(colour, phase, direction)], TWO - phase)
            for direction in range(TWO):
                self.ring(colour, phase, direction)[TWO].start()

    def settle(self, phase):
        for colour in range(COLOURS):
            for direction in range(TWO):
                _, own, fed = self.ring(colour, phase, direction)
                own.wait_recv()
                fed.wait_recv()
            self.add_into(self.block(colour, phase, ZERO), [self.got[phase].at[colour, direction] for direction in range(TWO)], TWO - phase)
            if phase < TWO:
                for kind in range(TWO):
                    for direction in range(TWO):
                        self.ring(colour, phase + ONE, direction)[kind].start()
            else:
                done = self.acc.at[colour, self.place[ZERO], self.place[ONE], self.place[TWO]]
                done[ALL] = done[ALL] * self.scale
                for give, keep in self.gives(colour):
                    keep.start()
                    give.start()

    def end(self):
        for colour in range(COLOURS):
            for give, keep in self.gives(colour):
                give.wait_recv()
                give.wait_send()
                keep.wait()
        for piece in range(len(self.pieces)):
            for copy in self.swaps(piece):
                copy.wait_send()
        for colour in range(COLOURS):
            for phase in range(THREE):
                for direction in range(TWO):
                    for copy in self.ring(colour, phase, direction):
                        copy.wait_send()


def rs_kernel(scale, *refs):
    scatter = Scatter(scale, [(ref, ZERO, ref.shape[THREE]) for ref in refs[:TWO]], refs[TWO:4], refs[4:])
    meet_neighbours(scatter.place)
    scatter.begin()
    for turn in range(THREE):
        scatter.absorb(turn)
    scatter.relay(ZERO)
    scatter.absorb(THREE)
    scatter.settle(ZERO)
    for phase in (ONE, TWO):
        scatter.relay(phase)
        scatter.settle(phase)
    scatter.end()


def as_torus(rows):
    return rows.reshape(SIDE, SIDE, SIDE, rows.shape[ZERO] // SIDE ** THREE, rows.shape[ONE])


def scatter_grads(g_attn, g_vec, scale):
    sources = [as_torus(g_attn), as_torus(g_vec)]
    heights = [src.shape[THREE] for src in sources]
    width = g_attn.shape[ONE]
    anywhere = pl.BlockSpec(memory_space=pl.ANY)
    return pl.pallas_call(
        functools.partial(rs_kernel, scale),
        in_specs=[anywhere] * TWO, out_specs=[anywhere] * TWO,
        out_shape=[jax.ShapeDtypeStruct((h, width), F32) for h in heights],
        scratch_shapes=Scatter.scratch_shapes(heights),
        compiler_params=pltpu.CompilerParams(collective_id=ONE, has_side_effects=True, vmem_limit_bytes=VMEM_BYTES),
        cost_estimate=pl.CostEstimate(flops=10 ** 9, bytes_accessed=8 * width * g_attn.shape[ZERO], transcendentals=ZERO),
        name='scatter_grads',
    )(*sources)


class Gather:
    def __init__(self, send_sem, recv_sem, base=ZERO):
        self.send_sem, self.recv_sem = send_sem, recv_sem
        self.used = base
        self.core, self.chip, self.place = lax.axis_index('dp'), lax.axis_index('fsdp'), torus_place()
        self.sibling = (ONE - self.core, self.chip)
        self.started = []

    def remote(self, src, dst, device):
        i = self.used
        self.used += ONE
        return pltpu.make_async_remote_copy(src_ref=src, dst_ref=dst, send_sem=self.send_sem.at[i], recv_sem=self.recv_sem.at[i], device_id=device, device_id_type=MESH_ID)

    def start(self, copy):
        copy.start()
        self.started.append(copy)

    def ring(self, colour, phase, view, own=None, split=False):
        order = DIM_ORDER[colour]
        dim = order[phase]
        have = sorted(order[:phase])

        def index(shift, half=None):
            where = [self.place[ZERO], self.place[ONE], self.place[TWO]]
            where[dim] = lax.rem(self.place[dim] + shift + SIDE, SIDE)
            for i, h in enumerate(have):
                where[h] = slice(None) if half is None or i > ZERO else pl.ds(TWO * half, TWO)
            return tuple(where)

        out = []
        for direction, shift in enumerate((ONE, -ONE)):
            device = (self.core, chip_at(self.place, dim, shift))
            half = direction if phase == ZERO else None
            near_dst = view(index(ZERO), None)
            if split:
                near = [self.remote(view(index(ZERO, h), None), view(index(ZERO, h), None), device) for h in (direction, ONE - direction)]
            else:
                near = [self.remote(near_dst if own is None else own, near_dst, device)]
            out.append(dict(
                near=near,
                far=self.remote(view(index(-shift, direction), half), view(index(-shift, direction), half), device),
                near_at=index(-shift), far_at=index(TWO, direction)))
        return out


def ag_kernel(attn_ref, ffn_ref, vec_ref, oattn_ref, planes_ref, vec_out, attn_v, send_sem, recv_sem, load_sem):
    net = Gather(send_sem, recv_sem)
    core, place = net.core, net.place
    rows, width = attn_ref.shape
    band = rows // (TWO * COLOURS)
    vec_high = vec_ref.shape[ZERO]
    stores, finals = [], []

    def band_rows(colour):
        return pl.ds(pl.multiple_of((core * COLOURS + colour) * band, band), band)

    def columns(half):
        return slice(None) if half is None else pl.ds(half * (width // TWO), width // TWO)

    def attn_view(colour):
        return lambda where, half: attn_v.at[where + (band_rows(colour), columns(half))]

    def ffn_view(colour):
        last = DIM_ORDER[colour][TWO]
        return lambda where, half: planes_ref.at[(colour,) + tuple(w for d, w in enumerate(where) if d != last) + (slice(None), columns(half))]

    def vec_view(where, half):
        return vec_out.at[where + (slice(None) if half is None else pl.ds(half * (vec_high // TWO), vec_high // TWO), slice(None))]

    colours = range(COLOURS)
    attn_own = [attn_ref.at[band_rows(colour), :] for colour in colours]
    ffn_own = [ffn_ref.at[band_rows(colour), :] for colour in colours]
    rings = {('attn', phase): [net.ring(colour, phase, attn_view(colour), attn_own[colour] if phase == ZERO else None, phase > ZERO) for colour in colours] for phase in range(THREE)}
    rings |= {('ffn', phase): [net.ring(colour, phase, ffn_view(colour), ffn_own[colour] if phase == ZERO else None, phase > ZERO) for colour in colours] for phase in range(TWO)}
    rings |= {('vec', phase): [net.ring(ONE, phase, vec_view, vec_ref if phase == ZERO else None)] for phase in range(THREE)}

    def publish(at):
        keep = pltpu.make_async_copy(attn_v.at[at], oattn_ref.at[at], load_sem.at[len(stores)])
        keep.start()
        stores.append(keep)
        give = net.remote(attn_v.at[at], oattn_ref.at[at], net.sibling)
        net.start(give)
        finals.append(give)

    def send_near(name, phase):
        for ring in rings.get((name, phase), ()):
            for way in ring:
                for copy in way['near']:
                    net.start(copy)

    def pass_on(name, phase):
        for ring in rings.get((name, phase), ()):
            for way in ring:
                way['near'][ZERO].wait_recv()
                net.start(way['far'])
        if phase == TWO and name == 'attn':
            for colour in colours:
                for way in rings[(name, phase)][colour]:
                    way['near'][ONE].wait_recv()
                    publish(way['near_at'] + (band_rows(colour), slice(None)))

    def complete(name, phase):
        for colour, ring in enumerate(rings.get((name, phase), ())):
            for way in ring:
                way['far'].wait_recv()
                if phase == ONE and name != 'vec':
                    way['near'][ONE].wait_recv()
            if phase < TWO and (name, phase + ONE) in rings:
                for way in rings[(name, phase + ONE)][colour]:
                    for copy in way['near']:
                        net.start(copy)
            if phase == TWO and name == 'attn':
                for way in ring:
                    publish(way['far_at'] + (band_rows(colour), slice(None)))
        if phase == ONE and name == 'attn':
            for colour in colours:
                last = DIM_ORDER[colour][TWO]
                publish(tuple(place[d] if d == last else slice(None) for d in range(THREE)) + (band_rows(colour), slice(None)))

    for colour in colours:
        attn_v[(place[ZERO], place[ONE], place[TWO]) + (band_rows(colour), slice(None))] = attn_ref[band_rows(colour), :]
        kept = [place[d] for d in range(THREE) if d != DIM_ORDER[colour][TWO]]
        planes_ref[(colour, kept[ZERO], kept[ONE])] = ffn_ref[band_rows(colour), :]
    vec_out[place[ZERO], place[ONE], place[TWO]] = vec_ref[ALL]
    meet_neighbours(place)
    names = ('attn', 'vec', 'ffn')
    for name in names:
        send_near(name, ZERO)
    for phase in range(THREE):
        for name in names:
            pass_on(name, phase)
        for name in names:
            complete(name, phase)
    for copy in finals:
        copy.wait_recv()
    for copy in net.started:
        copy.wait_send()
    for copy in stores:
        copy.wait()


def gather_params(attn_w, ffn_w, vec_rows):
    rows, width = attn_w.shape
    full = (SIDE, SIDE, SIDE, rows, width)
    n_copies = COLOURS * (4 * TWO + 6 * THREE) + 4 * THREE + COLOURS * 5
    vmem = pl.BlockSpec(memory_space=pltpu.VMEM)
    return pl.pallas_call(
        ag_kernel,
        in_specs=[vmem] * THREE, out_specs=[pl.BlockSpec(memory_space=pl.ANY), vmem, vmem],
        out_shape=[jax.ShapeDtypeStruct(full, BF16), jax.ShapeDtypeStruct((COLOURS, SIDE, SIDE, rows // (TWO * COLOURS), width), BF16),
                   jax.ShapeDtypeStruct((SIDE, SIDE, SIDE) + vec_rows.shape, F32)],
        scratch_shapes=[pltpu.VMEM(full, BF16), pltpu.SemaphoreType.DMA((n_copies,)), pltpu.SemaphoreType.DMA((n_copies,)), pltpu.SemaphoreType.DMA((COLOURS * 5,))],
        compiler_params=pltpu.CompilerParams(collective_id=TWO, has_side_effects=True, vmem_limit_bytes=VMEM_BYTES),
        cost_estimate=pl.CostEstimate(flops=10 ** 9, bytes_accessed=4 * rows * width * SIDE ** THREE, transcendentals=ZERO),
        name='gather_params',
    )(attn_w, ffn_w, vec_rows)


class LastPhase:
    def __init__(self, planes, out, near, far, send_sem, recv_sem, load_sem):
        self.planes, self.out, self.near, self.far = planes, out, near, far
        self.send_sem, self.recv_sem, self.load_sem = send_sem, recv_sem, load_sem
        self.core, self.chip, self.place = lax.axis_index('dp'), lax.axis_index('fsdp'), torus_place()
        self.band = planes.shape[THREE]

    @staticmethod
    def scratch_shapes(planes):
        colours, side, _, band, width = planes.shape
        sems = [pltpu.SemaphoreType.DMA((11 * COLOURS,)), pltpu.SemaphoreType.DMA((11 * COLOURS,)), pltpu.SemaphoreType.DMA((5 * COLOURS,))]
        return [pltpu.VMEM((colours, TWO, side, side, band, width), BF16), pltpu.VMEM((colours, TWO, side // TWO, side, band, width), BF16)] + sems

    def remote(self, i, src, dst, device):
        return pltpu.make_async_remote_copy(src_ref=src, dst_ref=dst, send_sem=self.send_sem.at[i], recv_sem=self.recv_sem.at[i], device_id=device, device_id_type=MESH_ID)

    def ring(self, colour, direction):
        device = (self.core, chip_at(self.place, DIM_ORDER[colour][TWO], ONE - TWO * direction))
        i = 11 * colour + THREE * direction
        got = self.near.at[colour, direction]
        near = [self.remote(i + n, self.planes.at[colour, pl.ds(TWO * half, TWO)], got.at[pl.ds(TWO * half, TWO)], device) for n, half in enumerate((direction, ONE - direction))]
        return near + [self.remote(i + TWO, got.at[pl.ds(TWO * direction, TWO)], self.far.at[colour, direction], device)]

    def shares(self, colour):
        last = DIM_ORDER[colour][TWO]
        rows = pl.ds(pl.multiple_of((self.core * COLOURS + colour) * self.band, self.band), self.band)
        views = [(self.planes.at[colour], ZERO, None)]
        views += [(self.near.at[colour, direction], TWO * direction - ONE, None) for direction in range(TWO)]
        views += [(self.far.at[colour, direction], TWO, direction) for direction in range(TWO)]
        out = []
        for n, (src, shift, half) in enumerate(views):
            where = [slice(None)] * THREE
            where[last] = lax.rem(self.place[last] + shift + SIDE, SIDE)
            if half is not None:
                where[min(d for d in range(THREE) if d != last)] = pl.ds(TWO * half, TWO)
            dst = self.out.at[tuple(where) + (rows, slice(None))]
            out.append((self.remote(11 * colour + 6 + n, src, dst, (ONE - self.core, self.chip)), pltpu.make_async_copy(src, dst, self.load_sem.at[5 * colour + n])))
        return out

    def share(self, colour, which):
        for n in which:
            give, keep = self.shares(colour)[n]
            give.start()
            keep.start()

    def begin(self):
        for colour in range(COLOURS):
            for direction in range(TWO):
                for copy in self.ring(colour, direction)[:TWO]:
                    copy.start()
        for colour in range(COLOURS):
            self.share(colour, (ZERO,))

    def pass_on(self):
        for colour in range(COLOURS):
            for direction in range(TWO):
                first, _, far = self.ring(colour, direction)
                first.wait_recv()
                far.start()
        for colour in range(COLOURS):
            for direction in range(TWO):
                self.ring(colour, direction)[ONE].wait_recv()
            self.share(colour, (ONE, TWO))

    def complete(self):
        for colour in range(COLOURS):
            for direction in range(TWO):
                self.ring(colour, direction)[TWO].wait_recv()
            self.share(colour, (THREE, 4))

    def end(self):
        for colour in range(COLOURS):
            for give, keep in self.shares(colour):
                give.wait_recv()
                give.wait_send()
                keep.wait()
            for direction in range(TWO):
                for copy in self.ring(colour, direction):
                    copy.wait_send()


def dot(lhs, rhs, contract=((ONE,), (ZERO,))):
    return lax.dot_general(lhs, rhs, (contract, ((), ())), preferred_element_type=F32)


def dot_nt(lhs, rhs):
    return dot(lhs, rhs, ((ONE,), (ONE,)))


def dot_tn(lhs, rhs):
    return dot(lhs, rhs, ((ZERO,), (ZERO,)))


def norm_rows(resid, gain, shift):
    mean = jnp.mean(resid, axis=-ONE, keepdims=True)
    centred = resid - mean
    inv_std = lax.rsqrt(jnp.mean(centred * centred, axis=-ONE, keepdims=True) + LN_EPS)
    normed = centred * inv_std
    return (normed * gain + shift).astype(BF16), normed, inv_std


def norm_rows_bwd(d_out, normed, inv_std, gain):
    d_norm = d_out * gain
    return inv_std * (d_norm - jnp.mean(d_norm, axis=-ONE, keepdims=True) - normed * jnp.mean(d_norm * normed, axis=-ONE, keepdims=True))


def col_sum(values):
    return jnp.sum(values, axis=ZERO, keepdims=True)


def lane_row(head, dtype=BF16):
    lane = lax.broadcasted_iota(jnp.int32, (ONE, PAIR), ONE)
    return jnp.where((lane >= HEAD_DIM * head) & (lane < HEAD_DIM * (head + ONE)), 1.0, 0.0).astype(dtype)


def spare_lane(head):
    lane = lax.broadcasted_iota(jnp.int32, (ONE, PAIR), ONE)
    return jnp.where(lane == HEAD_DIM * (ONE - head), 1.0, 0.0)


def mask_fill(n_rows, n_valid):
    row = lax.broadcasted_iota(jnp.int32, (n_rows, PAIR), ZERO)
    return jnp.where(row >= n_valid, MASK_FILL, 0.0)


def head_masks(pair_q, pair_k, head, fill):
    q_f = pair_q * lane_row(head) + spare_lane(head).astype(BF16)
    k_f = pair_k * lane_row(head) + (fill * spare_lane(head)).astype(BF16)
    return q_f, k_f


def half_only(pair, head):
    return pair * lane_row(head)


def join_halves(first, second):
    lane = lax.broadcasted_iota(jnp.int32, first.shape, ONE)
    return jnp.where(lane < HEAD_DIM, first, second)


def score_blocks(n_heads, n_q, n_k, causal, step):
    if not causal:
        return [(head, ZERO, n_q, n_k) for head in range(n_heads)]
    return [(head, first, step, first + step) for head in range(n_heads) for first in range(ZERO, n_q, step)]


def scores_t(q_f, k_f, causal, first):
    s_t = dot_nt(k_f, q_f)
    if causal:
        key_i = lax.broadcasted_iota(jnp.int32, s_t.shape, ZERO)
        qry_i = lax.broadcasted_iota(jnp.int32, s_t.shape, ONE) + first
        s_t = jnp.where(key_i <= qry_i, s_t, MASK_FILL)
    return s_t


def pair_of(group, head):
    return group[:, head // TWO * PAIR:(head // TWO + ONE) * PAIR]


def masked_pairs(q_g, k_g, n_valid):
    fill = mask_fill(k_g.shape[ZERO], n_valid)
    cache = {}

    def get(head):
        if head not in cache:
            cache[head] = head_masks(pair_of(q_g, head), pair_of(k_g, head), head % TWO, fill)
        return cache[head]

    return get


def stack_heads(parts, n_heads):
    return jnp.concatenate([jnp.concatenate(parts[head], axis=ONE) for head in range(n_heads)], axis=ZERO)


def run_ahead(blocks, produce, transform, consume, delay):
    ahead = produce(blocks[ZERO])
    waiting = []
    for i, block in enumerate(blocks):
        now = ahead
        if i + ONE < len(blocks):
            ahead = produce(blocks[i + ONE])
        waiting.append((block, transform(block, now)))
        if len(waiting) > delay:
            consume(*waiting.pop(ZERO))
    for item in waiting:
        consume(*item)


def attend_group(q_g, k_g, v_g, n_valid, causal, lse_ref):
    n_heads = GROUP // HEAD_DIM
    o_parts = [[] for _ in range(n_heads)]
    v_t = v_g.T
    masked = masked_pairs(q_g, k_g, n_valid)

    def produce(block):
        head, first, n_q, n_k = block
        q_f, k_f = masked(head)
        return scores_t(q_f[first:first + n_q], k_f[:n_k], causal, first)

    def transform(block, s_t):
        head, first, n_q, n_k = block
        top = jnp.max(s_t, axis=ZERO, keepdims=True)
        e_t = jnp.exp(s_t - top)
        total = jnp.sum(e_t, axis=ZERO, keepdims=True)
        lse_ref[ZERO, ZERO, head // TWO, head % TWO:head % TWO + ONE, first:first + n_q] = top + jnp.log(total)
        return (e_t * (1.0 / total)).astype(BF16)

    def consume(block, p_t):
        head, first, n_q, n_k = block
        o_parts[head].append(dot(v_t[HEAD_DIM * head:HEAD_DIM * (head + ONE), :n_k], p_t))

    run_ahead(score_blocks(n_heads, q_g.shape[ZERO], k_g.shape[ZERO], causal, 128), produce, transform, consume, TWO)
    return stack_heads(o_parts, n_heads).T.astype(BF16)


def attend_group_bwd(d_o, q_g, k_g, v_g, n_valid, causal, lse_ref):
    n_heads = q_g.shape[ONE] // HEAD_DIM
    k_t = k_g.T
    dq_t, dk_h, dv_h = [[] for _ in range(n_heads)], [None] * n_heads, [None] * n_heads
    masked = masked_pairs(q_g, k_g, n_valid)
    v_half = {}

    def produce(block):
        head, first, n_q, n_k = block
        q_f, k_f = masked(head)
        if head not in v_half:
            v_half[head] = half_only(pair_of(v_g, head), head % TWO)
        rows = slice(first, first + n_q)
        return scores_t(q_f[rows], k_f[:n_k], causal, first), dot_nt(v_half[head][:n_k], pair_of(d_o, head)[rows])

    def transform(block, products):
        head, first, n_q, n_k = block
        s_t, dp_t = products
        p_t = jnp.exp(s_t - lse_ref[head // TWO, head % TWO:head % TWO + ONE, first:first + n_q])
        weighted = p_t * dp_t
        return p_t.astype(BF16), (weighted - p_t * jnp.sum(weighted, axis=ZERO, keepdims=True)).astype(BF16)

    def grow(old, new):
        if old is None:
            return new
        n_old = old.shape[ZERO]
        return old + new if n_old == new.shape[ZERO] else jnp.concatenate([old + new[:n_old], new[n_old:]], axis=ZERO)

    def consume(block, operands):
        head, first, n_q, n_k = block
        p_b, ds_t = operands
        rows = slice(first, first + n_q)
        dv_h[head] = grow(dv_h[head], dot(p_b, pair_of(d_o, head)[rows]))
        dk_h[head] = grow(dk_h[head], dot(ds_t, pair_of(q_g, head)[rows]))
        dq_t[head].append(dot(k_t[HEAD_DIM * head:HEAD_DIM * (head + ONE), :n_k], ds_t))

    run_ahead(score_blocks(n_heads, q_g.shape[ZERO], k_g.shape[ZERO], causal, 256), produce, transform, consume, ZERO)
    join = lambda parts: jnp.concatenate([join_halves(parts[h], parts[h + ONE]) for h in range(ZERO, n_heads, TWO)], axis=ONE)
    return stack_heads(dq_t, n_heads).T * 0.125, join(dk_h), join(dv_h)


def attn_fwd_kernel(causal, slots, guest, lens_ref, x_ref, kv_ref, wq_ref, wk_ref, wv_ref, w_all, bias_ref, rows_ref,
                    q_ref, k_ref, v_ref, o_ref, lse_ref, h_ref, normed_ref, inv_ref, o_all, wo_v, load_sem):
    q_row, k_row, v_row, o_row, gain_row, o_mat = slots
    sample, group = pl.program_id(ZERO), pl.program_id(ONE)
    d_model = wo_v.shape[ZERO]
    fetch = pltpu.make_async_copy(w_all.at[pl.ds(o_mat * d_model, d_model), :], wo_v, load_sem)

    @pl.when((sample == ZERO) & (group == ZERO))
    def _():
        fetch.start()

    turn = sample * pl.num_programs(ONE) + group
    if guest is not None:
        for where, steps in ((ZERO, (lambda: meet_neighbours(guest.place), guest.begin)), (THREE, (guest.pass_on,)), (5, (guest.complete,))):
            @pl.when(turn == where)
            def _():
                for step in steps:
                    step()

    x_b, kv_b = x_ref[ALL], kv_ref[ALL]
    q_g = ((dot(x_b, wq_ref[ALL]) + bias_ref[q_row:q_row + ONE, :]) * 0.125).astype(BF16)
    k_g = (dot(kv_b, wk_ref[ALL]) + bias_ref[k_row:k_row + ONE, :]).astype(BF16)
    v_g = (dot(kv_b, wv_ref[ALL]) + bias_ref[v_row:v_row + ONE, :]).astype(BF16)
    q_ref[ALL], k_ref[ALL], v_ref[ALL] = q_g, k_g, v_g
    o_g = attend_group(q_g, k_g, v_g, lens_ref[sample], causal, lse_ref)
    o_ref[ALL] = o_g
    o_all[:, pl.ds(pl.multiple_of(group * GROUP, GROUP), GROUP)] = o_g

    @pl.when((sample == ZERO) & (group == pl.num_programs(ONE) - ONE))
    def _():
        fetch.wait()

    @pl.when(group == pl.num_programs(ONE) - ONE)
    def _():
        resid = x_ref[ALL].astype(F32) + dot(o_all[ALL], wo_v[ALL]) + rows_ref[o_row:o_row + ONE, :]
        h_out, normed, inv_std = norm_rows(resid, rows_ref[gain_row:gain_row + ONE, :], rows_ref[gain_row + ONE:gain_row + TWO, :])
        h_ref[ALL], normed_ref[ALL], inv_ref[ALL] = h_out, normed, inv_std

    if guest is not None:
        @pl.when(turn == pl.num_programs(ZERO) * pl.num_programs(ONE) - ONE)
        def _():
            guest.end()


def attn_forward(x, kv, lens, attn_full, bias_rows, mats, slots, causal, planes=None, full_rows=None):
    d_model = x.shape[-ONE]
    n_batch = lens.shape[ZERO]
    n_q, n_k = x.shape[ZERO] // n_batch, kv.shape[ZERO] // n_batch
    n_groups = d_model // GROUP
    col = lambda mat: pl.BlockSpec((d_model, GROUP), lambda b, g: (mat, g))
    q_blk = pl.BlockSpec((n_q, GROUP), lambda b, g: (b, g))
    k_blk = pl.BlockSpec((n_k, GROUP), lambda b, g: (b, g))
    tok = lambda n: pl.BlockSpec((n, d_model), lambda b, g: (b, ZERO))
    n_heads_g = GROUP // HEAD_DIM
    out_shape = (
        jax.ShapeDtypeStruct(x.shape, BF16), jax.ShapeDtypeStruct(kv.shape, BF16), jax.ShapeDtypeStruct(kv.shape, BF16),
        jax.ShapeDtypeStruct(x.shape, BF16), jax.ShapeDtypeStruct((n_batch, n_groups, n_heads_g // TWO, TWO, n_q), F32),
        jax.ShapeDtypeStruct(x.shape, BF16), jax.ShapeDtypeStruct(x.shape, F32), jax.ShapeDtypeStruct((x.shape[ZERO], ONE), F32))
    kernel = functools.partial(attn_fwd_kernel, causal, slots + (mats[THREE],))
    in_specs = [pl.BlockSpec(memory_space=pltpu.SMEM), tok(n_q), tok(n_k), col(mats[ZERO]), col(mats[ONE]), col(mats[TWO]), pl.BlockSpec(memory_space=pl.ANY),
                pl.BlockSpec((bias_rows.shape[ZERO], GROUP), lambda b, g: (ZERO, g)), pl.BlockSpec(bias_rows.shape, lambda b, g: (ZERO, ZERO))]
    out_specs = [q_blk, k_blk, k_blk, q_blk, pl.BlockSpec((ONE, ONE, n_heads_g // TWO, TWO, n_q), lambda b, g: (b, g, ZERO, ZERO, ZERO)),
                 tok(n_q), tok(n_q), pl.BlockSpec((n_q, ONE), lambda b, g: (b, ZERO))]
    scratch = [pltpu.VMEM((n_q, d_model), BF16), pltpu.VMEM((d_model, d_model), BF16), pltpu.SemaphoreType.DMA]
    args = [lens, x, kv, attn_full, attn_full, attn_full, attn_full, bias_rows, bias_rows]
    params = dict(vmem_limit_bytes=VMEM_BYTES, dimension_semantics=('arbitrary', 'arbitrary'))
    if planes is None:
        body = functools.partial(kernel, None)
    else:
        n_in, n_out, n_own = len(args), len(out_specs), len(scratch)

        def body(*refs):
            ins, held, outs, whole, rest = refs[:n_in], refs[n_in], refs[n_in + ONE:n_in + ONE + n_out], refs[n_in + ONE + n_out], refs[n_in + TWO + n_out:]
            kernel(LastPhase(held, whole, *rest[n_own:]), *ins, *outs, *rest[:n_own])

        in_specs.append(pl.BlockSpec(memory_space=pltpu.VMEM))
        args.append(planes)
        out_specs.append(pl.BlockSpec(memory_space=pl.ANY))
        out_shape += (jax.ShapeDtypeStruct((SIDE, SIDE, SIDE, full_rows // SIDE ** THREE, d_model), BF16),)
        scratch += LastPhase.scratch_shapes(planes)
        params |= dict(collective_id=5, has_side_effects=True)
    return pl.pallas_call(
        body, grid=(n_batch, n_groups), in_specs=in_specs, out_specs=out_specs, out_shape=out_shape, scratch_shapes=scratch,
        compiler_params=pltpu.CompilerParams(**params),
        cost_estimate=pl.CostEstimate(flops=TWO * d_model * d_model * (TWO * x.shape[ZERO] + TWO * kv.shape[ZERO]) + 16 * x.shape[ZERO] * n_k * d_model, bytes_accessed=20 * x.shape[ZERO] * d_model, transcendentals=ZERO),
        name='attn_fwd',
    )(*args)


def attn_bwd_kernel(causal, gain_row, mats, guest, lens_ref, dres_ref, wo_ref, w_all, q_ref, k_ref, v_ref, lse_ref,
                    rows_ref, normed_ref, inv_ref, lhs_refs, dx_ref, dkv_ref, sums_ref, tail_ref, grads_ref,
                    rhs_q, rhs_k, lhs_q, lhs_k, do_v, w_v, grad_v, load_sem, store_sem):
    sample, group = pl.program_id(ZERO), pl.program_id(ONE)
    d_model = w_v.shape[ONE]
    n_q, n_k = q_ref.shape[ZERO], k_ref.shape[ZERO]
    last = pl.num_programs(ONE) - ONE
    fetches = [pltpu.make_async_copy(w_all.at[pl.ds(mat * d_model, d_model), :], w_v.at[i], load_sem.at[i]) for i, mat in enumerate(mats[:THREE])]
    dk_all, dv_all = (rhs_q.at[ONE], rhs_q.at[TWO]) if causal else (rhs_k.at[ZERO], rhs_k.at[ONE])
    d_all, dres_all = rhs_q.at[ZERO], rhs_q.at[THREE if causal else ONE]
    places = (lhs_q.at[ZERO], lhs_q.at[ONE]) if causal else (lhs_q.at[ZERO], lhs_k, lhs_q.at[ZERO])
    lhs_fetch = lambda i: pltpu.make_async_copy(lhs_refs[i], places[i], load_sem.at[THREE + i])
    store = lambda buf, mat: pltpu.make_async_copy(grad_v.at[buf], grads_ref.at[pl.ds(pl.multiple_of(mat * d_model, d_model), d_model), :], store_sem.at[buf])

    @pl.when((sample == ZERO) & (group == ZERO))
    def _():
        for fetch in fetches + [lhs_fetch(ZERO), lhs_fetch(ONE)]:
            fetch.start()

    turn = sample * pl.num_programs(ONE) + group
    q_rows = pl.ds(pl.multiple_of(sample * n_q, n_q), n_q)
    k_rows = pl.ds(pl.multiple_of(sample * n_k, n_k), n_k)
    d_o = dot_nt(dres_ref[ALL].astype(BF16), wo_ref[ALL]).astype(BF16)

    def keep(found, first, width):
        here = pl.ds(first, width)
        cols = pl.ds(pl.multiple_of(group * GROUP + first, PAIR), width)
        for i, (full, rows, value) in enumerate(zip((d_all, dk_all, dv_all), (q_rows, k_rows, k_rows), found)):
            sums_ref[ZERO, i:i + ONE, here] = col_sum(value)
            full[rows, cols] = value.astype(BF16)

    if causal:
        keep(attend_group_bwd(d_o, q_ref[ALL], k_ref[ALL], v_ref[ALL], lens_ref[sample], causal, lse_ref.at[ZERO, ZERO]), ZERO, GROUP)
    else:
        do_v[ALL] = d_o

        def one_pair(pair, _):
            guest(ZERO, TWO * turn + pair)
            first = pl.multiple_of(pair * PAIR, PAIR)
            here = pl.ds(first, PAIR)
            keep(attend_group_bwd(do_v[:, here], q_ref[:, here], k_ref[:, here], v_ref[:, here], lens_ref[sample], causal, lse_ref.at[ZERO, ZERO, pl.ds(pair, ONE)]), first, PAIR)
            return ZERO

        lax.fori_loop(ZERO, GROUP // PAIR, one_pair, ZERO)

    @pl.when(group == ZERO)
    def _():
        dres_all[q_rows, :] = dres_ref[ALL].astype(BF16)

    @pl.when((sample == ZERO) & (group == last))
    def _():
        for fetch in fetches:
            fetch.wait()

    guest(THREE, turn)

    @pl.when(group == last)
    def _():
        d_kv = dot_nt(dk_all[k_rows, :], w_v[ONE]) + dot_nt(dv_all[k_rows, :], w_v[TWO])
        d_h = dres_ref[ALL] + dot_nt(d_all[q_rows, :], w_v[ZERO])
        if causal:
            dx_ref[ALL] = (d_h + d_kv).astype(BF16)
            tail_ref[ALL] = jnp.zeros_like(tail_ref)
        else:
            dkv_ref[ALL] = d_kv.astype(BF16)
            normed = normed_ref[ALL]
            d_resid = norm_rows_bwd(d_h, normed, inv_ref[ALL], rows_ref[gain_row:gain_row + ONE, :])
            dx_ref[ALL] = d_resid
            tail_ref[ZERO, ZERO:ONE, :] = col_sum(d_resid)
            tail_ref[ZERO, ONE:TWO, :] = col_sum(d_h * normed)
            tail_ref[ZERO, TWO:THREE, :] = col_sum(d_h)

    @pl.when(turn == pl.num_programs(ZERO) * pl.num_programs(ONE) - ONE)
    def _():
        guest(TWO, 12)
        lhs_fetch(ZERO).wait()
        if causal:
            lhs_fetch(ONE).wait()

            def square(i, _):
                @pl.when(i >= TWO)
                def _():
                    store(i % TWO, mats[ZERO]).wait()

                grad_v[i % TWO] = dot_tn(lhs_q[i // THREE], rhs_q[i])
                store(i % TWO, mats[ZERO] + i).start()
                return ZERO

            lax.fori_loop(ZERO, 4, square, ZERO)
        else:
            def square_q(i, _):
                @pl.when(i == ONE)
                def _():
                    lhs_fetch(TWO).start()
                    lhs_fetch(TWO).wait()

                grad_v[i] = dot_tn(lhs_q[ZERO], rhs_q[i])
                store(i, mats[ZERO] + THREE * i).start()
                return ZERO

            def square_k(i, _):
                store(i, mats[ONE]).wait()
                grad_v[i] = dot_tn(lhs_k[ALL], rhs_k[i])
                store(i, mats[ONE] + i).start()
                return ZERO

            lax.fori_loop(ZERO, TWO, square_q, ZERO)
            guest(TWO, 13)
            lhs_fetch(ONE).wait()
            lax.fori_loop(ZERO, TWO, square_k, ZERO)
            guest(TWO, 14)
        for buf in range(TWO):
            store(buf, mats[ZERO]).wait()


def scatter_guest(scatter, plan, parity, position):
    steps = dict(end=scatter.end) | {('relay', p): functools.partial(scatter.relay, p) for p in range(THREE)}
    steps |= {('settle', p): functools.partial(scatter.settle, p) for p in range(THREE)} | {turn: functools.partial(scatter.absorb, turn) for turn in range(SIDE)}
    if parity == TWO:
        for name in plan.get(position, ()):
            steps[name]()
        return
    if parity == THREE:
        @pl.when(position == 5)
        def _():
            for name in plan['late']:
                steps[name]()
        return
    if parity == ZERO:
        @pl.when(position == ZERO)
        def _():
            meet_neighbours(scatter.place)
            scatter.begin()
    for where, names in plan.items():
        if where != 'late' and where < 12:
            @pl.when(position == where)
            def _():
                for name in names:
                    steps[name]()


def no_guest(parity, position):
    pass


def attn_backward(dres, q, k, v, lse, lens, attn_full, bias_rows, mats, causal, lhs_list, g_rows=None, scale=None, gain_row=ZERO, normed=None, inv_std=None, grads=None):
    d_model = q.shape[-ONE]
    n_batch = lens.shape[ZERO]
    n_q, n_k = q.shape[ZERO] // n_batch, k.shape[ZERO] // n_batch
    n_groups = d_model // GROUP
    row = lambda mat: pl.BlockSpec((GROUP, d_model), lambda b, g: (mat * n_groups + g, ZERO))
    q_blk = pl.BlockSpec((n_q, GROUP), lambda b, g: (b, g))
    k_blk = pl.BlockSpec((n_k, GROUP), lambda b, g: (b, g))
    tok = lambda n: pl.BlockSpec((n, d_model), lambda b, g: (b, ZERO))
    n_heads_g = GROUP // HEAD_DIM
    anywhere = pl.BlockSpec(memory_space=pl.ANY)
    in_specs = [pl.BlockSpec(memory_space=pltpu.SMEM), tok(n_q), row(mats[THREE]), anywhere, q_blk, k_blk, k_blk,
                pl.BlockSpec((ONE, ONE, n_heads_g // TWO, TWO, n_q), lambda b, g: (b, g, ZERO, ZERO, ZERO)), pl.BlockSpec(bias_rows.shape, lambda b, g: (ZERO, ZERO))]
    args = [lens, dres, attn_full, attn_full, q, k, v, lse, bias_rows]
    tail_shape = jax.ShapeDtypeStruct((n_batch, 8, d_model), F32)
    out_shape = [jax.ShapeDtypeStruct(q.shape, BF16 if causal else F32)]
    out_specs = [tok(n_q)]
    if not causal:
        late = dict(pipeline_mode=pl.Buffered(ONE))
        in_specs += [pl.BlockSpec((n_q, d_model), lambda b, g: (b, ZERO), **late), pl.BlockSpec((n_q, ONE), lambda b, g: (b, ZERO), **late)]
        args += [normed, inv_std]
        out_shape.append(jax.ShapeDtypeStruct(k.shape, BF16))
        out_specs.append(tok(n_k))
    n_lhs_at = len(args)
    args += list(lhs_list)
    in_specs += [anywhere] * len(lhs_list)
    out_shape += [tail_shape, tail_shape, jax.ShapeDtypeStruct(attn_full.shape, F32)]
    out_specs += [pl.BlockSpec((ONE, 8, GROUP), lambda b, g: (b, ZERO, g)), pl.BlockSpec((ONE, 8, d_model), lambda b, g: (b, ZERO, ZERO)), anywhere]
    held = lambda count, n: pltpu.VMEM((count, n_batch * n, d_model), BF16)
    own = [held(4, n_q), held(TWO, n_q)] if causal else [held(TWO, n_q), held(TWO, n_k), held(ONE, n_q), pltpu.VMEM((n_batch * n_k, d_model), BF16)]
    own += [] if causal else [pltpu.VMEM((n_q, GROUP), BF16)]
    own += [pltpu.VMEM((THREE, d_model, d_model), BF16), pltpu.VMEM((TWO, d_model, d_model), F32), pltpu.SemaphoreType.DMA((6,)), pltpu.SemaphoreType.DMA((TWO,))]
    kernel = functools.partial(attn_bwd_kernel, causal, gain_row, mats)
    params = dict(vmem_limit_bytes=VMEM_BYTES, dimension_semantics=('arbitrary', 'arbitrary'))
    aliases = {}
    if causal:
        args.append(grads)
        in_specs.append(anywhere)
        aliases = {len(args) - ONE: len(out_shape) - ONE}
    else:
        args.append(as_torus(g_rows))
        in_specs.append(anywhere)
        n_rows = args[-ONE].shape[THREE]
        out_shape.append(jax.ShapeDtypeStruct((n_rows, d_model), F32))
        out_specs.append(anywhere)
        params |= dict(collective_id=THREE, has_side_effects=True, vmem_limit_bytes=67043328)
    scratch = own + ([] if causal else Scatter.scratch_shapes([n_rows]))
    n_in, n_out, n_own = len(args), len(out_shape), len(own)

    def body(*refs):
        ins, outs, rest = refs[:n_in], refs[n_in:n_in + n_out], refs[n_in + n_out:]
        lhs_refs, mine = ins[n_lhs_at:-ONE], rest[:n_own]
        if causal:
            dx, sums, tail, grads_ref = outs
            kernel(no_guest, *ins[:n_lhs_at], None, None, lhs_refs, dx, None, sums, tail, grads_ref, mine[ZERO], None, mine[ONE], None, None, *mine[TWO:])
        else:
            dx, dkv, sums, tail, grads_ref, total = outs
            scatter = Scatter(scale, [(ins[-ONE], ZERO, n_rows)], [total], rest[n_own:])
            kernel(functools.partial(scatter_guest, scatter, CROSS_PLAN), *ins[:n_lhs_at], lhs_refs, dx, dkv, sums, tail, grads_ref, *mine)

    return pl.pallas_call(
        body, grid=(n_batch, n_groups), in_specs=in_specs, out_specs=out_specs, out_shape=out_shape, scratch_shapes=scratch, input_output_aliases=aliases,
        compiler_params=pltpu.CompilerParams(**params),
        cost_estimate=pl.CostEstimate(flops=TWO * d_model * d_model * (TWO * q.shape[ZERO] + TWO * k.shape[ZERO]) + 40 * q.shape[ZERO] * n_k * d_model, bytes_accessed=20 * q.shape[ZERO] * d_model, transcendentals=ZERO),
        name='attn_bwd',
    )(*args)


def ffn_kernel(n_blocks, h_ref, dy_ref, up_ref, down_ref, rows_ref, bias_ref, normed_ref, inv_ref,
               y_ref, grad_ref, dres2_ref, tail_ref, upsum_ref, left_all, right_all):
    step = pl.program_id(ZERO)
    block, d_model = h_ref.shape
    n_square = left_all.shape[TWO] // d_model

    @pl.when(step < n_blocks)
    def _():
        rows = pl.ds(pl.multiple_of(step * block, block), block)
        h_b = h_ref[ALL]
        right_all[ZERO, rows, :] = h_b
        up = dot_nt(h_b, up_ref[ALL]) + bias_ref[ALL]
        cdf = 0.5 * (1.0 + lax.erf(up * 0.7071067811865476))
        gelu = (up * cdf).astype(BF16)
        slope = cdf + up * (0.3989422804014327 * jnp.exp(-0.5 * up * up))
        left_all[ONE, rows, :] = gelu
        resid = h_b.astype(F32) + dot(gelu, down_ref[ALL]) + rows_ref[8:9, :]
        y_b, normed3, inv3 = norm_rows(resid, rows_ref[13:14, :], rows_ref[14:15, :])
        y_ref[ALL] = y_b
        dy = dy_ref[ALL].astype(F32)
        d_res3 = norm_rows_bwd(dy, normed3, inv3, rows_ref[13:14, :])
        d_res3_b = d_res3.astype(BF16)
        right_all[ONE, rows, :] = d_res3_b
        d_up = dot_nt(d_res3_b, down_ref[ALL]) * slope
        d_up_b = d_up.astype(BF16)
        left_all[ZERO, rows, :] = d_up_b
        d_h2 = d_res3 + dot(d_up_b, up_ref[ALL])
        normed2 = normed_ref[ALL]
        d_res2 = norm_rows_bwd(d_h2, normed2, inv_ref[ALL], rows_ref[11:12, :])
        dres2_ref[ALL] = d_res2
        tail = jnp.concatenate([col_sum(d_res2), col_sum(d_res3), col_sum(d_h2 * normed2), col_sum(d_h2), col_sum(dy * normed3), col_sum(dy),
                                jnp.zeros((TWO, dy.shape[ONE]), F32)], axis=ZERO)
        up_sum = col_sum(d_up)

        @pl.when(step == ZERO)
        def _():
            tail_ref[ALL] = tail
            upsum_ref[ALL] = up_sum

        @pl.when(step > ZERO)
        def _():
            tail_ref[ALL] += tail
            upsum_ref[ALL] += up_sum

    square = step - n_blocks
    cols = pl.ds(pl.multiple_of(lax.rem(square + TWO * n_square, n_square) * d_model, d_model), d_model)

    @pl.when(square >= ZERO)
    def _():
        which = square // n_square
        grad_ref[ALL] = dot_tn(left_all[which, :, cols], right_all[which])


def ffn_both(h2, dy, ffn_full, bias_rows, up_bias, normed2, inv2, block=256):
    n_tok, d_model = h2.shape
    ffn_dim = ffn_full.shape[ZERO] // TWO
    n_blocks = n_tok // block
    n_steps = n_blocks + ffn_full.shape[ZERO] // d_model
    at = lambda i: jnp.minimum(i, n_blocks - ONE)
    tok = pl.BlockSpec((block, d_model), lambda i: (at(i), ZERO))
    once = lambda shape, idx: pl.BlockSpec(shape, lambda i: idx, pipeline_mode=pl.Buffered(ONE))
    return pl.pallas_call(
        functools.partial(ffn_kernel, n_blocks), grid=(n_steps,),
        in_specs=[tok, tok, once((ffn_dim, d_model), (ZERO, ZERO)), once((ffn_dim, d_model), (ONE, ZERO)), once(bias_rows.shape, (ZERO, ZERO)), once((ONE, ffn_dim), (ZERO, ZERO)),
                  tok, pl.BlockSpec((block, ONE), lambda i: (at(i), ZERO))],
        out_specs=[tok, pl.BlockSpec((d_model, d_model), lambda i: (jnp.maximum(i - n_blocks, ZERO), ZERO)), tok, pl.BlockSpec((8, d_model), lambda i: (ZERO, ZERO)), pl.BlockSpec((ONE, ffn_dim), lambda i: (ZERO, ZERO))],
        out_shape=[jax.ShapeDtypeStruct(h2.shape, BF16), jax.ShapeDtypeStruct(ffn_full.shape, F32), jax.ShapeDtypeStruct(h2.shape, F32),
                   jax.ShapeDtypeStruct((8, d_model), F32), jax.ShapeDtypeStruct((ONE, ffn_dim), F32)],
        scratch_shapes=[pltpu.VMEM((TWO, n_tok, ffn_dim), BF16), pltpu.VMEM((TWO, n_tok, d_model), BF16)],
        compiler_params=pltpu.CompilerParams(vmem_limit_bytes=VMEM_BYTES, dimension_semantics=('arbitrary',)),
        cost_estimate=pl.CostEstimate(flops=12 * n_tok * d_model * ffn_dim, bytes_accessed=30 * n_tok * d_model, transcendentals=ZERO),
        name='ffn_both',
    )(h2, dy, ffn_full, ffn_full, bias_rows, up_bias, normed2, inv2)


CROSS_PLAN = {ONE: (ZERO,), TWO: (ONE,), THREE: (TWO,), 4: (THREE,), 5: (('relay', ZERO),), 9: (('settle', ZERO),), 10: (('relay', ONE),), 'late': (('settle', ONE),), 12: (('relay', TWO),), 13: (('settle', TWO),), 14: ('end',)}


def solution(mesh):
    n_fsdp = mesh.shape['fsdp']
    n_dp = mesh.shape['dp']
    batch_axes = ('dp', 'fsdp')
    act_spec = P(batch_axes, None, None)
    len_spec = P(batch_axes)
    row_spec = P('fsdp', None)
    vec_spec = P('fsdp')

    def device_step(dec_in, enc_out, src_lens, tgt_lens, y_cot, attn_w, ffn_w, vec_params):
        d_model, n_vec = dec_in.shape[TWO], vec_params.shape[ZERO]
        scale = 1.0 / (dec_in.shape[ZERO] * dec_in.shape[ONE] * n_fsdp * n_dp)
        x, enc, dy = (a.reshape(-ONE, d_model) for a in (dec_in, enc_out, y_cot))
        vec_rows = jnp.pad(vec_params.astype(F32), (ZERO, 16 * LANES - n_vec)).reshape(16, LANES)
        attn_tiles, planes, vec_tiles = gather_params(attn_w, ffn_w, vec_rows)
        attn_full = attn_tiles.reshape(-ONE, d_model)
        vec_f = vec_tiles.reshape(n_fsdp, 16, LANES)[:, :TWO].reshape(n_fsdp, TWO * LANES)[:, :n_vec].reshape(-ONE)
        bias_rows = jnp.pad(vec_f[:15 * d_model].reshape(15, d_model), ((ZERO, ONE), (ZERO, ZERO)))
        up_bias = vec_f[15 * d_model:].reshape(ONE, -ONE)
        q1, k1, v1, o1, lse1, h1, normed1, inv1 = attn_forward(x, x, tgt_lens, attn_full, bias_rows, (ZERO, ONE, TWO, THREE), (ZERO, ONE, TWO, THREE, 9), True)
        q2, k2, v2, o2, lse2, h2, normed2, inv2, ffn_tiles = attn_forward(h1, enc, src_lens, attn_full, bias_rows, (4, 5, 6, 7), (4, 5, 6, 7, 11), False, planes, ffn_w.shape[ZERO] * n_fsdp)
        ffn_full = ffn_tiles.reshape(-ONE, d_model)
        y, g_ffn, d_res2, ffn_tail, up_sum = ffn_both(h2, dy, ffn_full, bias_rows, up_bias, normed2, inv2)
        d_res1, d_enc, sums2, tail2, grads, ffn_out = attn_backward(d_res2, q2, k2, v2, lse2, src_lens, attn_full, bias_rows, (4, 5, 6, 7), False, (h1, enc, o2), g_ffn, scale, 9, normed1, inv1)
        d_x, sums1, _, grads = attn_backward(d_res1, q1, k1, v1, lse1, tgt_lens, attn_full, bias_rows, (ZERO, ONE, TWO, THREE), True, (x, o1), grads=grads)
        s1, s2, t2 = jnp.sum(sums1, axis=ZERO), jnp.sum(sums2, axis=ZERO), jnp.sum(tail2, axis=ZERO)
        g_vec = jnp.concatenate([s1[ZERO:THREE].reshape(-ONE), t2[ZERO], s2[ZERO:THREE].reshape(-ONE), ffn_tail[ZERO], ffn_tail[ONE], t2[ONE], t2[TWO], ffn_tail[TWO], ffn_tail[THREE], ffn_tail[4], ffn_tail[5], up_sum[ZERO]])
        g_rows = jnp.pad(g_vec.reshape(n_fsdp, ONE, n_vec), ((ZERO, ZERO), (ZERO, 7), (ZERO, d_model - n_vec))).reshape(n_fsdp * 8, -ONE)
        attn_out, vec_out = scatter_grads(grads, g_rows, scale)
        return y.reshape(dec_in.shape), d_x.reshape(dec_in.shape), d_enc.reshape(enc_out.shape), attn_out, ffn_out, vec_out[ZERO, :n_vec]

    return jax.shard_map(device_step, mesh=mesh, in_specs=(act_spec, act_spec, len_spec, len_spec, act_spec, row_spec, row_spec, vec_spec), out_specs=(act_spec, act_spec, act_spec, row_spec, row_spec, vec_spec), check_vma=False)
```

```python
import functools
import jax
import jax.numpy as jnp
from jax import lax
from jax.experimental import pallas as pl
from jax.experimental.pallas import tpu as pltpu
from jax.sharding import PartitionSpec as P

ZERO, ONE, TWO, THREE = range(4)
ALL = ...
HEAD_DIM = 64
LN_EPS = 1e-5
MASK_FILL = -1e30
VMEM_BYTES = 60 * 1024 * 1024
F32 = jnp.float32
BF16 = jnp.bfloat16
GROUP = 256
PAIR = 128


SIDE = 4
LANES = 128
COLOURS = THREE
STAGES = TWO
DIM_ORDER = ((TWO, ONE, ZERO), (ONE, ZERO, TWO), (ZERO, TWO, ONE))
MESH_ID = pl.DeviceIdType.MESH


def torus_place():
    chip = lax.axis_index('fsdp')
    return (chip // (SIDE * SIDE), lax.rem(chip // SIDE, SIDE), lax.rem(chip, SIDE))


def chip_at(place, dim, shift):
    moved = [lax.rem(p + shift + SIDE, SIDE) if d == dim else p for d, p in enumerate(place)]
    return (moved[ZERO] * SIDE + moved[ONE]) * SIDE + moved[TWO]


def meet_neighbours(place):
    barrier = pltpu.get_barrier_semaphore()
    core = lax.axis_index('dp')
    for dim in range(THREE):
        for shift in (ONE, -ONE):
            pl.semaphore_signal(barrier, inc=ONE, device_id=(core, chip_at(place, dim, shift)), device_id_type=MESH_ID)
    pl.semaphore_signal(barrier, inc=ONE, device_id=(ONE - core, lax.axis_index('fsdp')), device_id_type=MESH_ID)
    pl.semaphore_wait(barrier, 7)


class Scatter:
    def __init__(self, scale, sources, outs, scratch):
        self.scale, self.outs = scale, outs
        self.sources = [(ref, pl.ds(first, n)) for ref, first, n in sources]
        (self.acc, g1, d1, g2, d2, g3, d3, self.send_sem, self.recv_sem, self.load_sem, self.stage) = scratch
        self.got, self.far = (g1, g2, g3), (d1, d2, d3)
        self.heights = [n for _, _, n in sources]
        self.offsets = [sum(self.heights[:i]) for i in range(len(sources))]
        self.n_low = self.heights[ZERO] // TWO
        self.core, self.chip, self.place = lax.axis_index('dp'), lax.axis_index('fsdp'), torus_place()
        self.pieces = [(d, colour) for d in (TWO, ONE, THREE, ZERO) for colour in range(COLOURS)]

    @staticmethod
    def scratch_shapes(heights):
        h = sum(heights)
        n_low = heights[ZERO] // TWO
        buf = lambda *shape: pltpu.VMEM((COLOURS,) + shape + (LANES,), F32)
        n = Scatter.n_copies(len(heights))
        return [buf(SIDE, SIDE, SIDE, h), buf(TWO, SIDE, SIDE, h), buf(TWO, TWO, SIDE, h), buf(TWO, SIDE, h), buf(TWO, TWO, h), buf(TWO, h), buf(TWO, max(n_low, h - n_low)),
                pltpu.SemaphoreType.DMA((n,)), pltpu.SemaphoreType.DMA((n,)), pltpu.SemaphoreType.DMA((THREE + COLOURS, len(heights))),
                pltpu.VMEM((STAGES, SIDE, SIDE, h, LANES), F32)]

    @staticmethod
    def n_copies(n_parts):
        return 12 * n_parts + COLOURS * 18 + COLOURS * n_parts

    def parts(self, colour):
        return range(len(self.sources) if colour == ZERO else ONE)

    def height(self, colour):
        return sum(self.heights[i] for i in self.parts(colour))

    def remote(self, i, src, dst, device):
        return pltpu.make_async_remote_copy(src_ref=src, dst_ref=dst, send_sem=self.send_sem.at[i], recv_sem=self.recv_sem.at[i], device_id=device, device_id_type=MESH_ID)

    def columns(self, of_core, colour, part=ZERO):
        return pl.ds(pl.multiple_of((of_core * COLOURS + colour if part == ZERO else of_core) * LANES, LANES), LANES)

    def slot(self, d, colour):
        dim = DIM_ORDER[colour][ZERO]
        where = [slice(None)] * THREE
        where[dim] = lax.rem(self.place[dim] + d, SIDE)
        return tuple(where)

    def rows_of(self, part):
        return pl.ds(self.offsets[part], self.heights[part])

    def swaps(self, piece):
        d, colour = self.pieces[piece]
        where = self.slot(d, colour)
        n = len(self.sources)
        return [self.remote(piece * n + i, self.sources[i][ZERO].at[where + (self.sources[i][ONE], self.columns(ONE - self.core, colour, i))],
                            self.acc.at[(colour,) + where + (self.rows_of(i), slice(None))], (ONE - self.core, self.chip)) for i in self.parts(colour)]

    def loads(self, piece):
        d, colour = self.pieces[piece]
        where, buf = self.slot(d, colour), piece % STAGES
        return [pltpu.make_async_copy(self.sources[i][ZERO].at[where + (self.sources[i][ONE], self.columns(self.core, colour, i))],
                                      self.stage.at[buf, :, :, self.rows_of(i), :], self.load_sem.at[buf, i]) for i in self.parts(colour)]

    def split_rows(self, colour, half):
        return pl.ds(ZERO, self.n_low) if half == ZERO else pl.ds(self.n_low, self.height(colour) - self.n_low)

    def block(self, colour, phase, d, half=None):
        order = DIM_ORDER[colour]
        where = [None, None, None]
        for done in order[:phase]:
            where[done] = self.place[done]
        where[order[phase]] = lax.rem(self.place[order[phase]] + d, SIDE)
        for i, rest in enumerate(sorted(order[phase + ONE:])):
            where[rest] = slice(None) if half is None or i > ZERO else pl.ds(TWO * half, TWO)
        rows = self.split_rows(colour, half) if phase == TWO and half is not None else pl.ds(ZERO, self.height(colour))
        return self.acc.at[(colour,) + tuple(where) + (rows, slice(None))]

    def got_half(self, colour, phase, direction, half):
        if phase == TWO:
            return self.got[phase].at[colour, direction, self.split_rows(colour, half), :]
        return self.got_all(colour, phase, direction, pl.ds(TWO * half, TWO))

    def got_all(self, colour, phase, direction, which=slice(None)):
        rows = (pl.ds(ZERO, self.height(colour)), slice(None))
        blocks = ((which, slice(None)), (which,), ())[phase]
        return self.got[phase].at[(colour, direction) + blocks + rows]

    def far_part(self, colour, phase, direction):
        if phase == TWO:
            return self.far[phase].at[colour, direction, pl.ds(ZERO, self.n_low if direction == ZERO else self.height(colour) - self.n_low), :]
        return self.far[phase].at[(colour, direction) + (slice(None),) * (TWO - phase) + (pl.ds(ZERO, self.height(colour)), slice(None))]

    def ring(self, colour, phase, direction):
        shift = ONE - TWO * direction
        device = (self.core, chip_at(self.place, DIM_ORDER[colour][phase], shift))
        i = 12 * len(self.sources) + ((colour * THREE + phase) * TWO + direction) * THREE
        near = shift % SIDE
        return (self.remote(i, self.block(colour, phase, TWO, direction), self.far_part(colour, phase, direction), device),
                self.remote(i + ONE, self.block(colour, phase, near, ONE - direction), self.got_half(colour, phase, direction, ONE - direction), device),
                self.remote(i + TWO, self.block(colour, phase, near, direction), self.got_half(colour, phase, direction, direction), device))

    def gives(self, colour):
        n = len(self.sources)
        base = 12 * n + COLOURS * 18 + colour * n
        done = self.acc.at[colour, self.place[ZERO], self.place[ONE], self.place[TWO]]
        pairs = [(done.at[self.rows_of(i), :], self.outs[i].at[:, self.columns(self.core, colour, i)]) for i in self.parts(colour)]
        return [(self.remote(base + i, src, dst, (ONE - self.core, self.chip)), pltpu.make_async_copy(src, dst, self.load_sem.at[THREE + colour, i])) for i, (src, dst) in enumerate(pairs)]

    def add_into(self, dst, sources, n_lead):
        def body(i, _):
            total = dst[i]
            for src in sources:
                total = total + src[i]
            dst[i] = total
            return ZERO

        if n_lead == TWO:
            lax.fori_loop(ZERO, dst.shape[ZERO], body, ZERO)
        else:
            total = dst[ALL]
            for src in sources:
                total = total + src[ALL]
            dst[ALL] = total


    def begin(self):
        for piece in range(STAGES):
            for copy in self.loads(piece):
                copy.start()
        for piece in range(len(self.pieces)):
            for copy in self.swaps(piece):
                copy.start()

    def absorb(self, turn):
        for piece in range(turn * COLOURS, (turn + ONE) * COLOURS):
            d, colour = self.pieces[piece]
            for copy in self.loads(piece):
                copy.wait()
            for copy in self.swaps(piece):
                copy.wait_recv()
            rows = (pl.ds(ZERO, self.height(colour)), slice(None))
            self.add_into(self.acc.at[(colour,) + self.slot(d, colour) + rows], [self.stage.at[(piece % STAGES, slice(None), slice(None)) + rows]], TWO)
            if piece + STAGES < len(self.pieces):
                for copy in self.loads(piece + STAGES):
                    copy.start()
            if turn == ZERO:
                for direction in range(TWO):
                    self.ring(colour, ZERO, direction)[ZERO].start()
            elif turn < THREE:
                self.ring(colour, ZERO, turn - ONE)[ONE].start()

    def relay(self, phase):
        for colour in range(COLOURS):
            for direction in range(TWO):
                far, _, fed = self.ring(colour, phase, direction)
                far.wait_recv()
                self.add_into(self.block(colour, phase, (ONE - TWO * direction) % SIDE, direction), [self.far_part(colour, phase, direction)], TWO - phase)
            for direction in range(TWO):
                self.ring(colour, phase, direction)[TWO].start()

    def settle(self, phase):
        for colour in range(COLOURS):
            for direction in range(TWO):
                _, own, fed = self.ring(colour, phase, direction)
                own.wait_recv()
                fed.wait_recv()
            self.add_into(self.block(colour, phase, ZERO), [self.got_all(colour, phase, direction) for direction in range(TWO)], TWO - phase)
            if phase < TWO:
                for kind in range(TWO):
                    for direction in range(TWO):
                        self.ring(colour, phase + ONE, direction)[kind].start()
            else:
                done = self.block(colour, TWO, ZERO)
                done[ALL] = done[ALL] * self.scale
                for give, keep in self.gives(colour):
                    keep.start()
                    give.start()

    def end(self):
        for colour in range(COLOURS):
            for give, keep in self.gives(colour):
                give.wait_recv()
                give.wait_send()
                keep.wait()
        for piece in range(len(self.pieces)):
            for copy in self.swaps(piece):
                copy.wait_send()
        for colour in range(COLOURS):
            for phase in range(THREE):
                for direction in range(TWO):
                    for copy in self.ring(colour, phase, direction):
                        copy.wait_send()


def rs_kernel(scale, mats, g_ref, vec_ref, w_all, dres_ref, self_ref, cross_ref, out_ref, vec_out, dx_out, denc_out,
              w_v, dres_v, self_v, cross_v, dx_v, denc_v, load_sem, *scratch):
    scatter = Scatter(scale, [(ref, ZERO, ref.shape[THREE]) for ref in (g_ref, vec_ref)], [out_ref, vec_out], scratch)
    d_model = w_v.shape[ONE]
    step = 256
    loads = [pltpu.make_async_copy(w_all.at[pl.ds(mat * d_model, d_model), :], w_v.at[i], load_sem.at[i]) for i, mat in enumerate(mats)]
    loads += [pltpu.make_async_copy(src, dst, load_sem.at[len(mats) + i]) for i, (src, dst) in enumerate(((dres_ref, dres_v), (self_ref, self_v), (cross_ref, cross_v)))]
    stores = [pltpu.make_async_copy(src, dst, load_sem.at[len(mats) + THREE + i]) for i, (src, dst) in enumerate(((dx_v, dx_out), (denc_v, denc_out)))]

    def input_grads():
        for copy in loads:
            copy.wait()

        def decoder(i, _):
            rows = pl.ds(pl.multiple_of(i * step, step), step)
            total = dres_v[rows, :]
            for n in range(THREE):
                total = total + dot_nt(self_v[n, rows, :], w_v[n])
            dx_v[rows, :] = total.astype(BF16)
            return ZERO

        def encoder(i, _):
            rows = pl.ds(pl.multiple_of(i * step, step), step)
            denc_v[rows, :] = (dot_nt(cross_v[ZERO, rows, :], w_v[THREE]) + dot_nt(cross_v[ONE, rows, :], w_v[4])).astype(BF16)
            return ZERO

        lax.fori_loop(ZERO, dx_v.shape[ZERO] // step, decoder, ZERO)
        stores[ZERO].start()
        lax.fori_loop(ZERO, denc_v.shape[ZERO] // step, encoder, ZERO)
        stores[ONE].start()

    meet_neighbours(scatter.place)
    scatter.begin()
    for copy in loads:
        copy.start()
    for turn in range(THREE):
        scatter.absorb(turn)
    scatter.relay(ZERO)
    scatter.absorb(THREE)
    input_grads()
    scatter.settle(ZERO)
    for phase in (ONE, TWO):
        scatter.relay(phase)
        scatter.settle(phase)
    scatter.end()
    for copy in stores:
        copy.wait()


def as_torus(rows):
    return rows.reshape(SIDE, SIDE, SIDE, rows.shape[ZERO] // SIDE ** THREE, rows.shape[ONE])


def scatter_grads(g_attn, g_vec, scale, attn_full, mats, d_res, d_self, d_cross):
    sources = [as_torus(g_attn), as_torus(g_vec)]
    heights = [src.shape[THREE] for src in sources]
    d_model = g_attn.shape[ONE]
    anywhere = pl.BlockSpec(memory_space=pl.ANY)
    dx_shape, denc_shape = d_self.shape[ONE:], d_cross.shape[ONE:]
    return pl.pallas_call(
        functools.partial(rs_kernel, scale, mats),
        in_specs=[anywhere] * 6, out_specs=[anywhere] * 4,
        out_shape=[jax.ShapeDtypeStruct((h, src.shape[4]), F32) for h, src in zip(heights, sources)] + [jax.ShapeDtypeStruct(dx_shape, BF16), jax.ShapeDtypeStruct(denc_shape, BF16)],
        scratch_shapes=[pltpu.VMEM((len(mats), d_model, d_model), BF16), pltpu.VMEM(d_res.shape, F32), pltpu.VMEM(d_self.shape, BF16), pltpu.VMEM(d_cross.shape, BF16),
                        pltpu.VMEM(dx_shape, BF16), pltpu.VMEM(denc_shape, BF16), pltpu.SemaphoreType.DMA((len(mats) + 5,))] + Scatter.scratch_shapes(heights),
        compiler_params=pltpu.CompilerParams(collective_id=ONE, has_side_effects=True, vmem_limit_bytes=VMEM_BYTES),
        cost_estimate=pl.CostEstimate(flops=10 ** 9, bytes_accessed=8 * d_model * g_attn.shape[ZERO], transcendentals=ZERO),
        name='scatter_grads',
    )(*sources, attn_full, d_res, d_self, d_cross)


class Gather:
    def __init__(self, send_sem, recv_sem, base=ZERO):
        self.send_sem, self.recv_sem = send_sem, recv_sem
        self.used = base
        self.core, self.chip, self.place = lax.axis_index('dp'), lax.axis_index('fsdp'), torus_place()
        self.sibling = (ONE - self.core, self.chip)
        self.started = []

    def remote(self, src, dst, device):
        i = self.used
        self.used += ONE
        return pltpu.make_async_remote_copy(src_ref=src, dst_ref=dst, send_sem=self.send_sem.at[i], recv_sem=self.recv_sem.at[i], device_id=device, device_id_type=MESH_ID)

    def start(self, copy):
        copy.start()
        self.started.append(copy)

    def ring(self, colour, phase, view, own=None, split=False):
        order = DIM_ORDER[colour]
        dim = order[phase]
        have = sorted(order[:phase])

        def index(shift, half=None):
            where = [self.place[ZERO], self.place[ONE], self.place[TWO]]
            where[dim] = lax.rem(self.place[dim] + shift + SIDE, SIDE)
            for i, h in enumerate(have):
                where[h] = slice(None) if half is None or i > ZERO else pl.ds(TWO * half, TWO)
            return tuple(where)

        out = []
        for direction, shift in enumerate((ONE, -ONE)):
            device = (self.core, chip_at(self.place, dim, shift))
            half = direction if phase == ZERO else None
            near_dst = view(index(ZERO), None)
            if split:
                near = [self.remote(view(index(ZERO, h), None), view(index(ZERO, h), None), device) for h in (direction, ONE - direction)]
            else:
                near = [self.remote(near_dst if own is None else own, near_dst, device)]
            out.append(dict(
                near=near,
                far=self.remote(view(index(-shift, direction), half), view(index(-shift, direction), half), device),
                near_at=index(-shift), far_at=index(TWO, direction)))
        return out


def ag_kernel(attn_ref, ffn_ref, vec_ref, oattn_ref, planes_ref, vec_out, attn_v, send_sem, recv_sem, load_sem):
    net = Gather(send_sem, recv_sem)
    core, place = net.core, net.place
    rows, width = attn_ref.shape
    band = rows // (TWO * COLOURS)
    vec_high = vec_ref.shape[ZERO]
    stores, finals = [], []

    def band_rows(colour):
        return pl.ds(pl.multiple_of((core * COLOURS + colour) * band, band), band)

    def columns(half):
        return slice(None) if half is None else pl.ds(half * (width // TWO), width // TWO)

    def attn_view(colour):
        return lambda where, half: attn_v.at[where + (band_rows(colour), columns(half))]

    def ffn_view(colour):
        last = DIM_ORDER[colour][TWO]
        return lambda where, half: planes_ref.at[(colour,) + tuple(w for d, w in enumerate(where) if d != last) + (slice(None), columns(half))]

    def vec_view(where, half):
        return vec_out.at[where + (slice(None) if half is None else pl.ds(half * (vec_high // TWO), vec_high // TWO), slice(None))]

    colours = range(COLOURS)
    attn_own = [attn_ref.at[band_rows(colour), :] for colour in colours]
    ffn_own = [ffn_ref.at[band_rows(colour), :] for colour in colours]
    rings = {('attn', phase): [net.ring(colour, phase, attn_view(colour), attn_own[colour] if phase == ZERO else None, phase > ZERO) for colour in colours] for phase in range(THREE)}
    rings |= {('ffn', phase): [net.ring(colour, phase, ffn_view(colour), ffn_own[colour] if phase == ZERO else None, phase > ZERO) for colour in colours] for phase in range(TWO)}
    rings |= {('vec', phase): [net.ring(ONE, phase, vec_view, vec_ref if phase == ZERO else None)] for phase in range(THREE)}

    def publish(at):
        keep = pltpu.make_async_copy(attn_v.at[at], oattn_ref.at[at], load_sem.at[len(stores)])
        keep.start()
        stores.append(keep)
        give = net.remote(attn_v.at[at], oattn_ref.at[at], net.sibling)
        net.start(give)
        finals.append(give)

    def send_near(name, phase):
        for ring in rings.get((name, phase), ()):
            for way in ring:
                for copy in way['near']:
                    net.start(copy)

    def pass_on(name, phase):
        for ring in rings.get((name, phase), ()):
            for way in ring:
                way['near'][ZERO].wait_recv()
                net.start(way['far'])
        if phase == TWO and name == 'attn':
            for colour in colours:
                for way in rings[(name, phase)][colour]:
                    way['near'][ONE].wait_recv()
                    publish(way['near_at'] + (band_rows(colour), slice(None)))

    def complete(name, phase):
        for colour, ring in enumerate(rings.get((name, phase), ())):
            for way in ring:
                way['far'].wait_recv()
                if phase == ONE and name != 'vec':
                    way['near'][ONE].wait_recv()
            if phase < TWO and (name, phase + ONE) in rings:
                for way in rings[(name, phase + ONE)][colour]:
                    for copy in way['near']:
                        net.start(copy)
            if phase == TWO and name == 'attn':
                for way in ring:
                    publish(way['far_at'] + (band_rows(colour), slice(None)))
        if phase == ONE and name == 'attn':
            for colour in colours:
                last = DIM_ORDER[colour][TWO]
                publish(tuple(place[d] if d == last else slice(None) for d in range(THREE)) + (band_rows(colour), slice(None)))

    for colour in colours:
        attn_v[(place[ZERO], place[ONE], place[TWO]) + (band_rows(colour), slice(None))] = attn_ref[band_rows(colour), :]
        kept = [place[d] for d in range(THREE) if d != DIM_ORDER[colour][TWO]]
        planes_ref[(colour, kept[ZERO], kept[ONE])] = ffn_ref[band_rows(colour), :]
    vec_out[place[ZERO], place[ONE], place[TWO]] = vec_ref[ALL]
    meet_neighbours(place)
    names = ('attn', 'vec', 'ffn')
    for name in names:
        send_near(name, ZERO)
    for phase in range(THREE):
        for name in names:
            pass_on(name, phase)
        for name in names:
            complete(name, phase)
    for copy in finals:
        copy.wait_recv()
    for copy in net.started:
        copy.wait_send()
    for copy in stores:
        copy.wait()


def gather_params(attn_w, ffn_w, vec_rows):
    rows, width = attn_w.shape
    full = (SIDE, SIDE, SIDE, rows, width)
    n_copies = COLOURS * (4 * TWO + 6 * THREE) + 4 * THREE + COLOURS * 5
    vmem = pl.BlockSpec(memory_space=pltpu.VMEM)
    return pl.pallas_call(
        ag_kernel,
        in_specs=[vmem] * THREE, out_specs=[pl.BlockSpec(memory_space=pl.ANY), vmem, vmem],
        out_shape=[jax.ShapeDtypeStruct(full, BF16), jax.ShapeDtypeStruct((COLOURS, SIDE, SIDE, rows // (TWO * COLOURS), width), BF16),
                   jax.ShapeDtypeStruct((SIDE, SIDE, SIDE) + vec_rows.shape, F32)],
        scratch_shapes=[pltpu.VMEM(full, BF16), pltpu.SemaphoreType.DMA((n_copies,)), pltpu.SemaphoreType.DMA((n_copies,)), pltpu.SemaphoreType.DMA((COLOURS * 5,))],
        compiler_params=pltpu.CompilerParams(collective_id=TWO, has_side_effects=True, vmem_limit_bytes=VMEM_BYTES),
        cost_estimate=pl.CostEstimate(flops=10 ** 9, bytes_accessed=4 * rows * width * SIDE ** THREE, transcendentals=ZERO),
        name='gather_params',
    )(attn_w, ffn_w, vec_rows)


class LastPhase:
    def __init__(self, planes, out, near, far, send_sem, recv_sem, load_sem):
        self.planes, self.out, self.near, self.far = planes, out, near, far
        self.send_sem, self.recv_sem, self.load_sem = send_sem, recv_sem, load_sem
        self.core, self.chip, self.place = lax.axis_index('dp'), lax.axis_index('fsdp'), torus_place()
        self.band = planes.shape[THREE]

    @staticmethod
    def scratch_shapes(planes):
        colours, side, _, band, width = planes.shape
        sems = [pltpu.SemaphoreType.DMA((11 * COLOURS,)), pltpu.SemaphoreType.DMA((11 * COLOURS,)), pltpu.SemaphoreType.DMA((5 * COLOURS,))]
        return [pltpu.VMEM((colours, TWO, side, side, band, width), BF16), pltpu.VMEM((colours, TWO, side // TWO, side, band, width), BF16)] + sems

    def remote(self, i, src, dst, device):
        return pltpu.make_async_remote_copy(src_ref=src, dst_ref=dst, send_sem=self.send_sem.at[i], recv_sem=self.recv_sem.at[i], device_id=device, device_id_type=MESH_ID)

    def ring(self, colour, direction):
        device = (self.core, chip_at(self.place, DIM_ORDER[colour][TWO], ONE - TWO * direction))
        i = 11 * colour + THREE * direction
        got = self.near.at[colour, direction]
        near = [self.remote(i + n, self.planes.at[colour, pl.ds(TWO * half, TWO)], got.at[pl.ds(TWO * half, TWO)], device) for n, half in enumerate((direction, ONE - direction))]
        return near + [self.remote(i + TWO, got.at[pl.ds(TWO * direction, TWO)], self.far.at[colour, direction], device)]

    def shares(self, colour):
        last = DIM_ORDER[colour][TWO]
        rows = pl.ds(pl.multiple_of((self.core * COLOURS + colour) * self.band, self.band), self.band)
        views = [(self.planes.at[colour], ZERO, None)]
        views += [(self.near.at[colour, direction], TWO * direction - ONE, None) for direction in range(TWO)]
        views += [(self.far.at[colour, direction], TWO, direction) for direction in range(TWO)]
        out = []
        for n, (src, shift, half) in enumerate(views):
            where = [slice(None)] * THREE
            where[last] = lax.rem(self.place[last] + shift + SIDE, SIDE)
            if half is not None:
                where[min(d for d in range(THREE) if d != last)] = pl.ds(TWO * half, TWO)
            dst = self.out.at[tuple(where) + (rows, slice(None))]
            out.append((self.remote(11 * colour + 6 + n, src, dst, (ONE - self.core, self.chip)), pltpu.make_async_copy(src, dst, self.load_sem.at[5 * colour + n])))
        return out

    def share(self, colour, which):
        for n in which:
            give, keep = self.shares(colour)[n]
            give.start()
            keep.start()

    def begin(self):
        for colour in range(COLOURS):
            for direction in range(TWO):
                for copy in self.ring(colour, direction)[:TWO]:
                    copy.start()
        for colour in range(COLOURS):
            self.share(colour, (ZERO,))

    def pass_on(self):
        for colour in range(COLOURS):
            for direction in range(TWO):
                first, _, far = self.ring(colour, direction)
                first.wait_recv()
                far.start()
        for colour in range(COLOURS):
            for direction in range(TWO):
                self.ring(colour, direction)[ONE].wait_recv()
            self.share(colour, (ONE, TWO))

    def complete(self):
        for colour in range(COLOURS):
            for direction in range(TWO):
                self.ring(colour, direction)[TWO].wait_recv()
            self.share(colour, (THREE, 4))

    def end(self):
        for colour in range(COLOURS):
            for give, keep in self.shares(colour):
                give.wait_recv()
                give.wait_send()
                keep.wait()
            for direction in range(TWO):
                for copy in self.ring(colour, direction):
                    copy.wait_send()


def dot(lhs, rhs, contract=((ONE,), (ZERO,))):
    return lax.dot_general(lhs, rhs, (contract, ((), ())), preferred_element_type=F32)


def dot_nt(lhs, rhs):
    return dot(lhs, rhs, ((ONE,), (ONE,)))


def dot_tn(lhs, rhs):
    return dot(lhs, rhs, ((ZERO,), (ZERO,)))


def norm_rows(resid, gain, shift):
    mean = jnp.mean(resid, axis=-ONE, keepdims=True)
    centred = resid - mean
    inv_std = lax.rsqrt(jnp.mean(centred * centred, axis=-ONE, keepdims=True) + LN_EPS)
    normed = centred * inv_std
    return (normed * gain + shift).astype(BF16), normed, inv_std


def norm_rows_bwd(d_out, normed, inv_std, gain):
    d_norm = d_out * gain
    return inv_std * (d_norm - jnp.mean(d_norm, axis=-ONE, keepdims=True) - normed * jnp.mean(d_norm * normed, axis=-ONE, keepdims=True))


def col_sum(values):
    return jnp.sum(values, axis=ZERO, keepdims=True)


def lane_row(head, dtype=BF16):
    lane = lax.broadcasted_iota(jnp.int32, (ONE, PAIR), ONE)
    return jnp.where((lane >= HEAD_DIM * head) & (lane < HEAD_DIM * (head + ONE)), 1.0, 0.0).astype(dtype)


def spare_lane(head):
    lane = lax.broadcasted_iota(jnp.int32, (ONE, PAIR), ONE)
    return jnp.where(lane == HEAD_DIM * (ONE - head), 1.0, 0.0)


def mask_fill(n_rows, n_valid):
    row = lax.broadcasted_iota(jnp.int32, (n_rows, PAIR), ZERO)
    return jnp.where(row >= n_valid, MASK_FILL, 0.0)


def head_masks(pair_q, pair_k, head, fill):
    q_f = pair_q * lane_row(head) + spare_lane(head).astype(BF16)
    k_f = pair_k * lane_row(head) + (fill * spare_lane(head)).astype(BF16)
    return q_f, k_f


def half_only(pair, head):
    return pair * lane_row(head)


def join_halves(first, second):
    lane = lax.broadcasted_iota(jnp.int32, first.shape, ONE)
    return jnp.where(lane < HEAD_DIM, first, second)


def score_blocks(n_heads, n_q, n_k, causal, step):
    if not causal:
        return [(head, ZERO, n_q, n_k) for head in range(n_heads)]
    return [(head, first, step, first + step) for head in range(n_heads) for first in range(ZERO, n_q, step)]


def scores_t(q_f, k_f, causal, first):
    s_t = dot_nt(k_f, q_f)
    if causal:
        key_i = lax.broadcasted_iota(jnp.int32, s_t.shape, ZERO)
        qry_i = lax.broadcasted_iota(jnp.int32, s_t.shape, ONE) + first
        s_t = jnp.where(key_i <= qry_i, s_t, MASK_FILL)
    return s_t


def pair_of(group, head):
    return group[:, head // TWO * PAIR:(head // TWO + ONE) * PAIR]


def masked_pairs(q_g, k_g, n_valid):
    fill = mask_fill(k_g.shape[ZERO], n_valid)
    cache = {}

    def get(head):
        if head not in cache:
            cache[head] = head_masks(pair_of(q_g, head), pair_of(k_g, head), head % TWO, fill)
        return cache[head]

    return get


def stack_heads(parts, n_heads):
    return jnp.concatenate([jnp.concatenate(parts[head], axis=ONE) for head in range(n_heads)], axis=ZERO)


def run_ahead(blocks, produce, transform, consume, delay):
    ahead = produce(blocks[ZERO])
    waiting = []
    for i, block in enumerate(blocks):
        now = ahead
        if i + ONE < len(blocks):
            ahead = produce(blocks[i + ONE])
        waiting.append((block, transform(block, now)))
        if len(waiting) > delay:
            consume(*waiting.pop(ZERO))
    for item in waiting:
        consume(*item)


def attend_group(q_g, k_g, v_g, n_valid, causal, lse_ref):
    n_heads = GROUP // HEAD_DIM
    o_parts = [[] for _ in range(n_heads)]
    v_t = v_g.T
    masked = masked_pairs(q_g, k_g, n_valid)

    def produce(block):
        head, first, n_q, n_k = block
        q_f, k_f = masked(head)
        return scores_t(q_f[first:first + n_q], k_f[:n_k], causal, first)

    def transform(block, s_t):
        head, first, n_q, n_k = block
        top = jnp.max(s_t, axis=ZERO, keepdims=True)
        e_t = jnp.exp(s_t - top)
        total = jnp.sum(e_t, axis=ZERO, keepdims=True)
        lse_ref[ZERO, ZERO, head // TWO, head % TWO:head % TWO + ONE, first:first + n_q] = top + jnp.log(total)
        return (e_t * (1.0 / total)).astype(BF16)

    def consume(block, p_t):
        head, first, n_q, n_k = block
        o_parts[head].append(dot(v_t[HEAD_DIM * head:HEAD_DIM * (head + ONE), :n_k], p_t))

    run_ahead(score_blocks(n_heads, q_g.shape[ZERO], k_g.shape[ZERO], causal, 128), produce, transform, consume, TWO)
    return stack_heads(o_parts, n_heads).T.astype(BF16)


def attend_group_bwd(d_o, q_g, k_g, v_g, n_valid, causal, lse_ref):
    n_heads = q_g.shape[ONE] // HEAD_DIM
    k_t = k_g.T
    dq_t, dk_h, dv_h = [[] for _ in range(n_heads)], [None] * n_heads, [None] * n_heads
    masked = masked_pairs(q_g, k_g, n_valid)
    v_half = {}

    def produce(block):
        head, first, n_q, n_k = block
        q_f, k_f = masked(head)
        if head not in v_half:
            v_half[head] = half_only(pair_of(v_g, head), head % TWO)
        rows = slice(first, first + n_q)
        return scores_t(q_f[rows], k_f[:n_k], causal, first), dot_nt(v_half[head][:n_k], pair_of(d_o, head)[rows])

    def transform(block, products):
        head, first, n_q, n_k = block
        s_t, dp_t = products
        p_t = jnp.exp(s_t - lse_ref[head // TWO, head % TWO:head % TWO + ONE, first:first + n_q])
        weighted = p_t * dp_t
        return p_t.astype(BF16), (weighted - p_t * jnp.sum(weighted, axis=ZERO, keepdims=True)).astype(BF16)

    def grow(old, new):
        if old is None:
            return new
        n_old = old.shape[ZERO]
        return old + new if n_old == new.shape[ZERO] else jnp.concatenate([old + new[:n_old], new[n_old:]], axis=ZERO)

    def consume(block, operands):
        head, first, n_q, n_k = block
        p_b, ds_t = operands
        rows = slice(first, first + n_q)
        dv_h[head] = grow(dv_h[head], dot(p_b, pair_of(d_o, head)[rows]))
        dk_h[head] = grow(dk_h[head], dot(ds_t, pair_of(q_g, head)[rows]))
        dq_t[head].append(dot(k_t[HEAD_DIM * head:HEAD_DIM * (head + ONE), :n_k], ds_t))

    run_ahead(score_blocks(n_heads, q_g.shape[ZERO], k_g.shape[ZERO], causal, 256), produce, transform, consume, ZERO)
    join = lambda parts: jnp.concatenate([join_halves(parts[h], parts[h + ONE]) for h in range(ZERO, n_heads, TWO)], axis=ONE)
    return stack_heads(dq_t, n_heads).T * 0.125, join(dk_h), join(dv_h)


def attn_fwd_kernel(causal, slots, guest, lens_ref, x_ref, kv_ref, wq_ref, wk_ref, wv_ref, w_all, bias_ref, rows_ref,
                    q_ref, k_ref, v_ref, o_ref, lse_ref, h_ref, normed_ref, inv_ref, o_all, wo_v, load_sem):
    q_row, k_row, v_row, o_row, gain_row, o_mat = slots
    sample, group = pl.program_id(ZERO), pl.program_id(ONE)
    d_model = wo_v.shape[ZERO]
    fetch = pltpu.make_async_copy(w_all.at[pl.ds(o_mat * d_model, d_model), :], wo_v, load_sem)

    @pl.when((sample == ZERO) & (group == ZERO))
    def _():
        fetch.start()

    turn = sample * pl.num_programs(ONE) + group
    if guest is not None:
        for where, steps in ((ZERO, (lambda: meet_neighbours(guest.place), guest.begin)), (THREE, (guest.pass_on,)), (5, (guest.complete,))):
            @pl.when(turn == where)
            def _():
                for step in steps:
                    step()

    x_b, kv_b = x_ref[ALL], kv_ref[ALL]
    q_g = ((dot(x_b, wq_ref[ALL]) + bias_ref[q_row:q_row + ONE, :]) * 0.125).astype(BF16)
    k_g = (dot(kv_b, wk_ref[ALL]) + bias_ref[k_row:k_row + ONE, :]).astype(BF16)
    v_g = (dot(kv_b, wv_ref[ALL]) + bias_ref[v_row:v_row + ONE, :]).astype(BF16)
    q_ref[ALL], k_ref[ALL], v_ref[ALL] = q_g, k_g, v_g
    o_g = attend_group(q_g, k_g, v_g, lens_ref[sample], causal, lse_ref)
    o_ref[ALL] = o_g
    o_all[:, pl.ds(pl.multiple_of(group * GROUP, GROUP), GROUP)] = o_g

    @pl.when((sample == ZERO) & (group == pl.num_programs(ONE) - ONE))
    def _():
        fetch.wait()

    @pl.when(group == pl.num_programs(ONE) - ONE)
    def _():
        resid = x_ref[ALL].astype(F32) + dot(o_all[ALL], wo_v[ALL]) + rows_ref[o_row:o_row + ONE, :]
        h_out, normed, inv_std = norm_rows(resid, rows_ref[gain_row:gain_row + ONE, :], rows_ref[gain_row + ONE:gain_row + TWO, :])
        h_ref[ALL], normed_ref[ALL], inv_ref[ALL] = h_out, normed, inv_std

    if guest is not None:
        @pl.when(turn == pl.num_programs(ZERO) * pl.num_programs(ONE) - ONE)
        def _():
            guest.end()


def attn_forward(x, kv, lens, attn_full, bias_rows, mats, slots, causal, planes=None, full_rows=None):
    d_model = x.shape[-ONE]
    n_batch = lens.shape[ZERO]
    n_q, n_k = x.shape[ZERO] // n_batch, kv.shape[ZERO] // n_batch
    n_groups = d_model // GROUP
    col = lambda mat: pl.BlockSpec((d_model, GROUP), lambda b, g: (mat, g))
    q_blk = pl.BlockSpec((n_q, GROUP), lambda b, g: (b, g))
    k_blk = pl.BlockSpec((n_k, GROUP), lambda b, g: (b, g))
    tok = lambda n: pl.BlockSpec((n, d_model), lambda b, g: (b, ZERO))
    n_heads_g = GROUP // HEAD_DIM
    out_shape = (
        jax.ShapeDtypeStruct(x.shape, BF16), jax.ShapeDtypeStruct(kv.shape, BF16), jax.ShapeDtypeStruct(kv.shape, BF16),
        jax.ShapeDtypeStruct(x.shape, BF16), jax.ShapeDtypeStruct((n_batch, n_groups, n_heads_g // TWO, TWO, n_q), F32),
        jax.ShapeDtypeStruct(x.shape, BF16), jax.ShapeDtypeStruct(x.shape, F32), jax.ShapeDtypeStruct((x.shape[ZERO], ONE), F32))
    kernel = functools.partial(attn_fwd_kernel, causal, slots + (mats[THREE],))
    in_specs = [pl.BlockSpec(memory_space=pltpu.SMEM), tok(n_q), tok(n_k), col(mats[ZERO]), col(mats[ONE]), col(mats[TWO]), pl.BlockSpec(memory_space=pl.ANY),
                pl.BlockSpec((bias_rows.shape[ZERO], GROUP), lambda b, g: (ZERO, g)), pl.BlockSpec(bias_rows.shape, lambda b, g: (ZERO, ZERO))]
    out_specs = [q_blk, k_blk, k_blk, q_blk, pl.BlockSpec((ONE, ONE, n_heads_g // TWO, TWO, n_q), lambda b, g: (b, g, ZERO, ZERO, ZERO)),
                 tok(n_q), tok(n_q), pl.BlockSpec((n_q, ONE), lambda b, g: (b, ZERO))]
    scratch = [pltpu.VMEM((n_q, d_model), BF16), pltpu.VMEM((d_model, d_model), BF16), pltpu.SemaphoreType.DMA]
    args = [lens, x, kv, attn_full, attn_full, attn_full, attn_full, bias_rows, bias_rows]
    params = dict(vmem_limit_bytes=VMEM_BYTES, dimension_semantics=('arbitrary', 'arbitrary'))
    if planes is None:
        body = functools.partial(kernel, None)
    else:
        n_in, n_out, n_own = len(args), len(out_specs), len(scratch)

        def body(*refs):
            ins, held, outs, whole, rest = refs[:n_in], refs[n_in], refs[n_in + ONE:n_in + ONE + n_out], refs[n_in + ONE + n_out], refs[n_in + TWO + n_out:]
            kernel(LastPhase(held, whole, *rest[n_own:]), *ins, *outs, *rest[:n_own])

        in_specs.append(pl.BlockSpec(memory_space=pltpu.VMEM))
        args.append(planes)
        out_specs.append(pl.BlockSpec(memory_space=pl.ANY))
        out_shape += (jax.ShapeDtypeStruct((SIDE, SIDE, SIDE, full_rows // SIDE ** THREE, d_model), BF16),)
        scratch += LastPhase.scratch_shapes(planes)
        params |= dict(collective_id=5, has_side_effects=True)
    return pl.pallas_call(
        body, grid=(n_batch, n_groups), in_specs=in_specs, out_specs=out_specs, out_shape=out_shape, scratch_shapes=scratch,
        compiler_params=pltpu.CompilerParams(**params),
        cost_estimate=pl.CostEstimate(flops=TWO * d_model * d_model * (TWO * x.shape[ZERO] + TWO * kv.shape[ZERO]) + 16 * x.shape[ZERO] * n_k * d_model, bytes_accessed=20 * x.shape[ZERO] * d_model, transcendentals=ZERO),
        name='attn_fwd',
    )(*args)


def attn_bwd_kernel(causal, gain_row, mats, guest, lens_ref, dres_ref, wo_ref, w_all, q_ref, k_ref, v_ref, lse_ref,
                    rows_ref, normed_ref, inv_ref, lhs_refs, rows_out, dres_out, sums_ref, tail_ref, grads_ref,
                    rhs_q, rhs_k, lhs_q, lhs_k, do_v, w_v, grad_v, load_sem, store_sem):
    sample, group = pl.program_id(ZERO), pl.program_id(ONE)
    d_model = wo_ref.shape[ONE]
    n_q, n_k = q_ref.shape[ZERO], k_ref.shape[ZERO]
    last = pl.num_programs(ONE) - ONE
    fetches = [] if causal else [pltpu.make_async_copy(w_all.at[pl.ds(mats[ZERO] * d_model, d_model), :], w_v, load_sem.at[ZERO])]
    hand_on = pltpu.make_async_copy(rhs_q.at[pl.ds(ZERO, THREE)] if causal else rhs_k, rows_out, load_sem.at[ONE])
    dk_all, dv_all = (rhs_q.at[ONE], rhs_q.at[TWO]) if causal else (rhs_k.at[ZERO], rhs_k.at[ONE])
    d_all, dres_all = rhs_q.at[ZERO], rhs_q.at[THREE if causal else ONE]
    places = (lhs_q.at[ZERO], lhs_q.at[ONE]) if causal else (lhs_q.at[ZERO], lhs_k, lhs_q.at[ZERO])
    lhs_fetch = lambda i: pltpu.make_async_copy(lhs_refs[i], places[i], load_sem.at[THREE + i])
    store = lambda buf, mat: pltpu.make_async_copy(grad_v.at[buf], grads_ref.at[pl.ds(pl.multiple_of(mat * d_model, d_model), d_model), :], store_sem.at[buf])

    @pl.when((sample == ZERO) & (group == ZERO))
    def _():
        for fetch in fetches + [lhs_fetch(ZERO), lhs_fetch(ONE)]:
            fetch.start()

    turn = sample * pl.num_programs(ONE) + group
    q_rows = pl.ds(pl.multiple_of(sample * n_q, n_q), n_q)
    k_rows = pl.ds(pl.multiple_of(sample * n_k, n_k), n_k)
    d_o = dot_nt(dres_ref[ALL].astype(BF16), wo_ref[ALL]).astype(BF16)

    def keep(found, first, width):
        here = pl.ds(first, width)
        cols = pl.ds(pl.multiple_of(group * GROUP + first, PAIR), width)
        for i, (full, rows, value) in enumerate(zip((d_all, dk_all, dv_all), (q_rows, k_rows, k_rows), found)):
            sums_ref[ZERO, i:i + ONE, here] = col_sum(value)
            full[rows, cols] = value.astype(BF16)

    if causal:
        keep(attend_group_bwd(d_o, q_ref[ALL], k_ref[ALL], v_ref[ALL], lens_ref[sample], causal, lse_ref.at[ZERO, ZERO]), ZERO, GROUP)
    else:
        do_v[ALL] = d_o

        def one_pair(pair, _):
            guest(ZERO, TWO * turn + pair)
            first = pl.multiple_of(pair * PAIR, PAIR)
            here = pl.ds(first, PAIR)
            keep(attend_group_bwd(do_v[:, here], q_ref[:, here], k_ref[:, here], v_ref[:, here], lens_ref[sample], causal, lse_ref.at[ZERO, ZERO, pl.ds(pair, ONE)]), first, PAIR)
            return ZERO

        lax.fori_loop(ZERO, GROUP // PAIR, one_pair, ZERO)

    @pl.when(group == ZERO)
    def _():
        dres_all[q_rows, :] = dres_ref[ALL].astype(BF16)

    guest(THREE, turn)
    if causal:
        tail_ref[ALL] = jnp.zeros_like(tail_ref)
    else:
        @pl.when((sample == ZERO) & (group == last))
        def _():
            for fetch in fetches:
                fetch.wait()

        @pl.when(group == last)
        def _():
            d_h = dres_ref[ALL] + dot_nt(d_all[q_rows, :], w_v[ALL])
            normed = normed_ref[ALL]
            d_resid = norm_rows_bwd(d_h, normed, inv_ref[ALL], rows_ref[gain_row:gain_row + ONE, :])
            dres_out[ALL] = d_resid
            tail_ref[ZERO, ZERO:ONE, :] = col_sum(d_resid)
            tail_ref[ZERO, ONE:TWO, :] = col_sum(d_h * normed)
            tail_ref[ZERO, TWO:THREE, :] = col_sum(d_h)

    @pl.when(turn == pl.num_programs(ZERO) * pl.num_programs(ONE) - ONE)
    def _():
        hand_on.start()
        guest(TWO, 12)
        lhs_fetch(ZERO).wait()
        if causal:
            lhs_fetch(ONE).wait()

            def square(i, _):
                @pl.when(i >= TWO)
                def _():
                    store(i % TWO, mats[ZERO]).wait()

                grad_v[i % TWO] = dot_tn(lhs_q[i // THREE], rhs_q[i])
                store(i % TWO, mats[ZERO] + i).start()
                return ZERO

            lax.fori_loop(ZERO, 4, square, ZERO)
        else:
            def square_q(i, _):
                @pl.when(i == ONE)
                def _():
                    lhs_fetch(TWO).start()
                    lhs_fetch(TWO).wait()

                grad_v[i] = dot_tn(lhs_q[ZERO], rhs_q[i])
                store(i, mats[ZERO] + THREE * i).start()
                return ZERO

            def square_k(i, _):
                store(i, mats[ONE]).wait()
                grad_v[i] = dot_tn(lhs_k[ALL], rhs_k[i])
                store(i, mats[ONE] + i).start()
                return ZERO

            lax.fori_loop(ZERO, TWO, square_q, ZERO)
            guest(TWO, 13)
            lhs_fetch(ONE).wait()
            lax.fori_loop(ZERO, TWO, square_k, ZERO)
            guest(TWO, 14)
        for buf in range(TWO):
            store(buf, mats[ZERO]).wait()
        hand_on.wait()


def scatter_guest(scatter, plan, parity, position):
    steps = dict(end=scatter.end) | {('relay', p): functools.partial(scatter.relay, p) for p in range(THREE)}
    steps |= {('settle', p): functools.partial(scatter.settle, p) for p in range(THREE)} | {turn: functools.partial(scatter.absorb, turn) for turn in range(SIDE)}
    if parity == TWO:
        for name in plan.get(position, ()):
            steps[name]()
        return
    if parity == THREE:
        @pl.when(position == 5)
        def _():
            for name in plan['late']:
                steps[name]()
        return
    if parity == ZERO:
        @pl.when(position == ZERO)
        def _():
            meet_neighbours(scatter.place)
            scatter.begin()
    for where, names in plan.items():
        if where != 'late' and where < 12:
            @pl.when(position == where)
            def _():
                for name in names:
                    steps[name]()


def no_guest(parity, position):
    pass


def attn_backward(dres, q, k, v, lse, lens, attn_full, bias_rows, mats, causal, lhs_list, g_rows=None, scale=None, gain_row=ZERO, normed=None, inv_std=None, grads=None):
    d_model = q.shape[-ONE]
    n_batch = lens.shape[ZERO]
    n_q, n_k = q.shape[ZERO] // n_batch, k.shape[ZERO] // n_batch
    n_groups = d_model // GROUP
    row = lambda mat: pl.BlockSpec((GROUP, d_model), lambda b, g: (mat * n_groups + g, ZERO))
    q_blk = pl.BlockSpec((n_q, GROUP), lambda b, g: (b, g))
    k_blk = pl.BlockSpec((n_k, GROUP), lambda b, g: (b, g))
    tok = lambda n: pl.BlockSpec((n, d_model), lambda b, g: (b, ZERO))
    n_heads_g = GROUP // HEAD_DIM
    anywhere = pl.BlockSpec(memory_space=pl.ANY)
    in_specs = [pl.BlockSpec(memory_space=pltpu.SMEM), tok(n_q), row(mats[THREE]), anywhere, q_blk, k_blk, k_blk,
                pl.BlockSpec((ONE, ONE, n_heads_g // TWO, TWO, n_q), lambda b, g: (b, g, ZERO, ZERO, ZERO)), pl.BlockSpec(bias_rows.shape, lambda b, g: (ZERO, ZERO))]
    args = [lens, dres, attn_full, attn_full, q, k, v, lse, bias_rows]
    tail_shape = jax.ShapeDtypeStruct((n_batch, 8, d_model), F32)
    out_shape = [jax.ShapeDtypeStruct((THREE,) + q.shape if causal else (TWO,) + k.shape, BF16)]
    out_specs = [anywhere]
    if not causal:
        late = dict(pipeline_mode=pl.Buffered(ONE))
        in_specs += [pl.BlockSpec((n_q, d_model), lambda b, g: (b, ZERO), **late), pl.BlockSpec((n_q, ONE), lambda b, g: (b, ZERO), **late)]
        args += [normed, inv_std]
        out_shape.append(jax.ShapeDtypeStruct(q.shape, F32))
        out_specs.append(tok(n_q))
    n_lhs_at = len(args)
    args += list(lhs_list)
    in_specs += [anywhere] * len(lhs_list)
    out_shape += [tail_shape, tail_shape, jax.ShapeDtypeStruct(attn_full.shape, F32)]
    out_specs += [pl.BlockSpec((ONE, 8, GROUP), lambda b, g: (b, ZERO, g)), pl.BlockSpec((ONE, 8, d_model), lambda b, g: (b, ZERO, ZERO)), anywhere]
    held = lambda count, n: pltpu.VMEM((count, n_batch * n, d_model), BF16)
    own = [held(4, n_q), held(TWO, n_q)] if causal else [held(TWO, n_q), held(TWO, n_k), held(ONE, n_q), pltpu.VMEM((n_batch * n_k, d_model), BF16)]
    own += [] if causal else [pltpu.VMEM((n_q, GROUP), BF16)]
    own += [] if causal else [pltpu.VMEM((d_model, d_model), BF16)]
    own += [pltpu.VMEM((TWO, d_model, d_model), F32), pltpu.SemaphoreType.DMA((6,)), pltpu.SemaphoreType.DMA((TWO,))]
    kernel = functools.partial(attn_bwd_kernel, causal, gain_row, mats)
    params = dict(vmem_limit_bytes=VMEM_BYTES, dimension_semantics=('arbitrary', 'arbitrary'))
    aliases = {}
    if causal:
        args.append(grads)
        in_specs.append(anywhere)
        aliases = {len(args) - ONE: len(out_shape) - ONE}
    else:
        args.append(as_torus(g_rows))
        in_specs.append(anywhere)
        n_rows = args[-ONE].shape[THREE]
        out_shape.append(jax.ShapeDtypeStruct((n_rows, d_model), F32))
        out_specs.append(anywhere)
        params |= dict(collective_id=THREE, has_side_effects=True, vmem_limit_bytes=67043328)
    scratch = own + ([] if causal else Scatter.scratch_shapes([n_rows]))
    n_in, n_out, n_own = len(args), len(out_shape), len(own)

    def body(*refs):
        ins, outs, rest = refs[:n_in], refs[n_in:n_in + n_out], refs[n_in + n_out:]
        lhs_refs, mine = ins[n_lhs_at:-ONE], rest[:n_own]
        if causal:
            rows_out, sums, tail, grads_ref = outs
            kernel(no_guest, *ins[:n_lhs_at], None, None, lhs_refs, rows_out, None, sums, tail, grads_ref, mine[ZERO], None, mine[ONE], None, None, None, *mine[TWO:])
        else:
            rows_out, dres_out, sums, tail, grads_ref, total = outs
            scatter = Scatter(scale, [(ins[-ONE], ZERO, n_rows)], [total], rest[n_own:])
            kernel(functools.partial(scatter_guest, scatter, CROSS_PLAN), *ins[:n_lhs_at], lhs_refs, rows_out, dres_out, sums, tail, grads_ref, *mine)

    return pl.pallas_call(
        body, grid=(n_batch, n_groups), in_specs=in_specs, out_specs=out_specs, out_shape=out_shape, scratch_shapes=scratch, input_output_aliases=aliases,
        compiler_params=pltpu.CompilerParams(**params),
        cost_estimate=pl.CostEstimate(flops=TWO * d_model * d_model * (TWO * q.shape[ZERO] + TWO * k.shape[ZERO]) + 40 * q.shape[ZERO] * n_k * d_model, bytes_accessed=20 * q.shape[ZERO] * d_model, transcendentals=ZERO),
        name='attn_bwd',
    )(*args)


def ffn_kernel(n_blocks, h_ref, dy_ref, up_ref, down_ref, rows_ref, bias_ref, normed_ref, inv_ref,
               y_ref, grad_ref, dres2_ref, tail_ref, upsum_ref, left_all, right_all):
    step = pl.program_id(ZERO)
    block, d_model = h_ref.shape
    n_square = left_all.shape[TWO] // d_model

    @pl.when(step < n_blocks)
    def _():
        rows = pl.ds(pl.multiple_of(step * block, block), block)
        h_b = h_ref[ALL]
        right_all[ZERO, rows, :] = h_b
        up = dot_nt(h_b, up_ref[ALL]) + bias_ref[ALL]
        cdf = 0.5 * (1.0 + lax.erf(up * 0.7071067811865476))
        gelu = (up * cdf).astype(BF16)
        slope = cdf + up * (0.3989422804014327 * jnp.exp(-0.5 * up * up))
        left_all[ONE, rows, :] = gelu
        resid = h_b.astype(F32) + dot(gelu, down_ref[ALL]) + rows_ref[8:9, :]
        y_b, normed3, inv3 = norm_rows(resid, rows_ref[13:14, :], rows_ref[14:15, :])
        y_ref[ALL] = y_b
        dy = dy_ref[ALL].astype(F32)
        d_res3 = norm_rows_bwd(dy, normed3, inv3, rows_ref[13:14, :])
        d_res3_b = d_res3.astype(BF16)
        right_all[ONE, rows, :] = d_res3_b
        d_up = dot_nt(d_res3_b, down_ref[ALL]) * slope
        d_up_b = d_up.astype(BF16)
        left_all[ZERO, rows, :] = d_up_b
        d_h2 = d_res3 + dot(d_up_b, up_ref[ALL])
        normed2 = normed_ref[ALL]
        d_res2 = norm_rows_bwd(d_h2, normed2, inv_ref[ALL], rows_ref[11:12, :])
        dres2_ref[ALL] = d_res2
        tail = jnp.concatenate([col_sum(d_res2), col_sum(d_res3), col_sum(d_h2 * normed2), col_sum(d_h2), col_sum(dy * normed3), col_sum(dy),
                                jnp.zeros((TWO, dy.shape[ONE]), F32)], axis=ZERO)
        up_sum = col_sum(d_up)

        @pl.when(step == ZERO)
        def _():
            tail_ref[ALL] = tail
            upsum_ref[ALL] = up_sum

        @pl.when(step > ZERO)
        def _():
            tail_ref[ALL] += tail
            upsum_ref[ALL] += up_sum

    square = step - n_blocks
    cols = pl.ds(pl.multiple_of(lax.rem(square + TWO * n_square, n_square) * d_model, d_model), d_model)

    @pl.when(square >= ZERO)
    def _():
        which = square // n_square
        grad_ref[ALL] = dot_tn(left_all[which, :, cols], right_all[which])


def ffn_both(h2, dy, ffn_full, bias_rows, up_bias, normed2, inv2, block=256):
    n_tok, d_model = h2.shape
    ffn_dim = ffn_full.shape[ZERO] // TWO
    n_blocks = n_tok // block
    n_steps = n_blocks + ffn_full.shape[ZERO] // d_model
    at = lambda i: jnp.minimum(i, n_blocks - ONE)
    tok = pl.BlockSpec((block, d_model), lambda i: (at(i), ZERO))
    once = lambda shape, idx: pl.BlockSpec(shape, lambda i: idx, pipeline_mode=pl.Buffered(ONE))
    return pl.pallas_call(
        functools.partial(ffn_kernel, n_blocks), grid=(n_steps,),
        in_specs=[tok, tok, once((ffn_dim, d_model), (ZERO, ZERO)), once((ffn_dim, d_model), (ONE, ZERO)), once(bias_rows.shape, (ZERO, ZERO)), once((ONE, ffn_dim), (ZERO, ZERO)),
                  tok, pl.BlockSpec((block, ONE), lambda i: (at(i), ZERO))],
        out_specs=[tok, pl.BlockSpec((d_model, d_model), lambda i: (jnp.maximum(i - n_blocks, ZERO), ZERO)), tok, pl.BlockSpec((8, d_model), lambda i: (ZERO, ZERO)), pl.BlockSpec((ONE, ffn_dim), lambda i: (ZERO, ZERO))],
        out_shape=[jax.ShapeDtypeStruct(h2.shape, BF16), jax.ShapeDtypeStruct(ffn_full.shape, F32), jax.ShapeDtypeStruct(h2.shape, F32),
                   jax.ShapeDtypeStruct((8, d_model), F32), jax.ShapeDtypeStruct((ONE, ffn_dim), F32)],
        scratch_shapes=[pltpu.VMEM((TWO, n_tok, ffn_dim), BF16), pltpu.VMEM((TWO, n_tok, d_model), BF16)],
        compiler_params=pltpu.CompilerParams(vmem_limit_bytes=VMEM_BYTES, dimension_semantics=('arbitrary',)),
        cost_estimate=pl.CostEstimate(flops=12 * n_tok * d_model * ffn_dim, bytes_accessed=30 * n_tok * d_model, transcendentals=ZERO),
        name='ffn_both',
    )(h2, dy, ffn_full, ffn_full, bias_rows, up_bias, normed2, inv2)


CROSS_PLAN = {ONE: (ZERO,), TWO: (ONE,), THREE: (TWO,), 4: (THREE,), 5: (('relay', ZERO),), 9: (('settle', ZERO),), 10: (('relay', ONE),), 'late': (('settle', ONE),), 12: (('relay', TWO),), 13: (('settle', TWO),), 14: ('end',)}


def solution(mesh):
    n_fsdp = mesh.shape['fsdp']
    n_dp = mesh.shape['dp']
    batch_axes = ('dp', 'fsdp')
    act_spec = P(batch_axes, None, None)
    len_spec = P(batch_axes)
    row_spec = P('fsdp', None)
    vec_spec = P('fsdp')

    def device_step(dec_in, enc_out, src_lens, tgt_lens, y_cot, attn_w, ffn_w, vec_params):
        d_model, n_vec = dec_in.shape[TWO], vec_params.shape[ZERO]
        scale = 1.0 / (dec_in.shape[ZERO] * dec_in.shape[ONE] * n_fsdp * n_dp)
        x, enc, dy = (a.reshape(-ONE, d_model) for a in (dec_in, enc_out, y_cot))
        vec_rows = jnp.pad(vec_params.astype(F32), (ZERO, 16 * LANES - n_vec)).reshape(16, LANES)
        attn_tiles, planes, vec_tiles = gather_params(attn_w, ffn_w, vec_rows)
        attn_full = attn_tiles.reshape(-ONE, d_model)
        vec_f = vec_tiles.reshape(n_fsdp, 16, LANES)[:, :TWO].reshape(n_fsdp, TWO * LANES)[:, :n_vec].reshape(-ONE)
        bias_rows = jnp.pad(vec_f[:15 * d_model].reshape(15, d_model), ((ZERO, ONE), (ZERO, ZERO)))
        up_bias = vec_f[15 * d_model:].reshape(ONE, -ONE)
        q1, k1, v1, o1, lse1, h1, normed1, inv1 = attn_forward(x, x, tgt_lens, attn_full, bias_rows, (ZERO, ONE, TWO, THREE), (ZERO, ONE, TWO, THREE, 9), True)
        q2, k2, v2, o2, lse2, h2, normed2, inv2, ffn_tiles = attn_forward(h1, enc, src_lens, attn_full, bias_rows, (4, 5, 6, 7), (4, 5, 6, 7, 11), False, planes, ffn_w.shape[ZERO] * n_fsdp)
        ffn_full = ffn_tiles.reshape(-ONE, d_model)
        y, g_ffn, d_res2, ffn_tail, up_sum = ffn_both(h2, dy, ffn_full, bias_rows, up_bias, normed2, inv2)
        d_cross, d_res1, sums2, tail2, grads, ffn_out = attn_backward(d_res2, q2, k2, v2, lse2, src_lens, attn_full, bias_rows, (4, 5, 6, 7), False, (h1, enc, o2), g_ffn, scale, 9, normed1, inv1)
        d_self, sums1, _, grads = attn_backward(d_res1, q1, k1, v1, lse1, tgt_lens, attn_full, bias_rows, (ZERO, ONE, TWO, THREE), True, (x, o1), grads=grads)
        s1, s2, t2 = jnp.sum(sums1, axis=ZERO), jnp.sum(sums2, axis=ZERO), jnp.sum(tail2, axis=ZERO)
        g_vec = jnp.concatenate([s1[ZERO:THREE].reshape(-ONE), t2[ZERO], s2[ZERO:THREE].reshape(-ONE), ffn_tail[ZERO], ffn_tail[ONE], t2[ONE], t2[TWO], ffn_tail[TWO], ffn_tail[THREE], ffn_tail[4], ffn_tail[5], up_sum[ZERO]])
        g_rows = jnp.pad(g_vec.reshape(n_fsdp, ONE, n_vec), ((ZERO, ZERO), (ZERO, 7), (ZERO, TWO * LANES - n_vec))).reshape(n_fsdp * 8, -ONE)
        attn_out, vec_out, d_x, d_enc = scatter_grads(grads, g_rows, scale, attn_full, (ZERO, ONE, TWO, 5, 6), d_res1, d_self, d_cross)
        return y.reshape(dec_in.shape), d_x.reshape(dec_in.shape), d_enc.reshape(enc_out.shape), attn_out, ffn_out, vec_out[ZERO, :n_vec]

    return jax.shard_map(device_step, mesh=mesh, in_specs=(act_spec, act_spec, len_spec, len_spec, act_spec, row_spec, row_spec, vec_spec), out_specs=(act_spec, act_spec, act_spec, row_spec, row_spec, vec_spec), check_vma=False)
```

```python
import functools
import jax
import jax.numpy as jnp
from jax import lax
from jax.experimental import pallas as pl
from jax.experimental.pallas import tpu as pltpu
from jax.sharding import PartitionSpec as P

ZERO, ONE, TWO, THREE = range(4)
ALL = ...
HEAD_DIM = 64
LN_EPS = 1e-5
MASK_FILL = -1e30
VMEM_BYTES = 60 * 1024 * 1024
F32 = jnp.float32
BF16 = jnp.bfloat16
GROUP = 256
PAIR = 128


SIDE = 4
LANES = 128
COLOURS = THREE
STAGES = TWO
DIM_ORDER = ((TWO, ONE, ZERO), (ONE, ZERO, TWO), (ZERO, TWO, ONE))
MESH_ID = pl.DeviceIdType.MESH


def torus_place():
    chip = lax.axis_index('fsdp')
    return (chip // (SIDE * SIDE), lax.rem(chip // SIDE, SIDE), lax.rem(chip, SIDE))


def chip_at(place, dim, shift):
    moved = [lax.rem(p + shift + SIDE, SIDE) if d == dim else p for d, p in enumerate(place)]
    return (moved[ZERO] * SIDE + moved[ONE]) * SIDE + moved[TWO]


def meet_neighbours(place):
    barrier = pltpu.get_barrier_semaphore()
    core = lax.axis_index('dp')
    for dim in range(THREE):
        for shift in (ONE, -ONE):
            pl.semaphore_signal(barrier, inc=ONE, device_id=(core, chip_at(place, dim, shift)), device_id_type=MESH_ID)
    pl.semaphore_signal(barrier, inc=ONE, device_id=(ONE - core, lax.axis_index('fsdp')), device_id_type=MESH_ID)
    pl.semaphore_wait(barrier, 7)


class Scatter:
    def __init__(self, scale, sources, outs, scratch):
        self.scale, self.outs = scale, outs
        self.sources = [(ref, pl.ds(first, n)) for ref, first, n in sources]
        (self.acc, g1, d1, g2, d2, g3, d3, self.send_sem, self.recv_sem, self.load_sem, self.stage) = scratch
        self.got, self.far = (g1, g2, g3), (d1, d2, d3)
        self.heights = [n for _, _, n in sources]
        self.offsets = [sum(self.heights[:i]) for i in range(len(sources))]
        self.n_low = self.heights[ZERO] // TWO
        self.core, self.chip, self.place = lax.axis_index('dp'), lax.axis_index('fsdp'), torus_place()
        self.pieces = [(d, colour) for d in (TWO, ONE, THREE, ZERO) for colour in range(COLOURS)]

    @staticmethod
    def scratch_shapes(heights):
        h = sum(heights)
        n_low = heights[ZERO] // TWO
        buf = lambda *shape: pltpu.VMEM((COLOURS,) + shape + (LANES,), F32)
        n = Scatter.n_copies(len(heights))
        return [buf(SIDE, SIDE, SIDE, h), buf(TWO, SIDE, SIDE, h), buf(TWO, TWO, SIDE, h), buf(TWO, SIDE, h), buf(TWO, TWO, h), buf(TWO, h), buf(TWO, max(n_low, h - n_low)),
                pltpu.SemaphoreType.DMA((n,)), pltpu.SemaphoreType.DMA((n,)), pltpu.SemaphoreType.DMA((THREE + COLOURS, len(heights))),
                pltpu.VMEM((STAGES, SIDE, SIDE, h, LANES), F32)]

    @staticmethod
    def n_copies(n_parts):
        return 12 * n_parts + COLOURS * 18 + COLOURS * n_parts

    def parts(self, colour):
        return range(len(self.sources) if colour == ZERO else ONE)

    def height(self, colour):
        return sum(self.heights[i] for i in self.parts(colour))

    def remote(self, i, src, dst, device):
        return pltpu.make_async_remote_copy(src_ref=src, dst_ref=dst, send_sem=self.send_sem.at[i], recv_sem=self.recv_sem.at[i], device_id=device, device_id_type=MESH_ID)

    def columns(self, of_core, colour, part=ZERO):
        return pl.ds(pl.multiple_of((of_core * COLOURS + colour if part == ZERO else of_core) * LANES, LANES), LANES)

    def slot(self, d, colour):
        dim = DIM_ORDER[colour][ZERO]
        where = [slice(None)] * THREE
        where[dim] = lax.rem(self.place[dim] + d, SIDE)
        return tuple(where)

    def rows_of(self, part):
        return pl.ds(self.offsets[part], self.heights[part])

    def swaps(self, piece):
        d, colour = self.pieces[piece]
        where = self.slot(d, colour)
        n = len(self.sources)
        return [self.remote(piece * n + i, self.sources[i][ZERO].at[where + (self.sources[i][ONE], self.columns(ONE - self.core, colour, i))],
                            self.acc.at[(colour,) + where + (self.rows_of(i), slice(None))], (ONE - self.core, self.chip)) for i in self.parts(colour)]

    def loads(self, piece):
        d, colour = self.pieces[piece]
        where, buf = self.slot(d, colour), piece % STAGES
        return [pltpu.make_async_copy(self.sources[i][ZERO].at[where + (self.sources[i][ONE], self.columns(self.core, colour, i))],
                                      self.stage.at[buf, :, :, self.rows_of(i), :], self.load_sem.at[buf, i]) for i in self.parts(colour)]

    def split_rows(self, colour, half):
        return pl.ds(ZERO, self.n_low) if half == ZERO else pl.ds(self.n_low, self.height(colour) - self.n_low)

    def block(self, colour, phase, d, half=None):
        order = DIM_ORDER[colour]
        where = [None, None, None]
        for done in order[:phase]:
            where[done] = self.place[done]
        where[order[phase]] = lax.rem(self.place[order[phase]] + d, SIDE)
        for i, rest in enumerate(sorted(order[phase + ONE:])):
            where[rest] = slice(None) if half is None or i > ZERO else pl.ds(TWO * half, TWO)
        rows = self.split_rows(colour, half) if phase == TWO and half is not None else pl.ds(ZERO, self.height(colour))
        return self.acc.at[(colour,) + tuple(where) + (rows, slice(None))]

    def got_half(self, colour, phase, direction, half):
        if phase == TWO:
            return self.got[phase].at[colour, direction, self.split_rows(colour, half), :]
        return self.got_all(colour, phase, direction, pl.ds(TWO * half, TWO))

    def got_all(self, colour, phase, direction, which=slice(None)):
        rows = (pl.ds(ZERO, self.height(colour)), slice(None))
        blocks = ((which, slice(None)), (which,), ())[phase]
        return self.got[phase].at[(colour, direction) + blocks + rows]

    def far_part(self, colour, phase, direction):
        if phase == TWO:
            return self.far[phase].at[colour, direction, pl.ds(ZERO, self.n_low if direction == ZERO else self.height(colour) - self.n_low), :]
        return self.far[phase].at[(colour, direction) + (slice(None),) * (TWO - phase) + (pl.ds(ZERO, self.height(colour)), slice(None))]

    def ring(self, colour, phase, direction):
        shift = ONE - TWO * direction
        device = (self.core, chip_at(self.place, DIM_ORDER[colour][phase], shift))
        i = 12 * len(self.sources) + ((colour * THREE + phase) * TWO + direction) * THREE
        near = shift % SIDE
        return (self.remote(i, self.block(colour, phase, TWO, direction), self.far_part(colour, phase, direction), device),
                self.remote(i + ONE, self.block(colour, phase, near, ONE - direction), self.got_half(colour, phase, direction, ONE - direction), device),
                self.remote(i + TWO, self.block(colour, phase, near, direction), self.got_half(colour, phase, direction, direction), device))

    def gives(self, colour):
        n = len(self.sources)
        base = 12 * n + COLOURS * 18 + colour * n
        done = self.acc.at[colour, self.place[ZERO], self.place[ONE], self.place[TWO]]
        pairs = [(done.at[self.rows_of(i), :], self.outs[i].at[:, self.columns(self.core, colour, i)]) for i in self.parts(colour)]
        return [(self.remote(base + i, src, dst, (ONE - self.core, self.chip)), pltpu.make_async_copy(src, dst, self.load_sem.at[THREE + colour, i])) for i, (src, dst) in enumerate(pairs)]

    def add_into(self, dst, sources, n_lead):
        def body(i, _):
            total = dst[i]
            for src in sources:
                total = total + src[i]
            dst[i] = total
            return ZERO

        if n_lead == TWO:
            lax.fori_loop(ZERO, dst.shape[ZERO], body, ZERO)
        else:
            total = dst[ALL]
            for src in sources:
                total = total + src[ALL]
            dst[ALL] = total


    def begin(self):
        for piece in range(STAGES):
            for copy in self.loads(piece):
                copy.start()
        for piece in range(len(self.pieces)):
            for copy in self.swaps(piece):
                copy.start()

    def absorb(self, turn):
        for piece in range(turn * COLOURS, (turn + ONE) * COLOURS):
            d, colour = self.pieces[piece]
            for copy in self.loads(piece):
                copy.wait()
            for copy in self.swaps(piece):
                copy.wait_recv()
            rows = (pl.ds(ZERO, self.height(colour)), slice(None))
            self.add_into(self.acc.at[(colour,) + self.slot(d, colour) + rows], [self.stage.at[(piece % STAGES, slice(None), slice(None)) + rows]], TWO)
            if piece + STAGES < len(self.pieces):
                for copy in self.loads(piece + STAGES):
                    copy.start()
            if turn == ZERO:
                for direction in range(TWO):
                    self.ring(colour, ZERO, direction)[ZERO].start()
            elif turn < THREE:
                self.ring(colour, ZERO, turn - ONE)[ONE].start()

    def relay(self, phase):
        for colour in range(COLOURS):
            for direction in range(TWO):
                far, _, fed = self.ring(colour, phase, direction)
                far.wait_recv()
                self.add_into(self.block(colour, phase, (ONE - TWO * direction) % SIDE, direction), [self.far_part(colour, phase, direction)], TWO - phase)
            for direction in range(TWO):
                self.ring(colour, phase, direction)[TWO].start()

    def settle(self, phase):
        for colour in range(COLOURS):
            for direction in range(TWO):
                _, own, fed = self.ring(colour, phase, direction)
                own.wait_recv()
                fed.wait_recv()
            self.add_into(self.block(colour, phase, ZERO), [self.got_all(colour, phase, direction) for direction in range(TWO)], TWO - phase)
            if phase < TWO:
                for kind in range(TWO):
                    for direction in range(TWO):
                        self.ring(colour, phase + ONE, direction)[kind].start()
            else:
                done = self.block(colour, TWO, ZERO)
                done[ALL] = done[ALL] * self.scale
                for give, keep in self.gives(colour):
                    keep.start()
                    give.start()

    def end(self):
        for colour in range(COLOURS):
            for give, keep in self.gives(colour):
                give.wait_recv()
                give.wait_send()
                keep.wait()
        for piece in range(len(self.pieces)):
            for copy in self.swaps(piece):
                copy.wait_send()
        for colour in range(COLOURS):
            for phase in range(THREE):
                for direction in range(TWO):
                    for copy in self.ring(colour, phase, direction):
                        copy.wait_send()


def rs_kernel(scale, mats, g_ref, vec_ref, w_all, dres_ref, self_ref, cross_ref, out_ref, vec_out, dx_v, denc_v,
              w_v, dres_v, self_v, cross_v, load_sem, *scratch):
    scatter = Scatter(scale, [(ref, ZERO, ref.shape[THREE]) for ref in (g_ref, vec_ref)], [out_ref, vec_out], scratch)
    d_model = w_v.shape[ONE]
    step = 256
    loads = [pltpu.make_async_copy(w_all.at[pl.ds(mat * d_model, d_model), :], w_v.at[i], load_sem.at[i]) for i, mat in enumerate(mats)]
    loads += [pltpu.make_async_copy(src, dst, load_sem.at[len(mats) + i]) for i, (src, dst) in enumerate(((dres_ref, dres_v), (self_ref, self_v), (cross_ref, cross_v)))]

    def input_grads():
        for copy in loads:
            copy.wait()

        def decoder(i, _):
            rows = pl.ds(pl.multiple_of(i * step, step), step)
            total = dres_v[rows, :]
            for n in range(THREE):
                total = total + dot_nt(self_v[n, rows, :], w_v[n])
            dx_v[rows, :] = total.astype(BF16)
            return ZERO

        def encoder(i, _):
            rows = pl.ds(pl.multiple_of(i * step, step), step)
            denc_v[rows, :] = (dot_nt(cross_v[ZERO, rows, :], w_v[THREE]) + dot_nt(cross_v[ONE, rows, :], w_v[4])).astype(BF16)
            return ZERO

        lax.fori_loop(ZERO, dx_v.shape[ZERO] // step, decoder, ZERO)
        lax.fori_loop(ZERO, denc_v.shape[ZERO] // step, encoder, ZERO)

    meet_neighbours(scatter.place)
    scatter.begin()
    for copy in loads:
        copy.start()
    for turn in range(THREE):
        scatter.absorb(turn)
    scatter.relay(ZERO)
    scatter.absorb(THREE)
    input_grads()
    scatter.settle(ZERO)
    for phase in (ONE, TWO):
        scatter.relay(phase)
        scatter.settle(phase)
    scatter.end()


def as_torus(rows):
    return rows.reshape(SIDE, SIDE, SIDE, rows.shape[ZERO] // SIDE ** THREE, rows.shape[ONE])


def scatter_grads(g_attn, g_vec, scale, attn_full, mats, d_res, d_self, d_cross):
    sources = [as_torus(g_attn), as_torus(g_vec)]
    heights = [src.shape[THREE] for src in sources]
    d_model = g_attn.shape[ONE]
    anywhere = pl.BlockSpec(memory_space=pl.ANY)
    dx_shape, denc_shape = d_self.shape[ONE:], d_cross.shape[ONE:]
    return pl.pallas_call(
        functools.partial(rs_kernel, scale, mats),
        in_specs=[anywhere] * 6, out_specs=[anywhere] * TWO + [pl.BlockSpec(memory_space=pltpu.VMEM)] * TWO,
        out_shape=[jax.ShapeDtypeStruct((h, src.shape[4]), F32) for h, src in zip(heights, sources)] + [jax.ShapeDtypeStruct(dx_shape, BF16), jax.ShapeDtypeStruct(denc_shape, BF16)],
        scratch_shapes=[pltpu.VMEM((len(mats), d_model, d_model), BF16), pltpu.VMEM(d_res.shape, F32), pltpu.VMEM(d_self.shape, BF16), pltpu.VMEM(d_cross.shape, BF16),
                        pltpu.SemaphoreType.DMA((len(mats) + THREE,))] + Scatter.scratch_shapes(heights),
        compiler_params=pltpu.CompilerParams(collective_id=ONE, has_side_effects=True, vmem_limit_bytes=VMEM_BYTES),
        cost_estimate=pl.CostEstimate(flops=10 ** 9, bytes_accessed=8 * d_model * g_attn.shape[ZERO], transcendentals=ZERO),
        name='scatter_grads',
    )(*sources, attn_full, d_res, d_self, d_cross)


class Gather:
    def __init__(self, send_sem, recv_sem, base=ZERO):
        self.send_sem, self.recv_sem = send_sem, recv_sem
        self.used = base
        self.core, self.chip, self.place = lax.axis_index('dp'), lax.axis_index('fsdp'), torus_place()
        self.sibling = (ONE - self.core, self.chip)
        self.started = []

    def remote(self, src, dst, device):
        i = self.used
        self.used += ONE
        return pltpu.make_async_remote_copy(src_ref=src, dst_ref=dst, send_sem=self.send_sem.at[i], recv_sem=self.recv_sem.at[i], device_id=device, device_id_type=MESH_ID)

    def start(self, copy):
        copy.start()
        self.started.append(copy)

    def ring(self, colour, phase, view, own=None, split=False):
        order = DIM_ORDER[colour]
        dim = order[phase]
        have = sorted(order[:phase])

        def index(shift, half=None):
            where = [self.place[ZERO], self.place[ONE], self.place[TWO]]
            where[dim] = lax.rem(self.place[dim] + shift + SIDE, SIDE)
            for i, h in enumerate(have):
                where[h] = slice(None) if half is None or i > ZERO else pl.ds(TWO * half, TWO)
            return tuple(where)

        out = []
        for direction, shift in enumerate((ONE, -ONE)):
            device = (self.core, chip_at(self.place, dim, shift))
            half = direction if phase == ZERO else None
            near_dst = view(index(ZERO), None)
            if split:
                near = [self.remote(view(index(ZERO, h), None), view(index(ZERO, h), None), device) for h in (direction, ONE - direction)]
            else:
                near = [self.remote(near_dst if own is None else own, near_dst, device)]
            out.append(dict(
                near=near,
                far=self.remote(view(index(-shift, direction), half), view(index(-shift, direction), half), device),
                near_at=index(-shift), far_at=index(TWO, direction)))
        return out


def ag_kernel(attn_ref, ffn_ref, vec_ref, oattn_ref, planes_ref, vec_out, attn_v, send_sem, recv_sem, load_sem):
    net = Gather(send_sem, recv_sem)
    core, place = net.core, net.place
    rows, width = attn_ref.shape
    band = rows // (TWO * COLOURS)
    vec_high = vec_ref.shape[ZERO]
    stores, finals = [], []

    def band_rows(colour):
        return pl.ds(pl.multiple_of((core * COLOURS + colour) * band, band), band)

    def columns(half):
        return slice(None) if half is None else pl.ds(half * (width // TWO), width // TWO)

    def attn_view(colour):
        return lambda where, half: attn_v.at[where + (band_rows(colour), columns(half))]

    def ffn_view(colour):
        last = DIM_ORDER[colour][TWO]
        return lambda where, half: planes_ref.at[(colour,) + tuple(w for d, w in enumerate(where) if d != last) + (slice(None), columns(half))]

    def vec_view(where, half):
        return vec_out.at[where + (slice(None) if half is None else pl.ds(half * (vec_high // TWO), vec_high // TWO), slice(None))]

    colours = range(COLOURS)
    attn_own = [attn_ref.at[band_rows(colour), :] for colour in colours]
    ffn_own = [ffn_ref.at[band_rows(colour), :] for colour in colours]
    rings = {('attn', phase): [net.ring(colour, phase, attn_view(colour), attn_own[colour] if phase == ZERO else None, phase > ZERO) for colour in colours] for phase in range(THREE)}
    rings |= {('ffn', phase): [net.ring(colour, phase, ffn_view(colour), ffn_own[colour] if phase == ZERO else None, phase > ZERO) for colour in colours] for phase in range(TWO)}
    rings |= {('vec', phase): [net.ring(ONE, phase, vec_view, vec_ref if phase == ZERO else None)] for phase in range(THREE)}

    def publish(at):
        keep = pltpu.make_async_copy(attn_v.at[at], oattn_ref.at[at], load_sem.at[len(stores)])
        keep.start()
        stores.append(keep)
        give = net.remote(attn_v.at[at], oattn_ref.at[at], net.sibling)
        net.start(give)
        finals.append(give)

    def send_near(name, phase):
        for ring in rings.get((name, phase), ()):
            for way in ring:
                for copy in way['near']:
                    net.start(copy)

    def pass_on(name, phase):
        for ring in rings.get((name, phase), ()):
            for way in ring:
                way['near'][ZERO].wait_recv()
                net.start(way['far'])
        if phase == TWO and name == 'attn':
            for colour in colours:
                for way in rings[(name, phase)][colour]:
                    way['near'][ONE].wait_recv()
                    publish(way['near_at'] + (band_rows(colour), slice(None)))

    def complete(name, phase):
        for colour, ring in enumerate(rings.get((name, phase), ())):
            for way in ring:
                way['far'].wait_recv()
                if phase == ONE and name != 'vec':
                    way['near'][ONE].wait_recv()
            if phase < TWO and (name, phase + ONE) in rings:
                for way in rings[(name, phase + ONE)][colour]:
                    for copy in way['near']:
                        net.start(copy)
            if phase == TWO and name == 'attn':
                for way in ring:
                    publish(way['far_at'] + (band_rows(colour), slice(None)))
        if phase == ONE and name == 'attn':
            for colour in colours:
                last = DIM_ORDER[colour][TWO]
                publish(tuple(place[d] if d == last else slice(None) for d in range(THREE)) + (band_rows(colour), slice(None)))

    for colour in colours:
        attn_v[(place[ZERO], place[ONE], place[TWO]) + (band_rows(colour), slice(None))] = attn_ref[band_rows(colour), :]
        kept = [place[d] for d in range(THREE) if d != DIM_ORDER[colour][TWO]]
        planes_ref[(colour, kept[ZERO], kept[ONE])] = ffn_ref[band_rows(colour), :]
    vec_out[place[ZERO], place[ONE], place[TWO]] = vec_ref[ALL]
    meet_neighbours(place)
    names = ('attn', 'vec', 'ffn')
    for name in names:
        send_near(name, ZERO)
    for phase in range(THREE):
        for name in names:
            pass_on(name, phase)
        for name in names:
            complete(name, phase)
    for copy in finals:
        copy.wait_recv()
    for copy in net.started:
        copy.wait_send()
    for copy in stores:
        copy.wait()


def gather_params(attn_w, ffn_w, vec_rows):
    rows, width = attn_w.shape
    full = (SIDE, SIDE, SIDE, rows, width)
    n_copies = COLOURS * (4 * TWO + 6 * THREE) + 4 * THREE + COLOURS * 5
    vmem = pl.BlockSpec(memory_space=pltpu.VMEM)
    return pl.pallas_call(
        ag_kernel,
        in_specs=[vmem] * THREE, out_specs=[pl.BlockSpec(memory_space=pl.ANY), vmem, vmem],
        out_shape=[jax.ShapeDtypeStruct(full, BF16), jax.ShapeDtypeStruct((COLOURS, SIDE, SIDE, rows // (TWO * COLOURS), width), BF16),
                   jax.ShapeDtypeStruct((SIDE, SIDE, SIDE) + vec_rows.shape, F32)],
        scratch_shapes=[pltpu.VMEM(full, BF16), pltpu.SemaphoreType.DMA((n_copies,)), pltpu.SemaphoreType.DMA((n_copies,)), pltpu.SemaphoreType.DMA((COLOURS * 5,))],
        compiler_params=pltpu.CompilerParams(collective_id=TWO, has_side_effects=True, vmem_limit_bytes=VMEM_BYTES),
        cost_estimate=pl.CostEstimate(flops=10 ** 9, bytes_accessed=4 * rows * width * SIDE ** THREE, transcendentals=ZERO),
        name='gather_params',
    )(attn_w, ffn_w, vec_rows)


class LastPhase:
    def __init__(self, planes, out, near, far, send_sem, recv_sem, load_sem):
        self.planes, self.out, self.near, self.far = planes, out, near, far
        self.send_sem, self.recv_sem, self.load_sem = send_sem, recv_sem, load_sem
        self.core, self.chip, self.place = lax.axis_index('dp'), lax.axis_index('fsdp'), torus_place()
        self.band = planes.shape[THREE]

    @staticmethod
    def scratch_shapes(planes):
        colours, side, _, band, width = planes.shape
        sems = [pltpu.SemaphoreType.DMA((11 * COLOURS,)), pltpu.SemaphoreType.DMA((11 * COLOURS,)), pltpu.SemaphoreType.DMA((5 * COLOURS,))]
        return [pltpu.VMEM((colours, TWO, side, side, band, width), BF16), pltpu.VMEM((colours, TWO, side // TWO, side, band, width), BF16)] + sems

    def remote(self, i, src, dst, device):
        return pltpu.make_async_remote_copy(src_ref=src, dst_ref=dst, send_sem=self.send_sem.at[i], recv_sem=self.recv_sem.at[i], device_id=device, device_id_type=MESH_ID)

    def ring(self, colour, direction):
        device = (self.core, chip_at(self.place, DIM_ORDER[colour][TWO], ONE - TWO * direction))
        i = 11 * colour + THREE * direction
        got = self.near.at[colour, direction]
        near = [self.remote(i + n, self.planes.at[colour, pl.ds(TWO * half, TWO)], got.at[pl.ds(TWO * half, TWO)], device) for n, half in enumerate((direction, ONE - direction))]
        return near + [self.remote(i + TWO, got.at[pl.ds(TWO * direction, TWO)], self.far.at[colour, direction], device)]

    def shares(self, colour):
        last = DIM_ORDER[colour][TWO]
        rows = pl.ds(pl.multiple_of((self.core * COLOURS + colour) * self.band, self.band), self.band)
        views = [(self.planes.at[colour], ZERO, None)]
        views += [(self.near.at[colour, direction], TWO * direction - ONE, None) for direction in range(TWO)]
        views += [(self.far.at[colour, direction], TWO, direction) for direction in range(TWO)]
        out = []
        for n, (src, shift, half) in enumerate(views):
            where = [slice(None)] * THREE
            where[last] = lax.rem(self.place[last] + shift + SIDE, SIDE)
            if half is not None:
                where[min(d for d in range(THREE) if d != last)] = pl.ds(TWO * half, TWO)
            dst = self.out.at[tuple(where) + (rows, slice(None))]
            out.append((self.remote(11 * colour + 6 + n, src, dst, (ONE - self.core, self.chip)), pltpu.make_async_copy(src, dst, self.load_sem.at[5 * colour + n])))
        return out

    def share(self, colour, which):
        for n in which:
            give, keep = self.shares(colour)[n]
            give.start()
            keep.start()

    def begin(self):
        for colour in range(COLOURS):
            for direction in range(TWO):
                for copy in self.ring(colour, direction)[:TWO]:
                    copy.start()
        for colour in range(COLOURS):
            self.share(colour, (ZERO,))

    def pass_on(self):
        for colour in range(COLOURS):
            for direction in range(TWO):
                first, _, far = self.ring(colour, direction)
                first.wait_recv()
                far.start()

    def share_near(self):
        for colour in range(COLOURS):
            for direction in range(TWO):
                self.ring(colour, direction)[ONE].wait_recv()
            self.share(colour, (ONE, TWO))

    def complete(self):
        for colour in range(COLOURS):
            for direction in range(TWO):
                self.ring(colour, direction)[TWO].wait_recv()
            self.share(colour, (THREE, 4))

    def end(self):
        for colour in range(COLOURS):
            for give, keep in self.shares(colour):
                give.wait_recv()
                give.wait_send()
                keep.wait()
            for direction in range(TWO):
                for copy in self.ring(colour, direction):
                    copy.wait_send()


def dot(lhs, rhs, contract=((ONE,), (ZERO,))):
    return lax.dot_general(lhs, rhs, (contract, ((), ())), preferred_element_type=F32)


def dot_nt(lhs, rhs):
    return dot(lhs, rhs, ((ONE,), (ONE,)))


def dot_tn(lhs, rhs):
    return dot(lhs, rhs, ((ZERO,), (ZERO,)))


def norm_rows(resid, gain, shift):
    mean = jnp.mean(resid, axis=-ONE, keepdims=True)
    centred = resid - mean
    inv_std = lax.rsqrt(jnp.mean(centred * centred, axis=-ONE, keepdims=True) + LN_EPS)
    normed = centred * inv_std
    return (normed * gain + shift).astype(BF16), normed, inv_std


def norm_rows_bwd(d_out, normed, inv_std, gain):
    d_norm = d_out * gain
    return inv_std * (d_norm - jnp.mean(d_norm, axis=-ONE, keepdims=True) - normed * jnp.mean(d_norm * normed, axis=-ONE, keepdims=True))


def col_sum(values):
    return jnp.sum(values, axis=ZERO, keepdims=True)


def lane_row(head, dtype=BF16):
    lane = lax.broadcasted_iota(jnp.int32, (ONE, PAIR), ONE)
    return jnp.where((lane >= HEAD_DIM * head) & (lane < HEAD_DIM * (head + ONE)), 1.0, 0.0).astype(dtype)


def spare_lane(head):
    lane = lax.broadcasted_iota(jnp.int32, (ONE, PAIR), ONE)
    return jnp.where(lane == HEAD_DIM * (ONE - head), 1.0, 0.0)


def mask_fill(n_rows, n_valid):
    row = lax.broadcasted_iota(jnp.int32, (n_rows, PAIR), ZERO)
    return jnp.where(row >= n_valid, MASK_FILL, 0.0)


def head_masks(pair_q, pair_k, head, fill):
    q_f = pair_q * lane_row(head) + spare_lane(head).astype(BF16)
    k_f = pair_k * lane_row(head) + (fill * spare_lane(head)).astype(BF16)
    return q_f, k_f


def half_only(pair, head):
    return pair * lane_row(head)


def join_halves(first, second):
    lane = lax.broadcasted_iota(jnp.int32, first.shape, ONE)
    return jnp.where(lane < HEAD_DIM, first, second)


def score_blocks(n_heads, n_q, n_k, causal, step):
    if not causal:
        return [(head, ZERO, n_q, n_k) for head in range(n_heads)]
    return [(head, first, step, first + step) for head in range(n_heads) for first in range(ZERO, n_q, step)]


def scores_t(q_f, k_f, causal, first):
    s_t = dot_nt(k_f, q_f)
    if causal:
        key_i = lax.broadcasted_iota(jnp.int32, s_t.shape, ZERO)
        qry_i = lax.broadcasted_iota(jnp.int32, s_t.shape, ONE) + first
        s_t = jnp.where(key_i <= qry_i, s_t, MASK_FILL)
    return s_t


def pair_of(group, head):
    return group[:, head // TWO * PAIR:(head // TWO + ONE) * PAIR]


def masked_pairs(q_g, k_g, n_valid):
    fill = mask_fill(k_g.shape[ZERO], n_valid)
    cache = {}

    def get(head):
        if head not in cache:
            cache[head] = head_masks(pair_of(q_g, head), pair_of(k_g, head), head % TWO, fill)
        return cache[head]

    return get


def stack_heads(parts, n_heads):
    return jnp.concatenate([jnp.concatenate(parts[head], axis=ONE) for head in range(n_heads)], axis=ZERO)


def run_ahead(blocks, produce, transform, consume, delay):
    ahead = produce(blocks[ZERO])
    waiting = []
    for i, block in enumerate(blocks):
        now = ahead
        if i + ONE < len(blocks):
            ahead = produce(blocks[i + ONE])
        waiting.append((block, transform(block, now)))
        if len(waiting) > delay:
            consume(*waiting.pop(ZERO))
    for item in waiting:
        consume(*item)


def attend_group(q_g, k_g, v_g, n_valid, causal, lse_ref):
    n_heads = GROUP // HEAD_DIM
    o_parts = [[] for _ in range(n_heads)]
    v_t = v_g.T
    masked = masked_pairs(q_g, k_g, n_valid)

    def produce(block):
        head, first, n_q, n_k = block
        q_f, k_f = masked(head)
        return scores_t(q_f[first:first + n_q], k_f[:n_k], causal, first)

    def transform(block, s_t):
        head, first, n_q, n_k = block
        top = jnp.max(s_t, axis=ZERO, keepdims=True)
        e_t = jnp.exp(s_t - top)
        total = jnp.sum(e_t, axis=ZERO, keepdims=True)
        lse_ref[ZERO, ZERO, head // TWO, head % TWO:head % TWO + ONE, first:first + n_q] = top + jnp.log(total)
        return (e_t * (1.0 / total)).astype(BF16)

    def consume(block, p_t):
        head, first, n_q, n_k = block
        o_parts[head].append(dot(v_t[HEAD_DIM * head:HEAD_DIM * (head + ONE), :n_k], p_t))

    run_ahead(score_blocks(n_heads, q_g.shape[ZERO], k_g.shape[ZERO], causal, 128), produce, transform, consume, TWO)
    return stack_heads(o_parts, n_heads).T.astype(BF16)


def attend_group_bwd(d_o, q_g, k_g, v_g, n_valid, causal, lse_ref):
    n_heads = q_g.shape[ONE] // HEAD_DIM
    k_t = k_g.T
    dq_t, dk_h, dv_h = [[] for _ in range(n_heads)], [None] * n_heads, [None] * n_heads
    masked = masked_pairs(q_g, k_g, n_valid)
    v_half = {}

    def produce(block):
        head, first, n_q, n_k = block
        q_f, k_f = masked(head)
        if head not in v_half:
            v_half[head] = half_only(pair_of(v_g, head), head % TWO)
        rows = slice(first, first + n_q)
        return scores_t(q_f[rows], k_f[:n_k], causal, first), dot_nt(v_half[head][:n_k], pair_of(d_o, head)[rows])

    def transform(block, products):
        head, first, n_q, n_k = block
        s_t, dp_t = products
        p_t = jnp.exp(s_t - lse_ref[head // TWO, head % TWO:head % TWO + ONE, first:first + n_q])
        weighted = p_t * dp_t
        return p_t.astype(BF16), (weighted - p_t * jnp.sum(weighted, axis=ZERO, keepdims=True)).astype(BF16)

    def grow(old, new):
        if old is None:
            return new
        n_old = old.shape[ZERO]
        return old + new if n_old == new.shape[ZERO] else jnp.concatenate([old + new[:n_old], new[n_old:]], axis=ZERO)

    def consume(block, operands):
        head, first, n_q, n_k = block
        p_b, ds_t = operands
        rows = slice(first, first + n_q)
        dv_h[head] = grow(dv_h[head], dot(p_b, pair_of(d_o, head)[rows]))
        dk_h[head] = grow(dk_h[head], dot(ds_t, pair_of(q_g, head)[rows]))
        dq_t[head].append(dot(k_t[HEAD_DIM * head:HEAD_DIM * (head + ONE), :n_k], ds_t))

    run_ahead(score_blocks(n_heads, q_g.shape[ZERO], k_g.shape[ZERO], causal, 256), produce, transform, consume, ZERO)
    join = lambda parts: jnp.concatenate([join_halves(parts[h], parts[h + ONE]) for h in range(ZERO, n_heads, TWO)], axis=ONE)
    return stack_heads(dq_t, n_heads).T * 0.125, join(dk_h), join(dv_h)


def attn_fwd_kernel(causal, slots, guest, lens_ref, x_ref, kv_ref, wq_ref, wk_ref, wv_ref, w_all, bias_ref, rows_ref,
                    q_ref, k_ref, v_ref, o_ref, lse_ref, h_ref, normed_ref, inv_ref, o_all, wo_v, load_sem):
    q_row, k_row, v_row, o_row, gain_row, o_mat = slots
    sample, group = pl.program_id(ZERO), pl.program_id(ONE)
    d_model = wo_v.shape[ZERO]
    fetch = pltpu.make_async_copy(w_all.at[pl.ds(o_mat * d_model, d_model), :], wo_v, load_sem)

    @pl.when((sample == ZERO) & (group == ZERO))
    def _():
        fetch.start()

    turn = sample * pl.num_programs(ONE) + group
    if guest is not None:
        for where, steps in ((ZERO, (lambda: meet_neighbours(guest.place), guest.begin)), (TWO, (guest.pass_on,)), (THREE, (guest.share_near,)), (4, (guest.complete,))):
            @pl.when(turn == where)
            def _():
                for step in steps:
                    step()

    x_b, kv_b = x_ref[ALL], kv_ref[ALL]
    q_g = ((dot(x_b, wq_ref[ALL]) + bias_ref[q_row:q_row + ONE, :]) * 0.125).astype(BF16)
    k_g = (dot(kv_b, wk_ref[ALL]) + bias_ref[k_row:k_row + ONE, :]).astype(BF16)
    v_g = (dot(kv_b, wv_ref[ALL]) + bias_ref[v_row:v_row + ONE, :]).astype(BF16)
    q_ref[ALL], k_ref[ALL], v_ref[ALL] = q_g, k_g, v_g
    o_g = attend_group(q_g, k_g, v_g, lens_ref[sample], causal, lse_ref)
    o_ref[ALL] = o_g
    o_all[:, pl.ds(pl.multiple_of(group * GROUP, GROUP), GROUP)] = o_g

    @pl.when((sample == ZERO) & (group == pl.num_programs(ONE) - ONE))
    def _():
        fetch.wait()

    @pl.when(group == pl.num_programs(ONE) - ONE)
    def _():
        resid = x_ref[ALL].astype(F32) + dot(o_all[ALL], wo_v[ALL]) + rows_ref[o_row:o_row + ONE, :]
        h_out, normed, inv_std = norm_rows(resid, rows_ref[gain_row:gain_row + ONE, :], rows_ref[gain_row + ONE:gain_row + TWO, :])
        h_ref[ALL], normed_ref[ALL], inv_ref[ALL] = h_out, normed, inv_std

    if guest is not None:
        @pl.when(turn == pl.num_programs(ZERO) * pl.num_programs(ONE) - ONE)
        def _():
            guest.end()


def attn_forward(x, kv, lens, attn_full, bias_rows, mats, slots, causal, planes=None, full_rows=None):
    d_model = x.shape[-ONE]
    n_batch = lens.shape[ZERO]
    n_q, n_k = x.shape[ZERO] // n_batch, kv.shape[ZERO] // n_batch
    n_groups = d_model // GROUP
    col = lambda mat: pl.BlockSpec((d_model, GROUP), lambda b, g: (mat, g))
    q_blk = pl.BlockSpec((n_q, GROUP), lambda b, g: (b, g))
    k_blk = pl.BlockSpec((n_k, GROUP), lambda b, g: (b, g))
    tok = lambda n: pl.BlockSpec((n, d_model), lambda b, g: (b, ZERO))
    n_heads_g = GROUP // HEAD_DIM
    out_shape = (
        jax.ShapeDtypeStruct(x.shape, BF16), jax.ShapeDtypeStruct(kv.shape, BF16), jax.ShapeDtypeStruct(kv.shape, BF16),
        jax.ShapeDtypeStruct(x.shape, BF16), jax.ShapeDtypeStruct((n_batch, n_groups, n_heads_g // TWO, TWO, n_q), F32),
        jax.ShapeDtypeStruct(x.shape, BF16), jax.ShapeDtypeStruct(x.shape, F32), jax.ShapeDtypeStruct((x.shape[ZERO], ONE), F32))
    kernel = functools.partial(attn_fwd_kernel, causal, slots + (mats[THREE],))
    in_specs = [pl.BlockSpec(memory_space=pltpu.SMEM), tok(n_q), tok(n_k), col(mats[ZERO]), col(mats[ONE]), col(mats[TWO]), pl.BlockSpec(memory_space=pl.ANY),
                pl.BlockSpec((bias_rows.shape[ZERO], GROUP), lambda b, g: (ZERO, g)), pl.BlockSpec(bias_rows.shape, lambda b, g: (ZERO, ZERO))]
    out_specs = [q_blk, k_blk, k_blk, q_blk, pl.BlockSpec((ONE, ONE, n_heads_g // TWO, TWO, n_q), lambda b, g: (b, g, ZERO, ZERO, ZERO)),
                 tok(n_q), tok(n_q), pl.BlockSpec((n_q, ONE), lambda b, g: (b, ZERO))]
    scratch = [pltpu.VMEM((n_q, d_model), BF16), pltpu.VMEM((d_model, d_model), BF16), pltpu.SemaphoreType.DMA]
    args = [lens, x, kv, attn_full, attn_full, attn_full, attn_full, bias_rows, bias_rows]
    params = dict(vmem_limit_bytes=VMEM_BYTES, dimension_semantics=('arbitrary', 'arbitrary'))
    if planes is None:
        body = functools.partial(kernel, None)
    else:
        n_in, n_out, n_own = len(args), len(out_specs), len(scratch)

        def body(*refs):
            ins, held, outs, whole, rest = refs[:n_in], refs[n_in], refs[n_in + ONE:n_in + ONE + n_out], refs[n_in + ONE + n_out], refs[n_in + TWO + n_out:]
            kernel(LastPhase(held, whole, *rest[n_own:]), *ins, *outs, *rest[:n_own])

        in_specs.append(pl.BlockSpec(memory_space=pltpu.VMEM))
        args.append(planes)
        out_specs.append(pl.BlockSpec(memory_space=pl.ANY))
        out_shape += (jax.ShapeDtypeStruct((SIDE, SIDE, SIDE, full_rows // SIDE ** THREE, d_model), BF16),)
        scratch += LastPhase.scratch_shapes(planes)
        params |= dict(collective_id=5, has_side_effects=True)
    return pl.pallas_call(
        body, grid=(n_batch, n_groups), in_specs=in_specs, out_specs=out_specs, out_shape=out_shape, scratch_shapes=scratch,
        compiler_params=pltpu.CompilerParams(**params),
        cost_estimate=pl.CostEstimate(flops=TWO * d_model * d_model * (TWO * x.shape[ZERO] + TWO * kv.shape[ZERO]) + 16 * x.shape[ZERO] * n_k * d_model, bytes_accessed=20 * x.shape[ZERO] * d_model, transcendentals=ZERO),
        name='attn_fwd',
    )(*args)


def attn_bwd_kernel(causal, gain_row, mats, guest, lens_ref, dres_ref, wo_ref, w_all, q_ref, k_ref, v_ref, lse_ref,
                    rows_ref, normed_ref, inv_ref, lhs_refs, rows_out, dres_out, sums_ref, tail_ref, grads_ref,
                    rhs_q, rhs_k, lhs_q, lhs_k, do_v, w_v, grad_v, load_sem, store_sem):
    sample, group = pl.program_id(ZERO), pl.program_id(ONE)
    d_model = wo_ref.shape[ONE]
    n_q, n_k = q_ref.shape[ZERO], k_ref.shape[ZERO]
    last = pl.num_programs(ONE) - ONE
    fetches = [] if causal else [pltpu.make_async_copy(w_all.at[pl.ds(mats[ZERO] * d_model, d_model), :], w_v, load_sem.at[ZERO])]
    hand_on = pltpu.make_async_copy(rhs_q.at[pl.ds(ZERO, THREE)] if causal else rhs_k, rows_out, load_sem.at[ONE])
    dk_all, dv_all = (rhs_q.at[ONE], rhs_q.at[TWO]) if causal else (rhs_k.at[ZERO], rhs_k.at[ONE])
    d_all, dres_all = rhs_q.at[ZERO], rhs_q.at[THREE if causal else ONE]
    places = (lhs_q.at[ZERO], lhs_q.at[ONE]) if causal else (lhs_q.at[ZERO], lhs_k, lhs_q.at[ZERO])
    lhs_fetch = lambda i: pltpu.make_async_copy(lhs_refs[i], places[i], load_sem.at[THREE + i])
    store = lambda buf, mat: pltpu.make_async_copy(grad_v.at[buf], grads_ref.at[pl.ds(pl.multiple_of(mat * d_model, d_model), d_model), :], store_sem.at[buf])

    @pl.when((sample == ZERO) & (group == ZERO))
    def _():
        for fetch in fetches + [lhs_fetch(ZERO), lhs_fetch(ONE)]:
            fetch.start()

    turn = sample * pl.num_programs(ONE) + group
    q_rows = pl.ds(pl.multiple_of(sample * n_q, n_q), n_q)
    k_rows = pl.ds(pl.multiple_of(sample * n_k, n_k), n_k)
    d_o = dot_nt(dres_ref[ALL].astype(BF16), wo_ref[ALL]).astype(BF16)

    def keep(found, first, width):
        here = pl.ds(first, width)
        cols = pl.ds(pl.multiple_of(group * GROUP + first, PAIR), width)
        for i, (full, rows, value) in enumerate(zip((d_all, dk_all, dv_all), (q_rows, k_rows, k_rows), found)):
            sums_ref[ZERO, i:i + ONE, here] = col_sum(value)
            full[rows, cols] = value.astype(BF16)

    if causal:
        keep(attend_group_bwd(d_o, q_ref[ALL], k_ref[ALL], v_ref[ALL], lens_ref[sample], causal, lse_ref.at[ZERO, ZERO]), ZERO, GROUP)
    else:
        do_v[ALL] = d_o

        def one_pair(pair, _):
            guest(ZERO, TWO * turn + pair)
            first = pl.multiple_of(pair * PAIR, PAIR)
            here = pl.ds(first, PAIR)
            keep(attend_group_bwd(do_v[:, here], q_ref[:, here], k_ref[:, here], v_ref[:, here], lens_ref[sample], causal, lse_ref.at[ZERO, ZERO, pl.ds(pair, ONE)]), first, PAIR)
            return ZERO

        lax.fori_loop(ZERO, GROUP // PAIR, one_pair, ZERO)

    @pl.when(group == ZERO)
    def _():
        dres_all[q_rows, :] = dres_ref[ALL].astype(BF16)

    guest(THREE, turn)
    if causal:
        tail_ref[ALL] = jnp.zeros_like(tail_ref)
    else:
        @pl.when((sample == ZERO) & (group == last))
        def _():
            for fetch in fetches:
                fetch.wait()

        @pl.when(group == last)
        def _():
            d_h = dres_ref[ALL] + dot_nt(d_all[q_rows, :], w_v[ALL])
            normed = normed_ref[ALL]
            d_resid = norm_rows_bwd(d_h, normed, inv_ref[ALL], rows_ref[gain_row:gain_row + ONE, :])
            dres_out[ALL] = d_resid
            tail_ref[ZERO, ZERO:ONE, :] = col_sum(d_resid)
            tail_ref[ZERO, ONE:TWO, :] = col_sum(d_h * normed)
            tail_ref[ZERO, TWO:THREE, :] = col_sum(d_h)

    @pl.when(turn == pl.num_programs(ZERO) * pl.num_programs(ONE) - ONE)
    def _():
        hand_on.start()
        guest(TWO, 12)
        lhs_fetch(ZERO).wait()
        if causal:
            lhs_fetch(ONE).wait()

            def square(i, _):
                @pl.when(i >= TWO)
                def _():
                    store(i % TWO, mats[ZERO]).wait()

                grad_v[i % TWO] = dot_tn(lhs_q[i // THREE], rhs_q[i])
                store(i % TWO, mats[ZERO] + i).start()
                return ZERO

            lax.fori_loop(ZERO, 4, square, ZERO)
        else:
            def square_q(i, _):
                @pl.when(i == ONE)
                def _():
                    lhs_fetch(TWO).start()
                    lhs_fetch(TWO).wait()

                grad_v[i] = dot_tn(lhs_q[ZERO], rhs_q[i])
                store(i, mats[ZERO] + THREE * i).start()
                return ZERO

            def square_k(i, _):
                store(i, mats[ONE]).wait()
                grad_v[i] = dot_tn(lhs_k[ALL], rhs_k[i])
                store(i, mats[ONE] + i).start()
                return ZERO

            lax.fori_loop(ZERO, TWO, square_q, ZERO)
            guest(TWO, 13)
            lhs_fetch(ONE).wait()
            lax.fori_loop(ZERO, TWO, square_k, ZERO)
            guest(TWO, 14)
        for buf in range(TWO):
            store(buf, mats[ZERO]).wait()
        hand_on.wait()


def scatter_guest(scatter, plan, parity, position):
    steps = dict(end=scatter.end) | {('relay', p): functools.partial(scatter.relay, p) for p in range(THREE)}
    steps |= {('settle', p): functools.partial(scatter.settle, p) for p in range(THREE)} | {turn: functools.partial(scatter.absorb, turn) for turn in range(SIDE)}
    if parity == TWO:
        for name in plan.get(position, ()):
            steps[name]()
        return
    if parity == THREE:
        @pl.when(position == 5)
        def _():
            for name in plan['late']:
                steps[name]()
        return
    if parity == ZERO:
        @pl.when(position == ZERO)
        def _():
            meet_neighbours(scatter.place)
            scatter.begin()
    for where, names in plan.items():
        if where != 'late' and where < 12:
            @pl.when(position == where)
            def _():
                for name in names:
                    steps[name]()


def no_guest(parity, position):
    pass


def attn_backward(dres, q, k, v, lse, lens, attn_full, bias_rows, mats, causal, lhs_list, g_rows=None, scale=None, gain_row=ZERO, normed=None, inv_std=None, grads=None):
    d_model = q.shape[-ONE]
    n_batch = lens.shape[ZERO]
    n_q, n_k = q.shape[ZERO] // n_batch, k.shape[ZERO] // n_batch
    n_groups = d_model // GROUP
    row = lambda mat: pl.BlockSpec((GROUP, d_model), lambda b, g: (mat * n_groups + g, ZERO))
    q_blk = pl.BlockSpec((n_q, GROUP), lambda b, g: (b, g))
    k_blk = pl.BlockSpec((n_k, GROUP), lambda b, g: (b, g))
    tok = lambda n: pl.BlockSpec((n, d_model), lambda b, g: (b, ZERO))
    n_heads_g = GROUP // HEAD_DIM
    anywhere = pl.BlockSpec(memory_space=pl.ANY)
    in_specs = [pl.BlockSpec(memory_space=pltpu.SMEM), tok(n_q), row(mats[THREE]), anywhere, q_blk, k_blk, k_blk,
                pl.BlockSpec((ONE, ONE, n_heads_g // TWO, TWO, n_q), lambda b, g: (b, g, ZERO, ZERO, ZERO)), pl.BlockSpec(bias_rows.shape, lambda b, g: (ZERO, ZERO))]
    args = [lens, dres, attn_full, attn_full, q, k, v, lse, bias_rows]
    tail_shape = jax.ShapeDtypeStruct((n_batch, 8, d_model), F32)
    out_shape = [jax.ShapeDtypeStruct((THREE,) + q.shape if causal else (TWO,) + k.shape, BF16)]
    out_specs = [anywhere]
    if not causal:
        late = dict(pipeline_mode=pl.Buffered(ONE))
        in_specs += [pl.BlockSpec((n_q, d_model), lambda b, g: (b, ZERO), **late), pl.BlockSpec((n_q, ONE), lambda b, g: (b, ZERO), **late)]
        args += [normed, inv_std]
        out_shape.append(jax.ShapeDtypeStruct(q.shape, F32))
        out_specs.append(tok(n_q))
    n_lhs_at = len(args)
    args += list(lhs_list)
    in_specs += [anywhere] * len(lhs_list)
    out_shape += [tail_shape, tail_shape, jax.ShapeDtypeStruct(attn_full.shape, F32)]
    out_specs += [pl.BlockSpec((ONE, 8, GROUP), lambda b, g: (b, ZERO, g)), pl.BlockSpec((ONE, 8, d_model), lambda b, g: (b, ZERO, ZERO)), anywhere]
    held = lambda count, n: pltpu.VMEM((count, n_batch * n, d_model), BF16)
    own = [held(4, n_q), held(TWO, n_q)] if causal else [held(TWO, n_q), held(TWO, n_k), held(ONE, n_q), pltpu.VMEM((n_batch * n_k, d_model), BF16)]
    own += [] if causal else [pltpu.VMEM((n_q, GROUP), BF16)]
    own += [] if causal else [pltpu.VMEM((d_model, d_model), BF16)]
    own += [pltpu.VMEM((TWO, d_model, d_model), F32), pltpu.SemaphoreType.DMA((6,)), pltpu.SemaphoreType.DMA((TWO,))]
    kernel = functools.partial(attn_bwd_kernel, causal, gain_row, mats)
    params = dict(vmem_limit_bytes=VMEM_BYTES, dimension_semantics=('arbitrary', 'arbitrary'))
    aliases = {}
    if causal:
        args.append(grads)
        in_specs.append(anywhere)
        aliases = {len(args) - ONE: len(out_shape) - ONE}
    else:
        args.append(as_torus(g_rows))
        in_specs.append(anywhere)
        n_rows = args[-ONE].shape[THREE]
        out_shape.append(jax.ShapeDtypeStruct((n_rows, d_model), F32))
        out_specs.append(anywhere)
        params |= dict(collective_id=THREE, has_side_effects=True, vmem_limit_bytes=67043328)
    scratch = own + ([] if causal else Scatter.scratch_shapes([n_rows]))
    n_in, n_out, n_own = len(args), len(out_shape), len(own)

    def body(*refs):
        ins, outs, rest = refs[:n_in], refs[n_in:n_in + n_out], refs[n_in + n_out:]
        lhs_refs, mine = ins[n_lhs_at:-ONE], rest[:n_own]
        if causal:
            rows_out, sums, tail, grads_ref = outs
            kernel(no_guest, *ins[:n_lhs_at], None, None, lhs_refs, rows_out, None, sums, tail, grads_ref, mine[ZERO], None, mine[ONE], None, None, None, *mine[TWO:])
        else:
            rows_out, dres_out, sums, tail, grads_ref, total = outs
            scatter = Scatter(scale, [(ins[-ONE], ZERO, n_rows)], [total], rest[n_own:])
            kernel(functools.partial(scatter_guest, scatter, CROSS_PLAN), *ins[:n_lhs_at], lhs_refs, rows_out, dres_out, sums, tail, grads_ref, *mine)

    return pl.pallas_call(
        body, grid=(n_batch, n_groups), in_specs=in_specs, out_specs=out_specs, out_shape=out_shape, scratch_shapes=scratch, input_output_aliases=aliases,
        compiler_params=pltpu.CompilerParams(**params),
        cost_estimate=pl.CostEstimate(flops=TWO * d_model * d_model * (TWO * q.shape[ZERO] + TWO * k.shape[ZERO]) + 40 * q.shape[ZERO] * n_k * d_model, bytes_accessed=20 * q.shape[ZERO] * d_model, transcendentals=ZERO),
        name='attn_bwd',
    )(*args)


def ffn_kernel(n_blocks, h_ref, dy_ref, up_ref, down_ref, rows_ref, bias_ref, normed_ref, inv_ref,
               y_ref, grad_ref, dres2_ref, tail_ref, upsum_ref, left_all, right_all):
    step = pl.program_id(ZERO)
    block, d_model = h_ref.shape
    n_square = left_all.shape[TWO] // d_model

    @pl.when(step < n_blocks)
    def _():
        rows = pl.ds(pl.multiple_of(step * block, block), block)
        h_b = h_ref[ALL]
        right_all[ZERO, rows, :] = h_b
        up = dot_nt(h_b, up_ref[ALL]) + bias_ref[ALL]
        cdf = 0.5 * (1.0 + lax.erf(up * 0.7071067811865476))
        gelu = (up * cdf).astype(BF16)
        slope = cdf + up * (0.3989422804014327 * jnp.exp(-0.5 * up * up))
        left_all[ONE, rows, :] = gelu
        resid = h_b.astype(F32) + dot(gelu, down_ref[ALL]) + rows_ref[8:9, :]
        y_b, normed3, inv3 = norm_rows(resid, rows_ref[13:14, :], rows_ref[14:15, :])
        y_ref[ALL] = y_b
        dy = dy_ref[ALL].astype(F32)
        d_res3 = norm_rows_bwd(dy, normed3, inv3, rows_ref[13:14, :])
        d_res3_b = d_res3.astype(BF16)
        right_all[ONE, rows, :] = d_res3_b
        d_up = dot_nt(d_res3_b, down_ref[ALL]) * slope
        d_up_b = d_up.astype(BF16)
        left_all[ZERO, rows, :] = d_up_b
        d_h2 = d_res3 + dot(d_up_b, up_ref[ALL])
        normed2 = normed_ref[ALL]
        d_res2 = norm_rows_bwd(d_h2, normed2, inv_ref[ALL], rows_ref[11:12, :])
        dres2_ref[ALL] = d_res2
        tail = jnp.concatenate([col_sum(d_res2), col_sum(d_res3), col_sum(d_h2 * normed2), col_sum(d_h2), col_sum(dy * normed3), col_sum(dy),
                                jnp.zeros((TWO, dy.shape[ONE]), F32)], axis=ZERO)
        up_sum = col_sum(d_up)

        @pl.when(step == ZERO)
        def _():
            tail_ref[ALL] = tail
            upsum_ref[ALL] = up_sum

        @pl.when(step > ZERO)
        def _():
            tail_ref[ALL] += tail
            upsum_ref[ALL] += up_sum

    square = step - n_blocks
    cols = pl.ds(pl.multiple_of(lax.rem(square + TWO * n_square, n_square) * d_model, d_model), d_model)

    @pl.when(square >= ZERO)
    def _():
        which = square // n_square
        grad_ref[ALL] = dot_tn(left_all[which, :, cols], right_all[which])


def ffn_both(h2, dy, ffn_full, bias_rows, up_bias, normed2, inv2, block=256):
    n_tok, d_model = h2.shape
    ffn_dim = ffn_full.shape[ZERO] // TWO
    n_blocks = n_tok // block
    n_steps = n_blocks + ffn_full.shape[ZERO] // d_model
    at = lambda i: jnp.minimum(i, n_blocks - ONE)
    tok = pl.BlockSpec((block, d_model), lambda i: (at(i), ZERO))
    once = lambda shape, idx: pl.BlockSpec(shape, lambda i: idx, pipeline_mode=pl.Buffered(ONE))
    return pl.pallas_call(
        functools.partial(ffn_kernel, n_blocks), grid=(n_steps,),
        in_specs=[tok, tok, once((ffn_dim, d_model), (ZERO, ZERO)), once((ffn_dim, d_model), (ONE, ZERO)), once(bias_rows.shape, (ZERO, ZERO)), once((ONE, ffn_dim), (ZERO, ZERO)),
                  tok, pl.BlockSpec((block, ONE), lambda i: (at(i), ZERO))],
        out_specs=[tok, pl.BlockSpec((d_model, d_model), lambda i: (jnp.maximum(i - n_blocks, ZERO), ZERO)), tok, pl.BlockSpec((8, d_model), lambda i: (ZERO, ZERO)), pl.BlockSpec((ONE, ffn_dim), lambda i: (ZERO, ZERO))],
        out_shape=[jax.ShapeDtypeStruct(h2.shape, BF16), jax.ShapeDtypeStruct(ffn_full.shape, F32), jax.ShapeDtypeStruct(h2.shape, F32),
                   jax.ShapeDtypeStruct((8, d_model), F32), jax.ShapeDtypeStruct((ONE, ffn_dim), F32)],
        scratch_shapes=[pltpu.VMEM((TWO, n_tok, ffn_dim), BF16), pltpu.VMEM((TWO, n_tok, d_model), BF16)],
        compiler_params=pltpu.CompilerParams(vmem_limit_bytes=VMEM_BYTES, dimension_semantics=('arbitrary',)),
        cost_estimate=pl.CostEstimate(flops=12 * n_tok * d_model * ffn_dim, bytes_accessed=30 * n_tok * d_model, transcendentals=ZERO),
        name='ffn_both',
    )(h2, dy, ffn_full, ffn_full, bias_rows, up_bias, normed2, inv2)


CROSS_PLAN = {ONE: (ZERO,), TWO: (ONE,), THREE: (TWO,), 4: (THREE,), 5: (('relay', ZERO),), 9: (('settle', ZERO),), 10: (('relay', ONE),), 'late': (('settle', ONE),), 12: (('relay', TWO),), 13: (('settle', TWO),), 14: ('end',)}


def solution(mesh):
    n_fsdp = mesh.shape['fsdp']
    n_dp = mesh.shape['dp']
    batch_axes = ('dp', 'fsdp')
    act_spec = P(batch_axes, None, None)
    len_spec = P(batch_axes)
    row_spec = P('fsdp', None)
    vec_spec = P('fsdp')

    def device_step(dec_in, enc_out, src_lens, tgt_lens, y_cot, attn_w, ffn_w, vec_params):
        d_model, n_vec = dec_in.shape[TWO], vec_params.shape[ZERO]
        scale = 1.0 / (dec_in.shape[ZERO] * dec_in.shape[ONE] * n_fsdp * n_dp)
        x, enc, dy = (a.reshape(-ONE, d_model) for a in (dec_in, enc_out, y_cot))
        vec_rows = jnp.pad(vec_params.astype(F32), (ZERO, 16 * LANES - n_vec)).reshape(16, LANES)
        attn_tiles, planes, vec_tiles = gather_params(attn_w, ffn_w, vec_rows)
        attn_full = attn_tiles.reshape(-ONE, d_model)
        vec_f = vec_tiles.reshape(n_fsdp, 16, LANES)[:, :TWO].reshape(n_fsdp, TWO * LANES)[:, :n_vec].reshape(-ONE)
        bias_rows = jnp.pad(vec_f[:15 * d_model].reshape(15, d_model), ((ZERO, ONE), (ZERO, ZERO)))
        up_bias = vec_f[15 * d_model:].reshape(ONE, -ONE)
        q1, k1, v1, o1, lse1, h1, normed1, inv1 = attn_forward(x, x, tgt_lens, attn_full, bias_rows, (ZERO, ONE, TWO, THREE), (ZERO, ONE, TWO, THREE, 9), True)
        q2, k2, v2, o2, lse2, h2, normed2, inv2, ffn_tiles = attn_forward(h1, enc, src_lens, attn_full, bias_rows, (4, 5, 6, 7), (4, 5, 6, 7, 11), False, planes, ffn_w.shape[ZERO] * n_fsdp)
        ffn_full = ffn_tiles.reshape(-ONE, d_model)
        y, g_ffn, d_res2, ffn_tail, up_sum = ffn_both(h2, dy, ffn_full, bias_rows, up_bias, normed2, inv2)
        d_cross, d_res1, sums2, tail2, grads, ffn_out = attn_backward(d_res2, q2, k2, v2, lse2, src_lens, attn_full, bias_rows, (4, 5, 6, 7), False, (h1, enc, o2), g_ffn, scale, 9, normed1, inv1)
        d_self, sums1, _, grads = attn_backward(d_res1, q1, k1, v1, lse1, tgt_lens, attn_full, bias_rows, (ZERO, ONE, TWO, THREE), True, (x, o1), grads=grads)
        s1, s2, t2 = jnp.sum(sums1, axis=ZERO), jnp.sum(sums2, axis=ZERO), jnp.sum(tail2, axis=ZERO)
        g_vec = jnp.concatenate([s1[ZERO:THREE].reshape(-ONE), t2[ZERO], s2[ZERO:THREE].reshape(-ONE), ffn_tail[ZERO], ffn_tail[ONE], t2[ONE], t2[TWO], ffn_tail[TWO], ffn_tail[THREE], ffn_tail[4], ffn_tail[5], up_sum[ZERO]])
        g_rows = jnp.pad(g_vec.reshape(n_fsdp, ONE, n_vec), ((ZERO, ZERO), (ZERO, 7), (ZERO, TWO * LANES - n_vec))).reshape(n_fsdp * 8, -ONE)
        attn_out, vec_out, d_x, d_enc = scatter_grads(grads, g_rows, scale, attn_full, (ZERO, ONE, TWO, 5, 6), d_res1, d_self, d_cross)
        return y.reshape(dec_in.shape), d_x.reshape(dec_in.shape), d_enc.reshape(enc_out.shape), attn_out, ffn_out, vec_out[ZERO, :n_vec]

    return jax.shard_map(device_step, mesh=mesh, in_specs=(act_spec, act_spec, len_spec, len_spec, act_spec, row_spec, row_spec, vec_spec), out_specs=(act_spec, act_spec, act_spec, row_spec, row_spec, vec_spec), check_vma=False)
```

```python
import functools
import jax
import jax.numpy as jnp
from jax import lax
from jax.experimental import pallas as pl
from jax.experimental.pallas import tpu as pltpu
from jax.sharding import PartitionSpec as P

ZERO, ONE, TWO, THREE = range(4)
ALL = ...
HEAD_DIM = 64
LN_EPS = 1e-5
MASK_FILL = -1e30
VMEM_BYTES = 60 * 1024 * 1024
F32 = jnp.float32
BF16 = jnp.bfloat16
GROUP = 256
PAIR = 128


SIDE = 4
LANES = 128
COLOURS = THREE
STAGES = TWO
DIM_ORDER = ((TWO, ONE, ZERO), (ONE, ZERO, TWO), (ZERO, TWO, ONE))
MESH_ID = pl.DeviceIdType.MESH


def torus_place():
    chip = lax.axis_index('fsdp')
    return (chip // (SIDE * SIDE), lax.rem(chip // SIDE, SIDE), lax.rem(chip, SIDE))


def chip_at(place, dim, shift):
    moved = [lax.rem(p + shift + SIDE, SIDE) if d == dim else p for d, p in enumerate(place)]
    return (moved[ZERO] * SIDE + moved[ONE]) * SIDE + moved[TWO]


def meet_neighbours(place):
    barrier = pltpu.get_barrier_semaphore()
    core = lax.axis_index('dp')
    for dim in range(THREE):
        for shift in (ONE, -ONE):
            pl.semaphore_signal(barrier, inc=ONE, device_id=(core, chip_at(place, dim, shift)), device_id_type=MESH_ID)
    pl.semaphore_signal(barrier, inc=ONE, device_id=(ONE - core, lax.axis_index('fsdp')), device_id_type=MESH_ID)
    pl.semaphore_wait(barrier, 7)


class Scatter:
    def __init__(self, scale, sources, outs, scratch):
        self.scale, self.outs = scale, outs
        self.sources = [(ref, pl.ds(first, n)) for ref, first, n in sources]
        (self.acc, g1, d1, g2, d2, g3, d3, self.send_sem, self.recv_sem, self.load_sem, self.stage) = scratch
        self.got, self.far = (g1, g2, g3), (d1, d2, d3)
        self.heights = [n for _, _, n in sources]
        self.offsets = [sum(self.heights[:i]) for i in range(len(sources))]
        self.n_low = self.heights[ZERO] // TWO
        self.core, self.chip, self.place = lax.axis_index('dp'), lax.axis_index('fsdp'), torus_place()
        self.pieces = [(d, colour) for d in (TWO, ONE, THREE, ZERO) for colour in range(COLOURS)]

    @staticmethod
    def scratch_shapes(heights):
        h = sum(heights)
        n_low = heights[ZERO] // TWO
        buf = lambda *shape: pltpu.VMEM((COLOURS,) + shape + (LANES,), F32)
        n = Scatter.n_copies(len(heights))
        return [buf(SIDE, SIDE, SIDE, h), buf(TWO, SIDE, SIDE, h), buf(TWO, TWO, SIDE, h), buf(TWO, SIDE, h), buf(TWO, TWO, h), buf(TWO, h), buf(TWO, max(n_low, h - n_low)),
                pltpu.SemaphoreType.DMA((n,)), pltpu.SemaphoreType.DMA((n,)), pltpu.SemaphoreType.DMA((THREE + COLOURS, len(heights))),
                pltpu.VMEM((STAGES, SIDE, SIDE, h, LANES), F32)]

    @staticmethod
    def n_copies(n_parts):
        return 12 * n_parts + COLOURS * 18 + COLOURS * n_parts

    def parts(self, colour):
        return range(len(self.sources) if colour == ZERO else ONE)

    def height(self, colour):
        return sum(self.heights[i] for i in self.parts(colour))

    def remote(self, i, src, dst, device):
        return pltpu.make_async_remote_copy(src_ref=src, dst_ref=dst, send_sem=self.send_sem.at[i], recv_sem=self.recv_sem.at[i], device_id=device, device_id_type=MESH_ID)

    def columns(self, of_core, colour, part=ZERO):
        return pl.ds(pl.multiple_of((of_core * COLOURS + colour if part == ZERO else of_core) * LANES, LANES), LANES)

    def slot(self, d, colour):
        dim = DIM_ORDER[colour][ZERO]
        where = [slice(None)] * THREE
        where[dim] = lax.rem(self.place[dim] + d, SIDE)
        return tuple(where)

    def rows_of(self, part):
        return pl.ds(self.offsets[part], self.heights[part])

    def swaps(self, piece):
        d, colour = self.pieces[piece]
        where = self.slot(d, colour)
        n = len(self.sources)
        return [self.remote(piece * n + i, self.sources[i][ZERO].at[where + (self.sources[i][ONE], self.columns(ONE - self.core, colour, i))],
                            self.acc.at[(colour,) + where + (self.rows_of(i), slice(None))], (ONE - self.core, self.chip)) for i in self.parts(colour)]

    def loads(self, piece):
        d, colour = self.pieces[piece]
        where, buf = self.slot(d, colour), piece % STAGES
        return [pltpu.make_async_copy(self.sources[i][ZERO].at[where + (self.sources[i][ONE], self.columns(self.core, colour, i))],
                                      self.stage.at[buf, :, :, self.rows_of(i), :], self.load_sem.at[buf, i]) for i in self.parts(colour)]

    def split_rows(self, colour, half):
        return pl.ds(ZERO, self.n_low) if half == ZERO else pl.ds(self.n_low, self.height(colour) - self.n_low)

    def block(self, colour, phase, d, half=None):
        order = DIM_ORDER[colour]
        where = [None, None, None]
        for done in order[:phase]:
            where[done] = self.place[done]
        where[order[phase]] = lax.rem(self.place[order[phase]] + d, SIDE)
        for i, rest in enumerate(sorted(order[phase + ONE:])):
            where[rest] = slice(None) if half is None or i > ZERO else pl.ds(TWO * half, TWO)
        rows = self.split_rows(colour, half) if phase == TWO and half is not None else pl.ds(ZERO, self.height(colour))
        return self.acc.at[(colour,) + tuple(where) + (rows, slice(None))]

    def got_half(self, colour, phase, direction, half):
        if phase == TWO:
            return self.got[phase].at[colour, direction, self.split_rows(colour, half), :]
        return self.got_all(colour, phase, direction, pl.ds(TWO * half, TWO))

    def got_all(self, colour, phase, direction, which=slice(None)):
        rows = (pl.ds(ZERO, self.height(colour)), slice(None))
        blocks = ((which, slice(None)), (which,), ())[phase]
        return self.got[phase].at[(colour, direction) + blocks + rows]

    def far_part(self, colour, phase, direction):
        if phase == TWO:
            return self.far[phase].at[colour, direction, pl.ds(ZERO, self.n_low if direction == ZERO else self.height(colour) - self.n_low), :]
        return self.far[phase].at[(colour, direction) + (slice(None),) * (TWO - phase) + (pl.ds(ZERO, self.height(colour)), slice(None))]

    def ring(self, colour, phase, direction):
        shift = ONE - TWO * direction
        device = (self.core, chip_at(self.place, DIM_ORDER[colour][phase], shift))
        i = 12 * len(self.sources) + ((colour * THREE + phase) * TWO + direction) * THREE
        near = shift % SIDE
        return (self.remote(i, self.block(colour, phase, TWO, direction), self.far_part(colour, phase, direction), device),
                self.remote(i + ONE, self.block(colour, phase, near, ONE - direction), self.got_half(colour, phase, direction, ONE - direction), device),
                self.remote(i + TWO, self.block(colour, phase, near, direction), self.got_half(colour, phase, direction, direction), device))

    def gives(self, colour):
        n = len(self.sources)
        base = 12 * n + COLOURS * 18 + colour * n
        done = self.acc.at[colour, self.place[ZERO], self.place[ONE], self.place[TWO]]
        pairs = [(done.at[self.rows_of(i), :], self.outs[i].at[:, self.columns(self.core, colour, i)]) for i in self.parts(colour)]
        return [(self.remote(base + i, src, dst, (ONE - self.core, self.chip)), pltpu.make_async_copy(src, dst, self.load_sem.at[THREE + colour, i])) for i, (src, dst) in enumerate(pairs)]

    def add_into(self, dst, sources, n_lead):
        def body(i, _):
            total = dst[i]
            for src in sources:
                total = total + src[i]
            dst[i] = total
            return ZERO

        if n_lead == TWO:
            lax.fori_loop(ZERO, dst.shape[ZERO], body, ZERO)
        else:
            total = dst[ALL]
            for src in sources:
                total = total + src[ALL]
            dst[ALL] = total


    def begin(self):
        for piece in range(STAGES):
            for copy in self.loads(piece):
                copy.start()
        for piece in range(len(self.pieces)):
            for copy in self.swaps(piece):
                copy.start()

    def absorb(self, turn):
        for piece in range(turn * COLOURS, (turn + ONE) * COLOURS):
            d, colour = self.pieces[piece]
            for copy in self.loads(piece):
                copy.wait()
            for copy in self.swaps(piece):
                copy.wait_recv()
            rows = (pl.ds(ZERO, self.height(colour)), slice(None))
            self.add_into(self.acc.at[(colour,) + self.slot(d, colour) + rows], [self.stage.at[(piece % STAGES, slice(None), slice(None)) + rows]], TWO)
            if piece + STAGES < len(self.pieces):
                for copy in self.loads(piece + STAGES):
                    copy.start()
            if turn == ZERO:
                for direction in range(TWO):
                    self.ring(colour, ZERO, direction)[ZERO].start()
            elif turn < THREE:
                self.ring(colour, ZERO, turn - ONE)[ONE].start()

    def relay(self, phase):
        for colour in range(COLOURS):
            for direction in range(TWO):
                far, _, fed = self.ring(colour, phase, direction)
                far.wait_recv()
                self.add_into(self.block(colour, phase, (ONE - TWO * direction) % SIDE, direction), [self.far_part(colour, phase, direction)], TWO - phase)
            for direction in range(TWO):
                self.ring(colour, phase, direction)[TWO].start()

    def settle(self, phase):
        for colour in range(COLOURS):
            for direction in range(TWO):
                _, own, fed = self.ring(colour, phase, direction)
                own.wait_recv()
                fed.wait_recv()
            self.add_into(self.block(colour, phase, ZERO), [self.got_all(colour, phase, direction) for direction in range(TWO)], TWO - phase)
            if phase < TWO:
                for kind in range(TWO):
                    for direction in range(TWO):
                        self.ring(colour, phase + ONE, direction)[kind].start()
            else:
                done = self.block(colour, TWO, ZERO)
                done[ALL] = done[ALL] * self.scale
                for give, keep in self.gives(colour):
                    keep.start()
                    give.start()

    def end(self):
        for colour in range(COLOURS):
            for give, keep in self.gives(colour):
                give.wait_recv()
                give.wait_send()
                keep.wait()
        for piece in range(len(self.pieces)):
            for copy in self.swaps(piece):
                copy.wait_send()
        for colour in range(COLOURS):
            for phase in range(THREE):
                for direction in range(TWO):
                    for copy in self.ring(colour, phase, direction):
                        copy.wait_send()


def rs_kernel(scale, mats, g_ref, vec_ref, w_all, dres_ref, self_ref, cross_ref, out_ref, vec_out, dx_out, denc_out,
              w_v, dres_v, self_v, cross_v, dx_v, denc_v, load_sem, *scratch):
    scatter = Scatter(scale, [(ref, ZERO, ref.shape[THREE]) for ref in (g_ref, vec_ref)], [out_ref, vec_out], scratch)
    d_model = w_v.shape[ONE]
    step = 256
    loads = [pltpu.make_async_copy(w_all.at[pl.ds(mat * d_model, d_model), :], w_v.at[i], load_sem.at[i]) for i, mat in enumerate(mats)]
    loads += [pltpu.make_async_copy(src, dst, load_sem.at[len(mats) + i]) for i, (src, dst) in enumerate(((dres_ref, dres_v), (self_ref, self_v), (cross_ref, cross_v)))]
    stores = [pltpu.make_async_copy(src, dst, load_sem.at[len(mats) + THREE + i]) for i, (src, dst) in enumerate(((dx_v, dx_out), (denc_v, denc_out)))]

    def input_grads():
        for copy in loads:
            copy.wait()

        def decoder(i, _):
            rows = pl.ds(pl.multiple_of(i * step, step), step)
            total = dres_v[rows, :]
            for n in range(THREE):
                total = total + dot_nt(self_v[n, rows, :], w_v[n])
            dx_v[rows, :] = total.astype(BF16)
            return ZERO

        def encoder(i, _):
            rows = pl.ds(pl.multiple_of(i * step, step), step)
            denc_v[rows, :] = (dot_nt(cross_v[ZERO, rows, :], w_v[THREE]) + dot_nt(cross_v[ONE, rows, :], w_v[4])).astype(BF16)
            return ZERO

        lax.fori_loop(ZERO, dx_v.shape[ZERO] // step, decoder, ZERO)
        stores[ZERO].start()
        lax.fori_loop(ZERO, denc_v.shape[ZERO] // step, encoder, ZERO)
        stores[ONE].start()

    meet_neighbours(scatter.place)
    scatter.begin()
    for copy in loads:
        copy.start()
    for turn in range(THREE):
        scatter.absorb(turn)
    scatter.relay(ZERO)
    scatter.absorb(THREE)
    input_grads()
    scatter.settle(ZERO)
    for phase in (ONE, TWO):
        scatter.relay(phase)
        scatter.settle(phase)
    scatter.end()
    for copy in stores:
        copy.wait()


def as_torus(rows):
    return rows.reshape(SIDE, SIDE, SIDE, rows.shape[ZERO] // SIDE ** THREE, rows.shape[ONE])


def scatter_grads(g_attn, g_vec, scale, attn_full, mats, d_res, d_self, d_cross):
    sources = [as_torus(g_attn), as_torus(g_vec)]
    heights = [src.shape[THREE] for src in sources]
    d_model = g_attn.shape[ONE]
    anywhere = pl.BlockSpec(memory_space=pl.ANY)
    dx_shape, denc_shape = d_self.shape[ONE:], d_cross.shape[ONE:]
    return pl.pallas_call(
        functools.partial(rs_kernel, scale, mats),
        in_specs=[anywhere] * 6, out_specs=[anywhere] * 4,
        out_shape=[jax.ShapeDtypeStruct((h, src.shape[4]), F32) for h, src in zip(heights, sources)] + [jax.ShapeDtypeStruct(dx_shape, BF16), jax.ShapeDtypeStruct(denc_shape, BF16)],
        scratch_shapes=[pltpu.VMEM((len(mats), d_model, d_model), BF16), pltpu.VMEM(d_res.shape, F32), pltpu.VMEM(d_self.shape, BF16), pltpu.VMEM(d_cross.shape, BF16),
                        pltpu.VMEM(dx_shape, BF16), pltpu.VMEM(denc_shape, BF16), pltpu.SemaphoreType.DMA((len(mats) + 5,))] + Scatter.scratch_shapes(heights),
        compiler_params=pltpu.CompilerParams(collective_id=ONE, has_side_effects=True, vmem_limit_bytes=VMEM_BYTES),
        cost_estimate=pl.CostEstimate(flops=10 ** 9, bytes_accessed=8 * d_model * g_attn.shape[ZERO], transcendentals=ZERO),
        name='scatter_grads',
    )(*sources, attn_full, d_res, d_self, d_cross)


class Gather:
    def __init__(self, send_sem, recv_sem, base=ZERO):
        self.send_sem, self.recv_sem = send_sem, recv_sem
        self.used = base
        self.core, self.chip, self.place = lax.axis_index('dp'), lax.axis_index('fsdp'), torus_place()
        self.sibling = (ONE - self.core, self.chip)
        self.started = []

    def remote(self, src, dst, device):
        i = self.used
        self.used += ONE
        return pltpu.make_async_remote_copy(src_ref=src, dst_ref=dst, send_sem=self.send_sem.at[i], recv_sem=self.recv_sem.at[i], device_id=device, device_id_type=MESH_ID)

    def start(self, copy):
        copy.start()
        self.started.append(copy)

    def ring(self, colour, phase, view, own=None, split=False):
        order = DIM_ORDER[colour]
        dim = order[phase]
        have = sorted(order[:phase])

        def index(shift, half=None):
            where = [self.place[ZERO], self.place[ONE], self.place[TWO]]
            where[dim] = lax.rem(self.place[dim] + shift + SIDE, SIDE)
            for i, h in enumerate(have):
                where[h] = slice(None) if half is None or i > ZERO else pl.ds(TWO * half, TWO)
            return tuple(where)

        out = []
        for direction, shift in enumerate((ONE, -ONE)):
            device = (self.core, chip_at(self.place, dim, shift))
            half = direction if phase == ZERO else None
            near_dst = view(index(ZERO), None)
            if split:
                near = [self.remote(view(index(ZERO, h), None), view(index(ZERO, h), None), device) for h in (direction, ONE - direction)]
            else:
                near = [self.remote(near_dst if own is None else own, near_dst, device)]
            out.append(dict(
                near=near,
                far=self.remote(view(index(-shift, direction), half), view(index(-shift, direction), half), device),
                near_at=index(-shift), far_at=index(TWO, direction)))
        return out


def ag_kernel(attn_ref, ffn_ref, vec_ref, oattn_ref, planes_ref, vec_out, attn_v, send_sem, recv_sem, load_sem):
    net = Gather(send_sem, recv_sem)
    core, place = net.core, net.place
    rows, width = attn_ref.shape
    band = rows // (TWO * COLOURS)
    vec_high = vec_ref.shape[ZERO]
    stores, finals = [], []

    def band_rows(colour):
        return pl.ds(pl.multiple_of((core * COLOURS + colour) * band, band), band)

    def columns(half):
        return slice(None) if half is None else pl.ds(half * (width // TWO), width // TWO)

    def attn_view(colour):
        return lambda where, half: attn_v.at[where + (band_rows(colour), columns(half))]

    def ffn_view(colour):
        last = DIM_ORDER[colour][TWO]
        return lambda where, half: planes_ref.at[(colour,) + tuple(w for d, w in enumerate(where) if d != last) + (slice(None), columns(half))]

    def vec_view(where, half):
        return vec_out.at[where + (slice(None) if half is None else pl.ds(half * (vec_high // TWO), vec_high // TWO), slice(None))]

    colours = range(COLOURS)
    attn_own = [attn_ref.at[band_rows(colour), :] for colour in colours]
    ffn_own = [ffn_ref.at[band_rows(colour), :] for colour in colours]
    rings = {('attn', phase): [net.ring(colour, phase, attn_view(colour), attn_own[colour] if phase == ZERO else None, phase > ZERO) for colour in colours] for phase in range(THREE)}
    rings |= {('ffn', phase): [net.ring(colour, phase, ffn_view(colour), ffn_own[colour] if phase == ZERO else None, phase > ZERO) for colour in colours] for phase in range(TWO)}
    rings |= {('vec', phase): [net.ring(ONE, phase, vec_view, vec_ref if phase == ZERO else None)] for phase in range(THREE)}

    def publish(at):
        keep = pltpu.make_async_copy(attn_v.at[at], oattn_ref.at[at], load_sem.at[len(stores)])
        keep.start()
        stores.append(keep)
        give = net.remote(attn_v.at[at], oattn_ref.at[at], net.sibling)
        net.start(give)
        finals.append(give)

    def send_near(name, phase):
        for ring in rings.get((name, phase), ()):
            for way in ring:
                for copy in way['near']:
                    net.start(copy)

    def pass_on(name, phase):
        for ring in rings.get((name, phase), ()):
            for way in ring:
                way['near'][ZERO].wait_recv()
                net.start(way['far'])
        if phase == TWO and name == 'attn':
            for colour in colours:
                for way in rings[(name, phase)][colour]:
                    way['near'][ONE].wait_recv()
                    publish(way['near_at'] + (band_rows(colour), slice(None)))

    def complete(name, phase):
        for colour, ring in enumerate(rings.get((name, phase), ())):
            for way in ring:
                way['far'].wait_recv()
                if phase == ONE and name != 'vec':
                    way['near'][ONE].wait_recv()
            if phase < TWO and (name, phase + ONE) in rings:
                for way in rings[(name, phase + ONE)][colour]:
                    for copy in way['near']:
                        net.start(copy)
            if phase == TWO and name == 'attn':
                for way in ring:
                    publish(way['far_at'] + (band_rows(colour), slice(None)))
        if phase == ONE and name == 'attn':
            for colour in colours:
                last = DIM_ORDER[colour][TWO]
                publish(tuple(place[d] if d == last else slice(None) for d in range(THREE)) + (band_rows(colour), slice(None)))

    for colour in colours:
        attn_v[(place[ZERO], place[ONE], place[TWO]) + (band_rows(colour), slice(None))] = attn_ref[band_rows(colour), :]
        kept = [place[d] for d in range(THREE) if d != DIM_ORDER[colour][TWO]]
        planes_ref[(colour, kept[ZERO], kept[ONE])] = ffn_ref[band_rows(colour), :]
    vec_out[place[ZERO], place[ONE], place[TWO]] = vec_ref[ALL]
    meet_neighbours(place)
    names = ('attn', 'vec', 'ffn')
    for name in names:
        send_near(name, ZERO)
    for phase in range(THREE):
        for name in names:
            pass_on(name, phase)
        for name in names:
            complete(name, phase)
    for copy in finals:
        copy.wait_recv()
    for copy in net.started:
        copy.wait_send()
    for copy in stores:
        copy.wait()


def gather_params(attn_w, ffn_w, vec_rows):
    rows, width = attn_w.shape
    full = (SIDE, SIDE, SIDE, rows, width)
    n_copies = COLOURS * (4 * TWO + 6 * THREE) + 4 * THREE + COLOURS * 5
    vmem = pl.BlockSpec(memory_space=pltpu.VMEM)
    return pl.pallas_call(
        ag_kernel,
        in_specs=[vmem] * THREE, out_specs=[pl.BlockSpec(memory_space=pl.ANY), vmem, vmem],
        out_shape=[jax.ShapeDtypeStruct(full, BF16), jax.ShapeDtypeStruct((COLOURS, SIDE, SIDE, rows // (TWO * COLOURS), width), BF16),
                   jax.ShapeDtypeStruct((SIDE, SIDE, SIDE) + vec_rows.shape, F32)],
        scratch_shapes=[pltpu.VMEM(full, BF16), pltpu.SemaphoreType.DMA((n_copies,)), pltpu.SemaphoreType.DMA((n_copies,)), pltpu.SemaphoreType.DMA((COLOURS * 5,))],
        compiler_params=pltpu.CompilerParams(collective_id=TWO, has_side_effects=True, vmem_limit_bytes=VMEM_BYTES),
        cost_estimate=pl.CostEstimate(flops=10 ** 9, bytes_accessed=4 * rows * width * SIDE ** THREE, transcendentals=ZERO),
        name='gather_params',
    )(attn_w, ffn_w, vec_rows)


class LastPhase:
    def __init__(self, planes, out, near, far, send_sem, recv_sem, load_sem):
        self.planes, self.out, self.near, self.far = planes, out, near, far
        self.send_sem, self.recv_sem, self.load_sem = send_sem, recv_sem, load_sem
        self.core, self.chip, self.place = lax.axis_index('dp'), lax.axis_index('fsdp'), torus_place()
        self.band = planes.shape[THREE]

    @staticmethod
    def scratch_shapes(planes):
        colours, side, _, band, width = planes.shape
        sems = [pltpu.SemaphoreType.DMA((11 * COLOURS,)), pltpu.SemaphoreType.DMA((11 * COLOURS,)), pltpu.SemaphoreType.DMA((5 * COLOURS,))]
        return [pltpu.VMEM((colours, TWO, side, side, band, width), BF16), pltpu.VMEM((colours, TWO, side // TWO, side, band, width), BF16)] + sems

    def remote(self, i, src, dst, device):
        return pltpu.make_async_remote_copy(src_ref=src, dst_ref=dst, send_sem=self.send_sem.at[i], recv_sem=self.recv_sem.at[i], device_id=device, device_id_type=MESH_ID)

    def ring(self, colour, direction):
        device = (self.core, chip_at(self.place, DIM_ORDER[colour][TWO], ONE - TWO * direction))
        i = 11 * colour + THREE * direction
        got = self.near.at[colour, direction]
        near = [self.remote(i + n, self.planes.at[colour, pl.ds(TWO * half, TWO)], got.at[pl.ds(TWO * half, TWO)], device) for n, half in enumerate((direction, ONE - direction))]
        return near + [self.remote(i + TWO, got.at[pl.ds(TWO * direction, TWO)], self.far.at[colour, direction], device)]

    def shares(self, colour):
        last = DIM_ORDER[colour][TWO]
        rows = pl.ds(pl.multiple_of((self.core * COLOURS + colour) * self.band, self.band), self.band)
        views = [(self.planes.at[colour], ZERO, None)]
        views += [(self.near.at[colour, direction], TWO * direction - ONE, None) for direction in range(TWO)]
        views += [(self.far.at[colour, direction], TWO, direction) for direction in range(TWO)]
        out = []
        for n, (src, shift, half) in enumerate(views):
            where = [slice(None)] * THREE
            where[last] = lax.rem(self.place[last] + shift + SIDE, SIDE)
            if half is not None:
                where[min(d for d in range(THREE) if d != last)] = pl.ds(TWO * half, TWO)
            dst = self.out.at[tuple(where) + (rows, slice(None))]
            out.append((self.remote(11 * colour + 6 + n, src, dst, (ONE - self.core, self.chip)), pltpu.make_async_copy(src, dst, self.load_sem.at[5 * colour + n])))
        return out

    def share(self, colour, which):
        for n in which:
            give, keep = self.shares(colour)[n]
            give.start()
            keep.start()

    def begin(self):
        for colour in range(COLOURS):
            for direction in range(TWO):
                for copy in self.ring(colour, direction)[:TWO]:
                    copy.start()
        for colour in range(COLOURS):
            self.share(colour, (ZERO,))

    def pass_on(self):
        for colour in range(COLOURS):
            for direction in range(TWO):
                first, _, far = self.ring(colour, direction)
                first.wait_recv()
                far.start()
        for colour in range(COLOURS):
            for direction in range(TWO):
                self.ring(colour, direction)[ONE].wait_recv()
            self.share(colour, (ONE, TWO))

    def complete(self):
        for colour in range(COLOURS):
            for direction in range(TWO):
                self.ring(colour, direction)[TWO].wait_recv()
            self.share(colour, (THREE, 4))

    def end(self):
        for colour in range(COLOURS):
            for give, keep in self.shares(colour):
                give.wait_recv()
                give.wait_send()
                keep.wait()
            for direction in range(TWO):
                for copy in self.ring(colour, direction):
                    copy.wait_send()


def dot(lhs, rhs, contract=((ONE,), (ZERO,))):
    return lax.dot_general(lhs, rhs, (contract, ((), ())), preferred_element_type=F32)


def dot_nt(lhs, rhs):
    return dot(lhs, rhs, ((ONE,), (ONE,)))


def dot_tn(lhs, rhs):
    return dot(lhs, rhs, ((ZERO,), (ZERO,)))


def norm_rows(resid, gain, shift):
    mean = jnp.mean(resid, axis=-ONE, keepdims=True)
    centred = resid - mean
    inv_std = lax.rsqrt(jnp.mean(centred * centred, axis=-ONE, keepdims=True) + LN_EPS)
    normed = centred * inv_std
    return (normed * gain + shift).astype(BF16), normed, inv_std


def norm_rows_bwd(d_out, normed, inv_std, gain):
    d_norm = d_out * gain
    return inv_std * (d_norm - jnp.mean(d_norm, axis=-ONE, keepdims=True) - normed * jnp.mean(d_norm * normed, axis=-ONE, keepdims=True))


def col_sum(values):
    return jnp.sum(values, axis=ZERO, keepdims=True)


def lane_row(head, dtype=BF16):
    lane = lax.broadcasted_iota(jnp.int32, (ONE, PAIR), ONE)
    return jnp.where((lane >= HEAD_DIM * head) & (lane < HEAD_DIM * (head + ONE)), 1.0, 0.0).astype(dtype)


def spare_lane(head):
    lane = lax.broadcasted_iota(jnp.int32, (ONE, PAIR), ONE)
    return jnp.where(lane == HEAD_DIM * (ONE - head), 1.0, 0.0)


def mask_fill(n_rows, n_valid):
    row = lax.broadcasted_iota(jnp.int32, (n_rows, PAIR), ZERO)
    return jnp.where(row >= n_valid, MASK_FILL, 0.0)


def head_masks(pair_q, pair_k, head, fill):
    q_f = pair_q * lane_row(head) + spare_lane(head).astype(BF16)
    k_f = pair_k * lane_row(head) + (fill * spare_lane(head)).astype(BF16)
    return q_f, k_f


def half_only(pair, head):
    return pair * lane_row(head)


def join_halves(first, second):
    lane = lax.broadcasted_iota(jnp.int32, first.shape, ONE)
    return jnp.where(lane < HEAD_DIM, first, second)


def score_blocks(n_heads, n_q, n_k, causal, step):
    if not causal:
        return [(head, ZERO, n_q, n_k) for head in range(n_heads)]
    return [(head, first, step, first + step) for head in range(n_heads) for first in range(ZERO, n_q, step)]


def scores_t(q_f, k_f, causal, first):
    s_t = dot_nt(k_f, q_f)
    if causal:
        key_i = lax.broadcasted_iota(jnp.int32, s_t.shape, ZERO)
        qry_i = lax.broadcasted_iota(jnp.int32, s_t.shape, ONE) + first
        s_t = jnp.where(key_i <= qry_i, s_t, MASK_FILL)
    return s_t


def pair_of(group, head):
    return group[:, head // TWO * PAIR:(head // TWO + ONE) * PAIR]


def masked_pairs(q_g, k_g, n_valid):
    fill = mask_fill(k_g.shape[ZERO], n_valid)
    cache = {}

    def get(head):
        if head not in cache:
            cache[head] = head_masks(pair_of(q_g, head), pair_of(k_g, head), head % TWO, fill)
        return cache[head]

    return get


def stack_heads(parts, n_heads):
    return jnp.concatenate([jnp.concatenate(parts[head], axis=ONE) for head in range(n_heads)], axis=ZERO)


def run_ahead(blocks, produce, transform, consume, delay):
    ahead = produce(blocks[ZERO])
    waiting = []
    for i, block in enumerate(blocks):
        now = ahead
        if i + ONE < len(blocks):
            ahead = produce(blocks[i + ONE])
        waiting.append((block, transform(block, now)))
        if len(waiting) > delay:
            consume(*waiting.pop(ZERO))
    for item in waiting:
        consume(*item)


def attend_group(q_g, k_g, v_g, n_valid, causal, lse_ref):
    n_heads = GROUP // HEAD_DIM
    o_parts = [[] for _ in range(n_heads)]
    v_t = v_g.T
    masked = masked_pairs(q_g, k_g, n_valid)

    def produce(block):
        head, first, n_q, n_k = block
        q_f, k_f = masked(head)
        return scores_t(q_f[first:first + n_q], k_f[:n_k], causal, first)

    def transform(block, s_t):
        head, first, n_q, n_k = block
        top = jnp.max(s_t, axis=ZERO, keepdims=True)
        e_t = jnp.exp(s_t - top)
        total = jnp.sum(e_t, axis=ZERO, keepdims=True)
        lse_ref[ZERO, ZERO, head // TWO, head % TWO:head % TWO + ONE, first:first + n_q] = top + jnp.log(total)
        return (e_t * (1.0 / total)).astype(BF16)

    def consume(block, p_t):
        head, first, n_q, n_k = block
        o_parts[head].append(dot(v_t[HEAD_DIM * head:HEAD_DIM * (head + ONE), :n_k], p_t))

    run_ahead(score_blocks(n_heads, q_g.shape[ZERO], k_g.shape[ZERO], causal, 128), produce, transform, consume, TWO)
    return stack_heads(o_parts, n_heads).T.astype(BF16)


def attend_group_bwd(d_o, q_g, k_g, v_g, n_valid, causal, lse_ref):
    n_heads = q_g.shape[ONE] // HEAD_DIM
    k_t = k_g.T
    dq_t, dk_h, dv_h = [[] for _ in range(n_heads)], [None] * n_heads, [None] * n_heads
    masked = masked_pairs(q_g, k_g, n_valid)
    v_half = {}

    def produce(block):
        head, first, n_q, n_k = block
        q_f, k_f = masked(head)
        if head not in v_half:
            v_half[head] = half_only(pair_of(v_g, head), head % TWO)
        rows = slice(first, first + n_q)
        return scores_t(q_f[rows], k_f[:n_k], causal, first), dot_nt(v_half[head][:n_k], pair_of(d_o, head)[rows])

    def transform(block, products):
        head, first, n_q, n_k = block
        s_t, dp_t = products
        p_t = jnp.exp(s_t - lse_ref[head // TWO, head % TWO:head % TWO + ONE, first:first + n_q])
        weighted = p_t * dp_t
        return p_t.astype(BF16), (weighted - p_t * jnp.sum(weighted, axis=ZERO, keepdims=True)).astype(BF16)

    def grow(old, new):
        if old is None:
            return new
        n_old = old.shape[ZERO]
        return old + new if n_old == new.shape[ZERO] else jnp.concatenate([old + new[:n_old], new[n_old:]], axis=ZERO)

    def consume(block, operands):
        head, first, n_q, n_k = block
        p_b, ds_t = operands
        rows = slice(first, first + n_q)
        dv_h[head] = grow(dv_h[head], dot(p_b, pair_of(d_o, head)[rows]))
        dk_h[head] = grow(dk_h[head], dot(ds_t, pair_of(q_g, head)[rows]))
        dq_t[head].append(dot(k_t[HEAD_DIM * head:HEAD_DIM * (head + ONE), :n_k], ds_t))

    run_ahead(score_blocks(n_heads, q_g.shape[ZERO], k_g.shape[ZERO], causal, 256), produce, transform, consume, ZERO)
    join = lambda parts: jnp.concatenate([join_halves(parts[h], parts[h + ONE]) for h in range(ZERO, n_heads, TWO)], axis=ONE)
    return stack_heads(dq_t, n_heads).T * 0.125, join(dk_h), join(dv_h)


def attn_fwd_kernel(causal, slots, guest, lens_ref, x_ref, kv_ref, wq_ref, wk_ref, wv_ref, w_all, bias_ref, rows_ref,
                    q_ref, k_ref, v_ref, o_ref, lse_ref, h_ref, normed_ref, inv_ref, o_all, wo_v, load_sem):
    q_row, k_row, v_row, o_row, gain_row, o_mat = slots
    sample, group = pl.program_id(ZERO), pl.program_id(ONE)
    d_model = wo_v.shape[ZERO]
    fetch = pltpu.make_async_copy(w_all.at[pl.ds(o_mat * d_model, d_model), :], wo_v, load_sem)

    @pl.when((sample == ZERO) & (group == ZERO))
    def _():
        fetch.start()

    turn = sample * pl.num_programs(ONE) + group
    if guest is not None:
        for where, steps in ((ZERO, (lambda: meet_neighbours(guest.place), guest.begin)), (THREE, (guest.pass_on,)), (5, (guest.complete,))):
            @pl.when(turn == where)
            def _():
                for step in steps:
                    step()

    x_b, kv_b = x_ref[ALL], kv_ref[ALL]
    q_g = ((dot(x_b, wq_ref[ALL]) + bias_ref[q_row:q_row + ONE, :]) * 0.125).astype(BF16)
    k_g = (dot(kv_b, wk_ref[ALL]) + bias_ref[k_row:k_row + ONE, :]).astype(BF16)
    v_g = (dot(kv_b, wv_ref[ALL]) + bias_ref[v_row:v_row + ONE, :]).astype(BF16)
    q_ref[ALL], k_ref[ALL], v_ref[ALL] = q_g, k_g, v_g
    o_g = attend_group(q_g, k_g, v_g, lens_ref[sample], causal, lse_ref)
    o_ref[ALL] = o_g
    o_all[:, pl.ds(pl.multiple_of(group * GROUP, GROUP), GROUP)] = o_g

    @pl.when((sample == ZERO) & (group == pl.num_programs(ONE) - ONE))
    def _():
        fetch.wait()

    @pl.when(group == pl.num_programs(ONE) - ONE)
    def _():
        resid = x_ref[ALL].astype(F32) + dot(o_all[ALL], wo_v[ALL]) + rows_ref[o_row:o_row + ONE, :]
        h_out, normed, inv_std = norm_rows(resid, rows_ref[gain_row:gain_row + ONE, :], rows_ref[gain_row + ONE:gain_row + TWO, :])
        h_ref[ALL], normed_ref[ALL], inv_ref[ALL] = h_out, normed, inv_std

    if guest is not None:
        @pl.when(turn == pl.num_programs(ZERO) * pl.num_programs(ONE) - ONE)
        def _():
            guest.end()


def attn_forward(x, kv, lens, attn_full, bias_rows, mats, slots, causal, planes=None, full_rows=None):
    d_model = x.shape[-ONE]
    n_batch = lens.shape[ZERO]
    n_q, n_k = x.shape[ZERO] // n_batch, kv.shape[ZERO] // n_batch
    n_groups = d_model // GROUP
    col = lambda mat: pl.BlockSpec((d_model, GROUP), lambda b, g: (mat, g))
    q_blk = pl.BlockSpec((n_q, GROUP), lambda b, g: (b, g))
    k_blk = pl.BlockSpec((n_k, GROUP), lambda b, g: (b, g))
    tok = lambda n: pl.BlockSpec((n, d_model), lambda b, g: (b, ZERO))
    n_heads_g = GROUP // HEAD_DIM
    out_shape = (
        jax.ShapeDtypeStruct(x.shape, BF16), jax.ShapeDtypeStruct(kv.shape, BF16), jax.ShapeDtypeStruct(kv.shape, BF16),
        jax.ShapeDtypeStruct(x.shape, BF16), jax.ShapeDtypeStruct((n_batch, n_groups, n_heads_g // TWO, TWO, n_q), F32),
        jax.ShapeDtypeStruct(x.shape, BF16), jax.ShapeDtypeStruct(x.shape, F32), jax.ShapeDtypeStruct((x.shape[ZERO], ONE), F32))
    kernel = functools.partial(attn_fwd_kernel, causal, slots + (mats[THREE],))
    in_specs = [pl.BlockSpec(memory_space=pltpu.SMEM), tok(n_q), tok(n_k), col(mats[ZERO]), col(mats[ONE]), col(mats[TWO]), pl.BlockSpec(memory_space=pl.ANY),
                pl.BlockSpec((bias_rows.shape[ZERO], GROUP), lambda b, g: (ZERO, g)), pl.BlockSpec(bias_rows.shape, lambda b, g: (ZERO, ZERO))]
    out_specs = [q_blk, k_blk, k_blk, q_blk, pl.BlockSpec((ONE, ONE, n_heads_g // TWO, TWO, n_q), lambda b, g: (b, g, ZERO, ZERO, ZERO)),
                 tok(n_q), tok(n_q), pl.BlockSpec((n_q, ONE), lambda b, g: (b, ZERO))]
    scratch = [pltpu.VMEM((n_q, d_model), BF16), pltpu.VMEM((d_model, d_model), BF16), pltpu.SemaphoreType.DMA]
    args = [lens, x, kv, attn_full, attn_full, attn_full, attn_full, bias_rows, bias_rows]
    params = dict(vmem_limit_bytes=VMEM_BYTES, dimension_semantics=('arbitrary', 'arbitrary'))
    if planes is None:
        body = functools.partial(kernel, None)
    else:
        n_in, n_out, n_own = len(args), len(out_specs), len(scratch)

        def body(*refs):
            ins, held, outs, whole, rest = refs[:n_in], refs[n_in], refs[n_in + ONE:n_in + ONE + n_out], refs[n_in + ONE + n_out], refs[n_in + TWO + n_out:]
            kernel(LastPhase(held, whole, *rest[n_own:]), *ins, *outs, *rest[:n_own])

        in_specs.append(pl.BlockSpec(memory_space=pltpu.VMEM))
        args.append(planes)
        out_specs.append(pl.BlockSpec(memory_space=pl.ANY))
        out_shape += (jax.ShapeDtypeStruct((SIDE, SIDE, SIDE, full_rows // SIDE ** THREE, d_model), BF16),)
        scratch += LastPhase.scratch_shapes(planes)
        params |= dict(collective_id=5, has_side_effects=True)
    return pl.pallas_call(
        body, grid=(n_batch, n_groups), in_specs=in_specs, out_specs=out_specs, out_shape=out_shape, scratch_shapes=scratch,
        compiler_params=pltpu.CompilerParams(**params),
        cost_estimate=pl.CostEstimate(flops=TWO * d_model * d_model * (TWO * x.shape[ZERO] + TWO * kv.shape[ZERO]) + 16 * x.shape[ZERO] * n_k * d_model, bytes_accessed=20 * x.shape[ZERO] * d_model, transcendentals=ZERO),
        name='attn_fwd',
    )(*args)


def attn_bwd_kernel(causal, gain_row, mats, guest, lens_ref, dres_ref, wo_ref, w_all, q_ref, k_ref, v_ref, lse_ref,
                    rows_ref, normed_ref, inv_ref, lhs_refs, rows_out, dres_out, sums_ref, tail_ref, grads_ref,
                    rhs_q, rhs_k, lhs_q, lhs_k, do_v, w_v, grad_v, load_sem, store_sem):
    sample, group = pl.program_id(ZERO), pl.program_id(ONE)
    d_model = wo_ref.shape[ONE]
    n_q, n_k = q_ref.shape[ZERO], k_ref.shape[ZERO]
    last = pl.num_programs(ONE) - ONE
    fetches = [] if causal else [pltpu.make_async_copy(w_all.at[pl.ds(mats[ZERO] * d_model, d_model), :], w_v, load_sem.at[ZERO])]
    hand_on = pltpu.make_async_copy(rhs_q.at[pl.ds(ZERO, THREE)] if causal else rhs_k, rows_out, load_sem.at[ONE])
    dk_all, dv_all = (rhs_q.at[ONE], rhs_q.at[TWO]) if causal else (rhs_k.at[ZERO], rhs_k.at[ONE])
    d_all, dres_all = rhs_q.at[ZERO], rhs_q.at[THREE if causal else ONE]
    places = (lhs_q.at[ZERO], lhs_q.at[ONE]) if causal else (lhs_q.at[ZERO], lhs_k, lhs_q.at[ZERO])
    lhs_fetch = lambda i: pltpu.make_async_copy(lhs_refs[i], places[i], load_sem.at[THREE + i])
    store = lambda buf, mat: pltpu.make_async_copy(grad_v.at[buf], grads_ref.at[pl.ds(pl.multiple_of(mat * d_model, d_model), d_model), :], store_sem.at[buf])

    @pl.when((sample == ZERO) & (group == ZERO))
    def _():
        for fetch in fetches + [lhs_fetch(ZERO), lhs_fetch(ONE)]:
            fetch.start()

    turn = sample * pl.num_programs(ONE) + group
    q_rows = pl.ds(pl.multiple_of(sample * n_q, n_q), n_q)
    k_rows = pl.ds(pl.multiple_of(sample * n_k, n_k), n_k)
    d_o = dot_nt(dres_ref[ALL].astype(BF16), wo_ref[ALL]).astype(BF16)

    def keep(found, first, width):
        cols = pl.ds(pl.multiple_of(group * GROUP + first, PAIR), width)
        for i, (full, rows, value) in enumerate(zip((d_all, dk_all, dv_all), (q_rows, k_rows, k_rows), found)):
            sums_ref[i:i + ONE, cols] = col_sum(value) + jnp.where(sample == ZERO, 0.0, sums_ref[i:i + ONE, cols])
            full[rows, cols] = value.astype(BF16)

    if causal:
        keep(attend_group_bwd(d_o, q_ref[ALL], k_ref[ALL], v_ref[ALL], lens_ref[sample], causal, lse_ref.at[ZERO, ZERO]), ZERO, GROUP)
    else:
        do_v[ALL] = d_o

        def one_pair(pair, _):
            guest(ZERO, TWO * turn + pair)
            first = pl.multiple_of(pair * PAIR, PAIR)
            here = pl.ds(first, PAIR)
            keep(attend_group_bwd(do_v[:, here], q_ref[:, here], k_ref[:, here], v_ref[:, here], lens_ref[sample], causal, lse_ref.at[ZERO, ZERO, pl.ds(pair, ONE)]), first, PAIR)
            return ZERO

        lax.fori_loop(ZERO, GROUP // PAIR, one_pair, ZERO)

    @pl.when(group == ZERO)
    def _():
        dres_all[q_rows, :] = dres_ref[ALL].astype(BF16)

    guest(THREE, turn)
    if causal:
        tail_ref[ALL] = jnp.zeros_like(tail_ref)
    else:
        @pl.when((sample == ZERO) & (group == last))
        def _():
            for fetch in fetches:
                fetch.wait()

        @pl.when(group == last)
        def _():
            d_h = dres_ref[ALL] + dot_nt(d_all[q_rows, :], w_v[ALL])
            normed = normed_ref[ALL]
            d_resid = norm_rows_bwd(d_h, normed, inv_ref[ALL], rows_ref[gain_row:gain_row + ONE, :])
            dres_out[ALL] = d_resid
            for i, value in enumerate((d_resid, d_h * normed, d_h)):
                tail_ref[i:i + ONE, :] = col_sum(value) + jnp.where(sample == ZERO, 0.0, tail_ref[i:i + ONE, :])

    @pl.when(turn == pl.num_programs(ZERO) * pl.num_programs(ONE) - ONE)
    def _():
        hand_on.start()
        guest(TWO, 12)
        lhs_fetch(ZERO).wait()
        if causal:
            lhs_fetch(ONE).wait()

            def square(i, _):
                @pl.when(i >= TWO)
                def _():
                    store(i % TWO, mats[ZERO]).wait()

                grad_v[i % TWO] = dot_tn(lhs_q[i // THREE], rhs_q[i])
                store(i % TWO, mats[ZERO] + i).start()
                return ZERO

            lax.fori_loop(ZERO, 4, square, ZERO)
        else:
            def square_q(i, _):
                @pl.when(i == ONE)
                def _():
                    lhs_fetch(TWO).start()
                    lhs_fetch(TWO).wait()

                grad_v[i] = dot_tn(lhs_q[ZERO], rhs_q[i])
                store(i, mats[ZERO] + THREE * i).start()
                return ZERO

            def square_k(i, _):
                store(i, mats[ONE]).wait()
                grad_v[i] = dot_tn(lhs_k[ALL], rhs_k[i])
                store(i, mats[ONE] + i).start()
                return ZERO

            lax.fori_loop(ZERO, TWO, square_q, ZERO)
            guest(TWO, 13)
            lhs_fetch(ONE).wait()
            lax.fori_loop(ZERO, TWO, square_k, ZERO)
            guest(TWO, 14)
        for buf in range(TWO):
            store(buf, mats[ZERO]).wait()
        hand_on.wait()


def scatter_guest(scatter, plan, parity, position):
    steps = dict(end=scatter.end) | {('relay', p): functools.partial(scatter.relay, p) for p in range(THREE)}
    steps |= {('settle', p): functools.partial(scatter.settle, p) for p in range(THREE)} | {turn: functools.partial(scatter.absorb, turn) for turn in range(SIDE)}
    if parity == TWO:
        for name in plan.get(position, ()):
            steps[name]()
        return
    if parity == THREE:
        @pl.when(position == 5)
        def _():
            for name in plan['late']:
                steps[name]()
        return
    if parity == ZERO:
        @pl.when(position == ZERO)
        def _():
            meet_neighbours(scatter.place)
            scatter.begin()
    for where, names in plan.items():
        if where != 'late' and where < 12:
            @pl.when(position == where)
            def _():
                for name in names:
                    steps[name]()


def no_guest(parity, position):
    pass


def attn_backward(dres, q, k, v, lse, lens, attn_full, bias_rows, mats, causal, lhs_list, g_rows=None, scale=None, gain_row=ZERO, normed=None, inv_std=None, grads=None):
    d_model = q.shape[-ONE]
    n_batch = lens.shape[ZERO]
    n_q, n_k = q.shape[ZERO] // n_batch, k.shape[ZERO] // n_batch
    n_groups = d_model // GROUP
    row = lambda mat: pl.BlockSpec((GROUP, d_model), lambda b, g: (mat * n_groups + g, ZERO))
    q_blk = pl.BlockSpec((n_q, GROUP), lambda b, g: (b, g))
    k_blk = pl.BlockSpec((n_k, GROUP), lambda b, g: (b, g))
    tok = lambda n: pl.BlockSpec((n, d_model), lambda b, g: (b, ZERO))
    n_heads_g = GROUP // HEAD_DIM
    anywhere = pl.BlockSpec(memory_space=pl.ANY)
    in_specs = [pl.BlockSpec(memory_space=pltpu.SMEM), tok(n_q), row(mats[THREE]), anywhere, q_blk, k_blk, k_blk,
                pl.BlockSpec((ONE, ONE, n_heads_g // TWO, TWO, n_q), lambda b, g: (b, g, ZERO, ZERO, ZERO)), pl.BlockSpec(bias_rows.shape, lambda b, g: (ZERO, ZERO))]
    args = [lens, dres, attn_full, attn_full, q, k, v, lse, bias_rows]
    tail_shape = jax.ShapeDtypeStruct((8, d_model), F32)
    whole = pl.BlockSpec((8, d_model), lambda b, g: (ZERO, ZERO))
    out_shape = [jax.ShapeDtypeStruct((THREE,) + q.shape if causal else (TWO,) + k.shape, BF16)]
    out_specs = [anywhere]
    if not causal:
        late = dict(pipeline_mode=pl.Buffered(ONE))
        in_specs += [pl.BlockSpec((n_q, d_model), lambda b, g: (b, ZERO), **late), pl.BlockSpec((n_q, ONE), lambda b, g: (b, ZERO), **late)]
        args += [normed, inv_std]
        out_shape.append(jax.ShapeDtypeStruct(q.shape, F32))
        out_specs.append(tok(n_q))
    n_lhs_at = len(args)
    args += list(lhs_list)
    in_specs += [anywhere] * len(lhs_list)
    out_shape += [tail_shape, tail_shape, jax.ShapeDtypeStruct(attn_full.shape, F32)]
    out_specs += [whole, whole, anywhere]
    held = lambda count, n: pltpu.VMEM((count, n_batch * n, d_model), BF16)
    own = [held(4, n_q), held(TWO, n_q)] if causal else [held(TWO, n_q), held(TWO, n_k), held(ONE, n_q), pltpu.VMEM((n_batch * n_k, d_model), BF16)]
    own += [] if causal else [pltpu.VMEM((n_q, GROUP), BF16)]
    own += [] if causal else [pltpu.VMEM((d_model, d_model), BF16)]
    own += [pltpu.VMEM((TWO, d_model, d_model), F32), pltpu.SemaphoreType.DMA((6,)), pltpu.SemaphoreType.DMA((TWO,))]
    kernel = functools.partial(attn_bwd_kernel, causal, gain_row, mats)
    params = dict(vmem_limit_bytes=VMEM_BYTES, dimension_semantics=('arbitrary', 'arbitrary'))
    aliases = {}
    if causal:
        args.append(grads)
        in_specs.append(anywhere)
        aliases = {len(args) - ONE: len(out_shape) - ONE}
    else:
        args.append(as_torus(g_rows))
        in_specs.append(anywhere)
        n_rows = args[-ONE].shape[THREE]
        out_shape.append(jax.ShapeDtypeStruct((n_rows, d_model), F32))
        out_specs.append(anywhere)
        params |= dict(collective_id=THREE, has_side_effects=True, vmem_limit_bytes=67043328)
    scratch = own + ([] if causal else Scatter.scratch_shapes([n_rows]))
    n_in, n_out, n_own = len(args), len(out_shape), len(own)

    def body(*refs):
        ins, outs, rest = refs[:n_in], refs[n_in:n_in + n_out], refs[n_in + n_out:]
        lhs_refs, mine = ins[n_lhs_at:-ONE], rest[:n_own]
        if causal:
            rows_out, sums, tail, grads_ref = outs
            kernel(no_guest, *ins[:n_lhs_at], None, None, lhs_refs, rows_out, None, sums, tail, grads_ref, mine[ZERO], None, mine[ONE], None, None, None, *mine[TWO:])
        else:
            rows_out, dres_out, sums, tail, grads_ref, total = outs
            scatter = Scatter(scale, [(ins[-ONE], ZERO, n_rows)], [total], rest[n_own:])
            kernel(functools.partial(scatter_guest, scatter, CROSS_PLAN), *ins[:n_lhs_at], lhs_refs, rows_out, dres_out, sums, tail, grads_ref, *mine)

    return pl.pallas_call(
        body, grid=(n_batch, n_groups), in_specs=in_specs, out_specs=out_specs, out_shape=out_shape, scratch_shapes=scratch, input_output_aliases=aliases,
        compiler_params=pltpu.CompilerParams(**params),
        cost_estimate=pl.CostEstimate(flops=TWO * d_model * d_model * (TWO * q.shape[ZERO] + TWO * k.shape[ZERO]) + 40 * q.shape[ZERO] * n_k * d_model, bytes_accessed=20 * q.shape[ZERO] * d_model, transcendentals=ZERO),
        name='attn_bwd',
    )(*args)


def ffn_kernel(n_blocks, h_ref, dy_ref, up_ref, down_ref, rows_ref, bias_ref, normed_ref, inv_ref,
               y_ref, grad_ref, dres2_ref, tail_ref, upsum_ref, left_all, right_all):
    step = pl.program_id(ZERO)
    block, d_model = h_ref.shape
    n_square = left_all.shape[TWO] // d_model

    @pl.when(step < n_blocks)
    def _():
        rows = pl.ds(pl.multiple_of(step * block, block), block)
        h_b = h_ref[ALL]
        right_all[ZERO, rows, :] = h_b
        up = dot_nt(h_b, up_ref[ALL]) + bias_ref[ALL]
        cdf = 0.5 * (1.0 + lax.erf(up * 0.7071067811865476))
        gelu = (up * cdf).astype(BF16)
        slope = cdf + up * (0.3989422804014327 * jnp.exp(-0.5 * up * up))
        left_all[ONE, rows, :] = gelu
        resid = h_b.astype(F32) + dot(gelu, down_ref[ALL]) + rows_ref[8:9, :]
        y_b, normed3, inv3 = norm_rows(resid, rows_ref[13:14, :], rows_ref[14:15, :])
        y_ref[ALL] = y_b
        dy = dy_ref[ALL].astype(F32)
        d_res3 = norm_rows_bwd(dy, normed3, inv3, rows_ref[13:14, :])
        d_res3_b = d_res3.astype(BF16)
        right_all[ONE, rows, :] = d_res3_b
        d_up = dot_nt(d_res3_b, down_ref[ALL]) * slope
        d_up_b = d_up.astype(BF16)
        left_all[ZERO, rows, :] = d_up_b
        d_h2 = d_res3 + dot(d_up_b, up_ref[ALL])
        normed2 = normed_ref[ALL]
        d_res2 = norm_rows_bwd(d_h2, normed2, inv_ref[ALL], rows_ref[11:12, :])
        dres2_ref[ALL] = d_res2
        tail = jnp.concatenate([col_sum(d_res2), col_sum(d_res3), col_sum(d_h2 * normed2), col_sum(d_h2), col_sum(dy * normed3), col_sum(dy),
                                jnp.zeros((TWO, dy.shape[ONE]), F32)], axis=ZERO)
        up_sum = col_sum(d_up)

        @pl.when(step == ZERO)
        def _():
            tail_ref[ALL] = tail
            upsum_ref[ALL] = up_sum

        @pl.when(step > ZERO)
        def _():
            tail_ref[ALL] += tail
            upsum_ref[ALL] += up_sum

    square = step - n_blocks
    cols = pl.ds(pl.multiple_of(lax.rem(square + TWO * n_square, n_square) * d_model, d_model), d_model)

    @pl.when(square >= ZERO)
    def _():
        which = square // n_square
        grad_ref[ALL] = dot_tn(left_all[which, :, cols], right_all[which])


def ffn_both(h2, dy, ffn_full, bias_rows, up_bias, normed2, inv2, block=256):
    n_tok, d_model = h2.shape
    ffn_dim = ffn_full.shape[ZERO] // TWO
    n_blocks = n_tok // block
    n_steps = n_blocks + ffn_full.shape[ZERO] // d_model
    at = lambda i: jnp.minimum(i, n_blocks - ONE)
    tok = pl.BlockSpec((block, d_model), lambda i: (at(i), ZERO))
    once = lambda shape, idx: pl.BlockSpec(shape, lambda i: idx, pipeline_mode=pl.Buffered(ONE))
    return pl.pallas_call(
        functools.partial(ffn_kernel, n_blocks), grid=(n_steps,),
        in_specs=[tok, tok, once((ffn_dim, d_model), (ZERO, ZERO)), once((ffn_dim, d_model), (ONE, ZERO)), once(bias_rows.shape, (ZERO, ZERO)), once((ONE, ffn_dim), (ZERO, ZERO)),
                  tok, pl.BlockSpec((block, ONE), lambda i: (at(i), ZERO))],
        out_specs=[tok, pl.BlockSpec((d_model, d_model), lambda i: (jnp.maximum(i - n_blocks, ZERO), ZERO)), tok, pl.BlockSpec((8, d_model), lambda i: (ZERO, ZERO)), pl.BlockSpec((ONE, ffn_dim), lambda i: (ZERO, ZERO))],
        out_shape=[jax.ShapeDtypeStruct(h2.shape, BF16), jax.ShapeDtypeStruct(ffn_full.shape, F32), jax.ShapeDtypeStruct(h2.shape, F32),
                   jax.ShapeDtypeStruct((8, d_model), F32), jax.ShapeDtypeStruct((ONE, ffn_dim), F32)],
        scratch_shapes=[pltpu.VMEM((TWO, n_tok, ffn_dim), BF16), pltpu.VMEM((TWO, n_tok, d_model), BF16)],
        compiler_params=pltpu.CompilerParams(vmem_limit_bytes=VMEM_BYTES, dimension_semantics=('arbitrary',)),
        cost_estimate=pl.CostEstimate(flops=12 * n_tok * d_model * ffn_dim, bytes_accessed=30 * n_tok * d_model, transcendentals=ZERO),
        name='ffn_both',
    )(h2, dy, ffn_full, ffn_full, bias_rows, up_bias, normed2, inv2)


CROSS_PLAN = {ONE: (ZERO,), THREE: (ONE, TWO), 5: (('relay', ZERO),), 6: (THREE,), 9: (('settle', ZERO),), 11: (('relay', ONE),), 'late': (), 12: (('settle', ONE),), 13: (('relay', TWO),), 14: (('settle', TWO), 'end')}


def solution(mesh):
    n_fsdp = mesh.shape['fsdp']
    n_dp = mesh.shape['dp']
    batch_axes = ('dp', 'fsdp')
    act_spec = P(batch_axes, None, None)
    len_spec = P(batch_axes)
    row_spec = P('fsdp', None)
    vec_spec = P('fsdp')

    def device_step(dec_in, enc_out, src_lens, tgt_lens, y_cot, attn_w, ffn_w, vec_params):
        d_model, n_vec = dec_in.shape[TWO], vec_params.shape[ZERO]
        scale = 1.0 / (dec_in.shape[ZERO] * dec_in.shape[ONE] * n_fsdp * n_dp)
        x, enc, dy = (a.reshape(-ONE, d_model) for a in (dec_in, enc_out, y_cot))
        vec_rows = jnp.pad(vec_params.astype(F32), (ZERO, 16 * LANES - n_vec)).reshape(16, LANES)
        attn_tiles, planes, vec_tiles = gather_params(attn_w, ffn_w, vec_rows)
        attn_full = attn_tiles.reshape(-ONE, d_model)
        vec_f = vec_tiles.reshape(n_fsdp, 16, LANES)[:, :TWO].reshape(n_fsdp, TWO * LANES)[:, :n_vec].reshape(-ONE)
        bias_rows = jnp.pad(vec_f[:15 * d_model].reshape(15, d_model), ((ZERO, ONE), (ZERO, ZERO)))
        up_bias = vec_f[15 * d_model:].reshape(ONE, -ONE)
        q1, k1, v1, o1, lse1, h1, normed1, inv1 = attn_forward(x, x, tgt_lens, attn_full, bias_rows, (ZERO, ONE, TWO, THREE), (ZERO, ONE, TWO, THREE, 9), True)
        q2, k2, v2, o2, lse2, h2, normed2, inv2, ffn_tiles = attn_forward(h1, enc, src_lens, attn_full, bias_rows, (4, 5, 6, 7), (4, 5, 6, 7, 11), False, planes, ffn_w.shape[ZERO] * n_fsdp)
        ffn_full = ffn_tiles.reshape(-ONE, d_model)
        y, g_ffn, d_res2, ffn_tail, up_sum = ffn_both(h2, dy, ffn_full, bias_rows, up_bias, normed2, inv2)
        d_cross, d_res1, sums2, tail2, grads, ffn_out = attn_backward(d_res2, q2, k2, v2, lse2, src_lens, attn_full, bias_rows, (4, 5, 6, 7), False, (h1, enc, o2), g_ffn, scale, 9, normed1, inv1)
        d_self, sums1, _, grads = attn_backward(d_res1, q1, k1, v1, lse1, tgt_lens, attn_full, bias_rows, (ZERO, ONE, TWO, THREE), True, (x, o1), grads=grads)
        g_vec = jnp.concatenate([sums1[ZERO:THREE].reshape(-ONE), tail2[ZERO], sums2[ZERO:THREE].reshape(-ONE), ffn_tail[ZERO], ffn_tail[ONE], tail2[ONE], tail2[TWO], ffn_tail[TWO], ffn_tail[THREE], ffn_tail[4], ffn_tail[5], up_sum[ZERO]])
        g_rows = jnp.pad(g_vec.reshape(n_fsdp, ONE, n_vec), ((ZERO, ZERO), (ZERO, 7), (ZERO, TWO * LANES - n_vec))).reshape(n_fsdp * 8, -ONE)
        attn_out, vec_out, d_x, d_enc = scatter_grads(grads, g_rows, scale, attn_full, (ZERO, ONE, TWO, 5, 6), d_res1, d_self, d_cross)
        return y.reshape(dec_in.shape), d_x.reshape(dec_in.shape), d_enc.reshape(enc_out.shape), attn_out, ffn_out, vec_out[ZERO, :n_vec]

    return jax.shard_map(device_step, mesh=mesh, in_specs=(act_spec, act_spec, len_spec, len_spec, act_spec, row_spec, row_spec, vec_spec), out_specs=(act_spec, act_spec, act_spec, row_spec, row_spec, vec_spec), check_vma=False)
```

```python
import functools
import jax
import jax.numpy as jnp
from jax import lax
from jax.experimental import pallas as pl
from jax.experimental.pallas import tpu as pltpu
from jax.sharding import PartitionSpec as P

ZERO, ONE, TWO, THREE = range(4)
ALL = ...
HEAD_DIM = 64
LN_EPS = 1e-5
MASK_FILL = -1e30
VMEM_BYTES = 60 * 1024 * 1024
F32 = jnp.float32
BF16 = jnp.bfloat16
GROUP = 256
PAIR = 128


SIDE = 4
LANES = 128
COLOURS = THREE
STAGES = TWO
DIM_ORDER = ((TWO, ONE, ZERO), (ONE, ZERO, TWO), (ZERO, TWO, ONE))
MESH_ID = pl.DeviceIdType.MESH


def torus_place():
    chip = lax.axis_index('fsdp')
    return (chip // (SIDE * SIDE), lax.rem(chip // SIDE, SIDE), lax.rem(chip, SIDE))


def chip_at(place, dim, shift):
    moved = [lax.rem(p + shift + SIDE, SIDE) if d == dim else p for d, p in enumerate(place)]
    return (moved[ZERO] * SIDE + moved[ONE]) * SIDE + moved[TWO]


def meet_neighbours(place):
    barrier = pltpu.get_barrier_semaphore()
    core = lax.axis_index('dp')
    for dim in range(THREE):
        for shift in (ONE, -ONE):
            pl.semaphore_signal(barrier, inc=ONE, device_id=(core, chip_at(place, dim, shift)), device_id_type=MESH_ID)
    pl.semaphore_signal(barrier, inc=ONE, device_id=(ONE - core, lax.axis_index('fsdp')), device_id_type=MESH_ID)
    pl.semaphore_wait(barrier, 7)


class Scatter:
    def __init__(self, scale, sources, outs, scratch):
        self.scale, self.outs = scale, outs
        self.sources = [(ref, pl.ds(first, n)) for ref, first, n in sources]
        (self.acc, g1, d1, g2, d2, g3, d3, self.send_sem, self.recv_sem, self.load_sem, self.stage) = scratch
        self.got, self.far = (g1, g2, g3), (d1, d2, d3)
        self.heights = [n for _, _, n in sources]
        self.offsets = [sum(self.heights[:i]) for i in range(len(sources))]
        self.n_low = self.heights[ZERO] // TWO
        self.core, self.chip, self.place = lax.axis_index('dp'), lax.axis_index('fsdp'), torus_place()
        self.pieces = [(d, colour) for d in (TWO, ONE, THREE, ZERO) for colour in range(COLOURS)]

    @staticmethod
    def scratch_shapes(heights):
        h = sum(heights)
        n_low = heights[ZERO] // TWO
        buf = lambda *shape: pltpu.VMEM((COLOURS,) + shape + (LANES,), F32)
        n = Scatter.n_copies(len(heights))
        return [buf(SIDE, SIDE, SIDE, h), buf(TWO, SIDE, SIDE, h), buf(TWO, TWO, SIDE, h), buf(TWO, SIDE, h), buf(TWO, TWO, h), buf(TWO, h), buf(TWO, max(n_low, h - n_low)),
                pltpu.SemaphoreType.DMA((n,)), pltpu.SemaphoreType.DMA((n,)), pltpu.SemaphoreType.DMA((THREE + COLOURS, len(heights))),
                pltpu.VMEM((STAGES, SIDE, SIDE, h, LANES), F32)]

    @staticmethod
    def n_copies(n_parts):
        return 12 * n_parts + COLOURS * 18 + COLOURS * n_parts

    def parts(self, colour):
        return range(len(self.sources) if colour == ZERO else ONE)

    def height(self, colour):
        return sum(self.heights[i] for i in self.parts(colour))

    def remote(self, i, src, dst, device):
        return pltpu.make_async_remote_copy(src_ref=src, dst_ref=dst, send_sem=self.send_sem.at[i], recv_sem=self.recv_sem.at[i], device_id=device, device_id_type=MESH_ID)

    def columns(self, of_core, colour, part=ZERO):
        return pl.ds(pl.multiple_of((of_core * COLOURS + colour if part == ZERO else of_core) * LANES, LANES), LANES)

    def slot(self, d, colour):
        dim = DIM_ORDER[colour][ZERO]
        where = [slice(None)] * THREE
        where[dim] = lax.rem(self.place[dim] + d, SIDE)
        return tuple(where)

    def rows_of(self, part):
        return pl.ds(self.offsets[part], self.heights[part])

    def swaps(self, piece):
        d, colour = self.pieces[piece]
        where = self.slot(d, colour)
        n = len(self.sources)
        return [self.remote(piece * n + i, self.sources[i][ZERO].at[where + (self.sources[i][ONE], self.columns(ONE - self.core, colour, i))],
                            self.acc.at[(colour,) + where + (self.rows_of(i), slice(None))], (ONE - self.core, self.chip)) for i in self.parts(colour)]

    def loads(self, piece):
        d, colour = self.pieces[piece]
        where, buf = self.slot(d, colour), piece % STAGES
        return [pltpu.make_async_copy(self.sources[i][ZERO].at[where + (self.sources[i][ONE], self.columns(self.core, colour, i))],
                                      self.stage.at[buf, :, :, self.rows_of(i), :], self.load_sem.at[buf, i]) for i in self.parts(colour)]

    def split_rows(self, colour, half):
        return pl.ds(ZERO, self.n_low) if half == ZERO else pl.ds(self.n_low, self.height(colour) - self.n_low)

    def block(self, colour, phase, d, half=None):
        order = DIM_ORDER[colour]
        where = [None, None, None]
        for done in order[:phase]:
            where[done] = self.place[done]
        where[order[phase]] = lax.rem(self.place[order[phase]] + d, SIDE)
        for i, rest in enumerate(sorted(order[phase + ONE:])):
            where[rest] = slice(None) if half is None or i > ZERO else pl.ds(TWO * half, TWO)
        rows = self.split_rows(colour, half) if phase == TWO and half is not None else pl.ds(ZERO, self.height(colour))
        return self.acc.at[(colour,) + tuple(where) + (rows, slice(None))]

    def got_half(self, colour, phase, direction, half):
        if phase == TWO:
            return self.got[phase].at[colour, direction, self.split_rows(colour, half), :]
        return self.got_all(colour, phase, direction, pl.ds(TWO * half, TWO))

    def got_all(self, colour, phase, direction, which=slice(None)):
        rows = (pl.ds(ZERO, self.height(colour)), slice(None))
        blocks = ((which, slice(None)), (which,), ())[phase]
        return self.got[phase].at[(colour, direction) + blocks + rows]

    def far_part(self, colour, phase, direction):
        if phase == TWO:
            return self.far[phase].at[colour, direction, pl.ds(ZERO, self.n_low if direction == ZERO else self.height(colour) - self.n_low), :]
        return self.far[phase].at[(colour, direction) + (slice(None),) * (TWO - phase) + (pl.ds(ZERO, self.height(colour)), slice(None))]

    def ring(self, colour, phase, direction):
        shift = ONE - TWO * direction
        device = (self.core, chip_at(self.place, DIM_ORDER[colour][phase], shift))
        i = 12 * len(self.sources) + ((colour * THREE + phase) * TWO + direction) * THREE
        near = shift % SIDE
        return (self.remote(i, self.block(colour, phase, TWO, direction), self.far_part(colour, phase, direction), device),
                self.remote(i + ONE, self.block(colour, phase, near, ONE - direction), self.got_half(colour, phase, direction, ONE - direction), device),
                self.remote(i + TWO, self.block(colour, phase, near, direction), self.got_half(colour, phase, direction, direction), device))

    def gives(self, colour):
        n = len(self.sources)
        base = 12 * n + COLOURS * 18 + colour * n
        done = self.acc.at[colour, self.place[ZERO], self.place[ONE], self.place[TWO]]
        pairs = [(done.at[self.rows_of(i), :], self.outs[i].at[:, self.columns(self.core, colour, i)]) for i in self.parts(colour)]
        return [(self.remote(base + i, src, dst, (ONE - self.core, self.chip)), pltpu.make_async_copy(src, dst, self.load_sem.at[THREE + colour, i])) for i, (src, dst) in enumerate(pairs)]

    def add_into(self, dst, sources, n_lead):
        def body(i, _):
            total = dst[i]
            for src in sources:
                total = total + src[i]
            dst[i] = total
            return ZERO

        if n_lead == TWO:
            lax.fori_loop(ZERO, dst.shape[ZERO], body, ZERO)
        else:
            total = dst[ALL]
            for src in sources:
                total = total + src[ALL]
            dst[ALL] = total


    def begin(self):
        for piece in range(STAGES):
            for copy in self.loads(piece):
                copy.start()
        for piece in range(len(self.pieces)):
            for copy in self.swaps(piece):
                copy.start()

    def absorb(self, turn):
        for piece in range(turn * COLOURS, (turn + ONE) * COLOURS):
            d, colour = self.pieces[piece]
            for copy in self.loads(piece):
                copy.wait()
            for copy in self.swaps(piece):
                copy.wait_recv()
            rows = (pl.ds(ZERO, self.height(colour)), slice(None))
            self.add_into(self.acc.at[(colour,) + self.slot(d, colour) + rows], [self.stage.at[(piece % STAGES, slice(None), slice(None)) + rows]], TWO)
            if piece + STAGES < len(self.pieces):
                for copy in self.loads(piece + STAGES):
                    copy.start()
            if turn == ZERO:
                for direction in range(TWO):
                    self.ring(colour, ZERO, direction)[ZERO].start()
            elif turn < THREE:
                self.ring(colour, ZERO, turn - ONE)[ONE].start()

    def relay(self, phase):
        for colour in range(COLOURS):
            for direction in range(TWO):
                far, _, fed = self.ring(colour, phase, direction)
                far.wait_recv()
                self.add_into(self.block(colour, phase, (ONE - TWO * direction) % SIDE, direction), [self.far_part(colour, phase, direction)], TWO - phase)
            for direction in range(TWO):
                self.ring(colour, phase, direction)[TWO].start()

    def settle(self, phase):
        for colour in range(COLOURS):
            for direction in range(TWO):
                _, own, fed = self.ring(colour, phase, direction)
                own.wait_recv()
                fed.wait_recv()
            self.add_into(self.block(colour, phase, ZERO), [self.got_all(colour, phase, direction) for direction in range(TWO)], TWO - phase)
            if phase < TWO:
                for kind in range(TWO):
                    for direction in range(TWO):
                        self.ring(colour, phase + ONE, direction)[kind].start()
            else:
                done = self.block(colour, TWO, ZERO)
                done[ALL] = done[ALL] * self.scale
                for give, keep in self.gives(colour):
                    keep.start()
                    give.start()

    def end(self):
        for colour in range(COLOURS):
            for give, keep in self.gives(colour):
                give.wait_recv()
                give.wait_send()
                keep.wait()
        for piece in range(len(self.pieces)):
            for copy in self.swaps(piece):
                copy.wait_send()
        for colour in range(COLOURS):
            for phase in range(THREE):
                for direction in range(TWO):
                    for copy in self.ring(colour, phase, direction):
                        copy.wait_send()


def rs_kernel(scale, mats, g_ref, vec_ref, w_all, dres_ref, self_ref, cross_ref, out_ref, vec_out, dx_out, denc_out,
              w_v, dres_v, self_v, cross_v, dx_v, denc_v, load_sem, *scratch):
    scatter = Scatter(scale, [(ref, ZERO, ref.shape[THREE]) for ref in (g_ref, vec_ref)], [out_ref, vec_out], scratch)
    d_model = w_v.shape[ONE]
    step = 256
    loads = [pltpu.make_async_copy(w_all.at[pl.ds(mat * d_model, d_model), :], w_v.at[i], load_sem.at[i]) for i, mat in enumerate(mats)]
    loads += [pltpu.make_async_copy(src, dst, load_sem.at[len(mats) + i]) for i, (src, dst) in enumerate(((dres_ref, dres_v), (self_ref, self_v), (cross_ref, cross_v)))]
    stores = [pltpu.make_async_copy(src, dst, load_sem.at[len(mats) + THREE + i]) for i, (src, dst) in enumerate(((dx_v, dx_out), (denc_v, denc_out)))]

    def input_grads():
        for copy in loads:
            copy.wait()

        def decoder(i, _):
            rows = pl.ds(pl.multiple_of(i * step, step), step)
            total = dres_v[rows, :]
            for n in range(THREE):
                total = total + dot_nt(self_v[n, rows, :], w_v[n])
            dx_v[rows, :] = total.astype(BF16)
            return ZERO

        def encoder(i, _):
            rows = pl.ds(pl.multiple_of(i * step, step), step)
            denc_v[rows, :] = (dot_nt(cross_v[ZERO, rows, :], w_v[THREE]) + dot_nt(cross_v[ONE, rows, :], w_v[4])).astype(BF16)
            return ZERO

        lax.fori_loop(ZERO, dx_v.shape[ZERO] // step, decoder, ZERO)
        stores[ZERO].start()
        lax.fori_loop(ZERO, denc_v.shape[ZERO] // step, encoder, ZERO)
        stores[ONE].start()

    meet_neighbours(scatter.place)
    scatter.begin()
    for copy in loads:
        copy.start()
    for turn in range(THREE):
        scatter.absorb(turn)
    scatter.relay(ZERO)
    scatter.absorb(THREE)
    input_grads()
    scatter.settle(ZERO)
    for phase in (ONE, TWO):
        scatter.relay(phase)
        scatter.settle(phase)
    scatter.end()
    for copy in stores:
        copy.wait()


def as_torus(rows):
    return rows.reshape(SIDE, SIDE, SIDE, rows.shape[ZERO] // SIDE ** THREE, rows.shape[ONE])


def scatter_grads(g_attn, g_vec, scale, attn_full, mats, d_res, d_self, d_cross):
    sources = [as_torus(g_attn), as_torus(g_vec)]
    heights = [src.shape[THREE] for src in sources]
    d_model = g_attn.shape[ONE]
    anywhere = pl.BlockSpec(memory_space=pl.ANY)
    dx_shape, denc_shape = d_self.shape[ONE:], d_cross.shape[ONE:]
    return pl.pallas_call(
        functools.partial(rs_kernel, scale, mats),
        in_specs=[anywhere] * 6, out_specs=[anywhere] * 4,
        out_shape=[jax.ShapeDtypeStruct((h, src.shape[4]), F32) for h, src in zip(heights, sources)] + [jax.ShapeDtypeStruct(dx_shape, BF16), jax.ShapeDtypeStruct(denc_shape, BF16)],
        scratch_shapes=[pltpu.VMEM((len(mats), d_model, d_model), BF16), pltpu.VMEM(d_res.shape, F32), pltpu.VMEM(d_self.shape, BF16), pltpu.VMEM(d_cross.shape, BF16),
                        pltpu.VMEM(dx_shape, BF16), pltpu.VMEM(denc_shape, BF16), pltpu.SemaphoreType.DMA((len(mats) + 5,))] + Scatter.scratch_shapes(heights),
        compiler_params=pltpu.CompilerParams(collective_id=ONE, has_side_effects=True, vmem_limit_bytes=VMEM_BYTES),
        cost_estimate=pl.CostEstimate(flops=10 ** 9, bytes_accessed=8 * d_model * g_attn.shape[ZERO], transcendentals=ZERO),
        name='scatter_grads',
    )(*sources, attn_full, d_res, d_self, d_cross)


class Gather:
    def __init__(self, send_sem, recv_sem, base=ZERO):
        self.send_sem, self.recv_sem = send_sem, recv_sem
        self.used = base
        self.core, self.chip, self.place = lax.axis_index('dp'), lax.axis_index('fsdp'), torus_place()
        self.sibling = (ONE - self.core, self.chip)
        self.started = []

    def remote(self, src, dst, device):
        i = self.used
        self.used += ONE
        return pltpu.make_async_remote_copy(src_ref=src, dst_ref=dst, send_sem=self.send_sem.at[i], recv_sem=self.recv_sem.at[i], device_id=device, device_id_type=MESH_ID)

    def start(self, copy):
        copy.start()
        self.started.append(copy)

    def ring(self, colour, phase, view, own=None, split=False):
        order = DIM_ORDER[colour]
        dim = order[phase]
        have = sorted(order[:phase])

        def index(shift, half=None):
            where = [self.place[ZERO], self.place[ONE], self.place[TWO]]
            where[dim] = lax.rem(self.place[dim] + shift + SIDE, SIDE)
            for i, h in enumerate(have):
                where[h] = slice(None) if half is None or i > ZERO else pl.ds(TWO * half, TWO)
            return tuple(where)

        out = []
        for direction, shift in enumerate((ONE, -ONE)):
            device = (self.core, chip_at(self.place, dim, shift))
            half = direction if phase == ZERO else None
            near_dst = view(index(ZERO), None)
            if split:
                near = [self.remote(view(index(ZERO, h), None), view(index(ZERO, h), None), device) for h in (direction, ONE - direction)]
            else:
                near = [self.remote(near_dst if own is None else own, near_dst, device)]
            out.append(dict(
                near=near,
                far=self.remote(view(index(-shift, direction), half), view(index(-shift, direction), half), device),
                near_at=index(-shift), far_at=index(TWO, direction)))
        return out


def ag_kernel(attn_ref, ffn_ref, vec_ref, oattn_ref, planes_ref, vec_out, attn_v, send_sem, recv_sem, load_sem):
    net = Gather(send_sem, recv_sem)
    core, place = net.core, net.place
    rows, width = attn_ref.shape
    band = rows // (TWO * COLOURS)
    vec_high = vec_ref.shape[ZERO]
    stores, finals = [], []

    def band_rows(colour):
        return pl.ds(pl.multiple_of((core * COLOURS + colour) * band, band), band)

    def columns(half):
        return slice(None) if half is None else pl.ds(half * (width // TWO), width // TWO)

    def attn_view(colour):
        return lambda where, half: attn_v.at[where + (band_rows(colour), columns(half))]

    def ffn_view(colour):
        last = DIM_ORDER[colour][TWO]
        return lambda where, half: planes_ref.at[(colour,) + tuple(w for d, w in enumerate(where) if d != last) + (slice(None), columns(half))]

    def vec_view(where, half):
        return vec_out.at[where + (slice(None) if half is None else pl.ds(half * (vec_high // TWO), vec_high // TWO), slice(None))]

    colours = range(COLOURS)
    attn_own = [attn_ref.at[band_rows(colour), :] for colour in colours]
    ffn_own = [ffn_ref.at[band_rows(colour), :] for colour in colours]
    rings = {('attn', phase): [net.ring(colour, phase, attn_view(colour), attn_own[colour] if phase == ZERO else None, phase > ZERO) for colour in colours] for phase in range(THREE)}
    rings |= {('ffn', phase): [net.ring(colour, phase, ffn_view(colour), ffn_own[colour] if phase == ZERO else None, phase > ZERO) for colour in colours] for phase in range(TWO)}
    rings |= {('vec', phase): [net.ring(ONE, phase, vec_view, vec_ref if phase == ZERO else None)] for phase in range(THREE)}

    def publish(at):
        keep = pltpu.make_async_copy(attn_v.at[at], oattn_ref.at[at], load_sem.at[len(stores)])
        keep.start()
        stores.append(keep)
        give = net.remote(attn_v.at[at], oattn_ref.at[at], net.sibling)
        net.start(give)
        finals.append(give)

    def send_near(name, phase):
        for ring in rings.get((name, phase), ()):
            for way in ring:
                for copy in way['near']:
                    net.start(copy)

    def pass_on(name, phase):
        for ring in rings.get((name, phase), ()):
            for way in ring:
                way['near'][ZERO].wait_recv()
                net.start(way['far'])
        if phase == TWO and name == 'attn':
            for colour in colours:
                for way in rings[(name, phase)][colour]:
                    way['near'][ONE].wait_recv()
                    publish(way['near_at'] + (band_rows(colour), slice(None)))

    def complete(name, phase):
        for colour, ring in enumerate(rings.get((name, phase), ())):
            for way in ring:
                way['far'].wait_recv()
                if phase == ONE and name != 'vec':
                    way['near'][ONE].wait_recv()
            if phase < TWO and (name, phase + ONE) in rings:
                for way in rings[(name, phase + ONE)][colour]:
                    for copy in way['near']:
                        net.start(copy)
            if phase == TWO and name == 'attn':
                for way in ring:
                    publish(way['far_at'] + (band_rows(colour), slice(None)))
        if phase == ONE and name == 'attn':
            for colour in colours:
                last = DIM_ORDER[colour][TWO]
                publish(tuple(place[d] if d == last else slice(None) for d in range(THREE)) + (band_rows(colour), slice(None)))

    for colour in colours:
        attn_v[(place[ZERO], place[ONE], place[TWO]) + (band_rows(colour), slice(None))] = attn_ref[band_rows(colour), :]
        kept = [place[d] for d in range(THREE) if d != DIM_ORDER[colour][TWO]]
        planes_ref[(colour, kept[ZERO], kept[ONE])] = ffn_ref[band_rows(colour), :]
    vec_out[place[ZERO], place[ONE], place[TWO]] = vec_ref[ALL]
    meet_neighbours(place)
    names = ('attn', 'vec', 'ffn')
    for name in names:
        send_near(name, ZERO)
    for phase in range(THREE):
        for name in names:
            pass_on(name, phase)
        for name in names:
            complete(name, phase)
    for copy in finals:
        copy.wait_recv()
    for copy in net.started:
        copy.wait_send()
    for copy in stores:
        copy.wait()


def gather_params(attn_w, ffn_w, vec_rows):
    rows, width = attn_w.shape
    full = (SIDE, SIDE, SIDE, rows, width)
    n_copies = COLOURS * (4 * TWO + 6 * THREE) + 4 * THREE + COLOURS * 5
    vmem = pl.BlockSpec(memory_space=pltpu.VMEM)
    return pl.pallas_call(
        ag_kernel,
        in_specs=[vmem] * THREE, out_specs=[pl.BlockSpec(memory_space=pl.ANY), vmem, vmem],
        out_shape=[jax.ShapeDtypeStruct(full, BF16), jax.ShapeDtypeStruct((COLOURS, SIDE, SIDE, rows // (TWO * COLOURS), width), BF16),
                   jax.ShapeDtypeStruct((SIDE, SIDE, SIDE) + vec_rows.shape, F32)],
        scratch_shapes=[pltpu.VMEM(full, BF16), pltpu.SemaphoreType.DMA((n_copies,)), pltpu.SemaphoreType.DMA((n_copies,)), pltpu.SemaphoreType.DMA((COLOURS * 5,))],
        compiler_params=pltpu.CompilerParams(collective_id=TWO, has_side_effects=True, vmem_limit_bytes=VMEM_BYTES),
        cost_estimate=pl.CostEstimate(flops=10 ** 9, bytes_accessed=4 * rows * width * SIDE ** THREE, transcendentals=ZERO),
        name='gather_params',
    )(attn_w, ffn_w, vec_rows)


class LastPhase:
    def __init__(self, planes, out, near, far, send_sem, recv_sem, load_sem):
        self.planes, self.out, self.near, self.far = planes, out, near, far
        self.send_sem, self.recv_sem, self.load_sem = send_sem, recv_sem, load_sem
        self.core, self.chip, self.place = lax.axis_index('dp'), lax.axis_index('fsdp'), torus_place()
        self.band = planes.shape[THREE]

    @staticmethod
    def scratch_shapes(planes):
        colours, side, _, band, width = planes.shape
        sems = [pltpu.SemaphoreType.DMA((11 * COLOURS,)), pltpu.SemaphoreType.DMA((11 * COLOURS,)), pltpu.SemaphoreType.DMA((5 * COLOURS,))]
        return [pltpu.VMEM((colours, TWO, side, side, band, width), BF16), pltpu.VMEM((colours, TWO, side // TWO, side, band, width), BF16)] + sems

    def remote(self, i, src, dst, device):
        return pltpu.make_async_remote_copy(src_ref=src, dst_ref=dst, send_sem=self.send_sem.at[i], recv_sem=self.recv_sem.at[i], device_id=device, device_id_type=MESH_ID)

    def ring(self, colour, direction):
        device = (self.core, chip_at(self.place, DIM_ORDER[colour][TWO], ONE - TWO * direction))
        i = 11 * colour + THREE * direction
        got = self.near.at[colour, direction]
        near = [self.remote(i + n, self.planes.at[colour, pl.ds(TWO * half, TWO)], got.at[pl.ds(TWO * half, TWO)], device) for n, half in enumerate((direction, ONE - direction))]
        return near + [self.remote(i + TWO, got.at[pl.ds(TWO * direction, TWO)], self.far.at[colour, direction], device)]

    def shares(self, colour):
        last = DIM_ORDER[colour][TWO]
        rows = pl.ds(pl.multiple_of((self.core * COLOURS + colour) * self.band, self.band), self.band)
        views = [(self.planes.at[colour], ZERO, None)]
        views += [(self.near.at[colour, direction], TWO * direction - ONE, None) for direction in range(TWO)]
        views += [(self.far.at[colour, direction], TWO, direction) for direction in range(TWO)]
        out = []
        for n, (src, shift, half) in enumerate(views):
            where = [slice(None)] * THREE
            where[last] = lax.rem(self.place[last] + shift + SIDE, SIDE)
            if half is not None:
                where[min(d for d in range(THREE) if d != last)] = pl.ds(TWO * half, TWO)
            dst = self.out.at[tuple(where) + (rows, slice(None))]
            out.append((self.remote(11 * colour + 6 + n, src, dst, (ONE - self.core, self.chip)), pltpu.make_async_copy(src, dst, self.load_sem.at[5 * colour + n])))
        return out

    def share(self, colour, which):
        for n in which:
            give, keep = self.shares(colour)[n]
            give.start()
            keep.start()

    def begin(self):
        for colour in range(COLOURS):
            for direction in range(TWO):
                for copy in self.ring(colour, direction)[:TWO]:
                    copy.start()
        for colour in range(COLOURS):
            self.share(colour, (ZERO,))

    def pass_on(self):
        for colour in range(COLOURS):
            for direction in range(TWO):
                first, _, far = self.ring(colour, direction)
                first.wait_recv()
                far.start()
        for colour in range(COLOURS):
            for direction in range(TWO):
                self.ring(colour, direction)[ONE].wait_recv()
            self.share(colour, (ONE, TWO))

    def complete(self):
        for colour in range(COLOURS):
            for direction in range(TWO):
                self.ring(colour, direction)[TWO].wait_recv()
            self.share(colour, (THREE, 4))

    def end(self):
        for colour in range(COLOURS):
            for give, keep in self.shares(colour):
                give.wait_recv()
                give.wait_send()
                keep.wait()
            for direction in range(TWO):
                for copy in self.ring(colour, direction):
                    copy.wait_send()


def dot(lhs, rhs, contract=((ONE,), (ZERO,))):
    return lax.dot_general(lhs, rhs, (contract, ((), ())), preferred_element_type=F32)


def dot_nt(lhs, rhs):
    return dot(lhs, rhs, ((ONE,), (ONE,)))


def dot_tn(lhs, rhs):
    return dot(lhs, rhs, ((ZERO,), (ZERO,)))


def norm_rows(resid, gain, shift):
    mean = jnp.mean(resid, axis=-ONE, keepdims=True)
    centred = resid - mean
    inv_std = lax.rsqrt(jnp.mean(centred * centred, axis=-ONE, keepdims=True) + LN_EPS)
    normed = centred * inv_std
    return (normed * gain + shift).astype(BF16), normed, inv_std


def norm_rows_bwd(d_out, normed, inv_std, gain):
    d_norm = d_out * gain
    return inv_std * (d_norm - jnp.mean(d_norm, axis=-ONE, keepdims=True) - normed * jnp.mean(d_norm * normed, axis=-ONE, keepdims=True))


def col_sum(values):
    return jnp.sum(values, axis=ZERO, keepdims=True)


def lane_row(head, dtype=BF16):
    lane = lax.broadcasted_iota(jnp.int32, (ONE, PAIR), ONE)
    return jnp.where((lane >= HEAD_DIM * head) & (lane < HEAD_DIM * (head + ONE)), 1.0, 0.0).astype(dtype)


def spare_lane(head):
    lane = lax.broadcasted_iota(jnp.int32, (ONE, PAIR), ONE)
    return jnp.where(lane == HEAD_DIM * (ONE - head), 1.0, 0.0)


def mask_fill(n_rows, n_valid):
    row = lax.broadcasted_iota(jnp.int32, (n_rows, PAIR), ZERO)
    return jnp.where(row >= n_valid, MASK_FILL, 0.0)


def head_masks(pair_q, pair_k, head, fill):
    q_f = pair_q * lane_row(head) + spare_lane(head).astype(BF16)
    k_f = pair_k * lane_row(head) + (fill * spare_lane(head)).astype(BF16)
    return q_f, k_f


def half_only(pair, head):
    return pair * lane_row(head)


def join_halves(first, second):
    lane = lax.broadcasted_iota(jnp.int32, first.shape, ONE)
    return jnp.where(lane < HEAD_DIM, first, second)


def score_blocks(n_heads, n_q, n_k, causal, step):
    if not causal:
        return [(head, ZERO, n_q, n_k) for head in range(n_heads)]
    return [(head, first, step, first + step) for head in range(n_heads) for first in range(ZERO, n_q, step)]


def scores_t(q_f, k_f, causal, first):
    s_t = dot_nt(k_f, q_f)
    if causal:
        key_i = lax.broadcasted_iota(jnp.int32, s_t.shape, ZERO)
        qry_i = lax.broadcasted_iota(jnp.int32, s_t.shape, ONE) + first
        s_t = jnp.where(key_i <= qry_i, s_t, MASK_FILL)
    return s_t


def pair_of(group, head):
    return group[:, head // TWO * PAIR:(head // TWO + ONE) * PAIR]


def masked_pairs(q_g, k_g, n_valid):
    fill = mask_fill(k_g.shape[ZERO], n_valid)
    cache = {}

    def get(head):
        if head not in cache:
            cache[head] = head_masks(pair_of(q_g, head), pair_of(k_g, head), head % TWO, fill)
        return cache[head]

    return get


def stack_heads(parts, n_heads):
    return jnp.concatenate([jnp.concatenate(parts[head], axis=ONE) for head in range(n_heads)], axis=ZERO)


def run_ahead(blocks, produce, transform, consume, delay):
    ahead = produce(blocks[ZERO])
    waiting = []
    for i, block in enumerate(blocks):
        now = ahead
        if i + ONE < len(blocks):
            ahead = produce(blocks[i + ONE])
        waiting.append((block, transform(block, now)))
        if len(waiting) > delay:
            consume(*waiting.pop(ZERO))
    for item in waiting:
        consume(*item)


def attend_group(q_g, k_g, v_g, n_valid, causal, lse_ref):
    n_heads = GROUP // HEAD_DIM
    o_parts = [[] for _ in range(n_heads)]
    v_t = v_g.T
    masked = masked_pairs(q_g, k_g, n_valid)

    def produce(block):
        head, first, n_q, n_k = block
        q_f, k_f = masked(head)
        return scores_t(q_f[first:first + n_q], k_f[:n_k], causal, first)

    def transform(block, s_t):
        head, first, n_q, n_k = block
        top = jnp.max(s_t, axis=ZERO, keepdims=True)
        e_t = jnp.exp(s_t - top)
        total = jnp.sum(e_t, axis=ZERO, keepdims=True)
        lse_ref[ZERO, ZERO, head // TWO, head % TWO:head % TWO + ONE, first:first + n_q] = top + jnp.log(total)
        return (e_t * (1.0 / total)).astype(BF16)

    def consume(block, p_t):
        head, first, n_q, n_k = block
        o_parts[head].append(dot(v_t[HEAD_DIM * head:HEAD_DIM * (head + ONE), :n_k], p_t))

    run_ahead(score_blocks(n_heads, q_g.shape[ZERO], k_g.shape[ZERO], causal, 128), produce, transform, consume, TWO)
    return stack_heads(o_parts, n_heads).T.astype(BF16)


def attend_group_bwd(d_o, q_g, k_g, v_g, n_valid, causal, lse_ref):
    n_heads = q_g.shape[ONE] // HEAD_DIM
    k_t = k_g.T
    dq_t, dk_h, dv_h = [[] for _ in range(n_heads)], [None] * n_heads, [None] * n_heads
    masked = masked_pairs(q_g, k_g, n_valid)
    v_half = {}

    def produce(block):
        head, first, n_q, n_k = block
        q_f, k_f = masked(head)
        if head not in v_half:
            v_half[head] = half_only(pair_of(v_g, head), head % TWO)
        rows = slice(first, first + n_q)
        return scores_t(q_f[rows], k_f[:n_k], causal, first), dot_nt(v_half[head][:n_k], pair_of(d_o, head)[rows])

    def transform(block, products):
        head, first, n_q, n_k = block
        s_t, dp_t = products
        p_t = jnp.exp(s_t - lse_ref[head // TWO, head % TWO:head % TWO + ONE, first:first + n_q])
        weighted = p_t * dp_t
        return p_t.astype(BF16), (weighted - p_t * jnp.sum(weighted, axis=ZERO, keepdims=True)).astype(BF16)

    def grow(old, new):
        if old is None:
            return new
        n_old = old.shape[ZERO]
        return old + new if n_old == new.shape[ZERO] else jnp.concatenate([old + new[:n_old], new[n_old:]], axis=ZERO)

    def consume(block, operands):
        head, first, n_q, n_k = block
        p_b, ds_t = operands
        rows = slice(first, first + n_q)
        dv_h[head] = grow(dv_h[head], dot(p_b, pair_of(d_o, head)[rows]))
        dk_h[head] = grow(dk_h[head], dot(ds_t, pair_of(q_g, head)[rows]))
        dq_t[head].append(dot(k_t[HEAD_DIM * head:HEAD_DIM * (head + ONE), :n_k], ds_t))

    run_ahead(score_blocks(n_heads, q_g.shape[ZERO], k_g.shape[ZERO], causal, 256), produce, transform, consume, ZERO)
    join = lambda parts: jnp.concatenate([join_halves(parts[h], parts[h + ONE]) for h in range(ZERO, n_heads, TWO)], axis=ONE)
    return stack_heads(dq_t, n_heads).T * 0.125, join(dk_h), join(dv_h)


def attn_fwd_kernel(causal, slots, guest, lens_ref, x_ref, kv_ref, wq_ref, wk_ref, wv_ref, w_all, bias_ref, rows_ref,
                    q_ref, k_ref, v_ref, o_ref, lse_ref, h_ref, normed_ref, inv_ref, o_all, wo_v, load_sem):
    q_row, k_row, v_row, o_row, gain_row, o_mat = slots
    sample, group = pl.program_id(ZERO), pl.program_id(ONE)
    d_model = wo_v.shape[ZERO]
    fetch = pltpu.make_async_copy(w_all.at[pl.ds(o_mat * d_model, d_model), :], wo_v, load_sem)

    @pl.when((sample == ZERO) & (group == ZERO))
    def _():
        fetch.start()

    turn = sample * pl.num_programs(ONE) + group
    if guest is not None:
        for where, steps in ((ZERO, (lambda: meet_neighbours(guest.place), guest.begin)), (THREE, (guest.pass_on,)), (5, (guest.complete,))):
            @pl.when(turn == where)
            def _():
                for step in steps:
                    step()

    x_b, kv_b = x_ref[ALL], kv_ref[ALL]
    q_g = ((dot(x_b, wq_ref[ALL]) + bias_ref[q_row:q_row + ONE, :]) * 0.125).astype(BF16)
    k_g = (dot(kv_b, wk_ref[ALL]) + bias_ref[k_row:k_row + ONE, :]).astype(BF16)
    v_g = (dot(kv_b, wv_ref[ALL]) + bias_ref[v_row:v_row + ONE, :]).astype(BF16)
    q_ref[ALL], k_ref[ALL], v_ref[ALL] = q_g, k_g, v_g
    o_g = attend_group(q_g, k_g, v_g, lens_ref[sample], causal, lse_ref)
    o_ref[ALL] = o_g
    o_all[:, pl.ds(pl.multiple_of(group * GROUP, GROUP), GROUP)] = o_g

    @pl.when((sample == ZERO) & (group == pl.num_programs(ONE) - ONE))
    def _():
        fetch.wait()

    @pl.when(group == pl.num_programs(ONE) - ONE)
    def _():
        resid = x_ref[ALL].astype(F32) + dot(o_all[ALL], wo_v[ALL]) + rows_ref[o_row:o_row + ONE, :]
        h_out, normed, inv_std = norm_rows(resid, rows_ref[gain_row:gain_row + ONE, :], rows_ref[gain_row + ONE:gain_row + TWO, :])
        h_ref[ALL], normed_ref[ALL], inv_ref[ALL] = h_out, normed, inv_std

    if guest is not None:
        @pl.when(turn == pl.num_programs(ZERO) * pl.num_programs(ONE) - ONE)
        def _():
            guest.end()


def attn_forward(x, kv, lens, attn_full, bias_rows, mats, slots, causal, planes=None, full_rows=None):
    d_model = x.shape[-ONE]
    n_batch = lens.shape[ZERO]
    n_q, n_k = x.shape[ZERO] // n_batch, kv.shape[ZERO] // n_batch
    n_groups = d_model // GROUP
    col = lambda mat: pl.BlockSpec((d_model, GROUP), lambda b, g: (mat, g))
    q_blk = pl.BlockSpec((n_q, GROUP), lambda b, g: (b, g))
    k_blk = pl.BlockSpec((n_k, GROUP), lambda b, g: (b, g))
    tok = lambda n: pl.BlockSpec((n, d_model), lambda b, g: (b, ZERO))
    n_heads_g = GROUP // HEAD_DIM
    out_shape = (
        jax.ShapeDtypeStruct(x.shape, BF16), jax.ShapeDtypeStruct(kv.shape, BF16), jax.ShapeDtypeStruct(kv.shape, BF16),
        jax.ShapeDtypeStruct(x.shape, BF16), jax.ShapeDtypeStruct((n_batch, n_groups, n_heads_g // TWO, TWO, n_q), F32),
        jax.ShapeDtypeStruct(x.shape, BF16), jax.ShapeDtypeStruct(x.shape, F32), jax.ShapeDtypeStruct((x.shape[ZERO], ONE), F32))
    kernel = functools.partial(attn_fwd_kernel, causal, slots + (mats[THREE],))
    in_specs = [pl.BlockSpec(memory_space=pltpu.SMEM), tok(n_q), tok(n_k), col(mats[ZERO]), col(mats[ONE]), col(mats[TWO]), pl.BlockSpec(memory_space=pl.ANY),
                pl.BlockSpec((bias_rows.shape[ZERO], GROUP), lambda b, g: (ZERO, g)), pl.BlockSpec(bias_rows.shape, lambda b, g: (ZERO, ZERO))]
    out_specs = [q_blk, k_blk, k_blk, q_blk, pl.BlockSpec((ONE, ONE, n_heads_g // TWO, TWO, n_q), lambda b, g: (b, g, ZERO, ZERO, ZERO)),
                 tok(n_q), tok(n_q), pl.BlockSpec((n_q, ONE), lambda b, g: (b, ZERO))]
    scratch = [pltpu.VMEM((n_q, d_model), BF16), pltpu.VMEM((d_model, d_model), BF16), pltpu.SemaphoreType.DMA]
    args = [lens, x, kv, attn_full, attn_full, attn_full, attn_full, bias_rows, bias_rows]
    params = dict(vmem_limit_bytes=VMEM_BYTES, dimension_semantics=('arbitrary', 'arbitrary'))
    if planes is None:
        body = functools.partial(kernel, None)
    else:
        n_in, n_out, n_own = len(args), len(out_specs), len(scratch)

        def body(*refs):
            ins, held, outs, whole, rest = refs[:n_in], refs[n_in], refs[n_in + ONE:n_in + ONE + n_out], refs[n_in + ONE + n_out], refs[n_in + TWO + n_out:]
            kernel(LastPhase(held, whole, *rest[n_own:]), *ins, *outs, *rest[:n_own])

        in_specs.append(pl.BlockSpec(memory_space=pltpu.VMEM))
        args.append(planes)
        out_specs.append(pl.BlockSpec(memory_space=pl.ANY))
        out_shape += (jax.ShapeDtypeStruct((SIDE, SIDE, SIDE, full_rows // SIDE ** THREE, d_model), BF16),)
        scratch += LastPhase.scratch_shapes(planes)
        params |= dict(collective_id=5, has_side_effects=True)
    return pl.pallas_call(
        body, grid=(n_batch, n_groups), in_specs=in_specs, out_specs=out_specs, out_shape=out_shape, scratch_shapes=scratch,
        compiler_params=pltpu.CompilerParams(**params),
        cost_estimate=pl.CostEstimate(flops=TWO * d_model * d_model * (TWO * x.shape[ZERO] + TWO * kv.shape[ZERO]) + 16 * x.shape[ZERO] * n_k * d_model, bytes_accessed=20 * x.shape[ZERO] * d_model, transcendentals=ZERO),
        name='attn_fwd',
    )(*args)


def attn_bwd_kernel(causal, gain_row, mats, guest, lens_ref, dres_ref, wo_ref, w_all, q_ref, k_ref, v_ref, lse_ref,
                    rows_ref, normed_ref, inv_ref, lhs_refs, rows_out, dres_out, sums_ref, tail_ref, grads_ref,
                    rhs_q, rhs_k, lhs_q, lhs_k, do_v, w_v, grad_v, load_sem, store_sem):
    sample, group = pl.program_id(ZERO), pl.program_id(ONE)
    d_model = wo_ref.shape[ONE]
    n_q, n_k = q_ref.shape[ZERO], k_ref.shape[ZERO]
    last = pl.num_programs(ONE) - ONE
    fetches = [] if causal else [pltpu.make_async_copy(w_all.at[pl.ds(mats[ZERO] * d_model, d_model), :], w_v, load_sem.at[ZERO])]
    hand_on = pltpu.make_async_copy(rhs_q.at[pl.ds(ZERO, THREE)] if causal else rhs_k, rows_out, load_sem.at[ONE])
    dk_all, dv_all = (rhs_q.at[ONE], rhs_q.at[TWO]) if causal else (rhs_k.at[ZERO], rhs_k.at[ONE])
    d_all, dres_all = rhs_q.at[ZERO], rhs_q.at[THREE if causal else ONE]
    places = (lhs_q.at[ZERO], lhs_q.at[ONE]) if causal else (lhs_q.at[ZERO], lhs_k, lhs_q.at[ZERO])
    lhs_fetch = lambda i: pltpu.make_async_copy(lhs_refs[i], places[i], load_sem.at[THREE + i])
    store = lambda buf, mat: pltpu.make_async_copy(grad_v.at[buf], grads_ref.at[pl.ds(pl.multiple_of(mat * d_model, d_model), d_model), :], store_sem.at[buf])

    @pl.when((sample == ZERO) & (group == ZERO))
    def _():
        for fetch in fetches + [lhs_fetch(ZERO), lhs_fetch(ONE)]:
            fetch.start()

    turn = sample * pl.num_programs(ONE) + group
    q_rows = pl.ds(pl.multiple_of(sample * n_q, n_q), n_q)
    k_rows = pl.ds(pl.multiple_of(sample * n_k, n_k), n_k)
    d_o = dot_nt(dres_ref[ALL].astype(BF16), wo_ref[ALL]).astype(BF16)

    def keep(found, first, width):
        here = pl.ds(first, width)
        cols = pl.ds(pl.multiple_of(group * GROUP + first, PAIR), width)
        for i, (full, rows, value) in enumerate(zip((d_all, dk_all, dv_all), (q_rows, k_rows, k_rows), found)):
            sums_ref[ZERO, i:i + ONE, here] = col_sum(value)
            full[rows, cols] = value.astype(BF16)

    if causal:
        keep(attend_group_bwd(d_o, q_ref[ALL], k_ref[ALL], v_ref[ALL], lens_ref[sample], causal, lse_ref.at[ZERO, ZERO]), ZERO, GROUP)
    else:
        do_v[ALL] = d_o

        def one_pair(pair, _):
            guest(ZERO, TWO * turn + pair)
            first = pl.multiple_of(pair * PAIR, PAIR)
            here = pl.ds(first, PAIR)
            keep(attend_group_bwd(do_v[:, here], q_ref[:, here], k_ref[:, here], v_ref[:, here], lens_ref[sample], causal, lse_ref.at[ZERO, ZERO, pl.ds(pair, ONE)]), first, PAIR)
            return ZERO

        lax.fori_loop(ZERO, GROUP // PAIR, one_pair, ZERO)

    @pl.when(group == ZERO)
    def _():
        dres_all[q_rows, :] = dres_ref[ALL].astype(BF16)

    guest(THREE, turn)
    if causal:
        tail_ref[ALL] = jnp.zeros_like(tail_ref)
    else:
        @pl.when((sample == ZERO) & (group == last))
        def _():
            for fetch in fetches:
                fetch.wait()

        @pl.when(group == last)
        def _():
            d_h = dres_ref[ALL] + dot_nt(d_all[q_rows, :], w_v[ALL])
            normed = normed_ref[ALL]
            d_resid = norm_rows_bwd(d_h, normed, inv_ref[ALL], rows_ref[gain_row:gain_row + ONE, :])
            dres_out[ALL] = d_resid
            tail_ref[ZERO, ZERO:ONE, :] = col_sum(d_resid)
            tail_ref[ZERO, ONE:TWO, :] = col_sum(d_h * normed)
            tail_ref[ZERO, TWO:THREE, :] = col_sum(d_h)

    @pl.when(turn == pl.num_programs(ZERO) * pl.num_programs(ONE) - ONE)
    def _():
        hand_on.start()
        guest(TWO, 12)
        lhs_fetch(ZERO).wait()
        if causal:
            lhs_fetch(ONE).wait()

            def square(i, _):
                @pl.when(i >= TWO)
                def _():
                    store(i % TWO, mats[ZERO]).wait()

                grad_v[i % TWO] = dot_tn(lhs_q[i // THREE], rhs_q[i])
                store(i % TWO, mats[ZERO] + i).start()
                return ZERO

            lax.fori_loop(ZERO, 4, square, ZERO)
        else:
            def square_q(i, _):
                @pl.when(i == ONE)
                def _():
                    lhs_fetch(TWO).start()
                    lhs_fetch(TWO).wait()

                grad_v[i] = dot_tn(lhs_q[ZERO], rhs_q[i])
                store(i, mats[ZERO] + THREE * i).start()
                return ZERO

            def square_k(i, _):
                @pl.when(i == ONE)
                def _():
                    guest(TWO, 14)

                store(i, mats[ONE]).wait()
                grad_v[i] = dot_tn(lhs_k[ALL], rhs_k[i])
                store(i, mats[ONE] + i).start()
                return ZERO

            lax.fori_loop(ZERO, TWO, square_q, ZERO)
            guest(TWO, 13)
            lhs_fetch(ONE).wait()
            lax.fori_loop(ZERO, TWO, square_k, ZERO)
            guest(TWO, 15)
        for buf in range(TWO):
            store(buf, mats[ZERO]).wait()
        hand_on.wait()


def scatter_guest(scatter, plan, parity, position):
    steps = dict(end=scatter.end) | {('relay', p): functools.partial(scatter.relay, p) for p in range(THREE)}
    steps |= {('settle', p): functools.partial(scatter.settle, p) for p in range(THREE)} | {turn: functools.partial(scatter.absorb, turn) for turn in range(SIDE)}
    if parity == TWO:
        for name in plan.get(position, ()):
            steps[name]()
        return
    if parity == THREE:
        @pl.when(position == 5)
        def _():
            for name in plan['late']:
                steps[name]()
        return
    if parity == ZERO:
        @pl.when(position == ZERO)
        def _():
            meet_neighbours(scatter.place)
            scatter.begin()
    for where, names in plan.items():
        if where != 'late' and where < 12:
            @pl.when(position == where)
            def _():
                for name in names:
                    steps[name]()


def no_guest(parity, position):
    pass


def attn_backward(dres, q, k, v, lse, lens, attn_full, bias_rows, mats, causal, lhs_list, g_rows=None, scale=None, gain_row=ZERO, normed=None, inv_std=None, grads=None):
    d_model = q.shape[-ONE]
    n_batch = lens.shape[ZERO]
    n_q, n_k = q.shape[ZERO] // n_batch, k.shape[ZERO] // n_batch
    n_groups = d_model // GROUP
    row = lambda mat: pl.BlockSpec((GROUP, d_model), lambda b, g: (mat * n_groups + g, ZERO))
    q_blk = pl.BlockSpec((n_q, GROUP), lambda b, g: (b, g))
    k_blk = pl.BlockSpec((n_k, GROUP), lambda b, g: (b, g))
    tok = lambda n: pl.BlockSpec((n, d_model), lambda b, g: (b, ZERO))
    n_heads_g = GROUP // HEAD_DIM
    anywhere = pl.BlockSpec(memory_space=pl.ANY)
    in_specs = [pl.BlockSpec(memory_space=pltpu.SMEM), tok(n_q), row(mats[THREE]), anywhere, q_blk, k_blk, k_blk,
                pl.BlockSpec((ONE, ONE, n_heads_g // TWO, TWO, n_q), lambda b, g: (b, g, ZERO, ZERO, ZERO)), pl.BlockSpec(bias_rows.shape, lambda b, g: (ZERO, ZERO))]
    args = [lens, dres, attn_full, attn_full, q, k, v, lse, bias_rows]
    tail_shape = jax.ShapeDtypeStruct((n_batch, 8, d_model), F32)
    out_shape = [jax.ShapeDtypeStruct((THREE,) + q.shape if causal else (TWO,) + k.shape, BF16)]
    out_specs = [anywhere]
    if not causal:
        late = dict(pipeline_mode=pl.Buffered(ONE))
        in_specs += [pl.BlockSpec((n_q, d_model), lambda b, g: (b, ZERO), **late), pl.BlockSpec((n_q, ONE), lambda b, g: (b, ZERO), **late)]
        args += [normed, inv_std]
        out_shape.append(jax.ShapeDtypeStruct(q.shape, F32))
        out_specs.append(tok(n_q))
    n_lhs_at = len(args)
    args += list(lhs_list)
    in_specs += [anywhere] * len(lhs_list)
    out_shape += [tail_shape, tail_shape, jax.ShapeDtypeStruct(attn_full.shape, F32)]
    out_specs += [pl.BlockSpec((ONE, 8, GROUP), lambda b, g: (b, ZERO, g)), pl.BlockSpec((ONE, 8, d_model), lambda b, g: (b, ZERO, ZERO)), anywhere]
    held = lambda count, n: pltpu.VMEM((count, n_batch * n, d_model), BF16)
    own = [held(4, n_q), held(TWO, n_q)] if causal else [held(TWO, n_q), held(TWO, n_k), held(ONE, n_q), pltpu.VMEM((n_batch * n_k, d_model), BF16)]
    own += [] if causal else [pltpu.VMEM((n_q, GROUP), BF16)]
    own += [] if causal else [pltpu.VMEM((d_model, d_model), BF16)]
    own += [pltpu.VMEM((TWO, d_model, d_model), F32), pltpu.SemaphoreType.DMA((6,)), pltpu.SemaphoreType.DMA((TWO,))]
    kernel = functools.partial(attn_bwd_kernel, causal, gain_row, mats)
    params = dict(vmem_limit_bytes=VMEM_BYTES, dimension_semantics=('arbitrary', 'arbitrary'))
    aliases = {}
    if causal:
        args.append(grads)
        in_specs.append(anywhere)
        aliases = {len(args) - ONE: len(out_shape) - ONE}
    else:
        args.append(as_torus(g_rows))
        in_specs.append(anywhere)
        n_rows = args[-ONE].shape[THREE]
        out_shape.append(jax.ShapeDtypeStruct((n_rows, d_model), F32))
        out_specs.append(anywhere)
        params |= dict(collective_id=THREE, has_side_effects=True, vmem_limit_bytes=67043328)
    scratch = own + ([] if causal else Scatter.scratch_shapes([n_rows]))
    n_in, n_out, n_own = len(args), len(out_shape), len(own)

    def body(*refs):
        ins, outs, rest = refs[:n_in], refs[n_in:n_in + n_out], refs[n_in + n_out:]
        lhs_refs, mine = ins[n_lhs_at:-ONE], rest[:n_own]
        if causal:
            rows_out, sums, tail, grads_ref = outs
            kernel(no_guest, *ins[:n_lhs_at], None, None, lhs_refs, rows_out, None, sums, tail, grads_ref, mine[ZERO], None, mine[ONE], None, None, None, *mine[TWO:])
        else:
            rows_out, dres_out, sums, tail, grads_ref, total = outs
            scatter = Scatter(scale, [(ins[-ONE], ZERO, n_rows)], [total], rest[n_own:])
            kernel(functools.partial(scatter_guest, scatter, CROSS_PLAN), *ins[:n_lhs_at], lhs_refs, rows_out, dres_out, sums, tail, grads_ref, *mine)

    return pl.pallas_call(
        body, grid=(n_batch, n_groups), in_specs=in_specs, out_specs=out_specs, out_shape=out_shape, scratch_shapes=scratch, input_output_aliases=aliases,
        compiler_params=pltpu.CompilerParams(**params),
        cost_estimate=pl.CostEstimate(flops=TWO * d_model * d_model * (TWO * q.shape[ZERO] + TWO * k.shape[ZERO]) + 40 * q.shape[ZERO] * n_k * d_model, bytes_accessed=20 * q.shape[ZERO] * d_model, transcendentals=ZERO),
        name='attn_bwd',
    )(*args)


def ffn_kernel(n_blocks, h_ref, dy_ref, up_ref, down_ref, rows_ref, bias_ref, normed_ref, inv_ref,
               y_ref, grad_ref, dres2_ref, tail_ref, upsum_ref, left_all, right_all):
    step = pl.program_id(ZERO)
    block, d_model = h_ref.shape
    n_square = left_all.shape[TWO] // d_model

    @pl.when(step < n_blocks)
    def _():
        rows = pl.ds(pl.multiple_of(step * block, block), block)
        h_b = h_ref[ALL]
        right_all[ZERO, rows, :] = h_b
        up = dot_nt(h_b, up_ref[ALL]) + bias_ref[ALL]
        cdf = 0.5 * (1.0 + lax.erf(up * 0.7071067811865476))
        gelu = (up * cdf).astype(BF16)
        slope = cdf + up * (0.3989422804014327 * jnp.exp(-0.5 * up * up))
        left_all[ONE, rows, :] = gelu
        resid = h_b.astype(F32) + dot(gelu, down_ref[ALL]) + rows_ref[8:9, :]
        y_b, normed3, inv3 = norm_rows(resid, rows_ref[13:14, :], rows_ref[14:15, :])
        y_ref[ALL] = y_b
        dy = dy_ref[ALL].astype(F32)
        d_res3 = norm_rows_bwd(dy, normed3, inv3, rows_ref[13:14, :])
        d_res3_b = d_res3.astype(BF16)
        right_all[ONE, rows, :] = d_res3_b
        d_up = dot_nt(d_res3_b, down_ref[ALL]) * slope
        d_up_b = d_up.astype(BF16)
        left_all[ZERO, rows, :] = d_up_b
        d_h2 = d_res3 + dot(d_up_b, up_ref[ALL])
        normed2 = normed_ref[ALL]
        d_res2 = norm_rows_bwd(d_h2, normed2, inv_ref[ALL], rows_ref[11:12, :])
        dres2_ref[ALL] = d_res2
        tail = jnp.concatenate([col_sum(d_res2), col_sum(d_res3), col_sum(d_h2 * normed2), col_sum(d_h2), col_sum(dy * normed3), col_sum(dy),
                                jnp.zeros((TWO, dy.shape[ONE]), F32)], axis=ZERO)
        up_sum = col_sum(d_up)

        @pl.when(step == ZERO)
        def _():
            tail_ref[ALL] = tail
            upsum_ref[ALL] = up_sum

        @pl.when(step > ZERO)
        def _():
            tail_ref[ALL] += tail
            upsum_ref[ALL] += up_sum

    square = step - n_blocks
    cols = pl.ds(pl.multiple_of(lax.rem(square + TWO * n_square, n_square) * d_model, d_model), d_model)

    @pl.when(square >= ZERO)
    def _():
        which = square // n_square
        grad_ref[ALL] = dot_tn(left_all[which, :, cols], right_all[which])


def ffn_both(h2, dy, ffn_full, bias_rows, up_bias, normed2, inv2, block=256):
    n_tok, d_model = h2.shape
    ffn_dim = ffn_full.shape[ZERO] // TWO
    n_blocks = n_tok // block
    n_steps = n_blocks + ffn_full.shape[ZERO] // d_model
    at = lambda i: jnp.minimum(i, n_blocks - ONE)
    tok = pl.BlockSpec((block, d_model), lambda i: (at(i), ZERO))
    once = lambda shape, idx: pl.BlockSpec(shape, lambda i: idx, pipeline_mode=pl.Buffered(ONE))
    return pl.pallas_call(
        functools.partial(ffn_kernel, n_blocks), grid=(n_steps,),
        in_specs=[tok, tok, once((ffn_dim, d_model), (ZERO, ZERO)), once((ffn_dim, d_model), (ONE, ZERO)), once(bias_rows.shape, (ZERO, ZERO)), once((ONE, ffn_dim), (ZERO, ZERO)),
                  tok, pl.BlockSpec((block, ONE), lambda i: (at(i), ZERO))],
        out_specs=[tok, pl.BlockSpec((d_model, d_model), lambda i: (jnp.maximum(i - n_blocks, ZERO), ZERO)), tok, pl.BlockSpec((8, d_model), lambda i: (ZERO, ZERO)), pl.BlockSpec((ONE, ffn_dim), lambda i: (ZERO, ZERO))],
        out_shape=[jax.ShapeDtypeStruct(h2.shape, BF16), jax.ShapeDtypeStruct(ffn_full.shape, F32), jax.ShapeDtypeStruct(h2.shape, F32),
                   jax.ShapeDtypeStruct((8, d_model), F32), jax.ShapeDtypeStruct((ONE, ffn_dim), F32)],
        scratch_shapes=[pltpu.VMEM((TWO, n_tok, ffn_dim), BF16), pltpu.VMEM((TWO, n_tok, d_model), BF16)],
        compiler_params=pltpu.CompilerParams(vmem_limit_bytes=VMEM_BYTES, dimension_semantics=('arbitrary',)),
        cost_estimate=pl.CostEstimate(flops=12 * n_tok * d_model * ffn_dim, bytes_accessed=30 * n_tok * d_model, transcendentals=ZERO),
        name='ffn_both',
    )(h2, dy, ffn_full, ffn_full, bias_rows, up_bias, normed2, inv2)


CROSS_PLAN = {ONE: (ZERO,), THREE: (ONE, TWO), 5: (('relay', ZERO),), 6: (THREE,), 9: (('settle', ZERO),), 11: (('relay', ONE),), 'late': (), 12: (('settle', ONE),), 13: (('relay', TWO),), 14: (('settle', TWO),), 15: ('end',)}


def solution(mesh):
    n_fsdp = mesh.shape['fsdp']
    n_dp = mesh.shape['dp']
    batch_axes = ('dp', 'fsdp')
    act_spec = P(batch_axes, None, None)
    len_spec = P(batch_axes)
    row_spec = P('fsdp', None)
    vec_spec = P('fsdp')

    def device_step(dec_in, enc_out, src_lens, tgt_lens, y_cot, attn_w, ffn_w, vec_params):
        d_model, n_vec = dec_in.shape[TWO], vec_params.shape[ZERO]
        scale = 1.0 / (dec_in.shape[ZERO] * dec_in.shape[ONE] * n_fsdp * n_dp)
        x, enc, dy = (a.reshape(-ONE, d_model) for a in (dec_in, enc_out, y_cot))
        vec_rows = jnp.pad(vec_params.astype(F32), (ZERO, 16 * LANES - n_vec)).reshape(16, LANES)
        attn_tiles, planes, vec_tiles = gather_params(attn_w, ffn_w, vec_rows)
        attn_full = attn_tiles.reshape(-ONE, d_model)
        vec_f = vec_tiles.reshape(n_fsdp, 16, LANES)[:, :TWO].reshape(n_fsdp, TWO * LANES)[:, :n_vec].reshape(-ONE)
        bias_rows = jnp.pad(vec_f[:15 * d_model].reshape(15, d_model), ((ZERO, ONE), (ZERO, ZERO)))
        up_bias = vec_f[15 * d_model:].reshape(ONE, -ONE)
        q1, k1, v1, o1, lse1, h1, normed1, inv1 = attn_forward(x, x, tgt_lens, attn_full, bias_rows, (ZERO, ONE, TWO, THREE), (ZERO, ONE, TWO, THREE, 9), True)
        q2, k2, v2, o2, lse2, h2, normed2, inv2, ffn_tiles = attn_forward(h1, enc, src_lens, attn_full, bias_rows, (4, 5, 6, 7), (4, 5, 6, 7, 11), False, planes, ffn_w.shape[ZERO] * n_fsdp)
        ffn_full = ffn_tiles.reshape(-ONE, d_model)
        y, g_ffn, d_res2, ffn_tail, up_sum = ffn_both(h2, dy, ffn_full, bias_rows, up_bias, normed2, inv2)
        d_cross, d_res1, sums2, tail2, grads, ffn_out = attn_backward(d_res2, q2, k2, v2, lse2, src_lens, attn_full, bias_rows, (4, 5, 6, 7), False, (h1, enc, o2), g_ffn, scale, 9, normed1, inv1)
        d_self, sums1, _, grads = attn_backward(d_res1, q1, k1, v1, lse1, tgt_lens, attn_full, bias_rows, (ZERO, ONE, TWO, THREE), True, (x, o1), grads=grads)
        s1, s2, t2 = jnp.sum(sums1, axis=ZERO), jnp.sum(sums2, axis=ZERO), jnp.sum(tail2, axis=ZERO)
        g_vec = jnp.concatenate([s1[ZERO:THREE].reshape(-ONE), t2[ZERO], s2[ZERO:THREE].reshape(-ONE), ffn_tail[ZERO], ffn_tail[ONE], t2[ONE], t2[TWO], ffn_tail[TWO], ffn_tail[THREE], ffn_tail[4], ffn_tail[5], up_sum[ZERO]])
        g_rows = jnp.pad(g_vec.reshape(n_fsdp, ONE, n_vec), ((ZERO, ZERO), (ZERO, 7), (ZERO, TWO * LANES - n_vec))).reshape(n_fsdp * 8, -ONE)
        attn_out, vec_out, d_x, d_enc = scatter_grads(grads, g_rows, scale, attn_full, (ZERO, ONE, TWO, 5, 6), d_res1, d_self, d_cross)
        return y.reshape(dec_in.shape), d_x.reshape(dec_in.shape), d_enc.reshape(enc_out.shape), attn_out, ffn_out, vec_out[ZERO, :n_vec]

    return jax.shard_map(device_step, mesh=mesh, in_specs=(act_spec, act_spec, len_spec, len_spec, act_spec, row_spec, row_spec, vec_spec), out_specs=(act_spec, act_spec, act_spec, row_spec, row_spec, vec_spec), check_vma=False)
```

```python
import functools
import jax
import jax.numpy as jnp
from jax import lax
from jax.experimental import pallas as pl
from jax.experimental.pallas import tpu as pltpu
from jax.sharding import PartitionSpec as P

ZERO, ONE, TWO, THREE = range(4)
ALL = ...
HEAD_DIM = 64
LN_EPS = 1e-5
MASK_FILL = -1e30
VMEM_BYTES = 60 * 1024 * 1024
F32 = jnp.float32
BF16 = jnp.bfloat16
GROUP = 256
PAIR = 128


SIDE = 4
LANES = 128
COLOURS = THREE
STAGES = TWO
DIM_ORDER = ((TWO, ONE, ZERO), (ONE, ZERO, TWO), (ZERO, TWO, ONE))
MESH_ID = pl.DeviceIdType.MESH


def torus_place():
    chip = lax.axis_index('fsdp')
    return (chip // (SIDE * SIDE), lax.rem(chip // SIDE, SIDE), lax.rem(chip, SIDE))


def chip_at(place, dim, shift):
    moved = [lax.rem(p + shift + SIDE, SIDE) if d == dim else p for d, p in enumerate(place)]
    return (moved[ZERO] * SIDE + moved[ONE]) * SIDE + moved[TWO]


def meet_neighbours(place):
    barrier = pltpu.get_barrier_semaphore()
    core = lax.axis_index('dp')
    for dim in range(THREE):
        for shift in (ONE, -ONE):
            pl.semaphore_signal(barrier, inc=ONE, device_id=(core, chip_at(place, dim, shift)), device_id_type=MESH_ID)
    pl.semaphore_signal(barrier, inc=ONE, device_id=(ONE - core, lax.axis_index('fsdp')), device_id_type=MESH_ID)
    pl.semaphore_wait(barrier, 7)


class Scatter:
    def __init__(self, scale, sources, outs, scratch):
        self.scale, self.outs = scale, outs
        self.sources = [(ref, pl.ds(first, n)) for ref, first, n in sources]
        (self.acc, g1, d1, g2, d2, g3, d3, self.send_sem, self.recv_sem, self.load_sem, self.stage) = scratch
        self.got, self.far = (g1, g2, g3), (d1, d2, d3)
        self.heights = [n for _, _, n in sources]
        self.offsets = [sum(self.heights[:i]) for i in range(len(sources))]
        self.n_low = self.heights[ZERO] // TWO
        self.core, self.chip, self.place = lax.axis_index('dp'), lax.axis_index('fsdp'), torus_place()
        self.pieces = [(d, colour) for d in (TWO, ONE, THREE, ZERO) for colour in range(COLOURS)]

    @staticmethod
    def scratch_shapes(heights):
        h = sum(heights)
        n_low = heights[ZERO] // TWO
        buf = lambda *shape: pltpu.VMEM((COLOURS,) + shape + (LANES,), F32)
        n = Scatter.n_copies(len(heights))
        return [buf(SIDE, SIDE, SIDE, h), buf(TWO, SIDE, SIDE, h), buf(TWO, TWO, SIDE, h), buf(TWO, SIDE, h), buf(TWO, TWO, h), buf(TWO, h), buf(TWO, max(n_low, h - n_low)),
                pltpu.SemaphoreType.DMA((n,)), pltpu.SemaphoreType.DMA((n,)), pltpu.SemaphoreType.DMA((THREE + COLOURS, len(heights))),
                pltpu.VMEM((STAGES, SIDE, SIDE, h, LANES), F32)]

    @staticmethod
    def n_copies(n_parts):
        return 12 * n_parts + COLOURS * 18 + COLOURS * n_parts

    def parts(self, colour):
        return range(len(self.sources) if colour == ZERO else ONE)

    def height(self, colour):
        return sum(self.heights[i] for i in self.parts(colour))

    def remote(self, i, src, dst, device):
        return pltpu.make_async_remote_copy(src_ref=src, dst_ref=dst, send_sem=self.send_sem.at[i], recv_sem=self.recv_sem.at[i], device_id=device, device_id_type=MESH_ID)

    def columns(self, of_core, colour, part=ZERO):
        return pl.ds(pl.multiple_of((of_core * COLOURS + colour if part == ZERO else of_core) * LANES, LANES), LANES)

    def slot(self, d, colour):
        dim = DIM_ORDER[colour][ZERO]
        where = [slice(None)] * THREE
        where[dim] = lax.rem(self.place[dim] + d, SIDE)
        return tuple(where)

    def rows_of(self, part):
        return pl.ds(self.offsets[part], self.heights[part])

    def swaps(self, piece):
        d, colour = self.pieces[piece]
        where = self.slot(d, colour)
        n = len(self.sources)
        return [self.remote(piece * n + i, self.sources[i][ZERO].at[where + (self.sources[i][ONE], self.columns(ONE - self.core, colour, i))],
                            self.acc.at[(colour,) + where + (self.rows_of(i), slice(None))], (ONE - self.core, self.chip)) for i in self.parts(colour)]

    def loads(self, piece):
        d, colour = self.pieces[piece]
        where, buf = self.slot(d, colour), piece % STAGES
        return [pltpu.make_async_copy(self.sources[i][ZERO].at[where + (self.sources[i][ONE], self.columns(self.core, colour, i))],
                                      self.stage.at[buf, :, :, self.rows_of(i), :], self.load_sem.at[buf, i]) for i in self.parts(colour)]

    def split_rows(self, colour, half):
        return pl.ds(ZERO, self.n_low) if half == ZERO else pl.ds(self.n_low, self.height(colour) - self.n_low)

    def block(self, colour, phase, d, half=None):
        order = DIM_ORDER[colour]
        where = [None, None, None]
        for done in order[:phase]:
            where[done] = self.place[done]
        where[order[phase]] = lax.rem(self.place[order[phase]] + d, SIDE)
        for i, rest in enumerate(sorted(order[phase + ONE:])):
            where[rest] = slice(None) if half is None or i > ZERO else pl.ds(TWO * half, TWO)
        rows = self.split_rows(colour, half) if phase == TWO and half is not None else pl.ds(ZERO, self.height(colour))
        return self.acc.at[(colour,) + tuple(where) + (rows, slice(None))]

    def got_half(self, colour, phase, direction, half):
        if phase == TWO:
            return self.got[phase].at[colour, direction, self.split_rows(colour, half), :]
        return self.got_all(colour, phase, direction, pl.ds(TWO * half, TWO))

    def got_all(self, colour, phase, direction, which=slice(None)):
        rows = (pl.ds(ZERO, self.height(colour)), slice(None))
        blocks = ((which, slice(None)), (which,), ())[phase]
        return self.got[phase].at[(colour, direction) + blocks + rows]

    def far_part(self, colour, phase, direction):
        if phase == TWO:
            return self.far[phase].at[colour, direction, pl.ds(ZERO, self.n_low if direction == ZERO else self.height(colour) - self.n_low), :]
        return self.far[phase].at[(colour, direction) + (slice(None),) * (TWO - phase) + (pl.ds(ZERO, self.height(colour)), slice(None))]

    def ring(self, colour, phase, direction):
        shift = ONE - TWO * direction
        device = (self.core, chip_at(self.place, DIM_ORDER[colour][phase], shift))
        i = 12 * len(self.sources) + ((colour * THREE + phase) * TWO + direction) * THREE
        near = shift % SIDE
        return (self.remote(i, self.block(colour, phase, TWO, direction), self.far_part(colour, phase, direction), device),
                self.remote(i + ONE, self.block(colour, phase, near, ONE - direction), self.got_half(colour, phase, direction, ONE - direction), device),
                self.remote(i + TWO, self.block(colour, phase, near, direction), self.got_half(colour, phase, direction, direction), device))

    def gives(self, colour):
        n = len(self.sources)
        base = 12 * n + COLOURS * 18 + colour * n
        done = self.acc.at[colour, self.place[ZERO], self.place[ONE], self.place[TWO]]
        pairs = [(done.at[self.rows_of(i), :], self.outs[i].at[:, self.columns(self.core, colour, i)]) for i in self.parts(colour)]
        return [(self.remote(base + i, src, dst, (ONE - self.core, self.chip)), pltpu.make_async_copy(src, dst, self.load_sem.at[THREE + colour, i])) for i, (src, dst) in enumerate(pairs)]

    def add_into(self, dst, sources, n_lead):
        def body(i, _):
            total = dst[i]
            for src in sources:
                total = total + src[i]
            dst[i] = total
            return ZERO

        if n_lead == TWO:
            lax.fori_loop(ZERO, dst.shape[ZERO], body, ZERO)
        else:
            total = dst[ALL]
            for src in sources:
                total = total + src[ALL]
            dst[ALL] = total


    def begin(self):
        for piece in range(STAGES):
            for copy in self.loads(piece):
                copy.start()
        for piece in range(len(self.pieces)):
            for copy in self.swaps(piece):
                copy.start()

    def absorb(self, turn):
        for piece in range(turn * COLOURS, (turn + ONE) * COLOURS):
            d, colour = self.pieces[piece]
            for copy in self.loads(piece):
                copy.wait()
            for copy in self.swaps(piece):
                copy.wait_recv()
            rows = (pl.ds(ZERO, self.height(colour)), slice(None))
            self.add_into(self.acc.at[(colour,) + self.slot(d, colour) + rows], [self.stage.at[(piece % STAGES, slice(None), slice(None)) + rows]], TWO)
            if piece + STAGES < len(self.pieces):
                for copy in self.loads(piece + STAGES):
                    copy.start()
            if turn == ZERO:
                for direction in range(TWO):
                    self.ring(colour, ZERO, direction)[ZERO].start()
            elif turn < THREE:
                self.ring(colour, ZERO, turn - ONE)[ONE].start()

    def relay(self, phase):
        for colour in range(COLOURS):
            for direction in range(TWO):
                far, _, fed = self.ring(colour, phase, direction)
                far.wait_recv()
                self.add_into(self.block(colour, phase, (ONE - TWO * direction) % SIDE, direction), [self.far_part(colour, phase, direction)], TWO - phase)
            for direction in range(TWO):
                self.ring(colour, phase, direction)[TWO].start()

    def settle(self, phase):
        for colour in range(COLOURS):
            for direction in range(TWO):
                _, own, fed = self.ring(colour, phase, direction)
                own.wait_recv()
                fed.wait_recv()
            self.add_into(self.block(colour, phase, ZERO), [self.got_all(colour, phase, direction) for direction in range(TWO)], TWO - phase)
            if phase < TWO:
                for kind in range(TWO):
                    for direction in range(TWO):
                        self.ring(colour, phase + ONE, direction)[kind].start()
            else:
                done = self.block(colour, TWO, ZERO)
                done[ALL] = done[ALL] * self.scale
                for give, keep in self.gives(colour):
                    keep.start()
                    give.start()

    def end(self):
        for colour in range(COLOURS):
            for give, keep in self.gives(colour):
                give.wait_recv()
                give.wait_send()
                keep.wait()
        for piece in range(len(self.pieces)):
            for copy in self.swaps(piece):
                copy.wait_send()
        for colour in range(COLOURS):
            for phase in range(THREE):
                for direction in range(TWO):
                    for copy in self.ring(colour, phase, direction):
                        copy.wait_send()


def rs_kernel(scale, mats, g_ref, vec_ref, w_all, dres_ref, self_ref, cross_ref, out_ref, vec_out, dx_out, denc_out,
              w_v, dres_v, self_v, cross_v, dx_v, denc_v, load_sem, *scratch):
    scatter = Scatter(scale, [(ref, ZERO, ref.shape[THREE]) for ref in (g_ref, vec_ref)], [out_ref, vec_out], scratch)
    d_model = w_v.shape[ONE]
    step = 256
    loads = [pltpu.make_async_copy(w_all.at[pl.ds(mat * d_model, d_model), :], w_v.at[i], load_sem.at[i]) for i, mat in enumerate(mats)]
    loads += [pltpu.make_async_copy(src, dst, load_sem.at[len(mats) + i]) for i, (src, dst) in enumerate(((dres_ref, dres_v), (self_ref, self_v), (cross_ref, cross_v)))]
    stores = [pltpu.make_async_copy(src, dst, load_sem.at[len(mats) + THREE + i]) for i, (src, dst) in enumerate(((dx_v, dx_out), (denc_v, denc_out)))]

    def input_grads():
        for copy in loads:
            copy.wait()

        def decoder(i, _):
            rows = pl.ds(pl.multiple_of(i * step, step), step)
            total = dres_v[rows, :]
            for n in range(THREE):
                total = total + dot_nt(self_v[n, rows, :], w_v[n])
            dx_v[rows, :] = total.astype(BF16)
            return ZERO

        def encoder(i, _):
            rows = pl.ds(pl.multiple_of(i * step, step), step)
            denc_v[rows, :] = (dot_nt(cross_v[ZERO, rows, :], w_v[THREE]) + dot_nt(cross_v[ONE, rows, :], w_v[4])).astype(BF16)
            return ZERO

        lax.fori_loop(ZERO, dx_v.shape[ZERO] // step, decoder, ZERO)
        stores[ZERO].start()
        lax.fori_loop(ZERO, denc_v.shape[ZERO] // step, encoder, ZERO)
        stores[ONE].start()

    meet_neighbours(scatter.place)
    scatter.begin()
    for copy in loads:
        copy.start()
    for turn in range(THREE):
        scatter.absorb(turn)
    scatter.relay(ZERO)
    scatter.absorb(THREE)
    input_grads()
    scatter.settle(ZERO)
    for phase in (ONE, TWO):
        scatter.relay(phase)
        scatter.settle(phase)
    scatter.end()
    for copy in stores:
        copy.wait()


def as_torus(rows):
    return rows.reshape(SIDE, SIDE, SIDE, rows.shape[ZERO] // SIDE ** THREE, rows.shape[ONE])


def scatter_grads(g_attn, g_vec, scale, attn_full, mats, d_res, d_self, d_cross):
    sources = [as_torus(g_attn), as_torus(g_vec)]
    heights = [src.shape[THREE] for src in sources]
    d_model = g_attn.shape[ONE]
    anywhere = pl.BlockSpec(memory_space=pl.ANY)
    dx_shape, denc_shape = d_self.shape[ONE:], d_cross.shape[ONE:]
    return pl.pallas_call(
        functools.partial(rs_kernel, scale, mats),
        in_specs=[anywhere] * 6, out_specs=[anywhere] * 4,
        out_shape=[jax.ShapeDtypeStruct((h, src.shape[4]), F32) for h, src in zip(heights, sources)] + [jax.ShapeDtypeStruct(dx_shape, BF16), jax.ShapeDtypeStruct(denc_shape, BF16)],
        scratch_shapes=[pltpu.VMEM((len(mats), d_model, d_model), BF16), pltpu.VMEM(d_res.shape, F32), pltpu.VMEM(d_self.shape, BF16), pltpu.VMEM(d_cross.shape, BF16),
                        pltpu.VMEM(dx_shape, BF16), pltpu.VMEM(denc_shape, BF16), pltpu.SemaphoreType.DMA((len(mats) + 5,))] + Scatter.scratch_shapes(heights),
        compiler_params=pltpu.CompilerParams(collective_id=ONE, has_side_effects=True, vmem_limit_bytes=VMEM_BYTES),
        cost_estimate=pl.CostEstimate(flops=10 ** 9, bytes_accessed=8 * d_model * g_attn.shape[ZERO], transcendentals=ZERO),
        name='scatter_grads',
    )(*sources, attn_full, d_res, d_self, d_cross)


class Gather:
    def __init__(self, send_sem, recv_sem, base=ZERO):
        self.send_sem, self.recv_sem = send_sem, recv_sem
        self.used = base
        self.core, self.chip, self.place = lax.axis_index('dp'), lax.axis_index('fsdp'), torus_place()
        self.sibling = (ONE - self.core, self.chip)
        self.started = []

    def remote(self, src, dst, device):
        i = self.used
        self.used += ONE
        return pltpu.make_async_remote_copy(src_ref=src, dst_ref=dst, send_sem=self.send_sem.at[i], recv_sem=self.recv_sem.at[i], device_id=device, device_id_type=MESH_ID)

    def start(self, copy):
        copy.start()
        self.started.append(copy)

    def ring(self, colour, phase, view, own=None, split=False):
        order = DIM_ORDER[colour]
        dim = order[phase]
        have = sorted(order[:phase])

        def index(shift, half=None):
            where = [self.place[ZERO], self.place[ONE], self.place[TWO]]
            where[dim] = lax.rem(self.place[dim] + shift + SIDE, SIDE)
            for i, h in enumerate(have):
                where[h] = slice(None) if half is None or i > ZERO else pl.ds(TWO * half, TWO)
            return tuple(where)

        out = []
        for direction, shift in enumerate((ONE, -ONE)):
            device = (self.core, chip_at(self.place, dim, shift))
            half = direction if phase == ZERO else None
            near_dst = view(index(ZERO), None)
            if split:
                near = [self.remote(view(index(ZERO, h), None), view(index(ZERO, h), None), device) for h in (direction, ONE - direction)]
            else:
                near = [self.remote(near_dst if own is None else own, near_dst, device)]
            out.append(dict(
                near=near,
                far=self.remote(view(index(-shift, direction), half), view(index(-shift, direction), half), device),
                near_at=index(-shift), far_at=index(TWO, direction)))
        return out


def ag_kernel(attn_ref, ffn_ref, vec_ref, oattn_ref, planes_ref, vec_out, attn_v, send_sem, recv_sem, load_sem):
    net = Gather(send_sem, recv_sem)
    core, place = net.core, net.place
    rows, width = attn_ref.shape
    band = rows // (TWO * COLOURS)
    vec_high = vec_ref.shape[ZERO]
    stores, finals = [], []

    def band_rows(colour):
        return pl.ds(pl.multiple_of((core * COLOURS + colour) * band, band), band)

    def columns(half):
        return slice(None) if half is None else pl.ds(half * (width // TWO), width // TWO)

    def attn_view(colour):
        return lambda where, half: attn_v.at[where + (band_rows(colour), columns(half))]

    def ffn_view(colour):
        last = DIM_ORDER[colour][TWO]
        return lambda where, half: planes_ref.at[(colour,) + tuple(w for d, w in enumerate(where) if d != last) + (slice(None), columns(half))]

    def vec_view(where, half):
        return vec_out.at[where + (slice(None) if half is None else pl.ds(half * (vec_high // TWO), vec_high // TWO), slice(None))]

    colours = range(COLOURS)
    attn_own = [attn_ref.at[band_rows(colour), :] for colour in colours]
    ffn_own = [ffn_ref.at[band_rows(colour), :] for colour in colours]
    rings = {('attn', phase): [net.ring(colour, phase, attn_view(colour), attn_own[colour] if phase == ZERO else None, phase > ZERO) for colour in colours] for phase in range(THREE)}
    rings |= {('ffn', phase): [net.ring(colour, phase, ffn_view(colour), ffn_own[colour] if phase == ZERO else None, phase > ZERO) for colour in colours] for phase in range(TWO)}
    rings |= {('vec', phase): [net.ring(ONE, phase, vec_view, vec_ref if phase == ZERO else None)] for phase in range(THREE)}

    def publish(at):
        keep = pltpu.make_async_copy(attn_v.at[at], oattn_ref.at[at], load_sem.at[len(stores)])
        keep.start()
        stores.append(keep)
        give = net.remote(attn_v.at[at], oattn_ref.at[at], net.sibling)
        net.start(give)
        finals.append(give)

    def send_near(name, phase):
        for ring in rings.get((name, phase), ()):
            for way in ring:
                for copy in way['near']:
                    net.start(copy)

    def pass_on(name, phase):
        for ring in rings.get((name, phase), ()):
            for way in ring:
                way['near'][ZERO].wait_recv()
                net.start(way['far'])
        if phase == TWO and name == 'attn':
            for colour in colours:
                for way in rings[(name, phase)][colour]:
                    way['near'][ONE].wait_recv()
                    publish(way['near_at'] + (band_rows(colour), slice(None)))

    def complete(name, phase):
        for colour, ring in enumerate(rings.get((name, phase), ())):
            for way in ring:
                way['far'].wait_recv()
                if phase == ONE and name != 'vec':
                    way['near'][ONE].wait_recv()
            if phase < TWO and (name, phase + ONE) in rings:
                for way in rings[(name, phase + ONE)][colour]:
                    for copy in way['near']:
                        net.start(copy)
            if phase == TWO and name == 'attn':
                for way in ring:
                    publish(way['far_at'] + (band_rows(colour), slice(None)))
        if phase == ONE and name == 'attn':
            for colour in colours:
                last = DIM_ORDER[colour][TWO]
                publish(tuple(place[d] if d == last else slice(None) for d in range(THREE)) + (band_rows(colour), slice(None)))

    for colour in colours:
        attn_v[(place[ZERO], place[ONE], place[TWO]) + (band_rows(colour), slice(None))] = attn_ref[band_rows(colour), :]
        kept = [place[d] for d in range(THREE) if d != DIM_ORDER[colour][TWO]]
        planes_ref[(colour, kept[ZERO], kept[ONE])] = ffn_ref[band_rows(colour), :]
    vec_out[place[ZERO], place[ONE], place[TWO]] = vec_ref[ALL]
    meet_neighbours(place)
    names = ('attn', 'vec', 'ffn')
    for name in names:
        send_near(name, ZERO)
    for phase in range(THREE):
        for name in names:
            pass_on(name, phase)
        for name in names:
            complete(name, phase)
    for copy in finals:
        copy.wait_recv()
    for copy in net.started:
        copy.wait_send()
    for copy in stores:
        copy.wait()


def gather_params(attn_w, ffn_w, vec_rows):
    rows, width = attn_w.shape
    full = (SIDE, SIDE, SIDE, rows, width)
    n_copies = COLOURS * (4 * TWO + 6 * THREE) + 4 * THREE + COLOURS * 5
    vmem = pl.BlockSpec(memory_space=pltpu.VMEM)
    return pl.pallas_call(
        ag_kernel,
        in_specs=[vmem] * THREE, out_specs=[pl.BlockSpec(memory_space=pl.ANY), vmem, vmem],
        out_shape=[jax.ShapeDtypeStruct(full, BF16), jax.ShapeDtypeStruct((COLOURS, SIDE, SIDE, rows // (TWO * COLOURS), width), BF16),
                   jax.ShapeDtypeStruct((SIDE, SIDE, SIDE) + vec_rows.shape, F32)],
        scratch_shapes=[pltpu.VMEM(full, BF16), pltpu.SemaphoreType.DMA((n_copies,)), pltpu.SemaphoreType.DMA((n_copies,)), pltpu.SemaphoreType.DMA((COLOURS * 5,))],
        compiler_params=pltpu.CompilerParams(collective_id=TWO, has_side_effects=True, vmem_limit_bytes=VMEM_BYTES),
        cost_estimate=pl.CostEstimate(flops=10 ** 9, bytes_accessed=4 * rows * width * SIDE ** THREE, transcendentals=ZERO),
        name='gather_params',
    )(attn_w, ffn_w, vec_rows)


class LastPhase:
    def __init__(self, planes, out, near, far, send_sem, recv_sem, load_sem):
        self.planes, self.out, self.near, self.far = planes, out, near, far
        self.send_sem, self.recv_sem, self.load_sem = send_sem, recv_sem, load_sem
        self.core, self.chip, self.place = lax.axis_index('dp'), lax.axis_index('fsdp'), torus_place()
        self.band = planes.shape[THREE]

    @staticmethod
    def scratch_shapes(planes):
        colours, side, _, band, width = planes.shape
        sems = [pltpu.SemaphoreType.DMA((11 * COLOURS,)), pltpu.SemaphoreType.DMA((11 * COLOURS,)), pltpu.SemaphoreType.DMA((5 * COLOURS,))]
        return [pltpu.VMEM((colours, TWO, side, side, band, width), BF16), pltpu.VMEM((colours, TWO, side // TWO, side, band, width), BF16)] + sems

    def remote(self, i, src, dst, device):
        return pltpu.make_async_remote_copy(src_ref=src, dst_ref=dst, send_sem=self.send_sem.at[i], recv_sem=self.recv_sem.at[i], device_id=device, device_id_type=MESH_ID)

    def ring(self, colour, direction):
        device = (self.core, chip_at(self.place, DIM_ORDER[colour][TWO], ONE - TWO * direction))
        i = 11 * colour + THREE * direction
        got = self.near.at[colour, direction]
        near = [self.remote(i + n, self.planes.at[colour, pl.ds(TWO * half, TWO)], got.at[pl.ds(TWO * half, TWO)], device) for n, half in enumerate((direction, ONE - direction))]
        return near + [self.remote(i + TWO, got.at[pl.ds(TWO * direction, TWO)], self.far.at[colour, direction], device)]

    def shares(self, colour):
        last = DIM_ORDER[colour][TWO]
        rows = pl.ds(pl.multiple_of((self.core * COLOURS + colour) * self.band, self.band), self.band)
        views = [(self.planes.at[colour], ZERO, None)]
        views += [(self.near.at[colour, direction], TWO * direction - ONE, None) for direction in range(TWO)]
        views += [(self.far.at[colour, direction], TWO, direction) for direction in range(TWO)]
        out = []
        for n, (src, shift, half) in enumerate(views):
            where = [slice(None)] * THREE
            where[last] = lax.rem(self.place[last] + shift + SIDE, SIDE)
            if half is not None:
                where[min(d for d in range(THREE) if d != last)] = pl.ds(TWO * half, TWO)
            dst = self.out.at[tuple(where) + (rows, slice(None))]
            out.append((self.remote(11 * colour + 6 + n, src, dst, (ONE - self.core, self.chip)), pltpu.make_async_copy(src, dst, self.load_sem.at[5 * colour + n])))
        return out

    def share(self, colour, which):
        for n in which:
            give, keep = self.shares(colour)[n]
            give.start()
            keep.start()

    def begin(self):
        for colour in range(COLOURS):
            for direction in range(TWO):
                for copy in self.ring(colour, direction)[:TWO]:
                    copy.start()
        for colour in range(COLOURS):
            self.share(colour, (ZERO,))

    def pass_on(self):
        for colour in range(COLOURS):
            for direction in range(TWO):
                first, _, far = self.ring(colour, direction)
                first.wait_recv()
                far.start()
        for colour in range(COLOURS):
            for direction in range(TWO):
                self.ring(colour, direction)[ONE].wait_recv()
            self.share(colour, (ONE, TWO))

    def complete(self):
        for colour in range(COLOURS):
            for direction in range(TWO):
                self.ring(colour, direction)[TWO].wait_recv()
            self.share(colour, (THREE, 4))

    def end(self):
        for colour in range(COLOURS):
            for give, keep in self.shares(colour):
                give.wait_recv()
                give.wait_send()
                keep.wait()
            for direction in range(TWO):
                for copy in self.ring(colour, direction):
                    copy.wait_send()


def dot(lhs, rhs, contract=((ONE,), (ZERO,))):
    return lax.dot_general(lhs, rhs, (contract, ((), ())), preferred_element_type=F32)


def dot_nt(lhs, rhs):
    return dot(lhs, rhs, ((ONE,), (ONE,)))


def dot_tn(lhs, rhs):
    return dot(lhs, rhs, ((ZERO,), (ZERO,)))


def norm_rows(resid, gain, shift):
    mean = jnp.mean(resid, axis=-ONE, keepdims=True)
    centred = resid - mean
    inv_std = lax.rsqrt(jnp.mean(centred * centred, axis=-ONE, keepdims=True) + LN_EPS)
    normed = centred * inv_std
    return (normed * gain + shift).astype(BF16), normed, inv_std


def norm_rows_bwd(d_out, normed, inv_std, gain):
    d_norm = d_out * gain
    return inv_std * (d_norm - jnp.mean(d_norm, axis=-ONE, keepdims=True) - normed * jnp.mean(d_norm * normed, axis=-ONE, keepdims=True))


def col_sum(values):
    return jnp.sum(values, axis=ZERO, keepdims=True)


def lane_row(head, dtype=BF16):
    lane = lax.broadcasted_iota(jnp.int32, (ONE, PAIR), ONE)
    return jnp.where((lane >= HEAD_DIM * head) & (lane < HEAD_DIM * (head + ONE)), 1.0, 0.0).astype(dtype)


def spare_lane(head):
    lane = lax.broadcasted_iota(jnp.int32, (ONE, PAIR), ONE)
    return jnp.where(lane == HEAD_DIM * (ONE - head), 1.0, 0.0)


def mask_fill(n_rows, n_valid):
    row = lax.broadcasted_iota(jnp.int32, (n_rows, PAIR), ZERO)
    return jnp.where(row >= n_valid, MASK_FILL, 0.0)


def head_masks(pair_q, pair_k, head, fill):
    q_f = pair_q * lane_row(head) + spare_lane(head).astype(BF16)
    k_f = pair_k * lane_row(head) + (fill * spare_lane(head)).astype(BF16)
    return q_f, k_f


def half_only(pair, head):
    return pair * lane_row(head)


def join_halves(first, second):
    lane = lax.broadcasted_iota(jnp.int32, first.shape, ONE)
    return jnp.where(lane < HEAD_DIM, first, second)


def score_blocks(n_heads, n_q, n_k, causal, step):
    if not causal:
        return [(head, ZERO, n_q, n_k) for head in range(n_heads)]
    return [(head, first, step, first + step) for head in range(n_heads) for first in range(ZERO, n_q, step)]


def scores_t(q_f, k_f, causal, first):
    s_t = dot_nt(k_f, q_f)
    if causal:
        key_i = lax.broadcasted_iota(jnp.int32, s_t.shape, ZERO)
        qry_i = lax.broadcasted_iota(jnp.int32, s_t.shape, ONE) + first
        s_t = jnp.where(key_i <= qry_i, s_t, MASK_FILL)
    return s_t


def pair_of(group, head):
    return group[:, head // TWO * PAIR:(head // TWO + ONE) * PAIR]


def masked_pairs(q_g, k_g, n_valid):
    fill = mask_fill(k_g.shape[ZERO], n_valid)
    cache = {}

    def get(head):
        if head not in cache:
            cache[head] = head_masks(pair_of(q_g, head), pair_of(k_g, head), head % TWO, fill)
        return cache[head]

    return get


def stack_heads(parts, n_heads):
    return jnp.concatenate([jnp.concatenate(parts[head], axis=ONE) for head in range(n_heads)], axis=ZERO)


def run_ahead(blocks, produce, transform, consume, delay):
    ahead = produce(blocks[ZERO])
    waiting = []
    for i, block in enumerate(blocks):
        now = ahead
        if i + ONE < len(blocks):
            ahead = produce(blocks[i + ONE])
        waiting.append((block, transform(block, now)))
        if len(waiting) > delay:
            consume(*waiting.pop(ZERO))
    for item in waiting:
        consume(*item)


def attend_group(q_g, k_g, v_g, n_valid, causal, lse_ref):
    n_heads = GROUP // HEAD_DIM
    o_parts = [[] for _ in range(n_heads)]
    v_t = v_g.T
    masked = masked_pairs(q_g, k_g, n_valid)

    def produce(block):
        head, first, n_q, n_k = block
        q_f, k_f = masked(head)
        return scores_t(q_f[first:first + n_q], k_f[:n_k], causal, first)

    def transform(block, s_t):
        head, first, n_q, n_k = block
        top = jnp.max(s_t, axis=ZERO, keepdims=True)
        e_t = jnp.exp(s_t - top)
        total = jnp.sum(e_t, axis=ZERO, keepdims=True)
        lse_ref[ZERO, ZERO, head // TWO, head % TWO:head % TWO + ONE, first:first + n_q] = top + jnp.log(total)
        return (e_t * (1.0 / total)).astype(BF16)

    def consume(block, p_t):
        head, first, n_q, n_k = block
        o_parts[head].append(dot(v_t[HEAD_DIM * head:HEAD_DIM * (head + ONE), :n_k], p_t))

    run_ahead(score_blocks(n_heads, q_g.shape[ZERO], k_g.shape[ZERO], causal, 128), produce, transform, consume, TWO)
    return stack_heads(o_parts, n_heads).T.astype(BF16)


def attend_group_bwd(d_o, q_g, k_g, v_g, n_valid, causal, lse_ref):
    n_heads = q_g.shape[ONE] // HEAD_DIM
    k_t = k_g.T
    dq_t, dk_h, dv_h = [[] for _ in range(n_heads)], [None] * n_heads, [None] * n_heads
    masked = masked_pairs(q_g, k_g, n_valid)
    v_half = {}

    def produce(block):
        head, first, n_q, n_k = block
        q_f, k_f = masked(head)
        if head not in v_half:
            v_half[head] = half_only(pair_of(v_g, head), head % TWO)
        rows = slice(first, first + n_q)
        return scores_t(q_f[rows], k_f[:n_k], causal, first), dot_nt(v_half[head][:n_k], pair_of(d_o, head)[rows])

    def transform(block, products):
        head, first, n_q, n_k = block
        s_t, dp_t = products
        p_t = jnp.exp(s_t - lse_ref[head // TWO, head % TWO:head % TWO + ONE, first:first + n_q])
        weighted = p_t * dp_t
        return p_t.astype(BF16), (weighted - p_t * jnp.sum(weighted, axis=ZERO, keepdims=True)).astype(BF16)

    def grow(old, new):
        if old is None:
            return new
        n_old = old.shape[ZERO]
        return old + new if n_old == new.shape[ZERO] else jnp.concatenate([old + new[:n_old], new[n_old:]], axis=ZERO)

    def consume(block, operands):
        head, first, n_q, n_k = block
        p_b, ds_t = operands
        rows = slice(first, first + n_q)
        dv_h[head] = grow(dv_h[head], dot(p_b, pair_of(d_o, head)[rows]))
        dk_h[head] = grow(dk_h[head], dot(ds_t, pair_of(q_g, head)[rows]))
        dq_t[head].append(dot(k_t[HEAD_DIM * head:HEAD_DIM * (head + ONE), :n_k], ds_t))

    run_ahead(score_blocks(n_heads, q_g.shape[ZERO], k_g.shape[ZERO], causal, 256), produce, transform, consume, ZERO)
    join = lambda parts: jnp.concatenate([join_halves(parts[h], parts[h + ONE]) for h in range(ZERO, n_heads, TWO)], axis=ONE)
    return stack_heads(dq_t, n_heads).T * 0.125, join(dk_h), join(dv_h)


def attn_fwd_kernel(causal, slots, guest, lens_ref, x_ref, kv_ref, wq_ref, wk_ref, wv_ref, w_all, bias_ref, rows_ref,
                    q_ref, k_ref, v_ref, o_ref, lse_ref, h_ref, normed_ref, inv_ref, o_all, wo_v, load_sem):
    q_row, k_row, v_row, o_row, gain_row, o_mat = slots
    sample, group = pl.program_id(ZERO), pl.program_id(ONE)
    d_model = wo_v.shape[ZERO]
    fetch = pltpu.make_async_copy(w_all.at[pl.ds(o_mat * d_model, d_model), :], wo_v, load_sem)

    @pl.when((sample == ZERO) & (group == ZERO))
    def _():
        fetch.start()

    turn = sample * pl.num_programs(ONE) + group
    if guest is not None:
        for where, steps in ((ZERO, (lambda: meet_neighbours(guest.place), guest.begin)), (THREE, (guest.pass_on,)), (5, (guest.complete,))):
            @pl.when(turn == where)
            def _():
                for step in steps:
                    step()

    x_b, kv_b = x_ref[ALL], kv_ref[ALL]
    q_g = ((dot(x_b, wq_ref[ALL]) + bias_ref[q_row:q_row + ONE, :]) * 0.125).astype(BF16)
    k_g = (dot(kv_b, wk_ref[ALL]) + bias_ref[k_row:k_row + ONE, :]).astype(BF16)
    v_g = (dot(kv_b, wv_ref[ALL]) + bias_ref[v_row:v_row + ONE, :]).astype(BF16)
    q_ref[ALL], k_ref[ALL], v_ref[ALL] = q_g, k_g, v_g
    o_g = attend_group(q_g, k_g, v_g, lens_ref[sample], causal, lse_ref)
    o_ref[ALL] = o_g
    o_all[:, pl.ds(pl.multiple_of(group * GROUP, GROUP), GROUP)] = o_g

    @pl.when((sample == ZERO) & (group == pl.num_programs(ONE) - ONE))
    def _():
        fetch.wait()

    @pl.when(group == pl.num_programs(ONE) - ONE)
    def _():
        resid = x_ref[ALL].astype(F32) + dot(o_all[ALL], wo_v[ALL]) + rows_ref[o_row:o_row + ONE, :]
        h_out, normed, inv_std = norm_rows(resid, rows_ref[gain_row:gain_row + ONE, :], rows_ref[gain_row + ONE:gain_row + TWO, :])
        h_ref[ALL], normed_ref[ALL], inv_ref[ALL] = h_out, normed, inv_std

    if guest is not None:
        @pl.when(turn == pl.num_programs(ZERO) * pl.num_programs(ONE) - ONE)
        def _():
            guest.end()


def attn_forward(x, kv, lens, attn_full, bias_rows, mats, slots, causal, planes=None, full_rows=None):
    d_model = x.shape[-ONE]
    n_batch = lens.shape[ZERO]
    n_q, n_k = x.shape[ZERO] // n_batch, kv.shape[ZERO] // n_batch
    n_groups = d_model // GROUP
    col = lambda mat: pl.BlockSpec((d_model, GROUP), lambda b, g: (mat, g))
    q_blk = pl.BlockSpec((n_q, GROUP), lambda b, g: (b, g))
    k_blk = pl.BlockSpec((n_k, GROUP), lambda b, g: (b, g))
    tok = lambda n: pl.BlockSpec((n, d_model), lambda b, g: (b, ZERO))
    n_heads_g = GROUP // HEAD_DIM
    out_shape = (
        jax.ShapeDtypeStruct(x.shape, BF16), jax.ShapeDtypeStruct(kv.shape, BF16), jax.ShapeDtypeStruct(kv.shape, BF16),
        jax.ShapeDtypeStruct(x.shape, BF16), jax.ShapeDtypeStruct((n_batch, n_groups, n_heads_g // TWO, TWO, n_q), F32),
        jax.ShapeDtypeStruct(x.shape, BF16), jax.ShapeDtypeStruct(x.shape, F32), jax.ShapeDtypeStruct((x.shape[ZERO], ONE), F32))
    kernel = functools.partial(attn_fwd_kernel, causal, slots + (mats[THREE],))
    in_specs = [pl.BlockSpec(memory_space=pltpu.SMEM), tok(n_q), tok(n_k), col(mats[ZERO]), col(mats[ONE]), col(mats[TWO]), pl.BlockSpec(memory_space=pl.ANY),
                pl.BlockSpec((bias_rows.shape[ZERO], GROUP), lambda b, g: (ZERO, g)), pl.BlockSpec(bias_rows.shape, lambda b, g: (ZERO, ZERO))]
    out_specs = [q_blk, k_blk, k_blk, q_blk, pl.BlockSpec((ONE, ONE, n_heads_g // TWO, TWO, n_q), lambda b, g: (b, g, ZERO, ZERO, ZERO)),
                 tok(n_q), tok(n_q), pl.BlockSpec((n_q, ONE), lambda b, g: (b, ZERO))]
    scratch = [pltpu.VMEM((n_q, d_model), BF16), pltpu.VMEM((d_model, d_model), BF16), pltpu.SemaphoreType.DMA]
    args = [lens, x, kv, attn_full, attn_full, attn_full, attn_full, bias_rows, bias_rows]
    params = dict(vmem_limit_bytes=VMEM_BYTES, dimension_semantics=('arbitrary', 'arbitrary'))
    if planes is None:
        body = functools.partial(kernel, None)
    else:
        n_in, n_out, n_own = len(args), len(out_specs), len(scratch)

        def body(*refs):
            ins, held, outs, whole, rest = refs[:n_in], refs[n_in], refs[n_in + ONE:n_in + ONE + n_out], refs[n_in + ONE + n_out], refs[n_in + TWO + n_out:]
            kernel(LastPhase(held, whole, *rest[n_own:]), *ins, *outs, *rest[:n_own])

        in_specs.append(pl.BlockSpec(memory_space=pltpu.VMEM))
        args.append(planes)
        out_specs.append(pl.BlockSpec(memory_space=pl.ANY))
        out_shape += (jax.ShapeDtypeStruct((SIDE, SIDE, SIDE, full_rows // SIDE ** THREE, d_model), BF16),)
        scratch += LastPhase.scratch_shapes(planes)
        params |= dict(collective_id=5, has_side_effects=True)
    return pl.pallas_call(
        body, grid=(n_batch, n_groups), in_specs=in_specs, out_specs=out_specs, out_shape=out_shape, scratch_shapes=scratch,
        compiler_params=pltpu.CompilerParams(**params),
        cost_estimate=pl.CostEstimate(flops=TWO * d_model * d_model * (TWO * x.shape[ZERO] + TWO * kv.shape[ZERO]) + 16 * x.shape[ZERO] * n_k * d_model, bytes_accessed=20 * x.shape[ZERO] * d_model, transcendentals=ZERO),
        name='attn_fwd',
    )(*args)


def attn_bwd_kernel(causal, gain_row, mats, guest, lens_ref, dres_ref, wo_ref, w_all, q_ref, k_ref, v_ref, lse_ref,
                    rows_ref, normed_ref, inv_ref, lhs_refs, rows_out, dres_out, sums_ref, tail_ref, grads_ref,
                    rhs_q, rhs_k, lhs_q, lhs_k, do_v, w_v, grad_v, load_sem, store_sem):
    sample, group = pl.program_id(ZERO), pl.program_id(ONE)
    d_model = wo_ref.shape[ONE]
    n_q, n_k = q_ref.shape[ZERO], k_ref.shape[ZERO]
    last = pl.num_programs(ONE) - ONE
    fetches = [] if causal else [pltpu.make_async_copy(w_all.at[pl.ds(mats[ZERO] * d_model, d_model), :], w_v, load_sem.at[ZERO])]
    hand_on = pltpu.make_async_copy(rhs_q.at[pl.ds(ZERO, THREE)] if causal else rhs_k, rows_out, load_sem.at[ONE])
    dk_all, dv_all = (rhs_q.at[ONE], rhs_q.at[TWO]) if causal else (rhs_k.at[ZERO], rhs_k.at[ONE])
    d_all, dres_all = rhs_q.at[ZERO], rhs_q.at[THREE if causal else ONE]
    places = (lhs_q.at[ZERO], lhs_q.at[ONE]) if causal else (lhs_q.at[ZERO], lhs_k, lhs_q.at[ZERO])
    lhs_fetch = lambda i: pltpu.make_async_copy(lhs_refs[i], places[i], load_sem.at[THREE + i])
    store = lambda buf, mat: pltpu.make_async_copy(grad_v.at[buf], grads_ref.at[pl.ds(pl.multiple_of(mat * d_model, d_model), d_model), :], store_sem.at[buf])

    @pl.when((sample == ZERO) & (group == ZERO))
    def _():
        for fetch in fetches + [lhs_fetch(ZERO), lhs_fetch(ONE)]:
            fetch.start()

    turn = sample * pl.num_programs(ONE) + group
    q_rows = pl.ds(pl.multiple_of(sample * n_q, n_q), n_q)
    k_rows = pl.ds(pl.multiple_of(sample * n_k, n_k), n_k)
    d_o = dot_nt(dres_ref[ALL].astype(BF16), wo_ref[ALL]).astype(BF16)

    def keep(found, first, width):
        here = pl.ds(first, width)
        cols = pl.ds(pl.multiple_of(group * GROUP + first, PAIR), width)
        for i, (full, rows, value) in enumerate(zip((d_all, dk_all, dv_all), (q_rows, k_rows, k_rows), found)):
            sums_ref[ZERO, i:i + ONE, here] = col_sum(value)
            full[rows, cols] = value.astype(BF16)

    if causal:
        keep(attend_group_bwd(d_o, q_ref[ALL], k_ref[ALL], v_ref[ALL], lens_ref[sample], causal, lse_ref.at[ZERO, ZERO]), ZERO, GROUP)
    else:
        do_v[ALL] = d_o

        def one_pair(pair, _):
            guest(ZERO, TWO * turn + pair)
            first = pl.multiple_of(pair * PAIR, PAIR)
            here = pl.ds(first, PAIR)
            keep(attend_group_bwd(do_v[:, here], q_ref[:, here], k_ref[:, here], v_ref[:, here], lens_ref[sample], causal, lse_ref.at[ZERO, ZERO, pl.ds(pair, ONE)]), first, PAIR)
            return ZERO

        lax.fori_loop(ZERO, GROUP // PAIR, one_pair, ZERO)

    @pl.when(group == ZERO)
    def _():
        dres_all[q_rows, :] = dres_ref[ALL].astype(BF16)

    guest(THREE, turn)
    if causal:
        tail_ref[ALL] = jnp.zeros_like(tail_ref)
    else:
        @pl.when((sample == ZERO) & (group == last))
        def _():
            for fetch in fetches:
                fetch.wait()

        @pl.when(group == last)
        def _():
            d_h = dres_ref[ALL] + dot_nt(d_all[q_rows, :], w_v[ALL])
            normed = normed_ref[ALL]
            d_resid = norm_rows_bwd(d_h, normed, inv_ref[ALL], rows_ref[gain_row:gain_row + ONE, :])
            dres_out[ALL] = d_resid
            tail_ref[ZERO, ZERO:ONE, :] = col_sum(d_resid)
            tail_ref[ZERO, ONE:TWO, :] = col_sum(d_h * normed)
            tail_ref[ZERO, TWO:THREE, :] = col_sum(d_h)

    @pl.when(turn == pl.num_programs(ZERO) * pl.num_programs(ONE) - ONE)
    def _():
        hand_on.start()
        guest(TWO, 12)
        lhs_fetch(ZERO).wait()
        if causal:
            lhs_fetch(ONE).wait()

            def square(i, _):
                @pl.when(i >= TWO)
                def _():
                    store(i % TWO, mats[ZERO]).wait()

                grad_v[i % TWO] = dot_tn(lhs_q[i // THREE], rhs_q[i])
                store(i % TWO, mats[ZERO] + i).start()
                return ZERO

            lax.fori_loop(ZERO, 4, square, ZERO)
        else:
            def square_q(i, _):
                @pl.when(i == ONE)
                def _():
                    lhs_fetch(TWO).start()
                    lhs_fetch(TWO).wait()

                grad_v[i] = dot_tn(lhs_q[ZERO], rhs_q[i])
                store(i, mats[ZERO] + THREE * i).start()
                return ZERO

            def square_k(i, _):
                store(i, mats[ONE]).wait()
                grad_v[i] = dot_tn(lhs_k[ALL], rhs_k[i])
                store(i, mats[ONE] + i).start()
                return ZERO

            lax.fori_loop(ZERO, TWO, square_q, ZERO)
            guest(TWO, 13)
            lhs_fetch(ONE).wait()
            lax.fori_loop(ZERO, TWO, square_k, ZERO)
            guest(TWO, 14)
        for buf in range(TWO):
            store(buf, mats[ZERO]).wait()
        hand_on.wait()


def scatter_guest(scatter, plan, parity, position):
    steps = dict(end=scatter.end) | {('relay', p): functools.partial(scatter.relay, p) for p in range(THREE)}
    steps |= {('settle', p): functools.partial(scatter.settle, p) for p in range(THREE)} | {turn: functools.partial(scatter.absorb, turn) for turn in range(SIDE)}
    if parity == TWO:
        for name in plan.get(position, ()):
            steps[name]()
        return
    if parity == THREE:
        @pl.when(position == 5)
        def _():
            for name in plan['late']:
                steps[name]()
        return
    if parity == ZERO:
        @pl.when(position == ZERO)
        def _():
            meet_neighbours(scatter.place)
            scatter.begin()
    for where, names in plan.items():
        if where != 'late' and where < 12:
            @pl.when(position == where)
            def _():
                for name in names:
                    steps[name]()


def no_guest(parity, position):
    pass


def attn_backward(dres, q, k, v, lse, lens, attn_full, bias_rows, mats, causal, lhs_list, g_rows=None, scale=None, gain_row=ZERO, normed=None, inv_std=None, grads=None):
    d_model = q.shape[-ONE]
    n_batch = lens.shape[ZERO]
    n_q, n_k = q.shape[ZERO] // n_batch, k.shape[ZERO] // n_batch
    n_groups = d_model // GROUP
    row = lambda mat: pl.BlockSpec((GROUP, d_model), lambda b, g: (mat * n_groups + g, ZERO))
    q_blk = pl.BlockSpec((n_q, GROUP), lambda b, g: (b, g))
    k_blk = pl.BlockSpec((n_k, GROUP), lambda b, g: (b, g))
    tok = lambda n: pl.BlockSpec((n, d_model), lambda b, g: (b, ZERO))
    n_heads_g = GROUP // HEAD_DIM
    anywhere = pl.BlockSpec(memory_space=pl.ANY)
    in_specs = [pl.BlockSpec(memory_space=pltpu.SMEM), tok(n_q), row(mats[THREE]), anywhere, q_blk, k_blk, k_blk,
                pl.BlockSpec((ONE, ONE, n_heads_g // TWO, TWO, n_q), lambda b, g: (b, g, ZERO, ZERO, ZERO)), pl.BlockSpec(bias_rows.shape, lambda b, g: (ZERO, ZERO))]
    args = [lens, dres, attn_full, attn_full, q, k, v, lse, bias_rows]
    tail_shape = jax.ShapeDtypeStruct((n_batch, 8, d_model), F32)
    out_shape = [jax.ShapeDtypeStruct((THREE,) + q.shape if causal else (TWO,) + k.shape, BF16)]
    out_specs = [anywhere]
    if not causal:
        late = dict(pipeline_mode=pl.Buffered(ONE))
        in_specs += [pl.BlockSpec((n_q, d_model), lambda b, g: (b, ZERO), **late), pl.BlockSpec((n_q, ONE), lambda b, g: (b, ZERO), **late)]
        args += [normed, inv_std]
        out_shape.append(jax.ShapeDtypeStruct(q.shape, F32))
        out_specs.append(tok(n_q))
    n_lhs_at = len(args)
    args += list(lhs_list)
    in_specs += [anywhere] * len(lhs_list)
    out_shape += [tail_shape, tail_shape, jax.ShapeDtypeStruct(attn_full.shape, F32)]
    out_specs += [pl.BlockSpec((ONE, 8, GROUP), lambda b, g: (b, ZERO, g)), pl.BlockSpec((ONE, 8, d_model), lambda b, g: (b, ZERO, ZERO)), anywhere]
    held = lambda count, n: pltpu.VMEM((count, n_batch * n, d_model), BF16)
    own = [held(4, n_q), held(TWO, n_q)] if causal else [held(TWO, n_q), held(TWO, n_k), held(ONE, n_q), pltpu.VMEM((n_batch * n_k, d_model), BF16)]
    own += [] if causal else [pltpu.VMEM((n_q, GROUP), BF16)]
    own += [] if causal else [pltpu.VMEM((d_model, d_model), BF16)]
    own += [pltpu.VMEM((TWO, d_model, d_model), F32), pltpu.SemaphoreType.DMA((6,)), pltpu.SemaphoreType.DMA((TWO,))]
    kernel = functools.partial(attn_bwd_kernel, causal, gain_row, mats)
    params = dict(vmem_limit_bytes=VMEM_BYTES, dimension_semantics=('arbitrary', 'arbitrary'))
    aliases = {}
    if causal:
        args.append(grads)
        in_specs.append(anywhere)
        aliases = {len(args) - ONE: len(out_shape) - ONE}
    else:
        args.append(as_torus(g_rows))
        in_specs.append(anywhere)
        n_rows = args[-ONE].shape[THREE]
        out_shape.append(jax.ShapeDtypeStruct((n_rows, d_model), F32))
        out_specs.append(anywhere)
        params |= dict(collective_id=THREE, has_side_effects=True, vmem_limit_bytes=67043328)
    scratch = own + ([] if causal else Scatter.scratch_shapes([n_rows]))
    n_in, n_out, n_own = len(args), len(out_shape), len(own)

    def body(*refs):
        ins, outs, rest = refs[:n_in], refs[n_in:n_in + n_out], refs[n_in + n_out:]
        lhs_refs, mine = ins[n_lhs_at:-ONE], rest[:n_own]
        if causal:
            rows_out, sums, tail, grads_ref = outs
            kernel(no_guest, *ins[:n_lhs_at], None, None, lhs_refs, rows_out, None, sums, tail, grads_ref, mine[ZERO], None, mine[ONE], None, None, None, *mine[TWO:])
        else:
            rows_out, dres_out, sums, tail, grads_ref, total = outs
            scatter = Scatter(scale, [(ins[-ONE], ZERO, n_rows)], [total], rest[n_own:])
            kernel(functools.partial(scatter_guest, scatter, CROSS_PLAN), *ins[:n_lhs_at], lhs_refs, rows_out, dres_out, sums, tail, grads_ref, *mine)

    return pl.pallas_call(
        body, grid=(n_batch, n_groups), in_specs=in_specs, out_specs=out_specs, out_shape=out_shape, scratch_shapes=scratch, input_output_aliases=aliases,
        compiler_params=pltpu.CompilerParams(**params),
        cost_estimate=pl.CostEstimate(flops=TWO * d_model * d_model * (TWO * q.shape[ZERO] + TWO * k.shape[ZERO]) + 40 * q.shape[ZERO] * n_k * d_model, bytes_accessed=20 * q.shape[ZERO] * d_model, transcendentals=ZERO),
        name='attn_bwd',
    )(*args)


def ffn_kernel(n_blocks, h_ref, dy_ref, up_ref, down_ref, rows_ref, bias_ref, normed_ref, inv_ref,
               y_ref, grad_ref, dres2_ref, tail_ref, upsum_ref, left_all, right_all):
    step = pl.program_id(ZERO)
    block, d_model = h_ref.shape
    n_square = left_all.shape[TWO] // d_model

    @pl.when(step < n_blocks)
    def _():
        rows = pl.ds(pl.multiple_of(step * block, block), block)
        h_b = h_ref[ALL]
        right_all[ZERO, rows, :] = h_b
        up = dot_nt(h_b, up_ref[ALL]) + bias_ref[ALL]
        cdf = 0.5 * (1.0 + lax.erf(up * 0.7071067811865476))
        gelu = (up * cdf).astype(BF16)
        slope = cdf + up * (0.3989422804014327 * jnp.exp(-0.5 * up * up))
        left_all[ONE, rows, :] = gelu
        resid = h_b.astype(F32) + dot(gelu, down_ref[ALL]) + rows_ref[8:9, :]
        y_b, normed3, inv3 = norm_rows(resid, rows_ref[13:14, :], rows_ref[14:15, :])
        y_ref[ALL] = y_b
        dy = dy_ref[ALL].astype(F32)
        d_res3 = norm_rows_bwd(dy, normed3, inv3, rows_ref[13:14, :])
        d_res3_b = d_res3.astype(BF16)
        right_all[ONE, rows, :] = d_res3_b
        d_up = dot_nt(d_res3_b, down_ref[ALL]) * slope
        d_up_b = d_up.astype(BF16)
        left_all[ZERO, rows, :] = d_up_b
        d_h2 = d_res3 + dot(d_up_b, up_ref[ALL])
        normed2 = normed_ref[ALL]
        d_res2 = norm_rows_bwd(d_h2, normed2, inv_ref[ALL], rows_ref[11:12, :])
        dres2_ref[ALL] = d_res2
        tail = jnp.concatenate([col_sum(d_res2), col_sum(d_res3), col_sum(d_h2 * normed2), col_sum(d_h2), col_sum(dy * normed3), col_sum(dy),
                                jnp.zeros((TWO, dy.shape[ONE]), F32)], axis=ZERO)
        up_sum = col_sum(d_up)

        @pl.when(step == ZERO)
        def _():
            tail_ref[ALL] = tail
            upsum_ref[ALL] = up_sum

        @pl.when(step > ZERO)
        def _():
            tail_ref[ALL] += tail
            upsum_ref[ALL] += up_sum

    square = step - n_blocks
    cols = pl.ds(pl.multiple_of(lax.rem(square + TWO * n_square, n_square) * d_model, d_model), d_model)

    @pl.when(square >= ZERO)
    def _():
        which = square // n_square
        grad_ref[ALL] = dot_tn(left_all[which, :, cols], right_all[which])


def ffn_both(h2, dy, ffn_full, bias_rows, up_bias, normed2, inv2, block=256):
    n_tok, d_model = h2.shape
    ffn_dim = ffn_full.shape[ZERO] // TWO
    n_blocks = n_tok // block
    n_steps = n_blocks + ffn_full.shape[ZERO] // d_model
    at = lambda i: jnp.minimum(i, n_blocks - ONE)
    tok = pl.BlockSpec((block, d_model), lambda i: (at(i), ZERO))
    once = lambda shape, idx: pl.BlockSpec(shape, lambda i: idx, pipeline_mode=pl.Buffered(ONE))
    return pl.pallas_call(
        functools.partial(ffn_kernel, n_blocks), grid=(n_steps,),
        in_specs=[tok, tok, once((ffn_dim, d_model), (ZERO, ZERO)), once((ffn_dim, d_model), (ONE, ZERO)), once(bias_rows.shape, (ZERO, ZERO)), once((ONE, ffn_dim), (ZERO, ZERO)),
                  tok, pl.BlockSpec((block, ONE), lambda i: (at(i), ZERO))],
        out_specs=[tok, pl.BlockSpec((d_model, d_model), lambda i: (jnp.maximum(i - n_blocks, ZERO), ZERO)), tok, pl.BlockSpec((8, d_model), lambda i: (ZERO, ZERO)), pl.BlockSpec((ONE, ffn_dim), lambda i: (ZERO, ZERO))],
        out_shape=[jax.ShapeDtypeStruct(h2.shape, BF16), jax.ShapeDtypeStruct(ffn_full.shape, F32), jax.ShapeDtypeStruct(h2.shape, F32),
                   jax.ShapeDtypeStruct((8, d_model), F32), jax.ShapeDtypeStruct((ONE, ffn_dim), F32)],
        scratch_shapes=[pltpu.VMEM((TWO, n_tok, ffn_dim), BF16), pltpu.VMEM((TWO, n_tok, d_model), BF16)],
        compiler_params=pltpu.CompilerParams(vmem_limit_bytes=VMEM_BYTES, dimension_semantics=('arbitrary',)),
        cost_estimate=pl.CostEstimate(flops=12 * n_tok * d_model * ffn_dim, bytes_accessed=30 * n_tok * d_model, transcendentals=ZERO),
        name='ffn_both',
    )(h2, dy, ffn_full, ffn_full, bias_rows, up_bias, normed2, inv2)


CROSS_PLAN = {ONE: (ZERO,), THREE: (ONE, TWO), 5: (('relay', ZERO),), 6: (THREE,), 9: (('settle', ZERO),), 11: (('relay', ONE),), 'late': (), 12: (('settle', ONE),), 13: (('relay', TWO),), 14: (('settle', TWO), 'end')}


def solution(mesh):
    n_fsdp = mesh.shape['fsdp']
    n_dp = mesh.shape['dp']
    batch_axes = ('dp', 'fsdp')
    act_spec = P(batch_axes, None, None)
    len_spec = P(batch_axes)
    row_spec = P('fsdp', None)
    vec_spec = P('fsdp')

    def device_step(dec_in, enc_out, src_lens, tgt_lens, y_cot, attn_w, ffn_w, vec_params):
        d_model, n_vec = dec_in.shape[TWO], vec_params.shape[ZERO]
        scale = 1.0 / (dec_in.shape[ZERO] * dec_in.shape[ONE] * n_fsdp * n_dp)
        x, enc, dy = (a.reshape(-ONE, d_model) for a in (dec_in, enc_out, y_cot))
        vec_rows = jnp.pad(vec_params.astype(F32), (ZERO, 16 * LANES - n_vec)).reshape(16, LANES)
        attn_tiles, planes, vec_tiles = gather_params(attn_w, ffn_w, vec_rows)
        attn_full = attn_tiles.reshape(-ONE, d_model)
        vec_f = vec_tiles.reshape(n_fsdp, 16, LANES)[:, :TWO].reshape(n_fsdp, TWO * LANES)[:, :n_vec].reshape(-ONE)
        bias_rows = jnp.pad(vec_f[:15 * d_model].reshape(15, d_model), ((ZERO, ONE), (ZERO, ZERO)))
        up_bias = vec_f[15 * d_model:].reshape(ONE, -ONE)
        q1, k1, v1, o1, lse1, h1, normed1, inv1 = attn_forward(x, x, tgt_lens, attn_full, bias_rows, (ZERO, ONE, TWO, THREE), (ZERO, ONE, TWO, THREE, 9), True)
        q2, k2, v2, o2, lse2, h2, normed2, inv2, ffn_tiles = attn_forward(h1, enc, src_lens, attn_full, bias_rows, (4, 5, 6, 7), (4, 5, 6, 7, 11), False, planes, ffn_w.shape[ZERO] * n_fsdp)
        ffn_full = ffn_tiles.reshape(-ONE, d_model)
        y, g_ffn, d_res2, ffn_tail, up_sum = ffn_both(h2, dy, ffn_full, bias_rows, up_bias, normed2, inv2)
        d_cross, d_res1, sums2, tail2, grads, ffn_out = attn_backward(d_res2, q2, k2, v2, lse2, src_lens, attn_full, bias_rows, (4, 5, 6, 7), False, (h1, enc, o2), g_ffn, scale, 9, normed1, inv1)
        d_self, sums1, _, grads = attn_backward(d_res1, q1, k1, v1, lse1, tgt_lens, attn_full, bias_rows, (ZERO, ONE, TWO, THREE), True, (x, o1), grads=grads)
        s1, s2, t2 = jnp.sum(sums1, axis=ZERO), jnp.sum(sums2, axis=ZERO), jnp.sum(tail2, axis=ZERO)
        g_vec = jnp.concatenate([s1[ZERO:THREE].reshape(-ONE), t2[ZERO], s2[ZERO:THREE].reshape(-ONE), ffn_tail[ZERO], ffn_tail[ONE], t2[ONE], t2[TWO], ffn_tail[TWO], ffn_tail[THREE], ffn_tail[4], ffn_tail[5], up_sum[ZERO]])
        g_rows = jnp.pad(g_vec.reshape(n_fsdp, ONE, n_vec), ((ZERO, ZERO), (ZERO, 7), (ZERO, TWO * LANES - n_vec))).reshape(n_fsdp * 8, -ONE)
        attn_out, vec_out, d_x, d_enc = scatter_grads(grads, g_rows, scale, attn_full, (ZERO, ONE, TWO, 5, 6), d_res1, d_self, d_cross)
        return y.reshape(dec_in.shape), d_x.reshape(dec_in.shape), d_enc.reshape(enc_out.shape), attn_out, ffn_out, vec_out[ZERO, :n_vec]

    return jax.shard_map(device_step, mesh=mesh, in_specs=(act_spec, act_spec, len_spec, len_spec, act_spec, row_spec, row_spec, vec_spec), out_specs=(act_spec, act_spec, act_spec, row_spec, row_spec, vec_spec), check_vma=False)
```

```python
import functools
import jax
import jax.numpy as jnp
from jax import lax
from jax.experimental import pallas as pl
from jax.experimental.pallas import tpu as pltpu
from jax.sharding import PartitionSpec as P

ZERO, ONE, TWO, THREE = range(4)
ALL = ...
HEAD_DIM = 64
LN_EPS = 1e-5
MASK_FILL = -1e30
VMEM_BYTES = 60 * 1024 * 1024
F32 = jnp.float32
BF16 = jnp.bfloat16
GROUP = 256
PAIR = 128


SIDE = 4
LANES = 128
COLOURS = THREE
STAGES = TWO
DIM_ORDER = ((TWO, ONE, ZERO), (ONE, ZERO, TWO), (ZERO, TWO, ONE))
MESH_ID = pl.DeviceIdType.MESH


def torus_place():
    chip = lax.axis_index('fsdp')
    return (chip // (SIDE * SIDE), lax.rem(chip // SIDE, SIDE), lax.rem(chip, SIDE))


def chip_at(place, dim, shift):
    moved = [lax.rem(p + shift + SIDE, SIDE) if d == dim else p for d, p in enumerate(place)]
    return (moved[ZERO] * SIDE + moved[ONE]) * SIDE + moved[TWO]


def meet_neighbours(place):
    barrier = pltpu.get_barrier_semaphore()
    core = lax.axis_index('dp')
    for dim in range(THREE):
        for shift in (ONE, -ONE):
            pl.semaphore_signal(barrier, inc=ONE, device_id=(core, chip_at(place, dim, shift)), device_id_type=MESH_ID)
    pl.semaphore_signal(barrier, inc=ONE, device_id=(ONE - core, lax.axis_index('fsdp')), device_id_type=MESH_ID)
    pl.semaphore_wait(barrier, 7)


class Scatter:
    def __init__(self, scale, sources, outs, scratch):
        self.scale, self.outs = scale, outs
        self.sources = [(ref, pl.ds(first, n)) for ref, first, n in sources]
        (self.acc, g1, d1, g2, d2, g3, d3, self.send_sem, self.recv_sem, self.load_sem, self.stage) = scratch
        self.got, self.far = (g1, g2, g3), (d1, d2, d3)
        self.heights = [n for _, _, n in sources]
        self.offsets = [sum(self.heights[:i]) for i in range(len(sources))]
        self.n_low = self.heights[ZERO] // TWO
        self.core, self.chip, self.place = lax.axis_index('dp'), lax.axis_index('fsdp'), torus_place()
        self.pieces = [(d, colour) for d in (TWO, ONE, THREE, ZERO) for colour in range(COLOURS)]

    @staticmethod
    def scratch_shapes(heights):
        h = sum(heights)
        n_low = heights[ZERO] // TWO
        buf = lambda *shape: pltpu.VMEM((COLOURS,) + shape + (LANES,), F32)
        n = Scatter.n_copies(len(heights))
        return [buf(SIDE, SIDE, SIDE, h), buf(TWO, SIDE, SIDE, h), buf(TWO, TWO, SIDE, h), buf(TWO, SIDE, h), buf(TWO, TWO, h), buf(TWO, h), buf(TWO, max(n_low, h - n_low)),
                pltpu.SemaphoreType.DMA((n,)), pltpu.SemaphoreType.DMA((n,)), pltpu.SemaphoreType.DMA((THREE + COLOURS, len(heights))),
                pltpu.VMEM((STAGES, SIDE, SIDE, h, LANES), F32)]

    @staticmethod
    def n_copies(n_parts):
        return 12 * n_parts + COLOURS * 18 + COLOURS * n_parts

    def parts(self, colour):
        return range(len(self.sources) if colour == ZERO else ONE)

    def height(self, colour):
        return sum(self.heights[i] for i in self.parts(colour))

    def remote(self, i, src, dst, device):
        return pltpu.make_async_remote_copy(src_ref=src, dst_ref=dst, send_sem=self.send_sem.at[i], recv_sem=self.recv_sem.at[i], device_id=device, device_id_type=MESH_ID)

    def columns(self, of_core, colour, part=ZERO):
        return pl.ds(pl.multiple_of((of_core * COLOURS + colour if part == ZERO else of_core) * LANES, LANES), LANES)

    def slot(self, d, colour):
        dim = DIM_ORDER[colour][ZERO]
        where = [slice(None)] * THREE
        where[dim] = lax.rem(self.place[dim] + d, SIDE)
        return tuple(where)

    def rows_of(self, part):
        return pl.ds(self.offsets[part], self.heights[part])

    def swaps(self, piece):
        d, colour = self.pieces[piece]
        where = self.slot(d, colour)
        n = len(self.sources)
        return [self.remote(piece * n + i, self.sources[i][ZERO].at[where + (self.sources[i][ONE], self.columns(ONE - self.core, colour, i))],
                            self.acc.at[(colour,) + where + (self.rows_of(i), slice(None))], (ONE - self.core, self.chip)) for i in self.parts(colour)]

    def loads(self, piece):
        d, colour = self.pieces[piece]
        where, buf = self.slot(d, colour), piece % STAGES
        return [pltpu.make_async_copy(self.sources[i][ZERO].at[where + (self.sources[i][ONE], self.columns(self.core, colour, i))],
                                      self.stage.at[buf, :, :, self.rows_of(i), :], self.load_sem.at[buf, i]) for i in self.parts(colour)]

    def split_rows(self, colour, half):
        return pl.ds(ZERO, self.n_low) if half == ZERO else pl.ds(self.n_low, self.height(colour) - self.n_low)

    def block(self, colour, phase, d, half=None):
        order = DIM_ORDER[colour]
        where = [None, None, None]
        for done in order[:phase]:
            where[done] = self.place[done]
        where[order[phase]] = lax.rem(self.place[order[phase]] + d, SIDE)
        for i, rest in enumerate(sorted(order[phase + ONE:])):
            where[rest] = slice(None) if half is None or i > ZERO else pl.ds(TWO * half, TWO)
        rows = self.split_rows(colour, half) if phase == TWO and half is not None else pl.ds(ZERO, self.height(colour))
        return self.acc.at[(colour,) + tuple(where) + (rows, slice(None))]

    def got_half(self, colour, phase, direction, half):
        if phase == TWO:
            return self.got[phase].at[colour, direction, self.split_rows(colour, half), :]
        return self.got_all(colour, phase, direction, pl.ds(TWO * half, TWO))

    def got_all(self, colour, phase, direction, which=slice(None)):
        rows = (pl.ds(ZERO, self.height(colour)), slice(None))
        blocks = ((which, slice(None)), (which,), ())[phase]
        return self.got[phase].at[(colour, direction) + blocks + rows]

    def far_part(self, colour, phase, direction):
        if phase == TWO:
            return self.far[phase].at[colour, direction, pl.ds(ZERO, self.n_low if direction == ZERO else self.height(colour) - self.n_low), :]
        return self.far[phase].at[(colour, direction) + (slice(None),) * (TWO - phase) + (pl.ds(ZERO, self.height(colour)), slice(None))]

    def ring(self, colour, phase, direction):
        shift = ONE - TWO * direction
        device = (self.core, chip_at(self.place, DIM_ORDER[colour][phase], shift))
        i = 12 * len(self.sources) + ((colour * THREE + phase) * TWO + direction) * THREE
        near = shift % SIDE
        return (self.remote(i, self.block(colour, phase, TWO, direction), self.far_part(colour, phase, direction), device),
                self.remote(i + ONE, self.block(colour, phase, near, ONE - direction), self.got_half(colour, phase, direction, ONE - direction), device),
                self.remote(i + TWO, self.block(colour, phase, near, direction), self.got_half(colour, phase, direction, direction), device))

    def gives(self, colour):
        n = len(self.sources)
        base = 12 * n + COLOURS * 18 + colour * n
        done = self.acc.at[colour, self.place[ZERO], self.place[ONE], self.place[TWO]]
        pairs = [(done.at[self.rows_of(i), :], self.outs[i].at[:, self.columns(self.core, colour, i)]) for i in self.parts(colour)]
        return [(self.remote(base + i, src, dst, (ONE - self.core, self.chip)), pltpu.make_async_copy(src, dst, self.load_sem.at[THREE + colour, i])) for i, (src, dst) in enumerate(pairs)]

    def add_into(self, dst, sources, n_lead):
        def body(i, _):
            total = dst[i]
            for src in sources:
                total = total + src[i]
            dst[i] = total
            return ZERO

        if n_lead == TWO:
            lax.fori_loop(ZERO, dst.shape[ZERO], body, ZERO)
        else:
            total = dst[ALL]
            for src in sources:
                total = total + src[ALL]
            dst[ALL] = total


    def begin(self):
        for piece in range(STAGES):
            for copy in self.loads(piece):
                copy.start()
        for piece in range(len(self.pieces)):
            for copy in self.swaps(piece):
                copy.start()

    def absorb(self, turn):
        for piece in range(turn * COLOURS, (turn + ONE) * COLOURS):
            d, colour = self.pieces[piece]
            for copy in self.loads(piece):
                copy.wait()
            for copy in self.swaps(piece):
                copy.wait_recv()
            rows = (pl.ds(ZERO, self.height(colour)), slice(None))
            self.add_into(self.acc.at[(colour,) + self.slot(d, colour) + rows], [self.stage.at[(piece % STAGES, slice(None), slice(None)) + rows]], TWO)
            if piece + STAGES < len(self.pieces):
                for copy in self.loads(piece + STAGES):
                    copy.start()
            if turn == ZERO:
                for direction in range(TWO):
                    self.ring(colour, ZERO, direction)[ZERO].start()
            elif turn < THREE:
                self.ring(colour, ZERO, turn - ONE)[ONE].start()

    def relay(self, phase):
        for colour in range(COLOURS):
            for direction in range(TWO):
                far, _, fed = self.ring(colour, phase, direction)
                far.wait_recv()
                self.add_into(self.block(colour, phase, (ONE - TWO * direction) % SIDE, direction), [self.far_part(colour, phase, direction)], TWO - phase)
            for direction in range(TWO):
                self.ring(colour, phase, direction)[TWO].start()

    def settle(self, phase):
        for colour in range(COLOURS):
            for direction in range(TWO):
                _, own, fed = self.ring(colour, phase, direction)
                own.wait_recv()
                fed.wait_recv()
            self.add_into(self.block(colour, phase, ZERO), [self.got_all(colour, phase, direction) for direction in range(TWO)], TWO - phase)
            if phase < TWO:
                for kind in range(TWO):
                    for direction in range(TWO):
                        self.ring(colour, phase + ONE, direction)[kind].start()
            else:
                done = self.block(colour, TWO, ZERO)
                done[ALL] = done[ALL] * self.scale
                for give, keep in self.gives(colour):
                    keep.start()
                    give.start()

    def end(self):
        for colour in range(COLOURS):
            for give, keep in self.gives(colour):
                give.wait_recv()
                give.wait_send()
                keep.wait()
        for piece in range(len(self.pieces)):
            for copy in self.swaps(piece):
                copy.wait_send()
        for colour in range(COLOURS):
            for phase in range(THREE):
                for direction in range(TWO):
                    for copy in self.ring(colour, phase, direction):
                        copy.wait_send()


def rs_kernel(scale, mats, g_ref, vec_ref, w_all, dres_ref, self_ref, cross_ref, out_ref, vec_out, dx_out, denc_out,
              w_v, dres_v, self_v, cross_v, dx_v, denc_v, load_sem, *scratch):
    scatter = Scatter(scale, [(ref, ZERO, ref.shape[THREE]) for ref in (g_ref, vec_ref)], [out_ref, vec_out], scratch)
    d_model = w_v.shape[ONE]
    step = 256
    loads = [pltpu.make_async_copy(w_all.at[pl.ds(mat * d_model, d_model), :], w_v.at[i], load_sem.at[i]) for i, mat in enumerate(mats)]
    loads += [pltpu.make_async_copy(src, dst, load_sem.at[len(mats) + i]) for i, (src, dst) in enumerate(((dres_ref, dres_v), (self_ref, self_v), (cross_ref, cross_v)))]
    stores = [pltpu.make_async_copy(src, dst, load_sem.at[len(mats) + THREE + i]) for i, (src, dst) in enumerate(((dx_v, dx_out), (denc_v, denc_out)))]

    def input_grads():
        for copy in loads:
            copy.wait()

        def decoder(i, _):
            rows = pl.ds(pl.multiple_of(i * step, step), step)
            total = dres_v[rows, :]
            for n in range(THREE):
                total = total + dot_nt(self_v[n, rows, :], w_v[n])
            dx_v[rows, :] = total.astype(BF16)
            return ZERO

        def encoder(i, _):
            rows = pl.ds(pl.multiple_of(i * step, step), step)
            denc_v[rows, :] = (dot_nt(cross_v[ZERO, rows, :], w_v[THREE]) + dot_nt(cross_v[ONE, rows, :], w_v[4])).astype(BF16)
            return ZERO

        lax.fori_loop(ZERO, dx_v.shape[ZERO] // step, decoder, ZERO)
        stores[ZERO].start()
        lax.fori_loop(ZERO, denc_v.shape[ZERO] // step, encoder, ZERO)
        stores[ONE].start()

    meet_neighbours(scatter.place)
    scatter.begin()
    for turn in range(THREE):
        scatter.absorb(turn)
        if turn == ONE:
            for copy in loads:
                copy.start()
    scatter.relay(ZERO)
    scatter.absorb(THREE)
    input_grads()
    scatter.settle(ZERO)
    for phase in (ONE, TWO):
        scatter.relay(phase)
        scatter.settle(phase)
    scatter.end()
    for copy in stores:
        copy.wait()


def as_torus(rows):
    return rows.reshape(SIDE, SIDE, SIDE, rows.shape[ZERO] // SIDE ** THREE, rows.shape[ONE])


def scatter_grads(g_attn, g_vec, scale, attn_full, mats, d_res, d_self, d_cross):
    sources = [as_torus(g_attn), as_torus(g_vec)]
    heights = [src.shape[THREE] for src in sources]
    d_model = g_attn.shape[ONE]
    anywhere = pl.BlockSpec(memory_space=pl.ANY)
    dx_shape, denc_shape = d_self.shape[ONE:], d_cross.shape[ONE:]
    return pl.pallas_call(
        functools.partial(rs_kernel, scale, mats),
        in_specs=[anywhere] * 6, out_specs=[anywhere] * 4,
        out_shape=[jax.ShapeDtypeStruct((h, src.shape[4]), F32) for h, src in zip(heights, sources)] + [jax.ShapeDtypeStruct(dx_shape, BF16), jax.ShapeDtypeStruct(denc_shape, BF16)],
        scratch_shapes=[pltpu.VMEM((len(mats), d_model, d_model), BF16), pltpu.VMEM(d_res.shape, F32), pltpu.VMEM(d_self.shape, BF16), pltpu.VMEM(d_cross.shape, BF16),
                        pltpu.VMEM(dx_shape, BF16), pltpu.VMEM(denc_shape, BF16), pltpu.SemaphoreType.DMA((len(mats) + 5,))] + Scatter.scratch_shapes(heights),
        compiler_params=pltpu.CompilerParams(collective_id=ONE, has_side_effects=True, vmem_limit_bytes=VMEM_BYTES),
        cost_estimate=pl.CostEstimate(flops=10 ** 9, bytes_accessed=8 * d_model * g_attn.shape[ZERO], transcendentals=ZERO),
        name='scatter_grads',
    )(*sources, attn_full, d_res, d_self, d_cross)


class Gather:
    def __init__(self, send_sem, recv_sem, base=ZERO):
        self.send_sem, self.recv_sem = send_sem, recv_sem
        self.used = base
        self.core, self.chip, self.place = lax.axis_index('dp'), lax.axis_index('fsdp'), torus_place()
        self.sibling = (ONE - self.core, self.chip)
        self.started = []

    def remote(self, src, dst, device):
        i = self.used
        self.used += ONE
        return pltpu.make_async_remote_copy(src_ref=src, dst_ref=dst, send_sem=self.send_sem.at[i], recv_sem=self.recv_sem.at[i], device_id=device, device_id_type=MESH_ID)

    def start(self, copy):
        copy.start()
        self.started.append(copy)

    def ring(self, colour, phase, view, own=None, split=False):
        order = DIM_ORDER[colour]
        dim = order[phase]
        have = sorted(order[:phase])

        def index(shift, half=None):
            where = [self.place[ZERO], self.place[ONE], self.place[TWO]]
            where[dim] = lax.rem(self.place[dim] + shift + SIDE, SIDE)
            for i, h in enumerate(have):
                where[h] = slice(None) if half is None or i > ZERO else pl.ds(TWO * half, TWO)
            return tuple(where)

        out = []
        for direction, shift in enumerate((ONE, -ONE)):
            device = (self.core, chip_at(self.place, dim, shift))
            half = direction if phase == ZERO else None
            near_dst = view(index(ZERO), None)
            if split:
                near = [self.remote(view(index(ZERO, h), None), view(index(ZERO, h), None), device) for h in (direction, ONE - direction)]
            else:
                near = [self.remote(near_dst if own is None else own, near_dst, device)]
            out.append(dict(
                near=near,
                far=self.remote(view(index(-shift, direction), half), view(index(-shift, direction), half), device),
                near_at=index(-shift), far_at=index(TWO, direction)))
        return out


def ag_kernel(attn_ref, ffn_ref, vec_ref, oattn_ref, planes_ref, vec_out, attn_v, send_sem, recv_sem, load_sem):
    net = Gather(send_sem, recv_sem)
    core, place = net.core, net.place
    rows, width = attn_ref.shape
    band = rows // (TWO * COLOURS)
    vec_high = vec_ref.shape[ZERO]
    stores, finals = [], []

    def band_rows(colour):
        return pl.ds(pl.multiple_of((core * COLOURS + colour) * band, band), band)

    def columns(half):
        return slice(None) if half is None else pl.ds(half * (width // TWO), width // TWO)

    def attn_view(colour):
        return lambda where, half: attn_v.at[where + (band_rows(colour), columns(half))]

    def ffn_view(colour):
        last = DIM_ORDER[colour][TWO]
        return lambda where, half: planes_ref.at[(colour,) + tuple(w for d, w in enumerate(where) if d != last) + (slice(None), columns(half))]

    def vec_view(where, half):
        return vec_out.at[where + (slice(None) if half is None else pl.ds(half * (vec_high // TWO), vec_high // TWO), slice(None))]

    colours = range(COLOURS)
    attn_own = [attn_ref.at[band_rows(colour), :] for colour in colours]
    ffn_own = [ffn_ref.at[band_rows(colour), :] for colour in colours]
    rings = {('attn', phase): [net.ring(colour, phase, attn_view(colour), attn_own[colour] if phase == ZERO else None, phase > ZERO) for colour in colours] for phase in range(THREE)}
    rings |= {('ffn', phase): [net.ring(colour, phase, ffn_view(colour), ffn_own[colour] if phase == ZERO else None, phase > ZERO) for colour in colours] for phase in range(TWO)}
    rings |= {('vec', phase): [net.ring(ONE, phase, vec_view, vec_ref if phase == ZERO else None)] for phase in range(THREE)}

    def publish(at):
        keep = pltpu.make_async_copy(attn_v.at[at], oattn_ref.at[at], load_sem.at[len(stores)])
        keep.start()
        stores.append(keep)
        give = net.remote(attn_v.at[at], oattn_ref.at[at], net.sibling)
        net.start(give)
        finals.append(give)

    def send_near(name, phase):
        for ring in rings.get((name, phase), ()):
            for way in ring:
                for copy in way['near']:
                    net.start(copy)

    def pass_on(name, phase):
        for ring in rings.get((name, phase), ()):
            for way in ring:
                way['near'][ZERO].wait_recv()
                net.start(way['far'])
        if phase == TWO and name == 'attn':
            for colour in colours:
                for way in rings[(name, phase)][colour]:
                    way['near'][ONE].wait_recv()
                    publish(way['near_at'] + (band_rows(colour), slice(None)))

    def complete(name, phase):
        for colour, ring in enumerate(rings.get((name, phase), ())):
            for way in ring:
                way['far'].wait_recv()
                if phase == ONE and name != 'vec':
                    way['near'][ONE].wait_recv()
            if phase < TWO and (name, phase + ONE) in rings:
                for way in rings[(name, phase + ONE)][colour]:
                    for copy in way['near']:
                        net.start(copy)
            if phase == TWO and name == 'attn':
                for way in ring:
                    publish(way['far_at'] + (band_rows(colour), slice(None)))
        if phase == ONE and name == 'attn':
            for colour in colours:
                last = DIM_ORDER[colour][TWO]
                publish(tuple(place[d] if d == last else slice(None) for d in range(THREE)) + (band_rows(colour), slice(None)))

    for colour in colours:
        attn_v[(place[ZERO], place[ONE], place[TWO]) + (band_rows(colour), slice(None))] = attn_ref[band_rows(colour), :]
        kept = [place[d] for d in range(THREE) if d != DIM_ORDER[colour][TWO]]
        planes_ref[(colour, kept[ZERO], kept[ONE])] = ffn_ref[band_rows(colour), :]
    vec_out[place[ZERO], place[ONE], place[TWO]] = vec_ref[ALL]
    meet_neighbours(place)
    names = ('attn', 'vec', 'ffn')
    for name in names:
        send_near(name, ZERO)
    for phase in range(THREE):
        for name in names:
            pass_on(name, phase)
        for name in names:
            complete(name, phase)
    for copy in finals:
        copy.wait_recv()
    for copy in net.started:
        copy.wait_send()
    for copy in stores:
        copy.wait()


def gather_params(attn_w, ffn_w, vec_rows):
    rows, width = attn_w.shape
    full = (SIDE, SIDE, SIDE, rows, width)
    n_copies = COLOURS * (4 * TWO + 6 * THREE) + 4 * THREE + COLOURS * 5
    vmem = pl.BlockSpec(memory_space=pltpu.VMEM)
    return pl.pallas_call(
        ag_kernel,
        in_specs=[vmem] * THREE, out_specs=[pl.BlockSpec(memory_space=pl.ANY), vmem, vmem],
        out_shape=[jax.ShapeDtypeStruct(full, BF16), jax.ShapeDtypeStruct((COLOURS, SIDE, SIDE, rows // (TWO * COLOURS), width), BF16),
                   jax.ShapeDtypeStruct((SIDE, SIDE, SIDE) + vec_rows.shape, F32)],
        scratch_shapes=[pltpu.VMEM(full, BF16), pltpu.SemaphoreType.DMA((n_copies,)), pltpu.SemaphoreType.DMA((n_copies,)), pltpu.SemaphoreType.DMA((COLOURS * 5,))],
        compiler_params=pltpu.CompilerParams(collective_id=TWO, has_side_effects=True, vmem_limit_bytes=VMEM_BYTES),
        cost_estimate=pl.CostEstimate(flops=10 ** 9, bytes_accessed=4 * rows * width * SIDE ** THREE, transcendentals=ZERO),
        name='gather_params',
    )(attn_w, ffn_w, vec_rows)


class LastPhase:
    def __init__(self, planes, out, near, far, send_sem, recv_sem, load_sem):
        self.planes, self.out, self.near, self.far = planes, out, near, far
        self.send_sem, self.recv_sem, self.load_sem = send_sem, recv_sem, load_sem
        self.core, self.chip, self.place = lax.axis_index('dp'), lax.axis_index('fsdp'), torus_place()
        self.band = planes.shape[THREE]

    @staticmethod
    def scratch_shapes(planes):
        colours, side, _, band, width = planes.shape
        sems = [pltpu.SemaphoreType.DMA((11 * COLOURS,)), pltpu.SemaphoreType.DMA((11 * COLOURS,)), pltpu.SemaphoreType.DMA((5 * COLOURS,))]
        return [pltpu.VMEM((colours, TWO, side, side, band, width), BF16), pltpu.VMEM((colours, TWO, side // TWO, side, band, width), BF16)] + sems

    def remote(self, i, src, dst, device):
        return pltpu.make_async_remote_copy(src_ref=src, dst_ref=dst, send_sem=self.send_sem.at[i], recv_sem=self.recv_sem.at[i], device_id=device, device_id_type=MESH_ID)

    def ring(self, colour, direction):
        device = (self.core, chip_at(self.place, DIM_ORDER[colour][TWO], ONE - TWO * direction))
        i = 11 * colour + THREE * direction
        got = self.near.at[colour, direction]
        near = [self.remote(i + n, self.planes.at[colour, pl.ds(TWO * half, TWO)], got.at[pl.ds(TWO * half, TWO)], device) for n, half in enumerate((direction, ONE - direction))]
        return near + [self.remote(i + TWO, got.at[pl.ds(TWO * direction, TWO)], self.far.at[colour, direction], device)]

    def shares(self, colour):
        last = DIM_ORDER[colour][TWO]
        rows = pl.ds(pl.multiple_of((self.core * COLOURS + colour) * self.band, self.band), self.band)
        views = [(self.planes.at[colour], ZERO, None)]
        views += [(self.near.at[colour, direction], TWO * direction - ONE, None) for direction in range(TWO)]
        views += [(self.far.at[colour, direction], TWO, direction) for direction in range(TWO)]
        out = []
        for n, (src, shift, half) in enumerate(views):
            where = [slice(None)] * THREE
            where[last] = lax.rem(self.place[last] + shift + SIDE, SIDE)
            if half is not None:
                where[min(d for d in range(THREE) if d != last)] = pl.ds(TWO * half, TWO)
            dst = self.out.at[tuple(where) + (rows, slice(None))]
            out.append((self.remote(11 * colour + 6 + n, src, dst, (ONE - self.core, self.chip)), pltpu.make_async_copy(src, dst, self.load_sem.at[5 * colour + n])))
        return out

    def share(self, colour, which):
        for n in which:
            give, keep = self.shares(colour)[n]
            give.start()
            keep.start()

    def begin(self):
        for colour in range(COLOURS):
            for direction in range(TWO):
                for copy in self.ring(colour, direction)[:TWO]:
                    copy.start()
        for colour in range(COLOURS):
            self.share(colour, (ZERO,))

    def pass_on(self):
        for colour in range(COLOURS):
            for direction in range(TWO):
                first, _, far = self.ring(colour, direction)
                first.wait_recv()
                far.start()
        for colour in range(COLOURS):
            for direction in range(TWO):
                self.ring(colour, direction)[ONE].wait_recv()
            self.share(colour, (ONE, TWO))

    def complete(self):
        for colour in range(COLOURS):
            for direction in range(TWO):
                self.ring(colour, direction)[TWO].wait_recv()
            self.share(colour, (THREE, 4))

    def end(self):
        for colour in range(COLOURS):
            for give, keep in self.shares(colour):
                give.wait_recv()
                give.wait_send()
                keep.wait()
            for direction in range(TWO):
                for copy in self.ring(colour, direction):
                    copy.wait_send()


def dot(lhs, rhs, contract=((ONE,), (ZERO,))):
    return lax.dot_general(lhs, rhs, (contract, ((), ())), preferred_element_type=F32)


def dot_nt(lhs, rhs):
    return dot(lhs, rhs, ((ONE,), (ONE,)))


def dot_tn(lhs, rhs):
    return dot(lhs, rhs, ((ZERO,), (ZERO,)))


def norm_rows(resid, gain, shift):
    mean = jnp.mean(resid, axis=-ONE, keepdims=True)
    centred = resid - mean
    inv_std = lax.rsqrt(jnp.mean(centred * centred, axis=-ONE, keepdims=True) + LN_EPS)
    normed = centred * inv_std
    return (normed * gain + shift).astype(BF16), normed, inv_std


def norm_rows_bwd(d_out, normed, inv_std, gain):
    d_norm = d_out * gain
    return inv_std * (d_norm - jnp.mean(d_norm, axis=-ONE, keepdims=True) - normed * jnp.mean(d_norm * normed, axis=-ONE, keepdims=True))


def col_sum(values):
    return jnp.sum(values, axis=ZERO, keepdims=True)


def lane_row(head, dtype=BF16):
    lane = lax.broadcasted_iota(jnp.int32, (ONE, PAIR), ONE)
    return jnp.where((lane >= HEAD_DIM * head) & (lane < HEAD_DIM * (head + ONE)), 1.0, 0.0).astype(dtype)


def spare_lane(head):
    lane = lax.broadcasted_iota(jnp.int32, (ONE, PAIR), ONE)
    return jnp.where(lane == HEAD_DIM * (ONE - head), 1.0, 0.0)


def mask_fill(n_rows, n_valid):
    row = lax.broadcasted_iota(jnp.int32, (n_rows, PAIR), ZERO)
    return jnp.where(row >= n_valid, MASK_FILL, 0.0)


def head_masks(pair_q, pair_k, head, fill):
    q_f = pair_q * lane_row(head) + spare_lane(head).astype(BF16)
    k_f = pair_k * lane_row(head) + (fill * spare_lane(head)).astype(BF16)
    return q_f, k_f


def half_only(pair, head):
    return pair * lane_row(head)


def join_halves(first, second):
    lane = lax.broadcasted_iota(jnp.int32, first.shape, ONE)
    return jnp.where(lane < HEAD_DIM, first, second)


def score_blocks(n_heads, n_q, n_k, causal, step):
    if not causal:
        return [(head, ZERO, n_q, n_k) for head in range(n_heads)]
    return [(head, first, step, first + step) for head in range(n_heads) for first in range(ZERO, n_q, step)]


def scores_t(q_f, k_f, causal, first):
    s_t = dot_nt(k_f, q_f)
    if causal:
        key_i = lax.broadcasted_iota(jnp.int32, s_t.shape, ZERO)
        qry_i = lax.broadcasted_iota(jnp.int32, s_t.shape, ONE) + first
        s_t = jnp.where(key_i <= qry_i, s_t, MASK_FILL)
    return s_t


def pair_of(group, head):
    return group[:, head // TWO * PAIR:(head // TWO + ONE) * PAIR]


def masked_pairs(q_g, k_g, n_valid):
    fill = mask_fill(k_g.shape[ZERO], n_valid)
    cache = {}

    def get(head):
        if head not in cache:
            cache[head] = head_masks(pair_of(q_g, head), pair_of(k_g, head), head % TWO, fill)
        return cache[head]

    return get


def stack_heads(parts, n_heads):
    return jnp.concatenate([jnp.concatenate(parts[head], axis=ONE) for head in range(n_heads)], axis=ZERO)


def run_ahead(blocks, produce, transform, consume, delay):
    ahead = produce(blocks[ZERO])
    waiting = []
    for i, block in enumerate(blocks):
        now = ahead
        if i + ONE < len(blocks):
            ahead = produce(blocks[i + ONE])
        waiting.append((block, transform(block, now)))
        if len(waiting) > delay:
            consume(*waiting.pop(ZERO))
    for item in waiting:
        consume(*item)


def attend_group(q_g, k_g, v_g, n_valid, causal, lse_ref):
    n_heads = GROUP // HEAD_DIM
    o_parts = [[] for _ in range(n_heads)]
    v_t = v_g.T
    masked = masked_pairs(q_g, k_g, n_valid)

    def produce(block):
        head, first, n_q, n_k = block
        q_f, k_f = masked(head)
        return scores_t(q_f[first:first + n_q], k_f[:n_k], causal, first)

    def transform(block, s_t):
        head, first, n_q, n_k = block
        top = jnp.max(s_t, axis=ZERO, keepdims=True)
        e_t = jnp.exp(s_t - top)
        total = jnp.sum(e_t, axis=ZERO, keepdims=True)
        lse_ref[ZERO, ZERO, head // TWO, head % TWO:head % TWO + ONE, first:first + n_q] = top + jnp.log(total)
        return (e_t * (1.0 / total)).astype(BF16)

    def consume(block, p_t):
        head, first, n_q, n_k = block
        o_parts[head].append(dot(v_t[HEAD_DIM * head:HEAD_DIM * (head + ONE), :n_k], p_t))

    run_ahead(score_blocks(n_heads, q_g.shape[ZERO], k_g.shape[ZERO], causal, 128), produce, transform, consume, TWO)
    return stack_heads(o_parts, n_heads).T.astype(BF16)


def attend_group_bwd(d_o, q_g, k_g, v_g, n_valid, causal, lse_ref):
    n_heads = q_g.shape[ONE] // HEAD_DIM
    k_t = k_g.T
    dq_t, dk_h, dv_h = [[] for _ in range(n_heads)], [None] * n_heads, [None] * n_heads
    masked = masked_pairs(q_g, k_g, n_valid)
    v_half = {}

    def produce(block):
        head, first, n_q, n_k = block
        q_f, k_f = masked(head)
        if head not in v_half:
            v_half[head] = half_only(pair_of(v_g, head), head % TWO)
        rows = slice(first, first + n_q)
        return scores_t(q_f[rows], k_f[:n_k], causal, first), dot_nt(v_half[head][:n_k], pair_of(d_o, head)[rows])

    def transform(block, products):
        head, first, n_q, n_k = block
        s_t, dp_t = products
        p_t = jnp.exp(s_t - lse_ref[head // TWO, head % TWO:head % TWO + ONE, first:first + n_q])
        weighted = p_t * dp_t
        return p_t.astype(BF16), (weighted - p_t * jnp.sum(weighted, axis=ZERO, keepdims=True)).astype(BF16)

    def grow(old, new):
        if old is None:
            return new
        n_old = old.shape[ZERO]
        return old + new if n_old == new.shape[ZERO] else jnp.concatenate([old + new[:n_old], new[n_old:]], axis=ZERO)

    def consume(block, operands):
        head, first, n_q, n_k = block
        p_b, ds_t = operands
        rows = slice(first, first + n_q)
        dv_h[head] = grow(dv_h[head], dot(p_b, pair_of(d_o, head)[rows]))
        dk_h[head] = grow(dk_h[head], dot(ds_t, pair_of(q_g, head)[rows]))
        dq_t[head].append(dot(k_t[HEAD_DIM * head:HEAD_DIM * (head + ONE), :n_k], ds_t))

    run_ahead(score_blocks(n_heads, q_g.shape[ZERO], k_g.shape[ZERO], causal, 256), produce, transform, consume, ZERO)
    join = lambda parts: jnp.concatenate([join_halves(parts[h], parts[h + ONE]) for h in range(ZERO, n_heads, TWO)], axis=ONE)
    return stack_heads(dq_t, n_heads).T * 0.125, join(dk_h), join(dv_h)


def attn_fwd_kernel(causal, slots, guest, lens_ref, x_ref, kv_ref, wq_ref, wk_ref, wv_ref, w_all, bias_ref, rows_ref,
                    q_ref, k_ref, v_ref, o_ref, lse_ref, h_ref, normed_ref, inv_ref, o_all, wo_v, load_sem):
    q_row, k_row, v_row, o_row, gain_row, o_mat = slots
    sample, group = pl.program_id(ZERO), pl.program_id(ONE)
    d_model = wo_v.shape[ZERO]
    fetch = pltpu.make_async_copy(w_all.at[pl.ds(o_mat * d_model, d_model), :], wo_v, load_sem)

    @pl.when((sample == ZERO) & (group == ZERO))
    def _():
        fetch.start()

    turn = sample * pl.num_programs(ONE) + group
    if guest is not None:
        for where, steps in ((ZERO, (lambda: meet_neighbours(guest.place), guest.begin)), (THREE, (guest.pass_on,)), (5, (guest.complete,))):
            @pl.when(turn == where)
            def _():
                for step in steps:
                    step()

    x_b, kv_b = x_ref[ALL], kv_ref[ALL]
    q_g = ((dot(x_b, wq_ref[ALL]) + bias_ref[q_row:q_row + ONE, :]) * 0.125).astype(BF16)
    k_g = (dot(kv_b, wk_ref[ALL]) + bias_ref[k_row:k_row + ONE, :]).astype(BF16)
    v_g = (dot(kv_b, wv_ref[ALL]) + bias_ref[v_row:v_row + ONE, :]).astype(BF16)
    q_ref[ALL], k_ref[ALL], v_ref[ALL] = q_g, k_g, v_g
    o_g = attend_group(q_g, k_g, v_g, lens_ref[sample], causal, lse_ref)
    o_ref[ALL] = o_g
    o_all[:, pl.ds(pl.multiple_of(group * GROUP, GROUP), GROUP)] = o_g

    @pl.when((sample == ZERO) & (group == pl.num_programs(ONE) - ONE))
    def _():
        fetch.wait()

    @pl.when(group == pl.num_programs(ONE) - ONE)
    def _():
        resid = x_ref[ALL].astype(F32) + dot(o_all[ALL], wo_v[ALL]) + rows_ref[o_row:o_row + ONE, :]
        h_out, normed, inv_std = norm_rows(resid, rows_ref[gain_row:gain_row + ONE, :], rows_ref[gain_row + ONE:gain_row + TWO, :])
        h_ref[ALL], normed_ref[ALL], inv_ref[ALL] = h_out, normed, inv_std

    if guest is not None:
        @pl.when(turn == pl.num_programs(ZERO) * pl.num_programs(ONE) - ONE)
        def _():
            guest.end()


def attn_forward(x, kv, lens, attn_full, bias_rows, mats, slots, causal, planes=None, full_rows=None):
    d_model = x.shape[-ONE]
    n_batch = lens.shape[ZERO]
    n_q, n_k = x.shape[ZERO] // n_batch, kv.shape[ZERO] // n_batch
    n_groups = d_model // GROUP
    col = lambda mat: pl.BlockSpec((d_model, GROUP), lambda b, g: (mat, g))
    q_blk = pl.BlockSpec((n_q, GROUP), lambda b, g: (b, g))
    k_blk = pl.BlockSpec((n_k, GROUP), lambda b, g: (b, g))
    tok = lambda n: pl.BlockSpec((n, d_model), lambda b, g: (b, ZERO))
    n_heads_g = GROUP // HEAD_DIM
    out_shape = (
        jax.ShapeDtypeStruct(x.shape, BF16), jax.ShapeDtypeStruct(kv.shape, BF16), jax.ShapeDtypeStruct(kv.shape, BF16),
        jax.ShapeDtypeStruct(x.shape, BF16), jax.ShapeDtypeStruct((n_batch, n_groups, n_heads_g // TWO, TWO, n_q), F32),
        jax.ShapeDtypeStruct(x.shape, BF16), jax.ShapeDtypeStruct(x.shape, F32), jax.ShapeDtypeStruct((x.shape[ZERO], ONE), F32))
    kernel = functools.partial(attn_fwd_kernel, causal, slots + (mats[THREE],))
    in_specs = [pl.BlockSpec(memory_space=pltpu.SMEM), tok(n_q), tok(n_k), col(mats[ZERO]), col(mats[ONE]), col(mats[TWO]), pl.BlockSpec(memory_space=pl.ANY),
                pl.BlockSpec((bias_rows.shape[ZERO], GROUP), lambda b, g: (ZERO, g)), pl.BlockSpec(bias_rows.shape, lambda b, g: (ZERO, ZERO))]
    out_specs = [q_blk, k_blk, k_blk, q_blk, pl.BlockSpec((ONE, ONE, n_heads_g // TWO, TWO, n_q), lambda b, g: (b, g, ZERO, ZERO, ZERO)),
                 tok(n_q), tok(n_q), pl.BlockSpec((n_q, ONE), lambda b, g: (b, ZERO))]
    scratch = [pltpu.VMEM((n_q, d_model), BF16), pltpu.VMEM((d_model, d_model), BF16), pltpu.SemaphoreType.DMA]
    args = [lens, x, kv, attn_full, attn_full, attn_full, attn_full, bias_rows, bias_rows]
    params = dict(vmem_limit_bytes=VMEM_BYTES, dimension_semantics=('arbitrary', 'arbitrary'))
    if planes is None:
        body = functools.partial(kernel, None)
    else:
        n_in, n_out, n_own = len(args), len(out_specs), len(scratch)

        def body(*refs):
            ins, held, outs, whole, rest = refs[:n_in], refs[n_in], refs[n_in + ONE:n_in + ONE + n_out], refs[n_in + ONE + n_out], refs[n_in + TWO + n_out:]
            kernel(LastPhase(held, whole, *rest[n_own:]), *ins, *outs, *rest[:n_own])

        in_specs.append(pl.BlockSpec(memory_space=pltpu.VMEM))
        args.append(planes)
        out_specs.append(pl.BlockSpec(memory_space=pl.ANY))
        out_shape += (jax.ShapeDtypeStruct((SIDE, SIDE, SIDE, full_rows // SIDE ** THREE, d_model), BF16),)
        scratch += LastPhase.scratch_shapes(planes)
        params |= dict(collective_id=5, has_side_effects=True)
    return pl.pallas_call(
        body, grid=(n_batch, n_groups), in_specs=in_specs, out_specs=out_specs, out_shape=out_shape, scratch_shapes=scratch,
        compiler_params=pltpu.CompilerParams(**params),
        cost_estimate=pl.CostEstimate(flops=TWO * d_model * d_model * (TWO * x.shape[ZERO] + TWO * kv.shape[ZERO]) + 16 * x.shape[ZERO] * n_k * d_model, bytes_accessed=20 * x.shape[ZERO] * d_model, transcendentals=ZERO),
        name='attn_fwd',
    )(*args)


def attn_bwd_kernel(causal, gain_row, mats, guest, lens_ref, dres_ref, wo_ref, w_all, q_ref, k_ref, v_ref, lse_ref,
                    rows_ref, normed_ref, inv_ref, lhs_refs, rows_out, dres_out, sums_ref, tail_ref, grads_ref,
                    rhs_q, rhs_k, lhs_q, lhs_k, do_v, w_v, grad_v, load_sem, store_sem):
    sample, group = pl.program_id(ZERO), pl.program_id(ONE)
    d_model = wo_ref.shape[ONE]
    n_q, n_k = q_ref.shape[ZERO], k_ref.shape[ZERO]
    last = pl.num_programs(ONE) - ONE
    fetches = [] if causal else [pltpu.make_async_copy(w_all.at[pl.ds(mats[ZERO] * d_model, d_model), :], w_v, load_sem.at[ZERO])]
    hand_on = pltpu.make_async_copy(rhs_q.at[pl.ds(ZERO, THREE)] if causal else rhs_k, rows_out, load_sem.at[ONE])
    dk_all, dv_all = (rhs_q.at[ONE], rhs_q.at[TWO]) if causal else (rhs_k.at[ZERO], rhs_k.at[ONE])
    d_all, dres_all = rhs_q.at[ZERO], rhs_q.at[THREE if causal else ONE]
    places = (lhs_q.at[ZERO], lhs_q.at[ONE]) if causal else (lhs_q.at[ZERO], lhs_k, lhs_q.at[ZERO])
    lhs_fetch = lambda i: pltpu.make_async_copy(lhs_refs[i], places[i], load_sem.at[THREE + i])
    store = lambda buf, mat: pltpu.make_async_copy(grad_v.at[buf], grads_ref.at[pl.ds(pl.multiple_of(mat * d_model, d_model), d_model), :], store_sem.at[buf])

    @pl.when((sample == ZERO) & (group == ZERO))
    def _():
        for fetch in fetches + [lhs_fetch(ZERO), lhs_fetch(ONE)]:
            fetch.start()

    turn = sample * pl.num_programs(ONE) + group
    q_rows = pl.ds(pl.multiple_of(sample * n_q, n_q), n_q)
    k_rows = pl.ds(pl.multiple_of(sample * n_k, n_k), n_k)
    d_o = dot_nt(dres_ref[ALL].astype(BF16), wo_ref[ALL]).astype(BF16)

    def keep(found, first, width):
        here = pl.ds(first, width)
        cols = pl.ds(pl.multiple_of(group * GROUP + first, PAIR), width)
        for i, (full, rows, value) in enumerate(zip((d_all, dk_all, dv_all), (q_rows, k_rows, k_rows), found)):
            sums_ref[ZERO, i:i + ONE, here] = col_sum(value)
            full[rows, cols] = value.astype(BF16)

    if causal:
        keep(attend_group_bwd(d_o, q_ref[ALL], k_ref[ALL], v_ref[ALL], lens_ref[sample], causal, lse_ref.at[ZERO, ZERO]), ZERO, GROUP)
    else:
        do_v[ALL] = d_o

        def one_pair(pair, _):
            guest(ZERO, TWO * turn + pair)
            first = pl.multiple_of(pair * PAIR, PAIR)
            here = pl.ds(first, PAIR)
            keep(attend_group_bwd(do_v[:, here], q_ref[:, here], k_ref[:, here], v_ref[:, here], lens_ref[sample], causal, lse_ref.at[ZERO, ZERO, pl.ds(pair, ONE)]), first, PAIR)
            return ZERO

        lax.fori_loop(ZERO, GROUP // PAIR, one_pair, ZERO)

    @pl.when(group == ZERO)
    def _():
        dres_all[q_rows, :] = dres_ref[ALL].astype(BF16)

    guest(THREE, turn)
    if causal:
        tail_ref[ALL] = jnp.zeros_like(tail_ref)
    else:
        @pl.when((sample == ZERO) & (group == last))
        def _():
            for fetch in fetches:
                fetch.wait()

        @pl.when(group == last)
        def _():
            d_h = dres_ref[ALL] + dot_nt(d_all[q_rows, :], w_v[ALL])
            normed = normed_ref[ALL]
            d_resid = norm_rows_bwd(d_h, normed, inv_ref[ALL], rows_ref[gain_row:gain_row + ONE, :])
            dres_out[ALL] = d_resid
            tail_ref[ZERO, ZERO:ONE, :] = col_sum(d_resid)
            tail_ref[ZERO, ONE:TWO, :] = col_sum(d_h * normed)
            tail_ref[ZERO, TWO:THREE, :] = col_sum(d_h)

    @pl.when(turn == pl.num_programs(ZERO) * pl.num_programs(ONE) - ONE)
    def _():
        hand_on.start()
        guest(TWO, 12)
        lhs_fetch(ZERO).wait()
        if causal:
            lhs_fetch(ONE).wait()

            def square(i, _):
                @pl.when(i >= TWO)
                def _():
                    store(i % TWO, mats[ZERO]).wait()

                grad_v[i % TWO] = dot_tn(lhs_q[i // THREE], rhs_q[i])
                store(i % TWO, mats[ZERO] + i).start()
                return ZERO

            lax.fori_loop(ZERO, 4, square, ZERO)
        else:
            def square_q(i, _):
                @pl.when(i == ONE)
                def _():
                    lhs_fetch(TWO).start()
                    lhs_fetch(TWO).wait()

                grad_v[i] = dot_tn(lhs_q[ZERO], rhs_q[i])
                store(i, mats[ZERO] + THREE * i).start()
                return ZERO

            def square_k(i, _):
                @pl.when(i == ONE)
                def _():
                    guest(TWO, 14)

                store(i, mats[ONE]).wait()
                grad_v[i] = dot_tn(lhs_k[ALL], rhs_k[i])
                store(i, mats[ONE] + i).start()
                return ZERO

            lax.fori_loop(ZERO, TWO, square_q, ZERO)
            guest(TWO, 13)
            lhs_fetch(ONE).wait()
            lax.fori_loop(ZERO, TWO, square_k, ZERO)
            guest(TWO, 15)
        for buf in range(TWO):
            store(buf, mats[ZERO]).wait()
        hand_on.wait()


def scatter_guest(scatter, plan, parity, position):
    steps = dict(end=scatter.end) | {('relay', p): functools.partial(scatter.relay, p) for p in range(THREE)}
    steps |= {('settle', p): functools.partial(scatter.settle, p) for p in range(THREE)} | {turn: functools.partial(scatter.absorb, turn) for turn in range(SIDE)}
    if parity == TWO:
        for name in plan.get(position, ()):
            steps[name]()
        return
    if parity == THREE:
        @pl.when(position == 5)
        def _():
            for name in plan['late']:
                steps[name]()
        return
    if parity == ZERO:
        @pl.when(position == ZERO)
        def _():
            meet_neighbours(scatter.place)
            scatter.begin()
    for where, names in plan.items():
        if where != 'late' and where < 12:
            @pl.when(position == where)
            def _():
                for name in names:
                    steps[name]()


def no_guest(parity, position):
    pass


def attn_backward(dres, q, k, v, lse, lens, attn_full, bias_rows, mats, causal, lhs_list, g_rows=None, scale=None, gain_row=ZERO, normed=None, inv_std=None, grads=None):
    d_model = q.shape[-ONE]
    n_batch = lens.shape[ZERO]
    n_q, n_k = q.shape[ZERO] // n_batch, k.shape[ZERO] // n_batch
    n_groups = d_model // GROUP
    row = lambda mat: pl.BlockSpec((GROUP, d_model), lambda b, g: (mat * n_groups + g, ZERO))
    q_blk = pl.BlockSpec((n_q, GROUP), lambda b, g: (b, g))
    k_blk = pl.BlockSpec((n_k, GROUP), lambda b, g: (b, g))
    tok = lambda n: pl.BlockSpec((n, d_model), lambda b, g: (b, ZERO))
    n_heads_g = GROUP // HEAD_DIM
    anywhere = pl.BlockSpec(memory_space=pl.ANY)
    in_specs = [pl.BlockSpec(memory_space=pltpu.SMEM), tok(n_q), row(mats[THREE]), anywhere, q_blk, k_blk, k_blk,
                pl.BlockSpec((ONE, ONE, n_heads_g // TWO, TWO, n_q), lambda b, g: (b, g, ZERO, ZERO, ZERO)), pl.BlockSpec(bias_rows.shape, lambda b, g: (ZERO, ZERO))]
    args = [lens, dres, attn_full, attn_full, q, k, v, lse, bias_rows]
    tail_shape = jax.ShapeDtypeStruct((n_batch, 8, d_model), F32)
    out_shape = [jax.ShapeDtypeStruct((THREE,) + q.shape if causal else (TWO,) + k.shape, BF16)]
    out_specs = [anywhere]
    if not causal:
        late = dict(pipeline_mode=pl.Buffered(ONE))
        in_specs += [pl.BlockSpec((n_q, d_model), lambda b, g: (b, ZERO), **late), pl.BlockSpec((n_q, ONE), lambda b, g: (b, ZERO), **late)]
        args += [normed, inv_std]
        out_shape.append(jax.ShapeDtypeStruct(q.shape, F32))
        out_specs.append(tok(n_q))
    n_lhs_at = len(args)
    args += list(lhs_list)
    in_specs += [anywhere] * len(lhs_list)
    out_shape += [tail_shape, tail_shape, jax.ShapeDtypeStruct(attn_full.shape, F32)]
    out_specs += [pl.BlockSpec((ONE, 8, GROUP), lambda b, g: (b, ZERO, g)), pl.BlockSpec((ONE, 8, d_model), lambda b, g: (b, ZERO, ZERO)), anywhere]
    held = lambda count, n: pltpu.VMEM((count, n_batch * n, d_model), BF16)
    own = [held(4, n_q), held(TWO, n_q)] if causal else [held(TWO, n_q), held(TWO, n_k), held(ONE, n_q), pltpu.VMEM((n_batch * n_k, d_model), BF16)]
    own += [] if causal else [pltpu.VMEM((n_q, GROUP), BF16)]
    own += [] if causal else [pltpu.VMEM((d_model, d_model), BF16)]
    own += [pltpu.VMEM((TWO, d_model, d_model), F32), pltpu.SemaphoreType.DMA((6,)), pltpu.SemaphoreType.DMA((TWO,))]
    kernel = functools.partial(attn_bwd_kernel, causal, gain_row, mats)
    params = dict(vmem_limit_bytes=VMEM_BYTES, dimension_semantics=('arbitrary', 'arbitrary'))
    aliases = {}
    if causal:
        args.append(grads)
        in_specs.append(anywhere)
        aliases = {len(args) - ONE: len(out_shape) - ONE}
    else:
        args.append(as_torus(g_rows))
        in_specs.append(anywhere)
        n_rows = args[-ONE].shape[THREE]
        out_shape.append(jax.ShapeDtypeStruct((n_rows, d_model), F32))
        out_specs.append(anywhere)
        params |= dict(collective_id=THREE, has_side_effects=True, vmem_limit_bytes=67043328)
    scratch = own + ([] if causal else Scatter.scratch_shapes([n_rows]))
    n_in, n_out, n_own = len(args), len(out_shape), len(own)

    def body(*refs):
        ins, outs, rest = refs[:n_in], refs[n_in:n_in + n_out], refs[n_in + n_out:]
        lhs_refs, mine = ins[n_lhs_at:-ONE], rest[:n_own]
        if causal:
            rows_out, sums, tail, grads_ref = outs
            kernel(no_guest, *ins[:n_lhs_at], None, None, lhs_refs, rows_out, None, sums, tail, grads_ref, mine[ZERO], None, mine[ONE], None, None, None, *mine[TWO:])
        else:
            rows_out, dres_out, sums, tail, grads_ref, total = outs
            scatter = Scatter(scale, [(ins[-ONE], ZERO, n_rows)], [total], rest[n_own:])
            kernel(functools.partial(scatter_guest, scatter, CROSS_PLAN), *ins[:n_lhs_at], lhs_refs, rows_out, dres_out, sums, tail, grads_ref, *mine)

    return pl.pallas_call(
        body, grid=(n_batch, n_groups), in_specs=in_specs, out_specs=out_specs, out_shape=out_shape, scratch_shapes=scratch, input_output_aliases=aliases,
        compiler_params=pltpu.CompilerParams(**params),
        cost_estimate=pl.CostEstimate(flops=TWO * d_model * d_model * (TWO * q.shape[ZERO] + TWO * k.shape[ZERO]) + 40 * q.shape[ZERO] * n_k * d_model, bytes_accessed=20 * q.shape[ZERO] * d_model, transcendentals=ZERO),
        name='attn_bwd',
    )(*args)


def ffn_kernel(n_blocks, h_ref, dy_ref, up_ref, down_ref, rows_ref, bias_ref, normed_ref, inv_ref,
               y_ref, grad_ref, dres2_ref, tail_ref, upsum_ref, left_all, right_all):
    step = pl.program_id(ZERO)
    block, d_model = h_ref.shape
    n_square = left_all.shape[TWO] // d_model

    @pl.when(step < n_blocks)
    def _():
        rows = pl.ds(pl.multiple_of(step * block, block), block)
        h_b = h_ref[ALL]
        right_all[ZERO, rows, :] = h_b
        up = dot_nt(h_b, up_ref[ALL]) + bias_ref[ALL]
        cdf = 0.5 * (1.0 + lax.erf(up * 0.7071067811865476))
        gelu = (up * cdf).astype(BF16)
        slope = cdf + up * (0.3989422804014327 * jnp.exp(-0.5 * up * up))
        left_all[ONE, rows, :] = gelu
        resid = h_b.astype(F32) + dot(gelu, down_ref[ALL]) + rows_ref[8:9, :]
        y_b, normed3, inv3 = norm_rows(resid, rows_ref[13:14, :], rows_ref[14:15, :])
        y_ref[ALL] = y_b
        dy = dy_ref[ALL].astype(F32)
        d_res3 = norm_rows_bwd(dy, normed3, inv3, rows_ref[13:14, :])
        d_res3_b = d_res3.astype(BF16)
        right_all[ONE, rows, :] = d_res3_b
        d_up = dot_nt(d_res3_b, down_ref[ALL]) * slope
        d_up_b = d_up.astype(BF16)
        left_all[ZERO, rows, :] = d_up_b
        d_h2 = d_res3 + dot(d_up_b, up_ref[ALL])
        normed2 = normed_ref[ALL]
        d_res2 = norm_rows_bwd(d_h2, normed2, inv_ref[ALL], rows_ref[11:12, :])
        dres2_ref[ALL] = d_res2
        tail = jnp.concatenate([col_sum(d_res2), col_sum(d_res3), col_sum(d_h2 * normed2), col_sum(d_h2), col_sum(dy * normed3), col_sum(dy),
                                jnp.zeros((TWO, dy.shape[ONE]), F32)], axis=ZERO)
        up_sum = col_sum(d_up)

        @pl.when(step == ZERO)
        def _():
            tail_ref[ALL] = tail
            upsum_ref[ALL] = up_sum

        @pl.when(step > ZERO)
        def _():
            tail_ref[ALL] += tail
            upsum_ref[ALL] += up_sum

    square = step - n_blocks
    cols = pl.ds(pl.multiple_of(lax.rem(square + TWO * n_square, n_square) * d_model, d_model), d_model)

    @pl.when(square >= ZERO)
    def _():
        which = square // n_square
        grad_ref[ALL] = dot_tn(left_all[which, :, cols], right_all[which])


def ffn_both(h2, dy, ffn_full, bias_rows, up_bias, normed2, inv2, block=256):
    n_tok, d_model = h2.shape
    ffn_dim = ffn_full.shape[ZERO] // TWO
    n_blocks = n_tok // block
    n_steps = n_blocks + ffn_full.shape[ZERO] // d_model
    at = lambda i: jnp.minimum(i, n_blocks - ONE)
    tok = pl.BlockSpec((block, d_model), lambda i: (at(i), ZERO))
    once = lambda shape, idx: pl.BlockSpec(shape, lambda i: idx, pipeline_mode=pl.Buffered(ONE))
    return pl.pallas_call(
        functools.partial(ffn_kernel, n_blocks), grid=(n_steps,),
        in_specs=[tok, tok, once((ffn_dim, d_model), (ZERO, ZERO)), once((ffn_dim, d_model), (ONE, ZERO)), once(bias_rows.shape, (ZERO, ZERO)), once((ONE, ffn_dim), (ZERO, ZERO)),
                  tok, pl.BlockSpec((block, ONE), lambda i: (at(i), ZERO))],
        out_specs=[tok, pl.BlockSpec((d_model, d_model), lambda i: (jnp.maximum(i - n_blocks, ZERO), ZERO)), tok, pl.BlockSpec((8, d_model), lambda i: (ZERO, ZERO)), pl.BlockSpec((ONE, ffn_dim), lambda i: (ZERO, ZERO))],
        out_shape=[jax.ShapeDtypeStruct(h2.shape, BF16), jax.ShapeDtypeStruct(ffn_full.shape, F32), jax.ShapeDtypeStruct(h2.shape, F32),
                   jax.ShapeDtypeStruct((8, d_model), F32), jax.ShapeDtypeStruct((ONE, ffn_dim), F32)],
        scratch_shapes=[pltpu.VMEM((TWO, n_tok, ffn_dim), BF16), pltpu.VMEM((TWO, n_tok, d_model), BF16)],
        compiler_params=pltpu.CompilerParams(vmem_limit_bytes=VMEM_BYTES, dimension_semantics=('arbitrary',)),
        cost_estimate=pl.CostEstimate(flops=12 * n_tok * d_model * ffn_dim, bytes_accessed=30 * n_tok * d_model, transcendentals=ZERO),
        name='ffn_both',
    )(h2, dy, ffn_full, ffn_full, bias_rows, up_bias, normed2, inv2)


CROSS_PLAN = {ONE: (ZERO,), THREE: (ONE, TWO), 5: (('relay', ZERO),), 6: (THREE,), 9: (('settle', ZERO),), 11: (('relay', ONE),), 'late': (), 12: (('settle', ONE),), 13: (('relay', TWO),), 14: (('settle', TWO),), 15: ('end',)}


def solution(mesh):
    n_fsdp = mesh.shape['fsdp']
    n_dp = mesh.shape['dp']
    batch_axes = ('dp', 'fsdp')
    act_spec = P(batch_axes, None, None)
    len_spec = P(batch_axes)
    row_spec = P('fsdp', None)
    vec_spec = P('fsdp')

    def device_step(dec_in, enc_out, src_lens, tgt_lens, y_cot, attn_w, ffn_w, vec_params):
        d_model, n_vec = dec_in.shape[TWO], vec_params.shape[ZERO]
        scale = 1.0 / (dec_in.shape[ZERO] * dec_in.shape[ONE] * n_fsdp * n_dp)
        x, enc, dy = (a.reshape(-ONE, d_model) for a in (dec_in, enc_out, y_cot))
        vec_rows = jnp.pad(vec_params.astype(F32), (ZERO, 16 * LANES - n_vec)).reshape(16, LANES)
        attn_tiles, planes, vec_tiles = gather_params(attn_w, ffn_w, vec_rows)
        attn_full = attn_tiles.reshape(-ONE, d_model)
        vec_f = vec_tiles.reshape(n_fsdp, 16, LANES)[:, :TWO].reshape(n_fsdp, TWO * LANES)[:, :n_vec].reshape(-ONE)
        bias_rows = jnp.pad(vec_f[:15 * d_model].reshape(15, d_model), ((ZERO, ONE), (ZERO, ZERO)))
        up_bias = vec_f[15 * d_model:].reshape(ONE, -ONE)
        q1, k1, v1, o1, lse1, h1, normed1, inv1 = attn_forward(x, x, tgt_lens, attn_full, bias_rows, (ZERO, ONE, TWO, THREE), (ZERO, ONE, TWO, THREE, 9), True)
        q2, k2, v2, o2, lse2, h2, normed2, inv2, ffn_tiles = attn_forward(h1, enc, src_lens, attn_full, bias_rows, (4, 5, 6, 7), (4, 5, 6, 7, 11), False, planes, ffn_w.shape[ZERO] * n_fsdp)
        ffn_full = ffn_tiles.reshape(-ONE, d_model)
        y, g_ffn, d_res2, ffn_tail, up_sum = ffn_both(h2, dy, ffn_full, bias_rows, up_bias, normed2, inv2)
        d_cross, d_res1, sums2, tail2, grads, ffn_out = attn_backward(d_res2, q2, k2, v2, lse2, src_lens, attn_full, bias_rows, (4, 5, 6, 7), False, (h1, enc, o2), g_ffn, scale, 9, normed1, inv1)
        d_self, sums1, _, grads = attn_backward(d_res1, q1, k1, v1, lse1, tgt_lens, attn_full, bias_rows, (ZERO, ONE, TWO, THREE), True, (x, o1), grads=grads)
        s1, s2, t2 = jnp.sum(sums1, axis=ZERO), jnp.sum(sums2, axis=ZERO), jnp.sum(tail2, axis=ZERO)
        g_vec = jnp.concatenate([s1[ZERO:THREE].reshape(-ONE), t2[ZERO], s2[ZERO:THREE].reshape(-ONE), ffn_tail[ZERO], ffn_tail[ONE], t2[ONE], t2[TWO], ffn_tail[TWO], ffn_tail[THREE], ffn_tail[4], ffn_tail[5], up_sum[ZERO]])
        g_rows = jnp.pad(g_vec.reshape(n_fsdp, ONE, n_vec), ((ZERO, ZERO), (ZERO, 7), (ZERO, TWO * LANES - n_vec))).reshape(n_fsdp * 8, -ONE)
        attn_out, vec_out, d_x, d_enc = scatter_grads(grads, g_rows, scale, attn_full, (ZERO, ONE, TWO, 5, 6), d_res1, d_self, d_cross)
        return y.reshape(dec_in.shape), d_x.reshape(dec_in.shape), d_enc.reshape(enc_out.shape), attn_out, ffn_out, vec_out[ZERO, :n_vec]

    return jax.shard_map(device_step, mesh=mesh, in_specs=(act_spec, act_spec, len_spec, len_spec, act_spec, row_spec, row_spec, vec_spec), out_specs=(act_spec, act_spec, act_spec, row_spec, row_spec, vec_spec), check_vma=False)
```
